8 devices in a mesh: ep: 2 (over z, y), dp: 4 (over x, core).
Axes of the slice: x: 2, y: 2, z: 1, core: 2. Of those that a mesh axis runs over, the one named last changes fastest.
Arguments:
- tokens: bfloat16 [8192, 448], P(('dp', 'ep'))
- d_out: bfloat16 [8192, 448], P(('dp', 'ep'))
- expert_ids: int32 [2, 8192, 8], P(None, ('dp', 'ep'))
- gate_vals: float32 [2, 8192, 8], P(None, ('dp', 'ep'))
- w_mix: bfloat16 [2, 448, 448], replicated
- w_gate: bfloat16 [2, 64, 448, 320], P(None, 'ep')
- w_up: bfloat16 [2, 64, 448, 320], P(None, 'ep')
- w_down: bfloat16 [2, 64, 320, 448], P(None, 'ep')
Outputs:
- output 1: bfloat16 [8192, 448], P(('dp', 'ep'))
- output 2: bfloat16 [8192, 448], P(('dp', 'ep'))
- output 3: bfloat16 [2, 448, 448], replicated
- output 4: bfloat16 [2, 64, 448, 320], P(None, 'ep')
- output 5: bfloat16 [2, 64, 448, 320], P(None, 'ep')
- output 6: bfloat16 [2, 64, 320, 448], P(None, 'ep')
All inputs are finite; a program needn't handle non-finite values.
Results may differ from the reference program's by a relative error of at most 0.0171451.
Values are sent between devices in bfloat16 or wider.
A program may use at most 1 GiB of HBM per device.

```python
import jax
import jax.numpy as jnp

D = 448
FF = 320
EXPERTS = 64
TOP = 8
TOK = 1024
NDEV = 8
LAYERS = 2
CAP = 384
HOT = 8

N_TOK = TOK * NDEV
CAP_ALL = CAP * NDEV


def route_device(hot_mask, dev_key):
    key_rest, key_run, key_tok = jax.random.split(dev_key, 3)
    rest_copies = TOK * TOP - HOT * CAP
    base_count = rest_copies // (EXPERTS - HOT)
    extra_count = rest_copies % (EXPERTS - HOT)
    shuffled = jax.random.permutation(key_rest, EXPERTS)
    cold_sorted = 1 - hot_mask[shuffled]
    cold_rank = jnp.cumsum(cold_sorted) - 1
    bonus_sorted = cold_sorted * (cold_rank < extra_count).astype(jnp.int32)
    bonus = jnp.zeros((EXPERTS,), jnp.int32).at[shuffled].set(bonus_sorted)
    counts = jnp.where(hot_mask == 1, CAP, base_count + bonus)
    run_order = jax.random.permutation(key_run, EXPERTS)
    flat_ids = jnp.repeat(run_order, counts[run_order], total_repeat_length=TOK * TOP)
    table = flat_ids.reshape(TOP, TOK).T
    return table[jax.random.permutation(key_tok, TOK)]


def route_layer(layer_key):
    key_hot, key_dev = jax.random.split(layer_key)
    hot_ids = jax.random.permutation(key_hot, EXPERTS)[:HOT]
    hot_mask = jnp.zeros((EXPERTS,), jnp.int32).at[hot_ids].set(1)
    per_device = jax.vmap(route_device, in_axes=(None, 0))(hot_mask, jax.random.split(key_dev, NDEV))
    return per_device.reshape(N_TOK, TOP)


def setup_inputs(seed: int = 0) -> dict:
    keys = jax.random.split(jax.random.key(seed), 8)
    tokens = jax.random.normal(keys[0], (N_TOK, D), jnp.float32).astype(jnp.bfloat16)
    d_out = jax.random.normal(keys[1], (N_TOK, D), jnp.float32).astype(jnp.bfloat16)
    expert_ids = jax.vmap(route_layer)(jax.random.split(keys[2], LAYERS))
    gate_vals = jax.random.uniform(keys[3], (LAYERS, N_TOK, TOP), jnp.float32, 0.5, 1.5) * TOP ** -0.5
    w_mix = (jax.random.normal(keys[4], (LAYERS, D, D), jnp.float32) * D ** -0.5).astype(jnp.bfloat16)
    w_gate = (jax.random.normal(keys[5], (LAYERS, EXPERTS, D, FF), jnp.float32) * D ** -0.5).astype(jnp.bfloat16)
    w_up = (jax.random.normal(keys[6], (LAYERS, EXPERTS, D, FF), jnp.float32) * D ** -0.5).astype(jnp.bfloat16)
    w_down = (jax.random.normal(keys[7], (LAYERS, EXPERTS, FF, D), jnp.float32) * FF ** -0.5).astype(jnp.bfloat16)
    return {'tokens': tokens, 'd_out': d_out, 'expert_ids': expert_ids, 'gate_vals': gate_vals,
            'w_mix': w_mix, 'w_gate': w_gate, 'w_up': w_up, 'w_down': w_down}


def silu_parts(pre_gate):
    sig_val = jax.nn.sigmoid(pre_gate)
    return pre_gate * sig_val, sig_val * (1.0 + pre_gate * (1.0 - sig_val))


def copy_slots(expert_ids):
    flat_ids = expert_ids.reshape(-1)
    sort_order = jnp.argsort(flat_ids, stable=True)
    sorted_ids = flat_ids[sort_order]
    counts = jnp.bincount(flat_ids, length=EXPERTS)
    starts = jnp.cumsum(counts) - counts
    rows_sorted = sorted_ids * CAP_ALL + jnp.arange(flat_ids.shape[0]) - starts[sorted_ids]
    return jnp.zeros_like(flat_ids).at[sort_order].set(rows_sorted)


def layer_forward(x_in, expert_ids, gate_vals, w_mix, w_gate, w_up, w_down):
    mixed = x_in.astype(jnp.float32) + jnp.dot(x_in, w_mix, preferred_element_type=jnp.float32)
    u_act = mixed.astype(jnp.bfloat16)
    copy_rows = copy_slots(expert_ids)
    copy_tok = jnp.arange(N_TOK * TOP) // TOP
    expert_in = jnp.zeros((EXPERTS * CAP_ALL, D), jnp.bfloat16).at[copy_rows].set(u_act[copy_tok])
    expert_in = expert_in.reshape(EXPERTS, CAP_ALL, D)
    expert_f = expert_in.astype(jnp.float32)
    pre_gate = jnp.einsum('ecd,edf->ecf', expert_f, w_gate.astype(jnp.float32))
    pre_up = jnp.einsum('ecd,edf->ecf', expert_f, w_up.astype(jnp.float32))
    act, _ = silu_parts(pre_gate)
    hidden = (act * pre_up).astype(jnp.bfloat16)
    expert_out = jnp.einsum('ecf,efd->ecd', hidden.astype(jnp.float32), w_down.astype(jnp.float32)).astype(jnp.bfloat16)
    out_copy = expert_out.reshape(EXPERTS * CAP_ALL, D)[copy_rows].reshape(N_TOK, TOP, D)
    y_out = u_act.astype(jnp.float32) + jnp.sum(gate_vals[:, :, None] * out_copy.astype(jnp.float32), axis=1)
    return y_out.astype(jnp.bfloat16), (x_in, copy_rows, expert_in, pre_gate, pre_up, hidden)


def layer_backward(saved, d_y, gate_vals, w_mix, w_gate, w_up, w_down):
    x_in, copy_rows, expert_in, pre_gate, pre_up, hidden = saved
    g_dy = (gate_vals[:, :, None] * d_y.astype(jnp.float32)[:, None, :]).astype(jnp.bfloat16).reshape(N_TOK * TOP, D)
    d_buf = jnp.zeros((EXPERTS * CAP_ALL, D), jnp.bfloat16).at[copy_rows].set(g_dy).reshape(EXPERTS, CAP_ALL, D)
    d_buf_f = d_buf.astype(jnp.float32)
    d_hidden = jnp.einsum('ecd,efd->ecf', d_buf_f, w_down.astype(jnp.float32))
    act, act_slope = silu_parts(pre_gate)
    d_pre_gate = (d_hidden * pre_up * act_slope).astype(jnp.bfloat16).astype(jnp.float32)
    d_pre_up = (d_hidden * act).astype(jnp.bfloat16).astype(jnp.float32)
    d_expert_in = (jnp.einsum('ecf,edf->ecd', d_pre_gate, w_gate.astype(jnp.float32))
                   + jnp.einsum('ecf,edf->ecd', d_pre_up, w_up.astype(jnp.float32))).astype(jnp.bfloat16)
    expert_f = expert_in.astype(jnp.float32)
    g_gate = jnp.einsum('ecd,ecf->edf', expert_f, d_pre_gate).astype(jnp.bfloat16)
    g_up = jnp.einsum('ecd,ecf->edf', expert_f, d_pre_up).astype(jnp.bfloat16)
    g_down = jnp.einsum('ecf,ecd->efd', hidden.astype(jnp.float32), d_buf_f).astype(jnp.bfloat16)
    d_copy = d_expert_in.reshape(EXPERTS * CAP_ALL, D)[copy_rows].reshape(N_TOK, TOP, D)
    d_u = (d_y.astype(jnp.float32) + jnp.sum(gate_vals[:, :, None] * d_copy.astype(jnp.float32), axis=1)).astype(jnp.bfloat16)
    g_mix = jnp.dot(x_in.T, d_u, preferred_element_type=jnp.float32).astype(jnp.bfloat16)
    d_x = (d_u.astype(jnp.float32) + jnp.dot(d_u, w_mix.T, preferred_element_type=jnp.float32)).astype(jnp.bfloat16)
    return d_x, (g_mix, g_gate, g_up, g_down)


def reference(tokens, d_out, expert_ids, gate_vals, w_mix, w_gate, w_up, w_down):
    layer_in = tokens
    saved_all = []
    for layer in range(LAYERS):
        layer_in, saved = layer_forward(layer_in, expert_ids[layer], gate_vals[layer], w_mix[layer],
                                        w_gate[layer], w_up[layer], w_down[layer])
        saved_all.append(saved)
    d_y = d_out
    grads = []
    for layer in reversed(range(LAYERS)):
        d_y, grad_set = layer_backward(saved_all[layer], d_y, gate_vals[layer], w_mix[layer],
                                       w_gate[layer], w_up[layer], w_down[layer])
        grads.insert(0, grad_set)
    return (layer_in, d_y,
            jnp.stack([entry[0] for entry in grads]),
            jnp.stack([entry[1] for entry in grads]),
            jnp.stack([entry[2] for entry in grads]),
            jnp.stack([entry[3] for entry in grads]))
```

```python
import functools

import jax
import jax.numpy as jnp
from jax import lax
from jax.experimental import pallas as pl
from jax.experimental.pallas import tpu as pltpu
from jax.sharding import Mesh, PartitionSpec as P

F32, BF16, I32 = jnp.float32, jnp.bfloat16, jnp.int32
ROWS = 384
GRP = 8
CAP_FACTOR = 3
LANES = 128
VMEM_LIMIT = 62 * 1024 * 1024


def cdiv(a, b):
    return (a + b - 1) // b


def local_lists(expert_ids, gate_vals, n_exp):
    n_layers, n_tok, top = expert_ids.shape
    n = n_tok * top
    flat = expert_ids.reshape(n_layers, n)
    gates = gate_vals.reshape(n_layers, n)
    step = 2 * n
    big = n_exp * step + n
    real = flat * step + jnp.arange(n, dtype=I32)[None]
    counts = jnp.sum((flat[:, :, None] == jnp.arange(n_exp, dtype=I32)).astype(I32), axis=1)
    pad = (-counts) % GRP
    k = jnp.arange(GRP - 1, dtype=I32)
    fill = jnp.where(k[None, None] < pad[:, :, None],
                     jnp.arange(n_exp, dtype=I32)[None, :, None] * step + n, big)
    tail = 128 - (n_exp * (GRP - 1)) % 128
    keys = jnp.concatenate([real, fill.reshape(n_layers, -1), jnp.full((n_layers, tail), big, I32)], 1)
    gts = jnp.pad(gates, ((0, 0), (0, keys.shape[1] - n)))
    keys, gts = lax.sort((keys, gts), dimension=1, num_keys=1)
    low = keys % step
    tok = jnp.where(low >= n, -1, low // top)
    return tok, gts, (counts + pad) // GRP


def half_tables(tok, gts, groups, experts, n_tok, max_groups):
    n_src, length = tok.shape
    dummy = n_src * n_tok
    idx = jnp.where(tok < 0, dummy, tok + jnp.arange(n_src, dtype=I32)[:, None] * n_tok) * 4
    starts = jnp.cumsum(groups, axis=1) - groups
    cnt = groups[:, experts].T
    start = starts[:, experts].T
    off = jnp.cumsum(cnt, axis=1) - cnt
    total = jnp.sum(cnt, axis=1)
    g = jnp.arange(max_groups, dtype=I32)
    pos = jnp.full((experts.shape[0], max_groups), length - GRP, I32)
    for s in range(n_src):
        rel = g[None] - off[:, s:s + 1]
        inside = (rel >= 0) & (rel < cnt[:, s:s + 1])
        pos = jnp.where(inside, s * length + (start[:, s:s + 1] + rel) * GRP, pos)
    per_tile = ROWS // GRP
    tiles = jnp.maximum(1, (total + per_tile - 1) // per_tile)
    ends = jnp.cumsum(tiles)
    n_tiles = ends[-1]
    most = experts.shape[0] * (max_groups // per_tile) + 2
    t = jnp.minimum(jnp.arange(most, dtype=I32), n_tiles - 1)
    slot = jnp.sum((t[:, None] >= ends[None]).astype(I32), axis=1)
    first = jnp.sum(jnp.where(jnp.arange(experts.shape[0])[None] == slot[:, None], (ends - tiles)[None], 0), axis=1)
    goff = slot * max_groups + (t - first) * per_tile
    bounds = jnp.concatenate([jnp.zeros((1,), I32), ends])
    return bounds, goff, pos.reshape(-1), idx.reshape(-1), gts.reshape(-1)


def expert_kernel(cfg, *refs):
    fwd, bwd, own, n_tok, d, ff = cfg
    refs = list(refs)
    take = lambda n: [refs.pop(0) for _ in range(n)]
    bound_ref, goff_ref, gbase_ref, idx_ref, gate_ref, _ = take(6)
    u_ref = take(1)[0]
    dy_ref = take(1)[0] if bwd else None
    wg_ref, wu_ref, wd_ref = take(3)
    prev = take(3) if bwd and not own else None
    y_out = take(1)[0] if fwd else None
    du_out = take(1)[0] if bwd and own else None
    grads = take(3) if bwd else None
    tab_u = take(1)[0]
    tab_dy = take(1)[0] if bwd else None
    acc_y = take(1)[0] if fwd else None
    acc_du = take(1)[0] if bwd and own else None
    gat_u = take(1)[0]
    gat_c = take(1)[0] if bwd else None
    row_o = take(1)[0] if fwd else None
    row_v = take(1)[0] if bwd and own else None
    x_u = take(1)[0]
    x_c = take(1)[0] if bwd else None
    a_ref, b_ref = take(2)
    dh_ref = take(1)[0] if bwd else None
    h_ref = take(1)[0]
    da_ref, db_ref = take(2) if bwd else (None, None)
    sums = take(3) if bwd and not own else grads
    stage, sem = take(2) if own else (None, None)

    step = pl.program_id(0)
    n_grp = ROWS // GRP
    n_col = cdiv(d, LANES)
    widths = [min(LANES, d - LANES * j) for j in range(n_col)]
    outs = [(acc, row) for acc, row in ((acc_y, row_o), (acc_du, row_v)) if acc is not None]

    def aligned(v):
        return pl.multiple_of(v, 4)

    def gather(tile, q):
        pos = gbase_ref[goff_ref[tile] + q]
        for k in range(GRP):
            i = aligned(idx_ref[pos + k])
            dst = pl.ds(aligned((q * GRP + k) * 4), 4)
            gat_u[dst, :] = tab_u[pl.ds(i, 4), :]
            if bwd:
                gat_c[dst, :] = tab_dy[pl.ds(i, 4), :] * gate_ref[pos + k]

    def scatter(tile, q):
        pos = gbase_ref[goff_ref[tile] + q]
        new = []
        where = [pl.ds(aligned(idx_ref[pos + k]), 4) for k in range(GRP)]
        for k in range(GRP):
            gate = gate_ref[pos + k]
            src = pl.ds(aligned((q * GRP + k) * 4), 4)
            new.append([acc[where[k], :] + gate * row[src, :] for acc, row in outs])
        for k in range(GRP):
            for (acc, _), value in zip(outs, new[k]):
                acc[where[k], :] = value

    def convert():
        for gat, x in ((gat_u, x_u), (gat_c, x_c)):
            if gat is None:
                continue
            for j, w in enumerate(widths):
                for r in range(0, ROWS, 64):
                    rows = gat[pl.ds(4 * r + j, 64, stride=4), :]
                    x[r:r + 64, LANES * j:LANES * j + w] = rows[:, :w].astype(BF16)

    @pl.when(step == 0)
    def _():
        def fill(c, _):
            r = pl.multiple_of(c * 64, 64)
            for src, tab in ((u_ref, tab_u), (dy_ref, tab_dy)):
                if src is None:
                    continue
                for j, w in enumerate(widths):
                    vals = src[pl.ds(r, 64), LANES * j:LANES * j + w].astype(F32)
                    tab[pl.ds(4 * r + j, 64, stride=4), 0:w] = vals
            return 0

        lax.fori_loop(0, n_tok // 64, fill, 0)
        for tab in (tab_u, tab_dy):
            if tab is not None:
                tab[4 * n_tok:, :] = jnp.zeros((tab.shape[0] - 4 * n_tok, LANES), F32)
        for acc, row in outs:
            def clear(c, _, acc=acc):
                acc[pl.ds(pl.multiple_of(c * 512, 512), 512), :] = jnp.zeros((512, LANES), F32)
                return 0

            lax.fori_loop(0, 4 * n_tok // 512, clear, 0)
            acc[4 * n_tok:, :] = jnp.zeros((acc.shape[0] - 4 * n_tok, LANES), F32)
            row[...] = jnp.zeros(row.shape, F32)
        lax.fori_loop(0, n_grp, lambda q, _: (gather(0, q), 0)[1], 0)
        convert()

    if bwd:
        if own:
            for g in sums:
                g[...] = jnp.zeros(g.shape, F32)
        else:
            for g, p in zip(sums, prev):
                g[...] = p[...]

    dot = functools.partial(lax.dot_general, preferred_element_type=F32)
    nn = (((1,), (0,)), ((), ()))
    nt = (((1,), (1,)), ((), ()))
    tn = (((0,), (0,)), ((), ()))
    def put_rows(row, value):
        value = value.astype(BF16).astype(F32)
        for j, w in enumerate(widths):
            row[pl.ds(j, ROWS, stride=4), 0:w] = value[:, LANES * j:LANES * j + w]

    def tile(t, _):
        for q in range(n_grp):
            if outs:
                scatter(jnp.maximum(t - 1, 0), q)
            gather(t + 1, q)

        a_ref[...] = dot(x_u[...], wg_ref[0, 0], nn)
        b_ref[...] = dot(x_u[...], wu_ref[0, 0], nn)
        if bwd:
            dh_ref[...] = dot(x_c[...], wd_ref[0, 0], nt)
        for r in range(0, ROWS, 32):
            rows = slice(r, r + 32)
            a, b = a_ref[rows, :], b_ref[rows, :]
            sig = 0.5 * jnp.tanh(0.5 * a) + 0.5
            act = a * sig
            h_ref[rows, :] = (act * b).astype(BF16)
            if bwd:
                dh = dh_ref[rows, :]
                slope = sig * (1.0 + a * (1.0 - sig))
                da_ref[rows, :] = (dh * b * slope).astype(BF16)
                db_ref[rows, :] = (dh * act).astype(BF16)

        if fwd:
            put_rows(row_o, dot(h_ref[...], wd_ref[0, 0], nn))
        if bwd:
            if own:
                put_rows(row_v, dot(da_ref[...], wg_ref[0, 0], nt) + dot(db_ref[...], wu_ref[0, 0], nt))
            sums[0][0] += dot(x_u[...], da_ref[...], tn)
            sums[1][0] += dot(x_u[...], db_ref[...], tn)
            sums[2][0] += dot(h_ref[...], x_c[...], tn)
        convert()

        return 0

    lax.fori_loop(bound_ref[step], bound_ref[step + 1], tile, 0)
    if bwd and not own:
        for g, s in zip(grads, sums):
            g[...] = s[...].astype(BF16)

    if outs:
        @pl.when(step == pl.num_programs(0) - 1)
        def _():
            end = bound_ref[step + 1] - 1
            lax.fori_loop(0, n_grp, lambda q, _: (scatter(end, q), 0)[1], 0)
            chunk = stage.shape[1]
            for (acc, _), out in zip(outs, [o for o in (y_out, du_out) if o is not None]):
                copies = [None, None]
                for c in range(n_tok // chunk):
                    s = c % 2
                    if copies[s] is not None:
                        copies[s].wait()
                    for j, w in enumerate(widths):
                        stage[s, :, LANES * j:LANES * j + w] = acc[pl.ds(4 * chunk * c + j, chunk, stride=4), 0:w]
                    copies[s] = pltpu.make_async_copy(stage.at[s], out.at[pl.ds(c * chunk, chunk), :], sem.at[s])
                    copies[s].start()
                for copy in copies:
                    copy.wait()


def run_experts(tables, base, layer, u, dy, weights, prev, fwd, own):
    bounds, goff, gbase, idx, gate = tables
    bwd = dy is not None
    wg, wu, wd = weights
    n_tok, d = u.shape
    ff = wg.shape[3]
    n_exp = wg.shape[1] // 2
    scalars = (bounds, goff, gbase, idx, gate, base)

    whole = pl.BlockSpec((n_tok, d), lambda e, *_: (0, 0), pipeline_mode=pl.Buffered(1))

    def weight_spec(w):
        return pl.BlockSpec((1, 1) + w.shape[2:],
                            lambda e, *scalars: (layer, scalars[-1][0] + e, 0, 0))

    def grad_spec(w):
        return pl.BlockSpec((1,) + w.shape[2:], lambda e, *_: (e, 0, 0))

    operands = [u] + ([dy] if bwd else []) + [wg, wu, wd] + (list(prev) if prev else [])
    in_specs = [whole] + ([whole] if bwd else []) + [weight_spec(w) for w in weights]
    in_specs += [grad_spec(w) for w in weights] if prev else []
    out_shape, out_specs = [], []
    for use in (fwd, bwd and own):
        if use:
            out_shape.append(jax.ShapeDtypeStruct((n_tok, d), F32))
            out_specs.append(pl.BlockSpec(memory_space=pl.ANY))
    if bwd:
        for w in weights:
            out_shape.append(jax.ShapeDtypeStruct((n_exp,) + w.shape[2:], F32 if own else BF16))
            out_specs.append(grad_spec(w))
    table = pltpu.VMEM((4 * n_tok + 32, LANES), F32)
    rows = pltpu.VMEM((4 * ROWS, LANES), F32)
    mid = lambda dt: pltpu.VMEM((ROWS, ff), dt)
    x = pltpu.VMEM((ROWS, d), BF16)
    two = 1 + bwd
    scratch = [table] * two + [table] * (fwd + (bwd and own)) + [rows] * two + [rows] * (fwd + (bwd and own))
    scratch += [x] * two + [mid(F32)] * (2 + bwd) + [mid(BF16)] * (1 + 2 * bwd)
    if bwd and not own:
        scratch += [pltpu.VMEM((1,) + w.shape[2:], F32) for w in weights]
    if own:
        scratch += [pltpu.VMEM((2, 256, d), F32), pltpu.SemaphoreType.DMA((2,))]
    passes = (3 * fwd + (0 if fwd else 2)) + bwd * (4 + 2 * own)
    flops = 2 * d * ff * passes * n_tok * 2
    return pl.pallas_call(
        functools.partial(expert_kernel, (fwd, bwd, own, n_tok, d, ff)),
        out_shape=out_shape,
        grid_spec=pltpu.PrefetchScalarGridSpec(
            num_scalar_prefetch=6, grid=(n_exp,), in_specs=in_specs, out_specs=out_specs,
            scratch_shapes=scratch),
        compiler_params=pltpu.CompilerParams(dimension_semantics=("arbitrary",), vmem_limit_bytes=VMEM_LIMIT),
        cost_estimate=pl.CostEstimate(flops=flops, bytes_accessed=3 * 2 * n_exp * d * ff, transcendentals=0),
        name=f"experts_{'f' if fwd else ''}{'b' if bwd else ''}_{'own' if own else 'other'}_{layer}",
    )(*scalars, *operands)


def solution(mesh):
    ep_size, dp_size = mesh.shape['ep'], mesh.shape['dp']
    sub = Mesh(mesh.devices.reshape(ep_size, dp_size // 2, 2), ('ep', 'x', 'core'))
    tok_axes = ('x', 'core', 'ep')
    tok_spec = P(tok_axes, None)
    route_spec = P(None, tok_axes, None)
    whole_spec = P(None, None, None)
    expert_spec = P(None, 'ep', None, None)
    half_axes = ('core', 'ep')

    def device_step(tokens, d_out, expert_ids, gate_vals, w_mix, w_gate, w_up, w_down):
        n_layers = w_mix.shape[0]
        n_tok, d = tokens.shape
        top = expert_ids.shape[2]
        n_exp = w_gate.shape[1] * ep_size
        n_mine = w_gate.shape[1] // 2
        n_src = 2 * ep_size
        cap = CAP_FACTOR * n_tok * top // n_exp
        max_groups = cdiv(n_src * cdiv(cap, GRP), ROWS // GRP) * (ROWS // GRP)
        ix, ic, ie = lax.axis_index('x'), lax.axis_index('core'), lax.axis_index('ep')
        base = (ic * n_mine)[None].astype(I32)
        experts = ie * w_gate.shape[1] + ic * n_mine + jnp.arange(n_mine, dtype=I32)
        weights = (w_gate, w_up, w_down)

        tok, gts, groups = local_lists(expert_ids, gate_vals, n_exp)
        length = tok.shape[1]
        packed = jnp.concatenate([tok.astype(F32), gts, groups.astype(F32)], axis=1)
        packed = lax.all_gather(packed, tok_axes, axis=0, tiled=False)
        packed = packed.reshape(2, n_src, n_layers, -1)

        def tables(layer, other):
            part = lax.dynamic_index_in_dim(packed, (1 - ix) if other else ix, 0, keepdims=False)[:, layer]
            tk = part[:, :length].astype(I32)
            gr = part[:, 2 * length:].astype(I32)
            return half_tables(tk, part[:, length:2 * length], gr, experts, n_tok, max_groups)

        def own_half(block):
            return lax.all_gather(block, half_axes, axis=0, tiled=True)

        def other_half(own):
            mine = lax.dynamic_slice_in_dim(own, ic * 2 * n_tok, 2 * n_tok, 0)
            got = lax.ppermute(mine, 'x', [(0, 1), (1, 0)])
            return lax.all_gather(got, 'core', axis=0, tiled=True)

        def mix(x, w):
            return (x.astype(F32) + jnp.dot(x, w, preferred_element_type=F32)).astype(BF16)

        def mix_back(du, w):
            return (du.astype(F32) + jnp.einsum('te,de->td', du, w, preferred_element_type=F32)).astype(BF16)

        def my_block(half):
            return lax.dynamic_slice_in_dim(half, (ic * ep_size + ie) * n_tok, n_tok, 0)

        def reduce_half(part):
            return lax.psum_scatter(part, half_axes, scatter_dimension=0, tiled=True)

        tabs = [[tables(layer, other) for other in (False, True)] for layer in range(n_layers)]

        x0 = own_half(tokens)
        u0 = mix(x0, w_mix[0])
        (part,) = run_experts(tabs[0][0], base, 0, u0, None, weights, None, True, True)
        y0 = (my_block(u0).astype(F32) + reduce_half(part)).astype(BF16)
        x1 = own_half(y0)
        u1 = mix(x1, w_mix[1])
        dy = own_half(d_out)
        part, dpart, *g1 = run_experts(tabs[1][0], base, 1, u1, dy, weights, None, True, True)
        u1o = mix(other_half(x1), w_mix[1])
        dyo = other_half(dy)
        g1 = run_experts(tabs[1][1], base, 1, u1o, dyo, weights, g1, False, False)
        y1 = (my_block(u1).astype(F32) + reduce_half(part)).astype(BF16)
        du1 = (d_out.astype(F32) + reduce_half(dpart)).astype(BF16)
        dx1 = mix_back(du1, w_mix[1])
        dy = own_half(dx1)
        dpart, *g0 = run_experts(tabs[0][0], base, 0, u0, dy, weights, None, False, True)
        u0o = mix(other_half(x0), w_mix[0])
        dyo = other_half(dy)
        g0 = run_experts(tabs[0][1], base, 0, u0o, dyo, weights, g0, False, False)
        du0 = (dx1.astype(F32) + reduce_half(dpart)).astype(BF16)
        dx0 = mix_back(du0, w_mix[0])

        g_mix = jnp.stack([jnp.einsum('td,te->de', x, du, preferred_element_type=F32)
                           for x, du in ((tokens, du0), (y0, du1))])
        g_mix = lax.psum(g_mix, ('x', 'core', 'ep')).astype(BF16)
        outs = [lax.all_gather(jnp.stack([a, b]), 'core', axis=1, tiled=True) for a, b in zip(g0, g1)]
        return (y1, dx0, g_mix, *outs)

    return jax.shard_map(device_step, mesh=sub,
                         in_specs=(tok_spec, tok_spec, route_spec, route_spec, whole_spec,
                                   expert_spec, expert_spec, expert_spec),
                         out_specs=(tok_spec, tok_spec, whole_spec, expert_spec, expert_spec, expert_spec),
                         check_vma=False)
```

```python
import functools

import jax
import jax.numpy as jnp
from jax import lax
from jax.experimental import pallas as pl
from jax.experimental.pallas import tpu as pltpu
from jax.sharding import Mesh, PartitionSpec as P

F32, BF16, I32 = jnp.float32, jnp.bfloat16, jnp.int32
MESH = pl.DeviceIdType.MESH
ROWS = 384
GRP = 8
PITCH = 8
HALF = 4
CAP_FACTOR = 3
LANES = 128
N_SRC = 4
VMEM_LIMIT = 62 * 1024 * 1024


def cdiv(a, b):
    return (a + b - 1) // b


def spans(d):
    return [(LANES * j, min(LANES, d - LANES * j)) for j in range(cdiv(d, LANES))]


def sorted_list(expert_ids, gate_vals):
    n_tok, top = expert_ids.shape
    n = n_tok * top
    keys = expert_ids.reshape(n) * n + jnp.arange(n, dtype=I32)
    keys, gates = lax.sort((keys, gate_vals.reshape(n)), num_keys=1)
    return ((keys % n) // top).astype(F32), gates


def scalar_tables(cnt, first, n_local, core, list_len, max_groups):
    n_rel, n_layers, _ = cnt.shape
    n_mine = n_local // 2
    starts = jnp.cumsum(cnt, axis=2) - cnt
    cnt = lax.dynamic_slice_in_dim(cnt, first, n_local, 2)
    starts = lax.dynamic_slice_in_dim(starts, first, n_local, 2)
    per_tile = ROWS // GRP
    grp = (cnt + GRP - 1) // GRP
    halves = grp.reshape(2, N_SRC, n_layers, n_local).sum(1)
    tiles = jnp.maximum(1, (halves + per_tile - 1) // per_tile)
    load = 3 * tiles[0] + 2 * tiles[1]
    e = jnp.arange(n_local, dtype=I32)
    ahead = (load[:, None, :] > load[:, :, None]) | ((load[:, None, :] == load[:, :, None]) & (e[None, None] < e[None, :, None]))
    rank = jnp.sum(ahead.astype(I32), axis=2)
    k = jnp.arange(n_mine, dtype=I32)
    want = 2 * k + (k + core) % 2
    pick = (rank[:, None, :] == want[None, :, None]).astype(I32)

    def mine(v):
        return jnp.sum(pick * v[..., None, :], axis=-1)

    experts = mine(jnp.broadcast_to(e, (n_layers, n_local)))
    cnt4 = mine(cnt.reshape(2, N_SRC, n_layers, n_local))
    src = jnp.arange(N_SRC, dtype=I32)[None, :, None, None]
    start4 = mine(starts.reshape(2, N_SRC, n_layers, n_local)) + src * list_len
    ng = (cnt4 + GRP - 1) // GRP
    off = jnp.cumsum(ng, axis=1) - ng
    total = jnp.sum(ng, axis=1)
    g = jnp.arange(max_groups, dtype=I32)
    tails = N_SRC * list_len
    pos = jnp.full(total.shape + (max_groups,), tails + n_mine * N_SRC * GRP, I32)
    for s in range(N_SRC):
        rel = g - off[:, s][..., None]
        full = start4[:, s][..., None] + rel * GRP
        tail = tails + (k[None, None, :, None] * N_SRC + s) * GRP
        value = jnp.where(rel * GRP + GRP > cnt4[:, s][..., None], tail, full)
        pos = jnp.where((rel >= 0) & (rel < ng[:, s][..., None]), value, pos)
    n_tiles = jnp.maximum(1, (total + per_tile - 1) // per_tile)
    ends = jnp.cumsum(n_tiles, axis=2)
    most = n_mine * (max_groups // per_tile) + 2
    t = jnp.minimum(jnp.arange(most, dtype=I32), ends[..., -1:] - 1)
    past = (t[..., None] >= ends[:, :, None, :]).astype(I32)
    slot = jnp.sum(past, axis=3)
    before = jnp.max(past * ends[:, :, None, :], axis=3)
    goff = slot * max_groups + (t - before) * per_tile
    bounds = jnp.concatenate([jnp.zeros_like(ends[..., :1]), ends], axis=2)
    parts = [jnp.broadcast_to(experts[None], (2, n_layers, n_mine)), bounds, goff,
             start4.transpose(0, 2, 3, 1).reshape(2, n_layers, -1), cnt4.transpose(0, 2, 3, 1).reshape(2, n_layers, -1),
             pos.reshape(2, n_layers, -1)]
    where, at = [], 0
    for p in parts:
        where.append(at)
        at += p.shape[-1]
    flat = jnp.concatenate(parts, axis=2)
    return flat.reshape(-1), where, at


def expert_kernel(cfg, *refs):
    fwd, bwd, own, mix_dy, n_blk, d, ff, where, at0, list_at, list_len, n_exp, p_f32, n_alias = cfg
    refs = list(refs)
    take = lambda n: [refs.pop(0) for _ in range(n)]
    tab_ref = take(1)[0]
    idx_hbm, gate_hbm = take(2)
    x_refs = take(N_SRC)
    mix_ref = take(1)[0]
    dy_refs = take(N_SRC) if bwd else []
    mixb_ref = take(1)[0] if mix_dy else None
    wg_ref, wu_ref, wd_ref = take(3)
    prev = take(1)[0] if bwd and not own else None
    take(n_alias)
    y_outs = take(N_SRC) if fwd else []
    du_outs = take(N_SRC) if bwd and own else []
    grad = take(1)[0] if bwd and own else None
    finals = take(3) if bwd and not own else None
    sent = take(1)[0] if bwd and not own else None
    table = take(1)[0]
    acc = take(1)[0] if own else None
    gat_u = take(1)[0]
    gat_c = take(1)[0] if bwd else None
    row_o = take(1)[0] if fwd else None
    row_v = take(1)[0] if bwd and own else None
    gu_ref = take(1)[0]
    x_u = take(1)[0]
    x_c = take(1)[0] if bwd else None
    ab_ref = take(1)[0]
    dh_ref = take(1)[0] if bwd else None
    h_ref = take(1)[0]
    dab_ref = take(1)[0] if bwd else None
    sums = take(1)[0] if bwd and not own else None
    idx, gates, list_sem = take(3)
    stage_f, stage_b, out_sem = take(3) if own else (None, None, None)

    step = pl.program_id(0)
    n_grp = ROWS // GRP
    cols = spans(d)
    lo = ff // 256 * 256
    hi = ff - lo
    e_at, b_at, g_at, s_at, c_at, p_at = [at0 + w for w in where]
    outs = [(k, row) for k, row in ((0, row_o), (HALF, row_v)) if row is not None]
    dot = functools.partial(lax.dot_general, preferred_element_type=F32)
    nn = (((1,), (0,)), ((), ()))
    nt = (((1,), (1,)), ((), ()))
    tn = (((0,), (0,)), ((), ()))

    def al(v, m=HALF):
        return pl.multiple_of(v, m)

    def gather(tile, q):
        pos = tab_ref[p_at + tab_ref[g_at + tile] + q]
        for k in range(GRP):
            i = idx[pos + k]
            dst = pl.ds(al((q * GRP + k) * HALF), HALF)
            gat_u[dst, :] = table[pl.ds(al(i), HALF), :]
            if bwd:
                gat_c[dst, :] = table[pl.ds(al(i + HALF), HALF), :] * gates[pos + k]

    def scatter(tile, q):
        pos = tab_ref[p_at + tab_ref[g_at + tile] + q]
        new = []
        at = [idx[pos + k] for k in range(GRP)]
        for k in range(GRP):
            gate = gates[pos + k]
            src = pl.ds(al((q * GRP + k) * HALF), HALF)
            new.append([acc[pl.ds(al(at[k] + o), HALF), :] + gate * row[src, :] for o, row in outs])
        for k in range(GRP):
            for (o, _), value in zip(outs, new[k]):
                acc[pl.ds(al(at[k] + o), HALF), :] = value

    def convert():
        for gat, x in ((gat_u, x_u), (gat_c, x_c)):
            if gat is None:
                continue
            for j, (c, w) in enumerate(cols):
                for r in range(0, ROWS, 64):
                    rows = gat[pl.ds(HALF * r + j, 64, stride=HALF), :]
                    x[r:r + 64, c:c + w] = rows[:, :w].astype(BF16)

    @pl.when(step == 0)
    def _():
        src = pl.ds(list_at, N_SRC * list_len)
        dst = pl.ds(0, N_SRC * list_len)
        copies = [pltpu.make_async_copy(idx_hbm.at[src], idx.at[dst], list_sem.at[0]),
                  pltpu.make_async_copy(gate_hbm.at[src], gates.at[dst], list_sem.at[1])]
        for copy in copies:
            copy.start()
        if own:
            def clear(c, _):
                acc[pl.ds(al(c * 512, 512), 512), :] = jnp.zeros((512, LANES), F32)
                return 0

            lax.fori_loop(0, acc.shape[0] // 512, clear, 0)
            for _, row in outs:
                row[...] = jnp.zeros(row.shape, F32)
        table[PITCH * N_SRC * n_blk:, :] = jnp.zeros((table.shape[0] - PITCH * N_SRC * n_blk, LANES), F32)
        rows = 256
        plan = [(x_refs, mix_ref, nn, 0, fwd)]
        if bwd:
            plan.append((dy_refs, mixb_ref, nt, HALF, own))
        for srcs, m_ref, dims, o, seed in plan:
            for s, ref in enumerate(srcs):
                def fill(c, _, ref=ref, m_ref=m_ref, dims=dims, o=o, seed=seed, s=s):
                    r = al(c * rows, rows)
                    vals = ref[pl.ds(r, rows), :]
                    if m_ref is not None:
                        mixed = vals.astype(F32) + dot(vals, m_ref[...], dims)
                        vals = mixed.astype(BF16)
                    vals = vals.astype(F32)
                    at = PITCH * (s * n_blk + r) + o
                    for j, (cc, w) in enumerate(cols):
                        to = pl.ds(at + j, rows, stride=PITCH)
                        table[to, 0:w] = vals[:, cc:cc + w]
                        if seed and s == 0:
                            acc[to, 0:w] = vals[:, cc:cc + w]
                    return 0

                lax.fori_loop(0, n_blk // rows, fill, 0)
        for copy in copies:
            copy.wait()
        dummy = PITCH * N_SRC * n_blk

        def tail(q, _):
            n = tab_ref[c_at + q]
            left = n % GRP
            p = tab_ref[s_at + q] + n - left
            to = N_SRC * list_len + q * GRP
            for k in range(GRP):
                idx[to + k] = jnp.where(k < left, idx[p + k], dummy)
                gates[to + k] = jnp.where(k < left, gates[p + k], 0.0)
            return 0

        lax.fori_loop(0, n_exp * N_SRC, tail, 0)
        for k in range(GRP):
            idx[N_SRC * (list_len + n_exp * GRP) + k] = dummy
            gates[N_SRC * (list_len + n_exp * GRP) + k] = 0.0
        lax.fori_loop(0, n_grp, lambda q, _: (gather(0, q), 0)[1], 0)
        convert()

    for i, w in enumerate((wg_ref, wu_ref)):
        gu_ref[i * lo:(i + 1) * lo, :] = w[0, 0, 0:lo, :]
        gu_ref[2 * lo + i * hi:2 * lo + (i + 1) * hi, :] = w[0, 0, lo:, :]
    total = grad if own else sums
    if bwd:
        total[...] = jnp.zeros(total.shape, F32) if own else prev[0]

    def put_rows(row, value):
        value = value.astype(BF16).astype(F32)
        for j, (c, w) in enumerate(cols):
            row[pl.ds(j, ROWS, stride=HALF), 0:w] = value[:, c:c + w]

    low = lax.broadcasted_iota(I32, (16, 2 * hi), 1) < hi

    def middle(a, b, dh):
        sig = 0.5 * jnp.tanh(0.5 * a) + 0.5
        act = a * sig
        h = act * b
        if dh is None:
            return h, None, None
        slope = sig * (1.0 + a * (1.0 - sig))
        return h, dh * b * slope, dh * act

    def tile(t, _):
        for q in range(n_grp):
            if outs:
                scatter(jnp.maximum(t - 1, 0), q)
            gather(t + 1, q)
        ab_ref[...] = dot(x_u[...], gu_ref[...], nt)
        if bwd:
            dh_ref[...] = dot(x_c[...], wd_ref[0, 0], nt)
        for r in range(0, ROWS, 16):
            rows = slice(r, r + 16)
            for c in range(0, lo, LANES):
                h, da, db = middle(ab_ref[rows, c:c + LANES], ab_ref[rows, lo + c:lo + c + LANES],
                                   dh_ref[rows, c:c + LANES] if bwd else None)
                h_ref[rows, c:c + LANES] = h.astype(BF16)
                if bwd:
                    dab_ref[rows, c:c + LANES] = da.astype(BF16)
                    dab_ref[rows, lo + c:lo + c + LANES] = db.astype(BF16)
            a = ab_ref[rows, 2 * lo:]
            b = pltpu.roll(a, hi, 1)
            dh = dh_ref[rows, lo:] if bwd else None
            if bwd:
                dh = jnp.concatenate([dh, dh], axis=1)
            h, da, db = middle(a, b, dh)
            h_ref[rows, lo:] = h[:, :hi].astype(BF16)
            if bwd:
                dab_ref[rows, 2 * lo:] = jnp.where(low, da, pltpu.roll(db, hi, 1)).astype(BF16)
        if fwd:
            put_rows(row_o, dot(h_ref[...], wd_ref[0, 0], nn))
        if bwd:
            if own:
                put_rows(row_v, dot(dab_ref[...], gu_ref[...], nn))
            view = total.at[0] if own else total
            view[0:2 * ff, :] += dot(dab_ref[...], x_u[...], tn)
            view[2 * ff:, :] += dot(h_ref[...], x_c[...], tn)
        convert()
        return 0

    lax.fori_loop(tab_ref[b_at + step], tab_ref[b_at + step + 1], tile, 0)
    if bwd and not own:
        for out in ([f.at[0, 0] for f in finals], [sent.at[0, i] for i in range(3)]):
            for i in range(2):
                out[i][0:lo, :] = sums[i * lo:(i + 1) * lo, :].astype(BF16)
                out[i][lo:, :] = sums[2 * lo + i * hi:2 * lo + (i + 1) * hi, :].astype(BF16)
            out[2][...] = sums[2 * ff:, :].astype(BF16)

    if outs:
        @pl.when(step == pl.num_programs(0) - 1)
        def _():
            end = tab_ref[b_at + step + 1] - 1
            lax.fori_loop(0, n_grp, lambda q, _: (scatter(end, q), 0)[1], 0)
            chunk = stage_f.shape[1]
            flights = {}
            n = 0
            for (o, _), out in zip(reversed(outs), [v for v in (du_outs, y_outs) if v]):
                for s in range(N_SRC):
                    wide = s == 0 or p_f32
                    stage = stage_f if wide else stage_b
                    for c in range(n_blk // chunk):
                        key = (wide, n % 2)
                        if key in flights:
                            flights.pop(key).wait()
                        for j, (cc, w) in enumerate(cols):
                            rows = pl.ds(PITCH * (s * n_blk + c * chunk) + o + j, chunk, stride=PITCH)
                            stage[n % 2, :, cc:cc + w] = acc[rows, 0:w].astype(stage.dtype)
                        flights[key] = pltpu.make_async_copy(
                            stage.at[n % 2], out[s].at[pl.ds(c * chunk, chunk), :], out_sem.at[2 * wide + n % 2])
                        flights[key].start()
                        n += 1
            for copy in flights.values():
                copy.wait()


def run_experts(tabs, lists, layer, half, x, mix, dy, mix_back, weights, prev, finals, fwd, own, p_f32=False):
    tab, where, width = tabs
    idx, gates, list_len = lists
    bwd = dy is not None
    wg, wu, wd = weights
    n_blk, d = x[0].shape
    n_layers, n_local, ff, _ = wd.shape
    n_exp = n_local // 2
    row_id = half * n_layers + layer
    at0 = row_id * width
    e_at = at0 + where[0]

    whole = pl.BlockSpec((n_blk, d), lambda e, *_: (0, 0), pipeline_mode=pl.Buffered(1))
    square = pl.BlockSpec((d, d), lambda e, *_: (0, 0), pipeline_mode=pl.Buffered(1))
    anyspec = pl.BlockSpec(memory_space=pl.ANY)
    weight = pl.BlockSpec((1, 1, ff, d), lambda e, tab: (layer, tab[e_at + e], 0, 0))
    partial = pl.BlockSpec((1, 3 * ff, d), lambda e, *_: (e, 0, 0))

    operands = [idx, gates, *x, mix]
    in_specs = [anyspec, anyspec] + [whole] * N_SRC + [square]
    if bwd:
        operands += list(dy)
        in_specs += [whole] * N_SRC
    if mix_back is not None:
        operands.append(mix_back)
        in_specs.append(square)
    operands += [wg, wu, wd]
    in_specs += [weight] * 3
    out_shape, out_specs, aliases = [], [], {}
    for use in (fwd, bwd and own):
        if use:
            out_shape += [jax.ShapeDtypeStruct((n_blk, d), F32 if s == 0 or p_f32 else BF16) for s in range(N_SRC)]
            out_specs += [anyspec] * N_SRC
    if bwd and own:
        out_shape.append(jax.ShapeDtypeStruct((n_exp, 3 * ff, d), F32))
        out_specs.append(partial)
    if bwd and not own:
        operands.append(prev)
        in_specs.append(partial)
        for i, f in enumerate(finals or ()):
            aliases[1 + len(operands)] = i
            operands.append(f)
            in_specs.append(anyspec)
        out_shape += [jax.ShapeDtypeStruct((n_layers, n_local, ff, d), BF16)] * 3
        out_specs += [weight] * 3
        out_shape.append(jax.ShapeDtypeStruct((n_exp, 3, ff, d), BF16))
        out_specs.append(pl.BlockSpec((1, 3, ff, d), lambda e, *_: (e, 0, 0, 0)))
    table = pltpu.VMEM((PITCH * N_SRC * n_blk + 512, LANES), F32)
    rows = pltpu.VMEM((HALF * ROWS, LANES), F32)
    mid = lambda n, dt: pltpu.VMEM((ROWS, n), dt)
    scratch = [table] * (1 + own) + [rows] * (1 + bwd) + [rows] * (fwd + (bwd and own))
    scratch += [pltpu.VMEM((2 * ff, d), BF16)] + [mid(d, BF16)] * (1 + bwd) + [mid(2 * ff, F32)]
    scratch += [mid(ff, F32)] * bwd + [mid(ff, BF16)] + [mid(2 * ff, BF16)] * bwd
    if bwd and not own:
        scratch.append(pltpu.VMEM((3 * ff, d), F32))
    n_list = N_SRC * (list_len + n_exp * GRP) + 64
    scratch += [pltpu.SMEM((n_list,), I32), pltpu.SMEM((n_list,), F32), pltpu.SemaphoreType.DMA((2,))]
    if own:
        scratch += [pltpu.VMEM((2, 256, d), F32), pltpu.VMEM((2, 256, d), BF16), pltpu.SemaphoreType.DMA((4,))]
    passes = 2 + fwd + bwd * (4 + 2 * own)
    flops = 2 * d * ff * passes * n_blk * N_SRC * 2
    cfg = (fwd, bwd, own, mix_back is not None, n_blk, d, ff, where, at0, row_id * N_SRC * list_len, list_len, n_exp,
           p_f32, len(aliases))
    return pl.pallas_call(
        functools.partial(expert_kernel, cfg),
        out_shape=out_shape,
        grid_spec=pltpu.PrefetchScalarGridSpec(
            num_scalar_prefetch=1, grid=(n_exp,), in_specs=in_specs, out_specs=out_specs, scratch_shapes=scratch),
        input_output_aliases=aliases,
        compiler_params=pltpu.CompilerParams(dimension_semantics=("arbitrary",), vmem_limit_bytes=VMEM_LIMIT),
        cost_estimate=pl.CostEstimate(flops=flops, bytes_accessed=3 * 2 * n_exp * d * ff, transcendentals=0),
        name=f"experts_{'f' if fwd else ''}{'b' if bwd else ''}_{'own' if own else 'other'}_{layer}",
    )(tab, *operands)


def place_kernel(tab_ref, got_ref, *refs):
    for i, out in enumerate(refs[3:]):
        out[0, 0] = got_ref[0, i]


def place(tabs, layer, got, finals):
    partner, width = tabs
    n_exp, _, ff, d = got.shape
    at = layer * n_exp
    final = pl.BlockSpec((1, 1, ff, d), lambda e, tab: (layer, tab[at + e], 0, 0))
    return pl.pallas_call(
        place_kernel,
        out_shape=[jax.ShapeDtypeStruct(f.shape, f.dtype) for f in finals],
        grid_spec=pltpu.PrefetchScalarGridSpec(
            num_scalar_prefetch=1, grid=(n_exp,),
            in_specs=[pl.BlockSpec((1, 3, ff, d), lambda e, *_: (e, 0, 0, 0))] + [pl.BlockSpec(memory_space=pl.ANY)] * 3,
            out_specs=[final] * 3),
        input_output_aliases={2: 0, 3: 1, 4: 2},
        compiler_params=pltpu.CompilerParams(dimension_semantics=("arbitrary",)),
        cost_estimate=pl.CostEstimate(flops=0, bytes_accessed=4 * got.size, transcendentals=0),
        name=f"place_{layer}",
    )(partner, got, *finals)


def peer(rel):
    return {name: (lax.axis_index(name) + ((rel >> bit) & 1)) % 2 for bit, name in enumerate(("ep", "core", "x"))}


def meet(rels):
    barrier = pltpu.get_barrier_semaphore()
    for rel in rels:
        pl.semaphore_signal(barrier, inc=1, device_id=peer(rel), device_id_type=MESH)
    pl.semaphore_wait(barrier, len(rels))


def share_kernel(n_rel, mine_ref, all_ref, send_sem, recv_sem):
    meet(range(1, n_rel))
    copies = [pltpu.make_async_remote_copy(
        src_ref=mine_ref, dst_ref=all_ref.at[rel], send_sem=send_sem.at[rel], recv_sem=recv_sem.at[rel],
        device_id=peer(rel), device_id_type=MESH) for rel in range(1, n_rel)]
    for copy in copies:
        copy.start()
    all_ref[0] = mine_ref[...]
    for copy in copies:
        copy.wait()


def share(mine, n_rel):
    return pl.pallas_call(
        functools.partial(share_kernel, n_rel),
        out_shape=jax.ShapeDtypeStruct((n_rel,) + mine.shape, mine.dtype),
        in_specs=[pl.BlockSpec(memory_space=pltpu.VMEM)],
        out_specs=pl.BlockSpec(memory_space=pltpu.VMEM),
        scratch_shapes=[pltpu.SemaphoreType.DMA((n_rel,)), pltpu.SemaphoreType.DMA((n_rel,))],
        compiler_params=pltpu.CompilerParams(collective_id=0, has_side_effects=True),
        cost_estimate=pl.CostEstimate(flops=10 ** 7, bytes_accessed=mine.size * 4 * n_rel, transcendentals=0),
        name="share_lists",
    )(mine)


Y, CORE = 1, 2


def sum_kernel(n_chunk, p_own, p_y, p_core, p_diag, o_own, o_y, o_core, o_diag,
               mine, got, s_buf, r_buf, y_buf, load_sem, d2d_send, d2d_recv, ys_send, ys_recv,
               yg_send, yg_recv, cg_send, cg_recv, fg_send, fg_recv, put_sem):
    rows = p_own.shape[0] // n_chunk
    cut = [pl.ds(k * rows, rows) for k in range(n_chunk)]
    loads = [[pltpu.make_async_copy(src.at[cut[k]], mine.at[i, cut[k]], load_sem.at[i, k]) for k in range(n_chunk)]
             for i, src in enumerate((p_y, p_own))]
    for i in range(2):
        for k in range(n_chunk):
            loads[i][k].start()
    meet((Y, CORE))

    def remote(src, dst, send, recv, rel):
        return pltpu.make_async_remote_copy(src_ref=src, dst_ref=dst, send_sem=send, recv_sem=recv,
                                            device_id=peer(rel), device_id_type=MESH)

    d2d = [[remote(src.at[cut[k]], got.at[i, cut[k]], d2d_send.at[i, k], d2d_recv.at[i, k], CORE)
            for k in range(n_chunk)] for i, src in enumerate((p_diag, p_core))]
    for i in range(2):
        for k in range(n_chunk):
            d2d[i][k].start()
    over = [remote(s_buf.at[cut[k]], r_buf.at[cut[k]], ys_send.at[k], ys_recv.at[k], Y) for k in range(n_chunk)]
    for k in range(n_chunk):
        loads[0][k].wait()
        d2d[0][k].wait_recv()
        s_buf[cut[k], :] = (mine[0, cut[k], :] + got[0, cut[k], :]).astype(BF16)
        over[k].start()
    to_y = [remote(y_buf.at[cut[k]], o_y.at[cut[k]], yg_send.at[k], yg_recv.at[k], Y) for k in range(n_chunk)]
    to_core = [remote(y_buf.at[cut[k]], o_core.at[cut[k]], cg_send.at[k], cg_recv.at[k], CORE) for k in range(n_chunk)]
    puts = [pltpu.make_async_copy(y_buf.at[cut[k]], o_own.at[cut[k]], put_sem.at[k]) for k in range(n_chunk)]
    for k in range(n_chunk):
        loads[1][k].wait()
        d2d[1][k].wait_recv()
        over[k].wait_recv()
        total = mine[1, cut[k], :] + got[1, cut[k], :] + r_buf[cut[k], :].astype(F32)
        y_buf[cut[k], :] = total.astype(BF16)
        to_y[k].start()
        to_core[k].start()
        puts[k].start()
    on = [remote(o_y.at[cut[k]], o_diag.at[cut[k]], fg_send.at[k], fg_recv.at[k], CORE) for k in range(n_chunk)]
    for k in range(n_chunk):
        to_y[k].wait_recv()
        on[k].start()
    for k in range(n_chunk):
        for i in range(2):
            d2d[i][k].wait_send()
        over[k].wait_send()
        to_y[k].wait_send()
        to_core[k].wait()
        puts[k].wait()
        on[k].wait()


def sum_blocks(parts, n_chunk=4):
    n_blk, d = parts[0].shape
    anyspec = pl.BlockSpec(memory_space=pl.ANY)
    sem = lambda *s: pltpu.SemaphoreType.DMA(s)
    n = n_chunk
    return pl.pallas_call(
        functools.partial(sum_kernel, n_chunk),
        out_shape=[jax.ShapeDtypeStruct((n_blk, d), BF16)] * N_SRC,
        in_specs=[anyspec] * N_SRC,
        out_specs=[anyspec] * N_SRC,
        scratch_shapes=[pltpu.VMEM((2, n_blk, d), F32), pltpu.VMEM((2, n_blk, d), F32), pltpu.VMEM((n_blk, d), BF16),
                        pltpu.VMEM((n_blk, d), BF16), pltpu.VMEM((n_blk, d), BF16), sem(2, n), sem(2, n), sem(2, n),
                        sem(n), sem(n), sem(n), sem(n), sem(n), sem(n), sem(n), sem(n), sem(n)],
        compiler_params=pltpu.CompilerParams(collective_id=1, has_side_effects=True, vmem_limit_bytes=VMEM_LIMIT),
        cost_estimate=pl.CostEstimate(flops=10 ** 8, bytes_accessed=n_blk * d * 40, transcendentals=0),
        name="sum_blocks",
    )(*parts)


def solution(mesh):
    ep_size, dp_size = mesh.shape['ep'], mesh.shape['dp']
    sub = Mesh(mesh.devices.reshape(ep_size, dp_size // 2, 2), ('ep', 'x', 'core'))
    tok_axes = ('x', 'core', 'ep')
    tok_spec = P(tok_axes, None)
    route_spec = P(None, tok_axes, None)
    whole_spec = P(None, None, None)
    expert_spec = P(None, 'ep', None, None)
    flip = [(0, 1), (1, 0)]
    move = lambda v, axis: lax.ppermute(v, axis, flip)

    def device_step(tokens, d_out, expert_ids, gate_vals, w_mix, w_gate, w_up, w_down):
        n_layers = w_mix.shape[0]
        n_tok, d = tokens.shape
        top = expert_ids.shape[2]
        n_local, ff = w_gate.shape[1], w_gate.shape[3]
        n_exp = n_local * ep_size
        n = n_tok * top
        n_rel = 2 * N_SRC
        cap = cdiv(CAP_FACTOR * n, n_exp)
        per_tile = ROWS // GRP
        max_groups = cdiv(N_SRC * cdiv(cap, GRP), per_tile) * per_tile
        ic, ie = lax.axis_index('core'), lax.axis_index('ep')
        weights = (jnp.swapaxes(w_gate, 2, 3), jnp.swapaxes(w_up, 2, 3), w_down)

        def spread(own):
            far = move(own, 'ep')
            return [own, far, move(own, 'core'), move(far, 'core')]

        def across(blocks):
            a, b = move(blocks[0], 'x'), move(blocks[1], 'x')
            return [a, b, move(a, 'core'), move(b, 'core')]

        x0 = spread(tokens)
        lists = [sorted_list(expert_ids[l], gate_vals[l]) for l in range(n_layers)]
        counts = jnp.sum((expert_ids.reshape(n_layers, n, 1) == jnp.arange(n_exp, dtype=I32)).astype(F32), axis=1)
        packed = jnp.concatenate([jnp.concatenate([v[0] for v in lists] + [v[1] for v in lists]).reshape(-1, LANES),
                                  jnp.pad(counts, ((0, 8 - n_layers), (0, LANES - n_exp)))], axis=0)
        packed = share(packed, n_rel)
        n_rows = n // LANES
        cnt = packed[:, 2 * n_layers * n_rows:2 * n_layers * n_rows + n_layers, :n_exp].astype(I32)
        tab, where, width = scalar_tables(cnt, ie * n_local, n_local, ic, n, max_groups)
        halves = lambda v: v.reshape(2, N_SRC, n_layers, n_rows, LANES).transpose(0, 2, 1, 3, 4).reshape(-1)
        block = jnp.arange(n_rel, dtype=I32)[:, None, None] % N_SRC * n_tok
        idx = halves((packed[:, :n_layers * n_rows].astype(I32) + block) * PITCH)
        gates = halves(packed[:, n_layers * n_rows:2 * n_layers * n_rows])
        tabs = (tab, where, width)
        lists = (idx, gates, n)
        mine = jnp.concatenate([lax.slice_in_dim(tab, l * width, l * width + n_local // 2) for l in range(n_layers)])
        partner = (move(mine, 'core'), None)

        part = run_experts(tabs, lists, 0, 0, x0, w_mix[0], None, None, weights, None, None, True, True, p_f32=True)
        dy1 = spread(d_out)
        x1 = sum_blocks(part)
        x1o, dy1o, x0o = across(x1), across(dy1), across(x0)
        out = run_experts(tabs, lists, 1, 0, x1, w_mix[1], dy1, None, weights, None, None, True, True)
        y_part, du_part, g1 = out[:4], out[4:8], out[8]
        def sum_far(p):
            got = [lax.ppermute(p[1], 'ep', flip), lax.ppermute(p[2], 'core', flip),
                   lax.ppermute(p[3], ('ep', 'core'), [(0, 3), (1, 2), (2, 1), (3, 0)])]
            return sum([g.astype(F32) for g in got], p[0]).astype(BF16)

        du1 = sum_far(du_part)
        *finals, sent1 = run_experts(tabs, lists, 1, 1, x1o, w_mix[1], dy1o, None, weights, g1, None, False, False)
        du1 = spread(du1)
        du1o = across(du1)
        got1 = move(sent1, 'core')
        out = run_experts(tabs, lists, 0, 0, x0, w_mix[0], du1, w_mix[1], weights, None, None, False, True)
        du_part, g0 = out[:4], out[4]
        y1 = sum_far(y_part)
        du0 = sum_far(du_part)
        *finals, sent0 = run_experts(tabs, lists, 0, 1, x0o, w_mix[0], du1o, w_mix[1], weights, g0, finals, False, False)
        got0 = move(sent0, 'core')
        finals = place(partner, 1, got1, finals)

        tx = lambda x, du: jnp.einsum('td,te->de', x, du, preferred_element_type=F32)
        g_mix1 = tx(jnp.concatenate(list(x1) + list(x1o)), jnp.concatenate(list(du1) + list(du1o)))
        dx0 = (du0.astype(F32) + jnp.einsum('te,de->td', du0, w_mix[0], preferred_element_type=F32)).astype(BF16)
        g_mix0 = lax.psum(tx(tokens, du0).astype(BF16), tok_axes)
        g_mix = jnp.stack([g_mix0, g_mix1.astype(BF16)])
        finals = place(partner, 0, got0, finals)
        return (y1, dx0, g_mix, jnp.swapaxes(finals[0], 2, 3), jnp.swapaxes(finals[1], 2, 3), finals[2])

    return jax.shard_map(device_step, mesh=sub,
                         in_specs=(tok_spec, tok_spec, route_spec, route_spec, whole_spec,
                                   expert_spec, expert_spec, expert_spec),
                         out_specs=(tok_spec, tok_spec, whole_spec, expert_spec, expert_spec, expert_spec),
                         check_vma=False)
```

```python
import functools

import jax
import jax.numpy as jnp
from jax import lax
from jax.experimental import pallas as pl
from jax.experimental.pallas import tpu as pltpu
from jax.sharding import Mesh, PartitionSpec as P

F32, BF16, I32 = jnp.float32, jnp.bfloat16, jnp.int32
MESH = pl.DeviceIdType.MESH
ROWS = 384
GRP = 8
PITCH = 8
HALF = 4
CAP_FACTOR = 3
LANES = 128
N_SRC = 4
Y, CORE, X = 1, 2, 4
VMEM_LIMIT = 62 * 1024 * 1024
PER_TILE = ROWS // GRP
ROW_BOUND, ROW_GOFF, ROW_EXPERT, TAB_ROWS = 32, 33, 34, 40
SLOT_GROUPS = 256


def cdiv(a, b):
    return (a + b - 1) // b


def spans(d):
    return [(LANES * j, min(LANES, d - LANES * j)) for j in range(cdiv(d, LANES))]


any_space = pl.BlockSpec(memory_space=pl.ANY)
in_vmem = pl.BlockSpec(memory_space=pltpu.VMEM)


def sorted_list(expert_ids, gate_vals):
    n_tok, top = expert_ids.shape
    n = n_tok * top
    keys = expert_ids.reshape(n) * n + jnp.arange(n, dtype=I32)
    keys, gates = lax.sort((keys, gate_vals.reshape(n)), num_keys=1)
    return ((keys % n) // top).astype(F32), gates


def plan_kernel(n_layers, n_local, n_tok, list_rows, all_ref, tab_ref, idx_ref, gate_ref):
    n_mine = n_local // 2
    core, ep = lax.axis_index('core'), lax.axis_index('ep')
    list_len = list_rows * LANES
    lane = lambda n: lax.broadcasted_iota(I32, (n, LANES), 1).astype(F32)
    sub = lambda n: lax.broadcasted_iota(I32, (n, LANES), 0).astype(F32)
    over_lanes = lambda v: jnp.sum(v, axis=1, keepdims=True)
    over_subs = lambda v: jnp.sum(v, axis=0, keepdims=True)
    l16, s16 = lane(n_mine), sub(n_mine)
    for l in range(n_layers):
        cnt = all_ref[:, 2 * n_layers * list_rows + l, :]
        ends = cnt
        step = 1
        while step < 2 * n_local:
            ends = ends + jnp.where(lane(8) >= step, pltpu.roll(ends, step, 1), 0.0)
            step *= 2
        starts = ends - cnt
        second = (ep > 0)
        local = lambda v: jnp.where(lane(8) < n_local, jnp.where(second, pltpu.roll(v, LANES - n_local, 1), v), 0.0)
        cnt, starts = local(cnt), local(starts)
        grp = jnp.floor((cnt + (GRP - 0.5)) * (1.0 / GRP))
        tiles = [jnp.maximum(1.0, jnp.floor((over_subs(grp[h * N_SRC:(h + 1) * N_SRC]) + (PER_TILE - 0.5)) * (1.0 / PER_TILE)))
                 for h in range(2)]
        load = jnp.where(lane(1) < n_local, 3.0 * tiles[0] + 2.0 * tiles[1], -1.0)
        wide = jnp.broadcast_to(load, (n_local, LANES))
        col = over_lanes(jnp.where(lane(n_local) == sub(n_local), wide, 0.0))
        ahead = (col > wide) | ((col == wide) & (sub(n_local) < lane(n_local)))
        rank = over_subs(jnp.where(ahead, 1.0, 0.0))
        odd = s16 - 2.0 * jnp.floor(s16 * 0.5 + 0.25)
        flip = jnp.where(core > 0, 1.0 - odd, odd)
        pick = (jnp.broadcast_to(rank, (n_mine, LANES)) == 2.0 * s16 + flip) & (l16 < n_local)
        mine = lambda row: over_lanes(jnp.where(pick, jnp.broadcast_to(row, (n_mine, LANES)), 0.0))
        as_row = lambda c: over_subs(jnp.where(l16 == s16, c, 0.0))
        experts = as_row(mine(lane(1)))
        for h in range(2):
            at = (h * n_layers + l) * TAB_ROWS
            off = jnp.zeros((n_mine, 1), F32)
            pos = [jnp.zeros((n_mine, LANES), F32) for _ in range(SLOT_GROUPS // LANES)]
            for s in range(N_SRC):
                r = h * N_SRC + s
                c, st = mine(cnt[r:r + 1]), mine(starts[r:r + 1]) + float(s * list_len)
                ng = jnp.floor((c + (GRP - 0.5)) * (1.0 / GRP))
                for i in range(len(pos)):
                    rel = l16 + float(LANES * i) - off
                    code = (st + GRP * rel) * 16.0 + jnp.minimum(float(GRP), c - GRP * rel)
                    pos[i] = jnp.where((rel >= 0) & (rel < ng), code, pos[i])
                off = off + ng
            for i in range(len(pos)):
                tab_ref[pl.ds(at + i, n_mine, stride=len(pos)), :] = pos[i].astype(I32)
            n_tiles = jnp.maximum(1.0, jnp.floor((off + (PER_TILE - 0.5)) * (1.0 / PER_TILE)))
            bounds = over_subs(jnp.where(s16 < l16, n_tiles, 0.0))
            before = over_lanes(jnp.where(l16 == s16, jnp.broadcast_to(bounds, (n_mine, LANES)), 0.0))
            t = jnp.minimum(l16, over_subs(jnp.broadcast_to(n_tiles, (n_mine, LANES))) - 1.0)
            inside = (t >= before) & (t < before + n_tiles)
            goff = over_subs(jnp.where(inside, s16 * float(SLOT_GROUPS) + (t - before) * float(PER_TILE), 0.0))
            rows = [(ROW_BOUND, bounds), (ROW_GOFF, goff), (ROW_EXPERT, experts)]
            for row, value in rows:
                tab_ref[at + row:at + row + 1, :] = value.astype(I32)
    for h in range(2):
        for l in range(n_layers):
            pad = (h * n_layers + l) * (N_SRC * list_rows + 8) + N_SRC * list_rows
            gate_ref[pad:pad + 8, :] = jnp.zeros((8, LANES), F32)
            for s in range(N_SRC):
                to = ((h * n_layers + l) * N_SRC + s) * list_rows
                toks = all_ref[h * N_SRC + s, l * list_rows:(l + 1) * list_rows, :]
                idx_ref[to:to + list_rows, :] = ((toks + float(s * n_tok)) * float(PITCH)).astype(I32)
                to = (h * n_layers + l) * (N_SRC * list_rows + 8) + s * list_rows
                gate_ref[to:to + list_rows, :] = all_ref[
                    h * N_SRC + s, (n_layers + l) * list_rows:(n_layers + l + 1) * list_rows, :]


def plan(shared, n_layers, n_local, n_tok, list_rows):
    n_tab = 2 * n_layers * TAB_ROWS
    n_list = 2 * n_layers * N_SRC * list_rows
    n_gate = 2 * n_layers * (N_SRC * list_rows + 8)
    tab, idx, gates = pl.pallas_call(
        functools.partial(plan_kernel, n_layers, n_local, n_tok, list_rows),
        out_shape=[jax.ShapeDtypeStruct((n_tab, LANES), I32), jax.ShapeDtypeStruct((n_list, LANES), I32),
                   jax.ShapeDtypeStruct((n_gate, LANES), F32)],
        in_specs=[in_vmem], out_specs=[in_vmem] * 3,
        cost_estimate=pl.CostEstimate(flops=10 ** 7, bytes_accessed=10 ** 6, transcendentals=0),
        name="plan",
    )(shared)
    return tab.reshape(-1), idx.reshape(-1), gates


def expert_kernel(cfg, *refs):
    fwd, bwd, own, n_blk, d, ff, at0, list_at, list_len, p_f32, n_alias = cfg
    refs = list(refs)
    take = lambda n: [refs.pop(0) for _ in range(n)]
    tab_ref, idx_hbm, gate_ref = take(3)
    u_refs = take(N_SRC)
    dy_refs = take(N_SRC) if bwd else []
    wg_ref, wu_ref, wd_ref = take(3)
    prev = take(1)[0] if bwd and not own else None
    take(n_alias)
    y_outs = take(N_SRC) if fwd else []
    du_outs = take(N_SRC) if bwd and own else []
    grad = take(1)[0] if bwd and own else None
    finals = take(3) if bwd and not own else None
    sent = take(1)[0] if bwd and not own else None
    table, gat = take(2)
    acc, row_ref = take(2) if own else (None, None)
    gu_ref, g_ref, x_u = take(3)
    x_c = take(1)[0] if bwd else None
    ab_ref = take(1)[0]
    dh_ref = take(1)[0] if bwd else None
    h_ref = take(1)[0]
    dab_ref = take(1)[0] if bwd else None
    sums = take(1)[0] if bwd and not own else None
    idx, list_sem = take(2)
    stage_f, stage_b, out_sem = take(3) if own else (None, None, None)

    step = pl.program_id(0)
    cols = spans(d)
    lo = ff // 256 * 256
    hi = ff - lo
    b_at, g_at = at0 + ROW_BOUND * LANES, at0 + ROW_GOFF * LANES
    dot = functools.partial(lax.dot_general, preferred_element_type=F32)
    nn = (((1,), (0,)), ((), ()))
    nt = (((1,), (1,)), ((), ()))
    tn = (((0,), (0,)), ((), ()))
    al = lambda v, m=PITCH: pl.multiple_of(v, m)
    tok_rows = PITCH * N_SRC * n_blk

    glane = lax.broadcasted_iota(I32, (GRP, LANES), 1)
    gsub = lax.broadcasted_iota(I32, (GRP, LANES), 0)

    def group(tile, q):
        return tab_ref[at0 + tab_ref[g_at + tile] + q]

    def gather(tile, q):
        ids = idx.at[pl.ds(group(tile, q) >> 4, GRP)]
        for k in range(GRP):
            gat[pl.ds(al((q * GRP + k) * PITCH), PITCH), :] = table[pl.ds(al(ids[k]), PITCH), :]

    def gate_column(code):
        pos = code >> 4
        row, shift = pos >> 7, pos & (LANES - 1)
        want = glane == gsub + shift
        over = glane == gsub + (shift - LANES)
        here = gate_ref[pl.ds(row, GRP, stride=0), :]
        there = gate_ref[pl.ds(row + 1, GRP, stride=0), :]
        v = jnp.where(want, here, jnp.where(over, there, 0.0))
        return jnp.where(gsub < (code & 15), jnp.sum(v, axis=1, keepdims=True), 0.0)

    def scatter(tile, q):
        ids = idx.at[pl.ds(group(tile, q) >> 4, GRP)]
        new = []
        for k in range(GRP):
            at = pl.ds(al(ids[k]), PITCH)
            new.append((at, acc[at, :] + row_ref[pl.ds(al((q * GRP + k) * PITCH), PITCH), :]))
        for at, value in reversed(new):
            acc[at, :] = value

    def convert(tile):
        for q in range(0, PER_TILE, 2):
            part = []
            for p in (q, q + 1):
                code = group(tile, p)
                rows = [gat[pl.ds(GRP * PITCH * p + j, GRP, stride=PITCH), :] for j in range(PITCH if bwd else HALF)]
                real = gsub < (code & 15)
                gate = gate_column(code)
                g_ref[GRP * p:GRP * (p + 1), :] = gate
                part.append([jnp.where(real, v, 0.0) for v in rows[:HALF]] + [v * gate for v in rows[HALF:]])
            at = slice(GRP * q, GRP * (q + 2))
            for x, o in ((x_u, 0), (x_c, HALF)):
                if x is None:
                    continue
                for j, (c, w) in enumerate(cols):
                    both = jnp.concatenate([part[0][o + j], part[1][o + j]], axis=0)
                    x[at, c:c + w] = both[:, :w].astype(BF16)

    @pl.when(step == 0)
    def _():
        src = pl.ds(list_at, N_SRC * list_len)
        lists = pltpu.make_async_copy(idx_hbm.at[src], idx.at[pl.ds(0, N_SRC * list_len)], list_sem)
        lists.start()
        if own:
            def clear(c, _):
                for k in range(4):
                    acc[pl.ds(al(c * 2048 + 512 * k, 512), 512), :] = jnp.zeros((512, LANES), F32)
                return 0

            lax.fori_loop(0, tok_rows // 2048, clear, 0)
            row_ref[...] = jnp.zeros(row_ref.shape, F32)
        rows = 256
        for srcs, o, seed in ((u_refs, 0, fwd), (dy_refs, HALF, own)):
            for s, ref in enumerate(srcs):
                def fill(c, _, ref=ref, o=o, seed=seed, s=s):
                    r = al(c * rows, rows)
                    at = PITCH * (s * n_blk + r) + o
                    for j in range(HALF):
                        vals = ref[0, pl.ds(r, rows), LANES * j:LANES * (j + 1)].astype(F32)
                        to = pl.ds(at + j, rows, stride=PITCH)
                        table[to, :] = vals
                        if seed and s == 0:
                            acc[to, :] = vals
                    return 0

                lax.fori_loop(0, n_blk // rows, fill, 0)
        lists.wait()
        for k in range(GRP):
            idx[N_SRC * list_len + k] = 0

        def first(q, _):
            gather(0, 2 * q)
            gather(0, 2 * q + 1)
            return 0

        lax.fori_loop(0, PER_TILE // 2, first, 0)
        convert(0)

    for i, w in enumerate((wg_ref, wu_ref)):
        gu_ref[i * lo:(i + 1) * lo, :] = w[0, 0, 0:lo, :]
        gu_ref[2 * lo + i * hi:2 * lo + (i + 1) * hi, :] = w[0, 0, lo:, :]
    total = grad if own else sums
    if bwd:
        total[...] = jnp.zeros(total.shape, F32) if own else prev[0]

    def put_rows(o, value, s0=0):
        value = value.astype(BF16).astype(F32)
        n = value.shape[0]
        for j, (c, w) in enumerate(cols):
            row_ref[pl.ds(PITCH * s0 + o + j, n, stride=PITCH), 0:w] = value[:, c:c + w] * g_ref[s0:s0 + n, 0:w]

    low = lax.broadcasted_iota(I32, (16, 2 * hi), 1) < hi

    def middle(a, b, dh):
        sig = 0.5 * jnp.tanh(0.5 * a) + 0.5
        act = a * sig
        h = act * b
        if dh is None:
            return h, None, None
        slope = sig * (1.0 + a * (1.0 - sig))
        return h, dh * b * slope, dh * act

    def tile(t, _):
        for q in range(PER_TILE):
            if own:
                scatter(jnp.maximum(t - 1, 0), q)
            gather(t + 1, q)
        part = ROWS // 2
        for s0 in range(0, ROWS, part):
            sl = slice(s0, s0 + part)
            ab_ref[sl, :] = dot(x_u[sl, :], gu_ref[...], nt)
            if bwd:
                dh_ref[sl, :] = dot(x_c[sl, :], wd_ref[0, 0], nt)
        for r in range(0, ROWS, 16):
            rows = slice(r, r + 16)
            for c in range(0, lo, LANES):
                h, da, db = middle(ab_ref[rows, c:c + LANES], ab_ref[rows, lo + c:lo + c + LANES],
                                   dh_ref[rows, c:c + LANES] if bwd else None)
                h_ref[rows, c:c + LANES] = h.astype(BF16)
                if bwd:
                    dab_ref[rows, c:c + LANES] = da.astype(BF16)
                    dab_ref[rows, lo + c:lo + c + LANES] = db.astype(BF16)
            a = ab_ref[rows, 2 * lo:]
            b = pltpu.roll(a, hi, 1)
            dh = dh_ref[rows, lo:] if bwd else None
            if bwd:
                dh = jnp.concatenate([dh, dh], axis=1)
            h, da, db = middle(a, b, dh)
            h_ref[rows, lo:] = h[:, :hi].astype(BF16)
            if bwd:
                dab_ref[rows, 2 * lo:] = jnp.where(low, da, pltpu.roll(db, hi, 1)).astype(BF16)
        for s0 in range(0, ROWS, part):
            sl = slice(s0, s0 + part)
            if fwd:
                put_rows(0, dot(h_ref[sl, :], wd_ref[0, 0], nn), s0)
            if bwd and own:
                put_rows(HALF, dot(dab_ref[sl, :], gu_ref[...], nn), s0)
        if bwd:
            view = total.at[0] if own else total
            view[0:2 * ff, :] += dot(dab_ref[...], x_u[...], tn)
            view[2 * ff:, :] += dot(h_ref[...], x_c[...], tn)
        convert(t + 1)
        return 0

    lax.fori_loop(tab_ref[b_at + step], tab_ref[b_at + step + 1], tile, 0)
    if bwd and not own:
        for out in ([f.at[0, 0] for f in finals], [sent.at[0, i] for i in range(3)]):
            for i in range(2):
                out[i][0:lo, :] = sums[i * lo:(i + 1) * lo, :].astype(BF16)
                out[i][lo:, :] = sums[2 * lo + i * hi:2 * lo + (i + 1) * hi, :].astype(BF16)
            out[2][...] = sums[2 * ff:, :].astype(BF16)

    if own:
        @pl.when(step == pl.num_programs(0) - 1)
        def _():
            end = tab_ref[b_at + step + 1] - 1
            lax.fori_loop(0, PER_TILE, lambda q, _: (scatter(end, q), 0)[1], 0)
            chunk = stage_f.shape[1]
            flights = {}
            n = 0
            for o, out in ((HALF, du_outs), (0, y_outs)):
                for s in range(N_SRC if out else 0):
                    wide = s == 0 or p_f32
                    stage = stage_f if wide else stage_b
                    for c in range(n_blk // chunk):
                        key = (wide, n % 2)
                        if key in flights:
                            flights.pop(key).wait()
                        for j in range(HALF):
                            rows = pl.ds(PITCH * (s * n_blk + c * chunk) + o + j, chunk, stride=PITCH)
                            stage[n % 2, :, LANES * j:LANES * (j + 1)] = acc[rows, :].astype(stage.dtype)
                        flights[key] = pltpu.make_async_copy(
                            stage.at[n % 2], out[s].at[pl.ds(c * chunk, chunk), :], out_sem.at[2 * wide + n % 2])
                        flights[key].start()
                        n += 1
            for copy in flights.values():
                copy.wait()


def run_experts(routes, layer, half, u, dy, weights, prev, finals, fwd, own, p_f32=False):
    tab, idx, gates = routes
    bwd = dy is not None
    wg, wu, wd = weights
    _, n_blk, wide = u[0].shape
    n_layers, n_local, ff, d = wd.shape
    n_exp = n_local // 2
    row_id = half * n_layers + layer
    at0 = row_id * TAB_ROWS * LANES
    e_at = at0 + ROW_EXPERT * LANES
    list_len = idx.shape[0] // (2 * n_layers * N_SRC)

    block = lambda i: pl.BlockSpec((1, n_blk, wide), lambda e, *_: (i, 0, 0), pipeline_mode=pl.Buffered(1))
    blocks = [block(0), block(1)] * 2
    weight = pl.BlockSpec((1, 1, ff, d), lambda e, tab: (layer, tab[e_at + e], 0, 0))
    partial = pl.BlockSpec((1, 3 * ff, d), lambda e, *_: (e, 0, 0))

    four = lambda pairs: [pairs[0], pairs[0], pairs[1], pairs[1]]
    operands = [idx, gates] + four(u) + (four(dy) if bwd else []) + [wg, wu, wd]
    gate_rows = N_SRC * list_len // LANES + 8
    gate_spec = pl.BlockSpec((gate_rows, LANES), lambda e, *_: (row_id, 0), pipeline_mode=pl.Buffered(1))
    in_specs = [any_space, gate_spec] + blocks * (1 + bwd) + [weight] * 3
    out_shape, out_specs, aliases = [], [], {}
    for use in (fwd, bwd and own):
        if use:
            out_shape += [jax.ShapeDtypeStruct((n_blk, wide), F32 if s == 0 or p_f32 else BF16) for s in range(N_SRC)]
            out_specs += [any_space] * N_SRC
    if bwd and own:
        out_shape.append(jax.ShapeDtypeStruct((n_exp, 3 * ff, d), F32))
        out_specs.append(partial)
    if bwd and not own:
        operands.append(prev)
        in_specs.append(partial)
        for i, f in enumerate(finals or ()):
            aliases[1 + len(operands)] = i
            operands.append(f)
            in_specs.append(any_space)
        out_shape += [jax.ShapeDtypeStruct((n_layers, n_local, ff, d), BF16)] * 3
        out_specs += [weight] * 3
        out_shape.append(jax.ShapeDtypeStruct((n_exp, 3, ff, d), BF16))
        out_specs.append(pl.BlockSpec((1, 3, ff, d), lambda e, *_: (e, 0, 0, 0)))
    table = pltpu.VMEM((PITCH * N_SRC * n_blk, LANES), F32)
    rows = pltpu.VMEM((PITCH * ROWS, LANES), F32)
    mid = lambda n, dt: pltpu.VMEM((ROWS, n), dt)
    scratch = [table, rows] * (1 + own)
    scratch += [pltpu.VMEM((2 * ff, d), BF16), mid(LANES, F32)] + [mid(d, BF16)] * (1 + bwd) + [mid(2 * ff, F32)]
    scratch += [mid(ff, F32)] * bwd + [mid(ff, BF16)] + [mid(2 * ff, BF16)] * bwd
    if bwd and not own:
        scratch.append(pltpu.VMEM((3 * ff, d), F32))
    scratch += [pltpu.SMEM((N_SRC * list_len + 128,), I32), pltpu.SemaphoreType.DMA]
    if own:
        scratch += [pltpu.VMEM((2, 256, wide), F32), pltpu.VMEM((2, 256, wide), BF16), pltpu.SemaphoreType.DMA((4,))]
    passes = 2 + fwd + bwd * (4 + 2 * own)
    flops = 2 * d * ff * passes * n_blk * N_SRC * 2
    cfg = (fwd, bwd, own, n_blk, d, ff, at0, row_id * N_SRC * list_len, list_len, p_f32, len(aliases))
    return pl.pallas_call(
        functools.partial(expert_kernel, cfg),
        out_shape=out_shape,
        grid_spec=pltpu.PrefetchScalarGridSpec(
            num_scalar_prefetch=1, grid=(n_exp,), in_specs=in_specs, out_specs=out_specs, scratch_shapes=scratch),
        input_output_aliases=aliases,
        compiler_params=pltpu.CompilerParams(dimension_semantics=("arbitrary",), vmem_limit_bytes=VMEM_LIMIT),
        cost_estimate=pl.CostEstimate(flops=flops, bytes_accessed=3 * 2 * n_exp * d * ff, transcendentals=0),
        name=f"experts_{'f' if fwd else ''}{'b' if bwd else ''}_{'own' if own else 'other'}_{layer}",
    )(tab, *operands)


def place_kernel(layer, n_exp, tab_at, tab_ref, got_ref, *refs):
    outs, (buf, in_sem, out_sem) = refs[3:6], refs[6:]
    reads = [pltpu.make_async_copy(got_ref.at[i], buf.at[i], in_sem.at[i]) for i in range(n_exp)]
    for read in reads:
        read.start()
    writes = []
    for i, read in enumerate(reads):
        read.wait()
        e = tab_ref[tab_at + i]
        for k, out in enumerate(outs):
            writes.append(pltpu.make_async_copy(buf.at[i, k], out.at[layer, e], out_sem.at[i, k]))
            writes[-1].start()
    for write in writes:
        write.wait()


def place(partner, layer, got, finals):
    n_exp = got.shape[0]
    return pl.pallas_call(
        functools.partial(place_kernel, layer, n_exp, layer * n_exp),
        out_shape=[jax.ShapeDtypeStruct(f.shape, f.dtype) for f in finals],
        grid_spec=pltpu.PrefetchScalarGridSpec(
            num_scalar_prefetch=1, grid=(1,), in_specs=[any_space] * 4, out_specs=[any_space] * 3,
            scratch_shapes=[pltpu.VMEM(got.shape, got.dtype), pltpu.SemaphoreType.DMA((n_exp,)),
                            pltpu.SemaphoreType.DMA((n_exp, 3))]),
        input_output_aliases={2: 0, 3: 1, 4: 2},
        compiler_params=pltpu.CompilerParams(vmem_limit_bytes=VMEM_LIMIT),
        cost_estimate=pl.CostEstimate(flops=0, bytes_accessed=4 * got.size, transcendentals=0),
        name=f"place_{layer}",
    )(partner, got, *finals)


def peer(rel):
    return {name: (lax.axis_index(name) + ((rel >> bit) & 1)) % 2 for bit, name in enumerate(("ep", "core", "x"))}


def meet(rels):
    barrier = pltpu.get_barrier_semaphore()
    for rel in rels:
        pl.semaphore_signal(barrier, inc=1, device_id=peer(rel), device_id_type=MESH)
    pl.semaphore_wait(barrier, len(rels))


def remote(src, dst, send, recv, rel):
    return pltpu.make_async_remote_copy(src_ref=src, dst_ref=dst, send_sem=send, recv_sem=recv,
                                        device_id=peer(rel), device_id_type=MESH)


def share_kernel(n_rel, mine_ref, all_ref, send_sem, recv_sem):
    meet(range(1, n_rel))
    copies = [remote(mine_ref, all_ref.at[rel], send_sem.at[rel], recv_sem.at[rel], rel) for rel in range(1, n_rel)]
    for copy in copies:
        copy.start()
    all_ref[0] = mine_ref[...]
    for copy in copies:
        copy.wait()


def share(mine, n_rel):
    return pl.pallas_call(
        functools.partial(share_kernel, n_rel),
        out_shape=jax.ShapeDtypeStruct((n_rel,) + mine.shape, mine.dtype),
        in_specs=[in_vmem],
        out_specs=in_vmem,
        scratch_shapes=[pltpu.SemaphoreType.DMA((n_rel,)), pltpu.SemaphoreType.DMA((n_rel,))],
        compiler_params=pltpu.CompilerParams(collective_id=0, has_side_effects=True),
        cost_estimate=pl.CostEstimate(flops=10 ** 7, bytes_accessed=mine.size * 4 * n_rel, transcendentals=0),
        name="share_lists",
    )(mine)


def blocks_kernel(cfg, *refs):
    n_chunk, reduce, across, back, d = cfg
    refs = list(refs)
    take = lambda n: [refs.pop(0) for _ in range(n)]
    parts = take(N_SRC)
    m_ref, o_total, o_a, o_b = take(4)
    o_xa, o_xb = take(2) if across else (None, None)
    in_f, in_b, got_f, s_buf, r_buf, t_buf, u_buf, load, send, recv, put = take(11)
    n_rows = t_buf.shape[0] // n_chunk
    cut = [pl.ds(k * n_rows, n_rows) for k in range(n_chunk)]
    chunks = range(n_chunk)
    loads = {}
    for i, part in enumerate(parts[:2] if reduce else parts):
        buf = in_f.at[i] if reduce or i == 0 else in_b.at[i - 1]
        for k in chunks:
            loads[i, k] = pltpu.make_async_copy(part.at[cut[k]], buf.at[cut[k]], load.at[i, k])
    order = (1, 0) if reduce else range(N_SRC)
    for i in order:
        for k in chunks:
            loads[i, k].start()
    u_buf[...] = jnp.zeros(u_buf.shape, BF16)
    meet((Y, CORE, X) if across else (Y, CORE))
    links = []

    def link(src, dst, rel):
        n = len(links)
        links.append([remote(src.at[cut[k]], dst.at[cut[k]], send.at[n, k], recv.at[n, k], rel) for k in chunks])
        return links[-1]

    if reduce:
        first = link(parts[3], got_f.at[1], CORE)
        second = link(parts[2], got_f.at[0], CORE)
        over = link(s_buf, r_buf, Y)
        for copies in (first, second):
            for copy in copies:
                copy.start()
        for k in chunks:
            loads[1, k].wait()
            first[k].wait_recv()
            s_buf[cut[k], :] = (in_f[1, cut[k], :] + got_f[1, cut[k], :]).astype(BF16)
            over[k].start()
    to_y = link(u_buf, o_a.at[1], Y)
    to_core = link(u_buf, o_b.at[0], CORE)
    to_x = link(u_buf, o_xa.at[0], X) if across else None
    puts = []
    for k in chunks:
        if reduce:
            loads[0, k].wait()
            second[k].wait_recv()
            over[k].wait_recv()
            total = in_f[0, cut[k], :] + got_f[0, cut[k], :] + r_buf[cut[k], :].astype(F32)
        else:
            for i in range(N_SRC):
                loads[i, k].wait()
            total = in_f[0, cut[k], :]
            for i in range(N_SRC - 1):
                total = total + in_b[i, cut[k], :].astype(F32)
        total = total.astype(BF16)
        t_buf[cut[k], :] = total
        dims = (((1,), (1 if back else 0,)), ((), ()))
        mixed = lax.dot_general(total[:, :d], m_ref[...], dims, preferred_element_type=F32)
        u_buf[cut[k], 0:d] = (total[:, :d].astype(F32) + mixed).astype(BF16)
        to_y[k].start()
        to_core[k].start()
        if across:
            to_x[k].start()
        puts.append(pltpu.make_async_copy(u_buf.at[cut[k]], o_a.at[0, cut[k]], put.at[0, k]))
        puts.append(pltpu.make_async_copy(t_buf.at[cut[k]], o_total.at[cut[k]], put.at[1, k]))
        for copy in puts[-2:]:
            copy.start()
    on = link(o_a.at[1], o_b.at[1], CORE)
    on_x = link(o_a.at[1], o_xa.at[1], X) if across else None
    for k in chunks:
        to_y[k].wait_recv()
        on[k].start()
        if across:
            on_x[k].start()
    if across:
        last = [link(o_xa.at[i], o_xb.at[i], CORE) for i in range(2)]
        for i, arrived in enumerate((to_x, on_x)):
            for k in chunks:
                arrived[k].wait_recv()
                last[i][k].start()
    waited = [to_y] + ([first, second, over] if reduce else []) + ([to_x, on_x] if across else [])
    for copies in links:
        for copy in copies:
            if any(copies is w for w in waited):
                copy.wait_send()
            else:
                copy.wait()
    for copy in puts:
        copy.wait()


def complete_blocks(parts, m, reduce, across, back, ident, n_chunk=4):
    n_blk, wide = parts[0].shape
    d = m.shape[0]
    sem = lambda *s: pltpu.SemaphoreType.DMA(s)
    pair = jax.ShapeDtypeStruct((2, n_blk, wide), BF16)
    buf = lambda n, dt: pltpu.VMEM((n, n_blk, wide) if n else (n_blk, wide), dt)
    return pl.pallas_call(
        functools.partial(blocks_kernel, (n_chunk, reduce, across, back, d)),
        out_shape=[jax.ShapeDtypeStruct((n_blk, wide), BF16)] + [pair] * (4 if across else 2),
        in_specs=[any_space] * N_SRC + [in_vmem],
        out_specs=[any_space] * (5 if across else 3),
        scratch_shapes=[buf(2, F32), buf(3, BF16), buf(2, F32), buf(0, BF16), buf(0, BF16), buf(0, BF16), buf(0, BF16),
                        sem(4, n_chunk), sem(10, n_chunk), sem(10, n_chunk), sem(2, n_chunk)],
        compiler_params=pltpu.CompilerParams(collective_id=ident, has_side_effects=True, vmem_limit_bytes=VMEM_LIMIT),
        cost_estimate=pl.CostEstimate(flops=10 ** 8, bytes_accessed=n_blk * wide * 40, transcendentals=0),
        name=f"complete_blocks_{ident}",
    )(*parts, m)


def total_kernel(n_chunk, g_ref, o_ref, give, got, s_buf, y_buf, t_buf, x_buf, z_buf, send, recv):
    core = lax.axis_index('core')
    n_rows = o_ref.shape[1] // n_chunk
    cut = [pl.ds(k * n_rows, n_rows) for k in range(n_chunk)]
    first = core > 0
    give[...] = jnp.where(first, g_ref[0], g_ref[1])
    meet((Y, CORE, X))
    copies = [[remote(src.at[cut[k]], dst.at[cut[k]], send.at[i, k], recv.at[i, k], rel) for k in range(n_chunk)]
              for i, (src, dst, rel) in enumerate(((give, got, CORE), (s_buf, y_buf, Y), (t_buf, x_buf, X)))]
    for copy in copies[0]:
        copy.start()
    for k in range(n_chunk):
        copies[0][k].wait_recv()
        mine = jnp.where(first, g_ref[1, cut[k], :], g_ref[0, cut[k], :])
        s_buf[cut[k], :] = (mine + got[cut[k], :]).astype(BF16)
        copies[1][k].start()
    for k in range(n_chunk):
        copies[1][k].wait_recv()
        t_buf[cut[k], :] = (s_buf[cut[k], :].astype(F32) + y_buf[cut[k], :].astype(F32)).astype(BF16)
        copies[2][k].start()
    for k in range(n_chunk):
        copies[2][k].wait_recv()
        got[cut[k], :] = t_buf[cut[k], :].astype(F32) + x_buf[cut[k], :].astype(F32)
    for group in copies:
        for copy in group:
            copy.wait_send()
    s_buf[...] = got[...].astype(BF16)
    swap = remote(s_buf, z_buf, send.at[3, 0], recv.at[3, 0], CORE)
    swap.start()
    swap.wait()
    o_ref[0] = jnp.where(first, z_buf[...], s_buf[...])
    o_ref[1] = jnp.where(first, s_buf[...], z_buf[...])


def total_grads(g, ident, n_chunk=4):
    _, d, _ = g.shape
    buf = lambda dt: pltpu.VMEM((d, d), dt)
    return pl.pallas_call(
        functools.partial(total_kernel, n_chunk),
        out_shape=jax.ShapeDtypeStruct(g.shape, BF16),
        in_specs=[in_vmem], out_specs=in_vmem,
        scratch_shapes=[buf(F32), buf(F32), buf(BF16), buf(BF16), buf(BF16), buf(BF16), buf(BF16),
                        pltpu.SemaphoreType.DMA((4, n_chunk)), pltpu.SemaphoreType.DMA((4, n_chunk))],
        compiler_params=pltpu.CompilerParams(collective_id=ident, has_side_effects=True),
        cost_estimate=pl.CostEstimate(flops=10 ** 7, bytes_accessed=g.size * 8, transcendentals=0),
        name="total_grads",
    )(g)


def solution(mesh):
    ep_size, dp_size = mesh.shape['ep'], mesh.shape['dp']
    sub = Mesh(mesh.devices.reshape(ep_size, dp_size // 2, 2), ('ep', 'x', 'core'))
    tok_axes = ('x', 'core', 'ep')
    tok_spec = P(tok_axes, None)
    route_spec = P(None, tok_axes, None)
    whole_spec = P(None, None, None)
    expert_spec = P(None, 'ep', None, None)
    flip = [(0, 1), (1, 0)]
    move = lambda v, axis: lax.ppermute(v, axis, flip)
    move_diag = lambda v: lax.ppermute(v, ('ep', 'core'), [(0, 3), (1, 2), (2, 1), (3, 0)])
    fence = lax.optimization_barrier

    def device_step(tokens, d_out, expert_ids, gate_vals, w_mix, w_gate, w_up, w_down):
        n_layers, d = w_mix.shape[0], w_mix.shape[1]
        n_tok = tokens.shape[0]
        top = expert_ids.shape[2]
        n_local = w_gate.shape[1]
        n_exp = n_local * ep_size
        n = n_tok * top
        n_rel = 2 * N_SRC
        wide = cdiv(d, LANES) * LANES
        weights = (jnp.swapaxes(w_gate, 2, 3), jnp.swapaxes(w_up, 2, 3), w_down)
        pad = lambda v: jnp.pad(v, ((0, 0), (0, wide - d)))
        send_three = lambda p: [move(p[1], 'ep'), move(p[2], 'core'), move_diag(p[3])]

        def own_sum(p, got):
            return sum([g.astype(F32) for g in got], p)[:, :d].astype(BF16)

        u0 = pad((tokens.astype(F32) + jnp.dot(tokens, w_mix[0], preferred_element_type=F32)).astype(BF16))
        u0_far = move(u0, 'ep')
        lists = [sorted_list(expert_ids[l], gate_vals[l]) for l in range(n_layers)]
        counts = jnp.sum((expert_ids.reshape(n_layers, n, 1) == jnp.arange(n_exp, dtype=I32)).astype(F32), axis=1)
        packed = jnp.concatenate([jnp.concatenate([v[0] for v in lists] + [v[1] for v in lists]).reshape(-1, LANES),
                                  jnp.pad(counts, ((0, 8 - n_layers), (0, LANES - n_exp)))], axis=0)
        shared = share(packed, n_rel)
        routes = plan(shared, n_layers, n_local, n_tok, n // LANES)
        row = lambda l: lax.slice_in_dim(routes[0], (l * TAB_ROWS + ROW_EXPERT) * LANES,
                                         (l * TAB_ROWS + ROW_EXPERT) * LANES + n_local // 2)
        partner = move(jnp.concatenate([row(l) for l in range(n_layers)]), 'core')
        u0_a = jnp.stack([u0, u0_far])
        u0_b = move(u0_a, 'core')

        dy, shared = fence((pad(d_out), shared))
        dy_a = jnp.stack([dy, move(dy, 'ep')])
        part = run_experts(routes, 0, 0, (u0_a, u0_b), None, weights, None, None, True, True, p_f32=True)
        dy_b = move(dy_a, 'core')
        y0, u1_a, u1_b, u1_xa, u1_xb = complete_blocks(part, w_mix[1], True, True, False, 1)
        dy_a, u0_a2, y0 = fence((dy_a, u0_a, y0))
        dy_xa, u0_xa = move(dy_a, 'x'), move(u0_a2, 'x')
        out = run_experts(routes, 1, 0, (u1_a, u1_b), (dy_a, dy_b), weights, None, None, True, True)
        y_part, du_part, g1 = out[:4], out[4:8], out[8]
        dy_xb, u0_xb = move(dy_xa, 'core'), move(u0_xa, 'core')
        got = send_three(du_part)
        out = run_experts(routes, 1, 1, (u1_xa, u1_xb), (dy_xa, dy_xb), weights, g1, None, False, False)
        got, out = fence((got, out))
        *finals, sent1 = out
        du1, dx_a, dx_b = complete_blocks([du_part[0], *got], w_mix[1], False, False, True, 2)
        dx_a, y_part, sent1 = fence((dx_a, y_part, sent1))
        dx_xa = move(dx_a, 'x')
        got_y = send_three(y_part)
        got1 = move(sent1, 'core')
        out = run_experts(routes, 0, 0, (u0_a, u0_b), (dx_a, dx_b), weights, None, None, False, True)
        dx_xa, got_y, out = fence((dx_xa, got_y, out))
        du_part, g0 = out[:4], out[4]
        dx_xb = move(dx_xa, 'core')
        got = send_three(du_part)
        out = run_experts(routes, 0, 1, (u0_xa, u0_xb), (dx_xa, dx_xb), weights, g0, finals, False, False)
        got, got1, out = fence((got, got1, out))
        *finals, sent0 = out
        got0 = move(sent0, 'core')
        du0 = own_sum(du_part[0], got)
        finals = place(partner, 1, got1, finals)
        y1 = own_sum(y_part[0], got_y)
        tx = lambda x, du: jnp.einsum('td,te->de', x, du, preferred_element_type=F32)
        g_mix = total_grads(jnp.stack([tx(tokens, du0), tx(y0[:, :d], du1[:, :d])]), 3)
        dx0 = (du0.astype(F32) + jnp.einsum('te,de->td', du0, w_mix[0], preferred_element_type=F32)).astype(BF16)
        finals, got0, g_mix = fence((finals, got0, g_mix))
        finals = place(partner, 0, got0, finals)
        return (y1, dx0, g_mix, jnp.swapaxes(finals[0], 2, 3), jnp.swapaxes(finals[1], 2, 3), finals[2])

    return jax.shard_map(device_step, mesh=sub,
                         in_specs=(tok_spec, tok_spec, route_spec, route_spec, whole_spec,
                                   expert_spec, expert_spec, expert_spec),
                         out_specs=(tok_spec, tok_spec, whole_spec, expert_spec, expert_spec, expert_spec),
                         check_vma=False)
```

```python
import functools

import jax
import jax.numpy as jnp
from jax import lax
from jax.experimental import pallas as pl
from jax.experimental.pallas import tpu as pltpu
from jax.sharding import Mesh, PartitionSpec as P

F32, BF16, I32 = jnp.float32, jnp.bfloat16, jnp.int32
MESH = pl.DeviceIdType.MESH
ROWS = 384
GRP = 8
PITCH = 8
HALF = 4
CAP_FACTOR = 3
LANES = 128
N_SRC = 4
Y, CORE, X = 1, 2, 4
VMEM_LIMIT = 62 * 1024 * 1024
PER_TILE = ROWS // GRP
ROW_BOUND, ROW_GOFF, ROW_EXPERT, ROW_PARTNER, TAB_ROWS = 32, 33, 34, 35, 40
SLOT_GROUPS = 256


def cdiv(a, b):
    return (a + b - 1) // b


def spans(d):
    return [(LANES * j, min(LANES, d - LANES * j)) for j in range(cdiv(d, LANES))]


any_space = pl.BlockSpec(memory_space=pl.ANY)
in_vmem = pl.BlockSpec(memory_space=pltpu.VMEM)


def sorted_list(expert_ids, gate_vals):
    n_tok, top = expert_ids.shape
    n = n_tok * top
    keys = expert_ids.reshape(n) * n + jnp.arange(n, dtype=I32)
    keys, gates = lax.sort((keys, gate_vals.reshape(n)), num_keys=1)
    return ((keys % n) // top).astype(F32), gates


def plan_kernel(n_layers, n_local, n_tok, list_rows, all_ref, tab_ref, idx_ref, gate_ref):
    n_mine = n_local // 2
    core, ep = lax.axis_index('core'), lax.axis_index('ep')
    list_len = list_rows * LANES
    lane = lambda n: lax.broadcasted_iota(I32, (n, LANES), 1).astype(F32)
    sub = lambda n: lax.broadcasted_iota(I32, (n, LANES), 0).astype(F32)
    over_lanes = lambda v: jnp.sum(v, axis=1, keepdims=True)
    over_subs = lambda v: jnp.sum(v, axis=0, keepdims=True)
    l16, s16 = lane(n_mine), sub(n_mine)
    for l in range(n_layers):
        cnt = all_ref[:, 2 * n_layers * list_rows + l, :]
        ends = cnt
        step = 1
        while step < 2 * n_local:
            ends = ends + jnp.where(lane(8) >= step, pltpu.roll(ends, step, 1), 0.0)
            step *= 2
        starts = ends - cnt
        second = (ep > 0)
        local = lambda v: jnp.where(lane(8) < n_local, jnp.where(second, pltpu.roll(v, LANES - n_local, 1), v), 0.0)
        cnt, starts = local(cnt), local(starts)
        grp = jnp.floor((cnt + (GRP - 0.5)) * (1.0 / GRP))
        tiles = [jnp.maximum(1.0, jnp.floor((over_subs(grp[h * N_SRC:(h + 1) * N_SRC]) + (PER_TILE - 0.5)) * (1.0 / PER_TILE)))
                 for h in range(2)]
        load = jnp.where(lane(1) < n_local, 3.0 * tiles[0] + 2.0 * tiles[1], -1.0)
        wide = jnp.broadcast_to(load, (n_local, LANES))
        col = over_lanes(jnp.where(lane(n_local) == sub(n_local), wide, 0.0))
        ahead = (col > wide) | ((col == wide) & (sub(n_local) < lane(n_local)))
        rank = over_subs(jnp.where(ahead, 1.0, 0.0))
        odd = s16 - 2.0 * jnp.floor(s16 * 0.5 + 0.25)
        flip = jnp.where(core > 0, 1.0 - odd, odd)
        dealt = lambda f: (jnp.broadcast_to(rank, (n_mine, LANES)) == 2.0 * s16 + f) & (l16 < n_local)
        pick = dealt(flip)
        choose = lambda p, row: over_lanes(jnp.where(p, jnp.broadcast_to(row, (n_mine, LANES)), 0.0))
        mine = lambda row: choose(pick, row)
        as_row = lambda c: over_subs(jnp.where(l16 == s16, c, 0.0))
        experts = as_row(mine(lane(1)))
        partner = as_row(choose(dealt(1.0 - flip), lane(1)))
        for h in range(2):
            at = (h * n_layers + l) * TAB_ROWS
            off = jnp.zeros((n_mine, 1), F32)
            pos = [jnp.zeros((n_mine, LANES), F32) for _ in range(SLOT_GROUPS // LANES)]
            for s in range(N_SRC):
                r = h * N_SRC + s
                c, st = mine(cnt[r:r + 1]), mine(starts[r:r + 1]) + float(s * list_len)
                ng = jnp.floor((c + (GRP - 0.5)) * (1.0 / GRP))
                for i in range(len(pos)):
                    rel = l16 + float(LANES * i) - off
                    code = (st + GRP * rel) * 16.0 + jnp.minimum(float(GRP), c - GRP * rel)
                    pos[i] = jnp.where((rel >= 0) & (rel < ng), code, pos[i])
                off = off + ng
            for i in range(len(pos)):
                tab_ref[pl.ds(at + i, n_mine, stride=len(pos)), :] = pos[i].astype(I32)
            n_tiles = jnp.maximum(1.0, jnp.floor((off + (PER_TILE - 0.5)) * (1.0 / PER_TILE)))
            bounds = over_subs(jnp.where(s16 < l16, n_tiles, 0.0))
            before = over_lanes(jnp.where(l16 == s16, jnp.broadcast_to(bounds, (n_mine, LANES)), 0.0))
            t = jnp.minimum(l16, over_subs(jnp.broadcast_to(n_tiles, (n_mine, LANES))) - 1.0)
            inside = (t >= before) & (t < before + n_tiles)
            goff = over_subs(jnp.where(inside, s16 * float(SLOT_GROUPS) + (t - before) * float(PER_TILE), 0.0))
            rows = [(ROW_BOUND, bounds), (ROW_GOFF, goff), (ROW_EXPERT, experts), (ROW_PARTNER, partner)]
            for row, value in rows:
                tab_ref[at + row:at + row + 1, :] = value.astype(I32)
    for h in range(2):
        for l in range(n_layers):
            pad = (h * n_layers + l) * (N_SRC * list_rows + 8) + N_SRC * list_rows
            gate_ref[pad:pad + 8, :] = jnp.zeros((8, LANES), F32)
            for s in range(N_SRC):
                to = ((h * n_layers + l) * N_SRC + s) * list_rows
                toks = all_ref[h * N_SRC + s, l * list_rows:(l + 1) * list_rows, :]
                idx_ref[to:to + list_rows, :] = ((toks + float(s * n_tok)) * float(PITCH)).astype(I32)
                to = (h * n_layers + l) * (N_SRC * list_rows + 8) + s * list_rows
                gate_ref[to:to + list_rows, :] = all_ref[
                    h * N_SRC + s, (n_layers + l) * list_rows:(n_layers + l + 1) * list_rows, :]


def plan(shared, n_layers, n_local, n_tok, list_rows):
    n_tab = 2 * n_layers * TAB_ROWS
    n_list = 2 * n_layers * N_SRC * list_rows
    n_gate = 2 * n_layers * (N_SRC * list_rows + 8)
    tab, idx, gates = pl.pallas_call(
        functools.partial(plan_kernel, n_layers, n_local, n_tok, list_rows),
        out_shape=[jax.ShapeDtypeStruct((n_tab, LANES), I32), jax.ShapeDtypeStruct((n_list, LANES), I32),
                   jax.ShapeDtypeStruct((n_gate, LANES), F32)],
        in_specs=[in_vmem], out_specs=[in_vmem] * 3,
        cost_estimate=pl.CostEstimate(flops=10 ** 7, bytes_accessed=10 ** 6, transcendentals=0),
        name="plan",
    )(shared)
    return tab.reshape(-1), idx.reshape(-1), gates


def expert_kernel(cfg, *refs):
    fwd, bwd, own, layer, n_blk, d, ff, at0, list_at, list_len, p_f32, n_alias, got_layer, got_at = cfg
    refs = list(refs)
    take = lambda n: [refs.pop(0) for _ in range(n)]
    tab_ref, idx_hbm, gate_ref = take(3)
    u_refs = take(N_SRC)
    dy_refs = take(N_SRC) if bwd else []
    wg_ref, wu_ref, wd_ref = take(3)
    prev = take(1)[0] if bwd and not own else None
    got = take(1)[0] if got_layer is not None else None
    take(n_alias)
    y_outs = take(N_SRC) if fwd else []
    du_outs = take(N_SRC) if bwd and own else []
    grad = take(1)[0] if bwd and own else None
    finals = take(3) if bwd and not own else None
    sent = take(1)[0] if bwd and not own else None
    table, gat = take(2)
    acc, row_ref = take(2) if own else (None, None)
    gu_ref, g_ref, x_u = take(3)
    x_c = take(1)[0] if bwd else None
    ab_ref = take(1)[0]
    dh_ref = take(1)[0] if bwd else None
    h_ref = take(1)[0]
    dab_ref = take(1)[0] if bwd else None
    sums, fin_sem = take(2) if bwd and not own else (None, None)
    got_buf, read_sem, write_sem = take(3) if got is not None else (None, None, None)
    idx, list_sem = take(2)
    stage_f, stage_b, out_sem = take(3) if own else (None, None, None)

    step = pl.program_id(0)
    cols = spans(d)
    lo = ff // 256 * 256
    hi = ff - lo
    b_at, g_at = at0 + ROW_BOUND * LANES, at0 + ROW_GOFF * LANES
    dot = functools.partial(lax.dot_general, preferred_element_type=F32)
    nn = (((1,), (0,)), ((), ()))
    nt = (((1,), (1,)), ((), ()))
    tn = (((0,), (0,)), ((), ()))
    al = lambda v, m=PITCH: pl.multiple_of(v, m)
    tok_rows = PITCH * N_SRC * n_blk

    glane = lax.broadcasted_iota(I32, (GRP, LANES), 1)
    gsub = lax.broadcasted_iota(I32, (GRP, LANES), 0)

    def group(tile, q):
        return tab_ref[at0 + tab_ref[g_at + tile] + q]

    def gather(tile, q):
        ids = idx.at[pl.ds(group(tile, q) >> 4, GRP)]
        for k in range(GRP):
            gat[pl.ds(al((q * GRP + k) * PITCH), PITCH), :] = table[pl.ds(al(ids[k]), PITCH), :]

    def gate_column(code):
        pos = code >> 4
        row, shift = pos >> 7, pos & (LANES - 1)
        want = glane == gsub + shift
        over = glane == gsub + (shift - LANES)
        here = gate_ref[pl.ds(row, GRP, stride=0), :]
        there = gate_ref[pl.ds(row + 1, GRP, stride=0), :]
        v = jnp.where(want, here, jnp.where(over, there, 0.0))
        return jnp.where(gsub < (code & 15), jnp.sum(v, axis=1, keepdims=True), 0.0)

    def scatter(tile, q):
        ids = idx.at[pl.ds(group(tile, q) >> 4, GRP)]
        new = []
        for k in range(GRP):
            at = pl.ds(al(ids[k]), PITCH)
            new.append((at, acc[at, :] + row_ref[pl.ds(al((q * GRP + k) * PITCH), PITCH), :]))
        for at, value in reversed(new):
            acc[at, :] = value

    def convert(tile):
        for q in range(0, PER_TILE, 2):
            part = []
            for p in (q, q + 1):
                code = group(tile, p)
                rows = [gat[pl.ds(GRP * PITCH * p + j, GRP, stride=PITCH), :] for j in range(PITCH if bwd else HALF)]
                real = gsub < (code & 15)
                gate = gate_column(code)
                g_ref[GRP * p:GRP * (p + 1), :] = gate
                part.append([jnp.where(real, v, 0.0) for v in rows[:HALF]] + [v * gate for v in rows[HALF:]])
            at = slice(GRP * q, GRP * (q + 2))
            for x, o in ((x_u, 0), (x_c, HALF)):
                if x is None:
                    continue
                for j, (c, w) in enumerate(cols):
                    both = jnp.concatenate([part[0][o + j], part[1][o + j]], axis=0)
                    x[at, c:c + w] = both[:, :w].astype(BF16)

    @pl.when(step == 0)
    def _():
        src = pl.ds(list_at, N_SRC * list_len)
        lists = pltpu.make_async_copy(idx_hbm.at[src], idx.at[pl.ds(0, N_SRC * list_len)], list_sem)
        lists.start()
        if own:
            def clear(c, _):
                for k in range(4):
                    acc[pl.ds(al(c * 2048 + 512 * k, 512), 512), :] = jnp.zeros((512, LANES), F32)
                return 0

            lax.fori_loop(0, tok_rows // 2048, clear, 0)
            row_ref[...] = jnp.zeros(row_ref.shape, F32)
        rows = 256
        for srcs, o, seed in ((u_refs, 0, fwd), (dy_refs, HALF, own)):
            for s, ref in enumerate(srcs):
                def fill(c, _, ref=ref, o=o, seed=seed, s=s):
                    r = al(c * rows, rows)
                    at = PITCH * (s * n_blk + r) + o
                    for j in range(HALF):
                        vals = ref[0, pl.ds(r, rows), LANES * j:LANES * (j + 1)].astype(F32)
                        to = pl.ds(at + j, rows, stride=PITCH)
                        table[to, :] = vals
                        if seed and s == 0:
                            acc[to, :] = vals
                    return 0

                lax.fori_loop(0, n_blk // rows, fill, 0)
        lists.wait()
        for k in range(GRP):
            idx[N_SRC * list_len + k] = 0

        def first(q, _):
            gather(0, 2 * q)
            gather(0, 2 * q + 1)
            return 0

        lax.fori_loop(0, PER_TILE // 2, first, 0)
        convert(0)

    if got is not None:
        def read(e):
            return pltpu.make_async_copy(got.at[e], got_buf.at[e % 2], read_sem.at[e % 2])

        def writes(e):
            to = tab_ref[got_at + e]
            return [pltpu.make_async_copy(got_buf.at[e % 2, i], finals[i].at[got_layer, to], write_sem.at[e % 2, i])
                    for i in range(3)]

        @pl.when(step == 0)
        def _():
            read(step).start()

        read(step).wait()
        for write in writes(step):
            write.start()

        @pl.when(step > 0)
        def _():
            @pl.when(step < pl.num_programs(0) - 1)
            def _():
                for write in writes(step - 1):
                    write.wait()

        @pl.when(step < pl.num_programs(0) - 1)
        def _():
            read(step + 1).start()

    for i, w in enumerate((wg_ref, wu_ref)):
        gu_ref[i * lo:(i + 1) * lo, :] = w[0, 0, 0:lo, :]
        gu_ref[2 * lo + i * hi:2 * lo + (i + 1) * hi, :] = w[0, 0, lo:, :]
    total = grad if own else sums
    if bwd:
        total[...] = jnp.zeros(total.shape, F32) if own else prev[0]

    def put_rows(o, value, s0=0):
        value = value.astype(BF16).astype(F32)
        n = value.shape[0]
        for j, (c, w) in enumerate(cols):
            row_ref[pl.ds(PITCH * s0 + o + j, n, stride=PITCH), 0:w] = value[:, c:c + w] * g_ref[s0:s0 + n, 0:w]

    low = lax.broadcasted_iota(I32, (16, 2 * hi), 1) < hi

    def middle(a, b, dh):
        sig = 0.5 * jnp.tanh(0.5 * a) + 0.5
        act = a * sig
        h = act * b
        if dh is None:
            return h, None, None
        slope = sig * (1.0 + a * (1.0 - sig))
        return h, dh * b * slope, dh * act

    def tile(t, _):
        for q in range(PER_TILE):
            if own:
                scatter(jnp.maximum(t - 1, 0), q)
            gather(t + 1, q)
        part = ROWS // 2
        for s0 in range(0, ROWS, part):
            sl = slice(s0, s0 + part)
            ab_ref[sl, :] = dot(x_u[sl, :], gu_ref[...], nt)
            if bwd:
                dh_ref[sl, :] = dot(x_c[sl, :], wd_ref[0, 0], nt)
        for r in range(0, ROWS, 16):
            rows = slice(r, r + 16)
            for c in range(0, lo, LANES):
                h, da, db = middle(ab_ref[rows, c:c + LANES], ab_ref[rows, lo + c:lo + c + LANES],
                                   dh_ref[rows, c:c + LANES] if bwd else None)
                h_ref[rows, c:c + LANES] = h.astype(BF16)
                if bwd:
                    dab_ref[rows, c:c + LANES] = da.astype(BF16)
                    dab_ref[rows, lo + c:lo + c + LANES] = db.astype(BF16)
            a = ab_ref[rows, 2 * lo:]
            b = pltpu.roll(a, hi, 1)
            dh = dh_ref[rows, lo:] if bwd else None
            if bwd:
                dh = jnp.concatenate([dh, dh], axis=1)
            h, da, db = middle(a, b, dh)
            h_ref[rows, lo:] = h[:, :hi].astype(BF16)
            if bwd:
                dab_ref[rows, 2 * lo:] = jnp.where(low, da, pltpu.roll(db, hi, 1)).astype(BF16)
        for s0 in range(0, ROWS, part):
            sl = slice(s0, s0 + part)
            if fwd:
                put_rows(0, dot(h_ref[sl, :], wd_ref[0, 0], nn), s0)
            if bwd and own:
                put_rows(HALF, dot(dab_ref[sl, :], gu_ref[...], nn), s0)
        if bwd:
            view = total.at[0] if own else total
            view[0:2 * ff, :] += dot(dab_ref[...], x_u[...], tn)
            view[2 * ff:, :] += dot(h_ref[...], x_c[...], tn)
        convert(t + 1)
        return 0

    lax.fori_loop(tab_ref[b_at + step], tab_ref[b_at + step + 1], tile, 0)
    if bwd and not own:
        for i in range(2):
            sent[0, i, 0:lo, :] = sums[i * lo:(i + 1) * lo, :].astype(BF16)
            sent[0, i, lo:, :] = sums[2 * lo + i * hi:2 * lo + (i + 1) * hi, :].astype(BF16)
        sent[0, 2] = sums[2 * ff:, :].astype(BF16)
        final_step = step == pl.num_programs(0) - 1
        expert = tab_ref[at0 + ROW_EXPERT * LANES + step]
        keeps = [pltpu.make_async_copy(sent.at[0, i], finals[i].at[layer, expert], fin_sem.at[i]) for i in range(3)]

        @pl.when(step > 0)
        def _():
            for keep in keeps:
                keep.wait()

        for keep in keeps:
            keep.start()

        @pl.when(final_step)
        def _():
            for keep in keeps:
                keep.wait()
            if got is not None:
                for e in (step, step - 1):
                    for write in writes(e):
                        write.wait()

    if own:
        @pl.when(step == pl.num_programs(0) - 1)
        def _():
            end = tab_ref[b_at + step + 1] - 1
            lax.fori_loop(0, PER_TILE, lambda q, _: (scatter(end, q), 0)[1], 0)
            chunk = stage_f.shape[1]
            flights = {}
            n = 0
            for o, out in ((HALF, du_outs), (0, y_outs)):
                for s in range(N_SRC if out else 0):
                    wide = s == 0 or p_f32
                    stage = stage_f if wide else stage_b
                    for c in range(n_blk // chunk):
                        key = (wide, n % 2)
                        if key in flights:
                            flights.pop(key).wait()
                        for j in range(HALF):
                            rows = pl.ds(PITCH * (s * n_blk + c * chunk) + o + j, chunk, stride=PITCH)
                            stage[n % 2, :, LANES * j:LANES * (j + 1)] = acc[rows, :].astype(stage.dtype)
                        flights[key] = pltpu.make_async_copy(
                            stage.at[n % 2], out[s].at[pl.ds(c * chunk, chunk), :], out_sem.at[2 * wide + n % 2])
                        flights[key].start()
                        n += 1
            for copy in flights.values():
                copy.wait()


def run_experts(routes, layer, half, u, dy, weights, prev, finals, fwd, own, p_f32=False, got=None):
    tab, idx, gates = routes
    bwd = dy is not None
    wg, wu, wd = weights
    n_blk, wide = u[0][0].shape[-2:]
    n_layers, n_local, ff, d = wd.shape
    n_exp = n_local // 2
    row_id = half * n_layers + layer
    at0 = row_id * TAB_ROWS * LANES
    e_at = at0 + ROW_EXPERT * LANES
    list_len = idx.shape[0] // (2 * n_layers * N_SRC)

    block = lambda i: pl.BlockSpec((1, n_blk, wide), lambda e, *_: (i, 0, 0), pipeline_mode=pl.Buffered(1))
    blocks = lambda pieces: [block(i) for _, i in pieces]
    arrays = lambda pieces: [v for v, _ in pieces]
    weight = pl.BlockSpec((1, 1, ff, d), lambda e, tab: (layer, tab[e_at + e], 0, 0))
    partial = pl.BlockSpec((1, 3 * ff, d), lambda e, *_: (e, 0, 0))

    operands = [idx, gates] + arrays(u) + (arrays(dy) if bwd else []) + [wg, wu, wd]
    gate_rows = N_SRC * list_len // LANES + 8
    gate_spec = pl.BlockSpec((gate_rows, LANES), lambda e, *_: (row_id, 0), pipeline_mode=pl.Buffered(1))
    in_specs = [any_space, gate_spec] + blocks(u) + (blocks(dy) if bwd else []) + [weight] * 3
    out_shape, out_specs, aliases = [], [], {}
    for use in (fwd, bwd and own):
        if use:
            out_shape += [jax.ShapeDtypeStruct((n_blk, wide), F32 if s == 0 or p_f32 else BF16) for s in range(N_SRC)]
            out_specs += [any_space] * N_SRC
    if bwd and own:
        out_shape.append(jax.ShapeDtypeStruct((n_exp, 3 * ff, d), F32))
        out_specs.append(partial)
    if bwd and not own:
        operands.append(prev)
        in_specs.append(partial)
        if got is not None:
            operands.append(got)
            in_specs.append(any_space)
        for i, f in enumerate(finals or ()):
            aliases[1 + len(operands)] = i
            operands.append(f)
            in_specs.append(any_space)
        out_shape += [jax.ShapeDtypeStruct((n_layers, n_local, ff, d), BF16)] * 3
        out_specs += [any_space] * 3
        out_shape.append(jax.ShapeDtypeStruct((n_exp, 3, ff, d), BF16))
        out_specs.append(pl.BlockSpec((1, 3, ff, d), lambda e, *_: (e, 0, 0, 0)))
    table = pltpu.VMEM((PITCH * N_SRC * n_blk, LANES), F32)
    rows = pltpu.VMEM((PITCH * ROWS, LANES), F32)
    mid = lambda n, dt: pltpu.VMEM((ROWS, n), dt)
    scratch = [table, rows] * (1 + own)
    scratch += [pltpu.VMEM((2 * ff, d), BF16), mid(LANES, F32)] + [mid(d, BF16)] * (1 + bwd) + [mid(2 * ff, F32)]
    scratch += [mid(ff, F32)] * bwd + [mid(ff, BF16)] + [mid(2 * ff, BF16)] * bwd
    if bwd and not own:
        scratch += [pltpu.VMEM((3 * ff, d), F32), pltpu.SemaphoreType.DMA((3,))]
    if got is not None:
        scratch += [pltpu.VMEM((2, 3, ff, d), BF16), pltpu.SemaphoreType.DMA((2,)), pltpu.SemaphoreType.DMA((2, 3))]
    scratch += [pltpu.SMEM((N_SRC * list_len + 128,), I32), pltpu.SemaphoreType.DMA]
    if own:
        scratch += [pltpu.VMEM((2, 256, wide), F32), pltpu.VMEM((2, 256, wide), BF16), pltpu.SemaphoreType.DMA((4,))]
    passes = 2 + fwd + bwd * (4 + 2 * own)
    flops = 2 * d * ff * passes * n_blk * N_SRC * 2
    got_layer = None if got is None else 1 - layer
    cfg = (fwd, bwd, own, layer, n_blk, d, ff, at0, row_id * N_SRC * list_len, list_len, p_f32, len(aliases), got_layer,
           0 if got is None else (got_layer * TAB_ROWS + ROW_PARTNER) * LANES)
    return pl.pallas_call(
        functools.partial(expert_kernel, cfg),
        out_shape=out_shape,
        grid_spec=pltpu.PrefetchScalarGridSpec(
            num_scalar_prefetch=1, grid=(n_exp,), in_specs=in_specs, out_specs=out_specs, scratch_shapes=scratch),
        input_output_aliases=aliases,
        compiler_params=pltpu.CompilerParams(dimension_semantics=("arbitrary",), vmem_limit_bytes=VMEM_LIMIT),
        cost_estimate=pl.CostEstimate(flops=flops, bytes_accessed=3 * 2 * n_exp * d * ff, transcendentals=0),
        name=f"experts_{'f' if fwd else ''}{'b' if bwd else ''}_{'own' if own else 'other'}_{layer}",
    )(tab, *operands)


def place_kernel(layer, n_exp, tab_at, tab_ref, got_ref, *refs):
    outs, (buf, in_sem, out_sem) = refs[3:6], refs[6:]
    reads = [pltpu.make_async_copy(got_ref.at[i], buf.at[i], in_sem.at[i]) for i in range(n_exp)]
    for read in reads:
        read.start()
    writes = []
    for i, read in enumerate(reads):
        read.wait()
        e = tab_ref[tab_at + i]
        for k, out in enumerate(outs):
            writes.append(pltpu.make_async_copy(buf.at[i, k], out.at[layer, e], out_sem.at[i, k]))
            writes[-1].start()
    for write in writes:
        write.wait()


def place(tab, layer, got, finals):
    n_exp = got.shape[0]
    return pl.pallas_call(
        functools.partial(place_kernel, layer, n_exp, (layer * TAB_ROWS + ROW_PARTNER) * LANES),
        out_shape=[jax.ShapeDtypeStruct(f.shape, f.dtype) for f in finals],
        grid_spec=pltpu.PrefetchScalarGridSpec(
            num_scalar_prefetch=1, grid=(1,), in_specs=[any_space] * 4, out_specs=[any_space] * 3,
            scratch_shapes=[pltpu.VMEM(got.shape, got.dtype), pltpu.SemaphoreType.DMA((n_exp,)),
                            pltpu.SemaphoreType.DMA((n_exp, 3))]),
        input_output_aliases={2: 0, 3: 1, 4: 2},
        compiler_params=pltpu.CompilerParams(vmem_limit_bytes=VMEM_LIMIT),
        cost_estimate=pl.CostEstimate(flops=0, bytes_accessed=4 * got.size, transcendentals=0),
        name=f"place_{layer}",
    )(tab, got, *finals)


def peer(rel):
    return {name: (lax.axis_index(name) + ((rel >> bit) & 1)) % 2 for bit, name in enumerate(("ep", "core", "x"))}


def meet(rels):
    barrier = pltpu.get_barrier_semaphore()
    for rel in rels:
        pl.semaphore_signal(barrier, inc=1, device_id=peer(rel), device_id_type=MESH)
    pl.semaphore_wait(barrier, len(rels))


def remote(src, dst, send, recv, rel):
    return pltpu.make_async_remote_copy(src_ref=src, dst_ref=dst, send_sem=send, recv_sem=recv,
                                        device_id=peer(rel), device_id_type=MESH)


def share_kernel(n_rel, mine_ref, all_ref, send_sem, recv_sem):
    meet(range(1, n_rel))
    copies = [remote(mine_ref, all_ref.at[rel], send_sem.at[rel], recv_sem.at[rel], rel) for rel in range(1, n_rel)]
    for copy in copies:
        copy.start()
    all_ref[0] = mine_ref[...]
    for copy in copies:
        copy.wait()


def share(mine, n_rel):
    return pl.pallas_call(
        functools.partial(share_kernel, n_rel),
        out_shape=jax.ShapeDtypeStruct((n_rel,) + mine.shape, mine.dtype),
        in_specs=[in_vmem],
        out_specs=in_vmem,
        scratch_shapes=[pltpu.SemaphoreType.DMA((n_rel,)), pltpu.SemaphoreType.DMA((n_rel,))],
        compiler_params=pltpu.CompilerParams(collective_id=0, has_side_effects=True),
        cost_estimate=pl.CostEstimate(flops=10 ** 7, bytes_accessed=mine.size * 4 * n_rel, transcendentals=0),
        name="share_lists",
    )(mine)


def blocks_kernel(cfg, *refs):
    n_chunk, reduce, across, back, d = cfg
    refs = list(refs)
    take = lambda n: [refs.pop(0) for _ in range(n)]
    parts = take(N_SRC)
    m_ref, o_total, o_a, o_b = take(4)
    o_xa, o_xb = take(2) if across else (None, None)
    in_f, in_b, got_f, s_buf, r_buf, t_buf, u_buf, load, send, recv, put = take(11)
    n_rows = t_buf.shape[0] // n_chunk
    cut = [pl.ds(k * n_rows, n_rows) for k in range(n_chunk)]
    chunks = range(n_chunk)
    loads = {}
    for i, part in enumerate(parts[:2] if reduce else parts):
        buf = in_f.at[i] if reduce or i == 0 else in_b.at[i - 1]
        for k in chunks:
            loads[i, k] = pltpu.make_async_copy(part.at[cut[k]], buf.at[cut[k]], load.at[i, k])
    order = (1, 0) if reduce else range(N_SRC)
    for i in order:
        for k in chunks:
            loads[i, k].start()
    u_buf[...] = jnp.zeros(u_buf.shape, BF16)
    meet((Y, CORE, X) if across else (Y, CORE))
    links = []

    def link(src, dst, rel):
        n = len(links)
        links.append([remote(src.at[cut[k]], dst.at[cut[k]], send.at[n, k], recv.at[n, k], rel) for k in chunks])
        return links[-1]

    if reduce:
        first = link(parts[3], got_f.at[1], CORE)
        second = link(parts[2], got_f.at[0], CORE)
        over = link(s_buf, r_buf, Y)
        for copies in (first, second):
            for copy in copies:
                copy.start()
        for k in chunks:
            loads[1, k].wait()
            first[k].wait_recv()
            s_buf[cut[k], :] = (in_f[1, cut[k], :] + got_f[1, cut[k], :]).astype(BF16)
            over[k].start()
    to_y = link(u_buf, o_a.at[1], Y)
    to_core = link(u_buf, o_b.at[0], CORE)
    to_x = link(u_buf, o_xa.at[0], X) if across else None
    puts = []
    for k in chunks:
        if reduce:
            loads[0, k].wait()
            second[k].wait_recv()
            over[k].wait_recv()
            total = in_f[0, cut[k], :] + got_f[0, cut[k], :] + r_buf[cut[k], :].astype(F32)
        else:
            for i in range(N_SRC):
                loads[i, k].wait()
            total = in_f[0, cut[k], :]
            for i in range(N_SRC - 1):
                total = total + in_b[i, cut[k], :].astype(F32)
        total = total.astype(BF16)
        t_buf[cut[k], :] = total
        dims = (((1,), (1 if back else 0,)), ((), ()))
        mixed = lax.dot_general(total[:, :d], m_ref[...], dims, preferred_element_type=F32)
        u_buf[cut[k], 0:d] = (total[:, :d].astype(F32) + mixed).astype(BF16)
        to_y[k].start()
        to_core[k].start()
        if across:
            to_x[k].start()
        puts.append(pltpu.make_async_copy(u_buf.at[cut[k]], o_a.at[0, cut[k]], put.at[0, k]))
        puts.append(pltpu.make_async_copy(t_buf.at[cut[k]], o_total.at[cut[k]], put.at[1, k]))
        for copy in puts[-2:]:
            copy.start()
    on = link(o_a.at[1], o_b.at[1], CORE)
    on_x = link(o_a.at[1], o_xa.at[1], X) if across else None
    for k in chunks:
        to_y[k].wait_recv()
        on[k].start()
        if across:
            on_x[k].start()
    if across:
        last = [link(o_xa.at[i], o_xb.at[i], CORE) for i in range(2)]
        for i, arrived in enumerate((to_x, on_x)):
            for k in chunks:
                arrived[k].wait_recv()
                last[i][k].start()
    waited = [to_y] + ([first, second, over] if reduce else []) + ([to_x, on_x] if across else [])
    for copies in links:
        for copy in copies:
            if any(copies is w for w in waited):
                copy.wait_send()
            else:
                copy.wait()
    for copy in puts:
        copy.wait()


def complete_blocks(parts, m, reduce, across, back, ident, n_chunk=4):
    n_blk, wide = parts[0].shape
    d = m.shape[0]
    sem = lambda *s: pltpu.SemaphoreType.DMA(s)
    pair = jax.ShapeDtypeStruct((2, n_blk, wide), BF16)
    buf = lambda n, dt: pltpu.VMEM((n, n_blk, wide) if n else (n_blk, wide), dt)
    return pl.pallas_call(
        functools.partial(blocks_kernel, (n_chunk, reduce, across, back, d)),
        out_shape=[jax.ShapeDtypeStruct((n_blk, wide), BF16)] + [pair] * (4 if across else 2),
        in_specs=[any_space] * N_SRC + [in_vmem],
        out_specs=[any_space] * (5 if across else 3),
        scratch_shapes=[buf(2, F32), buf(3, BF16), buf(2, F32), buf(0, BF16), buf(0, BF16), buf(0, BF16), buf(0, BF16),
                        sem(4, n_chunk), sem(10, n_chunk), sem(10, n_chunk), sem(2, n_chunk)],
        compiler_params=pltpu.CompilerParams(collective_id=ident, has_side_effects=True, vmem_limit_bytes=VMEM_LIMIT),
        cost_estimate=pl.CostEstimate(flops=10 ** 8, bytes_accessed=n_blk * wide * 40, transcendentals=0),
        name=f"complete_blocks_{ident}",
    )(*parts, m)


def total_kernel(n_chunk, g_ref, o_ref, give, got, s_buf, y_buf, t_buf, x_buf, z_buf, send, recv):
    core = lax.axis_index('core')
    n_rows = o_ref.shape[1] // n_chunk
    cut = [pl.ds(k * n_rows, n_rows) for k in range(n_chunk)]
    first = core > 0
    give[...] = jnp.where(first, g_ref[0], g_ref[1])
    meet((Y, CORE, X))
    copies = [[remote(src.at[cut[k]], dst.at[cut[k]], send.at[i, k], recv.at[i, k], rel) for k in range(n_chunk)]
              for i, (src, dst, rel) in enumerate(((give, got, CORE), (s_buf, y_buf, Y), (t_buf, x_buf, X)))]
    for copy in copies[0]:
        copy.start()
    for k in range(n_chunk):
        copies[0][k].wait_recv()
        mine = jnp.where(first, g_ref[1, cut[k], :], g_ref[0, cut[k], :])
        s_buf[cut[k], :] = (mine + got[cut[k], :]).astype(BF16)
        copies[1][k].start()
    for k in range(n_chunk):
        copies[1][k].wait_recv()
        t_buf[cut[k], :] = (s_buf[cut[k], :].astype(F32) + y_buf[cut[k], :].astype(F32)).astype(BF16)
        copies[2][k].start()
    for k in range(n_chunk):
        copies[2][k].wait_recv()
        got[cut[k], :] = t_buf[cut[k], :].astype(F32) + x_buf[cut[k], :].astype(F32)
    for group in copies:
        for copy in group:
            copy.wait_send()
    s_buf[...] = got[...].astype(BF16)
    swap = remote(s_buf, z_buf, send.at[3, 0], recv.at[3, 0], CORE)
    swap.start()
    swap.wait()
    o_ref[0] = jnp.where(first, z_buf[...], s_buf[...])
    o_ref[1] = jnp.where(first, s_buf[...], z_buf[...])


def total_grads(g, ident, n_chunk=4):
    _, d, _ = g.shape
    buf = lambda dt: pltpu.VMEM((d, d), dt)
    return pl.pallas_call(
        functools.partial(total_kernel, n_chunk),
        out_shape=jax.ShapeDtypeStruct(g.shape, BF16),
        in_specs=[in_vmem], out_specs=in_vmem,
        scratch_shapes=[buf(F32), buf(F32), buf(BF16), buf(BF16), buf(BF16), buf(BF16), buf(BF16),
                        pltpu.SemaphoreType.DMA((4, n_chunk)), pltpu.SemaphoreType.DMA((4, n_chunk))],
        compiler_params=pltpu.CompilerParams(collective_id=ident, has_side_effects=True),
        cost_estimate=pl.CostEstimate(flops=10 ** 7, bytes_accessed=g.size * 8, transcendentals=0),
        name="total_grads",
    )(g)


def solution(mesh):
    ep_size, dp_size = mesh.shape['ep'], mesh.shape['dp']
    sub = Mesh(mesh.devices.reshape(ep_size, dp_size // 2, 2), ('ep', 'x', 'core'))
    tok_axes = ('x', 'core', 'ep')
    tok_spec = P(tok_axes, None)
    route_spec = P(None, tok_axes, None)
    whole_spec = P(None, None, None)
    expert_spec = P(None, 'ep', None, None)
    flip = [(0, 1), (1, 0)]
    move = lambda v, axis: lax.ppermute(v, axis, flip)
    move_diag = lambda v: lax.ppermute(v, ('ep', 'core'), [(0, 3), (1, 2), (2, 1), (3, 0)])
    fence = lax.optimization_barrier

    def device_step(tokens, d_out, expert_ids, gate_vals, w_mix, w_gate, w_up, w_down):
        n_layers, d = w_mix.shape[0], w_mix.shape[1]
        n_tok = tokens.shape[0]
        top = expert_ids.shape[2]
        n_local = w_gate.shape[1]
        n_exp = n_local * ep_size
        n = n_tok * top
        n_rel = 2 * N_SRC
        wide = cdiv(d, LANES) * LANES
        weights = (jnp.swapaxes(w_gate, 2, 3), jnp.swapaxes(w_up, 2, 3), w_down)
        pad = lambda v: jnp.pad(v, ((0, 0), (0, wide - d)))
        send_three = lambda p: [move(p[1], 'ep'), move(p[2], 'core'), move_diag(p[3])]

        def own_sum(p, got):
            return sum([g.astype(F32) for g in got], p)[:, :d].astype(BF16)

        one = lambda v: v.reshape(1, n_tok, wide)
        pairs = lambda a, b: [(a, 0), (a, 1), (b, 0), (b, 1)]

        u0 = pad((tokens.astype(F32) + jnp.dot(tokens, w_mix[0], preferred_element_type=F32)).astype(BF16))
        u0_far = move(u0, 'ep')
        lists = [sorted_list(expert_ids[l], gate_vals[l]) for l in range(n_layers)]
        counts = jnp.sum((expert_ids.reshape(n_layers, n, 1) == jnp.arange(n_exp, dtype=I32)).astype(F32), axis=1)
        packed = jnp.concatenate([jnp.concatenate([v[0] for v in lists] + [v[1] for v in lists]).reshape(-1, LANES),
                                  jnp.pad(counts, ((0, 8 - n_layers), (0, LANES - n_exp)))], axis=0)
        u0_far, packed = fence((u0_far, packed))
        shared = share(packed, n_rel)
        u0_a = jnp.stack([u0, u0_far])
        u0_b = move(u0_a, 'core')
        u0_half = pairs(u0_a, u0_b)
        dy, shared = fence((pad(d_out), shared))
        dy_y, dy_x = move(dy, 'ep'), move(dy, 'x')
        routes = plan(shared, n_layers, n_local, n_tok, n // LANES)
        part = run_experts(routes, 0, 0, u0_half, None, weights, None, None, True, True, p_f32=True)
        dy_y, dy_x, part = fence((dy_y, dy_x, part))
        dy_core, dy_diag, dy_xy, dy_xc = move(dy, 'core'), move(dy_y, 'core'), move(dy_y, 'x'), move(dy_x, 'core')
        y0, u1_a, u1_b = complete_blocks(part, w_mix[1], True, False, False, 1)
        dy_core, dy_diag, dy_xy, dy_xc, u0_a2, y0, u1_a, u1_b = fence(
            (dy_core, dy_diag, dy_xy, dy_xc, u0_a, y0, u1_a, u1_b))
        dy_xd = move(dy_xy, 'core')
        dy_half = [(one(v), 0) for v in (dy, dy_y, dy_core, dy_diag)]
        dy_other = [(one(v), 0) for v in (dy_x, dy_xy, dy_xc, dy_xd)]
        u1_xa, u0_xa = move(u1_a, 'x'), move(u0_a2, 'x')
        out = run_experts(routes, 1, 0, pairs(u1_a, u1_b), dy_half, weights, None, None, True, True)
        u1_xa, u0_xa, dy_xd, out = fence((u1_xa, u0_xa, dy_xd, out))
        dy_other[3] = (one(dy_xd), 0)
        y_part, du_part, g1 = out[:4], out[4:8], out[8]
        u1_xb = move(u1_xa, 'core')
        got = send_three(du_part)
        out = run_experts(routes, 1, 1, pairs(u1_xa, u1_xb), dy_other, weights, g1, None, False, False)
        got, u0_xa, out = fence((got, u0_xa, out))
        *finals, sent1 = out
        du1, dx_a, dx_b = complete_blocks([du_part[0], *got], w_mix[1], False, False, True, 2)
        dx_a, y_part, sent1, u0_xa = fence((dx_a, y_part, sent1, u0_xa))
        dx_xa = move(dx_a, 'x')
        got_y = send_three(y_part)
        got1 = move(sent1, 'core')
        u0_xb = move(u0_xa, 'core')
        out = run_experts(routes, 0, 0, u0_half, pairs(dx_a, dx_b), weights, None, None, False, True)
        dx_xa, got_y, got1, u0_xb, out = fence((dx_xa, got_y, got1, u0_xb, out))
        du_part, g0 = out[:4], out[4]
        dx_xb = move(dx_xa, 'core')
        got = send_three(du_part)
        out = run_experts(routes, 0, 1, pairs(u0_xa, u0_xb), pairs(dx_xa, dx_xb), weights, g0, finals, False, False,
                          got=got1)
        got, out = fence((got, out))
        *finals, sent0 = out
        got0 = move(sent0, 'core')
        du0 = own_sum(du_part[0], got)
        tx = lambda x, du: jnp.einsum('td,te->de', x, du, preferred_element_type=F32)
        g_mix = total_grads(jnp.stack([tx(tokens, du0), tx(y0[:, :d], du1[:, :d])]), 3)
        y1 = own_sum(y_part[0], got_y)
        dx0 = (du0.astype(F32) + jnp.einsum('te,de->td', du0, w_mix[0], preferred_element_type=F32)).astype(BF16)
        finals, got0, g_mix = fence((finals, got0, g_mix))
        finals = place(routes[0], 0, got0, finals)
        return (y1, dx0, g_mix, jnp.swapaxes(finals[0], 2, 3), jnp.swapaxes(finals[1], 2, 3), finals[2])

    return jax.shard_map(device_step, mesh=sub,
                         in_specs=(tok_spec, tok_spec, route_spec, route_spec, whole_spec,
                                   expert_spec, expert_spec, expert_spec),
                         out_specs=(tok_spec, tok_spec, whole_spec, expert_spec, expert_spec, expert_spec),
                         check_vma=False)
```

```python
import functools

import jax
import jax.numpy as jnp
from jax import lax
from jax.experimental import pallas as pl
from jax.experimental.pallas import tpu as pltpu
from jax.sharding import Mesh, PartitionSpec as P

F32, BF16, I32 = jnp.float32, jnp.bfloat16, jnp.int32
MESH = pl.DeviceIdType.MESH
ROWS = 384
GRP = 8
PITCH = 9
FULL = 8
HALF = 4
CAP_FACTOR = 3
LANES = 128
N_SRC = 4
Y, CORE, X = 1, 2, 4
VMEM_LIMIT = 62 * 1024 * 1024
PER_TILE = ROWS // GRP
ROW_BOUND, ROW_GOFF, ROW_EXPERT, ROW_PARTNER, TAB_ROWS = 32, 33, 34, 35, 40
SLOT_GROUPS = 256


def cdiv(a, b):
    return (a + b - 1) // b


def spans(d):
    return [(LANES * j, min(LANES, d - LANES * j)) for j in range(cdiv(d, LANES))]


any_space = pl.BlockSpec(memory_space=pl.ANY)
in_vmem = pl.BlockSpec(memory_space=pltpu.VMEM)


def sorted_list(expert_ids, gate_vals):
    n_tok, top = expert_ids.shape
    n = n_tok * top
    keys = expert_ids.reshape(n) * n + jnp.arange(n, dtype=I32)
    keys, gates = lax.sort((keys, gate_vals.reshape(n)), num_keys=1)
    return ((keys % n) // top).astype(F32), gates


def plan_kernel(n_layers, n_local, n_tok, list_rows, all_ref, tab_ref, idx_ref, gate_ref):
    n_mine = n_local // 2
    core, ep = lax.axis_index('core'), lax.axis_index('ep')
    list_len = list_rows * LANES
    lane = lambda n: lax.broadcasted_iota(I32, (n, LANES), 1).astype(F32)
    sub = lambda n: lax.broadcasted_iota(I32, (n, LANES), 0).astype(F32)
    over_lanes = lambda v: jnp.sum(v, axis=1, keepdims=True)
    over_subs = lambda v: jnp.sum(v, axis=0, keepdims=True)
    l16, s16 = lane(n_mine), sub(n_mine)
    for l in range(n_layers):
        cnt = all_ref[:, 2 * n_layers * list_rows + l, :]
        ends = cnt
        step = 1
        while step < 2 * n_local:
            ends = ends + jnp.where(lane(8) >= step, pltpu.roll(ends, step, 1), 0.0)
            step *= 2
        starts = ends - cnt
        second = (ep > 0)
        local = lambda v: jnp.where(lane(8) < n_local, jnp.where(second, pltpu.roll(v, LANES - n_local, 1), v), 0.0)
        cnt, starts = local(cnt), local(starts)
        grp = jnp.floor((cnt + (GRP - 0.5)) * (1.0 / GRP))
        tiles = [jnp.maximum(1.0, jnp.floor((over_subs(grp[h * N_SRC:(h + 1) * N_SRC]) + (PER_TILE - 0.5)) * (1.0 / PER_TILE)))
                 for h in range(2)]
        load = jnp.where(lane(1) < n_local, 3.0 * tiles[0] + 2.0 * tiles[1], -1.0)
        wide = jnp.broadcast_to(load, (n_local, LANES))
        col = over_lanes(jnp.where(lane(n_local) == sub(n_local), wide, 0.0))
        ahead = (col > wide) | ((col == wide) & (sub(n_local) < lane(n_local)))
        rank = over_subs(jnp.where(ahead, 1.0, 0.0))
        odd = s16 - 2.0 * jnp.floor(s16 * 0.5 + 0.25)
        flip = jnp.where(core > 0, 1.0 - odd, odd)
        dealt = lambda f: (jnp.broadcast_to(rank, (n_mine, LANES)) == 2.0 * s16 + f) & (l16 < n_local)
        pick = dealt(flip)
        choose = lambda p, row: over_lanes(jnp.where(p, jnp.broadcast_to(row, (n_mine, LANES)), 0.0))
        mine = lambda row: choose(pick, row)
        as_row = lambda c: over_subs(jnp.where(l16 == s16, c, 0.0))
        experts = as_row(mine(lane(1)))
        partner = as_row(choose(dealt(1.0 - flip), lane(1)))
        for h in range(2):
            at = (h * n_layers + l) * TAB_ROWS
            off = jnp.zeros((n_mine, 1), F32)
            pos = [jnp.zeros((n_mine, LANES), F32) for _ in range(SLOT_GROUPS // LANES)]
            for s in range(N_SRC):
                r = h * N_SRC + s
                c, st = mine(cnt[r:r + 1]), mine(starts[r:r + 1]) + float(s * list_len)
                ng = jnp.floor((c + (GRP - 0.5)) * (1.0 / GRP))
                for i in range(len(pos)):
                    rel = l16 + float(LANES * i) - off
                    code = (st + GRP * rel) * 16.0 + jnp.minimum(float(GRP), c - GRP * rel)
                    pos[i] = jnp.where((rel >= 0) & (rel < ng), code, pos[i])
                off = off + ng
            for i in range(len(pos)):
                tab_ref[pl.ds(at + i, n_mine, stride=len(pos)), :] = pos[i].astype(I32)
            n_tiles = jnp.maximum(1.0, jnp.floor((off + (PER_TILE - 0.5)) * (1.0 / PER_TILE)))
            bounds = over_subs(jnp.where(s16 < l16, n_tiles, 0.0))
            before = over_lanes(jnp.where(l16 == s16, jnp.broadcast_to(bounds, (n_mine, LANES)), 0.0))
            t = jnp.minimum(l16, over_subs(jnp.broadcast_to(n_tiles, (n_mine, LANES))) - 1.0)
            inside = (t >= before) & (t < before + n_tiles)
            goff = over_subs(jnp.where(inside, s16 * float(SLOT_GROUPS) + (t - before) * float(PER_TILE), 0.0))
            rows = [(ROW_BOUND, bounds), (ROW_GOFF, goff), (ROW_EXPERT, experts), (ROW_PARTNER, partner)]
            for row, value in rows:
                tab_ref[at + row:at + row + 1, :] = value.astype(I32)
    for h in range(2):
        for l in range(n_layers):
            pad = (h * n_layers + l) * (N_SRC * list_rows + 8) + N_SRC * list_rows
            gate_ref[pad:pad + 8, :] = jnp.zeros((8, LANES), F32)
            for s in range(N_SRC):
                to = ((h * n_layers + l) * N_SRC + s) * list_rows
                toks = all_ref[h * N_SRC + s, l * list_rows:(l + 1) * list_rows, :]
                idx_ref[to:to + list_rows, :] = ((toks + float(s * n_tok)) * float(PITCH)).astype(I32)
                to = (h * n_layers + l) * (N_SRC * list_rows + 8) + s * list_rows
                gate_ref[to:to + list_rows, :] = all_ref[
                    h * N_SRC + s, (n_layers + l) * list_rows:(n_layers + l + 1) * list_rows, :]


def plan(shared, n_layers, n_local, n_tok, list_rows):
    n_tab = 2 * n_layers * TAB_ROWS
    n_list = 2 * n_layers * N_SRC * list_rows
    n_gate = 2 * n_layers * (N_SRC * list_rows + 8)
    tab, idx, gates = pl.pallas_call(
        functools.partial(plan_kernel, n_layers, n_local, n_tok, list_rows),
        out_shape=[jax.ShapeDtypeStruct((n_tab, LANES), I32), jax.ShapeDtypeStruct((n_list, LANES), I32),
                   jax.ShapeDtypeStruct((n_gate, LANES), F32)],
        in_specs=[in_vmem], out_specs=[in_vmem] * 3,
        cost_estimate=pl.CostEstimate(flops=10 ** 7, bytes_accessed=10 ** 6, transcendentals=0),
        name="plan",
    )(shared)
    return tab.reshape(-1), idx.reshape(-1), gates


def expert_kernel(cfg, *refs):
    fwd, bwd, own, layer, n_blk, d, ff, n_exp, picks, row_id, list_len, p_f32, n_alias, got_layer = cfg
    refs = list(refs)
    take = lambda n: [refs.pop(0) for _ in range(n)]
    tab_hbm, idx_hbm, gate_hbm = take(3)
    u_pieces = take(N_SRC)
    dy_pieces = take(N_SRC) if bwd else []
    wg_hbm, wu_hbm, wd_hbm = take(3)
    prev = take(1)[0] if bwd and not own else None
    got = take(1)[0] if got_layer is not None else None
    take(n_alias)
    y_outs = take(N_SRC) if fwd else []
    du_outs = take(N_SRC) if bwd and own else []
    grad = take(1)[0] if bwd and own else None
    finals = take(3) if bwd and not own else None
    sent = take(1)[0] if bwd and not own else None
    tab_ref, idx, gate_ref, land, table, gat = take(6)
    acc, row_ref = take(2) if own else (None, None)
    gu_ref, wd_ref, g_ref, x_u = take(4)
    x_c = take(1)[0] if bwd else None
    ab_ref = take(1)[0]
    dh_ref = take(1)[0] if bwd else None
    h_ref = take(1)[0]
    dab_ref, sums = take(2) if bwd else (None, None)
    keep_buf = take(1)[0] if bwd and not own else None
    got_buf = take(1)[0] if got is not None else None
    list_sem, land_sem, w_sem = take(3)
    sum_sem = take(1)[0] if bwd else None
    keep_sem = take(1)[0] if bwd and not own else None
    read_sem, write_sem = take(2) if got is not None else (None, None)
    stage_f, stage_b, out_sem = take(3) if own else (None, None, None)

    copy = pltpu.make_async_copy
    cols = spans(d)
    lo = ff // 256 * 256
    hi = ff - lo
    dot = functools.partial(lax.dot_general, preferred_element_type=F32)
    nn = (((1,), (0,)), ((), ()))
    nt = (((1,), (1,)), ((), ()))
    tn = (((0,), (0,)), ((), ()))
    al = pl.multiple_of
    n_row = N_SRC * n_blk
    glane = lax.broadcasted_iota(I32, (GRP, LANES), 1)
    gsub = lax.broadcasted_iota(I32, (GRP, LANES), 0)

    def row_at(r):
        return pl.ds(r * PITCH, FULL)

    def group(tile, q):
        return tab_ref[tab_ref[ROW_GOFF * LANES + tile] + q]

    def gather(tile, q):
        ids = idx.at[pl.ds(group(tile, q) >> 4, GRP)]
        for k in range(GRP):
            gat[row_at(q * GRP + k), :] = table[pl.ds(ids[k], FULL), :]

    def gate_column(code):
        pos = code >> 4
        row, shift = pos >> 7, pos & (LANES - 1)
        want = glane == gsub + shift
        over = glane == gsub + (shift - LANES)
        here = gate_ref[pl.ds(row, GRP, stride=0), :]
        there = gate_ref[pl.ds(row + 1, GRP, stride=0), :]
        v = jnp.where(want, here, jnp.where(over, there, 0.0))
        return jnp.where(gsub < (code & 15), jnp.sum(v, axis=1, keepdims=True), 0.0)

    def scatter(tile, q):
        ids = idx.at[pl.ds(group(tile, q) >> 4, GRP)]
        new = []
        for k in range(GRP):
            at = pl.ds(ids[k], FULL)
            new.append((at, acc[at, :] + row_ref[row_at(q * GRP + k), :]))
        for at, value in reversed(new):
            acc[at, :] = value

    def convert(tile):
        for q in range(0, PER_TILE, 2):
            part = []
            for p in (q, q + 1):
                code = group(tile, p)
                rows = [gat[pl.ds(GRP * PITCH * p + j, GRP, stride=PITCH), :] for j in range(FULL if bwd else HALF)]
                real = gsub < (code & 15)
                gate = gate_column(code)
                g_ref[GRP * p:GRP * (p + 1), :] = gate
                part.append([jnp.where(real, v, 0.0) for v in rows[:HALF]] + [v * gate for v in rows[HALF:]])
            at = slice(GRP * q, GRP * (q + 2))
            for x, o in ((x_u, 0), (x_c, HALF)):
                if x is None:
                    continue
                for j, (c, w) in enumerate(cols):
                    both = jnp.concatenate([part[0][o + j], part[1][o + j]], axis=0)
                    x[at, c:c + w] = both[:, :w].astype(BF16)

    def put_rows(o, value, s0):
        value = value.astype(BF16).astype(F32)
        n = value.shape[0]
        for j, (c, w) in enumerate(cols):
            row_ref[pl.ds(PITCH * s0 + o + j, n, stride=PITCH), 0:w] = value[:, c:c + w] * g_ref[s0:s0 + n, 0:w]

    low = lax.broadcasted_iota(I32, (16, 2 * hi), 1) < hi

    def middle(a, b, dh):
        sig = 0.5 * jnp.tanh(0.5 * a) + 0.5
        act = a * sig
        h = act * b
        if dh is None:
            return h, None, None
        slope = sig * (1.0 + a * (1.0 - sig))
        return h, dh * b * slope, dh * act

    def weights(e, slot):
        at = (layer, tab_ref[ROW_EXPERT * LANES + e])
        moves = []
        for i, w in enumerate((wg_hbm, wu_hbm)):
            moves.append((w.at[at + (pl.ds(0, lo),)], gu_ref.at[slot, pl.ds(i * lo, lo)]))
            moves.append((w.at[at + (pl.ds(lo, hi),)], gu_ref.at[slot, pl.ds(2 * lo + i * hi, hi)]))
        moves.append((wd_hbm.at[at], wd_ref.at[slot]))
        return [copy(a, b, w_sem.at[slot, i]) for i, (a, b) in enumerate(moves)]

    def sums_in(e, slot):
        return copy(prev.at[e], sums.at[slot], sum_sem.at[slot])

    def sums_out(e, slot):
        return copy(sums.at[slot], grad.at[e], sum_sem.at[slot])

    def keeps(e, slot):
        at = (layer, tab_ref[ROW_EXPERT * LANES + e])
        return [copy(keep_buf.at[slot, i], finals[i].at[at], keep_sem.at[slot, i]) for i in range(3)] + [
            copy(keep_buf.at[slot], sent.at[e], keep_sem.at[slot, 3])]

    def read(e, slot):
        return copy(got.at[e], got_buf.at[slot], read_sem.at[slot])

    def writes(e, slot):
        to = tab_ref[TAB_ROWS * LANES + e]
        return [copy(got_buf.at[slot, i], finals[i].at[got_layer, to], write_sem.at[slot, i]) for i in range(3)]

    def start(moves):
        for m in moves:
            m.start()

    def wait(moves):
        for m in moves:
            m.wait()

    n_tab = TAB_ROWS * LANES
    lists = [copy(tab_hbm.at[pl.ds(row_id * n_tab, n_tab)], tab_ref.at[pl.ds(0, n_tab)], list_sem.at[0]),
             copy(idx_hbm.at[pl.ds(row_id * N_SRC * list_len, N_SRC * list_len)], idx.at[pl.ds(0, N_SRC * list_len)],
                  list_sem.at[1]),
             copy(gate_hbm.at[pl.ds(row_id * gate_ref.shape[0], gate_ref.shape[0])], gate_ref, list_sem.at[2])]
    if got is not None:
        at = (got_layer * TAB_ROWS + ROW_PARTNER) * LANES
        lists.append(copy(tab_hbm.at[pl.ds(at, LANES)], tab_ref.at[pl.ds(n_tab, LANES)], list_sem.at[3]))
    start(lists)
    pieces = []
    for s in range(N_SRC):
        pieces.append((u_pieces[s], picks[0][s], s, 0, fwd))
        if bwd:
            pieces.append((dy_pieces[s], picks[1][s], s, HALF, own))
    lands = [copy(ref.at[pick], land.at[i % 2], land_sem.at[i % 2]) for i, (ref, pick, *_) in enumerate(pieces)]
    start(lands[:2])
    lists[0].wait()
    start(weights(0, 0))
    if bwd and not own:
        sums_in(0, 0).start()
    if got is not None:
        lists[3].wait()
        read(0, 0).start()
    if own:
        def clear(c, _):
            for k in range(4):
                acc[pl.ds(al(c * 1152 + 288 * k, 8), 288), :] = jnp.zeros((288, LANES), F32)
            return 0

        lax.fori_loop(0, acc.shape[0] // 1152, clear, 0)
        row_ref[...] = jnp.zeros(row_ref.shape, F32)
    rows = 256
    for i, (_, _, s, o, seed) in enumerate(pieces):
        lands[i].wait()

        def fill(c, _, i=i, o=o, seed=seed, s=s):
            r = al(c * rows, rows)
            for j in range(HALF):
                vals = land[i % 2, pl.ds(r, rows), LANES * j:LANES * (j + 1)].astype(F32)
                to = pl.ds(PITCH * (s * n_blk + r) + o + j, rows, stride=PITCH)
                table[to, :] = vals
                if seed and s == 0:
                    acc[to, :] = vals
            return 0

        lax.fori_loop(0, n_blk // rows, fill, 0)
        if i + 2 < len(pieces):
            lands[i + 2].start()
    wait(lists[1:3])
    for k in range(GRP):
        idx[N_SRC * list_len + k] = 0

    def first(q, _):
        gather(0, 2 * q)
        gather(0, 2 * q + 1)
        return 0

    lax.fori_loop(0, PER_TILE // 2, first, 0)
    convert(0)

    def expert(e, _):
        slot = e & 1
        wait(weights(e, slot))
        if bwd and not own:
            sums_in(e, slot).wait()
        if got is not None:
            read(e, slot).wait()
            start(writes(e, slot))

            @pl.when((e > 0) & (e < n_exp - 1))
            def _():
                wait(writes(e - 1, 1 - slot))

        @pl.when(e < n_exp - 1)
        def _():
            start(weights(e + 1, 1 - slot))
            if bwd and not own:
                sums_in(e + 1, 1 - slot).start()
            if got is not None:
                read(e + 1, 1 - slot).start()

        if bwd and own:
            @pl.when(e > 1)
            def _():
                sums_out(e - 2, slot).wait()

            sums[slot] = jnp.zeros(sums.shape[1:], F32)

        def tile(t, _):
            for q in range(PER_TILE):
                if own:
                    scatter(jnp.maximum(t - 1, 0), q)
                gather(t + 1, q)
            half = ROWS // 2
            for s0 in range(0, ROWS, half):
                sl = slice(s0, s0 + half)
                ab_ref[sl, :] = dot(x_u[sl, :], gu_ref[slot], nt)
                if bwd:
                    dh_ref[sl, :] = dot(x_c[sl, :], wd_ref[slot], nt)
            for r in range(0, ROWS, 16):
                rows = slice(r, r + 16)
                for c in range(0, lo, LANES):
                    h, da, db = middle(ab_ref[rows, c:c + LANES], ab_ref[rows, lo + c:lo + c + LANES],
                                       dh_ref[rows, c:c + LANES] if bwd else None)
                    h_ref[rows, c:c + LANES] = h.astype(BF16)
                    if bwd:
                        dab_ref[rows, c:c + LANES] = da.astype(BF16)
                        dab_ref[rows, lo + c:lo + c + LANES] = db.astype(BF16)
                a = ab_ref[rows, 2 * lo:]
                b = pltpu.roll(a, hi, 1)
                dh = dh_ref[rows, lo:] if bwd else None
                if bwd:
                    dh = jnp.concatenate([dh, dh], axis=1)
                h, da, db = middle(a, b, dh)
                h_ref[rows, lo:] = h[:, :hi].astype(BF16)
                if bwd:
                    dab_ref[rows, 2 * lo:] = jnp.where(low, da, pltpu.roll(db, hi, 1)).astype(BF16)
            for s0 in range(0, ROWS, half):
                sl = slice(s0, s0 + half)
                if fwd:
                    put_rows(0, dot(h_ref[sl, :], wd_ref[slot], nn), s0)
                if bwd and own:
                    put_rows(HALF, dot(dab_ref[sl, :], gu_ref[slot], nn), s0)
            if bwd:
                view = sums.at[slot]
                view[0:2 * ff, :] += dot(dab_ref[...], x_u[...], tn)
                view[2 * ff:, :] += dot(h_ref[...], x_c[...], tn)
            convert(t + 1)
            return 0

        lax.fori_loop(tab_ref[ROW_BOUND * LANES + e], tab_ref[ROW_BOUND * LANES + e + 1], tile, 0)
        if bwd and own:
            sums_out(e, slot).start()
        if bwd and not own:
            @pl.when(e > 1)
            def _():
                wait(keeps(e - 2, slot))

            for i in range(2):
                keep_buf[slot, i, 0:lo, :] = sums[slot, i * lo:(i + 1) * lo, :].astype(BF16)
                keep_buf[slot, i, lo:, :] = sums[slot, 2 * lo + i * hi:2 * lo + (i + 1) * hi, :].astype(BF16)
            keep_buf[slot, 2] = sums[slot, 2 * ff:, :].astype(BF16)
            start(keeps(e, slot))
        return 0

    lax.fori_loop(0, n_exp, expert, 0)
    ends = ((n_exp - 2, (n_exp - 2) % 2), (n_exp - 1, (n_exp - 1) % 2))
    if own:
        end = tab_ref[ROW_BOUND * LANES + n_exp] - 1
        lax.fori_loop(0, PER_TILE, lambda q, _: (scatter(end, q), 0)[1], 0)
        chunk = stage_f.shape[1]
        flights = {}
        n = 0
        for o, out in ((HALF, du_outs), (0, y_outs)):
            for s in range(N_SRC if out else 0):
                wide = s == 0 or p_f32
                stage = stage_f if wide else stage_b
                for c in range(n_blk // chunk):
                    key = (wide, n % 2)
                    if key in flights:
                        flights.pop(key).wait()
                    for j in range(HALF):
                        at = pl.ds(PITCH * (s * n_blk + c * chunk) + o + j, chunk, stride=PITCH)
                        stage[n % 2, :, LANES * j:LANES * (j + 1)] = acc[at, :].astype(stage.dtype)
                    flights[key] = copy(stage.at[n % 2], out[s].at[pl.ds(c * chunk, chunk), :],
                                        out_sem.at[2 * wide + n % 2])
                    flights[key].start()
                    n += 1
        wait(flights.values())
        if bwd:
            for e, slot in ends:
                sums_out(e, slot).wait()
    else:
        for e, slot in ends:
            wait(keeps(e, slot))
            if got is not None:
                wait(writes(e, slot))


def run_experts(routes, layer, half, u, dy, weights, prev, finals, fwd, own, p_f32=False, got=None):
    tab, idx, gates = routes
    bwd = dy is not None
    wg, wu, wd = weights
    n_blk, wide = u[0][0].shape[-2:]
    n_layers, n_local, ff, d = wd.shape
    n_exp = n_local // 2
    row_id = half * n_layers + layer
    list_len = idx.shape[0] // (2 * n_layers * N_SRC)

    arrays = lambda pieces: [v for v, _ in pieces]
    operands = [tab, idx, gates] + arrays(u) + (arrays(dy) if bwd else []) + [wg, wu, wd]
    out_shape, aliases = [], {}
    for use in (fwd, bwd and own):
        if use:
            out_shape += [jax.ShapeDtypeStruct((n_blk, wide), F32 if s == 0 or p_f32 else BF16) for s in range(N_SRC)]
    if bwd and own:
        out_shape.append(jax.ShapeDtypeStruct((n_exp, 3 * ff, d), F32))
    if bwd and not own:
        operands.append(prev)
        if got is not None:
            operands.append(got)
        for i, f in enumerate(finals or ()):
            aliases[len(operands)] = i
            operands.append(f)
        out_shape += [jax.ShapeDtypeStruct((n_layers, n_local, ff, d), BF16)] * 3
        out_shape.append(jax.ShapeDtypeStruct((n_exp, 3, ff, d), BF16))
    sem = lambda *s: pltpu.SemaphoreType.DMA(s)
    mid = lambda n, dt: pltpu.VMEM((ROWS, n), dt)
    table, rows = pltpu.VMEM((PITCH * N_SRC * n_blk, LANES), F32), pltpu.VMEM((PITCH * ROWS, LANES), F32)
    scratch = [pltpu.SMEM(((TAB_ROWS + 1) * LANES,), I32), pltpu.SMEM((N_SRC * list_len + LANES,), I32),
               pltpu.VMEM((N_SRC * list_len // LANES + 8, LANES), F32), pltpu.VMEM((2, n_blk, wide), BF16)]
    scratch += [table, rows] * (1 + own)
    scratch += [pltpu.VMEM((2, 2 * ff, d), BF16), pltpu.VMEM((2, ff, d), BF16), mid(LANES, F32)]
    scratch += [mid(d, BF16)] * (1 + bwd) + [mid(2 * ff, F32)] + [mid(ff, F32)] * bwd + [mid(ff, BF16)]
    scratch += [mid(2 * ff, BF16), pltpu.VMEM((2, 3 * ff, d), F32)] * bwd
    if bwd and not own:
        scratch.append(pltpu.VMEM((2, 3, ff, d), BF16))
    if got is not None:
        scratch.append(pltpu.VMEM((2, 3, ff, d), BF16))
    scratch += [sem(4), sem(2), sem(2, 5)] + [sem(2)] * bwd
    if bwd and not own:
        scratch.append(sem(2, 4))
    if got is not None:
        scratch += [sem(2), sem(2, 3)]
    if own:
        scratch += [pltpu.VMEM((2, 256, wide), F32), pltpu.VMEM((2, 256, wide), BF16), sem(4)]
    passes = 2 + fwd + bwd * (4 + 2 * own)
    flops = 2 * d * ff * passes * n_blk * N_SRC * 2
    picks = [[i for _, i in u], [i for _, i in dy] if bwd else None]
    cfg = (fwd, bwd, own, layer, n_blk, d, ff, n_exp, picks, row_id, list_len, p_f32, len(aliases),
           None if got is None else 1 - layer)
    return pl.pallas_call(
        functools.partial(expert_kernel, cfg),
        out_shape=out_shape,
        in_specs=[any_space] * len(operands),
        out_specs=[any_space] * len(out_shape),
        scratch_shapes=scratch,
        input_output_aliases=aliases,
        compiler_params=pltpu.CompilerParams(
            vmem_limit_bytes=VMEM_LIMIT),
        cost_estimate=pl.CostEstimate(flops=flops, bytes_accessed=3 * 2 * n_exp * d * ff, transcendentals=0),
        name=f"experts_{'f' if fwd else ''}{'b' if bwd else ''}_{'own' if own else 'other'}_{layer}",
    )(*operands)


def place_kernel(layer, n_exp, tab_at, tab_ref, got_ref, *refs):
    outs, (buf, in_sem, out_sem) = refs[3:6], refs[6:]
    reads = [pltpu.make_async_copy(got_ref.at[i], buf.at[i], in_sem.at[i]) for i in range(n_exp)]
    for read in reads:
        read.start()
    writes = []
    for i, read in enumerate(reads):
        read.wait()
        e = tab_ref[tab_at + i]
        for k, out in enumerate(outs):
            writes.append(pltpu.make_async_copy(buf.at[i, k], out.at[layer, e], out_sem.at[i, k]))
            writes[-1].start()
    for write in writes:
        write.wait()


def place(tab, layer, got, finals):
    n_exp = got.shape[0]
    return pl.pallas_call(
        functools.partial(place_kernel, layer, n_exp, (layer * TAB_ROWS + ROW_PARTNER) * LANES),
        out_shape=[jax.ShapeDtypeStruct(f.shape, f.dtype) for f in finals],
        grid_spec=pltpu.PrefetchScalarGridSpec(
            num_scalar_prefetch=1, grid=(1,), in_specs=[any_space] * 4, out_specs=[any_space] * 3,
            scratch_shapes=[pltpu.VMEM(got.shape, got.dtype), pltpu.SemaphoreType.DMA((n_exp,)),
                            pltpu.SemaphoreType.DMA((n_exp, 3))]),
        input_output_aliases={2: 0, 3: 1, 4: 2},
        compiler_params=pltpu.CompilerParams(vmem_limit_bytes=VMEM_LIMIT),
        cost_estimate=pl.CostEstimate(flops=0, bytes_accessed=4 * got.size, transcendentals=0),
        name=f"place_{layer}",
    )(tab, got, *finals)


def peer(rel):
    return {name: (lax.axis_index(name) + ((rel >> bit) & 1)) % 2 for bit, name in enumerate(("ep", "core", "x"))}


def meet(rels):
    barrier = pltpu.get_barrier_semaphore()
    for rel in rels:
        pl.semaphore_signal(barrier, inc=1, device_id=peer(rel), device_id_type=MESH)
    pl.semaphore_wait(barrier, len(rels))


def remote(src, dst, send, recv, rel):
    return pltpu.make_async_remote_copy(src_ref=src, dst_ref=dst, send_sem=send, recv_sem=recv,
                                        device_id=peer(rel), device_id_type=MESH)


def share_kernel(n_rel, mine_ref, all_ref, send_sem, recv_sem):
    meet(range(1, n_rel))
    copies = [remote(mine_ref, all_ref.at[rel], send_sem.at[rel], recv_sem.at[rel], rel) for rel in range(1, n_rel)]
    for copy in copies:
        copy.start()
    all_ref[0] = mine_ref[...]
    for copy in copies:
        copy.wait()


def share(mine, n_rel):
    return pl.pallas_call(
        functools.partial(share_kernel, n_rel),
        out_shape=jax.ShapeDtypeStruct((n_rel,) + mine.shape, mine.dtype),
        in_specs=[in_vmem],
        out_specs=in_vmem,
        scratch_shapes=[pltpu.SemaphoreType.DMA((n_rel,)), pltpu.SemaphoreType.DMA((n_rel,))],
        compiler_params=pltpu.CompilerParams(collective_id=0, has_side_effects=True),
        cost_estimate=pl.CostEstimate(flops=10 ** 7, bytes_accessed=mine.size * 4 * n_rel, transcendentals=0),
        name="share_lists",
    )(mine)


def blocks_kernel(cfg, *refs):
    n_chunk, reduce, across, back, d = cfg
    refs = list(refs)
    take = lambda n: [refs.pop(0) for _ in range(n)]
    parts = take(N_SRC)
    m_ref, o_total, o_a, o_b = take(4)
    o_xa, o_xb = take(2) if across else (None, None)
    in_f, in_b, got_f, s_buf, r_buf, t_buf, u_buf, load, send, recv, put = take(11)
    n_rows = t_buf.shape[0] // n_chunk
    cut = [pl.ds(k * n_rows, n_rows) for k in range(n_chunk)]
    chunks = range(n_chunk)
    loads = {}
    for i, part in enumerate(parts[:2] if reduce else parts):
        buf = in_f.at[i] if reduce or i == 0 else in_b.at[i - 1]
        for k in chunks:
            loads[i, k] = pltpu.make_async_copy(part.at[cut[k]], buf.at[cut[k]], load.at[i, k])
    order = (1, 0) if reduce else range(N_SRC)
    for i in order:
        for k in chunks:
            loads[i, k].start()
    u_buf[...] = jnp.zeros(u_buf.shape, BF16)
    meet((Y, CORE, X) if across else (Y, CORE))
    links = []

    def link(src, dst, rel):
        n = len(links)
        links.append([remote(src.at[cut[k]], dst.at[cut[k]], send.at[n, k], recv.at[n, k], rel) for k in chunks])
        return links[-1]

    if reduce:
        first = link(parts[3], got_f.at[1], CORE)
        second = link(parts[2], got_f.at[0], CORE)
        over = link(s_buf, r_buf, Y)
        for copies in (first, second):
            for copy in copies:
                copy.start()
        for k in chunks:
            loads[1, k].wait()
            first[k].wait_recv()
            s_buf[cut[k], :] = (in_f[1, cut[k], :] + got_f[1, cut[k], :]).astype(BF16)
            over[k].start()
    to_y = link(u_buf, o_a.at[1], Y)
    to_core = link(u_buf, o_b.at[0], CORE)
    to_x = link(u_buf, o_xa.at[0], X) if across else None
    puts = []
    for k in chunks:
        if reduce:
            loads[0, k].wait()
            second[k].wait_recv()
            over[k].wait_recv()
            total = in_f[0, cut[k], :] + got_f[0, cut[k], :] + r_buf[cut[k], :].astype(F32)
        else:
            for i in range(N_SRC):
                loads[i, k].wait()
            total = in_f[0, cut[k], :]
            for i in range(N_SRC - 1):
                total = total + in_b[i, cut[k], :].astype(F32)
        total = total.astype(BF16)
        t_buf[cut[k], :] = total
        dims = (((1,), (1 if back else 0,)), ((), ()))
        mixed = lax.dot_general(total[:, :d], m_ref[...], dims, preferred_element_type=F32)
        u_buf[cut[k], 0:d] = (total[:, :d].astype(F32) + mixed).astype(BF16)
        to_y[k].start()
        to_core[k].start()
        if across:
            to_x[k].start()
        puts.append(pltpu.make_async_copy(u_buf.at[cut[k]], o_a.at[0, cut[k]], put.at[0, k]))
        puts.append(pltpu.make_async_copy(t_buf.at[cut[k]], o_total.at[cut[k]], put.at[1, k]))
        for copy in puts[-2:]:
            copy.start()
    on = link(o_a.at[1], o_b.at[1], CORE)
    on_x = link(o_a.at[1], o_xa.at[1], X) if across else None
    for k in chunks:
        to_y[k].wait_recv()
        on[k].start()
        if across:
            on_x[k].start()
    if across:
        last = [link(o_xa.at[i], o_xb.at[i], CORE) for i in range(2)]
        for i, arrived in enumerate((to_x, on_x)):
            for k in chunks:
                arrived[k].wait_recv()
                last[i][k].start()
    waited = [to_y] + ([first, second, over] if reduce else []) + ([to_x, on_x] if across else [])
    for copies in links:
        for copy in copies:
            if any(copies is w for w in waited):
                copy.wait_send()
            else:
                copy.wait()
    for copy in puts:
        copy.wait()


def complete_blocks(parts, m, reduce, across, back, ident, n_chunk=4):
    n_blk, wide = parts[0].shape
    d = m.shape[0]
    sem = lambda *s: pltpu.SemaphoreType.DMA(s)
    pair = jax.ShapeDtypeStruct((2, n_blk, wide), BF16)
    buf = lambda n, dt: pltpu.VMEM((n, n_blk, wide) if n else (n_blk, wide), dt)
    return pl.pallas_call(
        functools.partial(blocks_kernel, (n_chunk, reduce, across, back, d)),
        out_shape=[jax.ShapeDtypeStruct((n_blk, wide), BF16)] + [pair] * (4 if across else 2),
        in_specs=[any_space] * N_SRC + [in_vmem],
        out_specs=[any_space] * (5 if across else 3),
        scratch_shapes=[buf(2, F32), buf(3, BF16), buf(2, F32), buf(0, BF16), buf(0, BF16), buf(0, BF16), buf(0, BF16),
                        sem(4, n_chunk), sem(10, n_chunk), sem(10, n_chunk), sem(2, n_chunk)],
        compiler_params=pltpu.CompilerParams(collective_id=ident, has_side_effects=True, vmem_limit_bytes=VMEM_LIMIT),
        cost_estimate=pl.CostEstimate(flops=10 ** 8, bytes_accessed=n_blk * wide * 40, transcendentals=0),
        name=f"complete_blocks_{ident}",
    )(*parts, m)


def total_kernel(n_chunk, g_ref, o_ref, give, got, s_buf, y_buf, t_buf, x_buf, z_buf, send, recv):
    core = lax.axis_index('core')
    n_rows = o_ref.shape[1] // n_chunk
    cut = [pl.ds(k * n_rows, n_rows) for k in range(n_chunk)]
    first = core > 0
    give[...] = jnp.where(first, g_ref[0], g_ref[1])
    meet((Y, CORE, X))
    copies = [[remote(src.at[cut[k]], dst.at[cut[k]], send.at[i, k], recv.at[i, k], rel) for k in range(n_chunk)]
              for i, (src, dst, rel) in enumerate(((give, got, CORE), (s_buf, y_buf, Y), (t_buf, x_buf, X)))]
    for copy in copies[0]:
        copy.start()
    for k in range(n_chunk):
        copies[0][k].wait_recv()
        mine = jnp.where(first, g_ref[1, cut[k], :], g_ref[0, cut[k], :])
        s_buf[cut[k], :] = (mine + got[cut[k], :]).astype(BF16)
        copies[1][k].start()
    for k in range(n_chunk):
        copies[1][k].wait_recv()
        t_buf[cut[k], :] = (s_buf[cut[k], :].astype(F32) + y_buf[cut[k], :].astype(F32)).astype(BF16)
        copies[2][k].start()
    for k in range(n_chunk):
        copies[2][k].wait_recv()
        got[cut[k], :] = t_buf[cut[k], :].astype(F32) + x_buf[cut[k], :].astype(F32)
    for group in copies:
        for copy in group:
            copy.wait_send()
    s_buf[...] = got[...].astype(BF16)
    swap = remote(s_buf, z_buf, send.at[3, 0], recv.at[3, 0], CORE)
    swap.start()
    swap.wait()
    o_ref[0] = jnp.where(first, z_buf[...], s_buf[...])
    o_ref[1] = jnp.where(first, s_buf[...], z_buf[...])


def total_grads(g, ident, n_chunk=4):
    _, d, _ = g.shape
    buf = lambda dt: pltpu.VMEM((d, d), dt)
    return pl.pallas_call(
        functools.partial(total_kernel, n_chunk),
        out_shape=jax.ShapeDtypeStruct(g.shape, BF16),
        in_specs=[in_vmem], out_specs=in_vmem,
        scratch_shapes=[buf(F32), buf(F32), buf(BF16), buf(BF16), buf(BF16), buf(BF16), buf(BF16),
                        pltpu.SemaphoreType.DMA((4, n_chunk)), pltpu.SemaphoreType.DMA((4, n_chunk))],
        compiler_params=pltpu.CompilerParams(collective_id=ident, has_side_effects=True),
        cost_estimate=pl.CostEstimate(flops=10 ** 7, bytes_accessed=g.size * 8, transcendentals=0),
        name="total_grads",
    )(g)


def solution(mesh):
    ep_size, dp_size = mesh.shape['ep'], mesh.shape['dp']
    sub = Mesh(mesh.devices.reshape(ep_size, dp_size // 2, 2), ('ep', 'x', 'core'))
    tok_axes = ('x', 'core', 'ep')
    tok_spec = P(tok_axes, None)
    route_spec = P(None, tok_axes, None)
    whole_spec = P(None, None, None)
    expert_spec = P(None, 'ep', None, None)
    flip = [(0, 1), (1, 0)]
    move = lambda v, axis: lax.ppermute(v, axis, flip)
    move_diag = lambda v: lax.ppermute(v, ('ep', 'core'), [(0, 3), (1, 2), (2, 1), (3, 0)])
    fence = lax.optimization_barrier

    def device_step(tokens, d_out, expert_ids, gate_vals, w_mix, w_gate, w_up, w_down):
        n_layers, d = w_mix.shape[0], w_mix.shape[1]
        n_tok = tokens.shape[0]
        top = expert_ids.shape[2]
        n_local = w_gate.shape[1]
        n_exp = n_local * ep_size
        n = n_tok * top
        n_rel = 2 * N_SRC
        wide = cdiv(d, LANES) * LANES
        weights = (jnp.swapaxes(w_gate, 2, 3), jnp.swapaxes(w_up, 2, 3), w_down)
        pad = lambda v: jnp.pad(v, ((0, 0), (0, wide - d)))
        send_three = lambda p: [move(p[1], 'ep'), move(p[2], 'core'), move_diag(p[3])]

        def own_sum(p, got):
            return sum([g.astype(F32) for g in got], p)[:, :d].astype(BF16)

        one = lambda v: v.reshape(1, n_tok, wide)
        pairs = lambda a, b: [(a, 0), (a, 1), (b, 0), (b, 1)]

        u0 = pad((tokens.astype(F32) + jnp.dot(tokens, w_mix[0], preferred_element_type=F32)).astype(BF16))
        u0_far = move(u0, 'ep')
        lists = [sorted_list(expert_ids[l], gate_vals[l]) for l in range(n_layers)]
        counts = jnp.sum((expert_ids.reshape(n_layers, n, 1) == jnp.arange(n_exp, dtype=I32)).astype(F32), axis=1)
        packed = jnp.concatenate([jnp.concatenate([v[0] for v in lists] + [v[1] for v in lists]).reshape(-1, LANES),
                                  jnp.pad(counts, ((0, 8 - n_layers), (0, LANES - n_exp)))], axis=0)
        u0_far, packed = fence((u0_far, packed))
        shared = share(packed, n_rel)
        u0_a = jnp.stack([u0, u0_far])
        u0_b = move(u0_a, 'core')
        u0_half = pairs(u0_a, u0_b)
        dy, shared = fence((pad(d_out), shared))
        dy_y, dy_x = move(dy, 'ep'), move(dy, 'x')
        routes = plan(shared, n_layers, n_local, n_tok, n // LANES)
        part = run_experts(routes, 0, 0, u0_half, None, weights, None, None, True, True, p_f32=True)
        dy_y, dy_x, part = fence((dy_y, dy_x, part))
        dy_core, dy_diag, dy_xy, dy_xc = move(dy, 'core'), move(dy_y, 'core'), move(dy_y, 'x'), move(dy_x, 'core')
        y0, u1_a, u1_b = complete_blocks(part, w_mix[1], True, False, False, 1)
        dy_core, dy_diag, dy_xy, dy_xc, u0_a2, y0, u1_a, u1_b = fence(
            (dy_core, dy_diag, dy_xy, dy_xc, u0_a, y0, u1_a, u1_b))
        dy_xd = move(dy_xy, 'core')
        dy_half = [(one(v), 0) for v in (dy, dy_y, dy_core, dy_diag)]
        dy_other = [(one(v), 0) for v in (dy_x, dy_xy, dy_xc, dy_xd)]
        u1_xa, u0_xa = move(u1_a, 'x'), move(u0_a2, 'x')
        out = run_experts(routes, 1, 0, pairs(u1_a, u1_b), dy_half, weights, None, None, True, True)
        u1_xa, u0_xa, dy_xd, out = fence((u1_xa, u0_xa, dy_xd, out))
        dy_other[3] = (one(dy_xd), 0)
        y_part, du_part, g1 = out[:4], out[4:8], out[8]
        u1_xb = move(u1_xa, 'core')
        got = send_three(du_part)
        out = run_experts(routes, 1, 1, pairs(u1_xa, u1_xb), dy_other, weights, g1, None, False, False)
        got, u0_xa, out = fence((got, u0_xa, out))
        *finals, sent1 = out
        du1, dx_a, dx_b = complete_blocks([du_part[0], *got], w_mix[1], False, False, True, 2)
        dx_a, y_part, sent1, u0_xa = fence((dx_a, y_part, sent1, u0_xa))
        dx_xa = move(dx_a, 'x')
        got_y = send_three(y_part)
        got1 = move(sent1, 'core')
        u0_xb = move(u0_xa, 'core')
        out = run_experts(routes, 0, 0, u0_half, pairs(dx_a, dx_b), weights, None, None, False, True)
        dx_xa, got_y, got1, u0_xb, out = fence((dx_xa, got_y, got1, u0_xb, out))
        du_part, g0 = out[:4], out[4]
        dx_xb = move(dx_xa, 'core')
        got = send_three(du_part)
        out = run_experts(routes, 0, 1, pairs(u0_xa, u0_xb), pairs(dx_xa, dx_xb), weights, g0, finals, False, False,
                          got=got1)
        got, out = fence((got, out))
        *finals, sent0 = out
        got0 = move(sent0, 'core')
        du0 = own_sum(du_part[0], got)
        tx = lambda x, du: jnp.einsum('td,te->de', x, du, preferred_element_type=F32)
        g_mix = total_grads(jnp.stack([tx(tokens, du0), tx(y0[:, :d], du1[:, :d])]), 3)
        y1 = own_sum(y_part[0], got_y)
        dx0 = (du0.astype(F32) + jnp.einsum('te,de->td', du0, w_mix[0], preferred_element_type=F32)).astype(BF16)
        finals, got0, g_mix = fence((finals, got0, g_mix))
        finals = place(routes[0], 0, got0, finals)
        return (y1, dx0, g_mix, jnp.swapaxes(finals[0], 2, 3), jnp.swapaxes(finals[1], 2, 3), finals[2])

    return jax.shard_map(device_step, mesh=sub,
                         in_specs=(tok_spec, tok_spec, route_spec, route_spec, whole_spec,
                                   expert_spec, expert_spec, expert_spec),
                         out_specs=(tok_spec, tok_spec, whole_spec, expert_spec, expert_spec, expert_spec),
                         check_vma=False)
```

```python
import functools

import jax
import jax.numpy as jnp
from jax import lax
from jax.experimental import pallas as pl
from jax.experimental.pallas import tpu as pltpu
from jax.sharding import Mesh, PartitionSpec as P

F32, BF16, I32 = jnp.float32, jnp.bfloat16, jnp.int32
MESH = pl.DeviceIdType.MESH
ROWS = 384
GRP = 8
PITCH = 9
FULL = 8
HALF = 4
CAP_FACTOR = 3
LANES = 128
N_SRC = 4
Y, CORE, X = 1, 2, 4
VMEM_LIMIT = 62 * 1024 * 1024
PER_TILE = ROWS // GRP
ROW_BOUND, ROW_GOFF, ROW_EXPERT, ROW_PARTNER, TAB_ROWS = 32, 33, 34, 35, 40
SLOT_GROUPS = 256


def cdiv(a, b):
    return (a + b - 1) // b


def spans(d):
    return [(LANES * j, min(LANES, d - LANES * j)) for j in range(cdiv(d, LANES))]


any_space = pl.BlockSpec(memory_space=pl.ANY)
in_vmem = pl.BlockSpec(memory_space=pltpu.VMEM)


def sorted_list(expert_ids, gate_vals):
    n_tok, top = expert_ids.shape
    n = n_tok * top
    keys = expert_ids.reshape(n) * n + jnp.arange(n, dtype=I32)
    keys, gates = lax.sort((keys, gate_vals.reshape(n)), num_keys=1)
    return ((keys % n) // top).astype(F32), gates


def plan_kernel(n_layers, n_local, n_tok, list_rows, deal_ref, all_ref, tab_ref, idx_ref, gate_ref):
    n_mine = n_local // 2
    core, ep = lax.axis_index('core'), lax.axis_index('ep')
    list_len = list_rows * LANES
    lane = lambda n: lax.broadcasted_iota(I32, (n, LANES), 1).astype(F32)
    sub = lambda n: lax.broadcasted_iota(I32, (n, LANES), 0).astype(F32)
    over_lanes = lambda v: jnp.sum(v, axis=1, keepdims=True)
    over_subs = lambda v: jnp.sum(v, axis=0, keepdims=True)
    l16, s16 = lane(n_mine), sub(n_mine)
    groups = lambda c: jnp.floor((c + (GRP - 0.5)) * (1.0 / GRP))
    for l in range(n_layers):
        cnt = all_ref[:, 2 * n_layers * list_rows + l, :]
        ends = cnt
        step = 1
        while step < 2 * n_local:
            ends = ends + jnp.where(lane(N_SRC) >= step, pltpu.roll(ends, step, 1), 0.0)
            step *= 2
        starts = ends - cnt
        second = (ep > 0)
        local = lambda v: jnp.where(lane(N_SRC) < n_local, jnp.where(second, pltpu.roll(v, LANES - n_local, 1), v), 0.0)
        cnt, starts = local(cnt), local(starts)
        tiles = jnp.floor((over_subs(groups(local(deal_ref[:, 2 * n_layers * list_rows + l, :]))) + (PER_TILE - 0.5))
                          * (1.0 / PER_TILE))
        load = jnp.where(lane(1) < n_local, jnp.maximum(1.0, tiles), -1.0)
        wide = jnp.broadcast_to(load, (n_local, LANES))
        col = over_lanes(jnp.where(lane(n_local) == sub(n_local), wide, 0.0))
        ahead = (col > wide) | ((col == wide) & (sub(n_local) < lane(n_local)))
        rank = over_subs(jnp.where(ahead, 1.0, 0.0))
        odd = s16 - 2.0 * jnp.floor(s16 * 0.5 + 0.25)
        flip = jnp.where(core > 0, 1.0 - odd, odd)
        dealt = lambda f: (jnp.broadcast_to(rank, (n_mine, LANES)) == 2.0 * s16 + f) & (l16 < n_local)
        pick = dealt(flip)
        choose = lambda p, row: over_lanes(jnp.where(p, jnp.broadcast_to(row, (n_mine, LANES)), 0.0))
        mine = lambda row: choose(pick, row)
        as_row = lambda c: over_subs(jnp.where(l16 == s16, c, 0.0))
        experts = as_row(mine(lane(1)))
        partner = as_row(choose(dealt(1.0 - flip), lane(1)))
        at = l * TAB_ROWS
        off = jnp.zeros((n_mine, 1), F32)
        pos = [jnp.zeros((n_mine, LANES), F32) for _ in range(SLOT_GROUPS // LANES)]
        for s in range(N_SRC):
            c, st = mine(cnt[s:s + 1]), mine(starts[s:s + 1]) + float(s * list_len)
            ng = groups(c)
            for i in range(len(pos)):
                rel = l16 + float(LANES * i) - off
                code = (st + GRP * rel) * 16.0 + jnp.minimum(float(GRP), c - GRP * rel)
                pos[i] = jnp.where((rel >= 0) & (rel < ng), code, pos[i])
            off = off + ng
        for i in range(len(pos)):
            tab_ref[pl.ds(at + i, n_mine, stride=len(pos)), :] = pos[i].astype(I32)
        n_tiles = jnp.maximum(1.0, jnp.floor((off + (PER_TILE - 0.5)) * (1.0 / PER_TILE)))
        bounds = over_subs(jnp.where(s16 < l16, n_tiles, 0.0))
        before = over_lanes(jnp.where(l16 == s16, jnp.broadcast_to(bounds, (n_mine, LANES)), 0.0))
        t = jnp.minimum(l16, over_subs(jnp.broadcast_to(n_tiles, (n_mine, LANES))) - 1.0)
        inside = (t >= before) & (t < before + n_tiles)
        goff = over_subs(jnp.where(inside, s16 * float(SLOT_GROUPS) + (t - before) * float(PER_TILE), 0.0))
        rows = [(ROW_BOUND, bounds), (ROW_GOFF, goff), (ROW_EXPERT, experts), (ROW_PARTNER, partner)]
        for row, value in rows:
            tab_ref[at + row:at + row + 1, :] = value.astype(I32)
    for l in range(n_layers):
        pad = l * (N_SRC * list_rows + 8) + N_SRC * list_rows
        gate_ref[pad:pad + 8, :] = jnp.zeros((8, LANES), F32)
        for s in range(N_SRC):
            to = (l * N_SRC + s) * list_rows
            toks = all_ref[s, l * list_rows:(l + 1) * list_rows, :]
            idx_ref[to:to + list_rows, :] = ((toks + float(s * n_tok)) * float(PITCH)).astype(I32)
            to = l * (N_SRC * list_rows + 8) + s * list_rows
            gate_ref[to:to + list_rows, :] = all_ref[s, (n_layers + l) * list_rows:(n_layers + l + 1) * list_rows, :]


def plan(deal, shared, n_layers, n_local, n_tok, list_rows):
    n_tab = n_layers * TAB_ROWS
    n_list = n_layers * N_SRC * list_rows
    n_gate = n_layers * (N_SRC * list_rows + 8)
    tab, idx, gates = pl.pallas_call(
        functools.partial(plan_kernel, n_layers, n_local, n_tok, list_rows),
        out_shape=[jax.ShapeDtypeStruct((n_tab, LANES), I32), jax.ShapeDtypeStruct((n_list, LANES), I32),
                   jax.ShapeDtypeStruct((n_gate, LANES), F32)],
        in_specs=[in_vmem] * 2, out_specs=[in_vmem] * 3,
        cost_estimate=pl.CostEstimate(flops=10 ** 7, bytes_accessed=10 ** 6, transcendentals=0),
        name="plan",
    )(deal, shared)
    return tab.reshape(-1), idx.reshape(-1), gates


def expert_kernel(cfg, *refs):
    fwd, bwd, own, layer, n_blk, d, ff, n_exp, picks, row_id, list_len, p_f32, n_alias, got_layer = cfg
    refs = list(refs)
    take = lambda n: [refs.pop(0) for _ in range(n)]
    tab_hbm, idx_hbm, gate_hbm = take(3)
    u_pieces = take(N_SRC)
    dy_pieces = take(N_SRC) if bwd else []
    wg_hbm, wu_hbm, wd_hbm = take(3)
    prev = take(1)[0] if bwd and not own else None
    got = take(2) if got_layer is not None else None
    take(n_alias)
    y_outs = take(N_SRC) if fwd else []
    du_outs = take(N_SRC) if bwd and own else []
    grad = take(1)[0] if bwd and own else None
    finals = take(3) if bwd and not own else None
    sent = take(2) if bwd and not own else None
    tab_ref, idx, gate_ref, land, table, gat = take(6)
    acc, row_ref = take(2) if own else (None, None)
    gu_ref, wd_ref, g_ref, x_u = take(4)
    x_c = take(1)[0] if bwd else None
    ab_ref = take(1)[0]
    dh_ref = take(1)[0] if bwd else None
    h_ref = take(1)[0]
    dab_ref, sums = take(2) if bwd else (None, None)
    keep_buf = take(1)[0] if bwd and not own else None
    got_buf = take(1)[0] if got is not None else None
    list_sem, land_sem, w_sem = take(3)
    sum_sem = take(1)[0] if bwd else None
    keep_sem = take(1)[0] if bwd and not own else None
    read_sem, write_sem = take(2) if got is not None else (None, None)
    stage_f, out_sem = take(2) if own else (None, None)

    copy = pltpu.make_async_copy
    cols = spans(d)
    lo = ff // 256 * 256
    hi = ff - lo
    dot = functools.partial(lax.dot_general, preferred_element_type=F32)
    nn = (((1,), (0,)), ((), ()))
    nt = (((1,), (1,)), ((), ()))
    tn = (((0,), (0,)), ((), ()))
    al = pl.multiple_of
    n_row = N_SRC * n_blk
    glane = lax.broadcasted_iota(I32, (GRP, LANES), 1)
    gsub = lax.broadcasted_iota(I32, (GRP, LANES), 0)

    def row_at(r):
        return pl.ds(r * PITCH, FULL)

    def group(tile, q):
        return tab_ref[tab_ref[ROW_GOFF * LANES + tile] + q]

    def gather(tile, q):
        ids = idx.at[pl.ds(group(tile, q) >> 4, GRP)]
        for k in range(GRP):
            gat[row_at(q * GRP + k), :] = table[pl.ds(ids[k], FULL), :]

    def gate_column(code):
        pos = code >> 4
        row, shift = pos >> 7, pos & (LANES - 1)
        want = glane == gsub + shift
        over = glane == gsub + (shift - LANES)
        here = gate_ref[pl.ds(row, GRP, stride=0), :]
        there = gate_ref[pl.ds(row + 1, GRP, stride=0), :]
        v = jnp.where(want, here, jnp.where(over, there, 0.0))
        return jnp.where(gsub < (code & 15), jnp.sum(v, axis=1, keepdims=True), 0.0)

    def scatter(tile, q):
        ids = idx.at[pl.ds(group(tile, q) >> 4, GRP)]
        new = []
        for k in range(GRP):
            at = pl.ds(ids[k], FULL)
            new.append((at, acc[at, :] + row_ref[row_at(q * GRP + k), :]))
        for at, value in reversed(new):
            acc[at, :] = value

    def convert(tile):
        for q in range(0, PER_TILE, 2):
            part = []
            for p in (q, q + 1):
                code = group(tile, p)
                rows = [gat[pl.ds(GRP * PITCH * p + j, GRP, stride=PITCH), :] for j in range(FULL if bwd else HALF)]
                real = gsub < (code & 15)
                gate = gate_column(code)
                g_ref[GRP * p:GRP * (p + 1), :] = gate
                part.append([jnp.where(real, v, 0.0) for v in rows[:HALF]] + [v * gate for v in rows[HALF:]])
            at = slice(GRP * q, GRP * (q + 2))
            for x, o in ((x_u, 0), (x_c, HALF)):
                if x is None:
                    continue
                for j, (c, w) in enumerate(cols):
                    both = jnp.concatenate([part[0][o + j], part[1][o + j]], axis=0)
                    x[at, c:c + w] = both[:, :w].astype(BF16)

    def put_rows(o, value, s0):
        value = value.astype(BF16).astype(F32)
        n = value.shape[0]
        for j, (c, w) in enumerate(cols):
            row_ref[pl.ds(PITCH * s0 + o + j, n, stride=PITCH), 0:w] = value[:, c:c + w] * g_ref[s0:s0 + n, 0:w]

    low = lax.broadcasted_iota(I32, (16, 2 * hi), 1) < hi

    def middle(a, b, dh):
        sig = 0.5 * jnp.tanh(0.5 * a) + 0.5
        act = a * sig
        h = act * b
        if dh is None:
            return h, None, None
        slope = sig * (1.0 + a * (1.0 - sig))
        return h, dh * b * slope, dh * act

    def weights(e, slot):
        at = (layer, tab_ref[ROW_EXPERT * LANES + e])
        moves = []
        for i, w in enumerate((wg_hbm, wu_hbm)):
            moves.append((w.at[at + (pl.ds(0, lo),)], gu_ref.at[slot, pl.ds(i * lo, lo)]))
            moves.append((w.at[at + (pl.ds(lo, hi),)], gu_ref.at[slot, pl.ds(2 * lo + i * hi, hi)]))
        moves.append((wd_hbm.at[at], wd_ref.at[slot]))
        return [copy(a, b, w_sem.at[slot, i]) for i, (a, b) in enumerate(moves)]

    def sums_in(e, slot):
        return copy(prev.at[e], sums.at[slot], sum_sem.at[slot])

    def sums_out(e, slot):
        return copy(sums.at[slot], grad.at[e], sum_sem.at[slot])

    def keeps(e, slot):
        at = (layer, tab_ref[ROW_EXPERT * LANES + e])
        return [copy(keep_buf.at[slot, i], finals[i].at[at], keep_sem.at[slot, i]) for i in range(3)]

    def send(e, slot, part):
        return copy(keep_buf.at[slot], sent[part].at[e - part * (n_exp // 2)], keep_sem.at[slot, 3])

    def read(e, slot, part=0):
        return copy(got[part].at[e - part * (n_exp // 2)], got_buf.at[slot], read_sem.at[slot])

    def writes(e, slot):
        to = tab_ref[TAB_ROWS * LANES + e]
        return [copy(got_buf.at[slot, i], finals[i].at[got_layer, to], write_sem.at[slot, i]) for i in range(3)]

    def start(moves):
        for m in moves:
            m.start()

    def wait(moves):
        for m in moves:
            m.wait()

    n_tab = TAB_ROWS * LANES
    lists = [copy(tab_hbm.at[pl.ds(row_id * n_tab, n_tab)], tab_ref.at[pl.ds(0, n_tab)], list_sem.at[0]),
             copy(idx_hbm.at[pl.ds(row_id * N_SRC * list_len, N_SRC * list_len)], idx.at[pl.ds(0, N_SRC * list_len)],
                  list_sem.at[1]),
             copy(gate_hbm.at[pl.ds(row_id * gate_ref.shape[0], gate_ref.shape[0])], gate_ref, list_sem.at[2])]
    if got is not None:
        at = (got_layer * TAB_ROWS + ROW_PARTNER) * LANES
        lists.append(copy(tab_hbm.at[pl.ds(at, LANES)], tab_ref.at[pl.ds(n_tab, LANES)], list_sem.at[3]))
    start(lists)
    pieces = []
    for s in range(N_SRC):
        pieces.append((u_pieces[s], picks[0][s], s, 0, fwd))
        if bwd:
            pieces.append((dy_pieces[s], picks[1][s], s, HALF, own))
    lands = [copy(ref.at[pick], land.at[i % N_SRC], land_sem.at[i % N_SRC]) for i, (ref, pick, *_) in enumerate(pieces)]
    start(lands[:N_SRC])
    lists[0].wait()
    start(weights(0, 0))
    if bwd and not own:
        sums_in(0, 0).start()
    if got is not None:
        lists[3].wait()
        read(0, 0).start()
    if own:
        def clear(c, _):
            for k in range(4):
                acc[pl.ds(al(c * 1152 + 288 * k, 8), 288), :] = jnp.zeros((288, LANES), F32)
            return 0

        lax.fori_loop(0, acc.shape[0] // 1152, clear, 0)
        row_ref[...] = jnp.zeros(row_ref.shape, F32)
    rows = 256
    for i, (_, _, s, o, seed) in enumerate(pieces):
        lands[i].wait()

        def fill(c, _, i=i, o=o, seed=seed, s=s):
            r = al(c * rows, rows)
            for j in range(HALF):
                vals = land[i % N_SRC, pl.ds(r, rows), LANES * j:LANES * (j + 1)].astype(F32)
                to = pl.ds(PITCH * (s * n_blk + r) + o + j, rows, stride=PITCH)
                table[to, :] = vals
                if seed and s == 0:
                    acc[to, :] = vals
            return 0

        lax.fori_loop(0, n_blk // rows, fill, 0)
        if i + N_SRC < len(pieces):
            lands[i + N_SRC].start()
    wait(lists[1:3])
    for k in range(GRP):
        idx[N_SRC * list_len + k] = 0

    def first(q, _):
        gather(0, 2 * q)
        gather(0, 2 * q + 1)
        return 0

    lax.fori_loop(0, PER_TILE // 2, first, 0)
    convert(0)

    def expert(e, _):
        slot = e & 1
        wait(weights(e, slot))
        if bwd and not own:
            sums_in(e, slot).wait()
        if got is not None:
            read(0, slot).wait()
            start(writes(e, slot))

            @pl.when((e > 0) & (e < n_exp - 1))
            def _():
                wait(writes(e - 1, 1 - slot))

        @pl.when(e < n_exp - 1)
        def _():
            start(weights(e + 1, 1 - slot))
            if bwd and not own:
                sums_in(e + 1, 1 - slot).start()
            if got is not None:
                for part in range(2):
                    @pl.when((e + 1 >= n_exp // 2) if part else (e + 1 < n_exp // 2))
                    def _(part=part):
                        read(e + 1, 1 - slot, part).start()

        if bwd and own:
            @pl.when(e > 1)
            def _():
                sums_out(e - 2, slot).wait()

            sums[slot] = jnp.zeros(sums.shape[1:], F32)

        def tile(t, _):
            for q in range(PER_TILE):
                if own:
                    scatter(jnp.maximum(t - 1, 0), q)
                gather(t + 1, q)
            half = ROWS // 2
            for s0 in range(0, ROWS, half):
                sl = slice(s0, s0 + half)
                ab_ref[sl, :] = dot(x_u[sl, :], gu_ref[slot], nt)
                if bwd:
                    dh_ref[sl, :] = dot(x_c[sl, :], wd_ref[slot], nt)
            for r in range(0, ROWS, 16):
                rows = slice(r, r + 16)
                for c in range(0, lo, LANES):
                    h, da, db = middle(ab_ref[rows, c:c + LANES], ab_ref[rows, lo + c:lo + c + LANES],
                                       dh_ref[rows, c:c + LANES] if bwd else None)
                    h_ref[rows, c:c + LANES] = h.astype(BF16)
                    if bwd:
                        dab_ref[rows, c:c + LANES] = da.astype(BF16)
                        dab_ref[rows, lo + c:lo + c + LANES] = db.astype(BF16)
                a = ab_ref[rows, 2 * lo:]
                b = pltpu.roll(a, hi, 1)
                dh = dh_ref[rows, lo:] if bwd else None
                if bwd:
                    dh = jnp.concatenate([dh, dh], axis=1)
                h, da, db = middle(a, b, dh)
                h_ref[rows, lo:] = h[:, :hi].astype(BF16)
                if bwd:
                    dab_ref[rows, 2 * lo:] = jnp.where(low, da, pltpu.roll(db, hi, 1)).astype(BF16)
            for s0 in range(0, ROWS, half):
                sl = slice(s0, s0 + half)
                if fwd:
                    put_rows(0, dot(h_ref[sl, :], wd_ref[slot], nn), s0)
                if bwd and own:
                    put_rows(HALF, dot(dab_ref[sl, :], gu_ref[slot], nn), s0)
            if bwd:
                view = sums.at[slot]
                view[0:2 * ff, :] += dot(dab_ref[...], x_u[...], tn)
                view[2 * ff:, :] += dot(h_ref[...], x_c[...], tn)
            convert(t + 1)
            return 0

        lax.fori_loop(tab_ref[ROW_BOUND * LANES + e], tab_ref[ROW_BOUND * LANES + e + 1], tile, 0)
        if bwd and own:
            sums_out(e, slot).start()
        if bwd and not own:
            @pl.when(e > 1)
            def _():
                wait(keeps(e - 2, slot) + [send(0, slot, 0)])

            for i in range(2):
                keep_buf[slot, i, 0:lo, :] = sums[slot, i * lo:(i + 1) * lo, :].astype(BF16)
                keep_buf[slot, i, lo:, :] = sums[slot, 2 * lo + i * hi:2 * lo + (i + 1) * hi, :].astype(BF16)
            keep_buf[slot, 2] = sums[slot, 2 * ff:, :].astype(BF16)
            start(keeps(e, slot))
            for part in range(2):
                @pl.when((e >= n_exp // 2) if part else (e < n_exp // 2))
                def _(part=part):
                    send(e, slot, part).start()
        return 0

    lax.fori_loop(0, n_exp, expert, 0)
    ends = ((n_exp - 2, (n_exp - 2) % 2), (n_exp - 1, (n_exp - 1) % 2))
    if own:
        end = tab_ref[ROW_BOUND * LANES + n_exp] - 1
        lax.fori_loop(0, PER_TILE, lambda q, _: (scatter(end, q), 0)[1], 0)
        flights = {}
        for o, out in ((HALF, du_outs), (0, y_outs)):
            for s in range(N_SRC if out else 0):
                wide = s == 0 or p_f32
                stage = stage_f.at[s] if wide else land.at[s]
                if s in flights:
                    flights[s].wait()

                def fetch(c, _, stage=stage, s=s, o=o):
                    r = al(c * rows, rows)
                    for j in range(HALF):
                        at = pl.ds(PITCH * (s * n_blk + r) + o + j, rows, stride=PITCH)
                        stage[pl.ds(r, rows), LANES * j:LANES * (j + 1)] = acc[at, :].astype(stage.dtype)
                    return 0

                lax.fori_loop(0, n_blk // rows, fetch, 0)
                flights[s] = copy(stage, out[s], out_sem.at[s])
                flights[s].start()
        wait(flights.values())
        if bwd:
            for e, slot in ends:
                sums_out(e, slot).wait()
    else:
        for e, slot in ends:
            wait(keeps(e, slot) + [send(0, slot, 0)])
            if got is not None:
                wait(writes(e, slot))


def run_experts(routes, layer, u, dy, weights, prev, finals, fwd, own, p_f32=False, got=None):
    tab, idx, gates = routes
    bwd = dy is not None
    wg, wu, wd = weights
    n_blk, wide = u[0][0].shape[-2:]
    n_layers, n_local, ff, d = wd.shape
    n_exp = n_local // 2
    row_id = layer
    list_len = idx.shape[0] // (n_layers * N_SRC)

    arrays = lambda pieces: [v for v, _ in pieces]
    operands = [tab, idx, gates] + arrays(u) + (arrays(dy) if bwd else []) + [wg, wu, wd]
    out_shape, aliases = [], {}
    for use in (fwd, bwd and own):
        if use:
            out_shape += [jax.ShapeDtypeStruct((n_blk, wide), F32 if s == 0 or p_f32 else BF16) for s in range(N_SRC)]
    if bwd and own:
        out_shape.append(jax.ShapeDtypeStruct((n_exp, 3 * ff, d), F32))
    if bwd and not own:
        operands.append(prev)
        if got is not None:
            operands += got
        for i, f in enumerate(finals or ()):
            aliases[len(operands)] = i
            operands.append(f)
        out_shape += [jax.ShapeDtypeStruct((n_layers, n_local, ff, d), BF16)] * 3
        out_shape += [jax.ShapeDtypeStruct((n_exp // 2, 3, ff, d), BF16)] * 2
    sem = lambda *s: pltpu.SemaphoreType.DMA(s)
    mid = lambda n, dt: pltpu.VMEM((ROWS, n), dt)
    table, rows = pltpu.VMEM((PITCH * N_SRC * n_blk, LANES), F32), pltpu.VMEM((PITCH * ROWS, LANES), F32)
    scratch = [pltpu.SMEM(((TAB_ROWS + 1) * LANES,), I32), pltpu.SMEM((N_SRC * list_len + LANES,), I32),
               pltpu.VMEM((N_SRC * list_len // LANES + 8, LANES), F32), pltpu.VMEM((N_SRC, n_blk, wide), BF16)]
    scratch += [table, rows] * (1 + own)
    scratch += [pltpu.VMEM((2, 2 * ff, d), BF16), pltpu.VMEM((2, ff, d), BF16), mid(LANES, F32)]
    scratch += [mid(d, BF16)] * (1 + bwd) + [mid(2 * ff, F32)] + [mid(ff, F32)] * bwd + [mid(ff, BF16)]
    scratch += [mid(2 * ff, BF16), pltpu.VMEM((2, 3 * ff, d), F32)] * bwd
    if bwd and not own:
        scratch.append(pltpu.VMEM((2, 3, ff, d), BF16))
    if got is not None:
        scratch.append(pltpu.VMEM((2, 3, ff, d), BF16))
    scratch += [sem(4), sem(N_SRC), sem(2, 5)] + [sem(2)] * bwd
    if bwd and not own:
        scratch.append(sem(2, 4))
    if got is not None:
        scratch += [sem(2), sem(2, 3)]
    if own:
        scratch += [pltpu.VMEM((N_SRC if p_f32 else 1, n_blk, wide), F32), sem(N_SRC)]
    passes = 2 + fwd + bwd * (4 + 2 * own)
    flops = 2 * d * ff * passes * n_blk * N_SRC * 2
    picks = [[i for _, i in u], [i for _, i in dy] if bwd else None]
    cfg = (fwd, bwd, own, layer, n_blk, d, ff, n_exp, picks, row_id, list_len, p_f32, len(aliases),
           None if got is None else 1 - layer)
    return pl.pallas_call(
        functools.partial(expert_kernel, cfg),
        out_shape=out_shape,
        in_specs=[any_space] * len(operands),
        out_specs=[any_space] * len(out_shape),
        scratch_shapes=scratch,
        input_output_aliases=aliases,
        compiler_params=pltpu.CompilerParams(
            vmem_limit_bytes=VMEM_LIMIT),
        cost_estimate=pl.CostEstimate(flops=flops, bytes_accessed=3 * 2 * n_exp * d * ff, transcendentals=0),
        name=f"experts_{'f' if fwd else ''}{'b' if bwd else ''}_{'own' if own else 'other'}_{layer}",
    )(*operands)


def place_kernel(layer, n_exp, tab_ref, got_ref, *refs):
    outs, (buf, in_sem, out_sem) = refs[3:6], refs[6:]
    reads = [pltpu.make_async_copy(got_ref.at[i], buf.at[i], in_sem.at[i]) for i in range(n_exp)]
    for read in reads:
        read.start()
    writes = []
    for i, read in enumerate(reads):
        read.wait()
        e = tab_ref[i]
        for k, out in enumerate(outs):
            writes.append(pltpu.make_async_copy(buf.at[i, k], out.at[layer, e], out_sem.at[i, k]))
            writes[-1].start()
    for write in writes:
        write.wait()


def place(partner, layer, got, finals):
    n_exp = got.shape[0]
    return pl.pallas_call(
        functools.partial(place_kernel, layer, n_exp),
        out_shape=[jax.ShapeDtypeStruct(f.shape, f.dtype) for f in finals],
        grid_spec=pltpu.PrefetchScalarGridSpec(
            num_scalar_prefetch=1, grid=(1,), in_specs=[any_space] * 4, out_specs=[any_space] * 3,
            scratch_shapes=[pltpu.VMEM(got.shape, got.dtype), pltpu.SemaphoreType.DMA((n_exp,)),
                            pltpu.SemaphoreType.DMA((n_exp, 3))]),
        input_output_aliases={2: 0, 3: 1, 4: 2},
        compiler_params=pltpu.CompilerParams(vmem_limit_bytes=VMEM_LIMIT),
        cost_estimate=pl.CostEstimate(flops=0, bytes_accessed=4 * got.size, transcendentals=0),
        name=f"place_{layer}",
    )(partner, got, *finals)


def peer(rel):
    return {name: (lax.axis_index(name) + ((rel >> bit) & 1)) % 2 for bit, name in enumerate(("ep", "core", "x"))}


def meet(rels):
    barrier = pltpu.get_barrier_semaphore()
    for rel in rels:
        pl.semaphore_signal(barrier, inc=1, device_id=peer(rel), device_id_type=MESH)
    pl.semaphore_wait(barrier, len(rels))


def remote(src, dst, send, recv, rel):
    return pltpu.make_async_remote_copy(src_ref=src, dst_ref=dst, send_sem=send, recv_sem=recv,
                                        device_id=peer(rel), device_id_type=MESH)


def share_kernel(n_rel, mine_ref, all_ref, send_sem, recv_sem):
    meet(range(1, n_rel))
    copies = [remote(mine_ref, all_ref.at[rel], send_sem.at[rel], recv_sem.at[rel], rel) for rel in range(1, n_rel)]
    for copy in copies:
        copy.start()
    all_ref[0] = mine_ref[...]
    for copy in copies:
        copy.wait()


def share(mine, n_rel):
    return pl.pallas_call(
        functools.partial(share_kernel, n_rel),
        out_shape=jax.ShapeDtypeStruct((n_rel,) + mine.shape, mine.dtype),
        in_specs=[in_vmem],
        out_specs=in_vmem,
        scratch_shapes=[pltpu.SemaphoreType.DMA((n_rel,)), pltpu.SemaphoreType.DMA((n_rel,))],
        compiler_params=pltpu.CompilerParams(collective_id=0, has_side_effects=True),
        cost_estimate=pl.CostEstimate(flops=10 ** 7, bytes_accessed=mine.size * 4 * n_rel, transcendentals=0),
        name="share_lists",
    )(mine)


def blocks_kernel(cfg, *refs):
    n_chunk, reduce, across, back, d = cfg
    refs = list(refs)
    take = lambda n: [refs.pop(0) for _ in range(n)]
    parts = take(N_SRC)
    m_ref, o_total, o_a, o_b = take(4)
    o_xa, o_xb = take(2) if across else (None, None)
    in_f, in_b, got_f, s_buf, r_buf, t_buf, u_buf, load, send, recv, put = take(11)
    n_rows = t_buf.shape[0] // n_chunk
    cut = [pl.ds(k * n_rows, n_rows) for k in range(n_chunk)]
    chunks = range(n_chunk)
    loads = {}
    for i, part in enumerate(parts[:2] if reduce else parts):
        buf = in_f.at[i] if reduce or i == 0 else in_b.at[i - 1]
        for k in chunks:
            loads[i, k] = pltpu.make_async_copy(part.at[cut[k]], buf.at[cut[k]], load.at[i, k])
    order = (1, 0) if reduce else range(N_SRC)
    for i in order:
        for k in chunks:
            loads[i, k].start()
    u_buf[...] = jnp.zeros(u_buf.shape, BF16)
    meet((Y, CORE, X) if across else (Y, CORE))
    links = []

    def link(src, dst, rel):
        n = len(links)
        links.append([remote(src.at[cut[k]], dst.at[cut[k]], send.at[n, k], recv.at[n, k], rel) for k in chunks])
        return links[-1]

    if reduce:
        first = link(parts[3], got_f.at[1], CORE)
        second = link(parts[2], got_f.at[0], CORE)
        over = link(s_buf, r_buf, Y)
        for copies in (first, second):
            for copy in copies:
                copy.start()
        for k in chunks:
            loads[1, k].wait()
            first[k].wait_recv()
            s_buf[cut[k], :] = (in_f[1, cut[k], :] + got_f[1, cut[k], :]).astype(BF16)
            over[k].start()
    to_y = link(u_buf, o_a.at[1], Y)
    to_core = link(u_buf, o_b.at[0], CORE)
    to_x = link(u_buf, o_xa.at[0], X) if across else None
    puts = []
    for k in chunks:
        if reduce:
            loads[0, k].wait()
            second[k].wait_recv()
            over[k].wait_recv()
            total = in_f[0, cut[k], :] + got_f[0, cut[k], :] + r_buf[cut[k], :].astype(F32)
        else:
            for i in range(N_SRC):
                loads[i, k].wait()
            total = in_f[0, cut[k], :]
            for i in range(N_SRC - 1):
                total = total + in_b[i, cut[k], :].astype(F32)
        total = total.astype(BF16)
        t_buf[cut[k], :] = total
        dims = (((1,), (1 if back else 0,)), ((), ()))
        mixed = lax.dot_general(total[:, :d], m_ref[...], dims, preferred_element_type=F32)
        u_buf[cut[k], 0:d] = (total[:, :d].astype(F32) + mixed).astype(BF16)
        to_y[k].start()
        to_core[k].start()
        if across:
            to_x[k].start()
        puts.append(pltpu.make_async_copy(u_buf.at[cut[k]], o_a.at[0, cut[k]], put.at[0, k]))
        puts.append(pltpu.make_async_copy(t_buf.at[cut[k]], o_total.at[cut[k]], put.at[1, k]))
        for copy in puts[-2:]:
            copy.start()
    on = link(o_a.at[1], o_b.at[1], CORE)
    on_x = link(o_a.at[1], o_xa.at[1], X) if across else None
    for k in chunks:
        to_y[k].wait_recv()
        on[k].start()
        if across:
            on_x[k].start()
    if across:
        last = [link(o_xa.at[i], o_xb.at[i], CORE) for i in range(2)]
        for i, arrived in enumerate((to_x, on_x)):
            for k in chunks:
                arrived[k].wait_recv()
                last[i][k].start()
    waited = [to_y] + ([first, second, over] if reduce else []) + ([to_x, on_x] if across else [])
    for copies in links:
        for copy in copies:
            if any(copies is w for w in waited):
                copy.wait_send()
            else:
                copy.wait()
    for copy in puts:
        copy.wait()


def complete_blocks(parts, m, reduce, across, back, ident, n_chunk=4):
    n_blk, wide = parts[0].shape
    d = m.shape[0]
    sem = lambda *s: pltpu.SemaphoreType.DMA(s)
    pair = jax.ShapeDtypeStruct((2, n_blk, wide), BF16)
    buf = lambda n, dt: pltpu.VMEM((n, n_blk, wide) if n else (n_blk, wide), dt)
    return pl.pallas_call(
        functools.partial(blocks_kernel, (n_chunk, reduce, across, back, d)),
        out_shape=[jax.ShapeDtypeStruct((n_blk, wide), BF16)] + [pair] * (4 if across else 2),
        in_specs=[any_space] * N_SRC + [in_vmem],
        out_specs=[any_space] * (5 if across else 3),
        scratch_shapes=[buf(2, F32), buf(3, BF16), buf(2, F32), buf(0, BF16), buf(0, BF16), buf(0, BF16), buf(0, BF16),
                        sem(4, n_chunk), sem(10, n_chunk), sem(10, n_chunk), sem(2, n_chunk)],
        compiler_params=pltpu.CompilerParams(collective_id=ident, has_side_effects=True, vmem_limit_bytes=VMEM_LIMIT),
        cost_estimate=pl.CostEstimate(flops=10 ** 8, bytes_accessed=n_blk * wide * 40, transcendentals=0),
        name=f"complete_blocks_{ident}",
    )(*parts, m)


def solution(mesh):
    ep_size, dp_size = mesh.shape['ep'], mesh.shape['dp']
    sub = Mesh(mesh.devices.reshape(ep_size, dp_size // 2, 2), ('ep', 'x', 'core'))
    tok_axes = ('x', 'core', 'ep')
    tok_spec = P(tok_axes, None)
    route_spec = P(None, tok_axes, None)
    whole_spec = P(None, None, None)
    expert_spec = P(None, 'ep', None, None)
    flip = [(0, 1), (1, 0)]
    move = lambda v, axis: lax.ppermute(v, axis, flip)
    move_diag = lambda v: lax.ppermute(v, ('ep', 'core'), [(0, 3), (1, 2), (2, 1), (3, 0)])
    fence = lax.optimization_barrier

    def device_step(tokens, d_out, expert_ids, gate_vals, w_mix, w_gate, w_up, w_down):
        n_layers, d = w_mix.shape[0], w_mix.shape[1]
        n_tok = tokens.shape[0]
        top = expert_ids.shape[2]
        n_local = w_gate.shape[1]
        n_exp = n_local * ep_size
        n = n_tok * top
        n_rel = 2 * N_SRC
        wide = cdiv(d, LANES) * LANES
        weights = (jnp.swapaxes(w_gate, 2, 3), jnp.swapaxes(w_up, 2, 3), w_down)
        pad = lambda v: jnp.pad(v, ((0, 0), (0, wide - d)))
        send_three = lambda p: [move(p[1], 'ep'), move(p[2], 'core'), move_diag(p[3])]

        def own_sum(p, got):
            return sum([g.astype(F32) for g in got], p)[:, :d].astype(BF16)

        one = lambda v: v.reshape(1, n_tok, wide)
        pairs = lambda a, b: [(a, 0), (a, 1), (b, 0), (b, 1)]

        one = lambda v: v.reshape(1, n_tok, wide)
        pairs = lambda a, b: [(a, 0), (a, 1), (b, 0), (b, 1)]
        singles = lambda *v: [(one(a), 0) for a in v]

        u0 = pad((tokens.astype(F32) + jnp.dot(tokens, w_mix[0], preferred_element_type=F32)).astype(BF16))
        u0_y, u0_c = move(u0, 'ep'), move(u0, 'core')
        lists = [sorted_list(expert_ids[l], gate_vals[l]) for l in range(n_layers)]
        counts = jnp.sum((expert_ids.reshape(n_layers, n, 1) == jnp.arange(n_exp, dtype=I32)).astype(F32), axis=1)
        packed = jnp.concatenate([jnp.concatenate([v[0] for v in lists] + [v[1] for v in lists]).reshape(-1, LANES),
                                  jnp.pad(counts, ((0, 8 - n_layers), (0, LANES - n_exp)))], axis=0)
        dy = pad(d_out)
        u0_y, u0_c, packed, dy = fence((u0_y, u0_c, packed, dy))
        u0_d = move(u0_y, 'core')
        shared = share(packed, N_SRC)
        dy, shared = fence((dy, shared))
        shared_x = move(shared, 'x')
        dy_y, dy_x = move(dy, 'ep'), move(dy, 'x')
        sizes = (n_layers, n_local, n_tok, n // LANES)
        routes = plan(shared, shared, *sizes)
        u0_half = singles(u0, u0_y, u0_c, u0_d)
        part = run_experts(routes, 0, u0_half, None, weights, None, None, True, True, p_f32=True)
        dy_y, dy_x, shared_x, part = fence((dy_y, dy_x, shared_x, part))
        dy_c, dy_d, dy_xy, dy_xc = move(dy, 'core'), move(dy_y, 'core'), move(dy_y, 'x'), move(dy_x, 'core')
        y0, u1_a, u1_b = complete_blocks(part, w_mix[1], True, False, False, 1)
        dy_c, dy_d, dy_xy, dy_xc, u0_p, u0_q, y0, u1_a, u1_b, shared_x = fence(
            (dy_c, dy_d, dy_xy, dy_xc, u0, u0_y, y0, u1_a, u1_b, shared_x))
        routes_x = plan(shared, shared_x, *sizes)
        dy_xd = move(dy_xy, 'core')
        u1_xa, u0_x, u0_xy = move(u1_a, 'x'), move(u0_p, 'x'), move(u0_q, 'x')
        out = run_experts(routes, 1, pairs(u1_a, u1_b), singles(dy, dy_y, dy_c, dy_d), weights, None, None, True, True)
        u1_xa, u0_x, u0_xy, dy_xd, out = fence((u1_xa, u0_x, u0_xy, dy_xd, out))
        y_part, du_part, g1 = out[:4], out[4:8], out[8]
        u1_xb = move(u1_xa, 'core')
        got = send_three(du_part)
        out = run_experts(routes_x, 1, pairs(u1_xa, u1_xb), singles(dy_x, dy_xy, dy_xc, dy_xd), weights, g1, None,
                          False, False)
        got, u0_x, u0_xy, out = fence((got, u0_x, u0_xy, out))
        *finals, sent_a, sent_b = out
        du1, dx_a, dx_b = complete_blocks([du_part[0], *got], w_mix[1], False, False, True, 2)
        dx_a, y_part, sent_a, sent_b, u0_x, u0_xy = fence((dx_a, y_part, sent_a, sent_b, u0_x, u0_xy))
        dx_xa = move(dx_a, 'x')
        got_y = send_three(y_part)
        got1 = [move(sent_a, 'core'), move(sent_b, 'core')]
        u0_xc, u0_xd = move(u0_x, 'core'), move(u0_xy, 'core')
        out = run_experts(routes, 0, u0_half, pairs(dx_a, dx_b), weights, None, None, False, True)
        dx_xa, got_y, got1, u0_xc, u0_xd, out = fence((dx_xa, got_y, got1, u0_xc, u0_xd, out))
        du_part, g0 = out[:4], out[4]
        dx_xb = move(dx_xa, 'core')
        got = send_three(du_part)
        tx = lambda x, du: jnp.einsum('td,te->de', x, du, preferred_element_type=F32)
        y1 = own_sum(y_part[0], got_y)
        g_mix1 = tx(y0[:, :d], du1[:, :d])
        y1, g_mix1, du_part, dx_xb = fence((y1, g_mix1, du_part, dx_xb))
        out = run_experts(routes_x, 0, singles(u0_x, u0_xy, u0_xc, u0_xd), pairs(dx_xa, dx_xb), weights, g0, finals,
                          False, False, got=got1)
        got, out = fence((got, out))
        *finals, sent_a, sent_b = out
        got_a = move(sent_a, 'core')
        du0 = own_sum(du_part[0], got)
        g_mix0 = tx(tokens, du0)
        second = lax.axis_index('core') > 0
        give = move(jnp.where(second, g_mix0, g_mix1), 'core')
        sent_b, g_mix0 = fence((sent_b, g_mix0))
        got_b = move(sent_b, 'core')
        dx0 = (du0.astype(F32) + jnp.einsum('te,de->td', du0, w_mix[0], preferred_element_type=F32)).astype(BF16)
        part = (jnp.where(second, g_mix1, g_mix0) + give).astype(BF16)
        part_y = move(part, 'ep')
        row = lambda a: lax.slice_in_dim(routes[0], ROW_PARTNER * LANES + a, ROW_PARTNER * LANES + a + n_local // 4)
        part_y, got_a, finals = fence((part_y, got_a, finals))
        finals = place(row(0), 0, got_a, finals)
        part_y, finals = fence((part_y, finals))
        part = (part.astype(F32) + part_y.astype(F32)).astype(BF16)
        part_x = move(part, 'x')
        got_b, part_x, finals = fence((got_b, part_x, finals))
        finals = place(row(n_local // 4), 0, got_b, finals)
        part_x, finals = fence((part_x, finals))
        total = (part.astype(F32) + part_x.astype(F32)).astype(BF16)
        theirs = move(total, 'core')
        g_mix = jnp.where(second, jnp.stack([theirs, total]), jnp.stack([total, theirs]))
        return (y1, dx0, g_mix, jnp.swapaxes(finals[0], 2, 3), jnp.swapaxes(finals[1], 2, 3), finals[2])

    return jax.shard_map(device_step, mesh=sub,
                         in_specs=(tok_spec, tok_spec, route_spec, route_spec, whole_spec,
                                   expert_spec, expert_spec, expert_spec),
                         out_specs=(tok_spec, tok_spec, whole_spec, expert_spec, expert_spec, expert_spec),
                         check_vma=False)
```

```python
import functools

import jax
import jax.numpy as jnp
from jax import lax
from jax.experimental import pallas as pl
from jax.experimental.pallas import tpu as pltpu
from jax.sharding import Mesh, PartitionSpec as P

F32, BF16, I32 = jnp.float32, jnp.bfloat16, jnp.int32
MESH = pl.DeviceIdType.MESH
ROWS = 384
GRP = 8
PITCH = 9
FULL = 8
HALF = 4
CAP_FACTOR = 3
LANES = 128
N_SRC = 4
Y, CORE, X = 1, 2, 4
VMEM_LIMIT = 62 * 1024 * 1024
PER_TILE = ROWS // GRP
ROW_BOUND, ROW_GOFF, ROW_EXPERT, ROW_PARTNER, TAB_ROWS = 32, 33, 34, 35, 40
SLOT_GROUPS = 256


def cdiv(a, b):
    return (a + b - 1) // b


def spans(d):
    return [(LANES * j, min(LANES, d - LANES * j)) for j in range(cdiv(d, LANES))]


any_space = pl.BlockSpec(memory_space=pl.ANY)
in_vmem = pl.BlockSpec(memory_space=pltpu.VMEM)


def sorted_list(expert_ids, gate_vals):
    n_tok, top = expert_ids.shape
    n = n_tok * top
    keys = expert_ids.reshape(n) * n + jnp.arange(n, dtype=I32)
    keys, gates = lax.sort((keys, gate_vals.reshape(n)), num_keys=1, is_stable=False)
    return ((keys % n) // top).astype(F32), gates


def plan_kernel(n_layers, n_local, n_tok, list_rows, deal_ref, all_ref, tab_ref, idx_ref, gate_ref):
    n_mine = n_local // 2
    core, ep = lax.axis_index('core'), lax.axis_index('ep')
    list_len = list_rows * LANES
    lane = lambda n: lax.broadcasted_iota(I32, (n, LANES), 1).astype(F32)
    sub = lambda n: lax.broadcasted_iota(I32, (n, LANES), 0).astype(F32)
    over_lanes = lambda v: jnp.sum(v, axis=1, keepdims=True)
    over_subs = lambda v: jnp.sum(v, axis=0, keepdims=True)
    l16, s16 = lane(n_mine), sub(n_mine)
    groups = lambda c: jnp.floor((c + (GRP - 0.5)) * (1.0 / GRP))
    for l in range(n_layers):
        cnt = all_ref[:, 2 * n_layers * list_rows + l, :]
        ends = cnt
        step = 1
        while step < 2 * n_local:
            ends = ends + jnp.where(lane(N_SRC) >= step, pltpu.roll(ends, step, 1), 0.0)
            step *= 2
        starts = ends - cnt
        second = (ep > 0)
        local = lambda v: jnp.where(lane(N_SRC) < n_local, jnp.where(second, pltpu.roll(v, LANES - n_local, 1), v), 0.0)
        cnt, starts = local(cnt), local(starts)
        tiles = jnp.floor((over_subs(groups(local(deal_ref[:, 2 * n_layers * list_rows + l, :]))) + (PER_TILE - 0.5))
                          * (1.0 / PER_TILE))
        load = jnp.where(lane(1) < n_local, jnp.maximum(1.0, tiles), -1.0)
        wide = jnp.broadcast_to(load, (n_local, LANES))
        col = over_lanes(jnp.where(lane(n_local) == sub(n_local), wide, 0.0))
        ahead = (col > wide) | ((col == wide) & (sub(n_local) < lane(n_local)))
        rank = over_subs(jnp.where(ahead, 1.0, 0.0))
        odd = s16 - 2.0 * jnp.floor(s16 * 0.5 + 0.25)
        flip = jnp.where(core > 0, 1.0 - odd, odd)
        dealt = lambda f: (jnp.broadcast_to(rank, (n_mine, LANES)) == 2.0 * s16 + f) & (l16 < n_local)
        pick = dealt(flip)
        choose = lambda p, row: over_lanes(jnp.where(p, jnp.broadcast_to(row, (n_mine, LANES)), 0.0))
        mine = lambda row: choose(pick, row)
        as_row = lambda c: over_subs(jnp.where(l16 == s16, c, 0.0))
        experts = as_row(mine(lane(1)))
        partner = as_row(choose(dealt(1.0 - flip), lane(1)))
        at = l * TAB_ROWS
        off = jnp.zeros((n_mine, 1), F32)
        pos = [jnp.zeros((n_mine, LANES), F32) for _ in range(SLOT_GROUPS // LANES)]
        for s in range(N_SRC):
            c, st = mine(cnt[s:s + 1]), mine(starts[s:s + 1]) + float(s * list_len)
            ng = groups(c)
            for i in range(len(pos)):
                rel = l16 + float(LANES * i) - off
                code = (st + GRP * rel) * 16.0 + jnp.minimum(float(GRP), c - GRP * rel)
                pos[i] = jnp.where((rel >= 0) & (rel < ng), code, pos[i])
            off = off + ng
        for i in range(len(pos)):
            tab_ref[pl.ds(at + i, n_mine, stride=len(pos)), :] = pos[i].astype(I32)
        n_tiles = jnp.maximum(1.0, jnp.floor((off + (PER_TILE - 0.5)) * (1.0 / PER_TILE)))
        bounds = over_subs(jnp.where(s16 < l16, n_tiles, 0.0))
        before = over_lanes(jnp.where(l16 == s16, jnp.broadcast_to(bounds, (n_mine, LANES)), 0.0))
        t = jnp.minimum(l16, over_subs(jnp.broadcast_to(n_tiles, (n_mine, LANES))) - 1.0)
        inside = (t >= before) & (t < before + n_tiles)
        goff = over_subs(jnp.where(inside, s16 * float(SLOT_GROUPS) + (t - before) * float(PER_TILE), 0.0))
        rows = [(ROW_BOUND, bounds), (ROW_GOFF, goff), (ROW_EXPERT, experts), (ROW_PARTNER, partner)]
        for row, value in rows:
            tab_ref[at + row:at + row + 1, :] = value.astype(I32)
    for l in range(n_layers):
        pad = l * (N_SRC * list_rows + 8) + N_SRC * list_rows
        gate_ref[pad:pad + 8, :] = jnp.zeros((8, LANES), F32)
        for s in range(N_SRC):
            to = (l * N_SRC + s) * list_rows
            toks = all_ref[s, l * list_rows:(l + 1) * list_rows, :]
            idx_ref[to:to + list_rows, :] = ((toks + float(s * n_tok)) * float(PITCH)).astype(I32)
            to = l * (N_SRC * list_rows + 8) + s * list_rows
            gate_ref[to:to + list_rows, :] = all_ref[s, (n_layers + l) * list_rows:(n_layers + l + 1) * list_rows, :]


def plan(deal, shared, n_layers, n_local, n_tok, list_rows):
    n_tab = n_layers * TAB_ROWS
    n_list = n_layers * N_SRC * list_rows
    n_gate = n_layers * (N_SRC * list_rows + 8)
    tab, idx, gates = pl.pallas_call(
        functools.partial(plan_kernel, n_layers, n_local, n_tok, list_rows),
        out_shape=[jax.ShapeDtypeStruct((n_tab, LANES), I32), jax.ShapeDtypeStruct((n_list, LANES), I32),
                   jax.ShapeDtypeStruct((n_gate, LANES), F32)],
        in_specs=[in_vmem] * 2, out_specs=[in_vmem] * 3,
        cost_estimate=pl.CostEstimate(flops=10 ** 7, bytes_accessed=10 ** 6, transcendentals=0),
        name="plan",
    )(deal, shared)
    return tab.reshape(-1), idx.reshape(-1), gates


def expert_kernel(cfg, *refs):
    fwd, bwd, own, layer, n_blk, d, ff, n_exp, picks, row_id, list_len, p_f32, n_alias, got_layer = cfg
    refs = list(refs)
    take = lambda n: [refs.pop(0) for _ in range(n)]
    tab_hbm, idx_hbm, gate_hbm = take(3)
    u_pieces = take(N_SRC)
    dy_pieces = take(N_SRC) if bwd else []
    wg_hbm, wu_hbm, wd_hbm = take(3)
    prev = take(1)[0] if bwd and not own else None
    got = take(2) if got_layer is not None else None
    take(n_alias)
    y_outs = take(N_SRC) if fwd else []
    du_outs = take(N_SRC) if bwd and own else []
    grad = take(1)[0] if bwd and own else None
    finals = take(3) if bwd and not own else None
    sent = take(2) if bwd and not own else None
    tab_ref, idx, gate_ref, land, table, gat = take(6)
    acc, row_ref = take(2) if own else (None, None)
    gu_ref, wd_ref, g_ref, x_u = take(4)
    x_c = take(1)[0] if bwd else None
    ab_ref = take(1)[0]
    dh_ref = take(1)[0] if bwd else None
    h_ref = take(1)[0]
    dab_ref, sums = take(2) if bwd else (None, None)
    keep_buf = take(1)[0] if bwd and not own else None
    got_buf = take(1)[0] if got is not None else None
    list_sem, land_sem, w_sem = take(3)
    sum_sem = take(1)[0] if bwd else None
    keep_sem = take(1)[0] if bwd and not own else None
    read_sem, write_sem = take(2) if got is not None else (None, None)
    stage_f, out_sem = take(2) if own else (None, None)

    copy = pltpu.make_async_copy
    cols = spans(d)
    lo = ff // 256 * 256
    hi = ff - lo
    dot = functools.partial(lax.dot_general, preferred_element_type=F32)
    nn = (((1,), (0,)), ((), ()))
    nt = (((1,), (1,)), ((), ()))
    tn = (((0,), (0,)), ((), ()))
    al = pl.multiple_of
    n_row = N_SRC * n_blk
    glane = lax.broadcasted_iota(I32, (GRP, LANES), 1)
    gsub = lax.broadcasted_iota(I32, (GRP, LANES), 0)

    def row_at(r):
        return pl.ds(r * PITCH, FULL)

    def group(tile, q):
        return tab_ref[tab_ref[ROW_GOFF * LANES + tile] + q]

    def gather(tile, q):
        ids = idx.at[pl.ds(group(tile, q) >> 4, GRP)]
        for k in range(GRP):
            gat[row_at(q * GRP + k), :] = table[pl.ds(ids[k], FULL), :]

    def gate_column(code):
        pos = code >> 4
        row, shift = pos >> 7, pos & (LANES - 1)
        want = glane == gsub + shift
        over = glane == gsub + (shift - LANES)
        here = gate_ref[pl.ds(row, GRP, stride=0), :]
        there = gate_ref[pl.ds(row + 1, GRP, stride=0), :]
        v = jnp.where(want, here, jnp.where(over, there, 0.0))
        return jnp.where(gsub < (code & 15), jnp.sum(v, axis=1, keepdims=True), 0.0)

    def scatter(tile, q):
        ids = idx.at[pl.ds(group(tile, q) >> 4, GRP)]
        new = []
        for k in range(GRP):
            at = pl.ds(ids[k], FULL)
            new.append((at, acc[at, :] + row_ref[row_at(q * GRP + k), :]))
        for at, value in reversed(new):
            acc[at, :] = value

    def convert(tile):
        for q in range(0, PER_TILE, 2):
            part = []
            for p in (q, q + 1):
                code = group(tile, p)
                rows = [gat[pl.ds(GRP * PITCH * p + j, GRP, stride=PITCH), :] for j in range(FULL if bwd else HALF)]
                real = gsub < (code & 15)
                gate = gate_column(code)
                g_ref[GRP * p:GRP * (p + 1), :] = gate
                part.append([jnp.where(real, v, 0.0) for v in rows[:HALF]] + [v * gate for v in rows[HALF:]])
            at = slice(GRP * q, GRP * (q + 2))
            for x, o in ((x_u, 0), (x_c, HALF)):
                if x is None:
                    continue
                for j, (c, w) in enumerate(cols):
                    both = jnp.concatenate([part[0][o + j], part[1][o + j]], axis=0)
                    x[at, c:c + w] = both[:, :w].astype(BF16)

    def put_rows(o, value, s0):
        value = value.astype(BF16).astype(F32)
        n = value.shape[0]
        for j, (c, w) in enumerate(cols):
            row_ref[pl.ds(PITCH * s0 + o + j, n, stride=PITCH), 0:w] = value[:, c:c + w] * g_ref[s0:s0 + n, 0:w]

    low = lax.broadcasted_iota(I32, (16, 2 * hi), 1) < hi

    def middle(a, b, dh):
        sig = 0.5 * jnp.tanh(0.5 * a) + 0.5
        act = a * sig
        h = act * b
        if dh is None:
            return h, None, None
        slope = sig * (1.0 + a * (1.0 - sig))
        return h, dh * b * slope, dh * act

    def weights(e, slot):
        at = (layer, tab_ref[ROW_EXPERT * LANES + e])
        moves = []
        for i, w in enumerate((wg_hbm, wu_hbm)):
            moves.append((w.at[at + (pl.ds(0, lo),)], gu_ref.at[slot, pl.ds(i * lo, lo)]))
            moves.append((w.at[at + (pl.ds(lo, hi),)], gu_ref.at[slot, pl.ds(2 * lo + i * hi, hi)]))
        moves.append((wd_hbm.at[at], wd_ref.at[slot]))
        return [copy(a, b, w_sem.at[slot, i]) for i, (a, b) in enumerate(moves)]

    def sums_in(e, slot):
        return copy(prev.at[e], sums.at[slot], sum_sem.at[slot])

    def sums_out(e, slot):
        return copy(sums.at[slot], grad.at[e], sum_sem.at[slot])

    def keeps(e, slot):
        at = (layer, tab_ref[ROW_EXPERT * LANES + e])
        return [copy(keep_buf.at[slot, i], finals[i].at[at], keep_sem.at[slot, i]) for i in range(3)]

    def send(e, slot, part):
        return copy(keep_buf.at[slot], sent[part].at[e - part * (n_exp // 2)], keep_sem.at[slot, 3])

    def read(e, slot, part=0):
        return copy(got[part].at[e - part * (n_exp // 2)], got_buf.at[slot], read_sem.at[slot])

    def writes(e, slot):
        to = tab_ref[TAB_ROWS * LANES + e]
        return [copy(got_buf.at[slot, i], finals[i].at[got_layer, to], write_sem.at[slot, i]) for i in range(3)]

    def start(moves):
        for m in moves:
            m.start()

    def wait(moves):
        for m in moves:
            m.wait()

    n_tab = TAB_ROWS * LANES
    lists = [copy(tab_hbm.at[pl.ds(row_id * n_tab, n_tab)], tab_ref.at[pl.ds(0, n_tab)], list_sem.at[0]),
             copy(idx_hbm.at[pl.ds(row_id * N_SRC * list_len, N_SRC * list_len)], idx.at[pl.ds(0, N_SRC * list_len)],
                  list_sem.at[1]),
             copy(gate_hbm.at[pl.ds(row_id * gate_ref.shape[0], gate_ref.shape[0])], gate_ref, list_sem.at[2])]
    if got is not None:
        at = (got_layer * TAB_ROWS + ROW_PARTNER) * LANES
        lists.append(copy(tab_hbm.at[pl.ds(at, LANES)], tab_ref.at[pl.ds(n_tab, LANES)], list_sem.at[3]))
    start(lists)
    pieces = []
    for s in range(N_SRC):
        pieces.append((u_pieces[s], picks[0][s], s, 0, fwd))
        if bwd:
            pieces.append((dy_pieces[s], picks[1][s], s, HALF, own))
    lands = [copy(ref.at[pick], land.at[i % N_SRC], land_sem.at[i % N_SRC]) for i, (ref, pick, *_) in enumerate(pieces)]
    start(lands[:N_SRC])
    lists[0].wait()
    start(weights(0, 0))
    if bwd and not own:
        sums_in(0, 0).start()
    if got is not None:
        lists[3].wait()
        read(0, 0).start()
    if own:
        def clear(c, _):
            for k in range(4):
                acc[pl.ds(al(c * 1152 + 288 * k, 8), 288), :] = jnp.zeros((288, LANES), F32)
            return 0

        lax.fori_loop(0, acc.shape[0] // 1152, clear, 0)
        row_ref[...] = jnp.zeros(row_ref.shape, F32)
    rows = 256
    for i, (_, _, s, o, seed) in enumerate(pieces):
        lands[i].wait()

        def fill(c, _, i=i, o=o, seed=seed, s=s):
            r = al(c * rows, rows)
            for j in range(HALF):
                vals = land[i % N_SRC, pl.ds(r, rows), LANES * j:LANES * (j + 1)].astype(F32)
                to = pl.ds(PITCH * (s * n_blk + r) + o + j, rows, stride=PITCH)
                table[to, :] = vals
                if seed and s == 0:
                    acc[to, :] = vals
            return 0

        lax.fori_loop(0, n_blk // rows, fill, 0)
        if i + N_SRC < len(pieces):
            lands[i + N_SRC].start()
    wait(lists[1:3])
    for k in range(GRP):
        idx[N_SRC * list_len + k] = 0

    def first(q, _):
        gather(0, 2 * q)
        gather(0, 2 * q + 1)
        return 0

    lax.fori_loop(0, PER_TILE // 2, first, 0)
    convert(0)

    def expert(e, _):
        slot = e & 1
        wait(weights(e, slot))
        if bwd and not own:
            sums_in(e, slot).wait()
        if got is not None:
            read(0, slot).wait()
            start(writes(e, slot))

            @pl.when((e > 0) & (e < n_exp - 1))
            def _():
                wait(writes(e - 1, 1 - slot))

        @pl.when(e < n_exp - 1)
        def _():
            start(weights(e + 1, 1 - slot))
            if bwd and not own:
                sums_in(e + 1, 1 - slot).start()
            if got is not None:
                for part in range(2):
                    @pl.when((e + 1 >= n_exp // 2) if part else (e + 1 < n_exp // 2))
                    def _(part=part):
                        read(e + 1, 1 - slot, part).start()

        if bwd and own:
            @pl.when(e > 1)
            def _():
                sums_out(e - 2, slot).wait()

            sums[slot] = jnp.zeros(sums.shape[1:], F32)

        def tile(t, _):
            for q in range(PER_TILE):
                if own:
                    scatter(jnp.maximum(t - 1, 0), q)
                gather(t + 1, q)
            half = ROWS // 2
            for s0 in range(0, ROWS, half):
                sl = slice(s0, s0 + half)
                ab_ref[sl, :] = dot(x_u[sl, :], gu_ref[slot], nt)
                if bwd:
                    dh_ref[sl, :] = dot(x_c[sl, :], wd_ref[slot], nt)
            for r in range(0, ROWS, 16):
                rows = slice(r, r + 16)
                for c in range(0, lo, LANES):
                    h, da, db = middle(ab_ref[rows, c:c + LANES], ab_ref[rows, lo + c:lo + c + LANES],
                                       dh_ref[rows, c:c + LANES] if bwd else None)
                    h_ref[rows, c:c + LANES] = h.astype(BF16)
                    if bwd:
                        dab_ref[rows, c:c + LANES] = da.astype(BF16)
                        dab_ref[rows, lo + c:lo + c + LANES] = db.astype(BF16)
                a = ab_ref[rows, 2 * lo:]
                b = pltpu.roll(a, hi, 1)
                dh = dh_ref[rows, lo:] if bwd else None
                if bwd:
                    dh = jnp.concatenate([dh, dh], axis=1)
                h, da, db = middle(a, b, dh)
                h_ref[rows, lo:] = h[:, :hi].astype(BF16)
                if bwd:
                    dab_ref[rows, 2 * lo:] = jnp.where(low, da, pltpu.roll(db, hi, 1)).astype(BF16)
            for s0 in range(0, ROWS, half):
                sl = slice(s0, s0 + half)
                if fwd:
                    put_rows(0, dot(h_ref[sl, :], wd_ref[slot], nn), s0)
                if bwd and own:
                    put_rows(HALF, dot(dab_ref[sl, :], gu_ref[slot], nn), s0)
            if bwd:
                view = sums.at[slot]
                view[0:2 * ff, :] += dot(dab_ref[...], x_u[...], tn)
                view[2 * ff:, :] += dot(h_ref[...], x_c[...], tn)
            convert(t + 1)
            return 0

        lax.fori_loop(tab_ref[ROW_BOUND * LANES + e], tab_ref[ROW_BOUND * LANES + e + 1], tile, 0)
        if bwd and own:
            sums_out(e, slot).start()
        if bwd and not own:
            @pl.when(e > 1)
            def _():
                wait(keeps(e - 2, slot) + [send(0, slot, 0)])

            for i in range(2):
                keep_buf[slot, i, 0:lo, :] = sums[slot, i * lo:(i + 1) * lo, :].astype(BF16)
                keep_buf[slot, i, lo:, :] = sums[slot, 2 * lo + i * hi:2 * lo + (i + 1) * hi, :].astype(BF16)
            keep_buf[slot, 2] = sums[slot, 2 * ff:, :].astype(BF16)
            start(keeps(e, slot))
            for part in range(2):
                @pl.when((e >= n_exp // 2) if part else (e < n_exp // 2))
                def _(part=part):
                    send(e, slot, part).start()
        return 0

    lax.fori_loop(0, n_exp, expert, 0)
    ends = ((n_exp - 2, (n_exp - 2) % 2), (n_exp - 1, (n_exp - 1) % 2))
    if own:
        end = tab_ref[ROW_BOUND * LANES + n_exp] - 1
        lax.fori_loop(0, PER_TILE, lambda q, _: (scatter(end, q), 0)[1], 0)
        flights = {}
        for o, out in ((HALF, du_outs), (0, y_outs)):
            for s in range(N_SRC if out else 0):
                wide = s == 0 or p_f32
                stage = stage_f.at[s] if wide else land.at[s]
                if s in flights:
                    flights[s].wait()

                def fetch(c, _, stage=stage, s=s, o=o):
                    r = al(c * rows, rows)
                    for j in range(HALF):
                        at = pl.ds(PITCH * (s * n_blk + r) + o + j, rows, stride=PITCH)
                        stage[pl.ds(r, rows), LANES * j:LANES * (j + 1)] = acc[at, :].astype(stage.dtype)
                    return 0

                lax.fori_loop(0, n_blk // rows, fetch, 0)
                flights[s] = copy(stage, out[s], out_sem.at[s])
                flights[s].start()
        wait(flights.values())
        if bwd:
            for e, slot in ends:
                sums_out(e, slot).wait()
    else:
        for e, slot in ends:
            wait(keeps(e, slot) + [send(0, slot, 0)])
            if got is not None:
                wait(writes(e, slot))


def run_experts(routes, layer, u, dy, weights, prev, finals, fwd, own, p_f32=False, got=None):
    tab, idx, gates = routes
    bwd = dy is not None
    wg, wu, wd = weights
    n_blk, wide = u[0][0].shape[-2:]
    n_layers, n_local, ff, d = wd.shape
    n_exp = n_local // 2
    row_id = layer
    list_len = idx.shape[0] // (n_layers * N_SRC)

    arrays = lambda pieces: [v for v, _ in pieces]
    operands = [tab, idx, gates] + arrays(u) + (arrays(dy) if bwd else []) + [wg, wu, wd]
    out_shape, aliases = [], {}
    for use in (fwd, bwd and own):
        if use:
            out_shape += [jax.ShapeDtypeStruct((n_blk, wide), F32 if s == 0 or p_f32 else BF16) for s in range(N_SRC)]
    if bwd and own:
        out_shape.append(jax.ShapeDtypeStruct((n_exp, 3 * ff, d), F32))
    if bwd and not own:
        operands.append(prev)
        if got is not None:
            operands += got
        for i, f in enumerate(finals or ()):
            aliases[len(operands)] = i
            operands.append(f)
        out_shape += [jax.ShapeDtypeStruct((n_layers, n_local, ff, d), BF16)] * 3
        out_shape += [jax.ShapeDtypeStruct((n_exp // 2, 3, ff, d), BF16)] * 2
    sem = lambda *s: pltpu.SemaphoreType.DMA(s)
    mid = lambda n, dt: pltpu.VMEM((ROWS, n), dt)
    table, rows = pltpu.VMEM((PITCH * N_SRC * n_blk, LANES), F32), pltpu.VMEM((PITCH * ROWS, LANES), F32)
    scratch = [pltpu.SMEM(((TAB_ROWS + 1) * LANES,), I32), pltpu.SMEM((N_SRC * list_len + LANES,), I32),
               pltpu.VMEM((N_SRC * list_len // LANES + 8, LANES), F32), pltpu.VMEM((N_SRC, n_blk, wide), BF16)]
    scratch += [table, rows] * (1 + own)
    scratch += [pltpu.VMEM((2, 2 * ff, d), BF16), pltpu.VMEM((2, ff, d), BF16), mid(LANES, F32)]
    scratch += [mid(d, BF16)] * (1 + bwd) + [mid(2 * ff, F32)] + [mid(ff, F32)] * bwd + [mid(ff, BF16)]
    scratch += [mid(2 * ff, BF16), pltpu.VMEM((2, 3 * ff, d), F32)] * bwd
    if bwd and not own:
        scratch.append(pltpu.VMEM((2, 3, ff, d), BF16))
    if got is not None:
        scratch.append(pltpu.VMEM((2, 3, ff, d), BF16))
    scratch += [sem(4), sem(N_SRC), sem(2, 5)] + [sem(2)] * bwd
    if bwd and not own:
        scratch.append(sem(2, 4))
    if got is not None:
        scratch += [sem(2), sem(2, 3)]
    if own:
        scratch += [pltpu.VMEM((N_SRC if p_f32 else 1, n_blk, wide), F32), sem(N_SRC)]
    passes = 2 + fwd + bwd * (4 + 2 * own)
    flops = 2 * d * ff * passes * n_blk * N_SRC * 2
    hoist = 1400 if not own else 1200 if not bwd else 700 if fwd else 800
    picks = [[i for _, i in u], [i for _, i in dy] if bwd else None]
    cfg = (fwd, bwd, own, layer, n_blk, d, ff, n_exp, picks, row_id, list_len, p_f32, len(aliases),
           None if got is None else 1 - layer)
    return pl.pallas_call(
        functools.partial(expert_kernel, cfg),
        out_shape=out_shape,
        in_specs=[any_space] * len(operands),
        out_specs=[any_space] * len(out_shape),
        scratch_shapes=scratch,
        input_output_aliases=aliases,
        compiler_params=pltpu.CompilerParams(
            vmem_limit_bytes=VMEM_LIMIT),
        cost_estimate=pl.CostEstimate(flops=flops, bytes_accessed=3 * 2 * n_exp * d * ff, transcendentals=0),
        name=f"experts_{'f' if fwd else ''}{'b' if bwd else ''}_{'own' if own else 'other'}_{layer}",
    )(*operands)


def place_kernel(layer, n_exp, tab_ref, got_ref, *refs):
    outs, (buf, in_sem, out_sem) = refs[3:6], refs[6:]
    reads = [pltpu.make_async_copy(got_ref.at[i], buf.at[i], in_sem.at[i]) for i in range(n_exp)]
    for read in reads:
        read.start()
    writes = []
    for i, read in enumerate(reads):
        read.wait()
        e = tab_ref[i]
        for k, out in enumerate(outs):
            writes.append(pltpu.make_async_copy(buf.at[i, k], out.at[layer, e], out_sem.at[i, k]))
            writes[-1].start()
    for write in writes:
        write.wait()


def place(partner, layer, got, finals):
    n_exp = got.shape[0]
    return pl.pallas_call(
        functools.partial(place_kernel, layer, n_exp),
        out_shape=[jax.ShapeDtypeStruct(f.shape, f.dtype) for f in finals],
        grid_spec=pltpu.PrefetchScalarGridSpec(
            num_scalar_prefetch=1, grid=(1,), in_specs=[any_space] * 4, out_specs=[any_space] * 3,
            scratch_shapes=[pltpu.VMEM(got.shape, got.dtype), pltpu.SemaphoreType.DMA((n_exp,)),
                            pltpu.SemaphoreType.DMA((n_exp, 3))]),
        input_output_aliases={2: 0, 3: 1, 4: 2},
        compiler_params=pltpu.CompilerParams(vmem_limit_bytes=VMEM_LIMIT),
        cost_estimate=pl.CostEstimate(flops=0, bytes_accessed=4 * got.size, transcendentals=0),
        name=f"place_{layer}",
    )(partner, got, *finals)


def peer(rel):
    return {name: (lax.axis_index(name) + ((rel >> bit) & 1)) % 2 for bit, name in enumerate(("ep", "core", "x"))}


def meet(rels):
    barrier = pltpu.get_barrier_semaphore()
    for rel in rels:
        pl.semaphore_signal(barrier, inc=1, device_id=peer(rel), device_id_type=MESH)
    pl.semaphore_wait(barrier, len(rels))


def remote(src, dst, send, recv, rel):
    return pltpu.make_async_remote_copy(src_ref=src, dst_ref=dst, send_sem=send, recv_sem=recv,
                                        device_id=peer(rel), device_id_type=MESH)


def share_kernel(n_rel, mine_ref, all_ref, send_sem, recv_sem):
    meet(range(1, n_rel))
    copies = [remote(mine_ref, all_ref.at[rel], send_sem.at[rel], recv_sem.at[rel], rel) for rel in range(1, n_rel)]
    for copy in copies:
        copy.start()
    all_ref[0] = mine_ref[...]
    for copy in copies:
        copy.wait()


def share(mine, n_rel):
    return pl.pallas_call(
        functools.partial(share_kernel, n_rel),
        out_shape=jax.ShapeDtypeStruct((n_rel,) + mine.shape, mine.dtype),
        in_specs=[in_vmem],
        out_specs=in_vmem,
        scratch_shapes=[pltpu.SemaphoreType.DMA((n_rel,)), pltpu.SemaphoreType.DMA((n_rel,))],
        compiler_params=pltpu.CompilerParams(collective_id=0, has_side_effects=True),
        cost_estimate=pl.CostEstimate(flops=10 ** 7, bytes_accessed=mine.size * 4 * n_rel, transcendentals=0),
        name="share_lists",
    )(mine)


def blocks_kernel(cfg, *refs):
    n_chunk, reduce, across, back, d = cfg
    refs = list(refs)
    take = lambda n: [refs.pop(0) for _ in range(n)]
    parts = take(N_SRC)
    m_ref, o_total, o_a, o_b = take(4)
    o_xa, o_xb = take(2) if across else (None, None)
    in_f, in_b, got_f, s_buf, r_buf, t_buf, u_buf, load, send, recv, put = take(11)
    n_rows = t_buf.shape[0] // n_chunk
    cut = [pl.ds(k * n_rows, n_rows) for k in range(n_chunk)]
    chunks = range(n_chunk)
    loads = {}
    for i, part in enumerate(parts[:2] if reduce else parts):
        buf = in_f.at[i] if reduce or i == 0 else in_b.at[i - 1]
        for k in chunks:
            loads[i, k] = pltpu.make_async_copy(part.at[cut[k]], buf.at[cut[k]], load.at[i, k])
    order = (1, 0) if reduce else range(N_SRC)
    for i in order:
        for k in chunks:
            loads[i, k].start()
    u_buf[...] = jnp.zeros(u_buf.shape, BF16)
    meet((Y, CORE, X) if across else (Y, CORE))
    links = []

    def link(src, dst, rel):
        n = len(links)
        links.append([remote(src.at[cut[k]], dst.at[cut[k]], send.at[n, k], recv.at[n, k], rel) for k in chunks])
        return links[-1]

    if reduce:
        first = link(parts[3], got_f.at[1], CORE)
        second = link(parts[2], got_f.at[0], CORE)
        over = link(s_buf, r_buf, Y)
        for copies in (first, second):
            for copy in copies:
                copy.start()
        for k in chunks:
            loads[1, k].wait()
            first[k].wait_recv()
            s_buf[cut[k], :] = (in_f[1, cut[k], :] + got_f[1, cut[k], :]).astype(BF16)
            over[k].start()
    to_y = link(u_buf, o_a.at[1], Y)
    to_core = link(u_buf, o_b.at[0], CORE)
    to_x = link(u_buf, o_xa.at[0], X) if across else None
    puts = []
    for k in chunks:
        if reduce:
            loads[0, k].wait()
            second[k].wait_recv()
            over[k].wait_recv()
            total = in_f[0, cut[k], :] + got_f[0, cut[k], :] + r_buf[cut[k], :].astype(F32)
        else:
            for i in range(N_SRC):
                loads[i, k].wait()
            total = in_f[0, cut[k], :]
            for i in range(N_SRC - 1):
                total = total + in_b[i, cut[k], :].astype(F32)
        total = total.astype(BF16)
        t_buf[cut[k], :] = total
        dims = (((1,), (1 if back else 0,)), ((), ()))
        mixed = lax.dot_general(total[:, :d], m_ref[...], dims, preferred_element_type=F32)
        u_buf[cut[k], 0:d] = (total[:, :d].astype(F32) + mixed).astype(BF16)
        to_y[k].start()
        to_core[k].start()
        if across:
            to_x[k].start()
        puts.append(pltpu.make_async_copy(u_buf.at[cut[k]], o_a.at[0, cut[k]], put.at[0, k]))
        puts.append(pltpu.make_async_copy(t_buf.at[cut[k]], o_total.at[cut[k]], put.at[1, k]))
        for copy in puts[-2:]:
            copy.start()
    on = link(o_a.at[1], o_b.at[1], CORE)
    on_x = link(o_a.at[1], o_xa.at[1], X) if across else None
    for k in chunks:
        to_y[k].wait_recv()
        on[k].start()
        if across:
            on_x[k].start()
    if across:
        last = [link(o_xa.at[i], o_xb.at[i], CORE) for i in range(2)]
        for i, arrived in enumerate((to_x, on_x)):
            for k in chunks:
                arrived[k].wait_recv()
                last[i][k].start()
    waited = [to_y] + ([first, second, over] if reduce else []) + ([to_x, on_x] if across else [])
    for copies in links:
        for copy in copies:
            if any(copies is w for w in waited):
                copy.wait_send()
            else:
                copy.wait()
    for copy in puts:
        copy.wait()


def complete_blocks(parts, m, reduce, across, back, ident, n_chunk=4):
    n_blk, wide = parts[0].shape
    d = m.shape[0]
    sem = lambda *s: pltpu.SemaphoreType.DMA(s)
    pair = jax.ShapeDtypeStruct((2, n_blk, wide), BF16)
    buf = lambda n, dt: pltpu.VMEM((n, n_blk, wide) if n else (n_blk, wide), dt)
    return pl.pallas_call(
        functools.partial(blocks_kernel, (n_chunk, reduce, across, back, d)),
        out_shape=[jax.ShapeDtypeStruct((n_blk, wide), BF16)] + [pair] * (4 if across else 2),
        in_specs=[any_space] * N_SRC + [in_vmem],
        out_specs=[any_space] * (5 if across else 3),
        scratch_shapes=[buf(2, F32), buf(3, BF16), buf(2, F32), buf(0, BF16), buf(0, BF16), buf(0, BF16), buf(0, BF16),
                        sem(4, n_chunk), sem(10, n_chunk), sem(10, n_chunk), sem(2, n_chunk)],
        compiler_params=pltpu.CompilerParams(collective_id=ident, has_side_effects=True, vmem_limit_bytes=VMEM_LIMIT),
        cost_estimate=pl.CostEstimate(flops=10 ** 8, bytes_accessed=n_blk * wide * 40, transcendentals=0),
        name=f"complete_blocks_{ident}",
    )(*parts, m)


def solution(mesh):
    ep_size, dp_size = mesh.shape['ep'], mesh.shape['dp']
    sub = Mesh(mesh.devices.reshape(ep_size, dp_size // 2, 2), ('ep', 'x', 'core'))
    tok_axes = ('x', 'core', 'ep')
    tok_spec = P(tok_axes, None)
    route_spec = P(None, tok_axes, None)
    whole_spec = P(None, None, None)
    expert_spec = P(None, 'ep', None, None)
    flip = [(0, 1), (1, 0)]
    move = lambda v, axis: lax.ppermute(v, axis, flip)
    move_diag = lambda v: lax.ppermute(v, ('ep', 'core'), [(0, 3), (1, 2), (2, 1), (3, 0)])
    fence = lax.optimization_barrier

    def device_step(tokens, d_out, expert_ids, gate_vals, w_mix, w_gate, w_up, w_down):
        n_layers, d = w_mix.shape[0], w_mix.shape[1]
        n_tok = tokens.shape[0]
        top = expert_ids.shape[2]
        n_local = w_gate.shape[1]
        n_exp = n_local * ep_size
        n = n_tok * top
        n_rel = 2 * N_SRC
        wide = cdiv(d, LANES) * LANES
        weights = (jnp.swapaxes(w_gate, 2, 3), jnp.swapaxes(w_up, 2, 3), w_down)
        pad = lambda v: jnp.pad(v, ((0, 0), (0, wide - d)))
        send_three = lambda p: [move(p[1], 'ep'), move(p[2], 'core'), move_diag(p[3])]

        def own_sum(p, got):
            return sum([g.astype(F32) for g in got], p)[:, :d].astype(BF16)

        one = lambda v: v.reshape(1, n_tok, wide)
        pairs = lambda a, b: [(a, 0), (a, 1), (b, 0), (b, 1)]

        one = lambda v: v.reshape(1, n_tok, wide)
        pairs = lambda a, b: [(a, 0), (a, 1), (b, 0), (b, 1)]
        singles = lambda *v: [(one(a), 0) for a in v]

        u0 = pad((tokens.astype(F32) + jnp.dot(tokens, w_mix[0], preferred_element_type=F32)).astype(BF16))
        u0_y, u0_c = move(u0, 'ep'), move(u0, 'core')
        lists = [sorted_list(expert_ids[l], gate_vals[l]) for l in range(n_layers)]
        counts = jnp.sum((expert_ids.reshape(n_layers, n, 1) == jnp.arange(n_exp, dtype=I32)).astype(F32), axis=1)
        packed = jnp.concatenate([jnp.concatenate([v[0] for v in lists] + [v[1] for v in lists]).reshape(-1, LANES),
                                  jnp.pad(counts, ((0, 8 - n_layers), (0, LANES - n_exp)))], axis=0)
        dy = pad(d_out)
        u0_y, u0_c, packed, dy = fence((u0_y, u0_c, packed, dy))
        u0_d = move(u0_y, 'core')
        shared = share(packed, N_SRC)
        dy, shared = fence((dy, shared))
        shared_x = move(shared, 'x')
        dy_y, dy_x = move(dy, 'ep'), move(dy, 'x')
        sizes = (n_layers, n_local, n_tok, n // LANES)
        routes = plan(shared, shared, *sizes)
        u0_half = singles(u0, u0_y, u0_c, u0_d)
        part = run_experts(routes, 0, u0_half, None, weights, None, None, True, True, p_f32=True)
        dy_y, dy_x, shared_x, part = fence((dy_y, dy_x, shared_x, part))
        dy_c, dy_d, dy_xy, dy_xc = move(dy, 'core'), move(dy_y, 'core'), move(dy_y, 'x'), move(dy_x, 'core')
        y0, u1_a, u1_b = complete_blocks(part, w_mix[1], True, False, False, 1)
        dy_c, dy_d, dy_xy, dy_xc, u0_p, u0_q, y0, u1_a, u1_b, shared_x = fence(
            (dy_c, dy_d, dy_xy, dy_xc, u0, u0_y, y0, u1_a, u1_b, shared_x))
        routes_x = plan(shared, shared_x, *sizes)
        dy_xd = move(dy_xy, 'core')
        u1_xa = move(u1_a, 'x')
        out = run_experts(routes, 1, pairs(u1_a, u1_b), singles(dy, dy_y, dy_c, dy_d), weights, None, None, True, True)
        u1_xa, dy_xd, u0_p, u0_q, out = fence((u1_xa, dy_xd, u0_p, u0_q, out))
        y_part, du_part, g1 = out[:4], out[4:8], out[8]
        u1_xb = move(u1_xa, 'core')
        got = send_three(du_part)
        u0_x, u0_xy = move(u0_p, 'x'), move(u0_q, 'x')
        out = run_experts(routes_x, 1, pairs(u1_xa, u1_xb), singles(dy_x, dy_xy, dy_xc, dy_xd), weights, g1, None,
                          False, False)
        got, u0_x, u0_xy, out = fence((got, u0_x, u0_xy, out))
        *finals, sent_a, sent_b = out
        du1, dx_a, dx_b = complete_blocks([du_part[0], *got], w_mix[1], False, False, True, 2)
        tx = lambda x, du: jnp.einsum('td,te->de', x, du, preferred_element_type=F32)
        g_mix1 = tx(y0[:, :d], du1[:, :d])
        dx_a, y_part, sent_a, sent_b, u0_x, u0_xy, g_mix1 = fence((dx_a, y_part, sent_a, sent_b, u0_x, u0_xy, g_mix1))
        dx_xa = move(dx_a, 'x')
        theirs1 = move(g_mix1, 'core')
        got_y = send_three(y_part)
        u0_xc, u0_xd = move(u0_x, 'core'), move(u0_xy, 'core')
        got1 = [move(sent_a, 'core'), move(sent_b, 'core')]
        out = run_experts(routes, 0, u0_half, pairs(dx_a, dx_b), weights, None, None, False, True)
        dx_xa, got_y, got1, u0_xc, u0_xd, theirs1, out = fence((dx_xa, got_y, got1, u0_xc, u0_xd, theirs1, out))
        du_part, g0 = out[:4], out[4]
        dx_xb = move(dx_xa, 'core')
        got = send_three(du_part)
        part1 = (g_mix1 + theirs1).astype(BF16)
        theirs1 = move(part1, 'ep')
        y1 = own_sum(y_part[0], got_y)
        y1, du_part, dx_xb, part1 = fence((y1, du_part, dx_xb, part1))
        out = run_experts(routes_x, 0, singles(u0_x, u0_xy, u0_xc, u0_xd), pairs(dx_xa, dx_xb), weights, g0, finals,
                          False, False, got=got1)
        got, theirs1, out = fence((got, theirs1, out))
        *finals, sent_a, sent_b = out
        du0 = own_sum(du_part[0], got)
        g_mix0 = tx(tokens, du0)
        theirs0 = move(g_mix0, 'core')
        dx0 = (du0.astype(F32) + jnp.einsum('te,de->td', du0, w_mix[0], preferred_element_type=F32)).astype(BF16)
        part1 = (part1.astype(F32) + theirs1.astype(F32)).astype(BF16)
        theirs0, sent_a, sent_b, dx0, part1 = fence((theirs0, sent_a, sent_b, dx0, part1))
        got_a = move(sent_a, 'core')
        part0 = (g_mix0 + theirs0).astype(BF16)
        theirs0 = move(part0, 'ep')
        sent_b, part0 = fence((sent_b, part0))
        got_b = move(sent_b, 'core')
        row = lambda a: lax.slice_in_dim(routes[0], ROW_PARTNER * LANES + a, ROW_PARTNER * LANES + a + n_local // 4)
        got_a, theirs0, finals = fence((got_a, theirs0, finals))
        parts = jnp.stack([(part0.astype(F32) + theirs0.astype(F32)).astype(BF16), part1])
        theirs = move(parts, 'x')
        parts, got_a = fence((parts, got_a))
        finals = place(row(0), 0, got_a, finals)
        got_b, finals = fence((got_b, finals))
        finals = place(row(n_local // 4), 0, got_b, finals)
        theirs, finals = fence((theirs, finals))
        g_mix = (parts.astype(F32) + theirs.astype(F32)).astype(BF16)
        return (y1, dx0, g_mix, jnp.swapaxes(finals[0], 2, 3), jnp.swapaxes(finals[1], 2, 3), finals[2])

    return jax.shard_map(device_step, mesh=sub,
                         in_specs=(tok_spec, tok_spec, route_spec, route_spec, whole_spec,
                                   expert_spec, expert_spec, expert_spec),
                         out_specs=(tok_spec, tok_spec, whole_spec, expert_spec, expert_spec, expert_spec),
                         check_vma=False)
```

```python
import functools

import jax
import jax.numpy as jnp
from jax import lax
from jax.experimental import pallas as pl
from jax.experimental.pallas import tpu as pltpu
from jax.sharding import Mesh, PartitionSpec as P

F32, BF16, I32 = jnp.float32, jnp.bfloat16, jnp.int32
MESH = pl.DeviceIdType.MESH
ROWS = 384
GRP = 8
PITCH = 9
FULL = 8
HALF = 4
CAP_FACTOR = 3
LANES = 128
N_SRC = 4
Y, CORE, X = 1, 2, 4
VMEM_LIMIT = 62 * 1024 * 1024
PER_TILE = ROWS // GRP
ROW_BOUND, ROW_GOFF, ROW_EXPERT, ROW_PARTNER, TAB_ROWS = 32, 33, 34, 35, 40
SLOT_GROUPS = 256


def cdiv(a, b):
    return (a + b - 1) // b


def spans(d):
    return [(LANES * j, min(LANES, d - LANES * j)) for j in range(cdiv(d, LANES))]


any_space = pl.BlockSpec(memory_space=pl.ANY)
in_vmem = pl.BlockSpec(memory_space=pltpu.VMEM)


def sorted_list(expert_ids, gate_vals):
    n_tok, top = expert_ids.shape
    n = n_tok * top
    keys = expert_ids.reshape(n) * n + jnp.arange(n, dtype=I32)
    keys, gates = lax.sort((keys, gate_vals.reshape(n)), num_keys=1, is_stable=False)
    return ((keys % n) // top).astype(F32), gates


def plan_kernel(n_layers, n_local, n_tok, list_rows, deal_ref, all_ref, tab_ref, idx_ref, gate_ref):
    n_mine = n_local // 2
    core, ep = lax.axis_index('core'), lax.axis_index('ep')
    list_len = list_rows * LANES
    lane = lambda n: lax.broadcasted_iota(I32, (n, LANES), 1).astype(F32)
    sub = lambda n: lax.broadcasted_iota(I32, (n, LANES), 0).astype(F32)
    over_lanes = lambda v: jnp.sum(v, axis=1, keepdims=True)
    over_subs = lambda v: jnp.sum(v, axis=0, keepdims=True)
    l16, s16 = lane(n_mine), sub(n_mine)
    groups = lambda c: jnp.floor((c + (GRP - 0.5)) * (1.0 / GRP))
    for l in range(n_layers):
        cnt = all_ref[:, 2 * n_layers * list_rows + l, :]
        ends = cnt
        step = 1
        while step < 2 * n_local:
            ends = ends + jnp.where(lane(N_SRC) >= step, pltpu.roll(ends, step, 1), 0.0)
            step *= 2
        starts = ends - cnt
        second = (ep > 0)
        local = lambda v: jnp.where(lane(N_SRC) < n_local, jnp.where(second, pltpu.roll(v, LANES - n_local, 1), v), 0.0)
        cnt, starts = local(cnt), local(starts)
        tiles = jnp.floor((over_subs(groups(local(deal_ref[:, 2 * n_layers * list_rows + l, :]))) + (PER_TILE - 0.5))
                          * (1.0 / PER_TILE))
        load = jnp.where(lane(1) < n_local, jnp.maximum(1.0, tiles), -1.0)
        wide = jnp.broadcast_to(load, (n_local, LANES))
        col = over_lanes(jnp.where(lane(n_local) == sub(n_local), wide, 0.0))
        ahead = (col > wide) | ((col == wide) & (sub(n_local) < lane(n_local)))
        rank = over_subs(jnp.where(ahead, 1.0, 0.0))
        odd = s16 - 2.0 * jnp.floor(s16 * 0.5 + 0.25)
        flip = jnp.where(core > 0, 1.0 - odd, odd)
        dealt = lambda f: (jnp.broadcast_to(rank, (n_mine, LANES)) == 2.0 * s16 + f) & (l16 < n_local)
        pick = dealt(flip)
        choose = lambda p, row: over_lanes(jnp.where(p, jnp.broadcast_to(row, (n_mine, LANES)), 0.0))
        mine = lambda row: choose(pick, row)
        as_row = lambda c: over_subs(jnp.where(l16 == s16, c, 0.0))
        experts = as_row(mine(lane(1)))
        partner = as_row(choose(dealt(1.0 - flip), lane(1)))
        at = l * TAB_ROWS
        off = jnp.zeros((n_mine, 1), F32)
        pos = [jnp.zeros((n_mine, LANES), F32) for _ in range(SLOT_GROUPS // LANES)]
        for s in range(N_SRC):
            c, st = mine(cnt[s:s + 1]), mine(starts[s:s + 1]) + float(s * list_len)
            ng = groups(c)
            for i in range(len(pos)):
                rel = l16 + float(LANES * i) - off
                code = (st + GRP * rel) * 16.0 + jnp.minimum(float(GRP), c - GRP * rel)
                pos[i] = jnp.where((rel >= 0) & (rel < ng), code, pos[i])
            off = off + ng
        for i in range(len(pos)):
            tab_ref[pl.ds(at + i, n_mine, stride=len(pos)), :] = pos[i].astype(I32)
        n_tiles = jnp.maximum(1.0, jnp.floor((off + (PER_TILE - 0.5)) * (1.0 / PER_TILE)))
        bounds = over_subs(jnp.where(s16 < l16, n_tiles, 0.0))
        before = over_lanes(jnp.where(l16 == s16, jnp.broadcast_to(bounds, (n_mine, LANES)), 0.0))
        t = jnp.minimum(l16, over_subs(jnp.broadcast_to(n_tiles, (n_mine, LANES))) - 1.0)
        inside = (t >= before) & (t < before + n_tiles)
        goff = over_subs(jnp.where(inside, s16 * float(SLOT_GROUPS) + (t - before) * float(PER_TILE), 0.0))
        rows = [(ROW_BOUND, bounds), (ROW_GOFF, goff), (ROW_EXPERT, experts), (ROW_PARTNER, partner)]
        for row, value in rows:
            tab_ref[at + row:at + row + 1, :] = value.astype(I32)
    for l in range(n_layers):
        pad = l * (N_SRC * list_rows + 8) + N_SRC * list_rows
        gate_ref[pad:pad + 8, :] = jnp.zeros((8, LANES), F32)
        for s in range(N_SRC):
            to = (l * N_SRC + s) * list_rows
            toks = all_ref[s, l * list_rows:(l + 1) * list_rows, :]
            idx_ref[to:to + list_rows, :] = ((toks + float(s * n_tok)) * float(PITCH)).astype(I32)
            to = l * (N_SRC * list_rows + 8) + s * list_rows
            gate_ref[to:to + list_rows, :] = all_ref[s, (n_layers + l) * list_rows:(n_layers + l + 1) * list_rows, :]


def plan(deal, shared, n_layers, n_local, n_tok, list_rows):
    n_tab = n_layers * TAB_ROWS
    n_list = n_layers * N_SRC * list_rows
    n_gate = n_layers * (N_SRC * list_rows + 8)
    tab, idx, gates = pl.pallas_call(
        functools.partial(plan_kernel, n_layers, n_local, n_tok, list_rows),
        out_shape=[jax.ShapeDtypeStruct((n_tab, LANES), I32), jax.ShapeDtypeStruct((n_list, LANES), I32),
                   jax.ShapeDtypeStruct((n_gate, LANES), F32)],
        in_specs=[in_vmem] * 2, out_specs=[in_vmem] * 3,
        cost_estimate=pl.CostEstimate(flops=10 ** 7, bytes_accessed=10 ** 6, transcendentals=0),
        name="plan",
    )(deal, shared)
    return tab.reshape(-1), idx.reshape(-1), gates


def expert_kernel(cfg, *refs):
    fwd, bwd, own, layer, n_blk, d, ff, n_exp, picks, row_id, list_len, p_f32, n_alias, got_layer = cfg
    refs = list(refs)
    take = lambda n: [refs.pop(0) for _ in range(n)]
    tab_hbm, idx_hbm, gate_hbm = take(3)
    u_pieces = take(N_SRC)
    dy_pieces = take(N_SRC) if bwd else []
    wg_hbm, wu_hbm, wd_hbm = take(3)
    prev = take(1)[0] if bwd and not own else None
    got = take(2) if got_layer is not None else None
    take(n_alias)
    y_outs = take(N_SRC) if fwd else []
    du_outs = take(N_SRC) if bwd and own else []
    grad = take(1)[0] if bwd and own else None
    finals = take(3) if bwd and not own else None
    sent = take(2) if bwd and not own else None
    tab_ref, idx, gate_ref, land, table, gat = take(6)
    acc, row_ref = take(2) if own else (None, None)
    gu_ref, wd_ref, g_ref, x_u = take(4)
    x_c = take(1)[0] if bwd else None
    ab_ref = take(1)[0]
    dh_ref = take(1)[0] if bwd else None
    h_ref = take(1)[0]
    dab_ref, sums = take(2) if bwd else (None, None)
    keep_buf = take(1)[0] if bwd and not own else None
    got_buf = take(1)[0] if got is not None else None
    list_sem, land_sem, w_sem = take(3)
    sum_sem = take(1)[0] if bwd else None
    keep_sem = take(1)[0] if bwd and not own else None
    read_sem, write_sem = take(2) if got is not None else (None, None)
    stage_f, out_sem = take(2) if own else (None, None)

    copy = pltpu.make_async_copy
    cols = spans(d)
    lo = ff // 256 * 256
    hi = ff - lo
    dot = functools.partial(lax.dot_general, preferred_element_type=F32)
    nn = (((1,), (0,)), ((), ()))
    nt = (((1,), (1,)), ((), ()))
    tn = (((0,), (0,)), ((), ()))
    al = pl.multiple_of
    n_row = N_SRC * n_blk
    glane = lax.broadcasted_iota(I32, (GRP, LANES), 1)
    gsub = lax.broadcasted_iota(I32, (GRP, LANES), 0)

    def row_at(r):
        return pl.ds(r * PITCH, FULL)

    def codes_of(tile):
        at = ROW_GOFF * LANES + tile
        if own and bwd:
            return lambda q: tab_ref[tab_ref[at] + q]
        view = tab_ref.at[pl.ds(tab_ref[at], PER_TILE)]
        return lambda q: view[q]

    def gather(codes, q):
        ids = idx.at[pl.ds(codes(q) >> 4, GRP)]
        for k in range(GRP):
            gat[row_at(q * GRP + k), :] = table[pl.ds(ids[k], FULL), :]

    def gate_column(code):
        pos = code >> 4
        row, shift = pos >> 7, pos & (LANES - 1)
        want = glane == gsub + shift
        over = glane == gsub + (shift - LANES)
        here = gate_ref[pl.ds(row, GRP, stride=0), :]
        there = gate_ref[pl.ds(row + 1, GRP, stride=0), :]
        v = jnp.where(want, here, jnp.where(over, there, 0.0))
        return jnp.where(gsub < (code & 15), jnp.sum(v, axis=1, keepdims=True), 0.0)

    def scatter(codes, q):
        ids = idx.at[pl.ds(codes(q) >> 4, GRP)]
        new = []
        for k in range(GRP):
            at = pl.ds(ids[k], FULL)
            new.append((at, acc[at, :] + row_ref[row_at(q * GRP + k), :]))
        for at, value in reversed(new):
            acc[at, :] = value

    def convert(codes):
        for q in range(0, PER_TILE, 2):
            part = []
            for p in (q, q + 1):
                code = codes(p)
                rows = [gat[pl.ds(GRP * PITCH * p + j, GRP, stride=PITCH), :] for j in range(FULL if bwd else HALF)]
                real = gsub < (code & 15)
                gate = gate_column(code)
                g_ref[GRP * p:GRP * (p + 1), :] = gate
                part.append([jnp.where(real, v, 0.0) for v in rows[:HALF]] + [v * gate for v in rows[HALF:]])
            at = slice(GRP * q, GRP * (q + 2))
            for x, o in ((x_u, 0), (x_c, HALF)):
                if x is None:
                    continue
                for j, (c, w) in enumerate(cols):
                    both = jnp.concatenate([part[0][o + j], part[1][o + j]], axis=0)
                    x[at, c:c + w] = both[:, :w].astype(BF16)

    def put_rows(o, value, s0):
        value = value.astype(BF16).astype(F32)
        n = value.shape[0]
        for j, (c, w) in enumerate(cols):
            row_ref[pl.ds(PITCH * s0 + o + j, n, stride=PITCH), 0:w] = value[:, c:c + w] * g_ref[s0:s0 + n, 0:w]

    low = lax.broadcasted_iota(I32, (16, 2 * hi), 1) < hi

    def middle(a, b, dh):
        sig = 0.5 * jnp.tanh(0.5 * a) + 0.5
        act = a * sig
        h = act * b
        if dh is None:
            return h, None, None
        slope = sig * (1.0 + a * (1.0 - sig))
        return h, dh * b * slope, dh * act

    def weights(e, slot):
        at = (layer, tab_ref[ROW_EXPERT * LANES + e])
        moves = []
        for i, w in enumerate((wg_hbm, wu_hbm)):
            moves.append((w.at[at + (pl.ds(0, lo),)], gu_ref.at[slot, pl.ds(i * lo, lo)]))
            moves.append((w.at[at + (pl.ds(lo, hi),)], gu_ref.at[slot, pl.ds(2 * lo + i * hi, hi)]))
        moves.append((wd_hbm.at[at], wd_ref.at[slot]))
        return [copy(a, b, w_sem.at[slot, i]) for i, (a, b) in enumerate(moves)]

    def sums_in(e, slot):
        return copy(prev.at[e], sums.at[slot], sum_sem.at[slot])

    def sums_out(e, slot):
        return copy(sums.at[slot], grad.at[e], sum_sem.at[slot])

    def keeps(e, slot):
        at = (layer, tab_ref[ROW_EXPERT * LANES + e])
        return [copy(keep_buf.at[slot, i], finals[i].at[at], keep_sem.at[slot, i]) for i in range(3)]

    def send(e, slot, part):
        return copy(keep_buf.at[slot], sent[part].at[e - part * (n_exp // 2)], keep_sem.at[slot, 3])

    def read(e, slot, part=0):
        return copy(got[part].at[e - part * (n_exp // 2)], got_buf.at[slot], read_sem.at[slot])

    def writes(e, slot):
        to = tab_ref[TAB_ROWS * LANES + e]
        return [copy(got_buf.at[slot, i], finals[i].at[got_layer, to], write_sem.at[slot, i]) for i in range(3)]

    def start(moves):
        for m in moves:
            m.start()

    def wait(moves):
        for m in moves:
            m.wait()

    n_tab = TAB_ROWS * LANES
    lists = [copy(tab_hbm.at[pl.ds(row_id * n_tab, n_tab)], tab_ref.at[pl.ds(0, n_tab)], list_sem.at[0]),
             copy(idx_hbm.at[pl.ds(row_id * N_SRC * list_len, N_SRC * list_len)], idx.at[pl.ds(0, N_SRC * list_len)],
                  list_sem.at[1]),
             copy(gate_hbm.at[pl.ds(row_id * gate_ref.shape[0], gate_ref.shape[0])], gate_ref, list_sem.at[2])]
    if got is not None:
        at = (got_layer * TAB_ROWS + ROW_PARTNER) * LANES
        lists.append(copy(tab_hbm.at[pl.ds(at, LANES)], tab_ref.at[pl.ds(n_tab, LANES)], list_sem.at[3]))
    start(lists)
    pieces = []
    for s in range(N_SRC):
        pieces.append((u_pieces[s], picks[0][s], s, 0, fwd))
        if bwd:
            pieces.append((dy_pieces[s], picks[1][s], s, HALF, own))
    lands = [copy(ref.at[pick], land.at[i % N_SRC], land_sem.at[i % N_SRC]) for i, (ref, pick, *_) in enumerate(pieces)]
    start(lands[:N_SRC])
    lists[0].wait()
    start(weights(0, 0))
    if bwd and not own:
        sums_in(0, 0).start()
    if got is not None:
        lists[3].wait()
        read(0, 0).start()
    if own:
        def clear(c, _):
            for k in range(4):
                acc[pl.ds(al(c * 1152 + 288 * k, 8), 288), :] = jnp.zeros((288, LANES), F32)
            return 0

        lax.fori_loop(0, acc.shape[0] // 1152, clear, 0)
        row_ref[...] = jnp.zeros(row_ref.shape, F32)
    rows = 256
    for i, (_, _, s, o, seed) in enumerate(pieces):
        lands[i].wait()

        def fill(c, _, i=i, o=o, seed=seed, s=s):
            r = al(c * rows, rows)
            for j in range(HALF):
                vals = land[i % N_SRC, pl.ds(r, rows), LANES * j:LANES * (j + 1)].astype(F32)
                to = pl.ds(PITCH * (s * n_blk + r) + o + j, rows, stride=PITCH)
                table[to, :] = vals
                if seed and s == 0:
                    acc[to, :] = vals
            return 0

        lax.fori_loop(0, n_blk // rows, fill, 0)
        if i + N_SRC < len(pieces):
            lands[i + N_SRC].start()
    wait(lists[1:3])
    for k in range(GRP):
        idx[N_SRC * list_len + k] = 0

    def first(q, _):
        gather(begin, 2 * q)
        gather(begin, 2 * q + 1)
        return 0

    begin = codes_of(0)
    lax.fori_loop(0, PER_TILE // 2, first, 0)
    convert(begin)

    def expert(e, _):
        slot = e & 1
        wait(weights(e, slot))
        if bwd and not own:
            sums_in(e, slot).wait()
        if got is not None:
            read(0, slot).wait()
            start(writes(e, slot))

            @pl.when((e > 0) & (e < n_exp - 1))
            def _():
                wait(writes(e - 1, 1 - slot))

        @pl.when(e < n_exp - 1)
        def _():
            start(weights(e + 1, 1 - slot))
            if bwd and not own:
                sums_in(e + 1, 1 - slot).start()
            if got is not None:
                for part in range(2):
                    @pl.when((e + 1 >= n_exp // 2) if part else (e + 1 < n_exp // 2))
                    def _(part=part):
                        read(e + 1, 1 - slot, part).start()

        if bwd and own:
            @pl.when(e > 1)
            def _():
                sums_out(e - 2, slot).wait()

            sums[slot] = jnp.zeros(sums.shape[1:], F32)

        def tile(t, _):
            before, after = codes_of(jnp.maximum(t - 1, 0)), codes_of(t + 1)
            for q in range(PER_TILE):
                if own:
                    scatter(before, q)
                gather(after, q)
            half = ROWS // 2
            for s0 in range(0, ROWS, half):
                sl = slice(s0, s0 + half)
                ab_ref[sl, :] = dot(x_u[sl, :], gu_ref[slot], nt)
                if bwd:
                    dh_ref[sl, :] = dot(x_c[sl, :], wd_ref[slot], nt)
            for r in range(0, ROWS, 16):
                rows = slice(r, r + 16)
                for c in range(0, lo, LANES):
                    h, da, db = middle(ab_ref[rows, c:c + LANES], ab_ref[rows, lo + c:lo + c + LANES],
                                       dh_ref[rows, c:c + LANES] if bwd else None)
                    h_ref[rows, c:c + LANES] = h.astype(BF16)
                    if bwd:
                        dab_ref[rows, c:c + LANES] = da.astype(BF16)
                        dab_ref[rows, lo + c:lo + c + LANES] = db.astype(BF16)
                a = ab_ref[rows, 2 * lo:]
                b = pltpu.roll(a, hi, 1)
                dh = dh_ref[rows, lo:] if bwd else None
                if bwd:
                    dh = jnp.concatenate([dh, dh], axis=1)
                h, da, db = middle(a, b, dh)
                h_ref[rows, lo:] = h[:, :hi].astype(BF16)
                if bwd:
                    dab_ref[rows, 2 * lo:] = jnp.where(low, da, pltpu.roll(db, hi, 1)).astype(BF16)
            for s0 in range(0, ROWS, half):
                sl = slice(s0, s0 + half)
                if fwd:
                    put_rows(0, dot(h_ref[sl, :], wd_ref[slot], nn), s0)
                if bwd and own:
                    put_rows(HALF, dot(dab_ref[sl, :], gu_ref[slot], nn), s0)
            if bwd:
                view = sums.at[slot]
                view[0:2 * ff, :] += dot(dab_ref[...], x_u[...], tn)
                view[2 * ff:, :] += dot(h_ref[...], x_c[...], tn)
            convert(after)
            return 0

        lax.fori_loop(tab_ref[ROW_BOUND * LANES + e], tab_ref[ROW_BOUND * LANES + e + 1], tile, 0)
        if bwd and own:
            sums_out(e, slot).start()
        if bwd and not own:
            @pl.when(e > 1)
            def _():
                wait(keeps(e - 2, slot) + [send(0, slot, 0)])

            for i in range(2):
                keep_buf[slot, i, 0:lo, :] = sums[slot, i * lo:(i + 1) * lo, :].astype(BF16)
                keep_buf[slot, i, lo:, :] = sums[slot, 2 * lo + i * hi:2 * lo + (i + 1) * hi, :].astype(BF16)
            keep_buf[slot, 2] = sums[slot, 2 * ff:, :].astype(BF16)
            start(keeps(e, slot))
            for part in range(2):
                @pl.when((e >= n_exp // 2) if part else (e < n_exp // 2))
                def _(part=part):
                    send(e, slot, part).start()
        return 0

    lax.fori_loop(0, n_exp, expert, 0)
    ends = ((n_exp - 2, (n_exp - 2) % 2), (n_exp - 1, (n_exp - 1) % 2))
    if own:
        end = codes_of(tab_ref[ROW_BOUND * LANES + n_exp] - 1)
        lax.fori_loop(0, PER_TILE, lambda q, _: (scatter(end, q), 0)[1], 0)
        flights = {}
        for o, out in ((HALF, du_outs), (0, y_outs)):
            for s in range(N_SRC if out else 0):
                wide = s == 0 or p_f32
                stage = stage_f.at[s] if wide else land.at[s]
                if s in flights:
                    flights[s].wait()

                def fetch(c, _, stage=stage, s=s, o=o):
                    r = al(c * rows, rows)
                    for j in range(HALF):
                        at = pl.ds(PITCH * (s * n_blk + r) + o + j, rows, stride=PITCH)
                        stage[pl.ds(r, rows), LANES * j:LANES * (j + 1)] = acc[at, :].astype(stage.dtype)
                    return 0

                lax.fori_loop(0, n_blk // rows, fetch, 0)
                flights[s] = copy(stage, out[s], out_sem.at[s])
                flights[s].start()
        wait(flights.values())
        if bwd:
            for e, slot in ends:
                sums_out(e, slot).wait()
    else:
        for e, slot in ends:
            wait(keeps(e, slot) + [send(0, slot, 0)])
            if got is not None:
                wait(writes(e, slot))


def run_experts(routes, layer, u, dy, weights, prev, finals, fwd, own, p_f32=False, got=None):
    tab, idx, gates = routes
    bwd = dy is not None
    wg, wu, wd = weights
    n_blk, wide = u[0][0].shape[-2:]
    n_layers, n_local, ff, d = wd.shape
    n_exp = n_local // 2
    row_id = layer
    list_len = idx.shape[0] // (n_layers * N_SRC)

    arrays = lambda pieces: [v for v, _ in pieces]
    operands = [tab, idx, gates] + arrays(u) + (arrays(dy) if bwd else []) + [wg, wu, wd]
    out_shape, aliases = [], {}
    for use in (fwd, bwd and own):
        if use:
            out_shape += [jax.ShapeDtypeStruct((n_blk, wide), F32 if s == 0 or p_f32 else BF16) for s in range(N_SRC)]
    if bwd and own:
        out_shape.append(jax.ShapeDtypeStruct((n_exp, 3 * ff, d), F32))
    if bwd and not own:
        operands.append(prev)
        if got is not None:
            operands += got
        for i, f in enumerate(finals or ()):
            aliases[len(operands)] = i
            operands.append(f)
        out_shape += [jax.ShapeDtypeStruct((n_layers, n_local, ff, d), BF16)] * 3
        out_shape += [jax.ShapeDtypeStruct((n_exp // 2, 3, ff, d), BF16)] * 2
    sem = lambda *s: pltpu.SemaphoreType.DMA(s)
    mid = lambda n, dt: pltpu.VMEM((ROWS, n), dt)
    table, rows = pltpu.VMEM((PITCH * N_SRC * n_blk, LANES), F32), pltpu.VMEM((PITCH * ROWS, LANES), F32)
    scratch = [pltpu.SMEM(((TAB_ROWS + 1) * LANES,), I32), pltpu.SMEM((N_SRC * list_len + LANES,), I32),
               pltpu.VMEM((N_SRC * list_len // LANES + 8, LANES), F32), pltpu.VMEM((N_SRC, n_blk, wide), BF16)]
    scratch += [table, rows] * (1 + own)
    scratch += [pltpu.VMEM((2, 2 * ff, d), BF16), pltpu.VMEM((2, ff, d), BF16), mid(LANES, F32)]
    scratch += [mid(d, BF16)] * (1 + bwd) + [mid(2 * ff, F32)] + [mid(ff, F32)] * bwd + [mid(ff, BF16)]
    scratch += [mid(2 * ff, BF16), pltpu.VMEM((2, 3 * ff, d), F32)] * bwd
    if bwd and not own:
        scratch.append(pltpu.VMEM((2, 3, ff, d), BF16))
    if got is not None:
        scratch.append(pltpu.VMEM((2, 3, ff, d), BF16))
    scratch += [sem(4), sem(N_SRC), sem(2, 5)] + [sem(2)] * bwd
    if bwd and not own:
        scratch.append(sem(2, 4))
    if got is not None:
        scratch += [sem(2), sem(2, 3)]
    if own:
        scratch += [pltpu.VMEM((N_SRC if p_f32 else 1, n_blk, wide), F32), sem(N_SRC)]
    passes = 2 + fwd + bwd * (4 + 2 * own)
    flops = 2 * d * ff * passes * n_blk * N_SRC * 2
    hoist = 1400 if not own else 700 if fwd else 800
    picks = [[i for _, i in u], [i for _, i in dy] if bwd else None]
    cfg = (fwd, bwd, own, layer, n_blk, d, ff, n_exp, picks, row_id, list_len, p_f32, len(aliases),
           None if got is None else 1 - layer)
    return pl.pallas_call(
        functools.partial(expert_kernel, cfg),
        out_shape=out_shape,
        in_specs=[any_space] * len(operands),
        out_specs=[any_space] * len(out_shape),
        scratch_shapes=scratch,
        input_output_aliases=aliases,
        compiler_params=pltpu.CompilerParams(
            vmem_limit_bytes=VMEM_LIMIT),
        cost_estimate=pl.CostEstimate(flops=flops, bytes_accessed=3 * 2 * n_exp * d * ff, transcendentals=0),
        name=f"experts_{'f' if fwd else ''}{'b' if bwd else ''}_{'own' if own else 'other'}_{layer}",
    )(*operands)


def place_kernel(layer, n_exp, tab_ref, got_ref, *refs):
    outs, (buf, in_sem, out_sem) = refs[3:6], refs[6:]
    reads = [pltpu.make_async_copy(got_ref.at[i], buf.at[i], in_sem.at[i]) for i in range(n_exp)]
    for read in reads:
        read.start()
    writes = []
    for i, read in enumerate(reads):
        read.wait()
        e = tab_ref[i]
        for k, out in enumerate(outs):
            writes.append(pltpu.make_async_copy(buf.at[i, k], out.at[layer, e], out_sem.at[i, k]))
            writes[-1].start()
    for write in writes:
        write.wait()


def place(partner, layer, got, finals):
    n_exp = got.shape[0]
    return pl.pallas_call(
        functools.partial(place_kernel, layer, n_exp),
        out_shape=[jax.ShapeDtypeStruct(f.shape, f.dtype) for f in finals],
        grid_spec=pltpu.PrefetchScalarGridSpec(
            num_scalar_prefetch=1, grid=(1,), in_specs=[any_space] * 4, out_specs=[any_space] * 3,
            scratch_shapes=[pltpu.VMEM(got.shape, got.dtype), pltpu.SemaphoreType.DMA((n_exp,)),
                            pltpu.SemaphoreType.DMA((n_exp, 3))]),
        input_output_aliases={2: 0, 3: 1, 4: 2},
        compiler_params=pltpu.CompilerParams(vmem_limit_bytes=VMEM_LIMIT),
        cost_estimate=pl.CostEstimate(flops=0, bytes_accessed=4 * got.size, transcendentals=0),
        name=f"place_{layer}",
    )(partner, got, *finals)


def peer(rel):
    return {name: (lax.axis_index(name) + ((rel >> bit) & 1)) % 2 for bit, name in enumerate(("ep", "core", "x"))}


def meet(rels):
    barrier = pltpu.get_barrier_semaphore()
    for rel in rels:
        pl.semaphore_signal(barrier, inc=1, device_id=peer(rel), device_id_type=MESH)
    pl.semaphore_wait(barrier, len(rels))


def remote(src, dst, send, recv, rel):
    return pltpu.make_async_remote_copy(src_ref=src, dst_ref=dst, send_sem=send, recv_sem=recv,
                                        device_id=peer(rel), device_id_type=MESH)


def share_kernel(n_rel, mine_ref, all_ref, send_sem, recv_sem):
    meet(range(1, n_rel))
    copies = [remote(mine_ref, all_ref.at[rel], send_sem.at[rel], recv_sem.at[rel], rel) for rel in range(1, n_rel)]
    for copy in copies:
        copy.start()
    all_ref[0] = mine_ref[...]
    for copy in copies:
        copy.wait()


def share(mine, n_rel):
    return pl.pallas_call(
        functools.partial(share_kernel, n_rel),
        out_shape=jax.ShapeDtypeStruct((n_rel,) + mine.shape, mine.dtype),
        in_specs=[in_vmem],
        out_specs=in_vmem,
        scratch_shapes=[pltpu.SemaphoreType.DMA((n_rel,)), pltpu.SemaphoreType.DMA((n_rel,))],
        compiler_params=pltpu.CompilerParams(collective_id=0, has_side_effects=True),
        cost_estimate=pl.CostEstimate(flops=10 ** 7, bytes_accessed=mine.size * 4 * n_rel, transcendentals=0),
        name="share_lists",
    )(mine)


def blocks_kernel(cfg, *refs):
    n_chunk, reduce, back, d = cfg
    refs = list(refs)
    take = lambda n: [refs.pop(0) for _ in range(n)]
    parts = take(N_SRC)
    m_ref, o_total, o_a, o_b = take(4)
    in_f, in_b, got_f, s_wire, r_wire, u_wire, y_wire, t_buf, u_buf, y_buf, load, send, recv, put = take(14)
    n_rows = t_buf.shape[0] // n_chunk
    cut = [pl.ds(k * n_rows, n_rows) for k in range(n_chunk)]
    thin = [pl.ds(k * n_rows // 2, n_rows // 2) for k in range(n_chunk)]
    side = lax.broadcasted_iota(I32, (n_rows // 2, LANES), 1) < LANES // 2
    tiles = d // LANES
    turn = lambda v: pltpu.roll(v, LANES // 2, 1)
    lanes = lambda v, j: v[:, LANES * j:LANES * (j + 1)]

    def pack(wire, k, value):
        top, low = value[:n_rows // 2], value[n_rows // 2:]
        turned = [turn(lanes(low, j)) for j in range(tiles + 1)]
        parts = [lanes(top, j) for j in range(tiles)] + [jnp.where(side, lanes(top, tiles), turned[0])]
        parts += [jnp.where(side, turned[j], turned[j + 1]) for j in range(tiles)]
        for j, part in enumerate(parts):
            wire[thin[k], LANES * j:LANES * (j + 1)] = part.astype(BF16)

    def unpack(wire, k):
        value = wire[thin[k], :].astype(F32)
        turned = [turn(lanes(value, tiles + j)) for j in range(tiles + 1)]
        top = [lanes(value, j) for j in range(tiles)] + [jnp.where(side, lanes(value, tiles), 0.0)]
        low = [jnp.where(side, turned[j], turned[j + 1]) for j in range(tiles)] + [jnp.where(side, turned[tiles], 0.0)]
        return jnp.concatenate([jnp.concatenate(top, axis=1), jnp.concatenate(low, axis=1)], axis=0)

    chunks = range(n_chunk)
    loads = {}
    for i, part in enumerate(parts[:2] if reduce else parts):
        buf = in_f.at[i] if reduce or i == 0 else in_b.at[i - 1]
        for k in chunks:
            loads[i, k] = pltpu.make_async_copy(part.at[cut[k]], buf.at[cut[k]], load.at[i, k])
    order = (1, 0) if reduce else range(N_SRC)
    for i in order:
        for k in chunks:
            loads[i, k].start()
    u_buf[...] = jnp.zeros(u_buf.shape, BF16)
    meet((Y, CORE))
    links = []
    copy_in = pltpu.make_async_copy

    def link(src, dst, rel, cut=cut):
        n = len(links)
        links.append([remote(src.at[cut[k]], dst.at[cut[k]], send.at[n, k], recv.at[n, k], rel) for k in chunks])
        return links[-1]

    if reduce:
        first = link(parts[3], got_f.at[1], CORE)
        second = link(parts[2], got_f.at[0], CORE)
        over = link(s_wire, r_wire, Y, thin)
        for copies in (first, second):
            for copy in copies:
                copy.start()
        for k in chunks:
            loads[1, k].wait()
            first[k].wait_recv()
            pack(s_wire, k, in_f[1, cut[k], :] + got_f[1, cut[k], :])
            over[k].start()
    to_y = link(u_wire, y_wire, Y, thin)
    to_core = link(u_buf, o_b.at[0], CORE)
    puts = []
    for k in chunks:
        if reduce:
            loads[0, k].wait()
            second[k].wait_recv()
            over[k].wait_recv()
            total = in_f[0, cut[k], :] + got_f[0, cut[k], :] + unpack(r_wire, k)
        else:
            for i in range(N_SRC):
                loads[i, k].wait()
            total = in_f[0, cut[k], :]
            for i in range(N_SRC - 1):
                total = total + in_b[i, cut[k], :].astype(F32)
        total = total.astype(BF16)
        t_buf[cut[k], :] = total
        dims = (((1,), (1 if back else 0,)), ((), ()))
        mixed = lax.dot_general(total[:, :d], m_ref[...], dims, preferred_element_type=F32)
        u_buf[cut[k], 0:d] = (total[:, :d].astype(F32) + mixed).astype(BF16)
        pack(u_wire, k, u_buf[cut[k], :].astype(F32))
        to_y[k].start()
        to_core[k].start()
        puts.append(pltpu.make_async_copy(u_buf.at[cut[k]], o_a.at[0, cut[k]], put.at[0, k]))
        puts.append(pltpu.make_async_copy(t_buf.at[cut[k]], o_total.at[cut[k]], put.at[1, k]))
        for copy in puts[-2:]:
            copy.start()
    on = link(y_buf, o_b.at[1], CORE)
    for k in chunks:
        to_y[k].wait_recv()
        y_buf[cut[k], :] = unpack(y_wire, k).astype(BF16)
        on[k].start()
        puts.append(copy_in(y_buf.at[cut[k]], o_a.at[1, cut[k]], put.at[2, k]))
        puts[-1].start()
    waited = [to_y] + ([first, second, over] if reduce else [])
    for copies in links:
        for copy in copies:
            if any(copies is w for w in waited):
                copy.wait_send()
            else:
                copy.wait()
    for copy in puts:
        copy.wait()


def complete_blocks(parts, m, reduce, back, ident, n_chunk=4):
    n_blk, wide = parts[0].shape
    d = m.shape[0]
    sem = lambda *s: pltpu.SemaphoreType.DMA(s)
    pair = jax.ShapeDtypeStruct((2, n_blk, wide), BF16)
    buf = lambda n, dt: pltpu.VMEM((n, n_blk, wide) if n else (n_blk, wide), dt)
    return pl.pallas_call(
        functools.partial(blocks_kernel, (n_chunk, reduce, back, d)),
        out_shape=[jax.ShapeDtypeStruct((n_blk, wide), BF16)] + [pair] * 2,
        in_specs=[any_space] * N_SRC + [in_vmem],
        out_specs=[any_space] * 3,
        scratch_shapes=[buf(2, F32), buf(3, BF16), buf(2, F32)] + [pltpu.VMEM((n_blk // 2, 2 * d), BF16)] * 4 + [
            buf(0, BF16), buf(0, BF16), buf(0, BF16), sem(4, n_chunk), sem(6, n_chunk), sem(6, n_chunk), sem(3, n_chunk)],
        compiler_params=pltpu.CompilerParams(collective_id=ident, has_side_effects=True, vmem_limit_bytes=VMEM_LIMIT),
        cost_estimate=pl.CostEstimate(flops=10 ** 8, bytes_accessed=n_blk * wide * 40, transcendentals=0),
        name=f"complete_blocks_{ident}",
    )(*parts, m)


def solution(mesh):
    ep_size, dp_size = mesh.shape['ep'], mesh.shape['dp']
    sub = Mesh(mesh.devices.reshape(ep_size, dp_size // 2, 2), ('ep', 'x', 'core'))
    tok_axes = ('x', 'core', 'ep')
    tok_spec = P(tok_axes, None)
    route_spec = P(None, tok_axes, None)
    whole_spec = P(None, None, None)
    expert_spec = P(None, 'ep', None, None)
    flip = [(0, 1), (1, 0)]
    move = lambda v, axis: lax.ppermute(v, axis, flip)
    move_diag = lambda v: lax.ppermute(v, ('ep', 'core'), [(0, 3), (1, 2), (2, 1), (3, 0)])
    fence = lax.optimization_barrier

    def device_step(tokens, d_out, expert_ids, gate_vals, w_mix, w_gate, w_up, w_down):
        n_layers, d = w_mix.shape[0], w_mix.shape[1]
        n_tok = tokens.shape[0]
        top = expert_ids.shape[2]
        n_local = w_gate.shape[1]
        n_exp = n_local * ep_size
        n = n_tok * top
        n_rel = 2 * N_SRC
        wide = cdiv(d, LANES) * LANES
        weights = (jnp.swapaxes(w_gate, 2, 3), jnp.swapaxes(w_up, 2, 3), w_down)
        pad = lambda v: jnp.pad(v, ((0, 0), (0, wide - d)))
        send_three = lambda p: [move(p[1], 'ep'), move(p[2], 'core'), move_diag(p[3])]

        def own_sum(p, got):
            return sum([g.astype(F32) for g in got], p)[:, :d].astype(BF16)

        one = lambda v: v.reshape(1, n_tok, wide)
        pairs = lambda a, b: [(a, 0), (a, 1), (b, 0), (b, 1)]

        one = lambda v: v.reshape(1, n_tok, wide)
        pairs = lambda a, b: [(a, 0), (a, 1), (b, 0), (b, 1)]
        singles = lambda *v: [(one(a), 0) for a in v]

        u0 = pad((tokens.astype(F32) + jnp.dot(tokens, w_mix[0], preferred_element_type=F32)).astype(BF16))
        u0_y, u0_c = move(u0, 'ep'), move(u0, 'core')
        lists = [sorted_list(expert_ids[l], gate_vals[l]) for l in range(n_layers)]
        counts = jnp.sum((expert_ids.reshape(n_layers, n, 1) == jnp.arange(n_exp, dtype=I32)).astype(F32), axis=1)
        packed = jnp.concatenate([jnp.concatenate([v[0] for v in lists] + [v[1] for v in lists]).reshape(-1, LANES),
                                  jnp.pad(counts, ((0, 8 - n_layers), (0, LANES - n_exp)))], axis=0)
        dy = pad(d_out)
        u0_y, u0_c, packed, dy = fence((u0_y, u0_c, packed, dy))
        u0_d = move(u0_y, 'core')
        shared = share(packed, N_SRC)
        dy, shared = fence((dy, shared))
        shared_x = move(shared, 'x')
        dy_y, dy_x = move(dy, 'ep'), move(dy, 'x')
        sizes = (n_layers, n_local, n_tok, n // LANES)
        routes = plan(shared, shared, *sizes)
        u0_half = singles(u0, u0_y, u0_c, u0_d)
        part = run_experts(routes, 0, u0_half, None, weights, None, None, True, True, p_f32=True)
        dy_y, dy_x, shared_x, part = fence((dy_y, dy_x, shared_x, part))
        dy_c, dy_d, dy_xy, dy_xc = move(dy, 'core'), move(dy_y, 'core'), move(dy_y, 'x'), move(dy_x, 'core')
        y0, u1_a, u1_b = complete_blocks(part, w_mix[1], True, False, 1)
        dy_c, dy_d, dy_xy, dy_xc, u0_p, u0_q, y0, u1_a, u1_b, shared_x = fence(
            (dy_c, dy_d, dy_xy, dy_xc, u0, u0_y, y0, u1_a, u1_b, shared_x))
        routes_x = plan(shared, shared_x, *sizes)
        dy_xd = move(dy_xy, 'core')
        u1_xa = move(u1_a, 'x')
        out = run_experts(routes, 1, pairs(u1_a, u1_b), singles(dy, dy_y, dy_c, dy_d), weights, None, None, True, True)
        u1_xa, dy_xd, u0_p, u0_q, out = fence((u1_xa, dy_xd, u0_p, u0_q, out))
        y_part, du_part, g1 = out[:4], out[4:8], out[8]
        u1_xb = move(u1_xa, 'core')
        got = send_three(du_part)
        u0_x, u0_xy = move(u0_p, 'x'), move(u0_q, 'x')
        out = run_experts(routes_x, 1, pairs(u1_xa, u1_xb), singles(dy_x, dy_xy, dy_xc, dy_xd), weights, g1, None,
                          False, False)
        got, u0_x, u0_xy, out = fence((got, u0_x, u0_xy, out))
        *finals, sent_a, sent_b = out
        du1, dx_a, dx_b = complete_blocks([du_part[0], *got], w_mix[1], False, True, 2)
        tx = lambda x, du: jnp.einsum('td,te->de', x, du, preferred_element_type=F32)
        g_mix1 = tx(y0[:, :d], du1[:, :d])
        dx_a, y_part, sent_a, sent_b, u0_x, u0_xy, g_mix1 = fence((dx_a, y_part, sent_a, sent_b, u0_x, u0_xy, g_mix1))
        dx_xa = move(dx_a, 'x')
        theirs1 = move(g_mix1, 'core')
        got_y = send_three(y_part)
        u0_xc, u0_xd = move(u0_x, 'core'), move(u0_xy, 'core')
        got1 = [move(sent_a, 'core'), move(sent_b, 'core')]
        out = run_experts(routes, 0, u0_half, pairs(dx_a, dx_b), weights, None, None, False, True)
        dx_xa, got_y, got1, u0_xc, u0_xd, theirs1, out = fence((dx_xa, got_y, got1, u0_xc, u0_xd, theirs1, out))
        du_part, g0 = out[:4], out[4]
        dx_xb = move(dx_xa, 'core')
        got = send_three(du_part)
        part1 = (g_mix1 + theirs1).astype(BF16)
        theirs1 = move(part1, 'ep')
        y1 = own_sum(y_part[0], got_y)
        y1, du_part, dx_xb, part1 = fence((y1, du_part, dx_xb, part1))
        out = run_experts(routes_x, 0, singles(u0_x, u0_xy, u0_xc, u0_xd), pairs(dx_xa, dx_xb), weights, g0, finals,
                          False, False, got=got1)
        got, theirs1, out = fence((got, theirs1, out))
        *finals, sent_a, sent_b = out
        got_a = move(sent_a, 'core')
        got_b = move(sent_b, 'core')
        add = lambda a, b: a.astype(F32) + b.astype(F32)
        du0 = own_sum(du_part[0], got)
        part0 = tx(tokens, du0).astype(BF16)
        theirs0 = move(part0, 'ep')
        dx0 = (du0.astype(F32) + jnp.einsum('te,de->td', du0, w_mix[0], preferred_element_type=F32)).astype(BF16)
        part1 = add(part1, theirs1).astype(BF16)
        row = lambda a: lax.slice_in_dim(routes[0], ROW_PARTNER * LANES + a, ROW_PARTNER * LANES + a + n_local // 4)
        dx0, part1, got_a, finals = fence((dx0, part1, got_a, finals))
        finals = place(row(0), 0, got_a, finals)
        theirs0, finals = fence((theirs0, finals))
        parts = jnp.stack([add(part0, theirs0).astype(BF16), part1])
        theirs = move(parts, 'x')
        parts, got_b = fence((parts, got_b))
        finals = place(row(n_local // 4), 0, got_b, finals)
        theirs, finals = fence((theirs, finals))
        total = add(parts, theirs)
        total0 = total[0].astype(BF16)
        g_mix = jnp.stack([add(total0, move(total0, 'core')), total[1]]).astype(BF16)
        return (y1, dx0, g_mix, jnp.swapaxes(finals[0], 2, 3), jnp.swapaxes(finals[1], 2, 3), finals[2])

    return jax.shard_map(device_step, mesh=sub,
                         in_specs=(tok_spec, tok_spec, route_spec, route_spec, whole_spec,
                                   expert_spec, expert_spec, expert_spec),
                         out_specs=(tok_spec, tok_spec, whole_spec, expert_spec, expert_spec, expert_spec),
                         check_vma=False)
```

```python
import functools

import jax
import jax.numpy as jnp
from jax import lax
from jax.experimental import pallas as pl
from jax.experimental.pallas import tpu as pltpu
from jax.sharding import Mesh, PartitionSpec as P

F32, BF16, I32 = jnp.float32, jnp.bfloat16, jnp.int32
MESH = pl.DeviceIdType.MESH
ROWS = 384
GRP = 8
TOKEN = 8
PITCH = 9
FULL = 8
HALF = 4
CAP_FACTOR = 3
LANES = 128
N_SRC = 4
Y, CORE, X = 1, 2, 4
VMEM_LIMIT = 62 * 1024 * 1024
PER_TILE = ROWS // GRP
ROW_BOUND, ROW_GOFF, ROW_EXPERT, ROW_PARTNER, TAB_ROWS = 32, 33, 34, 35, 40
SLOT_GROUPS = 256


def cdiv(a, b):
    return (a + b - 1) // b


def spans(d):
    return [(LANES * j, min(LANES, d - LANES * j)) for j in range(cdiv(d, LANES))]


any_space = pl.BlockSpec(memory_space=pl.ANY)
in_vmem = pl.BlockSpec(memory_space=pltpu.VMEM)


def sorted_list(expert_ids, gate_vals):
    n_tok, top = expert_ids.shape
    n = n_tok * top
    keys = expert_ids.reshape(n) * n + jnp.arange(n, dtype=I32)
    keys, gates = lax.sort((keys, gate_vals.reshape(n)), num_keys=1, is_stable=False)
    return ((keys % n) // top).astype(F32), gates


def plan_kernel(n_layers, n_local, n_tok, list_rows, deal_ref, all_ref, tab_ref, idx_ref, gate_ref):
    n_mine = n_local // 2
    core, ep = lax.axis_index('core'), lax.axis_index('ep')
    list_len = list_rows * LANES
    lane = lambda n: lax.broadcasted_iota(I32, (n, LANES), 1).astype(F32)
    sub = lambda n: lax.broadcasted_iota(I32, (n, LANES), 0).astype(F32)
    over_lanes = lambda v: jnp.sum(v, axis=1, keepdims=True)
    over_subs = lambda v: jnp.sum(v, axis=0, keepdims=True)
    l16, s16 = lane(n_mine), sub(n_mine)
    groups = lambda c: jnp.floor((c + (GRP - 0.5)) * (1.0 / GRP))
    for l in range(n_layers):
        cnt = all_ref[:, 2 * n_layers * list_rows + l, :]
        ends = cnt
        step = 1
        while step < 2 * n_local:
            ends = ends + jnp.where(lane(N_SRC) >= step, pltpu.roll(ends, step, 1), 0.0)
            step *= 2
        starts = ends - cnt
        second = (ep > 0)
        local = lambda v: jnp.where(lane(N_SRC) < n_local, jnp.where(second, pltpu.roll(v, LANES - n_local, 1), v), 0.0)
        cnt, starts = local(cnt), local(starts)
        tiles = jnp.floor((over_subs(groups(local(deal_ref[:, 2 * n_layers * list_rows + l, :]))) + (PER_TILE - 0.5))
                          * (1.0 / PER_TILE))
        load = jnp.where(lane(1) < n_local, jnp.maximum(1.0, tiles), -1.0)
        wide = jnp.broadcast_to(load, (n_local, LANES))
        col = over_lanes(jnp.where(lane(n_local) == sub(n_local), wide, 0.0))
        ahead = (col > wide) | ((col == wide) & (sub(n_local) < lane(n_local)))
        rank = over_subs(jnp.where(ahead, 1.0, 0.0))
        odd = s16 - 2.0 * jnp.floor(s16 * 0.5 + 0.25)
        flip = jnp.where(core > 0, 1.0 - odd, odd)
        dealt = lambda f: (jnp.broadcast_to(rank, (n_mine, LANES)) == 2.0 * s16 + f) & (l16 < n_local)
        pick = dealt(flip)
        choose = lambda p, row: over_lanes(jnp.where(p, jnp.broadcast_to(row, (n_mine, LANES)), 0.0))
        mine = lambda row: choose(pick, row)
        as_row = lambda c: over_subs(jnp.where(l16 == s16, c, 0.0))
        experts = as_row(mine(lane(1)))
        partner = as_row(choose(dealt(1.0 - flip), lane(1)))
        at = l * TAB_ROWS
        off = jnp.zeros((n_mine, 1), F32)
        pos = [jnp.zeros((n_mine, LANES), F32) for _ in range(SLOT_GROUPS // LANES)]
        for s in range(N_SRC):
            c, st = mine(cnt[s:s + 1]), mine(starts[s:s + 1]) + float(s * list_len)
            ng = groups(c)
            for i in range(len(pos)):
                rel = l16 + float(LANES * i) - off
                code = (st + GRP * rel) * 16.0 + jnp.minimum(float(GRP), c - GRP * rel)
                pos[i] = jnp.where((rel >= 0) & (rel < ng), code, pos[i])
            off = off + ng
        for i in range(len(pos)):
            tab_ref[pl.ds(at + i, n_mine, stride=len(pos)), :] = pos[i].astype(I32)
        n_tiles = jnp.maximum(1.0, jnp.floor((off + (PER_TILE - 0.5)) * (1.0 / PER_TILE)))
        bounds = over_subs(jnp.where(s16 < l16, n_tiles, 0.0))
        before = over_lanes(jnp.where(l16 == s16, jnp.broadcast_to(bounds, (n_mine, LANES)), 0.0))
        t = jnp.minimum(l16, over_subs(jnp.broadcast_to(n_tiles, (n_mine, LANES))) - 1.0)
        inside = (t >= before) & (t < before + n_tiles)
        goff = over_subs(jnp.where(inside, s16 * float(SLOT_GROUPS) + (t - before) * float(PER_TILE), 0.0))
        rows = [(ROW_BOUND, bounds), (ROW_GOFF, goff), (ROW_EXPERT, experts), (ROW_PARTNER, partner)]
        for row, value in rows:
            tab_ref[at + row:at + row + 1, :] = value.astype(I32)
    for l in range(n_layers):
        pad = l * (N_SRC * list_rows + 8) + N_SRC * list_rows
        gate_ref[pad:pad + 8, :] = jnp.zeros((8, LANES), F32)
        for s in range(N_SRC):
            to = (l * N_SRC + s) * list_rows
            toks = all_ref[s, l * list_rows:(l + 1) * list_rows, :]
            idx_ref[to:to + list_rows, :] = ((toks + float(s * n_tok)) * float(TOKEN)).astype(I32)
            to = l * (N_SRC * list_rows + 8) + s * list_rows
            gate_ref[to:to + list_rows, :] = all_ref[s, (n_layers + l) * list_rows:(n_layers + l + 1) * list_rows, :]


def plan(deal, shared, n_layers, n_local, n_tok, list_rows):
    n_tab = n_layers * TAB_ROWS
    n_list = n_layers * N_SRC * list_rows
    n_gate = n_layers * (N_SRC * list_rows + 8)
    tab, idx, gates = pl.pallas_call(
        functools.partial(plan_kernel, n_layers, n_local, n_tok, list_rows),
        out_shape=[jax.ShapeDtypeStruct((n_tab, LANES), I32), jax.ShapeDtypeStruct((n_list, LANES), I32),
                   jax.ShapeDtypeStruct((n_gate, LANES), F32)],
        in_specs=[in_vmem] * 2, out_specs=[in_vmem] * 3,
        cost_estimate=pl.CostEstimate(flops=10 ** 7, bytes_accessed=10 ** 6, transcendentals=0),
        name="plan",
    )(deal, shared)
    return tab.reshape(-1), idx.reshape(-1), gates


def expert_kernel(cfg, *refs):
    fwd, bwd, own, layer, n_blk, d, ff, n_exp, picks, row_id, list_len, p_f32, n_alias, got_layer = cfg
    refs = list(refs)
    take = lambda n: [refs.pop(0) for _ in range(n)]
    tab_hbm, idx_hbm, gate_hbm = take(3)
    u_pieces = take(N_SRC)
    dy_pieces = take(N_SRC) if bwd else []
    wg_hbm, wu_hbm, wd_hbm = take(3)
    prev = take(1)[0] if bwd and not own else None
    got = take(2) if got_layer is not None else None
    take(n_alias)
    y_outs = take(N_SRC) if fwd else []
    du_outs = take(N_SRC) if bwd and own else []
    grad = take(1)[0] if bwd and own else None
    finals = take(3) if bwd and not own else None
    sent = take(2) if bwd and not own else None
    tab_ref, idx, gate_ref, land, table, gat = take(6)
    acc, row_ref = take(2) if own else (None, None)
    gu_ref, wd_ref, g_ref, x_u = take(4)
    x_c = take(1)[0] if bwd else None
    ab_ref = take(1)[0]
    dh_ref = take(1)[0] if bwd else None
    h_ref = take(1)[0]
    dab_ref, sums = take(2) if bwd else (None, None)
    keep_buf = take(1)[0] if bwd and not own else None
    got_buf = take(1)[0] if got is not None else None
    list_sem, land_sem, w_sem = take(3)
    sum_sem = take(1)[0] if bwd else None
    keep_sem = take(1)[0] if bwd and not own else None
    read_sem, write_sem = take(2) if got is not None else (None, None)
    stage_f, out_sem = take(2) if own else (None, None)

    copy = pltpu.make_async_copy
    cols = spans(d)
    lo = ff // 256 * 256
    hi = ff - lo
    dot = functools.partial(lax.dot_general, preferred_element_type=F32)
    nn = (((1,), (0,)), ((), ()))
    nt = (((1,), (1,)), ((), ()))
    tn = (((0,), (0,)), ((), ()))
    al = pl.multiple_of
    n_row = N_SRC * n_blk
    glane = lax.broadcasted_iota(I32, (GRP, LANES), 1)
    gsub = lax.broadcasted_iota(I32, (GRP, LANES), 0)

    def row_at(r):
        return pl.ds(r * PITCH, FULL)

    def codes_of(tile):
        at = ROW_GOFF * LANES + tile
        if own and bwd:
            return lambda q: tab_ref[tab_ref[at] + q]
        view = tab_ref.at[pl.ds(tab_ref[at], PER_TILE)]
        return lambda q: view[q]

    def gather(codes, q):
        ids = idx.at[pl.ds(codes(q) >> 4, GRP)]
        for k in range(GRP):
            gat[row_at(q * GRP + k), :] = table[pl.ds(al(ids[k], TOKEN), FULL), :]

    def gate_column(code):
        pos = code >> 4
        row, shift = pos >> 7, pos & (LANES - 1)
        want = glane == gsub + shift
        over = glane == gsub + (shift - LANES)
        here = gate_ref[pl.ds(row, GRP, stride=0), :]
        there = gate_ref[pl.ds(row + 1, GRP, stride=0), :]
        v = jnp.where(want, here, jnp.where(over, there, 0.0))
        return jnp.where(gsub < (code & 15), jnp.sum(v, axis=1, keepdims=True), 0.0)

    def scatter(codes, q):
        ids = idx.at[pl.ds(codes(q) >> 4, GRP)]
        new = []
        for k in range(GRP):
            at = pl.ds(al(ids[k], TOKEN), FULL)
            new.append((at, acc[at, :] + row_ref[row_at(q * GRP + k), :]))
        for at, value in reversed(new):
            acc[at, :] = value

    def convert(codes):
        for q in range(0, PER_TILE, 2):
            part = []
            for p in (q, q + 1):
                code = codes(p)
                rows = [gat[pl.ds(GRP * PITCH * p + j, GRP, stride=PITCH), :] for j in range(FULL if bwd else HALF)]
                real = gsub < (code & 15)
                gate = gate_column(code)
                g_ref[GRP * p:GRP * (p + 1), :] = gate
                part.append([jnp.where(real, v, 0.0) for v in rows[:HALF]] + [v * gate for v in rows[HALF:]])
            at = slice(GRP * q, GRP * (q + 2))
            for x, o in ((x_u, 0), (x_c, HALF)):
                if x is None:
                    continue
                for j, (c, w) in enumerate(cols):
                    both = jnp.concatenate([part[0][o + j], part[1][o + j]], axis=0)
                    x[at, c:c + w] = both[:, :w].astype(BF16)

    def put_rows(o, value, s0):
        value = value.astype(BF16).astype(F32)
        n = value.shape[0]
        for j, (c, w) in enumerate(cols):
            row_ref[pl.ds(PITCH * s0 + o + j, n, stride=PITCH), 0:w] = value[:, c:c + w] * g_ref[s0:s0 + n, 0:w]

    low = lax.broadcasted_iota(I32, (16, 2 * hi), 1) < hi

    def middle(a, b, dh):
        sig = 0.5 * jnp.tanh(0.5 * a) + 0.5
        act = a * sig
        h = act * b
        if dh is None:
            return h, None, None
        slope = sig * (1.0 + a * (1.0 - sig))
        return h, dh * b * slope, dh * act

    def weights(e, slot):
        at = (layer, tab_ref[ROW_EXPERT * LANES + e])
        moves = []
        for i, w in enumerate((wg_hbm, wu_hbm)):
            moves.append((w.at[at + (pl.ds(0, lo),)], gu_ref.at[slot, pl.ds(i * lo, lo)]))
            moves.append((w.at[at + (pl.ds(lo, hi),)], gu_ref.at[slot, pl.ds(2 * lo + i * hi, hi)]))
        moves.append((wd_hbm.at[at], wd_ref.at[slot]))
        return [copy(a, b, w_sem.at[slot, i]) for i, (a, b) in enumerate(moves)]

    def sums_in(e, slot):
        return copy(prev.at[e], sums.at[slot], sum_sem.at[slot])

    def sums_out(e, slot):
        return copy(sums.at[slot], grad.at[e], sum_sem.at[slot])

    def keeps(e, slot):
        at = (layer, tab_ref[ROW_EXPERT * LANES + e])
        return [copy(keep_buf.at[slot, i], finals[i].at[at], keep_sem.at[slot, i]) for i in range(3)]

    def send(e, slot, part):
        return copy(keep_buf.at[slot], sent[part].at[e - part * (n_exp // 2)], keep_sem.at[slot, 3])

    def read(e, slot, part=0):
        return copy(got[part].at[e - part * (n_exp // 2)], got_buf.at[slot], read_sem.at[slot])

    def writes(e, slot):
        to = tab_ref[TAB_ROWS * LANES + e]
        return [copy(got_buf.at[slot, i], finals[i].at[got_layer, to], write_sem.at[slot, i]) for i in range(3)]

    def start(moves):
        for m in moves:
            m.start()

    def wait(moves):
        for m in moves:
            m.wait()

    n_tab = TAB_ROWS * LANES
    lists = [copy(tab_hbm.at[pl.ds(row_id * n_tab, n_tab)], tab_ref.at[pl.ds(0, n_tab)], list_sem.at[0]),
             copy(idx_hbm.at[pl.ds(row_id * N_SRC * list_len, N_SRC * list_len)], idx.at[pl.ds(0, N_SRC * list_len)],
                  list_sem.at[1]),
             copy(gate_hbm.at[pl.ds(row_id * gate_ref.shape[0], gate_ref.shape[0])], gate_ref, list_sem.at[2])]
    if got is not None:
        at = (got_layer * TAB_ROWS + ROW_PARTNER) * LANES
        lists.append(copy(tab_hbm.at[pl.ds(at, LANES)], tab_ref.at[pl.ds(n_tab, LANES)], list_sem.at[3]))
    start(lists)
    pieces = []
    for s in range(N_SRC):
        pieces.append((u_pieces[s], picks[0][s], s, 0, fwd))
        if bwd:
            pieces.append((dy_pieces[s], picks[1][s], s, HALF, own))
    lands = [copy(ref.at[pick], land.at[i % N_SRC], land_sem.at[i % N_SRC]) for i, (ref, pick, *_) in enumerate(pieces)]
    start(lands[:N_SRC])
    lists[0].wait()
    start(weights(0, 0))
    if bwd and not own:
        sums_in(0, 0).start()
    if got is not None:
        lists[3].wait()
        read(0, 0).start()
    if own:
        def clear(c, _):
            for k in range(4):
                acc[pl.ds(al(c * 1024 + 256 * k, 8), 256), :] = jnp.zeros((256, LANES), F32)
            return 0

        lax.fori_loop(0, acc.shape[0] // 1024, clear, 0)
        row_ref[...] = jnp.zeros(row_ref.shape, F32)
    rows = 256
    for i, (_, _, s, o, seed) in enumerate(pieces):
        lands[i].wait()

        def fill(c, _, i=i, o=o, seed=seed, s=s):
            r = al(c * rows, rows)
            for j in range(HALF):
                vals = land[i % N_SRC, pl.ds(r, rows), LANES * j:LANES * (j + 1)].astype(F32)
                to = pl.ds(TOKEN * (s * n_blk + r) + o + j, rows, stride=TOKEN)
                table[to, :] = vals
                if seed and s == 0:
                    acc[to, :] = vals
            return 0

        lax.fori_loop(0, n_blk // rows, fill, 0)
        if i + N_SRC < len(pieces):
            lands[i + N_SRC].start()
    wait(lists[1:3])
    for k in range(GRP):
        idx[N_SRC * list_len + k] = 0

    def first(q, _):
        gather(begin, 2 * q)
        gather(begin, 2 * q + 1)
        return 0

    begin = codes_of(0)
    lax.fori_loop(0, PER_TILE // 2, first, 0)
    convert(begin)

    def expert(e, _):
        slot = e & 1
        wait(weights(e, slot))
        if bwd and not own:
            sums_in(e, slot).wait()
        if got is not None:
            read(0, slot).wait()
            start(writes(e, slot))

            @pl.when((e > 0) & (e < n_exp - 1))
            def _():
                wait(writes(e - 1, 1 - slot))

        @pl.when(e < n_exp - 1)
        def _():
            start(weights(e + 1, 1 - slot))
            if bwd and not own:
                sums_in(e + 1, 1 - slot).start()
            if got is not None:
                for part in range(2):
                    @pl.when((e + 1 >= n_exp // 2) if part else (e + 1 < n_exp // 2))
                    def _(part=part):
                        read(e + 1, 1 - slot, part).start()

        if bwd and own:
            @pl.when(e > 1)
            def _():
                sums_out(e - 2, slot).wait()

            sums[slot] = jnp.zeros(sums.shape[1:], F32)

        def tile(t, _):
            before, after = codes_of(jnp.maximum(t - 1, 0)), codes_of(t + 1)
            for q in range(PER_TILE):
                if own:
                    scatter(before, q)
                gather(after, q)
            half = ROWS // 2
            for s0 in range(0, ROWS, half):
                sl = slice(s0, s0 + half)
                ab_ref[sl, :] = dot(x_u[sl, :], gu_ref[slot], nt)
                if bwd:
                    dh_ref[sl, :] = dot(x_c[sl, :], wd_ref[slot], nt)
            for r in range(0, ROWS, 16):
                rows = slice(r, r + 16)
                for c in range(0, lo, LANES):
                    h, da, db = middle(ab_ref[rows, c:c + LANES], ab_ref[rows, lo + c:lo + c + LANES],
                                       dh_ref[rows, c:c + LANES] if bwd else None)
                    h_ref[rows, c:c + LANES] = h.astype(BF16)
                    if bwd:
                        dab_ref[rows, c:c + LANES] = da.astype(BF16)
                        dab_ref[rows, lo + c:lo + c + LANES] = db.astype(BF16)
                a = ab_ref[rows, 2 * lo:]
                b = pltpu.roll(a, hi, 1)
                dh = dh_ref[rows, lo:] if bwd else None
                if bwd:
                    dh = jnp.concatenate([dh, dh], axis=1)
                h, da, db = middle(a, b, dh)
                h_ref[rows, lo:] = h[:, :hi].astype(BF16)
                if bwd:
                    dab_ref[rows, 2 * lo:] = jnp.where(low, da, pltpu.roll(db, hi, 1)).astype(BF16)
            for s0 in range(0, ROWS, half):
                sl = slice(s0, s0 + half)
                if fwd:
                    put_rows(0, dot(h_ref[sl, :], wd_ref[slot], nn), s0)
                if bwd and own:
                    put_rows(HALF, dot(dab_ref[sl, :], gu_ref[slot], nn), s0)
            if bwd:
                view = sums.at[slot]
                view[0:2 * ff, :] += dot(dab_ref[...], x_u[...], tn)
                view[2 * ff:, :] += dot(h_ref[...], x_c[...], tn)
            convert(after)
            return 0

        lax.fori_loop(tab_ref[ROW_BOUND * LANES + e], tab_ref[ROW_BOUND * LANES + e + 1], tile, 0)
        if bwd and own:
            sums_out(e, slot).start()
        if bwd and not own:
            @pl.when(e > 1)
            def _():
                wait(keeps(e - 2, slot) + [send(0, slot, 0)])

            for i in range(2):
                keep_buf[slot, i, 0:lo, :] = sums[slot, i * lo:(i + 1) * lo, :].astype(BF16)
                keep_buf[slot, i, lo:, :] = sums[slot, 2 * lo + i * hi:2 * lo + (i + 1) * hi, :].astype(BF16)
            keep_buf[slot, 2] = sums[slot, 2 * ff:, :].astype(BF16)
            start(keeps(e, slot))
            for part in range(2):
                @pl.when((e >= n_exp // 2) if part else (e < n_exp // 2))
                def _(part=part):
                    send(e, slot, part).start()
        return 0

    lax.fori_loop(0, n_exp, expert, 0)
    ends = ((n_exp - 2, (n_exp - 2) % 2), (n_exp - 1, (n_exp - 1) % 2))
    if own:
        end = codes_of(tab_ref[ROW_BOUND * LANES + n_exp] - 1)
        lax.fori_loop(0, PER_TILE, lambda q, _: (scatter(end, q), 0)[1], 0)
        flights = {}
        for o, out in ((HALF, du_outs), (0, y_outs)):
            for s in range(N_SRC if out else 0):
                wide = s == 0 or p_f32
                stage = stage_f.at[s] if wide else land.at[s]
                if s in flights:
                    flights[s].wait()

                def fetch(c, _, stage=stage, s=s, o=o):
                    r = al(c * rows, rows)
                    for j in range(HALF):
                        at = pl.ds(TOKEN * (s * n_blk + r) + o + j, rows, stride=TOKEN)
                        stage[pl.ds(r, rows), LANES * j:LANES * (j + 1)] = acc[at, :].astype(stage.dtype)
                    return 0

                lax.fori_loop(0, n_blk // rows, fetch, 0)
                flights[s] = copy(stage, out[s], out_sem.at[s])
                flights[s].start()
        wait(flights.values())
        if bwd:
            for e, slot in ends:
                sums_out(e, slot).wait()
    else:
        for e, slot in ends:
            wait(keeps(e, slot) + [send(0, slot, 0)])
            if got is not None:
                wait(writes(e, slot))


def run_experts(routes, layer, u, dy, weights, prev, finals, fwd, own, p_f32=False, got=None):
    tab, idx, gates = routes
    bwd = dy is not None
    wg, wu, wd = weights
    n_blk, wide = u[0][0].shape[-2:]
    n_layers, n_local, ff, d = wd.shape
    n_exp = n_local // 2
    row_id = layer
    list_len = idx.shape[0] // (n_layers * N_SRC)

    arrays = lambda pieces: [v for v, _ in pieces]
    operands = [tab, idx, gates] + arrays(u) + (arrays(dy) if bwd else []) + [wg, wu, wd]
    out_shape, aliases = [], {}
    for use in (fwd, bwd and own):
        if use:
            out_shape += [jax.ShapeDtypeStruct((n_blk, wide), F32 if s == 0 or p_f32 else BF16) for s in range(N_SRC)]
    if bwd and own:
        out_shape.append(jax.ShapeDtypeStruct((n_exp, 3 * ff, d), F32))
    if bwd and not own:
        operands.append(prev)
        if got is not None:
            operands += got
        for i, f in enumerate(finals or ()):
            aliases[len(operands)] = i
            operands.append(f)
        out_shape += [jax.ShapeDtypeStruct((n_layers, n_local, ff, d), BF16)] * 3
        out_shape += [jax.ShapeDtypeStruct((n_exp // 2, 3, ff, d), BF16)] * 2
    sem = lambda *s: pltpu.SemaphoreType.DMA(s)
    mid = lambda n, dt: pltpu.VMEM((ROWS, n), dt)
    table, rows = pltpu.VMEM((TOKEN * N_SRC * n_blk, LANES), F32), pltpu.VMEM((PITCH * ROWS, LANES), F32)
    scratch = [pltpu.SMEM(((TAB_ROWS + 1) * LANES,), I32), pltpu.SMEM((N_SRC * list_len + LANES,), I32),
               pltpu.VMEM((N_SRC * list_len // LANES + 8, LANES), F32), pltpu.VMEM((N_SRC, n_blk, wide), BF16)]
    scratch += [table, rows] * (1 + own)
    scratch += [pltpu.VMEM((2, 2 * ff, d), BF16), pltpu.VMEM((2, ff, d), BF16), mid(LANES, F32)]
    scratch += [mid(d, BF16)] * (1 + bwd) + [mid(2 * ff, F32)] + [mid(ff, F32)] * bwd + [mid(ff, BF16)]
    scratch += [mid(2 * ff, BF16), pltpu.VMEM((2, 3 * ff, d), F32)] * bwd
    if bwd and not own:
        scratch.append(pltpu.VMEM((2, 3, ff, d), BF16))
    if got is not None:
        scratch.append(pltpu.VMEM((2, 3, ff, d), BF16))
    scratch += [sem(4), sem(N_SRC), sem(2, 5)] + [sem(2)] * bwd
    if bwd and not own:
        scratch.append(sem(2, 4))
    if got is not None:
        scratch += [sem(2), sem(2, 3)]
    if own:
        scratch += [pltpu.VMEM((N_SRC if p_f32 else 1, n_blk, wide), F32), sem(N_SRC)]
    passes = 2 + fwd + bwd * (4 + 2 * own)
    flops = 2 * d * ff * passes * n_blk * N_SRC * 2
    hoist = 1400 if not own else 700 if fwd else 800
    picks = [[i for _, i in u], [i for _, i in dy] if bwd else None]
    cfg = (fwd, bwd, own, layer, n_blk, d, ff, n_exp, picks, row_id, list_len, p_f32, len(aliases),
           None if got is None else 1 - layer)
    return pl.pallas_call(
        functools.partial(expert_kernel, cfg),
        out_shape=out_shape,
        in_specs=[any_space] * len(operands),
        out_specs=[any_space] * len(out_shape),
        scratch_shapes=scratch,
        input_output_aliases=aliases,
        compiler_params=pltpu.CompilerParams(
            vmem_limit_bytes=VMEM_LIMIT),
        cost_estimate=pl.CostEstimate(flops=flops, bytes_accessed=3 * 2 * n_exp * d * ff, transcendentals=0),
        name=f"experts_{'f' if fwd else ''}{'b' if bwd else ''}_{'own' if own else 'other'}_{layer}",
    )(*operands)


def place_kernel(layer, n_exp, tab_ref, got_ref, *refs):
    outs, (buf, in_sem, out_sem) = refs[3:6], refs[6:]
    reads = [pltpu.make_async_copy(got_ref.at[i], buf.at[i], in_sem.at[i]) for i in range(n_exp)]
    for read in reads:
        read.start()
    writes = []
    for i, read in enumerate(reads):
        read.wait()
        e = tab_ref[i]
        for k, out in enumerate(outs):
            writes.append(pltpu.make_async_copy(buf.at[i, k], out.at[layer, e], out_sem.at[i, k]))
            writes[-1].start()
    for write in writes:
        write.wait()


def place(partner, layer, got, finals):
    n_exp = got.shape[0]
    return pl.pallas_call(
        functools.partial(place_kernel, layer, n_exp),
        out_shape=[jax.ShapeDtypeStruct(f.shape, f.dtype) for f in finals],
        grid_spec=pltpu.PrefetchScalarGridSpec(
            num_scalar_prefetch=1, grid=(1,), in_specs=[any_space] * 4, out_specs=[any_space] * 3,
            scratch_shapes=[pltpu.VMEM(got.shape, got.dtype), pltpu.SemaphoreType.DMA((n_exp,)),
                            pltpu.SemaphoreType.DMA((n_exp, 3))]),
        input_output_aliases={2: 0, 3: 1, 4: 2},
        compiler_params=pltpu.CompilerParams(vmem_limit_bytes=VMEM_LIMIT),
        cost_estimate=pl.CostEstimate(flops=0, bytes_accessed=4 * got.size, transcendentals=0),
        name=f"place_{layer}",
    )(partner, got, *finals)


def peer(rel):
    return {name: (lax.axis_index(name) + ((rel >> bit) & 1)) % 2 for bit, name in enumerate(("ep", "core", "x"))}


def meet(rels):
    barrier = pltpu.get_barrier_semaphore()
    for rel in rels:
        pl.semaphore_signal(barrier, inc=1, device_id=peer(rel), device_id_type=MESH)
    pl.semaphore_wait(barrier, len(rels))


def remote(src, dst, send, recv, rel):
    return pltpu.make_async_remote_copy(src_ref=src, dst_ref=dst, send_sem=send, recv_sem=recv,
                                        device_id=peer(rel), device_id_type=MESH)


def share_kernel(n_rel, mine_ref, all_ref, send_sem, recv_sem):
    meet(range(1, n_rel))
    copies = [remote(mine_ref, all_ref.at[rel], send_sem.at[rel], recv_sem.at[rel], rel) for rel in range(1, n_rel)]
    for copy in copies:
        copy.start()
    all_ref[0] = mine_ref[...]
    for copy in copies:
        copy.wait()


def share(mine, n_rel):
    return pl.pallas_call(
        functools.partial(share_kernel, n_rel),
        out_shape=jax.ShapeDtypeStruct((n_rel,) + mine.shape, mine.dtype),
        in_specs=[in_vmem],
        out_specs=in_vmem,
        scratch_shapes=[pltpu.SemaphoreType.DMA((n_rel,)), pltpu.SemaphoreType.DMA((n_rel,))],
        compiler_params=pltpu.CompilerParams(collective_id=0, has_side_effects=True),
        cost_estimate=pl.CostEstimate(flops=10 ** 7, bytes_accessed=mine.size * 4 * n_rel, transcendentals=0),
        name="share_lists",
    )(mine)


def blocks_kernel(cfg, *refs):
    n_chunk, reduce, back, d = cfg
    refs = list(refs)
    take = lambda n: [refs.pop(0) for _ in range(n)]
    parts = take(N_SRC)
    m_ref, o_total, o_a, o_b = take(4)
    in_f, in_b, got_f, s_wire, r_wire, u_wire, y_wire, t_buf, u_buf, y_buf, load, send, recv, put = take(14)
    n_rows = t_buf.shape[0] // n_chunk
    cut = [pl.ds(k * n_rows, n_rows) for k in range(n_chunk)]
    thin = [pl.ds(k * n_rows // 2, n_rows // 2) for k in range(n_chunk)]
    side = lax.broadcasted_iota(I32, (n_rows // 2, LANES), 1) < LANES // 2
    tiles = d // LANES
    turn = lambda v: pltpu.roll(v, LANES // 2, 1)
    lanes = lambda v, j: v[:, LANES * j:LANES * (j + 1)]

    def pack(wire, k, value):
        top, low = value[:n_rows // 2], value[n_rows // 2:]
        turned = [turn(lanes(low, j)) for j in range(tiles + 1)]
        parts = [lanes(top, j) for j in range(tiles)] + [jnp.where(side, lanes(top, tiles), turned[0])]
        parts += [jnp.where(side, turned[j], turned[j + 1]) for j in range(tiles)]
        for j, part in enumerate(parts):
            wire[thin[k], LANES * j:LANES * (j + 1)] = part.astype(BF16)

    def unpack(wire, k):
        value = wire[thin[k], :].astype(F32)
        turned = [turn(lanes(value, tiles + j)) for j in range(tiles + 1)]
        top = [lanes(value, j) for j in range(tiles)] + [jnp.where(side, lanes(value, tiles), 0.0)]
        low = [jnp.where(side, turned[j], turned[j + 1]) for j in range(tiles)] + [jnp.where(side, turned[tiles], 0.0)]
        return jnp.concatenate([jnp.concatenate(top, axis=1), jnp.concatenate(low, axis=1)], axis=0)

    chunks = range(n_chunk)
    loads = {}
    for i, part in enumerate(parts[:2] if reduce else parts):
        buf = in_f.at[i] if reduce or i == 0 else in_b.at[i - 1]
        for k in chunks:
            loads[i, k] = pltpu.make_async_copy(part.at[cut[k]], buf.at[cut[k]], load.at[i, k])
    order = (1, 0) if reduce else range(N_SRC)
    for i in order:
        for k in chunks:
            loads[i, k].start()
    u_buf[...] = jnp.zeros(u_buf.shape, BF16)
    meet((Y, CORE))
    links = []
    copy_in = pltpu.make_async_copy

    def link(src, dst, rel, cut=cut):
        n = len(links)
        links.append([remote(src.at[cut[k]], dst.at[cut[k]], send.at[n, k], recv.at[n, k], rel) for k in chunks])
        return links[-1]

    if reduce:
        first = link(parts[3], got_f.at[1], CORE)
        second = link(parts[2], got_f.at[0], CORE)
        over = link(s_wire, r_wire, Y, thin)
        for copies in (first, second):
            for copy in copies:
                copy.start()
        for k in chunks:
            loads[1, k].wait()
            first[k].wait_recv()
            pack(s_wire, k, in_f[1, cut[k], :] + got_f[1, cut[k], :])
            over[k].start()
    to_y = link(u_wire, y_wire, Y, thin)
    to_core = link(u_buf, o_b.at[0], CORE)
    puts = []
    for k in chunks:
        if reduce:
            loads[0, k].wait()
            second[k].wait_recv()
            over[k].wait_recv()
            total = in_f[0, cut[k], :] + got_f[0, cut[k], :] + unpack(r_wire, k)
        else:
            for i in range(N_SRC):
                loads[i, k].wait()
            total = in_f[0, cut[k], :]
            for i in range(N_SRC - 1):
                total = total + in_b[i, cut[k], :].astype(F32)
        total = total.astype(BF16)
        t_buf[cut[k], :] = total
        dims = (((1,), (1 if back else 0,)), ((), ()))
        mixed = lax.dot_general(total[:, :d], m_ref[...], dims, preferred_element_type=F32)
        u_buf[cut[k], 0:d] = (total[:, :d].astype(F32) + mixed).astype(BF16)
        pack(u_wire, k, u_buf[cut[k], :].astype(F32))
        to_y[k].start()
        to_core[k].start()
        puts.append(pltpu.make_async_copy(u_buf.at[cut[k]], o_a.at[0, cut[k]], put.at[0, k]))
        puts.append(pltpu.make_async_copy(t_buf.at[cut[k]], o_total.at[cut[k]], put.at[1, k]))
        for copy in puts[-2:]:
            copy.start()
    on = link(y_buf, o_b.at[1], CORE)
    for k in chunks:
        to_y[k].wait_recv()
        y_buf[cut[k], :] = unpack(y_wire, k).astype(BF16)
        on[k].start()
        puts.append(copy_in(y_buf.at[cut[k]], o_a.at[1, cut[k]], put.at[2, k]))
        puts[-1].start()
    waited = [to_y] + ([first, second, over] if reduce else [])
    for copies in links:
        for copy in copies:
            if any(copies is w for w in waited):
                copy.wait_send()
            else:
                copy.wait()
    for copy in puts:
        copy.wait()


def complete_blocks(parts, m, reduce, back, ident, n_chunk=4):
    n_blk, wide = parts[0].shape
    d = m.shape[0]
    sem = lambda *s: pltpu.SemaphoreType.DMA(s)
    pair = jax.ShapeDtypeStruct((2, n_blk, wide), BF16)
    buf = lambda n, dt: pltpu.VMEM((n, n_blk, wide) if n else (n_blk, wide), dt)
    return pl.pallas_call(
        functools.partial(blocks_kernel, (n_chunk, reduce, back, d)),
        out_shape=[jax.ShapeDtypeStruct((n_blk, wide), BF16)] + [pair] * 2,
        in_specs=[any_space] * N_SRC + [in_vmem],
        out_specs=[any_space] * 3,
        scratch_shapes=[buf(2, F32), buf(3, BF16), buf(2, F32)] + [pltpu.VMEM((n_blk // 2, 2 * d), BF16)] * 4 + [
            buf(0, BF16), buf(0, BF16), buf(0, BF16), sem(4, n_chunk), sem(6, n_chunk), sem(6, n_chunk), sem(3, n_chunk)],
        compiler_params=pltpu.CompilerParams(collective_id=ident, has_side_effects=True, vmem_limit_bytes=VMEM_LIMIT),
        cost_estimate=pl.CostEstimate(flops=10 ** 8, bytes_accessed=n_blk * wide * 40, transcendentals=0),
        name=f"complete_blocks_{ident}",
    )(*parts, m)


def solution(mesh):
    ep_size, dp_size = mesh.shape['ep'], mesh.shape['dp']
    sub = Mesh(mesh.devices.reshape(ep_size, dp_size // 2, 2), ('ep', 'x', 'core'))
    tok_axes = ('x', 'core', 'ep')
    tok_spec = P(tok_axes, None)
    route_spec = P(None, tok_axes, None)
    whole_spec = P(None, None, None)
    expert_spec = P(None, 'ep', None, None)
    flip = [(0, 1), (1, 0)]
    move = lambda v, axis: lax.ppermute(v, axis, flip)
    move_diag = lambda v: lax.ppermute(v, ('ep', 'core'), [(0, 3), (1, 2), (2, 1), (3, 0)])
    fence = lax.optimization_barrier

    def device_step(tokens, d_out, expert_ids, gate_vals, w_mix, w_gate, w_up, w_down):
        n_layers, d = w_mix.shape[0], w_mix.shape[1]
        n_tok = tokens.shape[0]
        top = expert_ids.shape[2]
        n_local = w_gate.shape[1]
        n_exp = n_local * ep_size
        n = n_tok * top
        n_rel = 2 * N_SRC
        wide = cdiv(d, LANES) * LANES
        weights = (jnp.swapaxes(w_gate, 2, 3), jnp.swapaxes(w_up, 2, 3), w_down)
        pad = lambda v: jnp.pad(v, ((0, 0), (0, wide - d)))
        send_three = lambda p: [move(p[1], 'ep'), move(p[2], 'core'), move_diag(p[3])]

        def own_sum(p, got):
            return sum([g.astype(F32) for g in got], p)[:, :d].astype(BF16)

        one = lambda v: v.reshape(1, n_tok, wide)
        pairs = lambda a, b: [(a, 0), (a, 1), (b, 0), (b, 1)]

        one = lambda v: v.reshape(1, n_tok, wide)
        pairs = lambda a, b: [(a, 0), (a, 1), (b, 0), (b, 1)]
        singles = lambda *v: [(one(a), 0) for a in v]

        u0 = pad((tokens.astype(F32) + jnp.dot(tokens, w_mix[0], preferred_element_type=F32)).astype(BF16))
        u0_y, u0_c = move(u0, 'ep'), move(u0, 'core')
        lists = [sorted_list(expert_ids[l], gate_vals[l]) for l in range(n_layers)]
        counts = jnp.sum((expert_ids.reshape(n_layers, n, 1) == jnp.arange(n_exp, dtype=I32)).astype(F32), axis=1)
        packed = jnp.concatenate([jnp.concatenate([v[0] for v in lists] + [v[1] for v in lists]).reshape(-1, LANES),
                                  jnp.pad(counts, ((0, 8 - n_layers), (0, LANES - n_exp)))], axis=0)
        dy = pad(d_out)
        u0_y, u0_c, packed, dy = fence((u0_y, u0_c, packed, dy))
        u0_d = move(u0_y, 'core')
        shared = share(packed, N_SRC)
        dy, shared = fence((dy, shared))
        shared_x = move(shared, 'x')
        dy_y, dy_x = move(dy, 'ep'), move(dy, 'x')
        sizes = (n_layers, n_local, n_tok, n // LANES)
        routes = plan(shared, shared, *sizes)
        u0_half = singles(u0, u0_y, u0_c, u0_d)
        part = run_experts(routes, 0, u0_half, None, weights, None, None, True, True, p_f32=True)
        dy_y, dy_x, shared_x, part = fence((dy_y, dy_x, shared_x, part))
        dy_c, dy_d, dy_xy, dy_xc = move(dy, 'core'), move(dy_y, 'core'), move(dy_y, 'x'), move(dy_x, 'core')
        y0, u1_a, u1_b = complete_blocks(part, w_mix[1], True, False, 1)
        dy_c, dy_d, dy_xy, dy_xc, u0_p, u0_q, y0, u1_a, u1_b, shared_x = fence(
            (dy_c, dy_d, dy_xy, dy_xc, u0, u0_y, y0, u1_a, u1_b, shared_x))
        routes_x = plan(shared, shared_x, *sizes)
        dy_xd = move(dy_xy, 'core')
        u1_xa = move(u1_a, 'x')
        out = run_experts(routes, 1, pairs(u1_a, u1_b), singles(dy, dy_y, dy_c, dy_d), weights, None, None, True, True)
        u1_xa, dy_xd, u0_p, u0_q, out = fence((u1_xa, dy_xd, u0_p, u0_q, out))
        y_part, du_part, g1 = out[:4], out[4:8], out[8]
        u1_xb = move(u1_xa, 'core')
        got = send_three(du_part)
        u0_x, u0_xy = move(u0_p, 'x'), move(u0_q, 'x')
        out = run_experts(routes_x, 1, pairs(u1_xa, u1_xb), singles(dy_x, dy_xy, dy_xc, dy_xd), weights, g1, None,
                          False, False)
        got, u0_x, u0_xy, out = fence((got, u0_x, u0_xy, out))
        *finals, sent_a, sent_b = out
        du1, dx_a, dx_b = complete_blocks([du_part[0], *got], w_mix[1], False, True, 2)
        tx = lambda x, du: jnp.einsum('td,te->de', x, du, preferred_element_type=F32)
        g_mix1 = tx(y0[:, :d], du1[:, :d])
        dx_a, y_part, sent_a, sent_b, u0_x, u0_xy, g_mix1 = fence((dx_a, y_part, sent_a, sent_b, u0_x, u0_xy, g_mix1))
        dx_xa = move(dx_a, 'x')
        theirs1 = move(g_mix1, 'core')
        got_y = send_three(y_part)
        u0_xc, u0_xd = move(u0_x, 'core'), move(u0_xy, 'core')
        got1 = [move(sent_a, 'core'), move(sent_b, 'core')]
        out = run_experts(routes, 0, u0_half, pairs(dx_a, dx_b), weights, None, None, False, True)
        dx_xa, got_y, got1, u0_xc, u0_xd, theirs1, out = fence((dx_xa, got_y, got1, u0_xc, u0_xd, theirs1, out))
        du_part, g0 = out[:4], out[4]
        dx_xb = move(dx_xa, 'core')
        got = send_three(du_part)
        part1 = (g_mix1 + theirs1).astype(BF16)
        theirs1 = move(part1, 'ep')
        y1 = own_sum(y_part[0], got_y)
        y1, du_part, dx_xb, part1 = fence((y1, du_part, dx_xb, part1))
        out = run_experts(routes_x, 0, singles(u0_x, u0_xy, u0_xc, u0_xd), pairs(dx_xa, dx_xb), weights, g0, finals,
                          False, False, got=got1)
        got, theirs1, out = fence((got, theirs1, out))
        *finals, sent_a, sent_b = out
        got_a, got_b = move(sent_a, 'core'), move(sent_b, 'core')
        add = lambda a, b: a.astype(F32) + b.astype(F32)
        part1 = add(part1, theirs1).astype(BF16)
        theirs1 = move(part1, 'x')
        du0 = own_sum(du_part[0], got)
        part0 = tx(tokens, du0).astype(BF16)
        theirs0 = move(part0, 'ep')
        dx0 = (du0.astype(F32) + jnp.einsum('te,de->td', du0, w_mix[0], preferred_element_type=F32)).astype(BF16)
        row = lambda a: lax.slice_in_dim(routes[0], ROW_PARTNER * LANES + a, ROW_PARTNER * LANES + a + n_local // 4)
        dx0, got_a, finals = fence((dx0, got_a, finals))
        finals = place(row(0), 0, got_a, finals)
        theirs0, finals = fence((theirs0, finals))
        part0 = add(part0, theirs0).astype(BF16)
        theirs0 = move(part0, 'x')
        part0, got_b = fence((part0, got_b))
        finals = place(row(n_local // 4), 0, got_b, finals)
        theirs0, theirs1, finals = fence((theirs0, theirs1, finals))
        total0 = add(part0, theirs0).astype(BF16)
        g_mix = jnp.stack([add(total0, move(total0, 'core')), add(part1, theirs1)]).astype(BF16)
        return (y1, dx0, g_mix, jnp.swapaxes(finals[0], 2, 3), jnp.swapaxes(finals[1], 2, 3), finals[2])

    return jax.shard_map(device_step, mesh=sub,
                         in_specs=(tok_spec, tok_spec, route_spec, route_spec, whole_spec,
                                   expert_spec, expert_spec, expert_spec),
                         out_specs=(tok_spec, tok_spec, whole_spec, expert_spec, expert_spec, expert_spec),
                         check_vma=False)
```

```python
import functools

import jax
import jax.numpy as jnp
from jax import lax
from jax.experimental import pallas as pl
from jax.experimental.pallas import tpu as pltpu
from jax.sharding import Mesh, PartitionSpec as P

F32, BF16, I32 = jnp.float32, jnp.bfloat16, jnp.int32
MESH = pl.DeviceIdType.MESH
ROWS = 384
GRP = 8
PITCH = 9
DEPTH = 3
FULL = 8
HALF = 4
CAP_FACTOR = 3
LANES = 128
N_SRC = 4
Y, CORE, X = 1, 2, 4
VMEM_LIMIT = 62 * 1024 * 1024
PER_TILE = ROWS // GRP
ROW_BOUND, ROW_GOFF, ROW_EXPERT, ROW_PARTNER, TAB_ROWS = 32, 33, 34, 35, 40
SLOT_GROUPS = 256


def cdiv(a, b):
    return (a + b - 1) // b


def spans(d):
    return [(LANES * j, min(LANES, d - LANES * j)) for j in range(cdiv(d, LANES))]


any_space = pl.BlockSpec(memory_space=pl.ANY)
in_vmem = pl.BlockSpec(memory_space=pltpu.VMEM)


def sorted_list(expert_ids, gate_vals):
    n_tok, top = expert_ids.shape
    n = n_tok * top
    keys = expert_ids.reshape(n) * n + jnp.arange(n, dtype=I32)
    keys, gates = lax.sort((keys, gate_vals.reshape(n)), num_keys=1, is_stable=False)
    return ((keys % n) // top).astype(F32), gates


def plan_kernel(n_layers, n_local, n_tok, list_rows, deal_ref, all_ref, tab_ref, idx_ref, gate_ref):
    n_mine = n_local // 2
    core, ep = lax.axis_index('core'), lax.axis_index('ep')
    list_len = list_rows * LANES
    lane = lambda n: lax.broadcasted_iota(I32, (n, LANES), 1).astype(F32)
    sub = lambda n: lax.broadcasted_iota(I32, (n, LANES), 0).astype(F32)
    over_lanes = lambda v: jnp.sum(v, axis=1, keepdims=True)
    over_subs = lambda v: jnp.sum(v, axis=0, keepdims=True)
    l16, s16 = lane(n_mine), sub(n_mine)
    groups = lambda c: jnp.floor((c + (GRP - 0.5)) * (1.0 / GRP))
    for l in range(n_layers):
        cnt = all_ref[:, 2 * n_layers * list_rows + l, :]
        ends = cnt
        step = 1
        while step < 2 * n_local:
            ends = ends + jnp.where(lane(N_SRC) >= step, pltpu.roll(ends, step, 1), 0.0)
            step *= 2
        starts = ends - cnt
        second = (ep > 0)
        local = lambda v: jnp.where(lane(N_SRC) < n_local, jnp.where(second, pltpu.roll(v, LANES - n_local, 1), v), 0.0)
        cnt, starts = local(cnt), local(starts)
        tiles = jnp.floor((over_subs(groups(local(deal_ref[:, 2 * n_layers * list_rows + l, :]))) + (PER_TILE - 0.5))
                          * (1.0 / PER_TILE))
        load = jnp.where(lane(1) < n_local, jnp.maximum(1.0, tiles), -1.0)
        wide = jnp.broadcast_to(load, (n_local, LANES))
        col = over_lanes(jnp.where(lane(n_local) == sub(n_local), wide, 0.0))
        ahead = (col > wide) | ((col == wide) & (sub(n_local) < lane(n_local)))
        rank = over_subs(jnp.where(ahead, 1.0, 0.0))
        odd = s16 - 2.0 * jnp.floor(s16 * 0.5 + 0.25)
        flip = jnp.where(core > 0, 1.0 - odd, odd)
        dealt = lambda f: (jnp.broadcast_to(rank, (n_mine, LANES)) == 2.0 * s16 + f) & (l16 < n_local)
        pick = dealt(flip)
        choose = lambda p, row: over_lanes(jnp.where(p, jnp.broadcast_to(row, (n_mine, LANES)), 0.0))
        mine = lambda row: choose(pick, row)
        as_row = lambda c: over_subs(jnp.where(l16 == s16, c, 0.0))
        experts = as_row(mine(lane(1)))
        partner = as_row(choose(dealt(1.0 - flip), lane(1)))
        at = l * TAB_ROWS
        off = jnp.zeros((n_mine, 1), F32)
        pos = [jnp.zeros((n_mine, LANES), F32) for _ in range(SLOT_GROUPS // LANES)]
        for s in range(N_SRC):
            c, st = mine(cnt[s:s + 1]), mine(starts[s:s + 1]) + float(s * list_len)
            ng = groups(c)
            for i in range(len(pos)):
                rel = l16 + float(LANES * i) - off
                code = (st + GRP * rel) * 16.0 + jnp.minimum(float(GRP), c - GRP * rel)
                pos[i] = jnp.where((rel >= 0) & (rel < ng), code, pos[i])
            off = off + ng
        for i in range(len(pos)):
            tab_ref[pl.ds(at + i, n_mine, stride=len(pos)), :] = pos[i].astype(I32)
        n_tiles = jnp.maximum(1.0, jnp.floor((off + (PER_TILE - 0.5)) * (1.0 / PER_TILE)))
        bounds = over_subs(jnp.where(s16 < l16, n_tiles, 0.0))
        before = over_lanes(jnp.where(l16 == s16, jnp.broadcast_to(bounds, (n_mine, LANES)), 0.0))
        t = jnp.minimum(l16, over_subs(jnp.broadcast_to(n_tiles, (n_mine, LANES))) - 1.0)
        inside = (t >= before) & (t < before + n_tiles)
        goff = over_subs(jnp.where(inside, s16 * float(SLOT_GROUPS) + (t - before) * float(PER_TILE), 0.0))
        rows = [(ROW_BOUND, bounds), (ROW_GOFF, goff), (ROW_EXPERT, experts), (ROW_PARTNER, partner)]
        for row, value in rows:
            tab_ref[at + row:at + row + 1, :] = value.astype(I32)
    for l in range(n_layers):
        pad = l * (N_SRC * list_rows + 8) + N_SRC * list_rows
        gate_ref[pad:pad + 8, :] = jnp.zeros((8, LANES), F32)
        for s in range(N_SRC):
            to = (l * N_SRC + s) * list_rows
            toks = all_ref[s, l * list_rows:(l + 1) * list_rows, :]
            idx_ref[to:to + list_rows, :] = ((toks + float(s * n_tok)) * float(PITCH)).astype(I32)
            to = l * (N_SRC * list_rows + 8) + s * list_rows
            gate_ref[to:to + list_rows, :] = all_ref[s, (n_layers + l) * list_rows:(n_layers + l + 1) * list_rows, :]


def plan(deal, shared, n_layers, n_local, n_tok, list_rows):
    n_tab = n_layers * TAB_ROWS
    n_list = n_layers * N_SRC * list_rows
    n_gate = n_layers * (N_SRC * list_rows + 8)
    tab, idx, gates = pl.pallas_call(
        functools.partial(plan_kernel, n_layers, n_local, n_tok, list_rows),
        out_shape=[jax.ShapeDtypeStruct((n_tab, LANES), I32), jax.ShapeDtypeStruct((n_list, LANES), I32),
                   jax.ShapeDtypeStruct((n_gate, LANES), F32)],
        in_specs=[in_vmem] * 2, out_specs=[in_vmem] * 3,
        cost_estimate=pl.CostEstimate(flops=10 ** 7, bytes_accessed=10 ** 6, transcendentals=0),
        name="plan",
    )(deal, shared)
    return tab.reshape(-1), idx.reshape(-1), gates


def expert_kernel(cfg, *refs):
    fwd, bwd, own, layer, n_blk, d, ff, n_exp, picks, row_id, list_len, p_f32, n_alias, got_layer = cfg
    refs = list(refs)
    take = lambda n: [refs.pop(0) for _ in range(n)]
    tab_hbm, idx_hbm, gate_hbm = take(3)
    u_pieces = take(N_SRC)
    dy_pieces = take(N_SRC) if bwd else []
    wg_hbm, wu_hbm, wd_hbm = take(3)
    prev = take(1)[0] if bwd and not own else None
    got = take(2) if got_layer is not None else None
    take(n_alias)
    y_outs = take(N_SRC) if fwd else []
    du_outs = take(N_SRC) if bwd and own else []
    grad = take(1)[0] if bwd and own else None
    finals = take(3) if bwd and not own else None
    sent = take(2) if bwd and not own else None
    tab_ref, idx, gate_ref, land, table, gat = take(6)
    acc, row_ref = take(2) if own else (None, None)
    gu_ref, wd_ref, g_ref, x_u = take(4)
    x_c = take(1)[0] if bwd else None
    ab_ref = take(1)[0]
    dh_ref = take(1)[0] if bwd else None
    h_ref = take(1)[0]
    dab_ref, sums = take(2) if bwd else (None, None)
    keep_buf = take(1)[0] if bwd and not own else None
    got_buf = take(1)[0] if got is not None else None
    list_sem, land_sem, w_sem = take(3)
    sum_sem = take(1)[0] if bwd else None
    keep_sem = take(1)[0] if bwd and not own else None
    read_sem, write_sem = take(2) if got is not None else (None, None)
    stage_f, out_sem = take(2) if own else (None, None)

    copy = pltpu.make_async_copy
    cols = spans(d)
    lo = ff // 256 * 256
    hi = ff - lo
    dot = functools.partial(lax.dot_general, preferred_element_type=F32)
    nn = (((1,), (0,)), ((), ()))
    nt = (((1,), (1,)), ((), ()))
    tn = (((0,), (0,)), ((), ()))
    al = pl.multiple_of
    n_row = N_SRC * n_blk
    glane = lax.broadcasted_iota(I32, (GRP, LANES), 1)
    gsub = lax.broadcasted_iota(I32, (GRP, LANES), 0)

    def row_at(r):
        return pl.ds(r * PITCH, FULL)

    def codes_of(tile):
        at = ROW_GOFF * LANES + tile
        if own and bwd:
            return lambda q: tab_ref[tab_ref[at] + q]
        view = tab_ref.at[pl.ds(tab_ref[at], PER_TILE)]
        return lambda q: view[q]

    def gather(codes, q):
        ids = idx.at[pl.ds(codes(q) >> 4, GRP)]
        for k in range(GRP):
            gat[row_at(q * GRP + k), :] = table[pl.ds(ids[k], FULL), :]

    def gate_column(code):
        pos = code >> 4
        row, shift = pos >> 7, pos & (LANES - 1)
        want = glane == gsub + shift
        over = glane == gsub + (shift - LANES)
        here = gate_ref[pl.ds(row, GRP, stride=0), :]
        there = gate_ref[pl.ds(row + 1, GRP, stride=0), :]
        v = jnp.where(want, here, jnp.where(over, there, 0.0))
        return jnp.where(gsub < (code & 15), jnp.sum(v, axis=1, keepdims=True), 0.0)

    def scatter(codes, q):
        ids = idx.at[pl.ds(codes(q) >> 4, GRP)]
        new = []
        for k in range(GRP):
            at = pl.ds(ids[k], FULL)
            new.append((at, acc[at, :] + row_ref[row_at(q * GRP + k), :]))
        for at, value in reversed(new):
            acc[at, :] = value

    def convert(codes):
        for q in range(0, PER_TILE, 2):
            part = []
            for p in (q, q + 1):
                code = codes(p)
                rows = [gat[pl.ds(GRP * PITCH * p + j, GRP, stride=PITCH), :] for j in range(FULL if bwd else HALF)]
                real = gsub < (code & 15)
                gate = gate_column(code)
                g_ref[GRP * p:GRP * (p + 1), :] = gate
                part.append([jnp.where(real, v, 0.0) for v in rows[:HALF]] + [v * gate for v in rows[HALF:]])
            at = slice(GRP * q, GRP * (q + 2))
            for x, o in ((x_u, 0), (x_c, HALF)):
                if x is None:
                    continue
                for j, (c, w) in enumerate(cols):
                    both = jnp.concatenate([part[0][o + j], part[1][o + j]], axis=0)
                    x[at, c:c + w] = both[:, :w].astype(BF16)

    def put_rows(o, value, s0):
        value = value.astype(BF16).astype(F32)
        n = value.shape[0]
        for j, (c, w) in enumerate(cols):
            row_ref[pl.ds(PITCH * s0 + o + j, n, stride=PITCH), 0:w] = value[:, c:c + w] * g_ref[s0:s0 + n, 0:w]

    low = lax.broadcasted_iota(I32, (16, 2 * hi), 1) < hi

    def middle(a, b, dh):
        sig = 0.5 * jnp.tanh(0.5 * a) + 0.5
        act = a * sig
        h = act * b
        if dh is None:
            return h, None, None
        slope = sig * (1.0 + a * (1.0 - sig))
        return h, dh * b * slope, dh * act

    def weights(e, slot):
        at = (layer, tab_ref[ROW_EXPERT * LANES + e])
        moves = []
        for i, w in enumerate((wg_hbm, wu_hbm)):
            moves.append((w.at[at + (pl.ds(0, lo),)], gu_ref.at[slot, pl.ds(i * lo, lo)]))
            moves.append((w.at[at + (pl.ds(lo, hi),)], gu_ref.at[slot, pl.ds(2 * lo + i * hi, hi)]))
        moves.append((wd_hbm.at[at], wd_ref.at[slot]))
        return [copy(a, b, w_sem.at[slot, i]) for i, (a, b) in enumerate(moves)]

    def sums_in(e, slot):
        return copy(prev.at[e], sums.at[slot], sum_sem.at[slot])

    def sums_out(e, slot):
        return copy(sums.at[slot], grad.at[e], sum_sem.at[slot])

    def keeps(e, slot):
        at = (layer, tab_ref[ROW_EXPERT * LANES + e])
        return [copy(keep_buf.at[slot, i], finals[i].at[at], keep_sem.at[slot, i]) for i in range(3)]

    def send(e, slot, part):
        return copy(keep_buf.at[slot], sent[part].at[e - part * (n_exp // 2)], keep_sem.at[slot, 3])

    def read(e, slot, part=0):
        return copy(got[part].at[e - part * (n_exp // 2)], got_buf.at[slot], read_sem.at[slot])

    def writes(e, slot):
        to = tab_ref[TAB_ROWS * LANES + e]
        return [copy(got_buf.at[slot, i], finals[i].at[got_layer, to], write_sem.at[slot, i]) for i in range(3)]

    def start(moves):
        for m in moves:
            m.start()

    def wait(moves):
        for m in moves:
            m.wait()

    n_tab = TAB_ROWS * LANES
    lists = [copy(tab_hbm.at[pl.ds(row_id * n_tab, n_tab)], tab_ref.at[pl.ds(0, n_tab)], list_sem.at[0]),
             copy(idx_hbm.at[pl.ds(row_id * N_SRC * list_len, N_SRC * list_len)], idx.at[pl.ds(0, N_SRC * list_len)],
                  list_sem.at[1]),
             copy(gate_hbm.at[pl.ds(row_id * gate_ref.shape[0], gate_ref.shape[0])], gate_ref, list_sem.at[2])]
    if got is not None:
        at = (got_layer * TAB_ROWS + ROW_PARTNER) * LANES
        lists.append(copy(tab_hbm.at[pl.ds(at, LANES)], tab_ref.at[pl.ds(n_tab, LANES)], list_sem.at[3]))
    start(lists)
    pieces = []
    for s in range(N_SRC):
        pieces.append((u_pieces[s], picks[0][s], s, 0, fwd))
        if bwd:
            pieces.append((dy_pieces[s], picks[1][s], s, HALF, own))
    lands = [copy(ref.at[pick], land.at[i % N_SRC], land_sem.at[i % N_SRC]) for i, (ref, pick, *_) in enumerate(pieces)]
    start(lands[:N_SRC])
    lists[0].wait()
    for e in range(DEPTH - 1):
        start(weights(e, e))
        if bwd and not own:
            sums_in(e, e).start()
    if got is not None:
        lists[3].wait()
        read(0, 0).start()
    if own:
        def clear(c, _):
            for k in range(4):
                acc[pl.ds(al(c * 1152 + 288 * k, 8), 288), :] = jnp.zeros((288, LANES), F32)
            return 0

        lax.fori_loop(0, acc.shape[0] // 1152, clear, 0)
        row_ref[...] = jnp.zeros(row_ref.shape, F32)
    rows = 256
    for i, (_, _, s, o, seed) in enumerate(pieces):
        lands[i].wait()

        def fill(c, _, i=i, o=o, seed=seed, s=s):
            r = al(c * rows, rows)
            for j in range(HALF):
                vals = land[i % N_SRC, pl.ds(r, rows), LANES * j:LANES * (j + 1)].astype(F32)
                to = pl.ds(PITCH * (s * n_blk + r) + o + j, rows, stride=PITCH)
                table[to, :] = vals
                if seed and s == 0:
                    acc[to, :] = vals
            return 0

        lax.fori_loop(0, n_blk // rows, fill, 0)
        if i + N_SRC < len(pieces):
            lands[i + N_SRC].start()
    wait(lists[1:3])
    for k in range(GRP):
        idx[N_SRC * list_len + k] = 0

    def first(q, _):
        gather(begin, 2 * q)
        gather(begin, 2 * q + 1)
        return 0

    begin = codes_of(0)
    lax.fori_loop(0, PER_TILE // 2, first, 0)
    convert(begin)

    def expert(e, _):
        slot = e & 1
        deep = lax.rem(e, DEPTH)
        sum_slot = slot if own else deep
        wait(weights(e, deep))
        if bwd and not own:
            sums_in(e, deep).wait()
        if got is not None:
            read(0, slot).wait()
            start(writes(e, slot))

            @pl.when((e > 0) & (e < n_exp - 1))
            def _():
                wait(writes(e - 1, 1 - slot))

        @pl.when(e < n_exp - (DEPTH - 1))
        def _():
            ahead = lax.rem(e + DEPTH - 1, DEPTH)
            start(weights(e + DEPTH - 1, ahead))
            if bwd and not own:
                sums_in(e + DEPTH - 1, ahead).start()

        @pl.when(e < n_exp - 1)
        def _():
            if got is not None:
                for part in range(2):
                    @pl.when((e + 1 >= n_exp // 2) if part else (e + 1 < n_exp // 2))
                    def _(part=part):
                        read(e + 1, 1 - slot, part).start()

        if bwd and own:
            @pl.when(e > 1)
            def _():
                sums_out(e - 2, slot).wait()

            sums[slot] = jnp.zeros(sums.shape[1:], F32)

        def tile(t, _):
            before, after = codes_of(jnp.maximum(t - 1, 0)), codes_of(t + 1)
            for q in range(PER_TILE):
                if own:
                    scatter(before, q)
                gather(after, q)
            half = ROWS // 2
            for s0 in range(0, ROWS, half):
                sl = slice(s0, s0 + half)
                ab_ref[sl, :] = dot(x_u[sl, :], gu_ref[deep], nt)
                if bwd:
                    dh_ref[sl, :] = dot(x_c[sl, :], wd_ref[deep], nt)
            for r in range(0, ROWS, 16):
                rows = slice(r, r + 16)
                for c in range(0, lo, LANES):
                    h, da, db = middle(ab_ref[rows, c:c + LANES], ab_ref[rows, lo + c:lo + c + LANES],
                                       dh_ref[rows, c:c + LANES] if bwd else None)
                    h_ref[rows, c:c + LANES] = h.astype(BF16)
                    if bwd:
                        dab_ref[rows, c:c + LANES] = da.astype(BF16)
                        dab_ref[rows, lo + c:lo + c + LANES] = db.astype(BF16)
                a = ab_ref[rows, 2 * lo:]
                b = pltpu.roll(a, hi, 1)
                dh = dh_ref[rows, lo:] if bwd else None
                if bwd:
                    dh = jnp.concatenate([dh, dh], axis=1)
                h, da, db = middle(a, b, dh)
                h_ref[rows, lo:] = h[:, :hi].astype(BF16)
                if bwd:
                    dab_ref[rows, 2 * lo:] = jnp.where(low, da, pltpu.roll(db, hi, 1)).astype(BF16)
            for s0 in range(0, ROWS, half):
                sl = slice(s0, s0 + half)
                if fwd:
                    put_rows(0, dot(h_ref[sl, :], wd_ref[deep], nn), s0)
                if bwd and own:
                    put_rows(HALF, dot(dab_ref[sl, :], gu_ref[deep], nn), s0)
            if bwd:
                view = sums.at[sum_slot]
                view[0:2 * ff, :] += dot(dab_ref[...], x_u[...], tn)
                view[2 * ff:, :] += dot(h_ref[...], x_c[...], tn)
            convert(after)
            return 0

        lax.fori_loop(tab_ref[ROW_BOUND * LANES + e], tab_ref[ROW_BOUND * LANES + e + 1], tile, 0)
        if bwd and own:
            sums_out(e, slot).start()
        if bwd and not own:
            @pl.when(e > 1)
            def _():
                wait(keeps(e - 2, slot) + [send(0, slot, 0)])

            for i in range(2):
                keep_buf[slot, i, 0:lo, :] = sums[deep, i * lo:(i + 1) * lo, :].astype(BF16)
                keep_buf[slot, i, lo:, :] = sums[deep, 2 * lo + i * hi:2 * lo + (i + 1) * hi, :].astype(BF16)
            keep_buf[slot, 2] = sums[deep, 2 * ff:, :].astype(BF16)
            start(keeps(e, slot))
            for part in range(2):
                @pl.when((e >= n_exp // 2) if part else (e < n_exp // 2))
                def _(part=part):
                    send(e, slot, part).start()
        return 0

    lax.fori_loop(0, n_exp, expert, 0)
    ends = ((n_exp - 2, (n_exp - 2) % 2), (n_exp - 1, (n_exp - 1) % 2))
    if own:
        end = codes_of(tab_ref[ROW_BOUND * LANES + n_exp] - 1)
        lax.fori_loop(0, PER_TILE, lambda q, _: (scatter(end, q), 0)[1], 0)
        flights = {}
        for o, out in ((HALF, du_outs), (0, y_outs)):
            for s in range(N_SRC if out else 0):
                wide = s == 0 or p_f32
                stage = stage_f.at[s] if wide else land.at[s]
                if s in flights:
                    flights[s].wait()

                def fetch(c, _, stage=stage, s=s, o=o):
                    r = al(c * rows, rows)
                    for j in range(HALF):
                        at = pl.ds(PITCH * (s * n_blk + r) + o + j, rows, stride=PITCH)
                        stage[pl.ds(r, rows), LANES * j:LANES * (j + 1)] = acc[at, :].astype(stage.dtype)
                    return 0

                lax.fori_loop(0, n_blk // rows, fetch, 0)
                flights[s] = copy(stage, out[s], out_sem.at[s])
                flights[s].start()
        wait(flights.values())
        if bwd:
            for e, slot in ends:
                sums_out(e, slot).wait()
    else:
        for e, slot in ends:
            wait(keeps(e, slot) + [send(0, slot, 0)])
            if got is not None:
                wait(writes(e, slot))


def run_experts(routes, layer, u, dy, weights, prev, finals, fwd, own, p_f32=False, got=None):
    tab, idx, gates = routes
    bwd = dy is not None
    wg, wu, wd = weights
    n_blk, wide = u[0][0].shape[-2:]
    n_layers, n_local, ff, d = wd.shape
    n_exp = n_local // 2
    row_id = layer
    list_len = idx.shape[0] // (n_layers * N_SRC)

    arrays = lambda pieces: [v for v, _ in pieces]
    operands = [tab, idx, gates] + arrays(u) + (arrays(dy) if bwd else []) + [wg, wu, wd]
    out_shape, aliases = [], {}
    for use in (fwd, bwd and own):
        if use:
            out_shape += [jax.ShapeDtypeStruct((n_blk, wide), F32 if s == 0 or p_f32 else BF16) for s in range(N_SRC)]
    if bwd and own:
        out_shape.append(jax.ShapeDtypeStruct((n_exp, 3 * ff, d), F32))
    if bwd and not own:
        operands.append(prev)
        if got is not None:
            operands += got
        for i, f in enumerate(finals or ()):
            aliases[len(operands)] = i
            operands.append(f)
        out_shape += [jax.ShapeDtypeStruct((n_layers, n_local, ff, d), BF16)] * 3
        out_shape += [jax.ShapeDtypeStruct((n_exp // 2, 3, ff, d), BF16)] * 2
    sem = lambda *s: pltpu.SemaphoreType.DMA(s)
    mid = lambda n, dt: pltpu.VMEM((ROWS, n), dt)
    table, rows = pltpu.VMEM((PITCH * N_SRC * n_blk, LANES), F32), pltpu.VMEM((PITCH * ROWS, LANES), F32)
    scratch = [pltpu.SMEM(((TAB_ROWS + 1) * LANES,), I32), pltpu.SMEM((N_SRC * list_len + LANES,), I32),
               pltpu.VMEM((N_SRC * list_len // LANES + 8, LANES), F32), pltpu.VMEM((N_SRC, n_blk, wide), BF16)]
    scratch += [table, rows] * (1 + own)
    scratch += [pltpu.VMEM((DEPTH, 2 * ff, d), BF16), pltpu.VMEM((DEPTH, ff, d), BF16), mid(LANES, F32)]
    scratch += [mid(d, BF16)] * (1 + bwd) + [mid(2 * ff, F32)] + [mid(ff, F32)] * bwd + [mid(ff, BF16)]
    scratch += [mid(2 * ff, BF16), pltpu.VMEM((2 if own else DEPTH, 3 * ff, d), F32)] * bwd
    if bwd and not own:
        scratch.append(pltpu.VMEM((2, 3, ff, d), BF16))
    if got is not None:
        scratch.append(pltpu.VMEM((2, 3, ff, d), BF16))
    scratch += [sem(4), sem(N_SRC), sem(DEPTH, 5)] + [sem(DEPTH)] * bwd
    if bwd and not own:
        scratch.append(sem(2, 4))
    if got is not None:
        scratch += [sem(2), sem(2, 3)]
    if own:
        scratch += [pltpu.VMEM((N_SRC if p_f32 else 1, n_blk, wide), F32), sem(N_SRC)]
    passes = 2 + fwd + bwd * (4 + 2 * own)
    flops = 2 * d * ff * passes * n_blk * N_SRC * 2
    hoist = 1400 if not own else 700 if fwd else 800
    picks = [[i for _, i in u], [i for _, i in dy] if bwd else None]
    cfg = (fwd, bwd, own, layer, n_blk, d, ff, n_exp, picks, row_id, list_len, p_f32, len(aliases),
           None if got is None else 1 - layer)
    return pl.pallas_call(
        functools.partial(expert_kernel, cfg),
        out_shape=out_shape,
        in_specs=[any_space] * len(operands),
        out_specs=[any_space] * len(out_shape),
        scratch_shapes=scratch,
        input_output_aliases=aliases,
        compiler_params=pltpu.CompilerParams(
            vmem_limit_bytes=VMEM_LIMIT),
        cost_estimate=pl.CostEstimate(flops=flops, bytes_accessed=3 * 2 * n_exp * d * ff, transcendentals=0),
        name=f"experts_{'f' if fwd else ''}{'b' if bwd else ''}_{'own' if own else 'other'}_{layer}",
    )(*operands)


def place_kernel(layer, n_exp, tab_ref, got_ref, *refs):
    outs, (buf, in_sem, out_sem) = refs[3:6], refs[6:]
    reads = [pltpu.make_async_copy(got_ref.at[i], buf.at[i], in_sem.at[i]) for i in range(n_exp)]
    for read in reads:
        read.start()
    writes = []
    for i, read in enumerate(reads):
        read.wait()
        e = tab_ref[i]
        for k, out in enumerate(outs):
            writes.append(pltpu.make_async_copy(buf.at[i, k], out.at[layer, e], out_sem.at[i, k]))
            writes[-1].start()
    for write in writes:
        write.wait()


def place(partner, layer, got, finals):
    n_exp = got.shape[0]
    return pl.pallas_call(
        functools.partial(place_kernel, layer, n_exp),
        out_shape=[jax.ShapeDtypeStruct(f.shape, f.dtype) for f in finals],
        grid_spec=pltpu.PrefetchScalarGridSpec(
            num_scalar_prefetch=1, grid=(1,), in_specs=[any_space] * 4, out_specs=[any_space] * 3,
            scratch_shapes=[pltpu.VMEM(got.shape, got.dtype), pltpu.SemaphoreType.DMA((n_exp,)),
                            pltpu.SemaphoreType.DMA((n_exp, 3))]),
        input_output_aliases={2: 0, 3: 1, 4: 2},
        compiler_params=pltpu.CompilerParams(vmem_limit_bytes=VMEM_LIMIT),
        cost_estimate=pl.CostEstimate(flops=0, bytes_accessed=4 * got.size, transcendentals=0),
        name=f"place_{layer}",
    )(partner, got, *finals)


def peer(rel):
    return {name: (lax.axis_index(name) + ((rel >> bit) & 1)) % 2 for bit, name in enumerate(("ep", "core", "x"))}


def meet(rels):
    barrier = pltpu.get_barrier_semaphore()
    for rel in rels:
        pl.semaphore_signal(barrier, inc=1, device_id=peer(rel), device_id_type=MESH)
    pl.semaphore_wait(barrier, len(rels))


def remote(src, dst, send, recv, rel):
    return pltpu.make_async_remote_copy(src_ref=src, dst_ref=dst, send_sem=send, recv_sem=recv,
                                        device_id=peer(rel), device_id_type=MESH)


def share_kernel(n_rel, mine_ref, all_ref, send_sem, recv_sem):
    meet(range(1, n_rel))
    copies = [remote(mine_ref, all_ref.at[rel], send_sem.at[rel], recv_sem.at[rel], rel) for rel in range(1, n_rel)]
    for copy in copies:
        copy.start()
    all_ref[0] = mine_ref[...]
    for copy in copies:
        copy.wait()


def share(mine, n_rel):
    return pl.pallas_call(
        functools.partial(share_kernel, n_rel),
        out_shape=jax.ShapeDtypeStruct((n_rel,) + mine.shape, mine.dtype),
        in_specs=[in_vmem],
        out_specs=in_vmem,
        scratch_shapes=[pltpu.SemaphoreType.DMA((n_rel,)), pltpu.SemaphoreType.DMA((n_rel,))],
        compiler_params=pltpu.CompilerParams(collective_id=0, has_side_effects=True),
        cost_estimate=pl.CostEstimate(flops=10 ** 7, bytes_accessed=mine.size * 4 * n_rel, transcendentals=0),
        name="share_lists",
    )(mine)


def blocks_kernel(cfg, *refs):
    n_chunk, reduce, back, d = cfg
    refs = list(refs)
    take = lambda n: [refs.pop(0) for _ in range(n)]
    parts = take(N_SRC)
    m_ref, o_total, o_a, o_b = take(4)
    in_f, in_b, got_f, s_wire, r_wire, u_wire, y_wire, t_buf, u_buf, y_buf, load, send, recv, put = take(14)
    n_rows = t_buf.shape[0] // n_chunk
    cut = [pl.ds(k * n_rows, n_rows) for k in range(n_chunk)]
    thin = [pl.ds(k * n_rows // 2, n_rows // 2) for k in range(n_chunk)]
    side = lax.broadcasted_iota(I32, (n_rows // 2, LANES), 1) < LANES // 2
    tiles = d // LANES
    turn = lambda v: pltpu.roll(v, LANES // 2, 1)
    lanes = lambda v, j: v[:, LANES * j:LANES * (j + 1)]

    def pack(wire, k, value):
        top, low = value[:n_rows // 2], value[n_rows // 2:]
        turned = [turn(lanes(low, j)) for j in range(tiles + 1)]
        parts = [lanes(top, j) for j in range(tiles)] + [jnp.where(side, lanes(top, tiles), turned[0])]
        parts += [jnp.where(side, turned[j], turned[j + 1]) for j in range(tiles)]
        for j, part in enumerate(parts):
            wire[thin[k], LANES * j:LANES * (j + 1)] = part.astype(BF16)

    def unpack(wire, k):
        value = wire[thin[k], :].astype(F32)
        turned = [turn(lanes(value, tiles + j)) for j in range(tiles + 1)]
        top = [lanes(value, j) for j in range(tiles)] + [jnp.where(side, lanes(value, tiles), 0.0)]
        low = [jnp.where(side, turned[j], turned[j + 1]) for j in range(tiles)] + [jnp.where(side, turned[tiles], 0.0)]
        return jnp.concatenate([jnp.concatenate(top, axis=1), jnp.concatenate(low, axis=1)], axis=0)

    chunks = range(n_chunk)
    loads = {}
    for i, part in enumerate(parts[:2] if reduce else parts):
        buf = in_f.at[i] if reduce or i == 0 else in_b.at[i - 1]
        for k in chunks:
            loads[i, k] = pltpu.make_async_copy(part.at[cut[k]], buf.at[cut[k]], load.at[i, k])
    order = (1, 0) if reduce else range(N_SRC)
    for i in order:
        for k in chunks:
            loads[i, k].start()
    u_buf[...] = jnp.zeros(u_buf.shape, BF16)
    meet((Y, CORE))
    links = []
    copy_in = pltpu.make_async_copy

    def link(src, dst, rel, cut=cut):
        n = len(links)
        links.append([remote(src.at[cut[k]], dst.at[cut[k]], send.at[n, k], recv.at[n, k], rel) for k in chunks])
        return links[-1]

    if reduce:
        first = link(parts[3], got_f.at[1], CORE)
        second = link(parts[2], got_f.at[0], CORE)
        over = link(s_wire, r_wire, Y, thin)
        for copies in (first, second):
            for copy in copies:
                copy.start()
        for k in chunks:
            loads[1, k].wait()
            first[k].wait_recv()
            pack(s_wire, k, in_f[1, cut[k], :] + got_f[1, cut[k], :])
            over[k].start()
    to_y = link(u_wire, y_wire, Y, thin)
    to_core = link(u_buf, o_b.at[0], CORE)
    puts = []
    for k in chunks:
        if reduce:
            loads[0, k].wait()
            second[k].wait_recv()
            over[k].wait_recv()
            total = in_f[0, cut[k], :] + got_f[0, cut[k], :] + unpack(r_wire, k)
        else:
            for i in range(N_SRC):
                loads[i, k].wait()
            total = in_f[0, cut[k], :]
            for i in range(N_SRC - 1):
                total = total + in_b[i, cut[k], :].astype(F32)
        total = total.astype(BF16)
        t_buf[cut[k], :] = total
        dims = (((1,), (1 if back else 0,)), ((), ()))
        mixed = lax.dot_general(total[:, :d], m_ref[...], dims, preferred_element_type=F32)
        u_buf[cut[k], 0:d] = (total[:, :d].astype(F32) + mixed).astype(BF16)
        pack(u_wire, k, u_buf[cut[k], :].astype(F32))
        to_y[k].start()
        to_core[k].start()
        puts.append(pltpu.make_async_copy(u_buf.at[cut[k]], o_a.at[0, cut[k]], put.at[0, k]))
        puts.append(pltpu.make_async_copy(t_buf.at[cut[k]], o_total.at[cut[k]], put.at[1, k]))
        for copy in puts[-2:]:
            copy.start()
    on = link(y_buf, o_b.at[1], CORE)
    for k in chunks:
        to_y[k].wait_recv()
        y_buf[cut[k], :] = unpack(y_wire, k).astype(BF16)
        on[k].start()
        puts.append(copy_in(y_buf.at[cut[k]], o_a.at[1, cut[k]], put.at[2, k]))
        puts[-1].start()
    waited = [to_y] + ([first, second, over] if reduce else [])
    for copies in links:
        for copy in copies:
            if any(copies is w for w in waited):
                copy.wait_send()
            else:
                copy.wait()
    for copy in puts:
        copy.wait()


def complete_blocks(parts, m, reduce, back, ident, n_chunk=4):
    n_blk, wide = parts[0].shape
    d = m.shape[0]
    sem = lambda *s: pltpu.SemaphoreType.DMA(s)
    pair = jax.ShapeDtypeStruct((2, n_blk, wide), BF16)
    buf = lambda n, dt: pltpu.VMEM((n, n_blk, wide) if n else (n_blk, wide), dt)
    return pl.pallas_call(
        functools.partial(blocks_kernel, (n_chunk, reduce, back, d)),
        out_shape=[jax.ShapeDtypeStruct((n_blk, wide), BF16)] + [pair] * 2,
        in_specs=[any_space] * N_SRC + [in_vmem],
        out_specs=[any_space] * 3,
        scratch_shapes=[buf(2, F32), buf(3, BF16), buf(2, F32)] + [pltpu.VMEM((n_blk // 2, 2 * d), BF16)] * 4 + [
            buf(0, BF16), buf(0, BF16), buf(0, BF16), sem(4, n_chunk), sem(6, n_chunk), sem(6, n_chunk), sem(3, n_chunk)],
        compiler_params=pltpu.CompilerParams(collective_id=ident, has_side_effects=True, vmem_limit_bytes=VMEM_LIMIT),
        cost_estimate=pl.CostEstimate(flops=10 ** 8, bytes_accessed=n_blk * wide * 40, transcendentals=0),
        name=f"complete_blocks_{ident}",
    )(*parts, m)


def solution(mesh):
    ep_size, dp_size = mesh.shape['ep'], mesh.shape['dp']
    sub = Mesh(mesh.devices.reshape(ep_size, dp_size // 2, 2), ('ep', 'x', 'core'))
    tok_axes = ('x', 'core', 'ep')
    tok_spec = P(tok_axes, None)
    route_spec = P(None, tok_axes, None)
    whole_spec = P(None, None, None)
    expert_spec = P(None, 'ep', None, None)
    flip = [(0, 1), (1, 0)]
    move = lambda v, axis: lax.ppermute(v, axis, flip)
    move_diag = lambda v: lax.ppermute(v, ('ep', 'core'), [(0, 3), (1, 2), (2, 1), (3, 0)])
    fence = lax.optimization_barrier

    def device_step(tokens, d_out, expert_ids, gate_vals, w_mix, w_gate, w_up, w_down):
        n_layers, d = w_mix.shape[0], w_mix.shape[1]
        n_tok = tokens.shape[0]
        top = expert_ids.shape[2]
        n_local = w_gate.shape[1]
        n_exp = n_local * ep_size
        n = n_tok * top
        n_rel = 2 * N_SRC
        wide = cdiv(d, LANES) * LANES
        weights = (jnp.swapaxes(w_gate, 2, 3), jnp.swapaxes(w_up, 2, 3), w_down)
        pad = lambda v: jnp.pad(v, ((0, 0), (0, wide - d)))
        send_three = lambda p: [move(p[1], 'ep'), move(p[2], 'core'), move_diag(p[3])]

        def own_sum(p, got):
            return sum([g.astype(F32) for g in got], p)[:, :d].astype(BF16)

        one = lambda v: v.reshape(1, n_tok, wide)
        pairs = lambda a, b: [(a, 0), (a, 1), (b, 0), (b, 1)]

        one = lambda v: v.reshape(1, n_tok, wide)
        pairs = lambda a, b: [(a, 0), (a, 1), (b, 0), (b, 1)]
        singles = lambda *v: [(one(a), 0) for a in v]

        u0 = pad((tokens.astype(F32) + jnp.dot(tokens, w_mix[0], preferred_element_type=F32)).astype(BF16))
        u0_y, u0_c = move(u0, 'ep'), move(u0, 'core')
        lists = [sorted_list(expert_ids[l], gate_vals[l]) for l in range(n_layers)]
        counts = jnp.sum((expert_ids.reshape(n_layers, n, 1) == jnp.arange(n_exp, dtype=I32)).astype(F32), axis=1)
        packed = jnp.concatenate([jnp.concatenate([v[0] for v in lists] + [v[1] for v in lists]).reshape(-1, LANES),
                                  jnp.pad(counts, ((0, 8 - n_layers), (0, LANES - n_exp)))], axis=0)
        dy = pad(d_out)
        u0_y, u0_c, packed, dy = fence((u0_y, u0_c, packed, dy))
        u0_d = move(u0_y, 'core')
        shared = share(packed, N_SRC)
        dy, shared = fence((dy, shared))
        shared_x = move(shared, 'x')
        dy_y, dy_x = move(dy, 'ep'), move(dy, 'x')
        sizes = (n_layers, n_local, n_tok, n // LANES)
        routes = plan(shared, shared, *sizes)
        u0_half = singles(u0, u0_y, u0_c, u0_d)
        part = run_experts(routes, 0, u0_half, None, weights, None, None, True, True, p_f32=True)
        dy_y, dy_x, shared_x, part = fence((dy_y, dy_x, shared_x, part))
        dy_c, dy_d, dy_xy, dy_xc = move(dy, 'core'), move(dy_y, 'core'), move(dy_y, 'x'), move(dy_x, 'core')
        y0, u1_a, u1_b = complete_blocks(part, w_mix[1], True, False, 1)
        dy_c, dy_d, dy_xy, dy_xc, u0_p, u0_q, y0, u1_a, u1_b, shared_x = fence(
            (dy_c, dy_d, dy_xy, dy_xc, u0, u0_y, y0, u1_a, u1_b, shared_x))
        routes_x = plan(shared, shared_x, *sizes)
        dy_xd = move(dy_xy, 'core')
        u1_xa = move(u1_a, 'x')
        out = run_experts(routes, 1, pairs(u1_a, u1_b), singles(dy, dy_y, dy_c, dy_d), weights, None, None, True, True)
        u1_xa, dy_xd, u0_p, u0_q, out = fence((u1_xa, dy_xd, u0_p, u0_q, out))
        y_part, du_part, g1 = out[:4], out[4:8], out[8]
        u1_xb = move(u1_xa, 'core')
        got = send_three(du_part)
        u0_x, u0_xy = move(u0_p, 'x'), move(u0_q, 'x')
        out = run_experts(routes_x, 1, pairs(u1_xa, u1_xb), singles(dy_x, dy_xy, dy_xc, dy_xd), weights, g1, None,
                          False, False)
        got, u0_x, u0_xy, out = fence((got, u0_x, u0_xy, out))
        *finals, sent_a, sent_b = out
        du1, dx_a, dx_b = complete_blocks([du_part[0], *got], w_mix[1], False, True, 2)
        tx = lambda x, du: jnp.einsum('td,te->de', x, du, preferred_element_type=F32)
        g_mix1 = tx(y0[:, :d], du1[:, :d])
        dx_a, y_part, sent_a, sent_b, u0_x, u0_xy, g_mix1 = fence((dx_a, y_part, sent_a, sent_b, u0_x, u0_xy, g_mix1))
        dx_xa = move(dx_a, 'x')
        theirs1 = move(g_mix1, 'core')
        got_y = send_three(y_part)
        u0_xc, u0_xd = move(u0_x, 'core'), move(u0_xy, 'core')
        got1 = [move(sent_a, 'core'), move(sent_b, 'core')]
        out = run_experts(routes, 0, u0_half, pairs(dx_a, dx_b), weights, None, None, False, True)
        dx_xa, got_y, got1, u0_xc, u0_xd, theirs1, out = fence((dx_xa, got_y, got1, u0_xc, u0_xd, theirs1, out))
        du_part, g0 = out[:4], out[4]
        dx_xb = move(dx_xa, 'core')
        got = send_three(du_part)
        part1 = (g_mix1 + theirs1).astype(BF16)
        theirs1 = move(part1, 'ep')
        du_part, dx_xb, part1 = fence((du_part, dx_xb, part1))
        out = run_experts(routes_x, 0, singles(u0_x, u0_xy, u0_xc, u0_xd), pairs(dx_xa, dx_xb), weights, g0, finals,
                          False, False, got=got1)
        got, theirs1, got_y, y_own, out = fence((got, theirs1, got_y, y_part[0], out))
        *finals, sent_a, sent_b = out
        got_a, got_b = move(sent_a, 'core'), move(sent_b, 'core')
        add = lambda a, b: a.astype(F32) + b.astype(F32)
        part1 = add(part1, theirs1).astype(BF16)
        theirs1 = move(part1, 'x')
        du0 = own_sum(du_part[0], got)
        part0 = tx(tokens, du0).astype(BF16)
        theirs0 = move(part0, 'ep')
        dx0 = (du0.astype(F32) + jnp.einsum('te,de->td', du0, w_mix[0], preferred_element_type=F32)).astype(BF16)
        row = lambda a: lax.slice_in_dim(routes[0], ROW_PARTNER * LANES + a, ROW_PARTNER * LANES + a + n_local // 4)
        y1 = own_sum(y_own, got_y).T
        dx0, y1, got_a, finals = fence((dx0, y1, got_a, finals))
        finals = place(row(0), 0, got_a, finals)
        theirs0, finals = fence((theirs0, finals))
        part0 = add(part0, theirs0).astype(BF16)
        theirs0 = move(part0, 'x')
        part0, dx0, got_b = fence((part0, dx0.T, got_b))
        finals = place(row(n_local // 4), 0, got_b, finals)
        theirs0, theirs1, finals = fence((theirs0, theirs1, finals))
        total0 = add(part0, theirs0).astype(BF16)
        g_mix = jnp.stack([add(total0, move(total0, 'core')), add(part1, theirs1)]).astype(BF16)
        return (y1.T, dx0.T, g_mix, jnp.swapaxes(finals[0], 2, 3), jnp.swapaxes(finals[1], 2, 3), finals[2])

    return jax.shard_map(device_step, mesh=sub,
                         in_specs=(tok_spec, tok_spec, route_spec, route_spec, whole_spec,
                                   expert_spec, expert_spec, expert_spec),
                         out_specs=(tok_spec, tok_spec, whole_spec, expert_spec, expert_spec, expert_spec),
                         check_vma=False)
```

```python
import functools

import jax
import jax.numpy as jnp
from jax import lax
from jax.experimental import pallas as pl
from jax.experimental.pallas import tpu as pltpu
from jax.sharding import Mesh, PartitionSpec as P

F32, BF16, I32 = jnp.float32, jnp.bfloat16, jnp.int32
MESH = pl.DeviceIdType.MESH
ROWS = 384
GRP = 8
PITCH = 9
DEPTH = 3
FULL = 8
HALF = 4
CAP_FACTOR = 3
LANES = 128
N_SRC = 4
Y, CORE, X = 1, 2, 4
VMEM_LIMIT = 62 * 1024 * 1024
PER_TILE = ROWS // GRP
ROW_BOUND, ROW_GOFF, ROW_EXPERT, ROW_PARTNER, TAB_ROWS = 32, 33, 34, 35, 40
SLOT_GROUPS = 256


def cdiv(a, b):
    return (a + b - 1) // b


def spans(d):
    return [(LANES * j, min(LANES, d - LANES * j)) for j in range(cdiv(d, LANES))]


any_space = pl.BlockSpec(memory_space=pl.ANY)
in_vmem = pl.BlockSpec(memory_space=pltpu.VMEM)


def sorted_list(expert_ids, gate_vals):
    n_tok, top = expert_ids.shape
    n = n_tok * top
    keys = expert_ids.reshape(n) * n + jnp.arange(n, dtype=I32)
    keys, gates = lax.sort((keys, gate_vals.reshape(n)), num_keys=1, is_stable=False)
    return ((keys % n) // top).astype(F32), gates


def plan_kernel(n_layers, n_local, n_tok, list_rows, deal_ref, all_ref, tab_ref, idx_ref, gate_ref):
    n_mine = n_local // 2
    core, ep = lax.axis_index('core'), lax.axis_index('ep')
    list_len = list_rows * LANES
    lane = lambda n: lax.broadcasted_iota(I32, (n, LANES), 1).astype(F32)
    sub = lambda n: lax.broadcasted_iota(I32, (n, LANES), 0).astype(F32)
    over_lanes = lambda v: jnp.sum(v, axis=1, keepdims=True)
    over_subs = lambda v: jnp.sum(v, axis=0, keepdims=True)
    l16, s16 = lane(n_mine), sub(n_mine)
    groups = lambda c: jnp.floor((c + (GRP - 0.5)) * (1.0 / GRP))
    for l in range(n_layers):
        cnt = all_ref[:, 2 * n_layers * list_rows + l, :]
        ends = cnt
        step = 1
        while step < 2 * n_local:
            ends = ends + jnp.where(lane(N_SRC) >= step, pltpu.roll(ends, step, 1), 0.0)
            step *= 2
        starts = ends - cnt
        second = (ep > 0)
        local = lambda v: jnp.where(lane(N_SRC) < n_local, jnp.where(second, pltpu.roll(v, LANES - n_local, 1), v), 0.0)
        cnt, starts = local(cnt), local(starts)
        tiles = jnp.floor((over_subs(groups(local(deal_ref[:, 2 * n_layers * list_rows + l, :]))) + (PER_TILE - 0.5))
                          * (1.0 / PER_TILE))
        load = jnp.where(lane(1) < n_local, jnp.maximum(1.0, tiles), -1.0)
        wide = jnp.broadcast_to(load, (n_local, LANES))
        col = over_lanes(jnp.where(lane(n_local) == sub(n_local), wide, 0.0))
        ahead = (col > wide) | ((col == wide) & (sub(n_local) < lane(n_local)))
        rank = over_subs(jnp.where(ahead, 1.0, 0.0))
        odd = s16 - 2.0 * jnp.floor(s16 * 0.5 + 0.25)
        flip = jnp.where(core > 0, 1.0 - odd, odd)
        dealt = lambda f: (jnp.broadcast_to(rank, (n_mine, LANES)) == 2.0 * s16 + f) & (l16 < n_local)
        pick = dealt(flip)
        choose = lambda p, row: over_lanes(jnp.where(p, jnp.broadcast_to(row, (n_mine, LANES)), 0.0))
        mine = lambda row: choose(pick, row)
        as_row = lambda c: over_subs(jnp.where(l16 == s16, c, 0.0))
        experts = as_row(mine(lane(1)))
        partner = as_row(choose(dealt(1.0 - flip), lane(1)))
        at = l * TAB_ROWS
        off = jnp.zeros((n_mine, 1), F32)
        pos = [jnp.zeros((n_mine, LANES), F32) for _ in range(SLOT_GROUPS // LANES)]
        for s in range(N_SRC):
            c, st = mine(cnt[s:s + 1]), mine(starts[s:s + 1]) + float(s * list_len)
            ng = groups(c)
            for i in range(len(pos)):
                rel = l16 + float(LANES * i) - off
                code = (st + GRP * rel) * 16.0 + jnp.minimum(float(GRP), c - GRP * rel)
                pos[i] = jnp.where((rel >= 0) & (rel < ng), code, pos[i])
            off = off + ng
        for i in range(len(pos)):
            tab_ref[pl.ds(at + i, n_mine, stride=len(pos)), :] = pos[i].astype(I32)
        n_tiles = jnp.maximum(1.0, jnp.floor((off + (PER_TILE - 0.5)) * (1.0 / PER_TILE)))
        bounds = over_subs(jnp.where(s16 < l16, n_tiles, 0.0))
        before = over_lanes(jnp.where(l16 == s16, jnp.broadcast_to(bounds, (n_mine, LANES)), 0.0))
        t = jnp.minimum(l16, over_subs(jnp.broadcast_to(n_tiles, (n_mine, LANES))) - 1.0)
        inside = (t >= before) & (t < before + n_tiles)
        goff = over_subs(jnp.where(inside, s16 * float(SLOT_GROUPS) + (t - before) * float(PER_TILE), 0.0))
        rows = [(ROW_BOUND, bounds), (ROW_GOFF, goff), (ROW_EXPERT, experts), (ROW_PARTNER, partner)]
        for row, value in rows:
            tab_ref[at + row:at + row + 1, :] = value.astype(I32)
    for l in range(n_layers):
        pad = l * (N_SRC * list_rows + 8) + N_SRC * list_rows
        gate_ref[pad:pad + 8, :] = jnp.zeros((8, LANES), F32)
        for s in range(N_SRC):
            to = (l * N_SRC + s) * list_rows
            toks = all_ref[s, l * list_rows:(l + 1) * list_rows, :]
            idx_ref[to:to + list_rows, :] = ((toks + float(s * n_tok)) * float(PITCH)).astype(I32)
            to = l * (N_SRC * list_rows + 8) + s * list_rows
            gate_ref[to:to + list_rows, :] = all_ref[s, (n_layers + l) * list_rows:(n_layers + l + 1) * list_rows, :]


def plan_shapes(sizes):
    n_layers, _, _, list_rows = sizes
    rows = (n_layers * TAB_ROWS, n_layers * N_SRC * list_rows, n_layers * (N_SRC * list_rows + 8))
    return [jax.ShapeDtypeStruct((n, LANES), dt) for n, dt in zip(rows, (I32, I32, F32))]


def flat(tab, idx, gates):
    return tab.reshape(-1), idx.reshape(-1), gates


def plan(deal, shared, sizes):
    return flat(*pl.pallas_call(
        functools.partial(plan_kernel, *sizes),
        out_shape=plan_shapes(sizes),
        in_specs=[in_vmem] * 2, out_specs=[in_vmem] * 3,
        cost_estimate=pl.CostEstimate(flops=10 ** 7, bytes_accessed=10 ** 6, transcendentals=0),
        name="plan",
    )(deal, shared))


def expert_kernel(cfg, *refs):
    fwd, bwd, own, layer, n_blk, d, ff, n_exp, picks, row_id, list_len, p_f32, n_alias, got_layer = cfg
    refs = list(refs)
    take = lambda n: [refs.pop(0) for _ in range(n)]
    tab_hbm, idx_hbm, gate_hbm = take(3)
    u_pieces = take(N_SRC)
    dy_pieces = take(N_SRC) if bwd else []
    wg_hbm, wu_hbm, wd_hbm = take(3)
    prev = take(1)[0] if bwd and not own else None
    got = take(2) if got_layer is not None else None
    take(n_alias)
    y_outs = take(N_SRC) if fwd else []
    du_outs = take(N_SRC) if bwd and own else []
    grad = take(1)[0] if bwd and own else None
    finals = take(3) if bwd and not own or got_layer is not None else None
    sent = take(2) if bwd and not own else None
    tab_ref, idx, gate_ref, land, table, gat = take(6)
    acc, row_ref = take(2) if own else (None, None)
    gu_ref, wd_ref, g_ref, x_u = take(4)
    x_c = take(1)[0] if bwd else None
    ab_ref = take(1)[0]
    dh_ref = take(1)[0] if bwd else None
    h_ref = take(1)[0]
    dab_ref, sums = take(2) if bwd else (None, None)
    keep_buf = take(1)[0] if bwd and not own else None
    got_buf = take(1)[0] if got is not None else None
    list_sem, land_sem, w_sem = take(3)
    sum_sem = take(1)[0] if bwd else None
    keep_sem = take(1)[0] if bwd and not own else None
    read_sem, write_sem = take(2) if got is not None else (None, None)
    stage_f, out_sem = take(2) if own else (None, None)

    copy = pltpu.make_async_copy
    cols = spans(d)
    lo = ff // 256 * 256
    hi = ff - lo
    dot = functools.partial(lax.dot_general, preferred_element_type=F32)
    nn = (((1,), (0,)), ((), ()))
    nt = (((1,), (1,)), ((), ()))
    tn = (((0,), (0,)), ((), ()))
    al = pl.multiple_of
    n_row = N_SRC * n_blk
    glane = lax.broadcasted_iota(I32, (GRP, LANES), 1)
    gsub = lax.broadcasted_iota(I32, (GRP, LANES), 0)

    def row_at(r):
        return pl.ds(r * PITCH, FULL)

    def codes_of(tile):
        at = ROW_GOFF * LANES + tile
        if own and bwd:
            return lambda q: tab_ref[tab_ref[at] + q]
        view = tab_ref.at[pl.ds(tab_ref[at], PER_TILE)]
        return lambda q: view[q]

    def gather(codes, q):
        ids = idx.at[pl.ds(codes(q) >> 4, GRP)]
        for k in range(GRP):
            gat[row_at(q * GRP + k), :] = table[pl.ds(ids[k], FULL), :]

    def gate_column(code):
        pos = code >> 4
        row, shift = pos >> 7, pos & (LANES - 1)
        want = glane == gsub + shift
        over = glane == gsub + (shift - LANES)
        here = gate_ref[pl.ds(row, GRP, stride=0), :]
        there = gate_ref[pl.ds(row + 1, GRP, stride=0), :]
        v = jnp.where(want, here, jnp.where(over, there, 0.0))
        return jnp.where(gsub < (code & 15), jnp.sum(v, axis=1, keepdims=True), 0.0)

    def scatter(codes, q):
        ids = idx.at[pl.ds(codes(q) >> 4, GRP)]
        new = []
        for k in range(GRP):
            at = pl.ds(ids[k], FULL)
            new.append((at, acc[at, :] + row_ref[row_at(q * GRP + k), :]))
        for at, value in reversed(new):
            acc[at, :] = value

    def convert(codes):
        for q in range(0, PER_TILE, 2):
            part = []
            for p in (q, q + 1):
                code = codes(p)
                rows = [gat[pl.ds(GRP * PITCH * p + j, GRP, stride=PITCH), :] for j in range(FULL if bwd else HALF)]
                real = gsub < (code & 15)
                gate = gate_column(code)
                g_ref[GRP * p:GRP * (p + 1), :] = gate
                part.append([jnp.where(real, v, 0.0) for v in rows[:HALF]] + [v * gate for v in rows[HALF:]])
            at = slice(GRP * q, GRP * (q + 2))
            for x, o in ((x_u, 0), (x_c, HALF)):
                if x is None:
                    continue
                for j, (c, w) in enumerate(cols):
                    both = jnp.concatenate([part[0][o + j], part[1][o + j]], axis=0)
                    x[at, c:c + w] = both[:, :w].astype(BF16)

    def put_rows(o, value, s0):
        value = value.astype(BF16).astype(F32)
        n = value.shape[0]
        for j, (c, w) in enumerate(cols):
            row_ref[pl.ds(PITCH * s0 + o + j, n, stride=PITCH), 0:w] = value[:, c:c + w] * g_ref[s0:s0 + n, 0:w]

    low = lax.broadcasted_iota(I32, (16, 2 * hi), 1) < hi

    def middle(a, b, dh):
        sig = 0.5 * jnp.tanh(0.5 * a) + 0.5
        act = a * sig
        h = act * b
        if dh is None:
            return h, None, None
        slope = sig * (1.0 + a * (1.0 - sig))
        return h, dh * b * slope, dh * act

    def weights(e, slot):
        at = (layer, tab_ref[ROW_EXPERT * LANES + e])
        moves = []
        for i, w in enumerate((wg_hbm, wu_hbm)):
            moves.append((w.at[at + (pl.ds(0, lo),)], gu_ref.at[slot, pl.ds(i * lo, lo)]))
            moves.append((w.at[at + (pl.ds(lo, hi),)], gu_ref.at[slot, pl.ds(2 * lo + i * hi, hi)]))
        moves.append((wd_hbm.at[at], wd_ref.at[slot]))
        return [copy(a, b, w_sem.at[slot, i]) for i, (a, b) in enumerate(moves)]

    def sums_in(e, slot):
        return copy(prev.at[e], sums.at[slot], sum_sem.at[slot])

    def sums_out(e, slot):
        return copy(sums.at[slot], grad.at[e], sum_sem.at[slot])

    def keeps(e, slot):
        at = (layer, tab_ref[ROW_EXPERT * LANES + e])
        return [copy(keep_buf.at[slot, i], finals[i].at[at], keep_sem.at[slot, i]) for i in range(3)]

    def send(e, slot, part):
        return copy(keep_buf.at[slot], sent[part].at[e - part * (n_exp // 2)], keep_sem.at[slot, 3])

    def read(e, slot, part=0):
        return copy(got[part].at[e - part * (n_exp // 2)], got_buf.at[slot], read_sem.at[slot])

    def writes(e, slot):
        to = tab_ref[TAB_ROWS * LANES + e]
        return [copy(got_buf.at[slot, i], finals[i].at[got_layer, to], write_sem.at[slot, i]) for i in range(3)]

    def start(moves):
        for m in moves:
            m.start()

    def wait(moves):
        for m in moves:
            m.wait()

    n_tab = TAB_ROWS * LANES
    lists = [copy(tab_hbm.at[pl.ds(row_id * n_tab, n_tab)], tab_ref.at[pl.ds(0, n_tab)], list_sem.at[0]),
             copy(idx_hbm.at[pl.ds(row_id * N_SRC * list_len, N_SRC * list_len)], idx.at[pl.ds(0, N_SRC * list_len)],
                  list_sem.at[1]),
             copy(gate_hbm.at[pl.ds(row_id * gate_ref.shape[0], gate_ref.shape[0])], gate_ref, list_sem.at[2])]
    if got is not None:
        at = (got_layer * TAB_ROWS + ROW_PARTNER) * LANES
        lists.append(copy(tab_hbm.at[pl.ds(at, LANES)], tab_ref.at[pl.ds(n_tab, LANES)], list_sem.at[3]))
    start(lists)
    pieces = []
    for s in range(N_SRC):
        pieces.append((u_pieces[s], picks[0][s], s, 0, fwd))
        if bwd:
            pieces.append((dy_pieces[s], picks[1][s], s, HALF, own))
    lands = [copy(ref.at[pick], land.at[i % N_SRC], land_sem.at[i % N_SRC]) for i, (ref, pick, *_) in enumerate(pieces)]
    start(lands[:N_SRC])
    lists[0].wait()
    for e in range(DEPTH - 1):
        start(weights(e, e))
        if bwd and not own:
            sums_in(e, e).start()
    if got is not None:
        lists[3].wait()
        read(0, 0).start()
    if own:
        def clear(c, _):
            for k in range(4):
                acc[pl.ds(al(c * 1152 + 288 * k, 8), 288), :] = jnp.zeros((288, LANES), F32)
            return 0

        lax.fori_loop(0, acc.shape[0] // 1152, clear, 0)
        row_ref[...] = jnp.zeros(row_ref.shape, F32)
    rows = 256
    for i, (_, _, s, o, seed) in enumerate(pieces):
        lands[i].wait()

        def fill(c, _, i=i, o=o, seed=seed, s=s):
            r = al(c * rows, rows)
            for j in range(HALF):
                vals = land[i % N_SRC, pl.ds(r, rows), LANES * j:LANES * (j + 1)].astype(F32)
                to = pl.ds(PITCH * (s * n_blk + r) + o + j, rows, stride=PITCH)
                table[to, :] = vals
                if seed and s == 0:
                    acc[to, :] = vals
            return 0

        lax.fori_loop(0, n_blk // rows, fill, 0)
        if i + N_SRC < len(pieces):
            lands[i + N_SRC].start()
    wait(lists[1:3])
    for k in range(GRP):
        idx[N_SRC * list_len + k] = 0

    def first(q, _):
        gather(begin, 2 * q)
        gather(begin, 2 * q + 1)
        return 0

    begin = codes_of(0)
    lax.fori_loop(0, PER_TILE // 2, first, 0)
    convert(begin)

    def expert(e, _):
        slot = e & 1
        deep = lax.rem(e, DEPTH)
        sum_slot = slot if own else deep
        wait(weights(e, deep))
        if bwd and not own:
            sums_in(e, deep).wait()
        if got is not None:
            read(0, slot).wait()
            start(writes(e, slot))

            @pl.when((e > 0) & (e < n_exp - 1))
            def _():
                wait(writes(e - 1, 1 - slot))

        @pl.when(e < n_exp - (DEPTH - 1))
        def _():
            ahead = lax.rem(e + DEPTH - 1, DEPTH)
            start(weights(e + DEPTH - 1, ahead))
            if bwd and not own:
                sums_in(e + DEPTH - 1, ahead).start()

        @pl.when(e < n_exp - 1)
        def _():
            if got is not None:
                for part in range(2):
                    @pl.when((e + 1 >= n_exp // 2) if part else (e + 1 < n_exp // 2))
                    def _(part=part):
                        read(e + 1, 1 - slot, part).start()

        if bwd and own:
            @pl.when(e > 1)
            def _():
                sums_out(e - 2, slot).wait()

            sums[slot] = jnp.zeros(sums.shape[1:], F32)

        def tile(t, _):
            before, after = codes_of(jnp.maximum(t - 1, 0)), codes_of(t + 1)
            for q in range(PER_TILE):
                if own:
                    scatter(before, q)
                gather(after, q)
            half = ROWS // 2
            for s0 in range(0, ROWS, half):
                sl = slice(s0, s0 + half)
                ab_ref[sl, :] = dot(x_u[sl, :], gu_ref[deep], nt)
                if bwd:
                    dh_ref[sl, :] = dot(x_c[sl, :], wd_ref[deep], nt)
            for r in range(0, ROWS, 16):
                rows = slice(r, r + 16)
                for c in range(0, lo, LANES):
                    h, da, db = middle(ab_ref[rows, c:c + LANES], ab_ref[rows, lo + c:lo + c + LANES],
                                       dh_ref[rows, c:c + LANES] if bwd else None)
                    h_ref[rows, c:c + LANES] = h.astype(BF16)
                    if bwd:
                        dab_ref[rows, c:c + LANES] = da.astype(BF16)
                        dab_ref[rows, lo + c:lo + c + LANES] = db.astype(BF16)
                a = ab_ref[rows, 2 * lo:]
                b = pltpu.roll(a, hi, 1)
                dh = dh_ref[rows, lo:] if bwd else None
                if bwd:
                    dh = jnp.concatenate([dh, dh], axis=1)
                h, da, db = middle(a, b, dh)
                h_ref[rows, lo:] = h[:, :hi].astype(BF16)
                if bwd:
                    dab_ref[rows, 2 * lo:] = jnp.where(low, da, pltpu.roll(db, hi, 1)).astype(BF16)
            for s0 in range(0, ROWS, half):
                sl = slice(s0, s0 + half)
                if fwd:
                    put_rows(0, dot(h_ref[sl, :], wd_ref[deep], nn), s0)
                if bwd and own:
                    put_rows(HALF, dot(dab_ref[sl, :], gu_ref[deep], nn), s0)
            if bwd:
                view = sums.at[sum_slot]
                view[0:2 * ff, :] += dot(dab_ref[...], x_u[...], tn)
                view[2 * ff:, :] += dot(h_ref[...], x_c[...], tn)
            convert(after)
            return 0

        lax.fori_loop(tab_ref[ROW_BOUND * LANES + e], tab_ref[ROW_BOUND * LANES + e + 1], tile, 0)
        if bwd and own:
            sums_out(e, slot).start()
        if bwd and not own:
            @pl.when(e > 1)
            def _():
                wait(keeps(e - 2, slot) + [send(0, slot, 0)])

            for i in range(2):
                keep_buf[slot, i, 0:lo, :] = sums[deep, i * lo:(i + 1) * lo, :].astype(BF16)
                keep_buf[slot, i, lo:, :] = sums[deep, 2 * lo + i * hi:2 * lo + (i + 1) * hi, :].astype(BF16)
            keep_buf[slot, 2] = sums[deep, 2 * ff:, :].astype(BF16)
            start(keeps(e, slot))
            for part in range(2):
                @pl.when((e >= n_exp // 2) if part else (e < n_exp // 2))
                def _(part=part):
                    send(e, slot, part).start()
        return 0

    lax.fori_loop(0, n_exp, expert, 0)
    ends = ((n_exp - 2, (n_exp - 2) % 2), (n_exp - 1, (n_exp - 1) % 2))
    if own:
        end = codes_of(tab_ref[ROW_BOUND * LANES + n_exp] - 1)
        lax.fori_loop(0, PER_TILE, lambda q, _: (scatter(end, q), 0)[1], 0)
        flights = {}
        for o, out in ((HALF, du_outs), (0, y_outs)):
            for s in range(N_SRC if out else 0):
                wide = s == 0 or p_f32
                stage = stage_f.at[s] if wide else land.at[s]
                if s in flights:
                    flights[s].wait()

                def fetch(c, _, stage=stage, s=s, o=o):
                    r = al(c * rows, rows)
                    for j in range(HALF):
                        at = pl.ds(PITCH * (s * n_blk + r) + o + j, rows, stride=PITCH)
                        stage[pl.ds(r, rows), LANES * j:LANES * (j + 1)] = acc[at, :].astype(stage.dtype)
                    return 0

                lax.fori_loop(0, n_blk // rows, fetch, 0)
                flights[s] = copy(stage, out[s], out_sem.at[s])
                flights[s].start()
        wait(flights.values())
        if bwd:
            for e, slot in ends:
                sums_out(e, slot).wait()
    else:
        for e, slot in ends:
            wait(keeps(e, slot) + [send(0, slot, 0)])
    if got is not None:
        for e, slot in ends:
            wait(writes(e, slot))


def run_experts(routes, layer, u, dy, weights, prev, finals, fwd, own, p_f32=False, got=None):
    tab, idx, gates = routes
    bwd = dy is not None
    wg, wu, wd = weights
    n_blk, wide = u[0][0].shape[-2:]
    n_layers, n_local, ff, d = wd.shape
    n_exp = n_local // 2
    row_id = layer
    list_len = idx.shape[0] // (n_layers * N_SRC)

    arrays = lambda pieces: [v for v, _ in pieces]
    operands = [tab, idx, gates] + arrays(u) + (arrays(dy) if bwd else []) + [wg, wu, wd]
    out_shape, aliases = [], {}
    for use in (fwd, bwd and own):
        if use:
            out_shape += [jax.ShapeDtypeStruct((n_blk, wide), F32 if s == 0 or p_f32 else BF16) for s in range(N_SRC)]
    if bwd and own:
        out_shape.append(jax.ShapeDtypeStruct((n_exp, 3 * ff, d), F32))
    if bwd and not own:
        operands.append(prev)
    if got is not None:
        operands += got
    for i, f in enumerate(finals or ()):
        aliases[len(operands)] = len(out_shape) + i
        operands.append(f)
    if bwd and not own or finals:
        out_shape += [jax.ShapeDtypeStruct((n_layers, n_local, ff, d), BF16)] * 3
    if bwd and not own:
        out_shape += [jax.ShapeDtypeStruct((n_exp // 2, 3, ff, d), BF16)] * 2
    sem = lambda *s: pltpu.SemaphoreType.DMA(s)
    mid = lambda n, dt: pltpu.VMEM((ROWS, n), dt)
    table, rows = pltpu.VMEM((PITCH * N_SRC * n_blk, LANES), F32), pltpu.VMEM((PITCH * ROWS, LANES), F32)
    scratch = [pltpu.SMEM(((TAB_ROWS + 1) * LANES,), I32), pltpu.SMEM((N_SRC * list_len + LANES,), I32),
               pltpu.VMEM((N_SRC * list_len // LANES + 8, LANES), F32), pltpu.VMEM((N_SRC, n_blk, wide), BF16)]
    scratch += [table, rows] * (1 + own)
    scratch += [pltpu.VMEM((DEPTH, 2 * ff, d), BF16), pltpu.VMEM((DEPTH, ff, d), BF16), mid(LANES, F32)]
    scratch += [mid(d, BF16)] * (1 + bwd) + [mid(2 * ff, F32)] + [mid(ff, F32)] * bwd + [mid(ff, BF16)]
    scratch += [mid(2 * ff, BF16), pltpu.VMEM((2 if own else DEPTH, 3 * ff, d), F32)] * bwd
    if bwd and not own:
        scratch.append(pltpu.VMEM((2, 3, ff, d), BF16))
    if got is not None:
        scratch.append(pltpu.VMEM((2, 3, ff, d), BF16))
    scratch += [sem(4), sem(N_SRC), sem(DEPTH, 5)] + [sem(DEPTH)] * bwd
    if bwd and not own:
        scratch.append(sem(2, 4))
    if got is not None:
        scratch += [sem(2), sem(2, 3)]
    if own:
        scratch += [pltpu.VMEM((N_SRC if p_f32 else 1, n_blk, wide), F32), sem(N_SRC)]
    passes = 2 + fwd + bwd * (4 + 2 * own)
    flops = 2 * d * ff * passes * n_blk * N_SRC * 2
    hoist = 1400 if not own else 700 if fwd else 800
    picks = [[i for _, i in u], [i for _, i in dy] if bwd else None]
    cfg = (fwd, bwd, own, layer, n_blk, d, ff, n_exp, picks, row_id, list_len, p_f32, len(aliases),
           None if got is None else 1 - layer)
    return pl.pallas_call(
        functools.partial(expert_kernel, cfg),
        out_shape=out_shape,
        in_specs=[any_space] * len(operands),
        out_specs=[any_space] * len(out_shape),
        scratch_shapes=scratch,
        input_output_aliases=aliases,
        compiler_params=pltpu.CompilerParams(
            vmem_limit_bytes=VMEM_LIMIT),
        cost_estimate=pl.CostEstimate(flops=flops, bytes_accessed=3 * 2 * n_exp * d * ff, transcendentals=0),
        name=f"experts_{'f' if fwd else ''}{'b' if bwd else ''}_{'own' if own else 'other'}_{layer}",
    )(*operands)


def place_kernel(layer, n_exp, tab_ref, got_ref, *refs):
    outs, (buf, in_sem, out_sem) = refs[3:6], refs[6:]
    reads = [pltpu.make_async_copy(got_ref.at[i], buf.at[i], in_sem.at[i]) for i in range(n_exp)]
    for read in reads:
        read.start()
    writes = []
    for i, read in enumerate(reads):
        read.wait()
        e = tab_ref[i]
        for k, out in enumerate(outs):
            writes.append(pltpu.make_async_copy(buf.at[i, k], out.at[layer, e], out_sem.at[i, k]))
            writes[-1].start()
    for write in writes:
        write.wait()


def place(partner, layer, got, finals):
    n_exp = got.shape[0]
    return pl.pallas_call(
        functools.partial(place_kernel, layer, n_exp),
        out_shape=[jax.ShapeDtypeStruct(f.shape, f.dtype) for f in finals],
        grid_spec=pltpu.PrefetchScalarGridSpec(
            num_scalar_prefetch=1, grid=(1,), in_specs=[any_space] * 4, out_specs=[any_space] * 3,
            scratch_shapes=[pltpu.VMEM(got.shape, got.dtype), pltpu.SemaphoreType.DMA((n_exp,)),
                            pltpu.SemaphoreType.DMA((n_exp, 3))]),
        input_output_aliases={2: 0, 3: 1, 4: 2},
        compiler_params=pltpu.CompilerParams(vmem_limit_bytes=VMEM_LIMIT),
        cost_estimate=pl.CostEstimate(flops=0, bytes_accessed=4 * got.size, transcendentals=0),
        name=f"place_{layer}",
    )(partner, got, *finals)


def peer(rel):
    return {name: (lax.axis_index(name) + ((rel >> bit) & 1)) % 2 for bit, name in enumerate(("ep", "core", "x"))}


def meet(rels):
    barrier = pltpu.get_barrier_semaphore()
    for rel in rels:
        pl.semaphore_signal(barrier, inc=1, device_id=peer(rel), device_id_type=MESH)
    pl.semaphore_wait(barrier, len(rels))


def remote(src, dst, send, recv, rel):
    return pltpu.make_async_remote_copy(src_ref=src, dst_ref=dst, send_sem=send, recv_sem=recv,
                                        device_id=peer(rel), device_id_type=MESH)


def share_kernel(n_rel, mine_ref, all_ref, send_sem, recv_sem):
    meet(range(1, n_rel))
    copies = [remote(mine_ref, all_ref.at[rel], send_sem.at[rel], recv_sem.at[rel], rel) for rel in range(1, n_rel)]
    for copy in copies:
        copy.start()
    all_ref[0] = mine_ref[...]
    for copy in copies:
        copy.wait()


def share(mine, n_rel):
    return pl.pallas_call(
        functools.partial(share_kernel, n_rel),
        out_shape=jax.ShapeDtypeStruct((n_rel,) + mine.shape, mine.dtype),
        in_specs=[in_vmem],
        out_specs=in_vmem,
        scratch_shapes=[pltpu.SemaphoreType.DMA((n_rel,)), pltpu.SemaphoreType.DMA((n_rel,))],
        compiler_params=pltpu.CompilerParams(collective_id=0, has_side_effects=True),
        cost_estimate=pl.CostEstimate(flops=10 ** 7, bytes_accessed=mine.size * 4 * n_rel, transcendentals=0),
        name="share_lists",
    )(mine)


def blocks_kernel(cfg, *refs):
    n_chunk, reduce, back, d, sizes = cfg
    refs = list(refs)
    take = lambda n: [refs.pop(0) for _ in range(n)]
    parts = take(N_SRC)
    m_ref = take(1)[0]
    list_refs, left_ref = take(2) if sizes else (), take(1)[0] if back else None
    o_total, o_a, o_b = take(3)
    plan_refs, grad_ref = take(3) if sizes else (), take(1)[0] if back else None
    in_f, in_b, got_f, s_wire, r_wire, u_wire, y_wire, t_buf, u_buf, y_buf, load, send, recv, put = take(14)
    n_rows = t_buf.shape[0] // n_chunk
    cut = [pl.ds(k * n_rows, n_rows) for k in range(n_chunk)]
    thin = [pl.ds(k * n_rows // 2, n_rows // 2) for k in range(n_chunk)]
    side = lax.broadcasted_iota(I32, (n_rows // 2, LANES), 1) < LANES // 2
    tiles = d // LANES
    turn = lambda v: pltpu.roll(v, LANES // 2, 1)
    lanes = lambda v, j: v[:, LANES * j:LANES * (j + 1)]

    def pack(wire, k, value):
        top, low = value[:n_rows // 2], value[n_rows // 2:]
        turned = [turn(lanes(low, j)) for j in range(tiles + 1)]
        parts = [lanes(top, j) for j in range(tiles)] + [jnp.where(side, lanes(top, tiles), turned[0])]
        parts += [jnp.where(side, turned[j], turned[j + 1]) for j in range(tiles)]
        for j, part in enumerate(parts):
            wire[thin[k], LANES * j:LANES * (j + 1)] = part.astype(BF16)

    def unpack(wire, k):
        value = wire[thin[k], :].astype(F32)
        turned = [turn(lanes(value, tiles + j)) for j in range(tiles + 1)]
        top = [lanes(value, j) for j in range(tiles)] + [jnp.where(side, lanes(value, tiles), 0.0)]
        low = [jnp.where(side, turned[j], turned[j + 1]) for j in range(tiles)] + [jnp.where(side, turned[tiles], 0.0)]
        return jnp.concatenate([jnp.concatenate(top, axis=1), jnp.concatenate(low, axis=1)], axis=0)

    chunks = range(n_chunk)
    loads = {}
    for i, part in enumerate(parts[:2] if reduce else parts):
        buf = in_f.at[i] if reduce or i == 0 else in_b.at[i - 1]
        for k in chunks:
            loads[i, k] = pltpu.make_async_copy(part.at[cut[k]], buf.at[cut[k]], load.at[i, k])
    order = (1, 0) if reduce else range(N_SRC)
    for i in order:
        for k in chunks:
            loads[i, k].start()
    u_buf[...] = jnp.zeros(u_buf.shape, BF16)
    meet((Y, CORE))
    links = []
    copy_in = pltpu.make_async_copy

    def link(src, dst, rel, cut=cut):
        n = len(links)
        links.append([remote(src.at[cut[k]], dst.at[cut[k]], send.at[n, k], recv.at[n, k], rel) for k in chunks])
        return links[-1]

    if reduce:
        first = link(parts[3], got_f.at[1], CORE)
        second = link(parts[2], got_f.at[0], CORE)
        over = link(s_wire, r_wire, Y, thin)
        for copies in (first, second):
            for copy in copies:
                copy.start()
        for k in chunks:
            loads[1, k].wait()
            first[k].wait_recv()
            pack(s_wire, k, in_f[1, cut[k], :] + got_f[1, cut[k], :])
            over[k].start()
    to_y = link(u_wire, y_wire, Y, thin)
    to_core = link(u_buf, o_b.at[0], CORE)
    puts = []
    for k in chunks:
        if reduce:
            loads[0, k].wait()
            second[k].wait_recv()
            over[k].wait_recv()
            total = in_f[0, cut[k], :] + got_f[0, cut[k], :] + unpack(r_wire, k)
        else:
            for i in range(N_SRC):
                loads[i, k].wait()
            total = in_f[0, cut[k], :]
            for i in range(N_SRC - 1):
                total = total + in_b[i, cut[k], :].astype(F32)
        total = total.astype(BF16)
        t_buf[cut[k], :] = total
        dims = (((1,), (1 if back else 0,)), ((), ()))
        mixed = lax.dot_general(total[:, :d], m_ref[...], dims, preferred_element_type=F32)
        u_buf[cut[k], 0:d] = (total[:, :d].astype(F32) + mixed).astype(BF16)
        pack(u_wire, k, u_buf[cut[k], :].astype(F32))
        to_y[k].start()
        to_core[k].start()
        puts.append(pltpu.make_async_copy(u_buf.at[cut[k]], o_a.at[0, cut[k]], put.at[0, k]))
        puts.append(pltpu.make_async_copy(t_buf.at[cut[k]], o_total.at[cut[k]], put.at[1, k]))
        for copy in puts[-2:]:
            copy.start()
    if sizes:
        plan_kernel(*sizes, *list_refs, *plan_refs)
    if back:
        grad_ref[...] = lax.dot_general(left_ref[:, :d], t_buf[:, :d], (((0,), (0,)), ((), ())), preferred_element_type=F32)
    on = link(y_buf, o_b.at[1], CORE)
    for k in chunks:
        to_y[k].wait_recv()
        y_buf[cut[k], :] = unpack(y_wire, k).astype(BF16)
        on[k].start()
        puts.append(copy_in(y_buf.at[cut[k]], o_a.at[1, cut[k]], put.at[2, k]))
        puts[-1].start()
    waited = [to_y] + ([first, second, over] if reduce else [])
    for copies in links:
        for copy in copies:
            if any(copies is w for w in waited):
                copy.wait_send()
            else:
                copy.wait()
    for copy in puts:
        copy.wait()


def complete_blocks(parts, m, reduce, back, ident, sizes=None, lists=(), left=(), n_chunk=8):
    n_blk, wide = parts[0].shape
    d = m.shape[0]
    sem = lambda *s: pltpu.SemaphoreType.DMA(s)
    pair = jax.ShapeDtypeStruct((2, n_blk, wide), BF16)
    extra = plan_shapes(sizes) if sizes else []
    extra += [jax.ShapeDtypeStruct((d, d), F32)] * len(left)
    buf = lambda n, dt: pltpu.VMEM((n, n_blk, wide) if n else (n_blk, wide), dt)
    return pl.pallas_call(
        functools.partial(blocks_kernel, (n_chunk, reduce, back, d, sizes)),
        out_shape=[jax.ShapeDtypeStruct((n_blk, wide), BF16)] + [pair] * 2 + extra,
        in_specs=[any_space] * N_SRC + [in_vmem] * (1 + len(lists) + len(left)),
        out_specs=[any_space] * 3 + [in_vmem] * len(extra),
        scratch_shapes=[buf(2, F32), buf(3, BF16), buf(2, F32)] + [pltpu.VMEM((n_blk // 2, 2 * d), BF16)] * 4 + [
            buf(0, BF16), buf(0, BF16), buf(0, BF16), sem(4, n_chunk), sem(6, n_chunk), sem(6, n_chunk), sem(3, n_chunk)],
        compiler_params=pltpu.CompilerParams(collective_id=ident, has_side_effects=True, vmem_limit_bytes=VMEM_LIMIT),
        cost_estimate=pl.CostEstimate(flops=10 ** 8, bytes_accessed=n_blk * wide * 40, transcendentals=0),
        name=f"complete_blocks_{ident}",
    )(*parts, m, *lists, *left)


def solution(mesh):
    ep_size, dp_size = mesh.shape['ep'], mesh.shape['dp']
    sub = Mesh(mesh.devices.reshape(ep_size, dp_size // 2, 2), ('ep', 'x', 'core'))
    tok_axes = ('x', 'core', 'ep')
    tok_spec = P(tok_axes, None)
    route_spec = P(None, tok_axes, None)
    whole_spec = P(None, None, None)
    expert_spec = P(None, 'ep', None, None)
    flip = [(0, 1), (1, 0)]
    move = lambda v, axis: lax.ppermute(v, axis, flip)
    move_diag = lambda v: lax.ppermute(v, ('ep', 'core'), [(0, 3), (1, 2), (2, 1), (3, 0)])
    fence = lax.optimization_barrier

    def device_step(tokens, d_out, expert_ids, gate_vals, w_mix, w_gate, w_up, w_down):
        n_layers, d = w_mix.shape[0], w_mix.shape[1]
        n_tok = tokens.shape[0]
        top = expert_ids.shape[2]
        n_local = w_gate.shape[1]
        n_exp = n_local * ep_size
        n = n_tok * top
        n_rel = 2 * N_SRC
        wide = cdiv(d, LANES) * LANES
        weights = (jnp.swapaxes(w_gate, 2, 3), jnp.swapaxes(w_up, 2, 3), w_down)
        pad = lambda v: jnp.pad(v, ((0, 0), (0, wide - d)))
        send_three = lambda p: [move(p[1], 'ep'), move(p[2], 'core'), move_diag(p[3])]

        def own_sum(p, got):
            return sum([g.astype(F32) for g in got], p)[:, :d].astype(BF16)

        one = lambda v: v.reshape(1, n_tok, wide)
        pairs = lambda a, b: [(a, 0), (a, 1), (b, 0), (b, 1)]

        one = lambda v: v.reshape(1, n_tok, wide)
        pairs = lambda a, b: [(a, 0), (a, 1), (b, 0), (b, 1)]
        singles = lambda *v: [(one(a), 0) for a in v]

        u0 = pad((tokens.astype(F32) + jnp.dot(tokens, w_mix[0], preferred_element_type=F32)).astype(BF16))
        u0_y, u0_c = move(u0, 'ep'), move(u0, 'core')
        lists = [sorted_list(expert_ids[l], gate_vals[l]) for l in range(n_layers)]
        counts = jnp.sum((expert_ids.reshape(n_layers, n, 1) == jnp.arange(n_exp, dtype=I32)).astype(F32), axis=1)
        packed = jnp.concatenate([jnp.concatenate([v[0] for v in lists] + [v[1] for v in lists]).reshape(-1, LANES),
                                  jnp.pad(counts, ((0, 8 - n_layers), (0, LANES - n_exp)))], axis=0)
        dy = pad(d_out)
        u0_y, u0_c, packed, dy = fence((u0_y, u0_c, packed, dy))
        u0_d = move(u0_y, 'core')
        shared = share(packed, N_SRC)
        dy, shared = fence((dy, shared))
        shared_x = move(shared, 'x')
        dy_y, dy_x = move(dy, 'ep'), move(dy, 'x')
        sizes = (n_layers, n_local, n_tok, n // LANES)
        routes = plan(shared, shared, sizes)
        u0_half = singles(u0, u0_y, u0_c, u0_d)
        part = run_experts(routes, 0, u0_half, None, weights, None, None, True, True, p_f32=True)
        dy_y, dy_x, shared_x, part = fence((dy_y, dy_x, shared_x, part))
        dy_c, dy_d, dy_xy, dy_xc = move(dy, 'core'), move(dy_y, 'core'), move(dy_y, 'x'), move(dy_x, 'core')
        y0, u1_a, u1_b, *routes_x = complete_blocks(part, w_mix[1], True, False, 1, sizes, (shared, shared_x))
        routes_x = flat(*routes_x)
        dy_c, dy_d, dy_xy, dy_xc, u0_p, u0_q, y0, u1_a, u1_b = fence(
            (dy_c, dy_d, dy_xy, dy_xc, u0, u0_y, y0, u1_a, u1_b))
        dy_xd = move(dy_xy, 'core')
        u1_xa = move(u1_a, 'x')
        out = run_experts(routes, 1, pairs(u1_a, u1_b), singles(dy, dy_y, dy_c, dy_d), weights, None, None, True, True)
        u1_xa, dy_xd, u0_p, u0_q, out = fence((u1_xa, dy_xd, u0_p, u0_q, out))
        y_part, du_part, g1 = out[:4], out[4:8], out[8]
        u1_xb = move(u1_xa, 'core')
        got = send_three(du_part)
        u0_x, u0_xy = move(u0_p, 'x'), move(u0_q, 'x')
        out = run_experts(routes_x, 1, pairs(u1_xa, u1_xb), singles(dy_x, dy_xy, dy_xc, dy_xd), weights, g1, None,
                          False, False)
        got, u0_x, u0_xy, out = fence((got, u0_x, u0_xy, out))
        *finals, sent_a, sent_b = out
        got1 = [move(sent_a, 'core'), move(sent_b, 'core')]
        du1, dx_a, dx_b, g_mix1 = complete_blocks([du_part[0], *got], w_mix[1], False, True, 2, left=(y0,))
        tx = lambda x, du: jnp.einsum('td,te->de', x, du, preferred_element_type=F32)
        dx_a, y_part, got1, u0_x, u0_xy, g_mix1 = fence((dx_a, y_part, got1, u0_x, u0_xy, g_mix1))
        dx_xa = move(dx_a, 'x')
        theirs1 = move(g_mix1, 'core')
        got_y = send_three(y_part)
        u0_xc, u0_xd = move(u0_x, 'core'), move(u0_xy, 'core')
        out = run_experts(routes, 0, u0_half, pairs(dx_a, dx_b), weights, None, finals, False, True, got=got1)
        dx_xa, got_y, u0_xc, u0_xd, theirs1, out = fence((dx_xa, got_y, u0_xc, u0_xd, theirs1, out))
        du_part, g0, finals = out[:4], out[4], out[5:]
        dx_xb = move(dx_xa, 'core')
        got = send_three(du_part)
        part1 = (g_mix1 + theirs1).astype(BF16)
        theirs1 = move(part1, 'ep')
        du_part, dx_xb, part1 = fence((du_part, dx_xb, part1))
        out = run_experts(routes_x, 0, singles(u0_x, u0_xy, u0_xc, u0_xd), pairs(dx_xa, dx_xb), weights, g0, finals,
                          False, False)
        got, theirs1, got_y, y_own, out = fence((got, theirs1, got_y, y_part[0], out))
        *finals, sent_a, sent_b = out
        got_a, got_b = move(sent_a, 'core'), move(sent_b, 'core')
        add = lambda a, b: a.astype(F32) + b.astype(F32)
        part1 = add(part1, theirs1).astype(BF16)
        theirs1 = move(part1, 'x')
        du0 = own_sum(du_part[0], got)
        part0 = tx(tokens, du0).astype(BF16)
        theirs0 = move(part0, 'ep')
        dx0 = (du0.astype(F32) + jnp.einsum('te,de->td', du0, w_mix[0], preferred_element_type=F32)).astype(BF16)
        row = lambda a: lax.slice_in_dim(routes[0], ROW_PARTNER * LANES + a, ROW_PARTNER * LANES + a + n_local // 4)
        y1 = own_sum(y_own, got_y).T
        dx0, y1, got_a, finals = fence((dx0, y1, got_a, finals))
        finals = place(row(0), 0, got_a, finals)
        theirs0, finals = fence((theirs0, finals))
        part0 = add(part0, theirs0).astype(BF16)
        theirs0 = move(part0, 'x')
        part0, dx0, got_b = fence((part0, dx0.T, got_b))
        finals = place(row(n_local // 4), 0, got_b, finals)
        theirs0, theirs1, finals = fence((theirs0, theirs1, finals))
        total0 = add(part0, theirs0).astype(BF16)
        g_mix = jnp.stack([add(total0, move(total0, 'core')), add(part1, theirs1)]).astype(BF16)
        return (y1.T, dx0.T, g_mix, jnp.swapaxes(finals[0], 2, 3), jnp.swapaxes(finals[1], 2, 3), finals[2])

    return jax.shard_map(device_step, mesh=sub,
                         in_specs=(tok_spec, tok_spec, route_spec, route_spec, whole_spec,
                                   expert_spec, expert_spec, expert_spec),
                         out_specs=(tok_spec, tok_spec, whole_spec, expert_spec, expert_spec, expert_spec),
                         check_vma=False)
```

```python
import functools

import jax
import jax.numpy as jnp
from jax import lax
from jax.experimental import pallas as pl
from jax.experimental.pallas import tpu as pltpu
from jax.sharding import Mesh, PartitionSpec as P

F32, BF16, I32 = jnp.float32, jnp.bfloat16, jnp.int32
MESH = pl.DeviceIdType.MESH
ROWS = 384
GRP = 8
PITCH = 9
DEPTH = 3
FULL = 8
HALF = 4
CAP_FACTOR = 3
LANES = 128
N_SRC = 4
Y, CORE, X = 1, 2, 4
VMEM_LIMIT = 62 * 1024 * 1024
PER_TILE = ROWS // GRP
ROW_BOUND, ROW_GOFF, ROW_EXPERT, ROW_PARTNER, TAB_ROWS = 32, 33, 34, 35, 40
SLOT_GROUPS = 256


def cdiv(a, b):
    return (a + b - 1) // b


def spans(d):
    return [(LANES * j, min(LANES, d - LANES * j)) for j in range(cdiv(d, LANES))]


any_space = pl.BlockSpec(memory_space=pl.ANY)
in_vmem = pl.BlockSpec(memory_space=pltpu.VMEM)


def sorted_list(expert_ids, gate_vals):
    n_tok, top = expert_ids.shape
    n = n_tok * top
    keys = expert_ids.reshape(n) * n + jnp.arange(n, dtype=I32)
    keys, gates = lax.sort((keys, gate_vals.reshape(n)), num_keys=1, is_stable=False)
    return ((keys % n) // top).astype(F32), gates


def plan_kernel(n_layers, n_local, n_tok, list_rows, deal_ref, all_ref, tab_ref, idx_ref, gate_ref):
    n_mine = n_local // 2
    core, ep = lax.axis_index('core'), lax.axis_index('ep')
    list_len = list_rows * LANES
    lane = lambda n: lax.broadcasted_iota(I32, (n, LANES), 1).astype(F32)
    sub = lambda n: lax.broadcasted_iota(I32, (n, LANES), 0).astype(F32)
    over_lanes = lambda v: jnp.sum(v, axis=1, keepdims=True)
    over_subs = lambda v: jnp.sum(v, axis=0, keepdims=True)
    l16, s16 = lane(n_mine), sub(n_mine)
    groups = lambda c: jnp.floor((c + (GRP - 0.5)) * (1.0 / GRP))
    for l in range(n_layers):
        cnt = all_ref[:, 2 * n_layers * list_rows + l, :]
        ends = cnt
        step = 1
        while step < 2 * n_local:
            ends = ends + jnp.where(lane(N_SRC) >= step, pltpu.roll(ends, step, 1), 0.0)
            step *= 2
        starts = ends - cnt
        second = (ep > 0)
        local = lambda v: jnp.where(lane(N_SRC) < n_local, jnp.where(second, pltpu.roll(v, LANES - n_local, 1), v), 0.0)
        cnt, starts = local(cnt), local(starts)
        tiles = jnp.floor((over_subs(groups(local(deal_ref[:, 2 * n_layers * list_rows + l, :]))) + (PER_TILE - 0.5))
                          * (1.0 / PER_TILE))
        load = jnp.where(lane(1) < n_local, jnp.maximum(1.0, tiles), -1.0)
        wide = jnp.broadcast_to(load, (n_local, LANES))
        col = over_lanes(jnp.where(lane(n_local) == sub(n_local), wide, 0.0))
        ahead = (col > wide) | ((col == wide) & (sub(n_local) < lane(n_local)))
        rank = over_subs(jnp.where(ahead, 1.0, 0.0))
        odd = s16 - 2.0 * jnp.floor(s16 * 0.5 + 0.25)
        flip = jnp.where(core > 0, 1.0 - odd, odd)
        dealt = lambda f: (jnp.broadcast_to(rank, (n_mine, LANES)) == 2.0 * s16 + f) & (l16 < n_local)
        pick = dealt(flip)
        choose = lambda p, row: over_lanes(jnp.where(p, jnp.broadcast_to(row, (n_mine, LANES)), 0.0))
        mine = lambda row: choose(pick, row)
        as_row = lambda c: over_subs(jnp.where(l16 == s16, c, 0.0))
        experts = as_row(mine(lane(1)))
        partner = as_row(choose(dealt(1.0 - flip), lane(1)))
        at = l * TAB_ROWS
        off = jnp.zeros((n_mine, 1), F32)
        pos = [jnp.zeros((n_mine, LANES), F32) for _ in range(SLOT_GROUPS // LANES)]
        for s in range(N_SRC):
            c, st = mine(cnt[s:s + 1]), mine(starts[s:s + 1]) + float(s * list_len)
            ng = groups(c)
            for i in range(len(pos)):
                rel = l16 + float(LANES * i) - off
                code = (st + GRP * rel) * 16.0 + jnp.minimum(float(GRP), c - GRP * rel)
                pos[i] = jnp.where((rel >= 0) & (rel < ng), code, pos[i])
            off = off + ng
        for i in range(len(pos)):
            tab_ref[pl.ds(at + i, n_mine, stride=len(pos)), :] = pos[i].astype(I32)
        n_tiles = jnp.maximum(1.0, jnp.floor((off + (PER_TILE - 0.5)) * (1.0 / PER_TILE)))
        bounds = over_subs(jnp.where(s16 < l16, n_tiles, 0.0))
        before = over_lanes(jnp.where(l16 == s16, jnp.broadcast_to(bounds, (n_mine, LANES)), 0.0))
        t = jnp.minimum(l16, over_subs(jnp.broadcast_to(n_tiles, (n_mine, LANES))) - 1.0)
        inside = (t >= before) & (t < before + n_tiles)
        goff = over_subs(jnp.where(inside, s16 * float(SLOT_GROUPS) + (t - before) * float(PER_TILE), 0.0))
        rows = [(ROW_BOUND, bounds), (ROW_GOFF, goff), (ROW_EXPERT, experts), (ROW_PARTNER, partner)]
        for row, value in rows:
            tab_ref[at + row:at + row + 1, :] = value.astype(I32)
    for l in range(n_layers):
        pad = l * (N_SRC * list_rows + 8) + N_SRC * list_rows
        gate_ref[pad:pad + 8, :] = jnp.zeros((8, LANES), F32)
        for s in range(N_SRC):
            to = (l * N_SRC + s) * list_rows
            toks = all_ref[s, l * list_rows:(l + 1) * list_rows, :]
            idx_ref[to:to + list_rows, :] = ((toks + float(s * n_tok)) * float(PITCH)).astype(I32)
            to = l * (N_SRC * list_rows + 8) + s * list_rows
            gate_ref[to:to + list_rows, :] = all_ref[s, (n_layers + l) * list_rows:(n_layers + l + 1) * list_rows, :]


def plan_shapes(sizes):
    n_layers, _, _, list_rows = sizes
    rows = (n_layers * TAB_ROWS, n_layers * N_SRC * list_rows, n_layers * (N_SRC * list_rows + 8))
    return [jax.ShapeDtypeStruct((n, LANES), dt) for n, dt in zip(rows, (I32, I32, F32))]


def flat(tab, idx, gates):
    return tab.reshape(-1), idx.reshape(-1), gates


def plan(deal, shared, sizes):
    return flat(*pl.pallas_call(
        functools.partial(plan_kernel, *sizes),
        out_shape=plan_shapes(sizes),
        in_specs=[in_vmem] * 2, out_specs=[in_vmem] * 3,
        cost_estimate=pl.CostEstimate(flops=10 ** 7, bytes_accessed=10 ** 6, transcendentals=0),
        name="plan",
    )(deal, shared))


def expert_kernel(cfg, *refs):
    fwd, bwd, own, layer, n_blk, d, ff, n_exp, picks, row_id, list_len, p_f32, n_alias, got_layer = cfg
    save, load = fwd and not bwd, own and bwd and not fwd
    refs = list(refs)
    take = lambda n: [refs.pop(0) for _ in range(n)]
    tab_hbm, idx_hbm, gate_hbm = take(3)
    u_pieces = take(N_SRC) if not load else []
    dy_pieces = take(N_SRC) if bwd else []
    wg_hbm, wu_hbm, wd_hbm = take(3)
    ab_hbm, xu_hbm = take(2) if load else (None, None)
    prev = take(1)[0] if bwd and not own else None
    got = take(2) if got_layer is not None else None
    take(n_alias)
    y_outs = take(N_SRC) if fwd else []
    du_outs = take(N_SRC) if bwd and own else []
    grad = take(1)[0] if bwd and own else None
    finals = take(3) if bwd and not own or got_layer is not None else None
    sent = take(2) if bwd and not own else None
    ab_hbm, xu_hbm = take(2) if save else (ab_hbm, xu_hbm)
    tab_ref, idx, gate_ref, land, table, gat = take(6)
    acc, row_ref = take(2) if own else (None, None)
    gu_ref, wd_ref, g_ref, x_u = take(4)
    x_c = take(1)[0] if bwd else None
    ab_ref = take(1)[0]
    dh_ref = take(1)[0] if bwd else None
    h_ref = take(1)[0]
    dab_ref, sums = take(2) if bwd else (None, None)
    keep_buf = take(1)[0] if bwd and not own else None
    got_buf = take(1)[0] if got is not None else None
    list_sem, land_sem, w_sem = take(3)
    sum_sem = take(1)[0] if bwd else None
    keep_sem = take(1)[0] if bwd and not own else None
    read_sem, write_sem = take(2) if got is not None else (None, None)
    stage_f, out_sem = take(2) if own else (None, None)
    ab_sem, xu_sem = take(2) if save or load else (None, None)

    copy = pltpu.make_async_copy
    cols = spans(d)
    lo = ff // 256 * 256
    hi = ff - lo
    dot = functools.partial(lax.dot_general, preferred_element_type=F32)
    nn = (((1,), (0,)), ((), ()))
    nt = (((1,), (1,)), ((), ()))
    tn = (((0,), (0,)), ((), ()))
    al = pl.multiple_of
    n_row = N_SRC * n_blk
    glane = lax.broadcasted_iota(I32, (GRP, LANES), 1)
    gsub = lax.broadcasted_iota(I32, (GRP, LANES), 0)

    def row_at(r):
        return pl.ds(r * PITCH, FULL)

    def codes_of(tile):
        at = ROW_GOFF * LANES + tile
        if own and bwd:
            return lambda q: tab_ref[tab_ref[at] + q]
        view = tab_ref.at[pl.ds(tab_ref[at], PER_TILE)]
        return lambda q: view[q]

    def gather(codes, q):
        ids = idx.at[pl.ds(codes(q) >> 4, GRP)]
        for k in range(GRP):
            gat[row_at(q * GRP + k), :] = table[pl.ds(ids[k], FULL), :]

    def gate_column(code):
        pos = code >> 4
        row, shift = pos >> 7, pos & (LANES - 1)
        want = glane == gsub + shift
        over = glane == gsub + (shift - LANES)
        here = gate_ref[pl.ds(row, GRP, stride=0), :]
        there = gate_ref[pl.ds(row + 1, GRP, stride=0), :]
        v = jnp.where(want, here, jnp.where(over, there, 0.0))
        return jnp.where(gsub < (code & 15), jnp.sum(v, axis=1, keepdims=True), 0.0)

    def scatter(codes, q):
        ids = idx.at[pl.ds(codes(q) >> 4, GRP)]
        new = []
        for k in range(GRP):
            at = pl.ds(ids[k], FULL)
            new.append((at, acc[at, :] + row_ref[row_at(q * GRP + k), :]))
        for at, value in reversed(new):
            acc[at, :] = value

    def keep_ab(t):
        ends = (ab_ref.at[t & 1], ab_hbm.at[t])
        return copy(*(ends if save else ends[::-1]), ab_sem.at[t & 1])

    def keep_xu(t):
        ends = (x_u.at[t & 1], xu_hbm.at[t])
        return copy(*(ends if save else ends[::-1]), xu_sem.at[t & 1])

    def of(ref, t):
        return ref.at[t & 1] if save or load else ref

    def convert(codes, t):
        for q in range(0, PER_TILE, 2):
            part = []
            for p in (q, q + 1):
                code = codes(p)
                rows = [gat[pl.ds(GRP * PITCH * p + j, GRP, stride=PITCH), :]
                        for j in range(HALF if load else 0, FULL if bwd else HALF)]
                real = gsub < (code & 15)
                gate = gate_column(code)
                g_ref[GRP * p:GRP * (p + 1), :] = gate
                us, dys = ([], rows) if load else (rows[:HALF], rows[HALF:])
                part.append([jnp.where(real, v, 0.0) for v in us] + [v * gate for v in dys])
            at = slice(GRP * q, GRP * (q + 2))
            for x, o in ((None if load else of(x_u, t), 0), (x_c, 0 if load else HALF)):
                if x is None:
                    continue
                for j, (c, w) in enumerate(cols):
                    both = jnp.concatenate([part[0][o + j], part[1][o + j]], axis=0)
                    x[at, c:c + w] = both[:, :w].astype(BF16)

    def put_rows(o, value, s0):
        value = value.astype(BF16).astype(F32)
        n = value.shape[0]
        for j, (c, w) in enumerate(cols):
            row_ref[pl.ds(PITCH * s0 + o + j, n, stride=PITCH), 0:w] = value[:, c:c + w] * g_ref[s0:s0 + n, 0:w]

    low = lax.broadcasted_iota(I32, (16, 2 * hi), 1) < hi

    def middle(a, b, dh):
        sig = 0.5 * jnp.tanh(0.5 * a) + 0.5
        act = a * sig
        h = act * b
        if dh is None:
            return h, None, None
        slope = sig * (1.0 + a * (1.0 - sig))
        return h, dh * b * slope, dh * act

    def weights(e, slot):
        at = (layer, tab_ref[ROW_EXPERT * LANES + e])
        moves = []
        for i, w in enumerate((wg_hbm, wu_hbm)):
            moves.append((w.at[at + (pl.ds(0, lo),)], gu_ref.at[slot, pl.ds(i * lo, lo)]))
            moves.append((w.at[at + (pl.ds(lo, hi),)], gu_ref.at[slot, pl.ds(2 * lo + i * hi, hi)]))
        moves.append((wd_hbm.at[at], wd_ref.at[slot]))
        return [copy(a, b, w_sem.at[slot, i]) for i, (a, b) in enumerate(moves)]

    def sums_in(e, slot):
        return copy(prev.at[e], sums.at[slot], sum_sem.at[slot])

    def sums_out(e, slot):
        return copy(sums.at[slot], grad.at[e], sum_sem.at[slot])

    def keeps(e, slot):
        at = (layer, tab_ref[ROW_EXPERT * LANES + e])
        return [copy(keep_buf.at[slot, i], finals[i].at[at], keep_sem.at[slot, i]) for i in range(3)]

    def send(e, slot, part):
        return copy(keep_buf.at[slot], sent[part].at[e - part * (n_exp // 2)], keep_sem.at[slot, 3])

    def read(e, slot, part=0):
        return copy(got[part].at[e - part * (n_exp // 2)], got_buf.at[slot], read_sem.at[slot])

    def writes(e, slot):
        to = tab_ref[TAB_ROWS * LANES + e]
        return [copy(got_buf.at[slot, i], finals[i].at[got_layer, to], write_sem.at[slot, i]) for i in range(3)]

    def start(moves):
        for m in moves:
            m.start()

    def wait(moves):
        for m in moves:
            m.wait()

    n_tab = TAB_ROWS * LANES
    lists = [copy(tab_hbm.at[pl.ds(row_id * n_tab, n_tab)], tab_ref.at[pl.ds(0, n_tab)], list_sem.at[0]),
             copy(idx_hbm.at[pl.ds(row_id * N_SRC * list_len, N_SRC * list_len)], idx.at[pl.ds(0, N_SRC * list_len)],
                  list_sem.at[1]),
             copy(gate_hbm.at[pl.ds(row_id * gate_ref.shape[0], gate_ref.shape[0])], gate_ref, list_sem.at[2])]
    if got is not None:
        at = (got_layer * TAB_ROWS + ROW_PARTNER) * LANES
        lists.append(copy(tab_hbm.at[pl.ds(at, LANES)], tab_ref.at[pl.ds(n_tab, LANES)], list_sem.at[3]))
    start(lists)
    pieces = []
    for s in range(N_SRC):
        if not load:
            pieces.append((u_pieces[s], picks[0][s], s, 0, fwd))
        if bwd:
            pieces.append((dy_pieces[s], picks[1][s], s, HALF, own))
    lands = [copy(ref.at[pick], land.at[i % N_SRC], land_sem.at[i % N_SRC]) for i, (ref, pick, *_) in enumerate(pieces)]
    start(lands[:N_SRC])
    lists[0].wait()
    for e in range(DEPTH - 1):
        start(weights(e, e))
        if bwd and not own:
            sums_in(e, e).start()
    if got is not None:
        lists[3].wait()
        read(0, 0).start()
    if own:
        def clear(c, _):
            for k in range(4):
                acc[pl.ds(al(c * 1152 + 288 * k, 8), 288), :] = jnp.zeros((288, LANES), F32)
            return 0

        lax.fori_loop(0, acc.shape[0] // 1152, clear, 0)
        row_ref[...] = jnp.zeros(row_ref.shape, F32)
    rows = 256
    for i, (_, _, s, o, seed) in enumerate(pieces):
        lands[i].wait()

        def fill(c, _, i=i, o=o, seed=seed, s=s):
            r = al(c * rows, rows)
            for j in range(HALF):
                vals = land[i % N_SRC, pl.ds(r, rows), LANES * j:LANES * (j + 1)].astype(F32)
                to = pl.ds(PITCH * (s * n_blk + r) + o + j, rows, stride=PITCH)
                table[to, :] = vals
                if seed and s == 0:
                    acc[to, :] = vals
            return 0

        lax.fori_loop(0, n_blk // rows, fill, 0)
        if i + N_SRC < len(pieces):
            lands[i + N_SRC].start()
    wait(lists[1:3])
    for k in range(GRP):
        idx[N_SRC * list_len + k] = 0

    def first(q, _):
        gather(begin, 2 * q)
        gather(begin, 2 * q + 1)
        return 0

    begin = codes_of(0)
    lax.fori_loop(0, PER_TILE // 2, first, 0)
    convert(begin, 0)
    if save:
        keep_xu(0).start()
    if load:
        keep_ab(0).start()
        keep_xu(0).start()

    def expert(e, _):
        slot = e & 1
        deep = lax.rem(e, DEPTH)
        sum_slot = slot if own else deep
        wait(weights(e, deep))
        if bwd and not own:
            sums_in(e, deep).wait()
        if got is not None:
            read(0, slot).wait()
            start(writes(e, slot))

            @pl.when((e > 0) & (e < n_exp - 1))
            def _():
                wait(writes(e - 1, 1 - slot))

        @pl.when(e < n_exp - (DEPTH - 1))
        def _():
            ahead = lax.rem(e + DEPTH - 1, DEPTH)
            start(weights(e + DEPTH - 1, ahead))
            if bwd and not own:
                sums_in(e + DEPTH - 1, ahead).start()

        @pl.when(e < n_exp - 1)
        def _():
            if got is not None:
                for part in range(2):
                    @pl.when((e + 1 >= n_exp // 2) if part else (e + 1 < n_exp // 2))
                    def _(part=part):
                        read(e + 1, 1 - slot, part).start()

        if bwd and own:
            @pl.when(e > 1)
            def _():
                sums_out(e - 2, slot).wait()

            sums[slot] = jnp.zeros(sums.shape[1:], F32)

        def tile(t, _):
            if save:
                @pl.when(t > 1)
                def _():
                    keep_ab(t - 2).wait()

                @pl.when(t > 0)
                def _():
                    keep_xu(t - 1).wait()
            if load:
                keep_ab(t).wait()
                keep_xu(t).wait()
                keep_ab(t + 1).start()
                keep_xu(t + 1).start()
            ab, xu = of(ab_ref, t), of(x_u, t)
            before, after = codes_of(jnp.maximum(t - 1, 0)), codes_of(t + 1)
            for q in range(PER_TILE):
                if own:
                    scatter(before, q)
                gather(after, q)
            half = ROWS // 2
            for s0 in range(0, ROWS, half):
                sl = slice(s0, s0 + half)
                if not load:
                    ab[sl, :] = dot(xu[sl, :], gu_ref[deep], nt)
                if bwd:
                    dh_ref[sl, :] = dot(x_c[sl, :], wd_ref[deep], nt)
            for r in range(0, ROWS, 16):
                rows = slice(r, r + 16)
                for c in range(0, lo, LANES):
                    h, da, db = middle(ab[rows, c:c + LANES], ab[rows, lo + c:lo + c + LANES],
                                       dh_ref[rows, c:c + LANES] if bwd else None)
                    h_ref[rows, c:c + LANES] = h.astype(BF16)
                    if bwd:
                        dab_ref[rows, c:c + LANES] = da.astype(BF16)
                        dab_ref[rows, lo + c:lo + c + LANES] = db.astype(BF16)
                a = ab[rows, 2 * lo:]
                b = pltpu.roll(a, hi, 1)
                dh = dh_ref[rows, lo:] if bwd else None
                if bwd:
                    dh = jnp.concatenate([dh, dh], axis=1)
                h, da, db = middle(a, b, dh)
                h_ref[rows, lo:] = h[:, :hi].astype(BF16)
                if bwd:
                    dab_ref[rows, 2 * lo:] = jnp.where(low, da, pltpu.roll(db, hi, 1)).astype(BF16)
            for s0 in range(0, ROWS, half):
                sl = slice(s0, s0 + half)
                if fwd:
                    put_rows(0, dot(h_ref[sl, :], wd_ref[deep], nn), s0)
                if bwd and own:
                    put_rows(HALF, dot(dab_ref[sl, :], gu_ref[deep], nn), s0)
            if bwd:
                view = sums.at[sum_slot]
                view[0:2 * ff, :] += dot(dab_ref[...], xu[...], tn)
                view[2 * ff:, :] += dot(h_ref[...], x_c[...], tn)
            convert(after, t + 1)
            if save:
                keep_ab(t).start()
                keep_xu(t + 1).start()
            return 0

        lax.fori_loop(tab_ref[ROW_BOUND * LANES + e], tab_ref[ROW_BOUND * LANES + e + 1], tile, 0)
        if bwd and own:
            sums_out(e, slot).start()
        if bwd and not own:
            @pl.when(e > 1)
            def _():
                wait(keeps(e - 2, slot) + [send(0, slot, 0)])

            for i in range(2):
                keep_buf[slot, i, 0:lo, :] = sums[deep, i * lo:(i + 1) * lo, :].astype(BF16)
                keep_buf[slot, i, lo:, :] = sums[deep, 2 * lo + i * hi:2 * lo + (i + 1) * hi, :].astype(BF16)
            keep_buf[slot, 2] = sums[deep, 2 * ff:, :].astype(BF16)
            start(keeps(e, slot))
            for part in range(2):
                @pl.when((e >= n_exp // 2) if part else (e < n_exp // 2))
                def _(part=part):
                    send(e, slot, part).start()
        return 0

    lax.fori_loop(0, n_exp, expert, 0)
    ends = ((n_exp - 2, (n_exp - 2) % 2), (n_exp - 1, (n_exp - 1) % 2))
    n_tiles = tab_ref[ROW_BOUND * LANES + n_exp]
    if save:
        wait([keep_ab(n_tiles - 2), keep_ab(n_tiles - 1), keep_xu(n_tiles - 1)])
    if save or load:
        keep_xu(n_tiles).wait()
    if load:
        keep_ab(n_tiles).wait()
    if own:
        end = codes_of(tab_ref[ROW_BOUND * LANES + n_exp] - 1)
        lax.fori_loop(0, PER_TILE, lambda q, _: (scatter(end, q), 0)[1], 0)
        flights = {}
        for o, out in ((HALF, du_outs), (0, y_outs)):
            for s in range(N_SRC if out else 0):
                wide = s == 0 or p_f32
                stage = stage_f.at[s] if wide else land.at[s]
                if s in flights:
                    flights[s].wait()

                def fetch(c, _, stage=stage, s=s, o=o):
                    r = al(c * rows, rows)
                    for j in range(HALF):
                        at = pl.ds(PITCH * (s * n_blk + r) + o + j, rows, stride=PITCH)
                        stage[pl.ds(r, rows), LANES * j:LANES * (j + 1)] = acc[at, :].astype(stage.dtype)
                    return 0

                lax.fori_loop(0, n_blk // rows, fetch, 0)
                flights[s] = copy(stage, out[s], out_sem.at[s])
                flights[s].start()
        wait(flights.values())
        if bwd:
            for e, slot in ends:
                sums_out(e, slot).wait()
    else:
        for e, slot in ends:
            wait(keeps(e, slot) + [send(0, slot, 0)])
    if got is not None:
        for e, slot in ends:
            wait(writes(e, slot))


def run_experts(routes, layer, u, dy, weights, prev, finals, fwd, own, p_f32=False, got=None, kept=None):
    tab, idx, gates = routes
    bwd = dy is not None
    wg, wu, wd = weights
    save, load = fwd and not bwd, kept is not None
    n_blk, wide = (dy or u)[0][0].shape[-2:]
    n_layers, n_local, ff, d = wd.shape
    n_exp = n_local // 2
    row_id = layer
    list_len = idx.shape[0] // (n_layers * N_SRC)

    arrays = lambda pieces: [v for v, _ in pieces]
    operands = [tab, idx, gates] + ([] if load else arrays(u)) + (arrays(dy) if bwd else []) + [wg, wu, wd] + list(kept or ())
    out_shape, aliases = [], {}
    for use in (fwd, bwd and own):
        if use:
            out_shape += [jax.ShapeDtypeStruct((n_blk, wide), F32 if s == 0 or p_f32 else BF16) for s in range(N_SRC)]
    if bwd and own:
        out_shape.append(jax.ShapeDtypeStruct((n_exp, 3 * ff, d), F32))
    if bwd and not own:
        operands.append(prev)
    if got is not None:
        operands += got
    for i, f in enumerate(finals or ()):
        aliases[len(operands)] = len(out_shape) + i
        operands.append(f)
    if bwd and not own or finals:
        out_shape += [jax.ShapeDtypeStruct((n_layers, n_local, ff, d), BF16)] * 3
    if bwd and not own:
        out_shape += [jax.ShapeDtypeStruct((n_exp // 2, 3, ff, d), BF16)] * 2
    if save:
        most = n_exp * (SLOT_GROUPS // PER_TILE) + 2
        out_shape += [jax.ShapeDtypeStruct((most, ROWS, 2 * ff), F32), jax.ShapeDtypeStruct((most, ROWS, d), BF16)]
    sem = lambda *s: pltpu.SemaphoreType.DMA(s)
    mid = lambda n, dt: pltpu.VMEM((ROWS, n), dt)
    twin = lambda n, dt: pltpu.VMEM((2, ROWS, n), dt) if save or load else mid(n, dt)
    table, rows = pltpu.VMEM((PITCH * N_SRC * n_blk, LANES), F32), pltpu.VMEM((PITCH * ROWS, LANES), F32)
    scratch = [pltpu.SMEM(((TAB_ROWS + 1) * LANES,), I32), pltpu.SMEM((N_SRC * list_len + LANES,), I32),
               pltpu.VMEM((N_SRC * list_len // LANES + 8, LANES), F32), pltpu.VMEM((N_SRC, n_blk, wide), BF16)]
    scratch += [table, rows] * (1 + own)
    scratch += [pltpu.VMEM((DEPTH, 2 * ff, d), BF16), pltpu.VMEM((DEPTH, ff, d), BF16), mid(LANES, F32)]
    scratch += [twin(d, BF16)] + [mid(d, BF16)] * bwd + [twin(2 * ff, F32)] + [mid(ff, F32)] * bwd + [mid(ff, BF16)]
    scratch += [mid(2 * ff, BF16), pltpu.VMEM((2 if own else DEPTH, 3 * ff, d), F32)] * bwd
    if bwd and not own:
        scratch.append(pltpu.VMEM((2, 3, ff, d), BF16))
    if got is not None:
        scratch.append(pltpu.VMEM((2, 3, ff, d), BF16))
    scratch += [sem(4), sem(N_SRC), sem(DEPTH, 5)] + [sem(DEPTH)] * bwd
    if bwd and not own:
        scratch.append(sem(2, 4))
    if got is not None:
        scratch += [sem(2), sem(2, 3)]
    if own:
        scratch += [pltpu.VMEM((N_SRC if p_f32 else 1, n_blk, wide), F32), sem(N_SRC)]
    if save or load:
        scratch += [sem(2), sem(2)]
    passes = 2 + fwd + bwd * (4 + 2 * own)
    flops = 2 * d * ff * passes * n_blk * N_SRC * 2
    hoist = 1400 if not own else 600 if load else 750 if save else 700
    picks = [[i for _, i in u] if u else None, [i for _, i in dy] if bwd else None]
    cfg = (fwd, bwd, own, layer, n_blk, d, ff, n_exp, picks, row_id, list_len, p_f32, len(aliases),
           None if got is None else 1 - layer)
    return pl.pallas_call(
        functools.partial(expert_kernel, cfg),
        out_shape=out_shape,
        in_specs=[any_space] * len(operands),
        out_specs=[any_space] * len(out_shape),
        scratch_shapes=scratch,
        input_output_aliases=aliases,
        compiler_params=pltpu.CompilerParams(
            vmem_limit_bytes=VMEM_LIMIT),
        cost_estimate=pl.CostEstimate(flops=flops, bytes_accessed=3 * 2 * n_exp * d * ff, transcendentals=0),
        name=f"experts_{'f' if fwd else ''}{'b' if bwd else ''}_{'own' if own else 'other'}_{layer}",
    )(*operands)


def place_kernel(layer, n_exp, tab_ref, got_ref, *refs):
    outs, (buf, in_sem, out_sem) = refs[3:6], refs[6:]
    reads = [pltpu.make_async_copy(got_ref.at[i], buf.at[i], in_sem.at[i]) for i in range(n_exp)]
    for read in reads:
        read.start()
    writes = []
    for i, read in enumerate(reads):
        read.wait()
        e = tab_ref[i]
        for k, out in enumerate(outs):
            writes.append(pltpu.make_async_copy(buf.at[i, k], out.at[layer, e], out_sem.at[i, k]))
            writes[-1].start()
    for write in writes:
        write.wait()


def place(partner, layer, got, finals):
    n_exp = got.shape[0]
    return pl.pallas_call(
        functools.partial(place_kernel, layer, n_exp),
        out_shape=[jax.ShapeDtypeStruct(f.shape, f.dtype) for f in finals],
        grid_spec=pltpu.PrefetchScalarGridSpec(
            num_scalar_prefetch=1, grid=(1,), in_specs=[any_space] * 4, out_specs=[any_space] * 3,
            scratch_shapes=[pltpu.VMEM(got.shape, got.dtype), pltpu.SemaphoreType.DMA((n_exp,)),
                            pltpu.SemaphoreType.DMA((n_exp, 3))]),
        input_output_aliases={2: 0, 3: 1, 4: 2},
        compiler_params=pltpu.CompilerParams(vmem_limit_bytes=VMEM_LIMIT),
        cost_estimate=pl.CostEstimate(flops=0, bytes_accessed=4 * got.size, transcendentals=0),
        name=f"place_{layer}",
    )(partner, got, *finals)


def peer(rel):
    return {name: (lax.axis_index(name) + ((rel >> bit) & 1)) % 2 for bit, name in enumerate(("ep", "core", "x"))}


def meet(rels):
    barrier = pltpu.get_barrier_semaphore()
    for rel in rels:
        pl.semaphore_signal(barrier, inc=1, device_id=peer(rel), device_id_type=MESH)
    pl.semaphore_wait(barrier, len(rels))


def remote(src, dst, send, recv, rel):
    return pltpu.make_async_remote_copy(src_ref=src, dst_ref=dst, send_sem=send, recv_sem=recv,
                                        device_id=peer(rel), device_id_type=MESH)


def share_kernel(n_rel, mine_ref, all_ref, send_sem, recv_sem):
    meet(range(1, n_rel))
    copies = [remote(mine_ref, all_ref.at[rel], send_sem.at[rel], recv_sem.at[rel], rel) for rel in range(1, n_rel)]
    for copy in copies:
        copy.start()
    all_ref[0] = mine_ref[...]
    for copy in copies:
        copy.wait()


def share(mine, n_rel):
    return pl.pallas_call(
        functools.partial(share_kernel, n_rel),
        out_shape=jax.ShapeDtypeStruct((n_rel,) + mine.shape, mine.dtype),
        in_specs=[in_vmem],
        out_specs=in_vmem,
        scratch_shapes=[pltpu.SemaphoreType.DMA((n_rel,)), pltpu.SemaphoreType.DMA((n_rel,))],
        compiler_params=pltpu.CompilerParams(collective_id=0, has_side_effects=True),
        cost_estimate=pl.CostEstimate(flops=10 ** 7, bytes_accessed=mine.size * 4 * n_rel, transcendentals=0),
        name="share_lists",
    )(mine)


def blocks_kernel(cfg, *refs):
    n_chunk, reduce, back, d, sizes = cfg
    refs = list(refs)
    take = lambda n: [refs.pop(0) for _ in range(n)]
    parts = take(N_SRC)
    m_ref = take(1)[0]
    list_refs, left_ref = take(2) if sizes else (), take(1)[0] if back else None
    o_total, o_a, o_b = take(3)
    plan_refs, grad_ref = take(3) if sizes else (), take(1)[0] if back else None
    in_f, in_b, got_f, s_wire, r_wire, u_wire, y_wire, t_buf, u_buf, y_buf, load, send, recv, put = take(14)
    n_rows = t_buf.shape[0] // n_chunk
    cut = [pl.ds(k * n_rows, n_rows) for k in range(n_chunk)]
    thin = [pl.ds(k * n_rows // 2, n_rows // 2) for k in range(n_chunk)]
    side = lax.broadcasted_iota(I32, (n_rows // 2, LANES), 1) < LANES // 2
    tiles = d // LANES
    turn = lambda v: pltpu.roll(v, LANES // 2, 1)
    lanes = lambda v, j: v[:, LANES * j:LANES * (j + 1)]

    def pack(wire, k, value):
        top, low = value[:n_rows // 2], value[n_rows // 2:]
        turned = [turn(lanes(low, j)) for j in range(tiles + 1)]
        parts = [lanes(top, j) for j in range(tiles)] + [jnp.where(side, lanes(top, tiles), turned[0])]
        parts += [jnp.where(side, turned[j], turned[j + 1]) for j in range(tiles)]
        for j, part in enumerate(parts):
            wire[thin[k], LANES * j:LANES * (j + 1)] = part.astype(BF16)

    def unpack(wire, k):
        value = wire[thin[k], :].astype(F32)
        turned = [turn(lanes(value, tiles + j)) for j in range(tiles + 1)]
        top = [lanes(value, j) for j in range(tiles)] + [jnp.where(side, lanes(value, tiles), 0.0)]
        low = [jnp.where(side, turned[j], turned[j + 1]) for j in range(tiles)] + [jnp.where(side, turned[tiles], 0.0)]
        return jnp.concatenate([jnp.concatenate(top, axis=1), jnp.concatenate(low, axis=1)], axis=0)

    chunks = range(n_chunk)
    loads = {}
    for i, part in enumerate(parts[:2] if reduce else parts):
        buf = in_f.at[i] if reduce or i == 0 else in_b.at[i - 1]
        for k in chunks:
            loads[i, k] = pltpu.make_async_copy(part.at[cut[k]], buf.at[cut[k]], load.at[i, k])
    order = (1, 0) if reduce else range(N_SRC)
    for i in order:
        for k in chunks:
            loads[i, k].start()
    u_buf[...] = jnp.zeros(u_buf.shape, BF16)
    meet((Y, CORE))
    links = []
    copy_in = pltpu.make_async_copy

    def link(src, dst, rel, cut=cut):
        n = len(links)
        links.append([remote(src.at[cut[k]], dst.at[cut[k]], send.at[n, k], recv.at[n, k], rel) for k in chunks])
        return links[-1]

    if reduce:
        first = link(parts[3], got_f.at[1], CORE)
        second = link(parts[2], got_f.at[0], CORE)
        over = link(s_wire, r_wire, Y, thin)
        for copies in (first, second):
            for copy in copies:
                copy.start()
        for k in chunks:
            loads[1, k].wait()
            first[k].wait_recv()
            pack(s_wire, k, in_f[1, cut[k], :] + got_f[1, cut[k], :])
            over[k].start()
    to_y = link(u_wire, y_wire, Y, thin)
    to_core = link(u_buf, o_b.at[0], CORE)
    puts = []
    for k in chunks:
        if reduce:
            loads[0, k].wait()
            second[k].wait_recv()
            over[k].wait_recv()
            total = in_f[0, cut[k], :] + got_f[0, cut[k], :] + unpack(r_wire, k)
        else:
            for i in range(N_SRC):
                loads[i, k].wait()
            total = in_f[0, cut[k], :]
            for i in range(N_SRC - 1):
                total = total + in_b[i, cut[k], :].astype(F32)
        total = total.astype(BF16)
        t_buf[cut[k], :] = total
        dims = (((1,), (1 if back else 0,)), ((), ()))
        mixed = lax.dot_general(total[:, :d], m_ref[...], dims, preferred_element_type=F32)
        u_buf[cut[k], 0:d] = (total[:, :d].astype(F32) + mixed).astype(BF16)
        pack(u_wire, k, u_buf[cut[k], :].astype(F32))
        to_y[k].start()
        to_core[k].start()
        puts.append(pltpu.make_async_copy(u_buf.at[cut[k]], o_a.at[0, cut[k]], put.at[0, k]))
        puts.append(pltpu.make_async_copy(t_buf.at[cut[k]], o_total.at[cut[k]], put.at[1, k]))
        for copy in puts[-2:]:
            copy.start()
    if sizes:
        plan_kernel(*sizes, *list_refs, *plan_refs)
    if back:
        grad_ref[...] = lax.dot_general(left_ref[:, :d], t_buf[:, :d], (((0,), (0,)), ((), ())), preferred_element_type=F32)
    on = link(y_buf, o_b.at[1], CORE)
    for k in chunks:
        to_y[k].wait_recv()
        y_buf[cut[k], :] = unpack(y_wire, k).astype(BF16)
        on[k].start()
        puts.append(copy_in(y_buf.at[cut[k]], o_a.at[1, cut[k]], put.at[2, k]))
        puts[-1].start()
    waited = [to_y] + ([first, second, over] if reduce else [])
    for copies in links:
        for copy in copies:
            if any(copies is w for w in waited):
                copy.wait_send()
            else:
                copy.wait()
    for copy in puts:
        copy.wait()


def complete_blocks(parts, m, reduce, back, ident, sizes=None, lists=(), left=(), n_chunk=8):
    n_blk, wide = parts[0].shape
    d = m.shape[0]
    sem = lambda *s: pltpu.SemaphoreType.DMA(s)
    pair = jax.ShapeDtypeStruct((2, n_blk, wide), BF16)
    extra = plan_shapes(sizes) if sizes else []
    extra += [jax.ShapeDtypeStruct((d, d), F32)] * len(left)
    buf = lambda n, dt: pltpu.VMEM((n, n_blk, wide) if n else (n_blk, wide), dt)
    return pl.pallas_call(
        functools.partial(blocks_kernel, (n_chunk, reduce, back, d, sizes)),
        out_shape=[jax.ShapeDtypeStruct((n_blk, wide), BF16)] + [pair] * 2 + extra,
        in_specs=[any_space] * N_SRC + [in_vmem] * (1 + len(lists) + len(left)),
        out_specs=[any_space] * 3 + [in_vmem] * len(extra),
        scratch_shapes=[buf(2, F32), buf(3, BF16), buf(2, F32)] + [pltpu.VMEM((n_blk // 2, 2 * d), BF16)] * 4 + [
            buf(0, BF16), buf(0, BF16), buf(0, BF16), sem(4, n_chunk), sem(6, n_chunk), sem(6, n_chunk), sem(3, n_chunk)],
        compiler_params=pltpu.CompilerParams(collective_id=ident, has_side_effects=True, vmem_limit_bytes=VMEM_LIMIT),
        cost_estimate=pl.CostEstimate(flops=10 ** 8, bytes_accessed=n_blk * wide * 40, transcendentals=0),
        name=f"complete_blocks_{ident}",
    )(*parts, m, *lists, *left)


def solution(mesh):
    ep_size, dp_size = mesh.shape['ep'], mesh.shape['dp']
    sub = Mesh(mesh.devices.reshape(ep_size, dp_size // 2, 2), ('ep', 'x', 'core'))
    tok_axes = ('x', 'core', 'ep')
    tok_spec = P(tok_axes, None)
    route_spec = P(None, tok_axes, None)
    whole_spec = P(None, None, None)
    expert_spec = P(None, 'ep', None, None)
    flip = [(0, 1), (1, 0)]
    move = lambda v, axis: lax.ppermute(v, axis, flip)
    move_diag = lambda v: lax.ppermute(v, ('ep', 'core'), [(0, 3), (1, 2), (2, 1), (3, 0)])
    fence = lax.optimization_barrier

    def device_step(tokens, d_out, expert_ids, gate_vals, w_mix, w_gate, w_up, w_down):
        n_layers, d = w_mix.shape[0], w_mix.shape[1]
        n_tok = tokens.shape[0]
        top = expert_ids.shape[2]
        n_local = w_gate.shape[1]
        n_exp = n_local * ep_size
        n = n_tok * top
        n_rel = 2 * N_SRC
        wide = cdiv(d, LANES) * LANES
        weights = (jnp.swapaxes(w_gate, 2, 3), jnp.swapaxes(w_up, 2, 3), w_down)
        pad = lambda v: jnp.pad(v, ((0, 0), (0, wide - d)))
        send_three = lambda p: [move(p[1], 'ep'), move(p[2], 'core'), move_diag(p[3])]

        def own_sum(p, got):
            return sum([g.astype(F32) for g in got], p)[:, :d].astype(BF16)

        one = lambda v: v.reshape(1, n_tok, wide)
        pairs = lambda a, b: [(a, 0), (a, 1), (b, 0), (b, 1)]

        one = lambda v: v.reshape(1, n_tok, wide)
        pairs = lambda a, b: [(a, 0), (a, 1), (b, 0), (b, 1)]
        singles = lambda *v: [(one(a), 0) for a in v]

        u0 = pad((tokens.astype(F32) + jnp.dot(tokens, w_mix[0], preferred_element_type=F32)).astype(BF16))
        u0_y, u0_c = move(u0, 'ep'), move(u0, 'core')
        lists = [sorted_list(expert_ids[l], gate_vals[l]) for l in range(n_layers)]
        counts = jnp.sum((expert_ids.reshape(n_layers, n, 1) == jnp.arange(n_exp, dtype=I32)).astype(F32), axis=1)
        packed = jnp.concatenate([jnp.concatenate([v[0] for v in lists] + [v[1] for v in lists]).reshape(-1, LANES),
                                  jnp.pad(counts, ((0, 8 - n_layers), (0, LANES - n_exp)))], axis=0)
        dy = pad(d_out)
        u0_y, u0_c, packed, dy = fence((u0_y, u0_c, packed, dy))
        u0_d = move(u0_y, 'core')
        shared = share(packed, N_SRC)
        dy, shared = fence((dy, shared))
        shared_x = move(shared, 'x')
        dy_y, dy_x = move(dy, 'ep'), move(dy, 'x')
        sizes = (n_layers, n_local, n_tok, n // LANES)
        routes = plan(shared, shared, sizes)
        u0_half = singles(u0, u0_y, u0_c, u0_d)
        *part, ab0, xu0 = run_experts(routes, 0, u0_half, None, weights, None, None, True, True, p_f32=True)
        dy_y, dy_x, shared_x, part = fence((dy_y, dy_x, shared_x, part))
        dy_c, dy_d, dy_xy, dy_xc = move(dy, 'core'), move(dy_y, 'core'), move(dy_y, 'x'), move(dy_x, 'core')
        y0, u1_a, u1_b, *routes_x = complete_blocks(part, w_mix[1], True, False, 1, sizes, (shared, shared_x))
        routes_x = flat(*routes_x)
        dy_c, dy_d, dy_xy, dy_xc, u0_p, u0_q, y0, u1_a, u1_b = fence(
            (dy_c, dy_d, dy_xy, dy_xc, u0, u0_y, y0, u1_a, u1_b))
        dy_xd = move(dy_xy, 'core')
        u1_xa = move(u1_a, 'x')
        out = run_experts(routes, 1, pairs(u1_a, u1_b), singles(dy, dy_y, dy_c, dy_d), weights, None, None, True, True)
        u1_xa, dy_xd, u0_p, u0_q, out = fence((u1_xa, dy_xd, u0_p, u0_q, out))
        y_part, du_part, g1 = out[:4], out[4:8], out[8]
        u1_xb = move(u1_xa, 'core')
        got = send_three(du_part)
        u0_x, u0_xy = move(u0_p, 'x'), move(u0_q, 'x')
        out = run_experts(routes_x, 1, pairs(u1_xa, u1_xb), singles(dy_x, dy_xy, dy_xc, dy_xd), weights, g1, None,
                          False, False)
        got, u0_x, u0_xy, out = fence((got, u0_x, u0_xy, out))
        *finals, sent_a, sent_b = out
        got1 = [move(sent_a, 'core'), move(sent_b, 'core')]
        du1, dx_a, dx_b, g_mix1 = complete_blocks([du_part[0], *got], w_mix[1], False, True, 2, left=(y0,))
        tx = lambda x, du: jnp.einsum('td,te->de', x, du, preferred_element_type=F32)
        dx_a, y_part, got1, u0_x, u0_xy, g_mix1 = fence((dx_a, y_part, got1, u0_x, u0_xy, g_mix1))
        dx_xa = move(dx_a, 'x')
        theirs1 = move(g_mix1, 'core')
        got_y = send_three(y_part)
        u0_xc, u0_xd = move(u0_x, 'core'), move(u0_xy, 'core')
        out = run_experts(routes, 0, None, pairs(dx_a, dx_b), weights, None, finals, False, True, got=got1, kept=(ab0, xu0))
        dx_xa, got_y, u0_xc, u0_xd, theirs1, out = fence((dx_xa, got_y, u0_xc, u0_xd, theirs1, out))
        du_part, g0, finals = out[:4], out[4], out[5:]
        dx_xb = move(dx_xa, 'core')
        got = send_three(du_part)
        part1 = (g_mix1 + theirs1).astype(BF16)
        theirs1 = move(part1, 'ep')
        du_part, dx_xb, part1 = fence((du_part, dx_xb, part1))
        out = run_experts(routes_x, 0, singles(u0_x, u0_xy, u0_xc, u0_xd), pairs(dx_xa, dx_xb), weights, g0, finals,
                          False, False)
        got, theirs1, got_y, y_own, out = fence((got, theirs1, got_y, y_part[0], out))
        *finals, sent_a, sent_b = out
        got_a, got_b = move(sent_a, 'core'), move(sent_b, 'core')
        add = lambda a, b: a.astype(F32) + b.astype(F32)
        part1 = add(part1, theirs1).astype(BF16)
        theirs1 = move(part1, 'x')
        du0 = own_sum(du_part[0], got)
        part0 = tx(tokens, du0).astype(BF16)
        theirs0 = move(part0, 'ep')
        dx0 = (du0.astype(F32) + jnp.einsum('te,de->td', du0, w_mix[0], preferred_element_type=F32)).astype(BF16)
        row = lambda a: lax.slice_in_dim(routes[0], ROW_PARTNER * LANES + a, ROW_PARTNER * LANES + a + n_local // 4)
        y1 = own_sum(y_own, got_y).T
        dx0, y1, got_a, finals = fence((dx0, y1, got_a, finals))
        finals = place(row(0), 0, got_a, finals)
        theirs0, finals = fence((theirs0, finals))
        part0 = add(part0, theirs0).astype(BF16)
        theirs0 = move(part0, 'x')
        part0, dx0, got_b = fence((part0, dx0.T, got_b))
        finals = place(row(n_local // 4), 0, got_b, finals)
        theirs0, theirs1, finals = fence((theirs0, theirs1, finals))
        total0 = add(part0, theirs0).astype(BF16)
        g_mix = jnp.stack([add(total0, move(total0, 'core')), add(part1, theirs1)]).astype(BF16)
        return (y1.T, dx0.T, g_mix, jnp.swapaxes(finals[0], 2, 3), jnp.swapaxes(finals[1], 2, 3), finals[2])

    return jax.shard_map(device_step, mesh=sub,
                         in_specs=(tok_spec, tok_spec, route_spec, route_spec, whole_spec,
                                   expert_spec, expert_spec, expert_spec),
                         out_specs=(tok_spec, tok_spec, whole_spec, expert_spec, expert_spec, expert_spec),
                         check_vma=False)
```

```python
import functools

import jax
import jax.numpy as jnp
from jax import lax
from jax.experimental import pallas as pl
from jax.experimental.layout import Layout, with_layout_constraint
from jax.experimental.pallas import tpu as pltpu
from jax.sharding import Mesh, PartitionSpec as P

F32, BF16, I32 = jnp.float32, jnp.bfloat16, jnp.int32
MESH = pl.DeviceIdType.MESH
ROWS = 384
GRP = 8
PITCH = 9
HOT = 2
DEPTH = 3
FULL = 8
HALF = 4
CAP_FACTOR = 3
LANES = 128
N_SRC = 4
Y, CORE, X = 1, 2, 4
VMEM_LIMIT = 62 * 1024 * 1024
PER_TILE = ROWS // GRP
ROW_BOUND, ROW_GOFF, ROW_EXPERT, ROW_PARTNER, TAB_ROWS = 32, 33, 34, 35, 40
SLOT_GROUPS = 256


def cdiv(a, b):
    return (a + b - 1) // b


def spans(d):
    return [(LANES * j, min(LANES, d - LANES * j)) for j in range(cdiv(d, LANES))]


any_space = pl.BlockSpec(memory_space=pl.ANY)
in_vmem = pl.BlockSpec(memory_space=pltpu.VMEM)


def sorted_list(expert_ids, gate_vals):
    n_tok, top = expert_ids.shape
    n = n_tok * top
    keys = expert_ids.reshape(n) * n + jnp.arange(n, dtype=I32)
    keys, gates = lax.sort((keys, gate_vals.reshape(n)), num_keys=1, is_stable=False)
    return ((keys % n) // top).astype(F32), gates


def plan_kernel(n_layers, n_local, n_tok, list_rows, deal_ref, all_ref, tab_ref, idx_ref, gate_ref):
    n_mine = n_local // 2
    core, ep = lax.axis_index('core'), lax.axis_index('ep')
    list_len = list_rows * LANES
    lane = lambda n: lax.broadcasted_iota(I32, (n, LANES), 1).astype(F32)
    sub = lambda n: lax.broadcasted_iota(I32, (n, LANES), 0).astype(F32)
    over_lanes = lambda v: jnp.sum(v, axis=1, keepdims=True)
    over_subs = lambda v: jnp.sum(v, axis=0, keepdims=True)
    l16, s16 = lane(n_mine), sub(n_mine)
    groups = lambda c: jnp.floor((c + (GRP - 0.5)) * (1.0 / GRP))
    for l in range(n_layers):
        cnt = all_ref[:, 2 * n_layers * list_rows + l, :]
        ends = cnt
        step = 1
        while step < 2 * n_local:
            ends = ends + jnp.where(lane(N_SRC) >= step, pltpu.roll(ends, step, 1), 0.0)
            step *= 2
        starts = ends - cnt
        second = (ep > 0)
        local = lambda v: jnp.where(lane(v.shape[0]) < n_local,
                                    jnp.where(second, pltpu.roll(v, LANES - n_local, 1), v), 0.0)
        cnt, starts = local(cnt), local(starts)
        tiles = jnp.floor((over_subs(groups(local(deal_ref[:, l, :]))) + (PER_TILE - 0.5))
                          * (1.0 / PER_TILE))
        load = jnp.where(lane(1) < n_local, jnp.maximum(1.0, tiles), -1.0)
        wide = jnp.broadcast_to(load, (n_local, LANES))
        col = over_lanes(jnp.where(lane(n_local) == sub(n_local), wide, 0.0))
        ahead = (col > wide) | ((col == wide) & (sub(n_local) < lane(n_local)))
        rank = over_subs(jnp.where(ahead, 1.0, 0.0))
        odd = s16 - 2.0 * jnp.floor(s16 * 0.5 + 0.25)
        flip = jnp.where(core > 0, 1.0 - odd, odd)
        dealt = lambda f: (jnp.broadcast_to(rank, (n_mine, LANES)) == 2.0 * s16 + f) & (l16 < n_local)
        pick = dealt(flip)
        choose = lambda p, row: over_lanes(jnp.where(p, jnp.broadcast_to(row, (n_mine, LANES)), 0.0))
        mine = lambda row: choose(pick, row)
        as_row = lambda c: over_subs(jnp.where(l16 == s16, c, 0.0))
        experts = as_row(mine(lane(1)))
        partner = as_row(choose(dealt(1.0 - flip), lane(1)))
        at = l * TAB_ROWS
        off = jnp.zeros((n_mine, 1), F32)
        pos = [jnp.zeros((n_mine, LANES), F32) for _ in range(SLOT_GROUPS // LANES)]
        for s in range(N_SRC):
            c, st = mine(cnt[s:s + 1]), mine(starts[s:s + 1]) + float(s * list_len)
            ng = groups(c)
            for i in range(len(pos)):
                rel = l16 + float(LANES * i) - off
                code = (st + GRP * rel) * 16.0 + jnp.minimum(float(GRP), c - GRP * rel)
                pos[i] = jnp.where((rel >= 0) & (rel < ng), code, pos[i])
            off = off + ng
        for i in range(len(pos)):
            tab_ref[pl.ds(at + i, n_mine, stride=len(pos)), :] = pos[i].astype(I32)
        n_tiles = jnp.maximum(1.0, jnp.floor((off + (PER_TILE - 0.5)) * (1.0 / PER_TILE)))
        bounds = over_subs(jnp.where(s16 < l16, n_tiles, 0.0))
        before = over_lanes(jnp.where(l16 == s16, jnp.broadcast_to(bounds, (n_mine, LANES)), 0.0))
        t = jnp.minimum(l16, over_subs(jnp.broadcast_to(n_tiles, (n_mine, LANES))) - 1.0)
        inside = (t >= before) & (t < before + n_tiles)
        goff = over_subs(jnp.where(inside, s16 * float(SLOT_GROUPS) + (t - before) * float(PER_TILE), 0.0))
        rows = [(ROW_BOUND, bounds), (ROW_GOFF, goff), (ROW_EXPERT, experts), (ROW_PARTNER, partner)]
        for row, value in rows:
            tab_ref[at + row:at + row + 1, :] = value.astype(I32)
    for l in range(n_layers):
        pad = l * (N_SRC * list_rows + 8) + N_SRC * list_rows
        gate_ref[pad:pad + 8, :] = jnp.zeros((8, LANES), F32)
        for s in range(N_SRC):
            to = (l * N_SRC + s) * list_rows
            toks = all_ref[s, l * list_rows:(l + 1) * list_rows, :]
            idx_ref[to:to + list_rows, :] = ((toks + float(s * n_tok)) * float(PITCH)).astype(I32)
            to = l * (N_SRC * list_rows + 8) + s * list_rows
            gate_ref[to:to + list_rows, :] = all_ref[s, (n_layers + l) * list_rows:(n_layers + l + 1) * list_rows, :]


def plan_shapes(sizes):
    n_layers, _, _, list_rows = sizes
    rows = (n_layers * TAB_ROWS, n_layers * N_SRC * list_rows, n_layers * (N_SRC * list_rows + 8))
    return [jax.ShapeDtypeStruct((n, LANES), dt) for n, dt in zip(rows, (I32, I32, F32))]


def flat(tab, idx, gates):
    return tab.reshape(-1), idx.reshape(-1), gates


def plan(deal, shared, sizes):
    return flat(*pl.pallas_call(
        functools.partial(plan_kernel, *sizes),
        out_shape=plan_shapes(sizes),
        in_specs=[in_vmem] * 2, out_specs=[in_vmem] * 3,
        cost_estimate=pl.CostEstimate(flops=10 ** 7, bytes_accessed=10 ** 6, transcendentals=0),
        name="plan",
    )(deal, shared))


def expert_kernel(cfg, *refs):
    fwd, bwd, own, layer, n_blk, d, ff, n_exp, picks, row_id, list_len, p_f32, n_alias, got_layer = cfg
    save, load = fwd and not bwd, own and bwd and not fwd
    refs = list(refs)
    take = lambda n: [refs.pop(0) for _ in range(n)]
    tab_hbm, idx_hbm, gate_hbm = take(3)
    u_pieces = take(N_SRC) if not load else []
    dy_pieces = take(N_SRC) if bwd else []
    wg_hbm, wu_hbm, wd_hbm = take(3)
    ab_hbm, xu_hbm = take(2) if load else (None, None)
    prev = take(1)[0] if bwd and not own else None
    got = take(2) if got_layer is not None else None
    take(n_alias)
    y_outs = take(N_SRC) if fwd else []
    du_outs = take(N_SRC) if bwd and own else []
    grad, warm = take(2) if bwd and own else (None, None)
    finals = take(3) if bwd and not own or got_layer is not None else None
    sent = take(2) if bwd and not own else None
    ab_hbm, xu_hbm = take(2) if save else (ab_hbm, xu_hbm)
    tab_ref, idx, gate_ref, land, table, gat = take(6)
    acc, row_ref = take(2) if own else (None, None)
    gu_ref, wd_ref, g_ref, x_u = take(4)
    x_c = take(1)[0] if bwd else None
    ab_ref = take(1)[0]
    dh_ref = take(1)[0] if bwd else None
    h_ref = take(1)[0]
    dab_ref, sums = take(2) if bwd else (None, None)
    keep_buf = take(1)[0] if bwd and not own else None
    got_buf = take(1)[0] if got is not None else None
    list_sem, land_sem, w_sem = take(3)
    sum_sem = take(1)[0] if bwd else None
    keep_sem = take(1)[0] if bwd and not own else None
    read_sem, write_sem = take(2) if got is not None else (None, None)
    stage_f, out_sem = take(2) if own else (None, None)
    ab_sem, xu_sem = take(2) if save or load else (None, None)
    warm_buf, warm_sem = take(2) if bwd and own else (None, None)
    begin_e = 0 if own else HOT
    split = HOT + (n_exp - HOT) // 2

    copy = pltpu.make_async_copy
    cols = spans(d)
    lo = ff // 256 * 256
    hi = ff - lo
    dot = functools.partial(lax.dot_general, preferred_element_type=F32)
    nn = (((1,), (0,)), ((), ()))
    nt = (((1,), (1,)), ((), ()))
    tn = (((0,), (0,)), ((), ()))
    al = pl.multiple_of
    n_row = N_SRC * n_blk
    glane = lax.broadcasted_iota(I32, (GRP, LANES), 1)
    gsub = lax.broadcasted_iota(I32, (GRP, LANES), 0)

    def row_at(r):
        return pl.ds(r * PITCH, FULL)

    def codes_of(tile):
        at = ROW_GOFF * LANES + tile
        if own and bwd:
            return lambda q: tab_ref[tab_ref[at] + q]
        view = tab_ref.at[pl.ds(tab_ref[at], PER_TILE)]
        return lambda q: view[q]

    def gather(codes, q):
        ids = idx.at[pl.ds(codes(q) >> 4, GRP)]
        for k in range(GRP):
            gat[row_at(q * GRP + k), :] = table[pl.ds(ids[k], FULL), :]

    def gate_column(code):
        pos = code >> 4
        row, shift = pos >> 7, pos & (LANES - 1)
        want = glane == gsub + shift
        over = glane == gsub + (shift - LANES)
        here = gate_ref[pl.ds(row, GRP, stride=0), :]
        there = gate_ref[pl.ds(row + 1, GRP, stride=0), :]
        v = jnp.where(want, here, jnp.where(over, there, 0.0))
        return jnp.where(gsub < (code & 15), jnp.sum(v, axis=1, keepdims=True), 0.0)

    def scatter(codes, q):
        ids = idx.at[pl.ds(codes(q) >> 4, GRP)]
        new = []
        for k in range(GRP):
            at = pl.ds(ids[k], FULL)
            new.append((at, acc[at, :] + row_ref[row_at(q * GRP + k), :]))
        for at, value in reversed(new):
            acc[at, :] = value

    def keep_ab(t):
        ends = (ab_ref.at[t & 1], ab_hbm.at[t])
        return copy(*(ends if save else ends[::-1]), ab_sem.at[t & 1])

    def keep_xu(t):
        ends = (x_u.at[t & 1], xu_hbm.at[t])
        return copy(*(ends if save else ends[::-1]), xu_sem.at[t & 1])

    def of(ref, t):
        return ref.at[t & 1] if save or load else ref

    def convert(codes, t):
        for q in range(0, PER_TILE, 2):
            part = []
            for p in (q, q + 1):
                code = codes(p)
                rows = [gat[pl.ds(GRP * PITCH * p + j, GRP, stride=PITCH), :]
                        for j in range(HALF if load else 0, FULL if bwd else HALF)]
                real = gsub < (code & 15)
                gate = gate_column(code)
                g_ref[GRP * p:GRP * (p + 1), :] = gate
                us, dys = ([], rows) if load else (rows[:HALF], rows[HALF:])
                part.append([jnp.where(real, v, 0.0) for v in us] + [v * gate for v in dys])
            at = slice(GRP * q, GRP * (q + 2))
            for x, o in ((None if load else of(x_u, t), 0), (x_c, 0 if load else HALF)):
                if x is None:
                    continue
                for j, (c, w) in enumerate(cols):
                    both = jnp.concatenate([part[0][o + j], part[1][o + j]], axis=0)
                    x[at, c:c + w] = both[:, :w].astype(BF16)

    def put_rows(o, value, s0):
        value = value.astype(BF16).astype(F32)
        n = value.shape[0]
        for j, (c, w) in enumerate(cols):
            row_ref[pl.ds(PITCH * s0 + o + j, n, stride=PITCH), 0:w] = value[:, c:c + w] * g_ref[s0:s0 + n, 0:w]

    low = lax.broadcasted_iota(I32, (16, 2 * hi), 1) < hi

    def middle(a, b, dh):
        sig = 0.5 * jnp.tanh(0.5 * a) + 0.5
        act = a * sig
        h = act * b
        if dh is None:
            return h, None, None
        slope = sig * (1.0 + a * (1.0 - sig))
        return h, dh * b * slope, dh * act

    def weights(e, slot):
        at = (layer, tab_ref[ROW_EXPERT * LANES + e])
        moves = []
        for i, w in enumerate((wg_hbm, wu_hbm)):
            moves.append((w.at[at + (pl.ds(0, lo),)], gu_ref.at[slot, pl.ds(i * lo, lo)]))
            moves.append((w.at[at + (pl.ds(lo, hi),)], gu_ref.at[slot, pl.ds(2 * lo + i * hi, hi)]))
        moves.append((wd_hbm.at[at], wd_ref.at[slot]))
        return [copy(a, b, w_sem.at[slot, i]) for i, (a, b) in enumerate(moves)]

    def sums_in(e, slot):
        return copy(prev.at[e], sums.at[slot], sum_sem.at[slot])

    def sums_out(e, slot):
        return copy(sums.at[slot], grad.at[e], sum_sem.at[slot])

    def keeps(e, slot):
        at = (layer, tab_ref[ROW_EXPERT * LANES + e])
        return [copy(keep_buf.at[slot, i], finals[i].at[at], keep_sem.at[slot, i]) for i in range(3)]

    def send(e, slot, part):
        return copy(keep_buf.at[slot], sent[part].at[e - (split if part else HOT)], keep_sem.at[slot, 3])

    def read(e, slot, part=0):
        return copy(got[part].at[e - (split if part else HOT)], got_buf.at[slot], read_sem.at[slot])

    def warm_out(e):
        return copy(warm_buf, warm.at[e], warm_sem)

    def writes(e, slot):
        to = tab_ref[TAB_ROWS * LANES + e]
        return [copy(got_buf.at[slot, i], finals[i].at[got_layer, to], write_sem.at[slot, i]) for i in range(3)]

    def start(moves):
        for m in moves:
            m.start()

    def wait(moves):
        for m in moves:
            m.wait()

    n_tab = TAB_ROWS * LANES
    lists = [copy(tab_hbm.at[pl.ds(row_id * n_tab, n_tab)], tab_ref.at[pl.ds(0, n_tab)], list_sem.at[0]),
             copy(idx_hbm.at[pl.ds(row_id * N_SRC * list_len, N_SRC * list_len)], idx.at[pl.ds(0, N_SRC * list_len)],
                  list_sem.at[1]),
             copy(gate_hbm.at[pl.ds(row_id * gate_ref.shape[0], gate_ref.shape[0])], gate_ref, list_sem.at[2])]
    if got is not None:
        at = (got_layer * TAB_ROWS + ROW_PARTNER) * LANES
        lists.append(copy(tab_hbm.at[pl.ds(at, LANES)], tab_ref.at[pl.ds(n_tab, LANES)], list_sem.at[3]))
    start(lists)
    pieces = []
    for s in range(N_SRC):
        if not load:
            pieces.append((u_pieces[s], picks[0][s], s, 0, fwd))
        if bwd:
            pieces.append((dy_pieces[s], picks[1][s], s, HALF, own))
    lands = [copy(ref.at[pick], land.at[i % N_SRC], land_sem.at[i % N_SRC]) for i, (ref, pick, *_) in enumerate(pieces)]
    start(lands[:N_SRC])
    lists[0].wait()
    for e in range(begin_e, begin_e + DEPTH - 1):
        start(weights(e, e % DEPTH))
        if bwd and not own:
            sums_in(e, e % DEPTH).start()
    if got is not None:
        lists[3].wait()
        read(HOT, HOT % 2).start()
    if own:
        def clear(c, _):
            for k in range(4):
                acc[pl.ds(al(c * 1152 + 288 * k, 8), 288), :] = jnp.zeros((288, LANES), F32)
            return 0

        lax.fori_loop(0, acc.shape[0] // 1152, clear, 0)
        row_ref[...] = jnp.zeros(row_ref.shape, F32)
    rows = 256
    for i, (_, _, s, o, seed) in enumerate(pieces):
        lands[i].wait()

        def fill(c, _, i=i, o=o, seed=seed, s=s):
            r = al(c * rows, rows)
            for j in range(HALF):
                vals = land[i % N_SRC, pl.ds(r, rows), LANES * j:LANES * (j + 1)].astype(F32)
                to = pl.ds(PITCH * (s * n_blk + r) + o + j, rows, stride=PITCH)
                table[to, :] = vals
                if seed and s == 0:
                    acc[to, :] = vals
            return 0

        lax.fori_loop(0, n_blk // rows, fill, 0)
        if i + N_SRC < len(pieces):
            lands[i + N_SRC].start()
    wait(lists[1:3])
    for k in range(GRP):
        idx[N_SRC * list_len + k] = 0

    def first(q, _):
        gather(begin, 2 * q)
        gather(begin, 2 * q + 1)
        return 0

    first_tile = tab_ref[ROW_BOUND * LANES + begin_e]
    begin = codes_of(first_tile)
    lax.fori_loop(0, PER_TILE // 2, first, 0)
    convert(begin, 0)
    if save:
        keep_xu(0).start()
    if load:
        keep_ab(0).start()
        keep_xu(0).start()

    def expert(e, _):
        slot = e & 1
        deep = lax.rem(e, DEPTH)
        sum_slot = slot if own else deep
        wait(weights(e, deep))
        if bwd and not own:
            sums_in(e, deep).wait()
        if got is not None:
            @pl.when(e >= HOT)
            def _():
                read(HOT, slot).wait()
                start(writes(e, slot))

            @pl.when((e > HOT) & (e < n_exp - 1))
            def _():
                wait(writes(e - 1, 1 - slot))

        @pl.when(e < n_exp - (DEPTH - 1))
        def _():
            ahead = lax.rem(e + DEPTH - 1, DEPTH)
            start(weights(e + DEPTH - 1, ahead))
            if bwd and not own:
                sums_in(e + DEPTH - 1, ahead).start()

        if got is not None:
            for part in range(2):
                @pl.when((e + 1 >= split) & (e < n_exp - 1) if part else (e + 1 > HOT) & (e + 1 < split))
                def _(part=part):
                    read(e + 1, 1 - slot, part).start()

        if bwd and own:
            @pl.when(e > 1)
            def _():
                sums_out(e - 2, slot).wait()

            sums[slot] = jnp.zeros(sums.shape[1:], F32)

        def tile(t, _):
            if save:
                @pl.when(t > 1)
                def _():
                    keep_ab(t - 2).wait()

                @pl.when(t > 0)
                def _():
                    keep_xu(t - 1).wait()
            if load:
                keep_ab(t).wait()
                keep_xu(t).wait()
                keep_ab(t + 1).start()
                keep_xu(t + 1).start()
            ab, xu = of(ab_ref, t), of(x_u, t)
            before, after = codes_of(jnp.maximum(t - 1, first_tile)), codes_of(t + 1)
            for q in range(PER_TILE):
                if own:
                    scatter(before, q)
                gather(after, q)
            half = ROWS // 2
            for s0 in range(0, ROWS, half):
                sl = slice(s0, s0 + half)
                if not load:
                    ab[sl, :] = dot(xu[sl, :], gu_ref[deep], nt)
                if bwd:
                    dh_ref[sl, :] = dot(x_c[sl, :], wd_ref[deep], nt)
            for r in range(0, ROWS, 16):
                rows = slice(r, r + 16)
                for c in range(0, lo, LANES):
                    h, da, db = middle(ab[rows, c:c + LANES], ab[rows, lo + c:lo + c + LANES],
                                       dh_ref[rows, c:c + LANES] if bwd else None)
                    h_ref[rows, c:c + LANES] = h.astype(BF16)
                    if bwd:
                        dab_ref[rows, c:c + LANES] = da.astype(BF16)
                        dab_ref[rows, lo + c:lo + c + LANES] = db.astype(BF16)
                a = ab[rows, 2 * lo:]
                b = pltpu.roll(a, hi, 1)
                dh = dh_ref[rows, lo:] if bwd else None
                if bwd:
                    dh = jnp.concatenate([dh, dh], axis=1)
                h, da, db = middle(a, b, dh)
                h_ref[rows, lo:] = h[:, :hi].astype(BF16)
                if bwd:
                    dab_ref[rows, 2 * lo:] = jnp.where(low, da, pltpu.roll(db, hi, 1)).astype(BF16)
            for s0 in range(0, ROWS, half):
                sl = slice(s0, s0 + half)
                if fwd:
                    put_rows(0, dot(h_ref[sl, :], wd_ref[deep], nn), s0)
                if bwd and own:
                    put_rows(HALF, dot(dab_ref[sl, :], gu_ref[deep], nn), s0)
            if bwd:
                view = sums.at[sum_slot]
                view[0:2 * ff, :] += dot(dab_ref[...], xu[...], tn)
                view[2 * ff:, :] += dot(h_ref[...], x_c[...], tn)
            convert(after, t + 1)
            if save:
                keep_ab(t).start()
                keep_xu(t + 1).start()
            return 0

        lax.fori_loop(tab_ref[ROW_BOUND * LANES + e], tab_ref[ROW_BOUND * LANES + e + 1], tile, 0)
        if bwd and own:
            sums_out(e, slot).start()

            @pl.when(e < HOT)
            def _():
                @pl.when(e > 0)
                def _():
                    warm_out(0).wait()

                warm_buf[...] = sums[slot].astype(BF16)
                warm_out(e).start()
        if bwd and not own:
            @pl.when(e > HOT + 1)
            def _():
                wait(keeps(e - 2, slot) + [send(HOT, slot, 0)])

            for i in range(2):
                keep_buf[slot, i, 0:lo, :] = sums[deep, i * lo:(i + 1) * lo, :].astype(BF16)
                keep_buf[slot, i, lo:, :] = sums[deep, 2 * lo + i * hi:2 * lo + (i + 1) * hi, :].astype(BF16)
            keep_buf[slot, 2] = sums[deep, 2 * ff:, :].astype(BF16)
            start(keeps(e, slot))
            for part in range(2):
                @pl.when((e >= split) if part else (e < split))
                def _(part=part):
                    send(e, slot, part).start()
        return 0

    lax.fori_loop(begin_e, n_exp, expert, 0)
    ends = ((n_exp - 2, (n_exp - 2) % 2), (n_exp - 1, (n_exp - 1) % 2))
    n_tiles = tab_ref[ROW_BOUND * LANES + n_exp]
    if save:
        wait([keep_ab(n_tiles - 2), keep_ab(n_tiles - 1), keep_xu(n_tiles - 1)])
    if save or load:
        keep_xu(n_tiles).wait()
    if load:
        keep_ab(n_tiles).wait()
    if own:
        end = codes_of(tab_ref[ROW_BOUND * LANES + n_exp] - 1)
        lax.fori_loop(0, PER_TILE, lambda q, _: (scatter(end, q), 0)[1], 0)
        flights = {}
        for o, out in ((HALF, du_outs), (0, y_outs)):
            for s in range(N_SRC if out else 0):
                wide = s == 0 or p_f32
                stage = stage_f.at[s] if wide else land.at[s]
                if s in flights:
                    flights[s].wait()

                def fetch(c, _, stage=stage, s=s, o=o):
                    r = al(c * rows, rows)
                    for j in range(HALF):
                        at = pl.ds(PITCH * (s * n_blk + r) + o + j, rows, stride=PITCH)
                        stage[pl.ds(r, rows), LANES * j:LANES * (j + 1)] = acc[at, :].astype(stage.dtype)
                    return 0

                lax.fori_loop(0, n_blk // rows, fetch, 0)
                flights[s] = copy(stage, out[s], out_sem.at[s])
                flights[s].start()
        wait(flights.values())
        if bwd:
            for e, slot in ends:
                sums_out(e, slot).wait()
            warm_out(0).wait()
    else:
        for e, slot in ends:
            wait(keeps(e, slot) + [send(HOT, slot, 0)])
    if got is not None:
        for e, slot in ends:
            wait(writes(e, slot))


def run_experts(routes, layer, u, dy, weights, prev, finals, fwd, own, p_f32=False, got=None, kept=None):
    tab, idx, gates = routes
    bwd = dy is not None
    wg, wu, wd = weights
    save, load = fwd and not bwd, kept is not None
    n_blk, wide = (dy or u)[0][0].shape[-2:]
    n_layers, n_local, ff, d = wd.shape
    n_exp = n_local // 2
    row_id = layer
    list_len = idx.shape[0] // (n_layers * N_SRC)

    arrays = lambda pieces: [v for v, _ in pieces]
    operands = [tab, idx, gates] + ([] if load else arrays(u)) + (arrays(dy) if bwd else []) + [wg, wu, wd] + list(kept or ())
    out_shape, aliases = [], {}
    for use in (fwd, bwd and own):
        if use:
            out_shape += [jax.ShapeDtypeStruct((n_blk, wide), F32 if s == 0 or p_f32 else BF16) for s in range(N_SRC)]
    if bwd and own:
        out_shape += [jax.ShapeDtypeStruct((n_exp, 3 * ff, d), F32), jax.ShapeDtypeStruct((HOT, 3 * ff, d), BF16)]
    if bwd and not own:
        operands.append(prev)
    if got is not None:
        operands += got
    for i, f in enumerate(finals or ()):
        aliases[len(operands)] = len(out_shape) + i
        operands.append(f)
    if bwd and not own or finals:
        out_shape += [jax.ShapeDtypeStruct((n_layers, n_local, ff, d), BF16)] * 3
    if bwd and not own:
        out_shape += [jax.ShapeDtypeStruct(((n_exp - HOT) // 2, 3, ff, d), BF16)] * 2
    if save:
        most = n_exp * (SLOT_GROUPS // PER_TILE) + 2
        out_shape += [jax.ShapeDtypeStruct((most, ROWS, 2 * ff), F32), jax.ShapeDtypeStruct((most, ROWS, d), BF16)]
    sem = lambda *s: pltpu.SemaphoreType.DMA(s)
    mid = lambda n, dt: pltpu.VMEM((ROWS, n), dt)
    twin = lambda n, dt: pltpu.VMEM((2, ROWS, n), dt) if save or load else mid(n, dt)
    table, rows = pltpu.VMEM((PITCH * N_SRC * n_blk, LANES), F32), pltpu.VMEM((PITCH * ROWS, LANES), F32)
    scratch = [pltpu.SMEM(((TAB_ROWS + 1) * LANES,), I32), pltpu.SMEM((N_SRC * list_len + LANES,), I32),
               pltpu.VMEM((N_SRC * list_len // LANES + 8, LANES), F32), pltpu.VMEM((N_SRC, n_blk, wide), BF16)]
    scratch += [table, rows] * (1 + own)
    scratch += [pltpu.VMEM((DEPTH, 2 * ff, d), BF16), pltpu.VMEM((DEPTH, ff, d), BF16), mid(LANES, F32)]
    scratch += [twin(d, BF16)] + [mid(d, BF16)] * bwd + [twin(2 * ff, F32)] + [mid(ff, F32)] * bwd + [mid(ff, BF16)]
    scratch += [mid(2 * ff, BF16), pltpu.VMEM((2 if own else DEPTH, 3 * ff, d), F32)] * bwd
    if bwd and not own:
        scratch.append(pltpu.VMEM((2, 3, ff, d), BF16))
    if got is not None:
        scratch.append(pltpu.VMEM((2, 3, ff, d), BF16))
    scratch += [sem(4), sem(N_SRC), sem(DEPTH, 5)] + [sem(DEPTH)] * bwd
    if bwd and not own:
        scratch.append(sem(2, 4))
    if got is not None:
        scratch += [sem(2), sem(2, 3)]
    if own:
        scratch += [pltpu.VMEM((N_SRC if p_f32 else 1, n_blk, wide), F32), sem(N_SRC)]
    if save or load:
        scratch += [sem(2), sem(2)]
    if bwd and own:
        scratch += [pltpu.VMEM((3 * ff, d), BF16), pltpu.SemaphoreType.DMA]
    passes = 2 + fwd + bwd * (4 + 2 * own)
    flops = 2 * d * ff * passes * n_blk * N_SRC * 2
    hoist = 1400 if not own else 600 if load else 750 if save else 700
    picks = [[i for _, i in u] if u else None, [i for _, i in dy] if bwd else None]
    cfg = (fwd, bwd, own, layer, n_blk, d, ff, n_exp, picks, row_id, list_len, p_f32, len(aliases),
           None if got is None else 1 - layer)
    return pl.pallas_call(
        functools.partial(expert_kernel, cfg),
        out_shape=out_shape,
        in_specs=[any_space] * len(operands),
        out_specs=[any_space] * len(out_shape),
        scratch_shapes=scratch,
        input_output_aliases=aliases,
        compiler_params=pltpu.CompilerParams(
            vmem_limit_bytes=VMEM_LIMIT),
        cost_estimate=pl.CostEstimate(flops=flops, bytes_accessed=3 * 2 * n_exp * d * ff, transcendentals=0),
        name=f"experts_{'f' if fwd else ''}{'b' if bwd else ''}_{'own' if own else 'other'}_{layer}",
    )(*operands)


def place_kernel(layer, n_exp, tab_ref, got_ref, *refs):
    outs, (buf, in_sem, out_sem) = refs[3:6], refs[6:]
    reads = [pltpu.make_async_copy(got_ref.at[i], buf.at[i], in_sem.at[i]) for i in range(n_exp)]
    for read in reads:
        read.start()
    writes = []
    for i, read in enumerate(reads):
        read.wait()
        e = tab_ref[i]
        for k, out in enumerate(outs):
            writes.append(pltpu.make_async_copy(buf.at[i, k], out.at[layer, e], out_sem.at[i, k]))
            writes[-1].start()
    for write in writes:
        write.wait()


def place(partner, layer, got, finals):
    n_exp = got.shape[0]
    return pl.pallas_call(
        functools.partial(place_kernel, layer, n_exp),
        out_shape=[jax.ShapeDtypeStruct(f.shape, f.dtype) for f in finals],
        grid_spec=pltpu.PrefetchScalarGridSpec(
            num_scalar_prefetch=1, grid=(1,), in_specs=[any_space] * 4, out_specs=[any_space] * 3,
            scratch_shapes=[pltpu.VMEM(got.shape, got.dtype), pltpu.SemaphoreType.DMA((n_exp,)),
                            pltpu.SemaphoreType.DMA((n_exp, 3))]),
        input_output_aliases={2: 0, 3: 1, 4: 2},
        compiler_params=pltpu.CompilerParams(vmem_limit_bytes=VMEM_LIMIT),
        cost_estimate=pl.CostEstimate(flops=0, bytes_accessed=4 * got.size, transcendentals=0),
        name=f"place_{layer}",
    )(partner, got, *finals)


def place_hot_kernel(ff, tab_ref, *refs):
    sums, (outs, (buf, in_sem, out_sem)) = refs[:4], (refs[7:10], refs[10:])
    lo = ff // 256 * 256
    hi = ff - lo
    places = [(0, 0, lo, 0), (1, 0, lo, lo), (0, lo, hi, 2 * lo), (1, lo, hi, 2 * lo + hi), (2, 0, ff, 2 * ff)]
    reads, writes = [], []
    for i, ref in enumerate(sums):
        for k in range(HOT):
            reads.append(pltpu.make_async_copy(ref.at[k], buf.at[i * HOT + k], in_sem.at[i * HOT + k]))
            reads[-1].start()
    for n, read in enumerate(reads):
        read.wait()
        e = tab_ref[n]
        for j, (out, at, size, row) in enumerate(places):
            writes.append(pltpu.make_async_copy(buf.at[n, pl.ds(row, size)], outs[out].at[n // (2 * HOT), e, pl.ds(at, size)],
                                                out_sem.at[n, j]))
            writes[-1].start()
    for write in writes:
        write.wait()


def place_hot(experts, sums, finals):
    _, rows, d = sums[0].shape
    n = len(sums) * HOT
    return pl.pallas_call(
        functools.partial(place_hot_kernel, rows // 3),
        out_shape=[jax.ShapeDtypeStruct(f.shape, f.dtype) for f in finals],
        grid_spec=pltpu.PrefetchScalarGridSpec(
            num_scalar_prefetch=1, grid=(1,), in_specs=[any_space] * 7, out_specs=[any_space] * 3,
            scratch_shapes=[pltpu.VMEM((n, rows, d), BF16), pltpu.SemaphoreType.DMA((n,)), pltpu.SemaphoreType.DMA((n, 5))]),
        input_output_aliases={5: 0, 6: 1, 7: 2},
        compiler_params=pltpu.CompilerParams(vmem_limit_bytes=VMEM_LIMIT),
        cost_estimate=pl.CostEstimate(flops=0, bytes_accessed=4 * n * rows * d, transcendentals=0),
        name="place_hot",
    )(experts, *sums, *finals)


def peer(rel):
    return {name: (lax.axis_index(name) + ((rel >> bit) & 1)) % 2 for bit, name in enumerate(("ep", "core", "x"))}


def meet(rels):
    barrier = pltpu.get_barrier_semaphore()
    for rel in rels:
        pl.semaphore_signal(barrier, inc=1, device_id=peer(rel), device_id_type=MESH)
    pl.semaphore_wait(barrier, len(rels))


def remote(src, dst, send, recv, rel):
    return pltpu.make_async_remote_copy(src_ref=src, dst_ref=dst, send_sem=send, recv_sem=recv,
                                        device_id=peer(rel), device_id_type=MESH)


def share_kernel(n_src, mine_ref, all_ref, cnt_ref, send_sem, recv_sem):
    n_rel = 2 * n_src
    count_rows = cnt_ref.shape[1]
    counts = mine_ref.at[pl.ds(mine_ref.shape[0] - count_rows, count_rows)]
    meet(range(1, n_rel))
    copies = [remote(counts, cnt_ref.at[rel], send_sem.at[0, rel], recv_sem.at[0, rel], rel) for rel in range(1, n_rel)]
    copies += [remote(mine_ref, all_ref.at[rel], send_sem.at[1, rel], recv_sem.at[1, rel], rel) for rel in range(1, n_src)]
    for copy in copies:
        copy.start()
    all_ref[0] = mine_ref[...]
    cnt_ref[0] = counts[...]
    for copy in copies:
        copy.wait()


def share(mine, n_src, count_rows=8):
    n_rel = 2 * n_src
    return pl.pallas_call(
        functools.partial(share_kernel, n_src),
        out_shape=[jax.ShapeDtypeStruct((n_src,) + mine.shape, mine.dtype),
                   jax.ShapeDtypeStruct((n_rel, count_rows, mine.shape[1]), mine.dtype)],
        in_specs=[in_vmem],
        out_specs=[in_vmem] * 2,
        scratch_shapes=[pltpu.SemaphoreType.DMA((2, n_rel)), pltpu.SemaphoreType.DMA((2, n_rel))],
        compiler_params=pltpu.CompilerParams(collective_id=0, has_side_effects=True),
        cost_estimate=pl.CostEstimate(flops=10 ** 7, bytes_accessed=mine.size * 4 * n_rel, transcendentals=0),
        name="share_lists",
    )(mine)


def blocks_kernel(cfg, *refs):
    n_chunk, reduce, back, d, sizes = cfg
    refs = list(refs)
    take = lambda n: [refs.pop(0) for _ in range(n)]
    parts = take(N_SRC)
    m_ref = take(1)[0]
    list_refs, left_ref = take(2) if sizes else (), take(1)[0] if back else None
    o_total, o_a, o_b = take(3)
    plan_refs, grad_ref = take(3) if sizes else (), take(1)[0] if back else None
    in_f, in_b, got_f, s_wire, r_wire, u_wire, y_wire, t_buf, u_buf, y_buf, load, send, recv, put = take(14)
    n_rows = t_buf.shape[0] // n_chunk
    cut = [pl.ds(k * n_rows, n_rows) for k in range(n_chunk)]
    thin = [pl.ds(k * n_rows // 2, n_rows // 2) for k in range(n_chunk)]
    side = lax.broadcasted_iota(I32, (n_rows // 2, LANES), 1) < LANES // 2
    tiles = d // LANES
    turn = lambda v: pltpu.roll(v, LANES // 2, 1)
    lanes = lambda v, j: v[:, LANES * j:LANES * (j + 1)]

    def pack(wire, k, value):
        top, low = value[:n_rows // 2], value[n_rows // 2:]
        turned = [turn(lanes(low, j)) for j in range(tiles + 1)]
        parts = [lanes(top, j) for j in range(tiles)] + [jnp.where(side, lanes(top, tiles), turned[0])]
        parts += [jnp.where(side, turned[j], turned[j + 1]) for j in range(tiles)]
        for j, part in enumerate(parts):
            wire[thin[k], LANES * j:LANES * (j + 1)] = part.astype(BF16)

    def unpack(wire, k):
        value = wire[thin[k], :].astype(F32)
        turned = [turn(lanes(value, tiles + j)) for j in range(tiles + 1)]
        top = [lanes(value, j) for j in range(tiles)] + [jnp.where(side, lanes(value, tiles), 0.0)]
        low = [jnp.where(side, turned[j], turned[j + 1]) for j in range(tiles)] + [jnp.where(side, turned[tiles], 0.0)]
        return jnp.concatenate([jnp.concatenate(top, axis=1), jnp.concatenate(low, axis=1)], axis=0)

    chunks = range(n_chunk)
    loads = {}
    for i, part in enumerate(parts[:2] if reduce else parts):
        buf = in_f.at[i] if reduce or i == 0 else in_b.at[i - 1]
        for k in chunks:
            loads[i, k] = pltpu.make_async_copy(part.at[cut[k]], buf.at[cut[k]], load.at[i, k])
    order = (1, 0) if reduce else range(N_SRC)
    for i in order:
        for k in chunks:
            loads[i, k].start()
    u_buf[...] = jnp.zeros(u_buf.shape, BF16)
    meet((Y, CORE))
    links = []
    copy_in = pltpu.make_async_copy

    def link(src, dst, rel, cut=cut):
        n = len(links)
        links.append([remote(src.at[cut[k]], dst.at[cut[k]], send.at[n, k], recv.at[n, k], rel) for k in chunks])
        return links[-1]

    if reduce:
        first = link(parts[3], got_f.at[1], CORE)
        second = link(parts[2], got_f.at[0], CORE)
        over = link(s_wire, r_wire, Y, thin)
        for copies in (first, second):
            for copy in copies:
                copy.start()
        for k in chunks:
            loads[1, k].wait()
            first[k].wait_recv()
            pack(s_wire, k, in_f[1, cut[k], :] + got_f[1, cut[k], :])
            over[k].start()
    to_y = link(u_wire, y_wire, Y, thin)
    to_core = link(u_buf, o_b.at[0], CORE)
    puts = []
    for k in chunks:
        if reduce:
            loads[0, k].wait()
            second[k].wait_recv()
            over[k].wait_recv()
            total = in_f[0, cut[k], :] + got_f[0, cut[k], :] + unpack(r_wire, k)
        else:
            for i in range(N_SRC):
                loads[i, k].wait()
            total = in_f[0, cut[k], :]
            for i in range(N_SRC - 1):
                total = total + in_b[i, cut[k], :].astype(F32)
        total = total.astype(BF16)
        t_buf[cut[k], :] = total
        dims = (((1,), (1 if back else 0,)), ((), ()))
        mixed = lax.dot_general(total[:, :d], m_ref[...], dims, preferred_element_type=F32)
        u_buf[cut[k], 0:d] = (total[:, :d].astype(F32) + mixed).astype(BF16)
        pack(u_wire, k, u_buf[cut[k], :].astype(F32))
        to_y[k].start()
        to_core[k].start()
        puts.append(pltpu.make_async_copy(u_buf.at[cut[k]], o_a.at[0, cut[k]], put.at[0, k]))
        puts.append(pltpu.make_async_copy(t_buf.at[cut[k]], o_total.at[cut[k]], put.at[1, k]))
        for copy in puts[-2:]:
            copy.start()
    if sizes:
        plan_kernel(*sizes, *list_refs, *plan_refs)
    if back:
        grad_ref[...] = lax.dot_general(left_ref[:, :d], t_buf[:, :d], (((0,), (0,)), ((), ())), preferred_element_type=F32)
    on = link(y_buf, o_b.at[1], CORE)
    for k in chunks:
        to_y[k].wait_recv()
        y_buf[cut[k], :] = unpack(y_wire, k).astype(BF16)
        on[k].start()
        puts.append(copy_in(y_buf.at[cut[k]], o_a.at[1, cut[k]], put.at[2, k]))
        puts[-1].start()
    waited = [to_y] + ([first, second, over] if reduce else [])
    for copies in links:
        for copy in copies:
            if any(copies is w for w in waited):
                copy.wait_send()
            else:
                copy.wait()
    for copy in puts:
        copy.wait()


def complete_blocks(parts, m, reduce, back, ident, sizes=None, lists=(), left=(), n_chunk=4):
    n_blk, wide = parts[0].shape
    d = m.shape[0]
    sem = lambda *s: pltpu.SemaphoreType.DMA(s)
    pair = jax.ShapeDtypeStruct((2, n_blk, wide), BF16)
    extra = plan_shapes(sizes) if sizes else []
    extra += [jax.ShapeDtypeStruct((d, d), F32)] * len(left)
    buf = lambda n, dt: pltpu.VMEM((n, n_blk, wide) if n else (n_blk, wide), dt)
    return pl.pallas_call(
        functools.partial(blocks_kernel, (n_chunk, reduce, back, d, sizes)),
        out_shape=[jax.ShapeDtypeStruct((n_blk, wide), BF16)] + [pair] * 2 + extra,
        in_specs=[any_space] * N_SRC + [in_vmem] * (1 + len(lists) + len(left)),
        out_specs=[any_space] * 3 + [in_vmem] * len(extra),
        scratch_shapes=[buf(2, F32), buf(3, BF16), buf(2, F32)] + [pltpu.VMEM((n_blk // 2, 2 * d), BF16)] * 4 + [
            buf(0, BF16), buf(0, BF16), buf(0, BF16), sem(4, n_chunk), sem(6, n_chunk), sem(6, n_chunk), sem(3, n_chunk)],
        compiler_params=pltpu.CompilerParams(collective_id=ident, has_side_effects=True, vmem_limit_bytes=VMEM_LIMIT),
        cost_estimate=pl.CostEstimate(flops=10 ** 8, bytes_accessed=n_blk * wide * 40, transcendentals=0),
        name=f"complete_blocks_{ident}",
    )(*parts, m, *lists, *left)


def solution(mesh):
    ep_size, dp_size = mesh.shape['ep'], mesh.shape['dp']
    sub = Mesh(mesh.devices.reshape(ep_size, dp_size // 2, 2), ('ep', 'x', 'core'))
    tok_axes = ('x', 'core', 'ep')
    tok_spec = P(tok_axes, None)
    route_spec = P(None, tok_axes, None)
    whole_spec = P(None, None, None)
    expert_spec = P(None, 'ep', None, None)
    flip = [(0, 1), (1, 0)]
    move = lambda v, axis: lax.ppermute(v, axis, flip)
    move_diag = lambda v: lax.ppermute(v, ('ep', 'core'), [(0, 3), (1, 2), (2, 1), (3, 0)])
    fence = lax.optimization_barrier

    def device_step(tokens, d_out, expert_ids, gate_vals, w_mix, w_gate, w_up, w_down):
        n_layers, d = w_mix.shape[0], w_mix.shape[1]
        n_tok = tokens.shape[0]
        top = expert_ids.shape[2]
        n_local = w_gate.shape[1]
        n_exp = n_local * ep_size
        n = n_tok * top
        n_rel = 2 * N_SRC
        wide = cdiv(d, LANES) * LANES
        weights = (jnp.swapaxes(w_gate, 2, 3), jnp.swapaxes(w_up, 2, 3), w_down)
        pad = lambda v: jnp.pad(v, ((0, 0), (0, wide - d)))
        send_three = lambda p: [move(p[1], 'ep'), move(p[2], 'core'), move_diag(p[3])]

        def own_sum(p, got):
            return sum([g.astype(F32) for g in got], p)[:, :d].astype(BF16)

        one = lambda v: v.reshape(1, n_tok, wide)
        pairs = lambda a, b: [(a, 0), (a, 1), (b, 0), (b, 1)]

        one = lambda v: v.reshape(1, n_tok, wide)
        pairs = lambda a, b: [(a, 0), (a, 1), (b, 0), (b, 1)]
        singles = lambda *v: [(one(a), 0) for a in v]

        u0 = pad((tokens.astype(F32) + jnp.dot(tokens, w_mix[0], preferred_element_type=F32)).astype(BF16))
        u0_y, u0_c = move(u0, 'ep'), move(u0, 'core')
        lists = [sorted_list(expert_ids[l], gate_vals[l]) for l in range(n_layers)]
        counts = jnp.sum((expert_ids.reshape(n_layers, n, 1) == jnp.arange(n_exp, dtype=I32)).astype(F32), axis=1)
        packed = jnp.concatenate([jnp.concatenate([v[0] for v in lists] + [v[1] for v in lists]).reshape(-1, LANES),
                                  jnp.pad(counts, ((0, 8 - n_layers), (0, LANES - n_exp)))], axis=0)
        dy = pad(d_out)
        u0_y, u0_c, packed, dy = fence((u0_y, u0_c, packed, dy))
        u0_d = move(u0_y, 'core')
        shared, cnt = share(packed, N_SRC)
        dy, shared = fence((dy, shared))
        shared_x = move(shared, 'x')
        dy_y, dy_x = move(dy, 'ep'), move(dy, 'x')
        sizes = (n_layers, n_local, n_tok, n // LANES)
        routes = plan(cnt, shared, sizes)
        u0_half = singles(u0, u0_y, u0_c, u0_d)
        *part, ab0, xu0 = run_experts(routes, 0, u0_half, None, weights, None, None, True, True, p_f32=True)
        dy_y, dy_x, shared_x, part = fence((dy_y, dy_x, shared_x, part))
        dy_c, dy_d, dy_xy, dy_xc = move(dy, 'core'), move(dy_y, 'core'), move(dy_y, 'x'), move(dy_x, 'core')
        y0, u1_a, u1_b, *routes_x = complete_blocks(part, w_mix[1], True, False, 1, sizes, (cnt, shared_x))
        routes_x = flat(*routes_x)
        dy_c, dy_d, dy_xy, dy_xc, u0_p, u0_q, y0, u1_a, u1_b = fence(
            (dy_c, dy_d, dy_xy, dy_xc, u0, u0_y, y0, u1_a, u1_b))
        dy_xd = move(dy_xy, 'core')
        u1_xa = move(u1_a, 'x')
        out = run_experts(routes, 1, pairs(u1_a, u1_b), singles(dy, dy_y, dy_c, dy_d), weights, None, None, True, True)
        u1_xa, dy_xd, u0_p, u0_q, out = fence((u1_xa, dy_xd, u0_p, u0_q, out))
        y_part, du_part, g1, warm1 = out[:4], out[4:8], out[8], out[9]
        u1_xb = move(u1_xa, 'core')
        got = send_three(du_part)
        warm1_x = move(warm1, 'x')
        u0_x, u0_xy = move(u0_p, 'x'), move(u0_q, 'x')
        out = run_experts(routes_x, 1, pairs(u1_xa, u1_xb), singles(dy_x, dy_xy, dy_xc, dy_xd), weights, g1, None,
                          False, False)
        got, u0_x, u0_xy, warm1_x, out = fence((got, u0_x, u0_xy, warm1_x, out))
        *finals, sent_a, sent_b = out
        got1 = [move(sent_a, 'core'), move(sent_b, 'core')]
        du1, dx_a, dx_b, g_mix1 = complete_blocks([du_part[0], *got], w_mix[1], False, True, 2, left=(y0,))
        tx = lambda x, du: jnp.einsum('td,te->de', x, du, preferred_element_type=F32)
        both = lambda a, b: (a.astype(F32) + b.astype(F32)).astype(BF16)
        hot1 = both(warm1, warm1_x)
        dx_a, y_part, got1, u0_x, u0_xy, g_mix1, hot1 = fence((dx_a, y_part, got1, u0_x, u0_xy, g_mix1, hot1))
        hot1_c = move(hot1, 'core')
        dx_xa = move(dx_a, 'x')
        theirs1 = move(g_mix1, 'core')
        got_y = send_three(y_part)
        u0_xc, u0_xd = move(u0_x, 'core'), move(u0_xy, 'core')
        out = run_experts(routes, 0, None, pairs(dx_a, dx_b), weights, None, finals, False, True, got=got1, kept=(ab0, xu0))
        dx_xa, got_y, u0_xc, u0_xd, theirs1, hot1_c, out = fence((dx_xa, got_y, u0_xc, u0_xd, theirs1, hot1_c, out))
        du_part, g0, warm0, finals = out[:4], out[4], out[5], out[6:]
        warm0_x = move(warm0, 'x')
        dx_xb = move(dx_xa, 'core')
        got = send_three(du_part)
        part1 = (g_mix1 + theirs1).astype(BF16)
        theirs1 = move(part1, 'ep')
        du_part, dx_xb, part1 = fence((du_part, dx_xb, part1))
        out = run_experts(routes_x, 0, singles(u0_x, u0_xy, u0_xc, u0_xd), pairs(dx_xa, dx_xb), weights, g0, finals,
                          False, False)
        got, theirs1, got_y, y_own, warm0_x, out = fence((got, theirs1, got_y, y_part[0], warm0_x, out))
        *finals, sent_a, sent_b = out
        hot0 = both(warm0, warm0_x)
        got_a, got_b, hot0_c = move(sent_a, 'core'), move(sent_b, 'core'), move(hot0, 'core')
        add = lambda a, b: a.astype(F32) + b.astype(F32)
        part1 = add(part1, theirs1).astype(BF16)
        theirs1 = move(part1, 'x')
        du0 = own_sum(du_part[0], got)
        part0 = tx(tokens, du0).astype(BF16)
        theirs0 = move(part0, 'ep')
        dx0 = (du0.astype(F32) + jnp.einsum('te,de->td', du0, w_mix[0], preferred_element_type=F32)).astype(BF16)
        pinned = lambda v: with_layout_constraint(v.T, Layout((0, 1)))
        at = lambda l, row, a, size: lax.slice_in_dim(routes[0], (l * TAB_ROWS + row) * LANES + a,
                                                      (l * TAB_ROWS + row) * LANES + a + size)
        rest = (n_local // 2 - HOT) // 2
        hot_ids = jnp.concatenate([at(l, row, 0, HOT) for l in range(n_layers) for row in (ROW_EXPERT, ROW_PARTNER)])
        y1 = pinned(own_sum(y_own, got_y))
        dx0, y1, hot_ids, got_a, finals = fence((dx0, y1, hot_ids, got_a, finals))
        finals = place(at(0, ROW_PARTNER, HOT, rest), 0, got_a, finals)
        theirs0, finals = fence((theirs0, finals))
        part0 = add(part0, theirs0).astype(BF16)
        theirs0 = move(part0, 'x')
        part0, dx0, got_b = fence((part0, pinned(dx0), got_b))
        finals = place(at(0, ROW_PARTNER, HOT + rest, rest), 0, got_b, finals)
        hot0_c, finals = fence((hot0_c, finals))
        finals = place_hot(hot_ids, [hot0, hot0_c, hot1, hot1_c], finals)
        theirs0, theirs1, finals = fence((theirs0, theirs1, finals))
        total0 = add(part0, theirs0).astype(BF16)
        g_mix = jnp.stack([add(total0, move(total0, 'core')), add(part1, theirs1)]).astype(BF16)
        return (y1.T, dx0.T, g_mix, jnp.swapaxes(finals[0], 2, 3), jnp.swapaxes(finals[1], 2, 3), finals[2])

    return jax.shard_map(device_step, mesh=sub,
                         in_specs=(tok_spec, tok_spec, route_spec, route_spec, whole_spec,
                                   expert_spec, expert_spec, expert_spec),
                         out_specs=(tok_spec, tok_spec, whole_spec, expert_spec, expert_spec, expert_spec),
                         check_vma=False)
```

```python
import functools

import jax
import jax.numpy as jnp
from jax import lax
from jax.experimental import pallas as pl
from jax.experimental.pallas import tpu as pltpu
from jax.sharding import Mesh, PartitionSpec as P

F32, BF16, I32 = jnp.float32, jnp.bfloat16, jnp.int32
MESH = pl.DeviceIdType.MESH
ROWS = 384
GRP = 8
PITCH = 9
DEPTH = 3
FULL = 8
HALF = 4
CAP_FACTOR = 3
LANES = 128
N_SRC = 4
Y, CORE, X = 1, 2, 4
VMEM_LIMIT = 62 * 1024 * 1024
PER_TILE = ROWS // GRP
ROW_BOUND, ROW_GOFF, ROW_EXPERT, ROW_PARTNER, TAB_ROWS = 32, 33, 34, 35, 40
SLOT_GROUPS = 256


def cdiv(a, b):
    return (a + b - 1) // b


def spans(d):
    return [(LANES * j, min(LANES, d - LANES * j)) for j in range(cdiv(d, LANES))]


any_space = pl.BlockSpec(memory_space=pl.ANY)
in_vmem = pl.BlockSpec(memory_space=pltpu.VMEM)


def sorted_list(expert_ids, gate_vals):
    n_tok, top = expert_ids.shape
    n = n_tok * top
    keys = expert_ids.reshape(n) * n + jnp.arange(n, dtype=I32)
    keys, gates = lax.sort((keys, gate_vals.reshape(n)), num_keys=1, is_stable=False)
    return ((keys % n) // top).astype(F32), gates


def plan_kernel(n_layers, n_local, n_tok, list_rows, deal_ref, all_ref, tab_ref, idx_ref, gate_ref):
    n_mine = n_local // 2
    core, ep = lax.axis_index('core'), lax.axis_index('ep')
    list_len = list_rows * LANES
    lane = lambda n: lax.broadcasted_iota(I32, (n, LANES), 1).astype(F32)
    sub = lambda n: lax.broadcasted_iota(I32, (n, LANES), 0).astype(F32)
    over_lanes = lambda v: jnp.sum(v, axis=1, keepdims=True)
    over_subs = lambda v: jnp.sum(v, axis=0, keepdims=True)
    l16, s16 = lane(n_mine), sub(n_mine)
    groups = lambda c: jnp.floor((c + (GRP - 0.5)) * (1.0 / GRP))
    for l in range(n_layers):
        cnt = all_ref[:, 2 * n_layers * list_rows + l, :]
        ends = cnt
        step = 1
        while step < 2 * n_local:
            ends = ends + jnp.where(lane(N_SRC) >= step, pltpu.roll(ends, step, 1), 0.0)
            step *= 2
        starts = ends - cnt
        second = (ep > 0)
        local = lambda v: jnp.where(lane(N_SRC) < n_local, jnp.where(second, pltpu.roll(v, LANES - n_local, 1), v), 0.0)
        cnt, starts = local(cnt), local(starts)
        tiles = jnp.floor((over_subs(groups(local(deal_ref[:, 2 * n_layers * list_rows + l, :]))) + (PER_TILE - 0.5))
                          * (1.0 / PER_TILE))
        load = jnp.where(lane(1) < n_local, jnp.maximum(1.0, tiles), -1.0)
        wide = jnp.broadcast_to(load, (n_local, LANES))
        col = over_lanes(jnp.where(lane(n_local) == sub(n_local), wide, 0.0))
        ahead = (col > wide) | ((col == wide) & (sub(n_local) < lane(n_local)))
        rank = over_subs(jnp.where(ahead, 1.0, 0.0))
        odd = s16 - 2.0 * jnp.floor(s16 * 0.5 + 0.25)
        flip = jnp.where(core > 0, 1.0 - odd, odd)
        dealt = lambda f: (jnp.broadcast_to(rank, (n_mine, LANES)) == 2.0 * s16 + f) & (l16 < n_local)
        pick = dealt(flip)
        choose = lambda p, row: over_lanes(jnp.where(p, jnp.broadcast_to(row, (n_mine, LANES)), 0.0))
        mine = lambda row: choose(pick, row)
        as_row = lambda c: over_subs(jnp.where(l16 == s16, c, 0.0))
        experts = as_row(mine(lane(1)))
        partner = as_row(choose(dealt(1.0 - flip), lane(1)))
        at = l * TAB_ROWS
        off = jnp.zeros((n_mine, 1), F32)
        pos = [jnp.zeros((n_mine, LANES), F32) for _ in range(SLOT_GROUPS // LANES)]
        for s in range(N_SRC):
            c, st = mine(cnt[s:s + 1]), mine(starts[s:s + 1]) + float(s * list_len)
            ng = groups(c)
            for i in range(len(pos)):
                rel = l16 + float(LANES * i) - off
                code = (st + GRP * rel) * 16.0 + jnp.minimum(float(GRP), c - GRP * rel)
                pos[i] = jnp.where((rel >= 0) & (rel < ng), code, pos[i])
            off = off + ng
        for i in range(len(pos)):
            tab_ref[pl.ds(at + i, n_mine, stride=len(pos)), :] = pos[i].astype(I32)
        n_tiles = jnp.maximum(1.0, jnp.floor((off + (PER_TILE - 0.5)) * (1.0 / PER_TILE)))
        bounds = over_subs(jnp.where(s16 < l16, n_tiles, 0.0))
        before = over_lanes(jnp.where(l16 == s16, jnp.broadcast_to(bounds, (n_mine, LANES)), 0.0))
        t = jnp.minimum(l16, over_subs(jnp.broadcast_to(n_tiles, (n_mine, LANES))) - 1.0)
        inside = (t >= before) & (t < before + n_tiles)
        goff = over_subs(jnp.where(inside, s16 * float(SLOT_GROUPS) + (t - before) * float(PER_TILE), 0.0))
        rows = [(ROW_BOUND, bounds), (ROW_GOFF, goff), (ROW_EXPERT, experts), (ROW_PARTNER, partner)]
        for row, value in rows:
            tab_ref[at + row:at + row + 1, :] = value.astype(I32)
    for l in range(n_layers):
        pad = l * (N_SRC * list_rows + 8) + N_SRC * list_rows
        gate_ref[pad:pad + 8, :] = jnp.zeros((8, LANES), F32)
        for s in range(N_SRC):
            to = (l * N_SRC + s) * list_rows
            toks = all_ref[s, l * list_rows:(l + 1) * list_rows, :]
            idx_ref[to:to + list_rows, :] = ((toks + float(s * n_tok)) * float(PITCH)).astype(I32)
            to = l * (N_SRC * list_rows + 8) + s * list_rows
            gate_ref[to:to + list_rows, :] = all_ref[s, (n_layers + l) * list_rows:(n_layers + l + 1) * list_rows, :]


def plan_shapes(sizes):
    n_layers, _, _, list_rows = sizes
    rows = (n_layers * TAB_ROWS, n_layers * N_SRC * list_rows, n_layers * (N_SRC * list_rows + 8))
    return [jax.ShapeDtypeStruct((n, LANES), dt) for n, dt in zip(rows, (I32, I32, F32))]


def flat(tab, idx, gates):
    return tab.reshape(-1), idx.reshape(-1), gates


def plan(deal, shared, sizes):
    return flat(*pl.pallas_call(
        functools.partial(plan_kernel, *sizes),
        out_shape=plan_shapes(sizes),
        in_specs=[in_vmem] * 2, out_specs=[in_vmem] * 3,
        cost_estimate=pl.CostEstimate(flops=10 ** 7, bytes_accessed=10 ** 6, transcendentals=0),
        name="plan",
    )(deal, shared))


def expert_kernel(cfg, *refs):
    fwd, bwd, own, layer, n_blk, d, ff, n_exp, picks, row_id, list_len, p_f32, n_alias, got_layer = cfg
    save, load = fwd and not bwd, own and bwd and not fwd
    refs = list(refs)
    take = lambda n: [refs.pop(0) for _ in range(n)]
    tab_hbm, idx_hbm, gate_hbm = take(3)
    u_pieces = take(N_SRC) if not load else []
    dy_pieces = take(N_SRC) if bwd else []
    wg_hbm, wu_hbm, wd_hbm = take(3)
    ab_hbm, xu_hbm = take(2) if load else (None, None)
    prev = take(1)[0] if bwd and not own else None
    got = take(2) if got_layer is not None else None
    take(n_alias)
    y_outs = take(N_SRC) if fwd else []
    du_outs = take(N_SRC) if bwd and own else []
    grad = take(1)[0] if bwd and own else None
    finals = take(3) if bwd and not own or got_layer is not None else None
    sent = take(2) if bwd and not own else None
    ab_hbm, xu_hbm = take(2) if save else (ab_hbm, xu_hbm)
    tab_ref, idx, gate_ref, land, table, gat = take(6)
    acc, row_ref = take(2) if own else (None, None)
    gu_ref, wd_ref, g_ref, x_u = take(4)
    x_c = take(1)[0] if bwd else None
    ab_ref = take(1)[0]
    dh_ref = take(1)[0] if bwd else None
    h_ref = take(1)[0]
    dab_ref, sums = take(2) if bwd else (None, None)
    keep_buf = take(1)[0] if bwd and not own else None
    got_buf = take(1)[0] if got is not None else None
    list_sem, land_sem, w_sem = take(3)
    sum_sem = take(1)[0] if bwd else None
    keep_sem = take(1)[0] if bwd and not own else None
    read_sem, write_sem = take(2) if got is not None else (None, None)
    stage_f, out_sem = take(2) if own else (None, None)
    ab_sem, xu_sem = take(2) if save or load else (None, None)

    copy = pltpu.make_async_copy
    cols = spans(d)
    lo = ff // 256 * 256
    hi = ff - lo
    dot = functools.partial(lax.dot_general, preferred_element_type=F32)
    nn = (((1,), (0,)), ((), ()))
    nt = (((1,), (1,)), ((), ()))
    tn = (((0,), (0,)), ((), ()))
    al = pl.multiple_of
    n_row = N_SRC * n_blk
    glane = lax.broadcasted_iota(I32, (GRP, LANES), 1)
    gsub = lax.broadcasted_iota(I32, (GRP, LANES), 0)

    def row_at(r):
        return pl.ds(r * PITCH, FULL)

    def codes_of(tile):
        at = ROW_GOFF * LANES + tile
        if own and bwd:
            return lambda q: tab_ref[tab_ref[at] + q]
        view = tab_ref.at[pl.ds(tab_ref[at], PER_TILE)]
        return lambda q: view[q]

    def gather(codes, q):
        ids = idx.at[pl.ds(codes(q) >> 4, GRP)]
        for k in range(GRP):
            gat[row_at(q * GRP + k), :] = table[pl.ds(ids[k], FULL), :]

    def gate_column(code):
        pos = code >> 4
        row, shift = pos >> 7, pos & (LANES - 1)
        want = glane == gsub + shift
        over = glane == gsub + (shift - LANES)
        here = gate_ref[pl.ds(row, GRP, stride=0), :]
        there = gate_ref[pl.ds(row + 1, GRP, stride=0), :]
        v = jnp.where(want, here, jnp.where(over, there, 0.0))
        return jnp.where(gsub < (code & 15), jnp.sum(v, axis=1, keepdims=True), 0.0)

    def scatter(codes, q):
        ids = idx.at[pl.ds(codes(q) >> 4, GRP)]
        new = []
        for k in range(GRP):
            at = pl.ds(ids[k], FULL)
            new.append((at, acc[at, :] + row_ref[row_at(q * GRP + k), :]))
        for at, value in reversed(new):
            acc[at, :] = value

    def keep_ab(t):
        ends = (ab_ref.at[t & 1], ab_hbm.at[t])
        return copy(*(ends if save else ends[::-1]), ab_sem.at[t & 1])

    def keep_xu(t):
        ends = (x_u.at[t & 1], xu_hbm.at[t])
        return copy(*(ends if save else ends[::-1]), xu_sem.at[t & 1])

    def of(ref, t):
        return ref.at[t & 1] if save or load else ref

    def convert(codes, t):
        for q in range(0, PER_TILE, 2):
            part = []
            for p in (q, q + 1):
                code = codes(p)
                rows = [gat[pl.ds(GRP * PITCH * p + j, GRP, stride=PITCH), :]
                        for j in range(HALF if load else 0, FULL if bwd else HALF)]
                real = gsub < (code & 15)
                gate = gate_column(code)
                g_ref[GRP * p:GRP * (p + 1), :] = gate
                us, dys = ([], rows) if load else (rows[:HALF], rows[HALF:])
                part.append([jnp.where(real, v, 0.0) for v in us] + [v * gate for v in dys])
            at = slice(GRP * q, GRP * (q + 2))
            for x, o in ((None if load else of(x_u, t), 0), (x_c, 0 if load else HALF)):
                if x is None:
                    continue
                for j, (c, w) in enumerate(cols):
                    both = jnp.concatenate([part[0][o + j], part[1][o + j]], axis=0)
                    x[at, c:c + w] = both[:, :w].astype(BF16)

    def put_rows(o, value, s0):
        value = value.astype(BF16).astype(F32)
        n = value.shape[0]
        for j, (c, w) in enumerate(cols):
            row_ref[pl.ds(PITCH * s0 + o + j, n, stride=PITCH), 0:w] = value[:, c:c + w] * g_ref[s0:s0 + n, 0:w]

    low = lax.broadcasted_iota(I32, (16, 2 * hi), 1) < hi

    def middle(a, b, dh):
        sig = 0.5 * jnp.tanh(0.5 * a) + 0.5
        act = a * sig
        h = act * b
        if dh is None:
            return h, None, None
        slope = sig * (1.0 + a * (1.0 - sig))
        return h, dh * b * slope, dh * act

    def weights(e, slot):
        at = (layer, tab_ref[ROW_EXPERT * LANES + e])
        moves = []
        for i, w in enumerate((wg_hbm, wu_hbm)):
            moves.append((w.at[at + (pl.ds(0, lo),)], gu_ref.at[slot, pl.ds(i * lo, lo)]))
            moves.append((w.at[at + (pl.ds(lo, hi),)], gu_ref.at[slot, pl.ds(2 * lo + i * hi, hi)]))
        moves.append((wd_hbm.at[at], wd_ref.at[slot]))
        return [copy(a, b, w_sem.at[slot, i]) for i, (a, b) in enumerate(moves)]

    def sums_in(e, slot):
        return copy(prev.at[e], sums.at[slot], sum_sem.at[slot])

    def sums_out(e, slot):
        return copy(sums.at[slot], grad.at[e], sum_sem.at[slot])

    def keeps(e, slot):
        at = (layer, tab_ref[ROW_EXPERT * LANES + e])
        return [copy(keep_buf.at[slot, i], finals[i].at[at], keep_sem.at[slot, i]) for i in range(3)]

    def send(e, slot, part):
        return copy(keep_buf.at[slot], sent[part].at[e - part * (n_exp // 2)], keep_sem.at[slot, 3])

    def read(e, slot, part=0):
        return copy(got[part].at[e - part * (n_exp // 2)], got_buf.at[slot], read_sem.at[slot])

    def writes(e, slot):
        to = tab_ref[TAB_ROWS * LANES + e]
        return [copy(got_buf.at[slot, i], finals[i].at[got_layer, to], write_sem.at[slot, i]) for i in range(3)]

    def start(moves):
        for m in moves:
            m.start()

    def wait(moves):
        for m in moves:
            m.wait()

    n_tab = TAB_ROWS * LANES
    lists = [copy(tab_hbm.at[pl.ds(row_id * n_tab, n_tab)], tab_ref.at[pl.ds(0, n_tab)], list_sem.at[0]),
             copy(idx_hbm.at[pl.ds(row_id * N_SRC * list_len, N_SRC * list_len)], idx.at[pl.ds(0, N_SRC * list_len)],
                  list_sem.at[1]),
             copy(gate_hbm.at[pl.ds(row_id * gate_ref.shape[0], gate_ref.shape[0])], gate_ref, list_sem.at[2])]
    if got is not None:
        at = (got_layer * TAB_ROWS + ROW_PARTNER) * LANES
        lists.append(copy(tab_hbm.at[pl.ds(at, LANES)], tab_ref.at[pl.ds(n_tab, LANES)], list_sem.at[3]))
    start(lists)
    pieces = []
    for s in range(N_SRC):
        if not load:
            pieces.append((u_pieces[s], picks[0][s], s, 0, fwd))
        if bwd:
            pieces.append((dy_pieces[s], picks[1][s], s, HALF, own))
    lands = [copy(ref.at[pick], land.at[i % N_SRC], land_sem.at[i % N_SRC]) for i, (ref, pick, *_) in enumerate(pieces)]
    start(lands[:N_SRC])
    lists[0].wait()
    for e in range(DEPTH - 1):
        start(weights(e, e))
        if bwd and not own:
            sums_in(e, e).start()
    if got is not None:
        lists[3].wait()
        read(0, 0).start()
    if own:
        def clear(c, _):
            for k in range(4):
                acc[pl.ds(al(c * 1152 + 288 * k, 8), 288), :] = jnp.zeros((288, LANES), F32)
            return 0

        lax.fori_loop(0, acc.shape[0] // 1152, clear, 0)
        row_ref[...] = jnp.zeros(row_ref.shape, F32)
    rows = 256
    for i, (_, _, s, o, seed) in enumerate(pieces):
        lands[i].wait()

        def fill(c, _, i=i, o=o, seed=seed, s=s):
            r = al(c * rows, rows)
            for j in range(HALF):
                vals = land[i % N_SRC, pl.ds(r, rows), LANES * j:LANES * (j + 1)].astype(F32)
                to = pl.ds(PITCH * (s * n_blk + r) + o + j, rows, stride=PITCH)
                table[to, :] = vals
                if seed and s == 0:
                    acc[to, :] = vals
            return 0

        lax.fori_loop(0, n_blk // rows, fill, 0)
        if i + N_SRC < len(pieces):
            lands[i + N_SRC].start()
    wait(lists[1:3])
    for k in range(GRP):
        idx[N_SRC * list_len + k] = 0

    def first(q, _):
        gather(begin, 2 * q)
        gather(begin, 2 * q + 1)
        return 0

    begin = codes_of(0)
    lax.fori_loop(0, PER_TILE // 2, first, 0)
    convert(begin, 0)
    if save:
        keep_xu(0).start()
    if load:
        keep_ab(0).start()
        keep_xu(0).start()

    def expert(e, _):
        slot = e & 1
        deep = lax.rem(e, DEPTH)
        sum_slot = slot if own else deep
        wait(weights(e, deep))
        if bwd and not own:
            sums_in(e, deep).wait()
        if got is not None:
            read(0, slot).wait()
            start(writes(e, slot))

            @pl.when((e > 0) & (e < n_exp - 1))
            def _():
                wait(writes(e - 1, 1 - slot))

        @pl.when(e < n_exp - (DEPTH - 1))
        def _():
            ahead = lax.rem(e + DEPTH - 1, DEPTH)
            start(weights(e + DEPTH - 1, ahead))
            if bwd and not own:
                sums_in(e + DEPTH - 1, ahead).start()

        @pl.when(e < n_exp - 1)
        def _():
            if got is not None:
                for part in range(2):
                    @pl.when((e + 1 >= n_exp // 2) if part else (e + 1 < n_exp // 2))
                    def _(part=part):
                        read(e + 1, 1 - slot, part).start()

        if bwd and own:
            @pl.when(e > 1)
            def _():
                sums_out(e - 2, slot).wait()

            sums[slot] = jnp.zeros(sums.shape[1:], F32)

        def tile(t, _):
            if save:
                @pl.when(t > 1)
                def _():
                    keep_ab(t - 2).wait()

                @pl.when(t > 0)
                def _():
                    keep_xu(t - 1).wait()
            if load:
                keep_ab(t).wait()
                keep_xu(t).wait()
                keep_ab(t + 1).start()
                keep_xu(t + 1).start()
            ab, xu = of(ab_ref, t), of(x_u, t)
            before, after = codes_of(jnp.maximum(t - 1, 0)), codes_of(t + 1)
            for q in range(PER_TILE):
                if own:
                    scatter(before, q)
                gather(after, q)
            front = ROWS if own and bwd else ROWS // 2
            for s0 in range(0, ROWS, front):
                sl = slice(s0, s0 + front)
                if not load:
                    ab[sl, :] = dot(xu[sl, :], gu_ref[deep], nt)
                if bwd:
                    dh_ref[sl, :] = dot(x_c[sl, :], wd_ref[deep], nt)
            for r in range(0, ROWS, 16):
                rows = slice(r, r + 16)
                for c in range(0, lo, LANES):
                    h, da, db = middle(ab[rows, c:c + LANES], ab[rows, lo + c:lo + c + LANES],
                                       dh_ref[rows, c:c + LANES] if bwd else None)
                    h_ref[rows, c:c + LANES] = h.astype(BF16)
                    if bwd:
                        dab_ref[rows, c:c + LANES] = da.astype(BF16)
                        dab_ref[rows, lo + c:lo + c + LANES] = db.astype(BF16)
                a = ab[rows, 2 * lo:]
                b = pltpu.roll(a, hi, 1)
                dh = dh_ref[rows, lo:] if bwd else None
                if bwd:
                    dh = jnp.concatenate([dh, dh], axis=1)
                h, da, db = middle(a, b, dh)
                h_ref[rows, lo:] = h[:, :hi].astype(BF16)
                if bwd:
                    dab_ref[rows, 2 * lo:] = jnp.where(low, da, pltpu.roll(db, hi, 1)).astype(BF16)
            half = ROWS // 2
            for s0 in range(0, ROWS, half):
                sl = slice(s0, s0 + half)
                if fwd:
                    put_rows(0, dot(h_ref[sl, :], wd_ref[deep], nn), s0)
                if bwd and own:
                    put_rows(HALF, dot(dab_ref[sl, :], gu_ref[deep], nn), s0)
            if bwd:
                view = sums.at[sum_slot]
                view[0:2 * ff, :] += dot(dab_ref[...], xu[...], tn)
                view[2 * ff:, :] += dot(h_ref[...], x_c[...], tn)
            convert(after, t + 1)
            if save:
                keep_ab(t).start()
                keep_xu(t + 1).start()
            return 0

        lax.fori_loop(tab_ref[ROW_BOUND * LANES + e], tab_ref[ROW_BOUND * LANES + e + 1], tile, 0)
        if bwd and own:
            sums_out(e, slot).start()
        if bwd and not own:
            @pl.when(e > 1)
            def _():
                wait(keeps(e - 2, slot) + [send(0, slot, 0)])

            for i in range(2):
                keep_buf[slot, i, 0:lo, :] = sums[deep, i * lo:(i + 1) * lo, :].astype(BF16)
                keep_buf[slot, i, lo:, :] = sums[deep, 2 * lo + i * hi:2 * lo + (i + 1) * hi, :].astype(BF16)
            keep_buf[slot, 2] = sums[deep, 2 * ff:, :].astype(BF16)
            start(keeps(e, slot))
            for part in range(2):
                @pl.when((e >= n_exp // 2) if part else (e < n_exp // 2))
                def _(part=part):
                    send(e, slot, part).start()
        return 0

    lax.fori_loop(0, n_exp, expert, 0)
    ends = ((n_exp - 2, (n_exp - 2) % 2), (n_exp - 1, (n_exp - 1) % 2))
    n_tiles = tab_ref[ROW_BOUND * LANES + n_exp]
    if save:
        wait([keep_ab(n_tiles - 2), keep_ab(n_tiles - 1), keep_xu(n_tiles - 1)])
    if save or load:
        keep_xu(n_tiles).wait()
    if load:
        keep_ab(n_tiles).wait()
    if own:
        end = codes_of(tab_ref[ROW_BOUND * LANES + n_exp] - 1)
        lax.fori_loop(0, PER_TILE, lambda q, _: (scatter(end, q), 0)[1], 0)
        flights = {}
        for o, out in ((HALF, du_outs), (0, y_outs)):
            for s in range(N_SRC if out else 0):
                wide = s == 0 or p_f32
                stage = stage_f.at[s] if wide else land.at[s]
                if s in flights:
                    flights[s].wait()

                def fetch(c, _, stage=stage, s=s, o=o):
                    r = al(c * rows, rows)
                    for j in range(HALF):
                        at = pl.ds(PITCH * (s * n_blk + r) + o + j, rows, stride=PITCH)
                        stage[pl.ds(r, rows), LANES * j:LANES * (j + 1)] = acc[at, :].astype(stage.dtype)
                    return 0

                lax.fori_loop(0, n_blk // rows, fetch, 0)
                flights[s] = copy(stage, out[s], out_sem.at[s])
                flights[s].start()
        wait(flights.values())
        if bwd:
            for e, slot in ends:
                sums_out(e, slot).wait()
    else:
        for e, slot in ends:
            wait(keeps(e, slot) + [send(0, slot, 0)])
    if got is not None:
        for e, slot in ends:
            wait(writes(e, slot))


def run_experts(routes, layer, u, dy, weights, prev, finals, fwd, own, p_f32=False, got=None, kept=None):
    tab, idx, gates = routes
    bwd = dy is not None
    wg, wu, wd = weights
    save, load = fwd and not bwd, kept is not None
    n_blk, wide = (dy or u)[0][0].shape[-2:]
    n_layers, n_local, ff, d = wd.shape
    n_exp = n_local // 2
    row_id = layer
    list_len = idx.shape[0] // (n_layers * N_SRC)

    arrays = lambda pieces: [v for v, _ in pieces]
    operands = [tab, idx, gates] + ([] if load else arrays(u)) + (arrays(dy) if bwd else []) + [wg, wu, wd] + list(kept or ())
    out_shape, aliases = [], {}
    for use in (fwd, bwd and own):
        if use:
            out_shape += [jax.ShapeDtypeStruct((n_blk, wide), F32 if s == 0 or p_f32 else BF16) for s in range(N_SRC)]
    if bwd and own:
        out_shape.append(jax.ShapeDtypeStruct((n_exp, 3 * ff, d), F32))
    if bwd and not own:
        operands.append(prev)
    if got is not None:
        operands += got
    for i, f in enumerate(finals or ()):
        aliases[len(operands)] = len(out_shape) + i
        operands.append(f)
    if bwd and not own or finals:
        out_shape += [jax.ShapeDtypeStruct((n_layers, n_local, ff, d), BF16)] * 3
    if bwd and not own:
        out_shape += [jax.ShapeDtypeStruct((n_exp // 2, 3, ff, d), BF16)] * 2
    if save:
        most = n_exp * (SLOT_GROUPS // PER_TILE) + 2
        out_shape += [jax.ShapeDtypeStruct((most, ROWS, 2 * ff), F32), jax.ShapeDtypeStruct((most, ROWS, d), BF16)]
    sem = lambda *s: pltpu.SemaphoreType.DMA(s)
    mid = lambda n, dt: pltpu.VMEM((ROWS, n), dt)
    twin = lambda n, dt: pltpu.VMEM((2, ROWS, n), dt) if save or load else mid(n, dt)
    table, rows = pltpu.VMEM((PITCH * N_SRC * n_blk, LANES), F32), pltpu.VMEM((PITCH * ROWS, LANES), F32)
    scratch = [pltpu.SMEM(((TAB_ROWS + 1) * LANES,), I32), pltpu.SMEM((N_SRC * list_len + LANES,), I32),
               pltpu.VMEM((N_SRC * list_len // LANES + 8, LANES), F32), pltpu.VMEM((N_SRC, n_blk, wide), BF16)]
    scratch += [table, rows] * (1 + own)
    scratch += [pltpu.VMEM((DEPTH, 2 * ff, d), BF16), pltpu.VMEM((DEPTH, ff, d), BF16), mid(LANES, F32)]
    scratch += [twin(d, BF16)] + [mid(d, BF16)] * bwd + [twin(2 * ff, F32)] + [mid(ff, F32)] * bwd + [mid(ff, BF16)]
    scratch += [mid(2 * ff, BF16), pltpu.VMEM((2 if own else DEPTH, 3 * ff, d), F32)] * bwd
    if bwd and not own:
        scratch.append(pltpu.VMEM((2, 3, ff, d), BF16))
    if got is not None:
        scratch.append(pltpu.VMEM((2, 3, ff, d), BF16))
    scratch += [sem(4), sem(N_SRC), sem(DEPTH, 5)] + [sem(DEPTH)] * bwd
    if bwd and not own:
        scratch.append(sem(2, 4))
    if got is not None:
        scratch += [sem(2), sem(2, 3)]
    if own:
        scratch += [pltpu.VMEM((N_SRC if p_f32 else 1, n_blk, wide), F32), sem(N_SRC)]
    if save or load:
        scratch += [sem(2), sem(2)]
    passes = 2 + fwd + bwd * (4 + 2 * own)
    flops = 2 * d * ff * passes * n_blk * N_SRC * 2
    hoist = 1300 if not own else 600 if load else 750 if save else 900
    picks = [[i for _, i in u] if u else None, [i for _, i in dy] if bwd else None]
    cfg = (fwd, bwd, own, layer, n_blk, d, ff, n_exp, picks, row_id, list_len, p_f32, len(aliases),
           None if got is None else 1 - layer)
    return pl.pallas_call(
        functools.partial(expert_kernel, cfg),
        out_shape=out_shape,
        in_specs=[any_space] * len(operands),
        out_specs=[any_space] * len(out_shape),
        scratch_shapes=scratch,
        input_output_aliases=aliases,
        compiler_params=pltpu.CompilerParams(
            vmem_limit_bytes=VMEM_LIMIT),
        cost_estimate=pl.CostEstimate(flops=flops, bytes_accessed=3 * 2 * n_exp * d * ff, transcendentals=0),
        name=f"experts_{'f' if fwd else ''}{'b' if bwd else ''}_{'own' if own else 'other'}_{layer}",
    )(*operands)


def place_kernel(layer, n_exp, tab_ref, got_ref, *refs):
    outs, (buf, in_sem, out_sem) = refs[3:6], refs[6:]
    reads = [pltpu.make_async_copy(got_ref.at[i], buf.at[i], in_sem.at[i]) for i in range(n_exp)]
    for read in reads:
        read.start()
    writes = []
    for i, read in enumerate(reads):
        read.wait()
        e = tab_ref[i]
        for k, out in enumerate(outs):
            writes.append(pltpu.make_async_copy(buf.at[i, k], out.at[layer, e], out_sem.at[i, k]))
            writes[-1].start()
    for write in writes:
        write.wait()


def place(partner, layer, got, finals):
    n_exp = got.shape[0]
    return pl.pallas_call(
        functools.partial(place_kernel, layer, n_exp),
        out_shape=[jax.ShapeDtypeStruct(f.shape, f.dtype) for f in finals],
        grid_spec=pltpu.PrefetchScalarGridSpec(
            num_scalar_prefetch=1, grid=(1,), in_specs=[any_space] * 4, out_specs=[any_space] * 3,
            scratch_shapes=[pltpu.VMEM(got.shape, got.dtype), pltpu.SemaphoreType.DMA((n_exp,)),
                            pltpu.SemaphoreType.DMA((n_exp, 3))]),
        input_output_aliases={2: 0, 3: 1, 4: 2},
        compiler_params=pltpu.CompilerParams(vmem_limit_bytes=VMEM_LIMIT),
        cost_estimate=pl.CostEstimate(flops=0, bytes_accessed=4 * got.size, transcendentals=0),
        name=f"place_{layer}",
    )(partner, got, *finals)


def peer(rel):
    return {name: (lax.axis_index(name) + ((rel >> bit) & 1)) % 2 for bit, name in enumerate(("ep", "core", "x"))}


def meet(rels):
    barrier = pltpu.get_barrier_semaphore()
    for rel in rels:
        pl.semaphore_signal(barrier, inc=1, device_id=peer(rel), device_id_type=MESH)
    pl.semaphore_wait(barrier, len(rels))


def remote(src, dst, send, recv, rel):
    return pltpu.make_async_remote_copy(src_ref=src, dst_ref=dst, send_sem=send, recv_sem=recv,
                                        device_id=peer(rel), device_id_type=MESH)


def share_kernel(n_rel, mine_ref, all_ref, send_sem, recv_sem):
    meet(range(1, n_rel))
    copies = [remote(mine_ref, all_ref.at[rel], send_sem.at[rel], recv_sem.at[rel], rel) for rel in range(1, n_rel)]
    for copy in copies:
        copy.start()
    all_ref[0] = mine_ref[...]
    for copy in copies:
        copy.wait()


def share(mine, n_rel):
    return pl.pallas_call(
        functools.partial(share_kernel, n_rel),
        out_shape=jax.ShapeDtypeStruct((n_rel,) + mine.shape, mine.dtype),
        in_specs=[in_vmem],
        out_specs=in_vmem,
        scratch_shapes=[pltpu.SemaphoreType.DMA((n_rel,)), pltpu.SemaphoreType.DMA((n_rel,))],
        compiler_params=pltpu.CompilerParams(collective_id=0, has_side_effects=True),
        cost_estimate=pl.CostEstimate(flops=10 ** 7, bytes_accessed=mine.size * 4 * n_rel, transcendentals=0),
        name="share_lists",
    )(mine)


def blocks_kernel(cfg, *refs):
    n_chunk, reduce, back, d, sizes = cfg
    refs = list(refs)
    take = lambda n: [refs.pop(0) for _ in range(n)]
    parts = take(N_SRC)
    m_ref = take(1)[0]
    list_refs, left_ref = take(2) if sizes else (), take(1)[0] if back else None
    o_total, o_a, o_b = take(3)
    plan_refs, grad_ref = take(3) if sizes else (), take(1)[0] if back else None
    in_f, in_b, got_f, s_wire, r_wire, u_wire, y_wire, t_buf, u_buf, y_buf, load, send, recv, put = take(14)
    n_rows = t_buf.shape[0] // n_chunk
    cut = [pl.ds(k * n_rows, n_rows) for k in range(n_chunk)]
    thin = [pl.ds(k * n_rows // 2, n_rows // 2) for k in range(n_chunk)]
    side = lax.broadcasted_iota(I32, (n_rows // 2, LANES), 1) < LANES // 2
    tiles = d // LANES
    turn = lambda v: pltpu.roll(v, LANES // 2, 1)
    lanes = lambda v, j: v[:, LANES * j:LANES * (j + 1)]

    def pack(wire, k, value):
        top, low = value[:n_rows // 2], value[n_rows // 2:]
        turned = [turn(lanes(low, j)) for j in range(tiles + 1)]
        parts = [lanes(top, j) for j in range(tiles)] + [jnp.where(side, lanes(top, tiles), turned[0])]
        parts += [jnp.where(side, turned[j], turned[j + 1]) for j in range(tiles)]
        for j, part in enumerate(parts):
            wire[thin[k], LANES * j:LANES * (j + 1)] = part.astype(BF16)

    def unpack(wire, k):
        value = wire[thin[k], :].astype(F32)
        turned = [turn(lanes(value, tiles + j)) for j in range(tiles + 1)]
        top = [lanes(value, j) for j in range(tiles)] + [jnp.where(side, lanes(value, tiles), 0.0)]
        low = [jnp.where(side, turned[j], turned[j + 1]) for j in range(tiles)] + [jnp.where(side, turned[tiles], 0.0)]
        return jnp.concatenate([jnp.concatenate(top, axis=1), jnp.concatenate(low, axis=1)], axis=0)

    chunks = range(n_chunk)
    loads = {}
    for i, part in enumerate(parts[:2] if reduce else parts):
        buf = in_f.at[i] if reduce or i == 0 else in_b.at[i - 1]
        for k in chunks:
            loads[i, k] = pltpu.make_async_copy(part.at[cut[k]], buf.at[cut[k]], load.at[i, k])
    order = (1, 0) if reduce else range(N_SRC)
    for i in order:
        for k in chunks:
            loads[i, k].start()
    u_buf[...] = jnp.zeros(u_buf.shape, BF16)
    meet((Y, CORE))
    links = []
    copy_in = pltpu.make_async_copy

    def link(src, dst, rel, cut=cut):
        n = len(links)
        links.append([remote(src.at[cut[k]], dst.at[cut[k]], send.at[n, k], recv.at[n, k], rel) for k in chunks])
        return links[-1]

    if reduce:
        first = link(parts[3], got_f.at[1], CORE)
        second = link(parts[2], got_f.at[0], CORE)
        over = link(s_wire, r_wire, Y, thin)
        for copies in (first, second):
            for copy in copies:
                copy.start()
        for k in chunks:
            loads[1, k].wait()
            first[k].wait_recv()
            pack(s_wire, k, in_f[1, cut[k], :] + got_f[1, cut[k], :])
            over[k].start()
    to_y = link(u_wire, y_wire, Y, thin)
    to_core = link(u_buf, o_b.at[0], CORE)
    puts = []
    for k in chunks:
        if reduce:
            loads[0, k].wait()
            second[k].wait_recv()
            over[k].wait_recv()
            total = in_f[0, cut[k], :] + got_f[0, cut[k], :] + unpack(r_wire, k)
        else:
            for i in range(N_SRC):
                loads[i, k].wait()
            total = in_f[0, cut[k], :]
            for i in range(N_SRC - 1):
                total = total + in_b[i, cut[k], :].astype(F32)
        total = total.astype(BF16)
        t_buf[cut[k], :] = total
        dims = (((1,), (1 if back else 0,)), ((), ()))
        mixed = lax.dot_general(total[:, :d], m_ref[...], dims, preferred_element_type=F32)
        u_buf[cut[k], 0:d] = (total[:, :d].astype(F32) + mixed).astype(BF16)
        pack(u_wire, k, u_buf[cut[k], :].astype(F32))
        to_y[k].start()
        to_core[k].start()
        puts.append(pltpu.make_async_copy(u_buf.at[cut[k]], o_a.at[0, cut[k]], put.at[0, k]))
        puts.append(pltpu.make_async_copy(t_buf.at[cut[k]], o_total.at[cut[k]], put.at[1, k]))
        for copy in puts[-2:]:
            copy.start()
    if sizes:
        plan_kernel(*sizes, *list_refs, *plan_refs)
    if back:
        grad_ref[...] = lax.dot_general(left_ref[:, :d], t_buf[:, :d], (((0,), (0,)), ((), ())), preferred_element_type=F32)
    on = link(y_buf, o_b.at[1], CORE)
    for k in chunks:
        to_y[k].wait_recv()
        y_buf[cut[k], :] = unpack(y_wire, k).astype(BF16)
        on[k].start()
        puts.append(copy_in(y_buf.at[cut[k]], o_a.at[1, cut[k]], put.at[2, k]))
        puts[-1].start()
    waited = [to_y] + ([first, second, over] if reduce else [])
    for copies in links:
        for copy in copies:
            if any(copies is w for w in waited):
                copy.wait_send()
            else:
                copy.wait()
    for copy in puts:
        copy.wait()


def complete_blocks(parts, m, reduce, back, ident, sizes=None, lists=(), left=(), n_chunk=4):
    n_blk, wide = parts[0].shape
    d = m.shape[0]
    sem = lambda *s: pltpu.SemaphoreType.DMA(s)
    pair = jax.ShapeDtypeStruct((2, n_blk, wide), BF16)
    extra = plan_shapes(sizes) if sizes else []
    extra += [jax.ShapeDtypeStruct((d, d), F32)] * len(left)
    buf = lambda n, dt: pltpu.VMEM((n, n_blk, wide) if n else (n_blk, wide), dt)
    return pl.pallas_call(
        functools.partial(blocks_kernel, (n_chunk, reduce, back, d, sizes)),
        out_shape=[jax.ShapeDtypeStruct((n_blk, wide), BF16)] + [pair] * 2 + extra,
        in_specs=[any_space] * N_SRC + [in_vmem] * (1 + len(lists) + len(left)),
        out_specs=[any_space] * 3 + [in_vmem] * len(extra),
        scratch_shapes=[buf(2, F32), buf(3, BF16), buf(2, F32)] + [pltpu.VMEM((n_blk // 2, 2 * d), BF16)] * 4 + [
            buf(0, BF16), buf(0, BF16), buf(0, BF16), sem(4, n_chunk), sem(6, n_chunk), sem(6, n_chunk), sem(3, n_chunk)],
        compiler_params=pltpu.CompilerParams(collective_id=ident, has_side_effects=True, vmem_limit_bytes=VMEM_LIMIT),
        cost_estimate=pl.CostEstimate(flops=10 ** 8, bytes_accessed=n_blk * wide * 40, transcendentals=0),
        name=f"complete_blocks_{ident}",
    )(*parts, m, *lists, *left)


def solution(mesh):
    ep_size, dp_size = mesh.shape['ep'], mesh.shape['dp']
    sub = Mesh(mesh.devices.reshape(ep_size, dp_size // 2, 2), ('ep', 'x', 'core'))
    tok_axes = ('x', 'core', 'ep')
    tok_spec = P(tok_axes, None)
    route_spec = P(None, tok_axes, None)
    whole_spec = P(None, None, None)
    expert_spec = P(None, 'ep', None, None)
    flip = [(0, 1), (1, 0)]
    move = lambda v, axis: lax.ppermute(v, axis, flip)
    move_diag = lambda v: lax.ppermute(v, ('ep', 'core'), [(0, 3), (1, 2), (2, 1), (3, 0)])
    fence = lax.optimization_barrier

    def device_step(tokens, d_out, expert_ids, gate_vals, w_mix, w_gate, w_up, w_down):
        n_layers, d = w_mix.shape[0], w_mix.shape[1]
        n_tok = tokens.shape[0]
        top = expert_ids.shape[2]
        n_local = w_gate.shape[1]
        n_exp = n_local * ep_size
        n = n_tok * top
        n_rel = 2 * N_SRC
        wide = cdiv(d, LANES) * LANES
        weights = (jnp.swapaxes(w_gate, 2, 3), jnp.swapaxes(w_up, 2, 3), w_down)
        pad = lambda v: jnp.pad(v, ((0, 0), (0, wide - d)))
        send_three = lambda p: [move(p[1], 'ep'), move(p[2], 'core'), move_diag(p[3])]

        def own_sum(p, got):
            return sum([g.astype(F32) for g in got], p)[:, :d].astype(BF16)

        one = lambda v: v.reshape(1, n_tok, wide)
        pairs = lambda a, b: [(a, 0), (a, 1), (b, 0), (b, 1)]

        one = lambda v: v.reshape(1, n_tok, wide)
        pairs = lambda a, b: [(a, 0), (a, 1), (b, 0), (b, 1)]
        singles = lambda *v: [(one(a), 0) for a in v]

        u0 = pad((tokens.astype(F32) + jnp.dot(tokens, w_mix[0], preferred_element_type=F32)).astype(BF16))
        u0_y, u0_c = move(u0, 'ep'), move(u0, 'core')
        lists = [sorted_list(expert_ids[l], gate_vals[l]) for l in range(n_layers)]
        counts = jnp.sum((expert_ids.reshape(n_layers, n, 1) == jnp.arange(n_exp, dtype=I32)).astype(F32), axis=1)
        packed = jnp.concatenate([jnp.concatenate([v[0] for v in lists] + [v[1] for v in lists]).reshape(-1, LANES),
                                  jnp.pad(counts, ((0, 8 - n_layers), (0, LANES - n_exp)))], axis=0)
        dy = pad(d_out)
        u0_y, u0_c, packed, dy = fence((u0_y, u0_c, packed, dy))
        u0_d = move(u0_y, 'core')
        shared = share(packed, N_SRC)
        dy, shared = fence((dy, shared))
        shared_x = move(shared, 'x')
        dy_y, dy_x = move(dy, 'ep'), move(dy, 'x')
        sizes = (n_layers, n_local, n_tok, n // LANES)
        routes = plan(shared, shared, sizes)
        u0_half = singles(u0, u0_y, u0_c, u0_d)
        *part, ab0, xu0 = run_experts(routes, 0, u0_half, None, weights, None, None, True, True, p_f32=True)
        dy_y, dy_x, shared_x, part = fence((dy_y, dy_x, shared_x, part))
        dy_c, dy_d, dy_xy, dy_xc = move(dy, 'core'), move(dy_y, 'core'), move(dy_y, 'x'), move(dy_x, 'core')
        y0, u1_a, u1_b, *routes_x = complete_blocks(part, w_mix[1], True, False, 1, sizes, (shared, shared_x))
        routes_x = flat(*routes_x)
        dy_c, dy_d, dy_xy, dy_xc, u0_p, u0_q, y0, u1_a, u1_b = fence(
            (dy_c, dy_d, dy_xy, dy_xc, u0, u0_y, y0, u1_a, u1_b))
        dy_xd = move(dy_xy, 'core')
        u1_xa = move(u1_a, 'x')
        out = run_experts(routes, 1, pairs(u1_a, u1_b), singles(dy, dy_y, dy_c, dy_d), weights, None, None, True, True)
        u1_xa, dy_xd, u0_p, u0_q, out = fence((u1_xa, dy_xd, u0_p, u0_q, out))
        y_part, du_part, g1 = out[:4], out[4:8], out[8]
        u1_xb = move(u1_xa, 'core')
        got = send_three(du_part)
        u0_x, u0_xy = move(u0_p, 'x'), move(u0_q, 'x')
        out = run_experts(routes_x, 1, pairs(u1_xa, u1_xb), singles(dy_x, dy_xy, dy_xc, dy_xd), weights, g1, None,
                          False, False)
        got, u0_x, u0_xy, out = fence((got, u0_x, u0_xy, out))
        *finals, sent_a, sent_b = out
        got1 = [move(sent_a, 'core'), move(sent_b, 'core')]
        du1, dx_a, dx_b, g_mix1 = complete_blocks([du_part[0], *got], w_mix[1], False, True, 2, left=(y0,))
        tx = lambda x, du: jnp.einsum('td,te->de', x, du, preferred_element_type=F32)
        dx_a, y_part, got1, u0_x, u0_xy, g_mix1 = fence((dx_a, y_part, got1, u0_x, u0_xy, g_mix1))
        dx_xa = move(dx_a, 'x')
        theirs1 = move(g_mix1, 'core')
        got_y = send_three(y_part)
        u0_xc, u0_xd = move(u0_x, 'core'), move(u0_xy, 'core')
        out = run_experts(routes, 0, None, pairs(dx_a, dx_b), weights, None, finals, False, True, got=got1, kept=(ab0, xu0))
        dx_xa, got_y, u0_xc, u0_xd, theirs1, out = fence((dx_xa, got_y, u0_xc, u0_xd, theirs1, out))
        du_part, g0, finals = out[:4], out[4], out[5:]
        dx_xb = move(dx_xa, 'core')
        got = send_three(du_part)
        part1 = (g_mix1 + theirs1).astype(BF16)
        theirs1 = move(part1, 'ep')
        du_part, dx_xb, part1 = fence((du_part, dx_xb, part1))
        out = run_experts(routes_x, 0, singles(u0_x, u0_xy, u0_xc, u0_xd), pairs(dx_xa, dx_xb), weights, g0, finals,
                          False, False)
        got, theirs1, got_y, y_own, out = fence((got, theirs1, got_y, y_part[0], out))
        *finals, sent_a, sent_b = out
        got_a, got_b = move(sent_a, 'core'), move(sent_b, 'core')
        add = lambda a, b: a.astype(F32) + b.astype(F32)
        part1 = add(part1, theirs1).astype(BF16)
        theirs1 = move(part1, 'x')
        du0 = own_sum(du_part[0], got)
        part0 = tx(tokens, du0).astype(BF16)
        theirs0 = move(part0, 'ep')
        dx0 = (du0.astype(F32) + jnp.einsum('te,de->td', du0, w_mix[0], preferred_element_type=F32)).astype(BF16)
        row = lambda a: lax.slice_in_dim(routes[0], ROW_PARTNER * LANES + a, ROW_PARTNER * LANES + a + n_local // 4)
        y1 = own_sum(y_own, got_y).T
        dx0, y1, got_a, finals = fence((dx0, y1, got_a, finals))
        finals = place(row(0), 0, got_a, finals)
        theirs0, finals = fence((theirs0, finals))
        part0 = add(part0, theirs0).astype(BF16)
        theirs0 = move(part0, 'x')
        part0, dx0, got_b = fence((part0, dx0.T, got_b))
        finals = place(row(n_local // 4), 0, got_b, finals)
        theirs0, theirs1, finals = fence((theirs0, theirs1, finals))
        total0 = add(part0, theirs0).astype(BF16)
        g_mix = jnp.stack([add(total0, move(total0, 'core')), add(part1, theirs1)]).astype(BF16)
        return (y1.T, dx0.T, g_mix, jnp.swapaxes(finals[0], 2, 3), jnp.swapaxes(finals[1], 2, 3), finals[2])

    return jax.shard_map(device_step, mesh=sub,
                         in_specs=(tok_spec, tok_spec, route_spec, route_spec, whole_spec,
                                   expert_spec, expert_spec, expert_spec),
                         out_specs=(tok_spec, tok_spec, whole_spec, expert_spec, expert_spec, expert_spec),
                         check_vma=False)
```

```python
import functools

import jax
import jax.numpy as jnp
from jax import lax
from jax.experimental import pallas as pl
from jax.experimental.pallas import tpu as pltpu
from jax.sharding import Mesh, PartitionSpec as P

F32, BF16, I32 = jnp.float32, jnp.bfloat16, jnp.int32
MESH = pl.DeviceIdType.MESH
ROWS = 384
GRP = 8
PITCH = 9
DEPTH = 3
FULL = 8
HALF = 4
CAP_FACTOR = 3
LANES = 128
N_SRC = 4
Y, CORE, X = 1, 2, 4
VMEM_LIMIT = 62 * 1024 * 1024
PER_TILE = ROWS // GRP
ROW_BOUND, ROW_GOFF, ROW_EXPERT, ROW_PARTNER, TAB_ROWS = 32, 33, 34, 35, 40
SLOT_GROUPS = 256


def cdiv(a, b):
    return (a + b - 1) // b


def first_piece(n_exp):
    return n_exp * 5 // 8


def spans(d):
    return [(LANES * j, min(LANES, d - LANES * j)) for j in range(cdiv(d, LANES))]


any_space = pl.BlockSpec(memory_space=pl.ANY)
in_vmem = pl.BlockSpec(memory_space=pltpu.VMEM)


def sorted_list(expert_ids, gate_vals):
    n_tok, top = expert_ids.shape
    n = n_tok * top
    keys = expert_ids.T.reshape(n) * n + jnp.arange(n, dtype=I32)
    keys, gates = lax.sort((keys, gate_vals.T.reshape(n)), num_keys=1, is_stable=False)
    return (keys % n_tok).astype(F32), gates


def plan_kernel(n_layers, n_local, n_tok, list_rows, deal_ref, all_ref, tab_ref, idx_ref, gate_ref):
    n_mine = n_local // 2
    core, ep = lax.axis_index('core'), lax.axis_index('ep')
    list_len = list_rows * LANES
    lane = lambda n: lax.broadcasted_iota(I32, (n, LANES), 1).astype(F32)
    sub = lambda n: lax.broadcasted_iota(I32, (n, LANES), 0).astype(F32)
    over_lanes = lambda v: jnp.sum(v, axis=1, keepdims=True)
    over_subs = lambda v: jnp.sum(v, axis=0, keepdims=True)
    l16, s16 = lane(n_mine), sub(n_mine)
    groups = lambda c: jnp.floor((c + (GRP - 0.5)) * (1.0 / GRP))
    for l in range(n_layers):
        cnt = all_ref[:, 2 * n_layers * list_rows + l, :]
        ends = cnt
        step = 1
        while step < 2 * n_local:
            ends = ends + jnp.where(lane(N_SRC) >= step, pltpu.roll(ends, step, 1), 0.0)
            step *= 2
        starts = ends - cnt
        second = (ep > 0)
        local = lambda v: jnp.where(lane(N_SRC) < n_local, jnp.where(second, pltpu.roll(v, LANES - n_local, 1), v), 0.0)
        cnt, starts = local(cnt), local(starts)
        tiles = jnp.floor((over_subs(groups(local(deal_ref[:, 2 * n_layers * list_rows + l, :]))) + (PER_TILE - 0.5))
                          * (1.0 / PER_TILE))
        load = jnp.where(lane(1) < n_local, jnp.maximum(1.0, tiles), -1.0)
        wide = jnp.broadcast_to(load, (n_local, LANES))
        col = over_lanes(jnp.where(lane(n_local) == sub(n_local), wide, 0.0))
        ahead = (col > wide) | ((col == wide) & (sub(n_local) < lane(n_local)))
        rank = over_subs(jnp.where(ahead, 1.0, 0.0))
        odd = s16 - 2.0 * jnp.floor(s16 * 0.5 + 0.25)
        flip = jnp.where(core > 0, 1.0 - odd, odd)
        dealt = lambda f: (jnp.broadcast_to(rank, (n_mine, LANES)) == 2.0 * s16 + f) & (l16 < n_local)
        pick = dealt(flip)
        choose = lambda p, row: over_lanes(jnp.where(p, jnp.broadcast_to(row, (n_mine, LANES)), 0.0))
        mine = lambda row: choose(pick, row)
        as_row = lambda c: over_subs(jnp.where(l16 == s16, c, 0.0))
        experts = as_row(mine(lane(1)))
        partner = as_row(choose(dealt(1.0 - flip), lane(1)))
        at = l * TAB_ROWS
        off = jnp.zeros((n_mine, 1), F32)
        pos = [jnp.zeros((n_mine, LANES), F32) for _ in range(SLOT_GROUPS // LANES)]
        for s in range(N_SRC):
            c, st = mine(cnt[s:s + 1]), mine(starts[s:s + 1]) + float(s * list_len)
            ng = groups(c)
            for i in range(len(pos)):
                rel = l16 + float(LANES * i) - off
                code = (st + GRP * rel) * 16.0 + jnp.minimum(float(GRP), c - GRP * rel)
                pos[i] = jnp.where((rel >= 0) & (rel < ng), code, pos[i])
            off = off + ng
        for i in range(len(pos)):
            tab_ref[pl.ds(at + i, n_mine, stride=len(pos)), :] = pos[i].astype(I32)
        n_tiles = jnp.maximum(1.0, jnp.floor((off + (PER_TILE - 0.5)) * (1.0 / PER_TILE)))
        bounds = over_subs(jnp.where(s16 < l16, n_tiles, 0.0))
        before = over_lanes(jnp.where(l16 == s16, jnp.broadcast_to(bounds, (n_mine, LANES)), 0.0))
        t = jnp.minimum(l16, over_subs(jnp.broadcast_to(n_tiles, (n_mine, LANES))) - 1.0)
        inside = (t >= before) & (t < before + n_tiles)
        goff = over_subs(jnp.where(inside, s16 * float(SLOT_GROUPS) + (t - before) * float(PER_TILE), 0.0))
        rows = [(ROW_BOUND, bounds), (ROW_GOFF, goff), (ROW_EXPERT, experts), (ROW_PARTNER, partner)]
        for row, value in rows:
            tab_ref[at + row:at + row + 1, :] = value.astype(I32)
    for l in range(n_layers):
        pad = l * (N_SRC * list_rows + 8) + N_SRC * list_rows
        gate_ref[pad:pad + 8, :] = jnp.zeros((8, LANES), F32)
        for s in range(N_SRC):
            to = (l * N_SRC + s) * list_rows
            toks = all_ref[s, l * list_rows:(l + 1) * list_rows, :]
            idx_ref[to:to + list_rows, :] = ((toks + float(s * n_tok)) * float(PITCH)).astype(I32)
            to = l * (N_SRC * list_rows + 8) + s * list_rows
            gate_ref[to:to + list_rows, :] = all_ref[s, (n_layers + l) * list_rows:(n_layers + l + 1) * list_rows, :]


def plan_shapes(sizes):
    n_layers, _, _, list_rows = sizes
    rows = (n_layers * TAB_ROWS, n_layers * N_SRC * list_rows, n_layers * (N_SRC * list_rows + 8))
    return [jax.ShapeDtypeStruct((n, LANES), dt) for n, dt in zip(rows, (I32, I32, F32))]


def flat(tab, idx, gates):
    return tab.reshape(-1), idx.reshape(-1), gates


def plan(deal, shared, sizes):
    return flat(*pl.pallas_call(
        functools.partial(plan_kernel, *sizes),
        out_shape=plan_shapes(sizes),
        in_specs=[in_vmem] * 2, out_specs=[in_vmem] * 3,
        cost_estimate=pl.CostEstimate(flops=10 ** 7, bytes_accessed=10 ** 6, transcendentals=0),
        name="plan",
    )(deal, shared))


def expert_kernel(cfg, *refs):
    fwd, bwd, own, layer, n_blk, d, ff, n_exp, picks, row_id, list_len, p_f32, n_alias, got_layer = cfg
    save, load = fwd and not bwd, own and bwd and not fwd
    refs = list(refs)
    take = lambda n: [refs.pop(0) for _ in range(n)]
    tab_hbm, idx_hbm, gate_hbm = take(3)
    u_pieces = take(N_SRC) if not load else []
    dy_pieces = take(N_SRC) if bwd else []
    wg_hbm, wu_hbm, wd_hbm = take(3)
    ab_hbm, xu_hbm = take(2) if load else (None, None)
    prev = take(1)[0] if bwd and not own else None
    got = take(2) if got_layer is not None else None
    take(n_alias)
    y_outs = take(N_SRC) if fwd else []
    du_outs = take(N_SRC) if bwd and own else []
    grad = take(1)[0] if bwd and own else None
    finals = take(3) if bwd and not own or got_layer is not None else None
    sent = take(2) if bwd and not own else None
    ab_hbm, xu_hbm = take(2) if save else (ab_hbm, xu_hbm)
    tab_ref, idx, gate_ref, land, table, gat = take(6)
    acc, row_ref = take(2) if own else (None, None)
    gu_ref, wd_ref, g_ref, x_u = take(4)
    x_c = take(1)[0] if bwd else None
    ab_ref = take(1)[0]
    dh_ref = take(1)[0] if bwd else None
    h_ref = take(1)[0]
    dab_ref, sums = take(2) if bwd else (None, None)
    keep_buf = take(1)[0] if bwd and not own else None
    got_buf = take(1)[0] if got is not None else None
    list_sem, land_sem, w_sem = take(3)
    sum_sem = take(1)[0] if bwd else None
    keep_sem = take(1)[0] if bwd and not own else None
    read_sem, write_sem = take(2) if got is not None else (None, None)
    stage_f, out_sem = take(2) if own else (None, None)
    ab_sem, xu_sem = take(2) if save or load else (None, None)

    split = first_piece(n_exp)
    copy = pltpu.make_async_copy
    cols = spans(d)
    lo = ff // 256 * 256
    hi = ff - lo
    dot = functools.partial(lax.dot_general, preferred_element_type=F32)
    nn = (((1,), (0,)), ((), ()))
    nt = (((1,), (1,)), ((), ()))
    tn = (((0,), (0,)), ((), ()))
    al = pl.multiple_of
    n_row = N_SRC * n_blk
    glane = lax.broadcasted_iota(I32, (GRP, LANES), 1)
    gsub = lax.broadcasted_iota(I32, (GRP, LANES), 0)

    def row_at(r):
        return pl.ds(r * PITCH, FULL)

    def codes_of(tile):
        at = ROW_GOFF * LANES + tile
        if own and bwd:
            return lambda q: tab_ref[tab_ref[at] + q]
        view = tab_ref.at[pl.ds(tab_ref[at], PER_TILE)]
        return lambda q: view[q]

    def gather(codes, q):
        ids = idx.at[pl.ds(codes(q) >> 4, GRP)]
        for k in range(GRP):
            gat[row_at(q * GRP + k), :] = table[pl.ds(ids[k], FULL), :]

    def gate_column(code):
        pos = code >> 4
        row, shift = pos >> 7, pos & (LANES - 1)
        want = glane == gsub + shift
        over = glane == gsub + (shift - LANES)
        here = gate_ref[pl.ds(row, GRP, stride=0), :]
        there = gate_ref[pl.ds(row + 1, GRP, stride=0), :]
        v = jnp.where(want, here, jnp.where(over, there, 0.0))
        return jnp.where(gsub < (code & 15), jnp.sum(v, axis=1, keepdims=True), 0.0)

    def scatter(codes, q):
        ids = idx.at[pl.ds(codes(q) >> 4, GRP)]
        new = []
        for k in range(GRP):
            at = pl.ds(ids[k], FULL)
            new.append((at, acc[at, :] + row_ref[row_at(q * GRP + k), :]))
        for at, value in reversed(new):
            acc[at, :] = value

    def keep_ab(t):
        ends = (ab_ref.at[t & 1], ab_hbm.at[t])
        return copy(*(ends if save else ends[::-1]), ab_sem.at[t & 1])

    def keep_xu(t):
        ends = (x_u.at[t & 1], xu_hbm.at[t])
        return copy(*(ends if save else ends[::-1]), xu_sem.at[t & 1])

    def of(ref, t):
        return ref.at[t & 1] if save or load else ref

    def convert(codes, t):
        for q in range(0, PER_TILE, 2):
            part = []
            for p in (q, q + 1):
                code = codes(p)
                rows = [gat[pl.ds(GRP * PITCH * p + j, GRP, stride=PITCH), :]
                        for j in range(HALF if load else 0, FULL if bwd else HALF)]
                real = gsub < (code & 15)
                gate = gate_column(code)
                g_ref[GRP * p:GRP * (p + 1), :] = gate
                us, dys = ([], rows) if load else (rows[:HALF], rows[HALF:])
                part.append([jnp.where(real, v, 0.0) for v in us] + [v * gate for v in dys])
            at = slice(GRP * q, GRP * (q + 2))
            for x, o in ((None if load else of(x_u, t), 0), (x_c, 0 if load else HALF)):
                if x is None:
                    continue
                for j, (c, w) in enumerate(cols):
                    both = jnp.concatenate([part[0][o + j], part[1][o + j]], axis=0)
                    x[at, c:c + w] = both[:, :w].astype(BF16)

    def put_rows(o, value, s0):
        value = value.astype(BF16).astype(F32)
        n = value.shape[0]
        for j, (c, w) in enumerate(cols):
            row_ref[pl.ds(PITCH * s0 + o + j, n, stride=PITCH), 0:w] = value[:, c:c + w] * g_ref[s0:s0 + n, 0:w]

    low = lax.broadcasted_iota(I32, (16, 2 * hi), 1) < hi

    def middle(a, b, dh):
        sig = 0.5 * jnp.tanh(0.5 * a) + 0.5
        act = a * sig
        h = act * b
        if dh is None:
            return h, None, None
        slope = sig * (1.0 + a * (1.0 - sig))
        return h, dh * b * slope, dh * act

    def weights(e, slot):
        at = (layer, tab_ref[ROW_EXPERT * LANES + e])
        moves = []
        for i, w in enumerate((wg_hbm, wu_hbm)):
            moves.append((w.at[at + (pl.ds(0, lo),)], gu_ref.at[slot, pl.ds(i * lo, lo)]))
            moves.append((w.at[at + (pl.ds(lo, hi),)], gu_ref.at[slot, pl.ds(2 * lo + i * hi, hi)]))
        moves.append((wd_hbm.at[at], wd_ref.at[slot]))
        return [copy(a, b, w_sem.at[slot, i]) for i, (a, b) in enumerate(moves)]

    def sums_in(e, slot):
        return copy(prev.at[e], sums.at[slot], sum_sem.at[slot])

    def sums_out(e, slot):
        return copy(sums.at[slot], grad.at[e], sum_sem.at[slot])

    def keeps(e, slot):
        at = (layer, tab_ref[ROW_EXPERT * LANES + e])
        return [copy(keep_buf.at[slot, i], finals[i].at[at], keep_sem.at[slot, i]) for i in range(3)]

    def send(e, slot, part):
        return copy(keep_buf.at[slot], sent[part].at[e - part * split], keep_sem.at[slot, 3])

    def read(e, slot, part=0):
        return copy(got[part].at[e - part * split], got_buf.at[slot], read_sem.at[slot])

    def writes(e, slot):
        to = tab_ref[TAB_ROWS * LANES + e]
        return [copy(got_buf.at[slot, i], finals[i].at[got_layer, to], write_sem.at[slot, i]) for i in range(3)]

    def start(moves):
        for m in moves:
            m.start()

    def wait(moves):
        for m in moves:
            m.wait()

    n_tab = TAB_ROWS * LANES
    lists = [copy(tab_hbm.at[pl.ds(row_id * n_tab, n_tab)], tab_ref.at[pl.ds(0, n_tab)], list_sem.at[0]),
             copy(idx_hbm.at[pl.ds(row_id * N_SRC * list_len, N_SRC * list_len)], idx.at[pl.ds(0, N_SRC * list_len)],
                  list_sem.at[1]),
             copy(gate_hbm.at[pl.ds(row_id * gate_ref.shape[0], gate_ref.shape[0])], gate_ref, list_sem.at[2])]
    if got is not None:
        at = (got_layer * TAB_ROWS + ROW_PARTNER) * LANES
        lists.append(copy(tab_hbm.at[pl.ds(at, LANES)], tab_ref.at[pl.ds(n_tab, LANES)], list_sem.at[3]))
    start(lists)
    pieces = []
    for s in range(N_SRC):
        if not load:
            pieces.append((u_pieces[s], picks[0][s], s, 0, fwd))
        if bwd:
            pieces.append((dy_pieces[s], picks[1][s], s, HALF, own))
    lands = [copy(ref.at[pick], land.at[i % N_SRC], land_sem.at[i % N_SRC]) for i, (ref, pick, *_) in enumerate(pieces)]
    start(lands[:N_SRC])
    lists[0].wait()
    for e in range(DEPTH - 1):
        start(weights(e, e))
        if bwd and not own:
            sums_in(e, e).start()
    if got is not None:
        lists[3].wait()
        read(0, 0).start()
    if own:
        def clear(c, _):
            for k in range(4):
                acc[pl.ds(al(c * 1152 + 288 * k, 8), 288), :] = jnp.zeros((288, LANES), F32)
            return 0

        lax.fori_loop(0, acc.shape[0] // 1152, clear, 0)
        row_ref[...] = jnp.zeros(row_ref.shape, F32)
    rows = 256
    for i, (_, _, s, o, seed) in enumerate(pieces):
        lands[i].wait()

        def fill(c, _, i=i, o=o, seed=seed, s=s):
            r = al(c * rows, rows)
            for j in range(HALF):
                vals = land[i % N_SRC, pl.ds(r, rows), LANES * j:LANES * (j + 1)].astype(F32)
                to = pl.ds(PITCH * (s * n_blk + r) + o + j, rows, stride=PITCH)
                table[to, :] = vals
                if seed and s == 0:
                    acc[to, :] = vals
            return 0

        lax.fori_loop(0, n_blk // rows, fill, 0)
        if i + N_SRC < len(pieces):
            lands[i + N_SRC].start()
    wait(lists[1:3])
    for k in range(GRP):
        idx[N_SRC * list_len + k] = 0

    def first(q, _):
        gather(begin, 2 * q)
        gather(begin, 2 * q + 1)
        return 0

    begin = codes_of(0)
    lax.fori_loop(0, PER_TILE // 2, first, 0)
    convert(begin, 0)
    if save:
        keep_xu(0).start()
    if load:
        keep_ab(0).start()
        keep_xu(0).start()

    def expert(e, _):
        slot = e & 1
        deep = lax.rem(e, DEPTH)
        sum_slot = slot if own else deep
        wait(weights(e, deep))
        if bwd and not own:
            sums_in(e, deep).wait()
        if got is not None:
            read(0, slot).wait()
            start(writes(e, slot))

            @pl.when((e > 0) & (e < n_exp - 1))
            def _():
                wait(writes(e - 1, 1 - slot))

        @pl.when(e < n_exp - (DEPTH - 1))
        def _():
            ahead = lax.rem(e + DEPTH - 1, DEPTH)
            start(weights(e + DEPTH - 1, ahead))
            if bwd and not own:
                sums_in(e + DEPTH - 1, ahead).start()

        @pl.when(e < n_exp - 1)
        def _():
            if got is not None:
                for part in range(2):
                    @pl.when((e + 1 >= split) if part else (e + 1 < split))
                    def _(part=part):
                        read(e + 1, 1 - slot, part).start()

        if bwd and own:
            @pl.when(e > 1)
            def _():
                sums_out(e - 2, slot).wait()

            sums[slot] = jnp.zeros(sums.shape[1:], F32)

        def tile(t, _):
            if save:
                @pl.when(t > 1)
                def _():
                    keep_ab(t - 2).wait()

                @pl.when(t > 0)
                def _():
                    keep_xu(t - 1).wait()
            if load:
                keep_ab(t).wait()
                keep_xu(t).wait()
                keep_ab(t + 1).start()
                keep_xu(t + 1).start()
            ab, xu = of(ab_ref, t), of(x_u, t)
            before, after = codes_of(jnp.maximum(t - 1, 0)), codes_of(t + 1)
            for q in range(PER_TILE):
                if own:
                    scatter(before, q)
                gather(after, q)
            front = ROWS if own and bwd else ROWS // 2
            for s0 in range(0, ROWS, front):
                sl = slice(s0, s0 + front)
                if not load:
                    ab[sl, :] = dot(xu[sl, :], gu_ref[deep], nt)
                if bwd:
                    dh_ref[sl, :] = dot(x_c[sl, :], wd_ref[deep], nt)
            for r in range(0, ROWS, 16):
                rows = slice(r, r + 16)
                for c in range(0, lo, LANES):
                    h, da, db = middle(ab[rows, c:c + LANES], ab[rows, lo + c:lo + c + LANES],
                                       dh_ref[rows, c:c + LANES] if bwd else None)
                    h_ref[rows, c:c + LANES] = h.astype(BF16)
                    if bwd:
                        dab_ref[rows, c:c + LANES] = da.astype(BF16)
                        dab_ref[rows, lo + c:lo + c + LANES] = db.astype(BF16)
                a = ab[rows, 2 * lo:]
                b = pltpu.roll(a, hi, 1)
                dh = dh_ref[rows, lo:] if bwd else None
                if bwd:
                    dh = jnp.concatenate([dh, dh], axis=1)
                h, da, db = middle(a, b, dh)
                h_ref[rows, lo:] = h[:, :hi].astype(BF16)
                if bwd:
                    dab_ref[rows, 2 * lo:] = jnp.where(low, da, pltpu.roll(db, hi, 1)).astype(BF16)
            half = ROWS // 2
            for s0 in range(0, ROWS, half):
                sl = slice(s0, s0 + half)
                if fwd:
                    put_rows(0, dot(h_ref[sl, :], wd_ref[deep], nn), s0)
                if bwd and own:
                    put_rows(HALF, dot(dab_ref[sl, :], gu_ref[deep], nn), s0)
            if bwd:
                view = sums.at[sum_slot]
                view[0:2 * ff, :] += dot(dab_ref[...], xu[...], tn)
                view[2 * ff:, :] += dot(h_ref[...], x_c[...], tn)
            convert(after, t + 1)
            if save:
                keep_ab(t).start()
                keep_xu(t + 1).start()
            return 0

        lax.fori_loop(tab_ref[ROW_BOUND * LANES + e], tab_ref[ROW_BOUND * LANES + e + 1], tile, 0)
        if bwd and own:
            sums_out(e, slot).start()
        if bwd and not own:
            @pl.when(e > 1)
            def _():
                wait(keeps(e - 2, slot) + [send(0, slot, 0)])

            for i in range(2):
                keep_buf[slot, i, 0:lo, :] = sums[deep, i * lo:(i + 1) * lo, :].astype(BF16)
                keep_buf[slot, i, lo:, :] = sums[deep, 2 * lo + i * hi:2 * lo + (i + 1) * hi, :].astype(BF16)
            keep_buf[slot, 2] = sums[deep, 2 * ff:, :].astype(BF16)
            start(keeps(e, slot))
            for part in range(2):
                @pl.when((e >= split) if part else (e < split))
                def _(part=part):
                    send(e, slot, part).start()
        return 0

    lax.fori_loop(0, n_exp, expert, 0)
    ends = ((n_exp - 2, (n_exp - 2) % 2), (n_exp - 1, (n_exp - 1) % 2))
    n_tiles = tab_ref[ROW_BOUND * LANES + n_exp]
    if save:
        wait([keep_ab(n_tiles - 2), keep_ab(n_tiles - 1), keep_xu(n_tiles - 1)])
    if save or load:
        keep_xu(n_tiles).wait()
    if load:
        keep_ab(n_tiles).wait()
    if own:
        end = codes_of(tab_ref[ROW_BOUND * LANES + n_exp] - 1)
        lax.fori_loop(0, PER_TILE, lambda q, _: (scatter(end, q), 0)[1], 0)
        flights = {}
        for o, out in ((HALF, du_outs), (0, y_outs)):
            for s in range(N_SRC if out else 0):
                wide = s == 0 or p_f32
                stage = stage_f.at[s] if wide else land.at[s]
                if s in flights:
                    flights[s].wait()

                def fetch(c, _, stage=stage, s=s, o=o):
                    r = al(c * rows, rows)
                    for j in range(HALF):
                        at = pl.ds(PITCH * (s * n_blk + r) + o + j, rows, stride=PITCH)
                        stage[pl.ds(r, rows), LANES * j:LANES * (j + 1)] = acc[at, :].astype(stage.dtype)
                    return 0

                lax.fori_loop(0, n_blk // rows, fetch, 0)
                flights[s] = copy(stage, out[s], out_sem.at[s])
                flights[s].start()
        wait(flights.values())
        if bwd:
            for e, slot in ends:
                sums_out(e, slot).wait()
    else:
        for e, slot in ends:
            wait(keeps(e, slot) + [send(0, slot, 0)])
    if got is not None:
        for e, slot in ends:
            wait(writes(e, slot))


def run_experts(routes, layer, u, dy, weights, prev, finals, fwd, own, p_f32=False, got=None, kept=None):
    tab, idx, gates = routes
    bwd = dy is not None
    wg, wu, wd = weights
    save, load = fwd and not bwd, kept is not None
    n_blk, wide = (dy or u)[0][0].shape[-2:]
    n_layers, n_local, ff, d = wd.shape
    n_exp = n_local // 2
    row_id = layer
    list_len = idx.shape[0] // (n_layers * N_SRC)

    arrays = lambda pieces: [v for v, _ in pieces]
    operands = [tab, idx, gates] + ([] if load else arrays(u)) + (arrays(dy) if bwd else []) + [wg, wu, wd] + list(kept or ())
    out_shape, aliases = [], {}
    for use in (fwd, bwd and own):
        if use:
            out_shape += [jax.ShapeDtypeStruct((n_blk, wide), F32 if s == 0 or p_f32 else BF16) for s in range(N_SRC)]
    if bwd and own:
        out_shape.append(jax.ShapeDtypeStruct((n_exp, 3 * ff, d), F32))
    if bwd and not own:
        operands.append(prev)
    if got is not None:
        operands += got
    for i, f in enumerate(finals or ()):
        aliases[len(operands)] = len(out_shape) + i
        operands.append(f)
    if bwd and not own or finals:
        out_shape += [jax.ShapeDtypeStruct((n_layers, n_local, ff, d), BF16)] * 3
    if bwd and not own:
        out_shape += [jax.ShapeDtypeStruct((n, 3, ff, d), BF16) for n in (first_piece(n_exp), n_exp - first_piece(n_exp))]
    if save:
        most = n_exp * (SLOT_GROUPS // PER_TILE) + 2
        out_shape += [jax.ShapeDtypeStruct((most, ROWS, 2 * ff), F32), jax.ShapeDtypeStruct((most, ROWS, d), BF16)]
    sem = lambda *s: pltpu.SemaphoreType.DMA(s)
    mid = lambda n, dt: pltpu.VMEM((ROWS, n), dt)
    twin = lambda n, dt: pltpu.VMEM((2, ROWS, n), dt) if save or load else mid(n, dt)
    table, rows = pltpu.VMEM((PITCH * N_SRC * n_blk, LANES), F32), pltpu.VMEM((PITCH * ROWS, LANES), F32)
    scratch = [pltpu.SMEM(((TAB_ROWS + 1) * LANES,), I32), pltpu.SMEM((N_SRC * list_len + LANES,), I32),
               pltpu.VMEM((N_SRC * list_len // LANES + 8, LANES), F32), pltpu.VMEM((N_SRC, n_blk, wide), BF16)]
    scratch += [table, rows] * (1 + own)
    scratch += [pltpu.VMEM((DEPTH, 2 * ff, d), BF16), pltpu.VMEM((DEPTH, ff, d), BF16), mid(LANES, F32)]
    scratch += [twin(d, BF16)] + [mid(d, BF16)] * bwd + [twin(2 * ff, F32)] + [mid(ff, F32)] * bwd + [mid(ff, BF16)]
    scratch += [mid(2 * ff, BF16), pltpu.VMEM((2 if own else DEPTH, 3 * ff, d), F32)] * bwd
    if bwd and not own:
        scratch.append(pltpu.VMEM((2, 3, ff, d), BF16))
    if got is not None:
        scratch.append(pltpu.VMEM((2, 3, ff, d), BF16))
    scratch += [sem(4), sem(N_SRC), sem(DEPTH, 5)] + [sem(DEPTH)] * bwd
    if bwd and not own:
        scratch.append(sem(2, 4))
    if got is not None:
        scratch += [sem(2), sem(2, 3)]
    if own:
        scratch += [pltpu.VMEM((N_SRC if p_f32 else 1, n_blk, wide), F32), sem(N_SRC)]
    if save or load:
        scratch += [sem(2), sem(2)]
    passes = 2 + fwd + bwd * (4 + 2 * own)
    flops = 2 * d * ff * passes * n_blk * N_SRC * 2
    hoist = 1300 if not own else 600 if load else 750 if save else 900
    picks = [[i for _, i in u] if u else None, [i for _, i in dy] if bwd else None]
    cfg = (fwd, bwd, own, layer, n_blk, d, ff, n_exp, picks, row_id, list_len, p_f32, len(aliases),
           None if got is None else 1 - layer)
    return pl.pallas_call(
        functools.partial(expert_kernel, cfg),
        out_shape=out_shape,
        in_specs=[any_space] * len(operands),
        out_specs=[any_space] * len(out_shape),
        scratch_shapes=scratch,
        input_output_aliases=aliases,
        compiler_params=pltpu.CompilerParams(
            vmem_limit_bytes=VMEM_LIMIT),
        cost_estimate=pl.CostEstimate(flops=flops, bytes_accessed=3 * 2 * n_exp * d * ff, transcendentals=0),
        name=f"experts_{'f' if fwd else ''}{'b' if bwd else ''}_{'own' if own else 'other'}_{layer}",
    )(*operands)


def place_kernel(layer, n_exp, tab_ref, got_ref, *refs):
    outs, (buf, in_sem, out_sem) = refs[3:6], refs[6:]
    reads = [pltpu.make_async_copy(got_ref.at[i], buf.at[i], in_sem.at[i]) for i in range(n_exp)]
    for read in reads:
        read.start()
    writes = []
    for i, read in enumerate(reads):
        read.wait()
        e = tab_ref[i]
        for k, out in enumerate(outs):
            writes.append(pltpu.make_async_copy(buf.at[i, k], out.at[layer, e], out_sem.at[i, k]))
            writes[-1].start()
    for write in writes:
        write.wait()


def place(partner, layer, got, finals):
    n_exp = got.shape[0]
    return pl.pallas_call(
        functools.partial(place_kernel, layer, n_exp),
        out_shape=[jax.ShapeDtypeStruct(f.shape, f.dtype) for f in finals],
        grid_spec=pltpu.PrefetchScalarGridSpec(
            num_scalar_prefetch=1, grid=(1,), in_specs=[any_space] * 4, out_specs=[any_space] * 3,
            scratch_shapes=[pltpu.VMEM(got.shape, got.dtype), pltpu.SemaphoreType.DMA((n_exp,)),
                            pltpu.SemaphoreType.DMA((n_exp, 3))]),
        input_output_aliases={2: 0, 3: 1, 4: 2},
        compiler_params=pltpu.CompilerParams(vmem_limit_bytes=VMEM_LIMIT),
        cost_estimate=pl.CostEstimate(flops=0, bytes_accessed=4 * got.size, transcendentals=0),
        name=f"place_{layer}",
    )(partner, got, *finals)


def peer(rel):
    return {name: (lax.axis_index(name) + ((rel >> bit) & 1)) % 2 for bit, name in enumerate(("ep", "core", "x"))}


def meet(rels):
    barrier = pltpu.get_barrier_semaphore()
    for rel in rels:
        pl.semaphore_signal(barrier, inc=1, device_id=peer(rel), device_id_type=MESH)
    pl.semaphore_wait(barrier, len(rels))


def remote(src, dst, send, recv, rel):
    return pltpu.make_async_remote_copy(src_ref=src, dst_ref=dst, send_sem=send, recv_sem=recv,
                                        device_id=peer(rel), device_id_type=MESH)


def share_kernel(n_rel, mine_ref, all_ref, send_sem, recv_sem):
    meet(range(1, n_rel))
    copies = [remote(mine_ref, all_ref.at[rel], send_sem.at[rel], recv_sem.at[rel], rel) for rel in range(1, n_rel)]
    for copy in copies:
        copy.start()
    all_ref[0] = mine_ref[...]
    for copy in copies:
        copy.wait()


def share(mine, n_rel):
    return pl.pallas_call(
        functools.partial(share_kernel, n_rel),
        out_shape=jax.ShapeDtypeStruct((n_rel,) + mine.shape, mine.dtype),
        in_specs=[in_vmem],
        out_specs=in_vmem,
        scratch_shapes=[pltpu.SemaphoreType.DMA((n_rel,)), pltpu.SemaphoreType.DMA((n_rel,))],
        compiler_params=pltpu.CompilerParams(collective_id=0, has_side_effects=True),
        cost_estimate=pl.CostEstimate(flops=10 ** 7, bytes_accessed=mine.size * 4 * n_rel, transcendentals=0),
        name="share_lists",
    )(mine)


def blocks_kernel(cfg, *refs):
    n_chunk, reduce, back, d, sizes = cfg
    refs = list(refs)
    take = lambda n: [refs.pop(0) for _ in range(n)]
    parts = take(N_SRC)
    m_ref = take(1)[0]
    list_refs, left_ref = take(2) if sizes else (), take(1)[0] if back else None
    o_total, o_a, o_b = take(3)
    plan_refs, grad_ref = take(3) if sizes else (), take(1)[0] if back else None
    in_f, in_b, got_f, s_wire, r_wire, u_wire, y_wire, t_buf, u_buf, y_buf, load, send, recv, put = take(14)
    n_rows = t_buf.shape[0] // n_chunk
    cut = [pl.ds(k * n_rows, n_rows) for k in range(n_chunk)]
    thin = [pl.ds(k * n_rows // 2, n_rows // 2) for k in range(n_chunk)]
    side = lax.broadcasted_iota(I32, (n_rows // 2, LANES), 1) < LANES // 2
    tiles = d // LANES
    turn = lambda v: pltpu.roll(v, LANES // 2, 1)
    lanes = lambda v, j: v[:, LANES * j:LANES * (j + 1)]

    def pack(wire, k, value):
        top, low = value[:n_rows // 2], value[n_rows // 2:]
        turned = [turn(lanes(low, j)) for j in range(tiles + 1)]
        parts = [lanes(top, j) for j in range(tiles)] + [jnp.where(side, lanes(top, tiles), turned[0])]
        parts += [jnp.where(side, turned[j], turned[j + 1]) for j in range(tiles)]
        for j, part in enumerate(parts):
            wire[thin[k], LANES * j:LANES * (j + 1)] = part.astype(BF16)

    def unpack(wire, k):
        value = wire[thin[k], :].astype(F32)
        turned = [turn(lanes(value, tiles + j)) for j in range(tiles + 1)]
        top = [lanes(value, j) for j in range(tiles)] + [jnp.where(side, lanes(value, tiles), 0.0)]
        low = [jnp.where(side, turned[j], turned[j + 1]) for j in range(tiles)] + [jnp.where(side, turned[tiles], 0.0)]
        return jnp.concatenate([jnp.concatenate(top, axis=1), jnp.concatenate(low, axis=1)], axis=0)

    chunks = range(n_chunk)
    loads = {}
    for i, part in enumerate(parts[:2] if reduce else parts):
        buf = in_f.at[i] if reduce or i == 0 else in_b.at[i - 1]
        for k in chunks:
            loads[i, k] = pltpu.make_async_copy(part.at[cut[k]], buf.at[cut[k]], load.at[i, k])
    order = (1, 0) if reduce else range(N_SRC)
    for i in order:
        for k in chunks:
            loads[i, k].start()
    u_buf[...] = jnp.zeros(u_buf.shape, BF16)
    meet((Y, CORE))
    links = []
    copy_in = pltpu.make_async_copy

    def link(src, dst, rel, cut=cut):
        n = len(links)
        links.append([remote(src.at[cut[k]], dst.at[cut[k]], send.at[n, k], recv.at[n, k], rel) for k in chunks])
        return links[-1]

    if reduce:
        first = link(parts[3], got_f.at[1], CORE)
        second = link(parts[2], got_f.at[0], CORE)
        over = link(s_wire, r_wire, Y, thin)
        for copies in (first, second):
            for copy in copies:
                copy.start()
        for k in chunks:
            loads[1, k].wait()
            first[k].wait_recv()
            pack(s_wire, k, in_f[1, cut[k], :] + got_f[1, cut[k], :])
            over[k].start()
    to_y = link(u_wire, y_wire, Y, thin)
    to_core = link(u_buf, o_b.at[0], CORE)
    puts = []
    for k in chunks:
        if reduce:
            loads[0, k].wait()
            second[k].wait_recv()
            over[k].wait_recv()
            total = in_f[0, cut[k], :] + got_f[0, cut[k], :] + unpack(r_wire, k)
        else:
            for i in range(N_SRC):
                loads[i, k].wait()
            total = in_f[0, cut[k], :]
            for i in range(N_SRC - 1):
                total = total + in_b[i, cut[k], :].astype(F32)
        total = total.astype(BF16)
        t_buf[cut[k], :] = total
        dims = (((1,), (1 if back else 0,)), ((), ()))
        mixed = lax.dot_general(total[:, :d], m_ref[...], dims, preferred_element_type=F32)
        u_buf[cut[k], 0:d] = (total[:, :d].astype(F32) + mixed).astype(BF16)
        pack(u_wire, k, u_buf[cut[k], :].astype(F32))
        to_y[k].start()
        to_core[k].start()
        puts.append(pltpu.make_async_copy(u_buf.at[cut[k]], o_a.at[0, cut[k]], put.at[0, k]))
        puts.append(pltpu.make_async_copy(t_buf.at[cut[k]], o_total.at[cut[k]], put.at[1, k]))
        for copy in puts[-2:]:
            copy.start()
    if sizes:
        plan_kernel(*sizes, *list_refs, *plan_refs)
    if back:
        grad_ref[...] = lax.dot_general(left_ref[:, :d], t_buf[:, :d], (((0,), (0,)), ((), ())), preferred_element_type=F32)
    on = link(y_buf, o_b.at[1], CORE)
    for k in chunks:
        to_y[k].wait_recv()
        y_buf[cut[k], :] = unpack(y_wire, k).astype(BF16)
        on[k].start()
        puts.append(copy_in(y_buf.at[cut[k]], o_a.at[1, cut[k]], put.at[2, k]))
        puts[-1].start()
    waited = [to_y] + ([first, second, over] if reduce else [])
    for copies in links:
        for copy in copies:
            if any(copies is w for w in waited):
                copy.wait_send()
            else:
                copy.wait()
    for copy in puts:
        copy.wait()


def complete_blocks(parts, m, reduce, back, ident, sizes=None, lists=(), left=(), n_chunk=4):
    n_blk, wide = parts[0].shape
    d = m.shape[0]
    sem = lambda *s: pltpu.SemaphoreType.DMA(s)
    pair = jax.ShapeDtypeStruct((2, n_blk, wide), BF16)
    extra = plan_shapes(sizes) if sizes else []
    extra += [jax.ShapeDtypeStruct((d, d), F32)] * len(left)
    buf = lambda n, dt: pltpu.VMEM((n, n_blk, wide) if n else (n_blk, wide), dt)
    return pl.pallas_call(
        functools.partial(blocks_kernel, (n_chunk, reduce, back, d, sizes)),
        out_shape=[jax.ShapeDtypeStruct((n_blk, wide), BF16)] + [pair] * 2 + extra,
        in_specs=[any_space] * N_SRC + [in_vmem] * (1 + len(lists) + len(left)),
        out_specs=[any_space] * 3 + [in_vmem] * len(extra),
        scratch_shapes=[buf(2, F32), buf(3, BF16), buf(2, F32)] + [pltpu.VMEM((n_blk // 2, 2 * d), BF16)] * 4 + [
            buf(0, BF16), buf(0, BF16), buf(0, BF16), sem(4, n_chunk), sem(6, n_chunk), sem(6, n_chunk), sem(3, n_chunk)],
        compiler_params=pltpu.CompilerParams(collective_id=ident, has_side_effects=True, vmem_limit_bytes=VMEM_LIMIT),
        cost_estimate=pl.CostEstimate(flops=10 ** 8, bytes_accessed=n_blk * wide * 40, transcendentals=0),
        name=f"complete_blocks_{ident}",
    )(*parts, m, *lists, *left)


def solution(mesh):
    ep_size, dp_size = mesh.shape['ep'], mesh.shape['dp']
    sub = Mesh(mesh.devices.reshape(ep_size, dp_size // 2, 2), ('ep', 'x', 'core'))
    tok_axes = ('x', 'core', 'ep')
    tok_spec = P(tok_axes, None)
    route_spec = P(None, tok_axes, None)
    whole_spec = P(None, None, None)
    expert_spec = P(None, 'ep', None, None)
    flip = [(0, 1), (1, 0)]
    move = lambda v, axis: lax.ppermute(v, axis, flip)
    move_diag = lambda v: lax.ppermute(v, ('ep', 'core'), [(0, 3), (1, 2), (2, 1), (3, 0)])
    fence = lax.optimization_barrier

    def device_step(tokens, d_out, expert_ids, gate_vals, w_mix, w_gate, w_up, w_down):
        n_layers, d = w_mix.shape[0], w_mix.shape[1]
        n_tok = tokens.shape[0]
        top = expert_ids.shape[2]
        n_local = w_gate.shape[1]
        n_exp = n_local * ep_size
        n = n_tok * top
        n_rel = 2 * N_SRC
        wide = cdiv(d, LANES) * LANES
        weights = (jnp.swapaxes(w_gate, 2, 3), jnp.swapaxes(w_up, 2, 3), w_down)
        pad = lambda v: jnp.pad(v, ((0, 0), (0, wide - d)))
        send_three = lambda p: [move(p[1], 'ep'), move(p[2], 'core'), move_diag(p[3])]

        def own_sum(p, got):
            return sum([g.astype(F32) for g in got], p)[:, :d].astype(BF16)

        one = lambda v: v.reshape(1, n_tok, wide)
        pairs = lambda a, b: [(a, 0), (a, 1), (b, 0), (b, 1)]

        one = lambda v: v.reshape(1, n_tok, wide)
        pairs = lambda a, b: [(a, 0), (a, 1), (b, 0), (b, 1)]
        singles = lambda *v: [(one(a), 0) for a in v]

        u0 = pad((tokens.astype(F32) + jnp.dot(tokens, w_mix[0], preferred_element_type=F32)).astype(BF16))
        u0_y, u0_c = move(u0, 'ep'), move(u0, 'core')
        lists = [sorted_list(expert_ids[l], gate_vals[l]) for l in range(n_layers)]
        counts = jnp.sum((expert_ids.transpose(0, 2, 1).reshape(n_layers, n, 1) == jnp.arange(n_exp, dtype=I32)).astype(F32), axis=1)
        packed = jnp.concatenate([jnp.concatenate([v[0] for v in lists] + [v[1] for v in lists]).reshape(-1, LANES),
                                  jnp.pad(counts, ((0, 8 - n_layers), (0, LANES - n_exp)))], axis=0)
        dy = pad(d_out)
        u0_y, u0_c, packed, dy = fence((u0_y, u0_c, packed, dy))
        u0_d = move(u0_y, 'core')
        shared = share(packed, N_SRC)
        dy, shared = fence((dy, shared))
        shared_x = move(shared, 'x')
        dy_y, dy_x = move(dy, 'ep'), move(dy, 'x')
        sizes = (n_layers, n_local, n_tok, n // LANES)
        routes = plan(shared, shared, sizes)
        u0_half = singles(u0, u0_y, u0_c, u0_d)
        *part, ab0, xu0 = run_experts(routes, 0, u0_half, None, weights, None, None, True, True, p_f32=True)
        dy_y, dy_x, shared_x, part = fence((dy_y, dy_x, shared_x, part))
        dy_c, dy_d, dy_xy, dy_xc = move(dy, 'core'), move(dy_y, 'core'), move(dy_y, 'x'), move(dy_x, 'core')
        y0, u1_a, u1_b, *routes_x = complete_blocks(part, w_mix[1], True, False, 1, sizes, (shared, shared_x))
        routes_x = flat(*routes_x)
        dy_c, dy_d, dy_xy, dy_xc, u0_p, u0_q, y0, u1_a, u1_b = fence(
            (dy_c, dy_d, dy_xy, dy_xc, u0, u0_y, y0, u1_a, u1_b))
        dy_xd = move(dy_xy, 'core')
        u1_xa = move(u1_a, 'x')
        out = run_experts(routes, 1, pairs(u1_a, u1_b), singles(dy, dy_y, dy_c, dy_d), weights, None, None, True, True)
        u1_xa, dy_xd, u0_p, u0_q, out = fence((u1_xa, dy_xd, u0_p, u0_q, out))
        y_part, du_part, g1 = out[:4], out[4:8], out[8]
        u1_xb = move(u1_xa, 'core')
        got = send_three(du_part)
        u0_x, u0_xy = move(u0_p, 'x'), move(u0_q, 'x')
        out = run_experts(routes_x, 1, pairs(u1_xa, u1_xb), singles(dy_x, dy_xy, dy_xc, dy_xd), weights, g1, None,
                          False, False)
        got, u0_x, u0_xy, out = fence((got, u0_x, u0_xy, out))
        *finals, sent_a, sent_b = out
        got1 = [move(sent_a, 'core'), move(sent_b, 'core')]
        du1, dx_a, dx_b, g_mix1 = complete_blocks([du_part[0], *got], w_mix[1], False, True, 2, left=(y0,))
        tx = lambda x, du: jnp.einsum('td,te->de', x, du, preferred_element_type=F32)
        dx_a, y_part, got1, u0_x, u0_xy, g_mix1 = fence((dx_a, y_part, got1, u0_x, u0_xy, g_mix1))
        dx_xa = move(dx_a, 'x')
        theirs1 = move(g_mix1, 'core')
        got_y = send_three(y_part)
        u0_xc, u0_xd = move(u0_x, 'core'), move(u0_xy, 'core')
        out = run_experts(routes, 0, None, pairs(dx_a, dx_b), weights, None, finals, False, True, got=got1, kept=(ab0, xu0))
        dx_xa, got_y, u0_xc, u0_xd, theirs1, out = fence((dx_xa, got_y, u0_xc, u0_xd, theirs1, out))
        du_part, g0, finals = out[:4], out[4], out[5:]
        dx_xb = move(dx_xa, 'core')
        got = send_three(du_part)
        part1 = (g_mix1 + theirs1).astype(BF16)
        theirs1 = move(part1, 'ep')
        du_part, dx_xb, part1 = fence((du_part, dx_xb, part1))
        out = run_experts(routes_x, 0, singles(u0_x, u0_xy, u0_xc, u0_xd), pairs(dx_xa, dx_xb), weights, g0, finals,
                          False, False)
        got, theirs1, got_y, y_own, out = fence((got, theirs1, got_y, y_part[0], out))
        *finals, sent_a, sent_b = out
        got_a, got_b = move(sent_a, 'core'), move(sent_b, 'core')
        add = lambda a, b: a.astype(F32) + b.astype(F32)
        part1 = add(part1, theirs1).astype(BF16)
        theirs1 = move(part1, 'x')
        du0 = own_sum(du_part[0], got)
        part0 = tx(tokens, du0).astype(BF16)
        theirs0 = move(part0, 'ep')
        dx0 = (du0.astype(F32) + jnp.einsum('te,de->td', du0, w_mix[0], preferred_element_type=F32)).astype(BF16)
        row = lambda a, b: lax.slice_in_dim(routes[0], ROW_PARTNER * LANES + a, ROW_PARTNER * LANES + b)
        piece = first_piece(n_local // 2)
        y1 = own_sum(y_own, got_y).T
        dx0, y1, got_a, finals = fence((dx0, y1, got_a, finals))
        finals = place(row(0, piece), 0, got_a, finals)
        theirs0, finals = fence((theirs0, finals))
        part0 = add(part0, theirs0).astype(BF16)
        theirs0 = move(part0, 'x')
        part0, dx0, got_b = fence((part0, dx0.T, got_b))
        finals = place(row(piece, n_local // 2), 0, got_b, finals)
        theirs0, theirs1, finals = fence((theirs0, theirs1, finals))
        total0 = add(part0, theirs0).astype(BF16)
        g_mix = jnp.stack([add(total0, move(total0, 'core')), add(part1, theirs1)]).astype(BF16)
        return (y1.T, dx0.T, g_mix, jnp.swapaxes(finals[0], 2, 3), jnp.swapaxes(finals[1], 2, 3), finals[2])

    return jax.shard_map(device_step, mesh=sub,
                         in_specs=(tok_spec, tok_spec, route_spec, route_spec, whole_spec,
                                   expert_spec, expert_spec, expert_spec),
                         out_specs=(tok_spec, tok_spec, whole_spec, expert_spec, expert_spec, expert_spec),
                         check_vma=False)
```

```python
import functools

import jax
import jax.numpy as jnp
from jax import lax
from jax.experimental import pallas as pl
from jax.experimental.pallas import tpu as pltpu
from jax.sharding import Mesh, PartitionSpec as P

F32, BF16, I32 = jnp.float32, jnp.bfloat16, jnp.int32
MESH = pl.DeviceIdType.MESH
ROWS = 384
GRP = 8
PITCH = 9
DEPTH = 3
FULL = 8
HALF = 4
CAP_FACTOR = 3
LANES = 128
N_SRC = 4
Y, CORE, X = 1, 2, 4
VMEM_LIMIT = 62 * 1024 * 1024
PER_TILE = ROWS // GRP
ROW_BOUND, ROW_GOFF, ROW_EXPERT, ROW_PARTNER, TAB_ROWS = 32, 33, 34, 35, 40
SLOT_GROUPS = 256


def cdiv(a, b):
    return (a + b - 1) // b


def first_piece(n_exp):
    return n_exp * 5 // 8


def spans(d):
    return [(LANES * j, min(LANES, d - LANES * j)) for j in range(cdiv(d, LANES))]


any_space = pl.BlockSpec(memory_space=pl.ANY)
in_vmem = pl.BlockSpec(memory_space=pltpu.VMEM)


def sorted_list(expert_ids, gate_vals):
    n_tok, top = expert_ids.shape
    n = n_tok * top
    keys = expert_ids.T.reshape(n) * n + jnp.arange(n, dtype=I32)
    keys, gates = lax.sort((keys, gate_vals.T.reshape(n)), num_keys=1, is_stable=False)
    return (keys % n_tok).astype(F32), gates


def plan_kernel(n_layers, n_local, n_tok, list_rows, deal_ref, all_ref, tab_ref, idx_ref, gate_ref):
    n_mine = n_local // 2
    core, ep = lax.axis_index('core'), lax.axis_index('ep')
    list_len = list_rows * LANES
    lane = lambda n: lax.broadcasted_iota(I32, (n, LANES), 1).astype(F32)
    sub = lambda n: lax.broadcasted_iota(I32, (n, LANES), 0).astype(F32)
    over_lanes = lambda v: jnp.sum(v, axis=1, keepdims=True)
    over_subs = lambda v: jnp.sum(v, axis=0, keepdims=True)
    l16, s16 = lane(n_mine), sub(n_mine)
    groups = lambda c: jnp.floor((c + (GRP - 0.5)) * (1.0 / GRP))
    for l in range(n_layers):
        cnt = all_ref[:, 2 * n_layers * list_rows + l, :]
        ends = cnt
        step = 1
        while step < 2 * n_local:
            ends = ends + jnp.where(lane(N_SRC) >= step, pltpu.roll(ends, step, 1), 0.0)
            step *= 2
        starts = ends - cnt
        second = (ep > 0)
        local = lambda v: jnp.where(lane(N_SRC) < n_local, jnp.where(second, pltpu.roll(v, LANES - n_local, 1), v), 0.0)
        cnt, starts = local(cnt), local(starts)
        tiles = jnp.floor((over_subs(groups(local(deal_ref[:, 2 * n_layers * list_rows + l, :]))) + (PER_TILE - 0.5))
                          * (1.0 / PER_TILE))
        load = jnp.where(lane(1) < n_local, jnp.maximum(1.0, tiles), -1.0)
        wide = jnp.broadcast_to(load, (n_local, LANES))
        col = over_lanes(jnp.where(lane(n_local) == sub(n_local), wide, 0.0))
        ahead = (col > wide) | ((col == wide) & (sub(n_local) < lane(n_local)))
        rank = over_subs(jnp.where(ahead, 1.0, 0.0))
        odd = s16 - 2.0 * jnp.floor(s16 * 0.5 + 0.25)
        flip = jnp.where(core > 0, 1.0 - odd, odd)
        dealt = lambda f: (jnp.broadcast_to(rank, (n_mine, LANES)) == 2.0 * s16 + f) & (l16 < n_local)
        pick = dealt(flip)
        choose = lambda p, row: over_lanes(jnp.where(p, jnp.broadcast_to(row, (n_mine, LANES)), 0.0))
        mine = lambda row: choose(pick, row)
        as_row = lambda c: over_subs(jnp.where(l16 == s16, c, 0.0))
        experts = as_row(mine(lane(1)))
        partner = as_row(choose(dealt(1.0 - flip), lane(1)))
        at = l * TAB_ROWS
        off = jnp.zeros((n_mine, 1), F32)
        pos = [jnp.zeros((n_mine, LANES), F32) for _ in range(SLOT_GROUPS // LANES)]
        for s in range(N_SRC):
            c, st = mine(cnt[s:s + 1]), mine(starts[s:s + 1]) + float(s * list_len)
            ng = groups(c)
            for i in range(len(pos)):
                rel = l16 + float(LANES * i) - off
                code = (st + GRP * rel) * 16.0 + jnp.minimum(float(GRP), c - GRP * rel)
                pos[i] = jnp.where((rel >= 0) & (rel < ng), code, pos[i])
            off = off + ng
        for i in range(len(pos)):
            tab_ref[pl.ds(at + i, n_mine, stride=len(pos)), :] = pos[i].astype(I32)
        n_tiles = jnp.maximum(1.0, jnp.floor((off + (PER_TILE - 0.5)) * (1.0 / PER_TILE)))
        bounds = over_subs(jnp.where(s16 < l16, n_tiles, 0.0))
        before = over_lanes(jnp.where(l16 == s16, jnp.broadcast_to(bounds, (n_mine, LANES)), 0.0))
        t = jnp.minimum(l16, over_subs(jnp.broadcast_to(n_tiles, (n_mine, LANES))) - 1.0)
        inside = (t >= before) & (t < before + n_tiles)
        goff = over_subs(jnp.where(inside, s16 * float(SLOT_GROUPS) + (t - before) * float(PER_TILE), 0.0))
        rows = [(ROW_BOUND, bounds), (ROW_GOFF, goff), (ROW_EXPERT, experts), (ROW_PARTNER, partner)]
        for row, value in rows:
            tab_ref[at + row:at + row + 1, :] = value.astype(I32)
    for l in range(n_layers):
        pad = l * (N_SRC * list_rows + 8) + N_SRC * list_rows
        gate_ref[pad:pad + 8, :] = jnp.zeros((8, LANES), F32)
        for s in range(N_SRC):
            to = (l * N_SRC + s) * list_rows
            toks = all_ref[s, l * list_rows:(l + 1) * list_rows, :]
            idx_ref[to:to + list_rows, :] = ((toks + float(s * n_tok)) * float(PITCH)).astype(I32)
            to = l * (N_SRC * list_rows + 8) + s * list_rows
            gate_ref[to:to + list_rows, :] = all_ref[s, (n_layers + l) * list_rows:(n_layers + l + 1) * list_rows, :]


def plan_shapes(sizes):
    n_layers, _, _, list_rows = sizes
    rows = (n_layers * TAB_ROWS, n_layers * N_SRC * list_rows, n_layers * (N_SRC * list_rows + 8))
    return [jax.ShapeDtypeStruct((n, LANES), dt) for n, dt in zip(rows, (I32, I32, F32))]


def flat(tab, idx, gates):
    return tab.reshape(-1), idx.reshape(-1), gates


def plan(deal, shared, sizes):
    return flat(*pl.pallas_call(
        functools.partial(plan_kernel, *sizes),
        out_shape=plan_shapes(sizes),
        in_specs=[in_vmem] * 2, out_specs=[in_vmem] * 3,
        cost_estimate=pl.CostEstimate(flops=10 ** 7, bytes_accessed=10 ** 6, transcendentals=0),
        name="plan",
    )(deal, shared))


def expert_kernel(cfg, *refs):
    fwd, bwd, own, layer, n_blk, d, ff, n_exp, picks, row_id, list_len, p_f32, n_alias, got_layer = cfg
    save, load = fwd and not bwd, own and bwd and not fwd
    refs = list(refs)
    take = lambda n: [refs.pop(0) for _ in range(n)]
    tab_hbm, idx_hbm, gate_hbm = take(3)
    u_pieces = take(N_SRC) if not load else []
    dy_pieces = take(N_SRC) if bwd else []
    wg_hbm, wu_hbm, wd_hbm = take(3)
    ab_hbm, xu_hbm = take(2) if load else (None, None)
    prev = take(1)[0] if bwd and not own else None
    got = take(2) if got_layer is not None else None
    take(n_alias)
    y_outs = take(N_SRC) if fwd else []
    du_outs = take(N_SRC) if bwd and own else []
    grad = take(1)[0] if bwd and own else None
    finals = take(3) if bwd and not own or got_layer is not None else None
    sent = take(2) if bwd and not own else None
    ab_hbm, xu_hbm = take(2) if save else (ab_hbm, xu_hbm)
    tab_ref, idx, gate_ref, land, table, gat = take(6)
    acc, row_ref = take(2) if own else (None, None)
    gu_ref, wd_ref, g_ref, x_u = take(4)
    x_c = take(1)[0] if bwd else None
    ab_ref = take(1)[0]
    dh_ref = take(1)[0] if bwd else None
    h_ref = take(1)[0]
    dab_ref, sums = take(2) if bwd else (None, None)
    keep_buf = take(1)[0] if bwd and not own else None
    got_buf = take(1)[0] if got is not None else None
    list_sem, land_sem, w_sem = take(3)
    sum_sem = take(1)[0] if bwd else None
    keep_sem = take(1)[0] if bwd and not own else None
    read_sem, write_sem = take(2) if got is not None else (None, None)
    stage_f, out_sem = take(2) if own else (None, None)
    ab_sem, xu_sem = take(2) if save or load else (None, None)

    split = first_piece(n_exp)
    copy = pltpu.make_async_copy
    cols = spans(d)
    lo = ff // 256 * 256
    hi = ff - lo
    dot = functools.partial(lax.dot_general, preferred_element_type=F32)
    nn = (((1,), (0,)), ((), ()))
    nt = (((1,), (1,)), ((), ()))
    tn = (((0,), (0,)), ((), ()))
    al = pl.multiple_of
    n_row = N_SRC * n_blk
    glane = lax.broadcasted_iota(I32, (GRP, LANES), 1)
    gsub = lax.broadcasted_iota(I32, (GRP, LANES), 0)

    def row_at(r):
        return pl.ds(r * PITCH, FULL)

    def codes_of(tile):
        at = ROW_GOFF * LANES + tile
        if own and bwd:
            return lambda q: tab_ref[tab_ref[at] + q]
        view = tab_ref.at[pl.ds(tab_ref[at], PER_TILE)]
        return lambda q: view[q]

    def gather(codes, q):
        ids = idx.at[pl.ds(codes(q) >> 4, GRP)]
        for k in range(GRP):
            gat[row_at(q * GRP + k), :] = table[pl.ds(ids[k], FULL), :]

    def gate_column(code):
        pos = code >> 4
        row, shift = pos >> 7, pos & (LANES - 1)
        want = glane == gsub + shift
        over = glane == gsub + (shift - LANES)
        here = gate_ref[pl.ds(row, GRP, stride=0), :]
        there = gate_ref[pl.ds(row + 1, GRP, stride=0), :]
        v = jnp.where(want, here, jnp.where(over, there, 0.0))
        return jnp.where(gsub < (code & 15), jnp.sum(v, axis=1, keepdims=True), 0.0)

    def scatter(codes, q):
        ids = idx.at[pl.ds(codes(q) >> 4, GRP)]
        new = []
        for k in range(GRP):
            at = pl.ds(ids[k], FULL)
            new.append((at, acc[at, :] + row_ref[row_at(q * GRP + k), :]))
        for at, value in reversed(new):
            acc[at, :] = value

    def keep_ab(t):
        ends = (ab_ref.at[t & 1], ab_hbm.at[t])
        return copy(*(ends if save else ends[::-1]), ab_sem.at[t & 1])

    def keep_xu(t):
        ends = (x_u.at[t & 1], xu_hbm.at[t])
        return copy(*(ends if save else ends[::-1]), xu_sem.at[t & 1])

    def of(ref, t):
        return ref.at[t & 1] if save or load else ref

    def convert(codes, t):
        for q in range(0, PER_TILE, 2):
            part = []
            for p in (q, q + 1):
                code = codes(p)
                rows = [gat[pl.ds(GRP * PITCH * p + j, GRP, stride=PITCH), :]
                        for j in range(HALF if load else 0, FULL if bwd else HALF)]
                real = gsub < (code & 15)
                gate = gate_column(code)
                g_ref[GRP * p:GRP * (p + 1), :] = gate
                us, dys = ([], rows) if load else (rows[:HALF], rows[HALF:])
                part.append([jnp.where(real, v, 0.0) for v in us] + [v * gate for v in dys])
            at = slice(GRP * q, GRP * (q + 2))
            for x, o in ((None if load else of(x_u, t), 0), (x_c, 0 if load else HALF)):
                if x is None:
                    continue
                for j, (c, w) in enumerate(cols):
                    both = jnp.concatenate([part[0][o + j], part[1][o + j]], axis=0)
                    x[at, c:c + w] = both[:, :w].astype(BF16)

    def put_rows(o, value, s0):
        value = value.astype(BF16).astype(F32)
        n = value.shape[0]
        for j, (c, w) in enumerate(cols):
            row_ref[pl.ds(PITCH * s0 + o + j, n, stride=PITCH), 0:w] = value[:, c:c + w] * g_ref[s0:s0 + n, 0:w]

    low = lax.broadcasted_iota(I32, (16, 2 * hi), 1) < hi

    def middle(a, b, dh):
        sig = 0.5 * jnp.tanh(0.5 * a) + 0.5
        act = a * sig
        h = act * b
        if dh is None:
            return h, None, None
        slope = sig * (1.0 + a * (1.0 - sig))
        return h, dh * b * slope, dh * act

    def weights(e, slot):
        at = (layer, tab_ref[ROW_EXPERT * LANES + e])
        moves = []
        for i, w in enumerate((wg_hbm, wu_hbm)):
            moves.append((w.at[at + (pl.ds(0, lo),)], gu_ref.at[slot, pl.ds(i * lo, lo)]))
            moves.append((w.at[at + (pl.ds(lo, hi),)], gu_ref.at[slot, pl.ds(2 * lo + i * hi, hi)]))
        moves.append((wd_hbm.at[at], wd_ref.at[slot]))
        return [copy(a, b, w_sem.at[slot, i]) for i, (a, b) in enumerate(moves)]

    def sums_in(e, slot):
        return copy(prev.at[e], sums.at[slot], sum_sem.at[slot])

    def sums_out(e, slot):
        return copy(sums.at[slot], grad.at[e], sum_sem.at[slot])

    def keeps(e, slot):
        at = (layer, tab_ref[ROW_EXPERT * LANES + e])
        return [copy(keep_buf.at[slot, i], finals[i].at[at], keep_sem.at[slot, i]) for i in range(3)]

    def send(e, slot, part):
        return copy(keep_buf.at[slot], sent[part].at[e - part * split], keep_sem.at[slot, 3])

    def read(e, slot, part=0):
        return copy(got[part].at[e - part * split], got_buf.at[slot], read_sem.at[slot])

    def writes(e, slot):
        to = tab_ref[TAB_ROWS * LANES + e]
        return [copy(got_buf.at[slot, i], finals[i].at[got_layer, to], write_sem.at[slot, i]) for i in range(3)]

    def start(moves):
        for m in moves:
            m.start()

    def wait(moves):
        for m in moves:
            m.wait()

    n_tab = TAB_ROWS * LANES
    lists = [copy(tab_hbm.at[pl.ds(row_id * n_tab, n_tab)], tab_ref.at[pl.ds(0, n_tab)], list_sem.at[0]),
             copy(idx_hbm.at[pl.ds(row_id * N_SRC * list_len, N_SRC * list_len)], idx.at[pl.ds(0, N_SRC * list_len)],
                  list_sem.at[1]),
             copy(gate_hbm.at[pl.ds(row_id * gate_ref.shape[0], gate_ref.shape[0])], gate_ref, list_sem.at[2])]
    if got is not None:
        at = (got_layer * TAB_ROWS + ROW_PARTNER) * LANES
        lists.append(copy(tab_hbm.at[pl.ds(at, LANES)], tab_ref.at[pl.ds(n_tab, LANES)], list_sem.at[3]))
    start(lists)
    pieces = []
    for s in range(N_SRC):
        if not load:
            pieces.append((u_pieces[s], picks[0][s], s, 0, fwd))
        if bwd:
            pieces.append((dy_pieces[s], picks[1][s], s, HALF, own))
    lands = [copy(ref.at[pick], land.at[i % N_SRC], land_sem.at[i % N_SRC]) for i, (ref, pick, *_) in enumerate(pieces)]
    start(lands[:N_SRC])
    lists[0].wait()
    for e in range(DEPTH - 1):
        start(weights(e, e))
        if bwd and not own:
            sums_in(e, e).start()
    if got is not None:
        lists[3].wait()
        read(0, 0).start()
    if own:
        def clear(c, _):
            for k in range(4):
                acc[pl.ds(al(c * 1152 + 288 * k, 8), 288), :] = jnp.zeros((288, LANES), F32)
            return 0

        lax.fori_loop(0, acc.shape[0] // 1152, clear, 0)
        row_ref[...] = jnp.zeros(row_ref.shape, F32)
    rows = 256
    for i, (_, _, s, o, seed) in enumerate(pieces):
        lands[i].wait()

        def fill(c, _, i=i, o=o, seed=seed, s=s):
            r = al(c * rows, rows)
            for j in range(HALF):
                vals = land[i % N_SRC, pl.ds(r, rows), LANES * j:LANES * (j + 1)].astype(F32)
                to = pl.ds(PITCH * (s * n_blk + r) + o + j, rows, stride=PITCH)
                table[to, :] = vals
                if seed and s == 0:
                    acc[to, :] = vals
            return 0

        lax.fori_loop(0, n_blk // rows, fill, 0)
        if i + N_SRC < len(pieces):
            lands[i + N_SRC].start()
    wait(lists[1:3])
    for k in range(GRP):
        idx[N_SRC * list_len + k] = 0

    def first(q, _):
        gather(begin, 2 * q)
        gather(begin, 2 * q + 1)
        return 0

    begin = codes_of(0)
    lax.fori_loop(0, PER_TILE // 2, first, 0)
    convert(begin, 0)
    if save:
        keep_xu(0).start()
    if load:
        keep_ab(0).start()
        keep_xu(0).start()

    def expert(e, _):
        slot = e & 1
        deep = lax.rem(e, DEPTH)
        sum_slot = slot if own else deep
        wait(weights(e, deep))
        if bwd and not own:
            sums_in(e, deep).wait()
        if got is not None:
            read(0, slot).wait()
            start(writes(e, slot))

            @pl.when((e > 0) & (e < n_exp - 1))
            def _():
                wait(writes(e - 1, 1 - slot))

        @pl.when(e < n_exp - (DEPTH - 1))
        def _():
            ahead = lax.rem(e + DEPTH - 1, DEPTH)
            start(weights(e + DEPTH - 1, ahead))
            if bwd and not own:
                sums_in(e + DEPTH - 1, ahead).start()

        @pl.when(e < n_exp - 1)
        def _():
            if got is not None:
                for part in range(2):
                    @pl.when((e + 1 >= split) if part else (e + 1 < split))
                    def _(part=part):
                        read(e + 1, 1 - slot, part).start()

        if bwd and own:
            @pl.when(e > 1)
            def _():
                sums_out(e - 2, slot).wait()

            sums[slot] = jnp.zeros(sums.shape[1:], F32)

        def tile(t, _):
            if save:
                @pl.when(t > 1)
                def _():
                    keep_ab(t - 2).wait()

                @pl.when(t > 0)
                def _():
                    keep_xu(t - 1).wait()
            if load:
                keep_ab(t).wait()
                keep_xu(t).wait()
                keep_ab(t + 1).start()
                keep_xu(t + 1).start()
            ab, xu = of(ab_ref, t), of(x_u, t)
            before, after = codes_of(jnp.maximum(t - 1, 0)), codes_of(t + 1)
            for q in range(PER_TILE):
                if own:
                    scatter(before, q)
                gather(after, q)
            front = ROWS if own and bwd else ROWS // 2
            for s0 in range(0, ROWS, front):
                sl = slice(s0, s0 + front)
                if not load:
                    ab[sl, :] = dot(xu[sl, :], gu_ref[deep], nt)
                if bwd:
                    dh_ref[sl, :] = dot(x_c[sl, :], wd_ref[deep], nt)
            for r in range(0, ROWS, 16):
                rows = slice(r, r + 16)
                for c in range(0, lo, LANES):
                    h, da, db = middle(ab[rows, c:c + LANES], ab[rows, lo + c:lo + c + LANES],
                                       dh_ref[rows, c:c + LANES] if bwd else None)
                    h_ref[rows, c:c + LANES] = h.astype(BF16)
                    if bwd:
                        dab_ref[rows, c:c + LANES] = da.astype(BF16)
                        dab_ref[rows, lo + c:lo + c + LANES] = db.astype(BF16)
                a = ab[rows, 2 * lo:]
                b = pltpu.roll(a, hi, 1)
                dh = dh_ref[rows, lo:] if bwd else None
                if bwd:
                    dh = jnp.concatenate([dh, dh], axis=1)
                h, da, db = middle(a, b, dh)
                h_ref[rows, lo:] = h[:, :hi].astype(BF16)
                if bwd:
                    dab_ref[rows, 2 * lo:] = jnp.where(low, da, pltpu.roll(db, hi, 1)).astype(BF16)
            half = ROWS // 2
            for s0 in range(0, ROWS, half):
                sl = slice(s0, s0 + half)
                if fwd:
                    put_rows(0, dot(h_ref[sl, :], wd_ref[deep], nn), s0)
                if bwd and own:
                    put_rows(HALF, dot(dab_ref[sl, :], gu_ref[deep], nn), s0)
            if bwd:
                view = sums.at[sum_slot]
                view[0:2 * ff, :] += dot(dab_ref[...], xu[...], tn)
                view[2 * ff:, :] += dot(h_ref[...], x_c[...], tn)
            convert(after, t + 1)
            if save:
                keep_ab(t).start()
                keep_xu(t + 1).start()
            return 0

        lax.fori_loop(tab_ref[ROW_BOUND * LANES + e], tab_ref[ROW_BOUND * LANES + e + 1], tile, 0)
        if bwd and own:
            sums_out(e, slot).start()
        if bwd and not own:
            @pl.when(e > 1)
            def _():
                wait(keeps(e - 2, slot) + [send(0, slot, 0)])

            for i in range(2):
                keep_buf[slot, i, 0:lo, :] = sums[deep, i * lo:(i + 1) * lo, :].astype(BF16)
                keep_buf[slot, i, lo:, :] = sums[deep, 2 * lo + i * hi:2 * lo + (i + 1) * hi, :].astype(BF16)
            keep_buf[slot, 2] = sums[deep, 2 * ff:, :].astype(BF16)
            start(keeps(e, slot))
            for part in range(2):
                @pl.when((e >= split) if part else (e < split))
                def _(part=part):
                    send(e, slot, part).start()
        return 0

    lax.fori_loop(0, n_exp, expert, 0)
    ends = ((n_exp - 2, (n_exp - 2) % 2), (n_exp - 1, (n_exp - 1) % 2))
    n_tiles = tab_ref[ROW_BOUND * LANES + n_exp]
    if save:
        wait([keep_ab(n_tiles - 2), keep_ab(n_tiles - 1), keep_xu(n_tiles - 1)])
    if save or load:
        keep_xu(n_tiles).wait()
    if load:
        keep_ab(n_tiles).wait()
    if own:
        end = codes_of(tab_ref[ROW_BOUND * LANES + n_exp] - 1)
        lax.fori_loop(0, PER_TILE, lambda q, _: (scatter(end, q), 0)[1], 0)
        flights = {}
        for o, out in ((HALF, du_outs), (0, y_outs)):
            for s in range(N_SRC if out else 0):
                wide = s == 0 or p_f32
                stage = stage_f.at[s] if wide else land.at[s]
                if s in flights:
                    flights[s].wait()

                def fetch(c, _, stage=stage, s=s, o=o):
                    r = al(c * rows, rows)
                    for j in range(HALF):
                        at = pl.ds(PITCH * (s * n_blk + r) + o + j, rows, stride=PITCH)
                        stage[pl.ds(r, rows), LANES * j:LANES * (j + 1)] = acc[at, :].astype(stage.dtype)
                    return 0

                lax.fori_loop(0, n_blk // rows, fetch, 0)
                flights[s] = copy(stage, out[s], out_sem.at[s])
                flights[s].start()
        wait(flights.values())
        if bwd:
            for e, slot in ends:
                sums_out(e, slot).wait()
    else:
        for e, slot in ends:
            wait(keeps(e, slot) + [send(0, slot, 0)])
    if got is not None:
        for e, slot in ends:
            wait(writes(e, slot))


def run_experts(routes, layer, u, dy, weights, prev, finals, fwd, own, p_f32=False, got=None, kept=None):
    tab, idx, gates = routes
    bwd = dy is not None
    wg, wu, wd = weights
    save, load = fwd and not bwd, kept is not None
    n_blk, wide = (dy or u)[0][0].shape[-2:]
    n_layers, n_local, ff, d = wd.shape
    n_exp = n_local // 2
    row_id = layer
    list_len = idx.shape[0] // (n_layers * N_SRC)

    arrays = lambda pieces: [v for v, _ in pieces]
    operands = [tab, idx, gates] + ([] if load else arrays(u)) + (arrays(dy) if bwd else []) + [wg, wu, wd] + list(kept or ())
    out_shape, aliases = [], {}
    for use in (fwd, bwd and own):
        if use:
            out_shape += [jax.ShapeDtypeStruct((n_blk, wide), F32 if s == 0 or p_f32 else BF16) for s in range(N_SRC)]
    if bwd and own:
        out_shape.append(jax.ShapeDtypeStruct((n_exp, 3 * ff, d), F32))
    if bwd and not own:
        operands.append(prev)
    if got is not None:
        operands += got
    for i, f in enumerate(finals or ()):
        aliases[len(operands)] = len(out_shape) + i
        operands.append(f)
    if bwd and not own or finals:
        out_shape += [jax.ShapeDtypeStruct((n_layers, n_local, ff, d), BF16)] * 3
    if bwd and not own:
        out_shape += [jax.ShapeDtypeStruct((n, 3, ff, d), BF16) for n in (first_piece(n_exp), n_exp - first_piece(n_exp))]
    if save:
        most = n_exp * (SLOT_GROUPS // PER_TILE) + 2
        out_shape += [jax.ShapeDtypeStruct((most, ROWS, 2 * ff), F32), jax.ShapeDtypeStruct((most, ROWS, d), BF16)]
    sem = lambda *s: pltpu.SemaphoreType.DMA(s)
    mid = lambda n, dt: pltpu.VMEM((ROWS, n), dt)
    twin = lambda n, dt: pltpu.VMEM((2, ROWS, n), dt) if save or load else mid(n, dt)
    table, rows = pltpu.VMEM((PITCH * N_SRC * n_blk, LANES), F32), pltpu.VMEM((PITCH * ROWS, LANES), F32)
    scratch = [pltpu.SMEM(((TAB_ROWS + 1) * LANES,), I32), pltpu.SMEM((N_SRC * list_len + LANES,), I32),
               pltpu.VMEM((N_SRC * list_len // LANES + 8, LANES), F32), pltpu.VMEM((N_SRC, n_blk, wide), BF16)]
    scratch += [table, rows] * (1 + own)
    scratch += [pltpu.VMEM((DEPTH, 2 * ff, d), BF16), pltpu.VMEM((DEPTH, ff, d), BF16), mid(LANES, F32)]
    scratch += [twin(d, BF16)] + [mid(d, BF16)] * bwd + [twin(2 * ff, F32)] + [mid(ff, F32)] * bwd + [mid(ff, BF16)]
    scratch += [mid(2 * ff, BF16), pltpu.VMEM((2 if own else DEPTH, 3 * ff, d), F32)] * bwd
    if bwd and not own:
        scratch.append(pltpu.VMEM((2, 3, ff, d), BF16))
    if got is not None:
        scratch.append(pltpu.VMEM((2, 3, ff, d), BF16))
    scratch += [sem(4), sem(N_SRC), sem(DEPTH, 5)] + [sem(DEPTH)] * bwd
    if bwd and not own:
        scratch.append(sem(2, 4))
    if got is not None:
        scratch += [sem(2), sem(2, 3)]
    if own:
        scratch += [pltpu.VMEM((N_SRC if p_f32 else 1, n_blk, wide), F32), sem(N_SRC)]
    if save or load:
        scratch += [sem(2), sem(2)]
    passes = 2 + fwd + bwd * (4 + 2 * own)
    flops = 2 * d * ff * passes * n_blk * N_SRC * 2
    hoist = 1300 if not own else 600 if load else 750 if save else 900
    picks = [[i for _, i in u] if u else None, [i for _, i in dy] if bwd else None]
    cfg = (fwd, bwd, own, layer, n_blk, d, ff, n_exp, picks, row_id, list_len, p_f32, len(aliases),
           None if got is None else 1 - layer)
    return pl.pallas_call(
        functools.partial(expert_kernel, cfg),
        out_shape=out_shape,
        in_specs=[any_space] * len(operands),
        out_specs=[any_space] * len(out_shape),
        scratch_shapes=scratch,
        input_output_aliases=aliases,
        compiler_params=pltpu.CompilerParams(
            vmem_limit_bytes=VMEM_LIMIT),
        cost_estimate=pl.CostEstimate(flops=flops, bytes_accessed=3 * 2 * n_exp * d * ff, transcendentals=0),
        name=f"experts_{'f' if fwd else ''}{'b' if bwd else ''}_{'own' if own else 'other'}_{layer}",
    )(*operands)


def place_kernel(layer, n_exp, tab_ref, got_ref, *refs):
    outs, (buf, in_sem, out_sem) = refs[3:6], refs[6:]
    reads = [pltpu.make_async_copy(got_ref.at[i], buf.at[i], in_sem.at[i]) for i in range(n_exp)]
    for read in reads:
        read.start()
    writes = []
    for i, read in enumerate(reads):
        read.wait()
        e = tab_ref[i]
        for k, out in enumerate(outs):
            writes.append(pltpu.make_async_copy(buf.at[i, k], out.at[layer, e], out_sem.at[i, k]))
            writes[-1].start()
    for write in writes:
        write.wait()


def place(partner, layer, got, finals):
    n_exp = got.shape[0]
    return pl.pallas_call(
        functools.partial(place_kernel, layer, n_exp),
        out_shape=[jax.ShapeDtypeStruct(f.shape, f.dtype) for f in finals],
        grid_spec=pltpu.PrefetchScalarGridSpec(
            num_scalar_prefetch=1, grid=(1,), in_specs=[any_space] * 4, out_specs=[any_space] * 3,
            scratch_shapes=[pltpu.VMEM(got.shape, got.dtype), pltpu.SemaphoreType.DMA((n_exp,)),
                            pltpu.SemaphoreType.DMA((n_exp, 3))]),
        input_output_aliases={2: 0, 3: 1, 4: 2},
        compiler_params=pltpu.CompilerParams(vmem_limit_bytes=VMEM_LIMIT),
        cost_estimate=pl.CostEstimate(flops=0, bytes_accessed=4 * got.size, transcendentals=0),
        name=f"place_{layer}",
    )(partner, got, *finals)


def peer(rel):
    return {name: (lax.axis_index(name) + ((rel >> bit) & 1)) % 2 for bit, name in enumerate(("ep", "core", "x"))}


def meet(rels):
    barrier = pltpu.get_barrier_semaphore()
    for rel in rels:
        pl.semaphore_signal(barrier, inc=1, device_id=peer(rel), device_id_type=MESH)
    pl.semaphore_wait(barrier, len(rels))


def remote(src, dst, send, recv, rel):
    return pltpu.make_async_remote_copy(src_ref=src, dst_ref=dst, send_sem=send, recv_sem=recv,
                                        device_id=peer(rel), device_id_type=MESH)


def share_kernel(n_rel, mine_ref, all_ref, send_sem, recv_sem):
    meet(range(1, n_rel))
    copies = [remote(mine_ref, all_ref.at[rel], send_sem.at[rel], recv_sem.at[rel], rel) for rel in range(1, n_rel)]
    for copy in copies:
        copy.start()
    all_ref[0] = mine_ref[...]
    for copy in copies:
        copy.wait()


def share(mine, n_rel):
    return pl.pallas_call(
        functools.partial(share_kernel, n_rel),
        out_shape=jax.ShapeDtypeStruct((n_rel,) + mine.shape, mine.dtype),
        in_specs=[in_vmem],
        out_specs=in_vmem,
        scratch_shapes=[pltpu.SemaphoreType.DMA((n_rel,)), pltpu.SemaphoreType.DMA((n_rel,))],
        compiler_params=pltpu.CompilerParams(collective_id=0, has_side_effects=True),
        cost_estimate=pl.CostEstimate(flops=10 ** 7, bytes_accessed=mine.size * 4 * n_rel, transcendentals=0),
        name="share_lists",
    )(mine)


def blocks_kernel(cfg, *refs):
    n_chunk, reduce, back, d, sizes = cfg
    refs = list(refs)
    take = lambda n: [refs.pop(0) for _ in range(n)]
    parts = take(N_SRC)
    m_ref = take(1)[0]
    list_refs, left_ref = take(2) if sizes else (), take(1)[0] if back else None
    o_total, o_a, o_b = take(3)
    plan_refs, grad_ref = take(3) if sizes else (), take(1)[0] if back else None
    in_f, in_b, got_f, s_wire, r_wire, u_wire, y_wire, t_buf, u_buf, y_buf, load, send, recv, put = take(14)
    n_rows = t_buf.shape[0] // n_chunk
    cut = [pl.ds(k * n_rows, n_rows) for k in range(n_chunk)]
    thin = [pl.ds(k * n_rows // 2, n_rows // 2) for k in range(n_chunk)]
    side = lax.broadcasted_iota(I32, (n_rows // 2, LANES), 1) < LANES // 2
    tiles = d // LANES
    turn = lambda v: pltpu.roll(v, LANES // 2, 1)
    lanes = lambda v, j: v[:, LANES * j:LANES * (j + 1)]

    def pack(wire, k, value):
        top, low = value[:n_rows // 2], value[n_rows // 2:]
        turned = [turn(lanes(low, j)) for j in range(tiles + 1)]
        parts = [lanes(top, j) for j in range(tiles)] + [jnp.where(side, lanes(top, tiles), turned[0])]
        parts += [jnp.where(side, turned[j], turned[j + 1]) for j in range(tiles)]
        for j, part in enumerate(parts):
            wire[thin[k], LANES * j:LANES * (j + 1)] = part.astype(BF16)

    def unpack(wire, k):
        value = wire[thin[k], :].astype(F32)
        turned = [turn(lanes(value, tiles + j)) for j in range(tiles + 1)]
        top = [lanes(value, j) for j in range(tiles)] + [jnp.where(side, lanes(value, tiles), 0.0)]
        low = [jnp.where(side, turned[j], turned[j + 1]) for j in range(tiles)] + [jnp.where(side, turned[tiles], 0.0)]
        return jnp.concatenate([jnp.concatenate(top, axis=1), jnp.concatenate(low, axis=1)], axis=0)

    chunks = range(n_chunk)
    loads = {}
    for i, part in enumerate(parts[:2] if reduce else parts):
        buf = in_f.at[i] if reduce or i == 0 else in_b.at[i - 1]
        for k in chunks:
            loads[i, k] = pltpu.make_async_copy(part.at[cut[k]], buf.at[cut[k]], load.at[i, k])
    order = (1, 0) if reduce else range(N_SRC)
    for i in order:
        for k in chunks:
            loads[i, k].start()
    u_buf[...] = jnp.zeros(u_buf.shape, BF16)
    meet((Y, CORE))
    links = []
    copy_in = pltpu.make_async_copy

    def link(src, dst, rel, cut=cut):
        n = len(links)
        links.append([remote(src.at[cut[k]], dst.at[cut[k]], send.at[n, k], recv.at[n, k], rel) for k in chunks])
        return links[-1]

    if reduce:
        first = link(parts[3], got_f.at[1], CORE)
        second = link(parts[2], got_f.at[0], CORE)
        over = link(s_wire, r_wire, Y, thin)
        for copies in (first, second):
            for copy in copies:
                copy.start()
        for k in chunks:
            loads[1, k].wait()
            first[k].wait_recv()
            pack(s_wire, k, in_f[1, cut[k], :] + got_f[1, cut[k], :])
            over[k].start()
    to_y = link(u_wire, y_wire, Y, thin)
    to_core = link(u_buf, o_b.at[0], CORE)
    puts = []
    for k in chunks:
        if reduce:
            loads[0, k].wait()
            second[k].wait_recv()
            over[k].wait_recv()
            total = in_f[0, cut[k], :] + got_f[0, cut[k], :] + unpack(r_wire, k)
        else:
            for i in range(N_SRC):
                loads[i, k].wait()
            total = in_f[0, cut[k], :]
            for i in range(N_SRC - 1):
                total = total + in_b[i, cut[k], :].astype(F32)
        total = total.astype(BF16)
        t_buf[cut[k], :] = total
        dims = (((1,), (1 if back else 0,)), ((), ()))
        mixed = lax.dot_general(total[:, :d], m_ref[...], dims, preferred_element_type=F32)
        u_buf[cut[k], 0:d] = (total[:, :d].astype(F32) + mixed).astype(BF16)
        pack(u_wire, k, u_buf[cut[k], :].astype(F32))
        to_y[k].start()
        to_core[k].start()
        puts.append(pltpu.make_async_copy(u_buf.at[cut[k]], o_a.at[0, cut[k]], put.at[0, k]))
        puts.append(pltpu.make_async_copy(t_buf.at[cut[k]], o_total.at[cut[k]], put.at[1, k]))
        for copy in puts[-2:]:
            copy.start()
    if sizes:
        plan_kernel(*sizes, *list_refs, *plan_refs)
    if back:
        grad_ref[...] = lax.dot_general(left_ref[:, :d], t_buf[:, :d], (((0,), (0,)), ((), ())), preferred_element_type=F32)
    on = link(y_buf, o_b.at[1], CORE)
    for k in chunks:
        to_y[k].wait_recv()
        y_buf[cut[k], :] = unpack(y_wire, k).astype(BF16)
        on[k].start()
        puts.append(copy_in(y_buf.at[cut[k]], o_a.at[1, cut[k]], put.at[2, k]))
        puts[-1].start()
    waited = [to_y] + ([first, second, over] if reduce else [])
    for copies in links:
        for copy in copies:
            if any(copies is w for w in waited):
                copy.wait_send()
            else:
                copy.wait()
    for copy in puts:
        copy.wait()


def complete_blocks(parts, m, reduce, back, ident, sizes=None, lists=(), left=(), n_chunk=4):
    n_blk, wide = parts[0].shape
    d = m.shape[0]
    sem = lambda *s: pltpu.SemaphoreType.DMA(s)
    pair = jax.ShapeDtypeStruct((2, n_blk, wide), BF16)
    extra = plan_shapes(sizes) if sizes else []
    extra += [jax.ShapeDtypeStruct((d, d), F32)] * len(left)
    buf = lambda n, dt: pltpu.VMEM((n, n_blk, wide) if n else (n_blk, wide), dt)
    return pl.pallas_call(
        functools.partial(blocks_kernel, (n_chunk, reduce, back, d, sizes)),
        out_shape=[jax.ShapeDtypeStruct((n_blk, wide), BF16)] + [pair] * 2 + extra,
        in_specs=[any_space] * N_SRC + [in_vmem] * (1 + len(lists) + len(left)),
        out_specs=[any_space] * 3 + [in_vmem] * len(extra),
        scratch_shapes=[buf(2, F32), buf(3, BF16), buf(2, F32)] + [pltpu.VMEM((n_blk // 2, 2 * d), BF16)] * 4 + [
            buf(0, BF16), buf(0, BF16), buf(0, BF16), sem(4, n_chunk), sem(6, n_chunk), sem(6, n_chunk), sem(3, n_chunk)],
        compiler_params=pltpu.CompilerParams(collective_id=ident, has_side_effects=True, vmem_limit_bytes=VMEM_LIMIT),
        cost_estimate=pl.CostEstimate(flops=10 ** 8, bytes_accessed=n_blk * wide * 40, transcendentals=0),
        name=f"complete_blocks_{ident}",
    )(*parts, m, *lists, *left)


def solution(mesh):
    ep_size, dp_size = mesh.shape['ep'], mesh.shape['dp']
    sub = Mesh(mesh.devices.reshape(ep_size, dp_size // 2, 2), ('ep', 'x', 'core'))
    tok_axes = ('x', 'core', 'ep')
    tok_spec = P(tok_axes, None)
    route_spec = P(None, tok_axes, None)
    whole_spec = P(None, None, None)
    expert_spec = P(None, 'ep', None, None)
    flip = [(0, 1), (1, 0)]
    move = lambda v, axis: lax.ppermute(v, axis, flip)
    move_diag = lambda v: lax.ppermute(v, ('ep', 'core'), [(0, 3), (1, 2), (2, 1), (3, 0)])
    fence = lax.optimization_barrier

    def device_step(tokens, d_out, expert_ids, gate_vals, w_mix, w_gate, w_up, w_down):
        n_layers, d = w_mix.shape[0], w_mix.shape[1]
        n_tok = tokens.shape[0]
        top = expert_ids.shape[2]
        n_local = w_gate.shape[1]
        n_exp = n_local * ep_size
        n = n_tok * top
        n_rel = 2 * N_SRC
        wide = cdiv(d, LANES) * LANES
        weights = (jnp.swapaxes(w_gate, 2, 3), jnp.swapaxes(w_up, 2, 3), w_down)
        pad = lambda v: jnp.pad(v, ((0, 0), (0, wide - d)))
        send_three = lambda p: [move(p[1], 'ep'), move(p[2], 'core'), move_diag(p[3])]

        def own_sum(p, got):
            return sum([g.astype(F32) for g in got], p)[:, :d].astype(BF16)

        one = lambda v: v.reshape(1, n_tok, wide)
        pairs = lambda a, b: [(a, 0), (a, 1), (b, 0), (b, 1)]

        one = lambda v: v.reshape(1, n_tok, wide)
        pairs = lambda a, b: [(a, 0), (a, 1), (b, 0), (b, 1)]
        singles = lambda *v: [(one(a), 0) for a in v]

        u0 = pad((tokens.astype(F32) + jnp.dot(tokens, w_mix[0], preferred_element_type=F32)).astype(BF16))
        u0_y, u0_c = move(u0, 'ep'), move(u0, 'core')
        lists = [sorted_list(expert_ids[l], gate_vals[l]) for l in range(n_layers)]
        counts = jnp.sum((expert_ids.transpose(0, 2, 1).reshape(n_layers, n, 1) == jnp.arange(n_exp, dtype=I32)).astype(F32), axis=1)
        packed = jnp.concatenate([jnp.concatenate([v[0] for v in lists] + [v[1] for v in lists]).reshape(-1, LANES),
                                  jnp.pad(counts, ((0, 8 - n_layers), (0, LANES - n_exp)))], axis=0)
        dy = pad(d_out)
        packed, dy = fence((packed, dy))
        shared = share(packed, N_SRC)
        u0_y, u0_c, dy, shared = fence((u0_y, u0_c, dy, shared))
        u0_d = move(u0_y, 'core')
        shared_x = move(shared, 'x')
        dy_y, dy_x = move(dy, 'ep'), move(dy, 'x')
        sizes = (n_layers, n_local, n_tok, n // LANES)
        routes = plan(shared, shared, sizes)
        u0_half = singles(u0, u0_y, u0_c, u0_d)
        piece = first_piece(n_local // 2)
        row = lambda a, b: lax.slice_in_dim(routes[0], ROW_PARTNER * LANES + a, ROW_PARTNER * LANES + b)
        rows = [row(0, piece), row(piece, n_local // 2)]
        *part, ab0, xu0 = run_experts(routes, 0, u0_half, None, weights, None, None, True, True, p_f32=True)
        dy_y, dy_x, shared_x, part = fence((dy_y, dy_x, shared_x, part))
        dy_c, dy_d, dy_xy, dy_xc = move(dy, 'core'), move(dy_y, 'core'), move(dy_y, 'x'), move(dy_x, 'core')
        y0, u1_a, u1_b, *routes_x = complete_blocks(part, w_mix[1], True, False, 1, sizes, (shared, shared_x))
        routes_x = flat(*routes_x)
        dy_c, dy_d, dy_xy, dy_xc, u0_p, u0_q, y0, u1_a, u1_b = fence(
            (dy_c, dy_d, dy_xy, dy_xc, u0, u0_y, y0, u1_a, u1_b))
        dy_xd = move(dy_xy, 'core')
        u1_xa = move(u1_a, 'x')
        out = run_experts(routes, 1, pairs(u1_a, u1_b), singles(dy, dy_y, dy_c, dy_d), weights, None, None, True, True)
        u1_xa, dy_xd, u0_p, u0_q, out = fence((u1_xa, dy_xd, u0_p, u0_q, out))
        y_part, du_part, g1 = out[:4], out[4:8], out[8]
        u1_xb = move(u1_xa, 'core')
        got = send_three(du_part)
        u0_x, u0_xy = move(u0_p, 'x'), move(u0_q, 'x')
        out = run_experts(routes_x, 1, pairs(u1_xa, u1_xb), singles(dy_x, dy_xy, dy_xc, dy_xd), weights, g1, None,
                          False, False)
        got, u0_x, u0_xy, out = fence((got, u0_x, u0_xy, out))
        *finals, sent_a, sent_b = out
        got1 = [move(sent_a, 'core'), move(sent_b, 'core')]
        du1, dx_a, dx_b, g_mix1 = complete_blocks([du_part[0], *got], w_mix[1], False, True, 2, left=(y0,))
        tx = lambda x, du: jnp.einsum('td,te->de', x, du, preferred_element_type=F32)
        dx_a, y_part, got1, u0_x, u0_xy, g_mix1 = fence((dx_a, y_part, got1, u0_x, u0_xy, g_mix1))
        dx_xa = move(dx_a, 'x')
        theirs1 = move(g_mix1, 'core')
        got_y = send_three(y_part)
        u0_xc, u0_xd = move(u0_x, 'core'), move(u0_xy, 'core')
        out = run_experts(routes, 0, None, pairs(dx_a, dx_b), weights, None, finals, False, True, got=got1, kept=(ab0, xu0))
        dx_xa, got_y, u0_xc, u0_xd, theirs1, out = fence((dx_xa, got_y, u0_xc, u0_xd, theirs1, out))
        du_part, g0, finals = out[:4], out[4], out[5:]
        dx_xb = move(dx_xa, 'core')
        got = send_three(du_part)
        part1 = (g_mix1 + theirs1).astype(BF16)
        theirs1 = move(part1, 'ep')
        du_part, dx_xb, part1 = fence((du_part, dx_xb, part1))
        out = run_experts(routes_x, 0, singles(u0_x, u0_xy, u0_xc, u0_xd), pairs(dx_xa, dx_xb), weights, g0, finals,
                          False, False)
        got, theirs1, got_y, y_own, rows, out = fence((got, theirs1, got_y, y_part[0], rows, out))
        *finals, sent_a, sent_b = out
        got_a, got_b = move(sent_a, 'core'), move(sent_b, 'core')
        add = lambda a, b: a.astype(F32) + b.astype(F32)
        part1 = add(part1, theirs1).astype(BF16)
        theirs1 = move(part1, 'x')
        du0 = own_sum(du_part[0], got)
        part0 = tx(tokens, du0).astype(BF16)
        swap = [(0, 3), (1, 2), (2, 1), (3, 0)]
        theirs0 = [move(part0, 'ep'), move(part0, 'x'), lax.ppermute(part0, ('ep', 'x'), swap)]
        dx0 = (du0.astype(F32) + jnp.einsum('te,de->td', du0, w_mix[0], preferred_element_type=F32)).astype(BF16)
        y1 = own_sum(y_own, got_y).T
        dx0, y1, got_a, finals = fence((dx0, y1, got_a, finals))
        finals = place(rows[0], 0, got_a, finals)
        dx0, got_b, finals = fence((dx0.T, got_b, finals))
        finals = place(rows[1], 0, got_b, finals)
        theirs0, theirs1, finals = fence((theirs0, theirs1, finals))
        total0 = (add(part0, theirs0[0]) + add(theirs0[1], theirs0[2])).astype(BF16)
        g_mix = jnp.stack([add(total0, move(total0, 'core')), add(part1, theirs1)]).astype(BF16)
        return (y1.T, dx0.T, g_mix, jnp.swapaxes(finals[0], 2, 3), jnp.swapaxes(finals[1], 2, 3), finals[2])

    return jax.shard_map(device_step, mesh=sub,
                         in_specs=(tok_spec, tok_spec, route_spec, route_spec, whole_spec,
                                   expert_spec, expert_spec, expert_spec),
                         out_specs=(tok_spec, tok_spec, whole_spec, expert_spec, expert_spec, expert_spec),
                         check_vma=False)
```

```python
import functools

import jax
import jax.numpy as jnp
from jax import lax
from jax.experimental import pallas as pl
from jax.experimental.pallas import tpu as pltpu
from jax.sharding import Mesh, PartitionSpec as P

F32, BF16, I32 = jnp.float32, jnp.bfloat16, jnp.int32
MESH = pl.DeviceIdType.MESH
ROWS = 384
GRP = 8
PITCH = 9
DEPTH = 3
FULL = 8
HALF = 4
CAP_FACTOR = 3
LANES = 128
N_SRC = 4
Y, CORE, X = 1, 2, 4
VMEM_LIMIT = 62 * 1024 * 1024
PER_TILE = ROWS // GRP
ROW_BOUND, ROW_GOFF, ROW_EXPERT, ROW_PARTNER, TAB_ROWS = 32, 33, 34, 35, 40
SLOT_GROUPS = 256


def cdiv(a, b):
    return (a + b - 1) // b


def first_piece(n_exp):
    return n_exp * 5 // 8


def spans(d):
    return [(LANES * j, min(LANES, d - LANES * j)) for j in range(cdiv(d, LANES))]


any_space = pl.BlockSpec(memory_space=pl.ANY)
in_vmem = pl.BlockSpec(memory_space=pltpu.VMEM)


def sorted_list(expert_ids, gate_vals):
    n_tok, top = expert_ids.shape
    n = n_tok * top
    keys = expert_ids.T.reshape(n) * n + jnp.arange(n, dtype=I32)
    keys, gates = lax.sort((keys, gate_vals.T.reshape(n)), num_keys=1, is_stable=False)
    return (keys % n_tok).astype(F32), gates


def plan_kernel(n_layers, n_local, n_tok, list_rows, deal_ref, all_ref, tab_ref, idx_ref, gate_ref):
    n_mine = n_local // 2
    core, ep = lax.axis_index('core'), lax.axis_index('ep')
    list_len = list_rows * LANES
    lane = lambda n: lax.broadcasted_iota(I32, (n, LANES), 1).astype(F32)
    sub = lambda n: lax.broadcasted_iota(I32, (n, LANES), 0).astype(F32)
    over_lanes = lambda v: jnp.sum(v, axis=1, keepdims=True)
    over_subs = lambda v: jnp.sum(v, axis=0, keepdims=True)
    l16, s16 = lane(n_mine), sub(n_mine)
    groups = lambda c: jnp.floor((c + (GRP - 0.5)) * (1.0 / GRP))
    for l in range(n_layers):
        cnt = all_ref[:, 2 * n_layers * list_rows + l, :]
        ends = cnt
        step = 1
        while step < 2 * n_local:
            ends = ends + jnp.where(lane(N_SRC) >= step, pltpu.roll(ends, step, 1), 0.0)
            step *= 2
        starts = ends - cnt
        second = (ep > 0)
        local = lambda v: jnp.where(lane(N_SRC) < n_local, jnp.where(second, pltpu.roll(v, LANES - n_local, 1), v), 0.0)
        cnt, starts = local(cnt), local(starts)
        tiles = jnp.floor((over_subs(groups(local(deal_ref[:, 2 * n_layers * list_rows + l, :]))) + (PER_TILE - 0.5))
                          * (1.0 / PER_TILE))
        load = jnp.where(lane(1) < n_local, jnp.maximum(1.0, tiles), -1.0)
        wide = jnp.broadcast_to(load, (n_local, LANES))
        col = over_lanes(jnp.where(lane(n_local) == sub(n_local), wide, 0.0))
        ahead = (col > wide) | ((col == wide) & (sub(n_local) < lane(n_local)))
        rank = over_subs(jnp.where(ahead, 1.0, 0.0))
        odd = s16 - 2.0 * jnp.floor(s16 * 0.5 + 0.25)
        flip = jnp.where(core > 0, 1.0 - odd, odd)
        dealt = lambda f: (jnp.broadcast_to(rank, (n_mine, LANES)) == 2.0 * s16 + f) & (l16 < n_local)
        pick = dealt(flip)
        choose = lambda p, row: over_lanes(jnp.where(p, jnp.broadcast_to(row, (n_mine, LANES)), 0.0))
        mine = lambda row: choose(pick, row)
        as_row = lambda c: over_subs(jnp.where(l16 == s16, c, 0.0))
        experts = as_row(mine(lane(1)))
        partner = as_row(choose(dealt(1.0 - flip), lane(1)))
        at = l * TAB_ROWS
        off = jnp.zeros((n_mine, 1), F32)
        pos = [jnp.zeros((n_mine, LANES), F32) for _ in range(SLOT_GROUPS // LANES)]
        for s in range(N_SRC):
            c, st = mine(cnt[s:s + 1]), mine(starts[s:s + 1]) + float(s * list_len)
            ng = groups(c)
            for i in range(len(pos)):
                rel = l16 + float(LANES * i) - off
                code = (st + GRP * rel) * 16.0 + jnp.minimum(float(GRP), c - GRP * rel)
                pos[i] = jnp.where((rel >= 0) & (rel < ng), code, pos[i])
            off = off + ng
        for i in range(len(pos)):
            tab_ref[pl.ds(at + i, n_mine, stride=len(pos)), :] = pos[i].astype(I32)
        n_tiles = jnp.maximum(1.0, jnp.floor((off + (PER_TILE - 0.5)) * (1.0 / PER_TILE)))
        bounds = over_subs(jnp.where(s16 < l16, n_tiles, 0.0))
        before = over_lanes(jnp.where(l16 == s16, jnp.broadcast_to(bounds, (n_mine, LANES)), 0.0))
        t = jnp.minimum(l16, over_subs(jnp.broadcast_to(n_tiles, (n_mine, LANES))) - 1.0)
        inside = (t >= before) & (t < before + n_tiles)
        goff = over_subs(jnp.where(inside, s16 * float(SLOT_GROUPS) + (t - before) * float(PER_TILE), 0.0))
        rows = [(ROW_BOUND, bounds), (ROW_GOFF, goff), (ROW_EXPERT, experts), (ROW_PARTNER, partner)]
        for row, value in rows:
            tab_ref[at + row:at + row + 1, :] = value.astype(I32)
    for l in range(n_layers):
        pad = l * (N_SRC * list_rows + 8) + N_SRC * list_rows
        gate_ref[pad:pad + 8, :] = jnp.zeros((8, LANES), F32)
        for s in range(N_SRC):
            to = (l * N_SRC + s) * list_rows
            toks = all_ref[s, l * list_rows:(l + 1) * list_rows, :]
            idx_ref[to:to + list_rows, :] = ((toks + float(s * n_tok)) * float(PITCH)).astype(I32)
            to = l * (N_SRC * list_rows + 8) + s * list_rows
            gate_ref[to:to + list_rows, :] = all_ref[s, (n_layers + l) * list_rows:(n_layers + l + 1) * list_rows, :]


def plan_shapes(sizes):
    n_layers, _, _, list_rows = sizes
    rows = (n_layers * TAB_ROWS, n_layers * N_SRC * list_rows, n_layers * (N_SRC * list_rows + 8))
    return [jax.ShapeDtypeStruct((n, LANES), dt) for n, dt in zip(rows, (I32, I32, F32))]


def flat(tab, idx, gates):
    return tab.reshape(-1), idx.reshape(-1), gates


def plan(deal, shared, sizes):
    return flat(*pl.pallas_call(
        functools.partial(plan_kernel, *sizes),
        out_shape=plan_shapes(sizes),
        in_specs=[in_vmem] * 2, out_specs=[in_vmem] * 3,
        cost_estimate=pl.CostEstimate(flops=10 ** 7, bytes_accessed=10 ** 6, transcendentals=0),
        name="plan",
    )(deal, shared))


def expert_kernel(cfg, *refs):
    fwd, bwd, own, layer, n_blk, d, ff, n_exp, picks, row_id, list_len, p_f32, n_alias, got_layer = cfg
    save, load = fwd and not bwd, own and bwd and not fwd
    refs = list(refs)
    take = lambda n: [refs.pop(0) for _ in range(n)]
    tab_hbm, idx_hbm, gate_hbm = take(3)
    u_pieces = take(N_SRC) if not load else []
    dy_pieces = take(N_SRC) if bwd else []
    wg_hbm, wu_hbm, wd_hbm = take(3)
    ab_hbm, xu_hbm = take(2) if load else (None, None)
    prev = take(1)[0] if bwd and not own else None
    got = take(2) if got_layer is not None else None
    take(n_alias)
    y_outs = take(N_SRC) if fwd else []
    du_outs = take(N_SRC) if bwd and own else []
    grad = take(1)[0] if bwd and own else None
    finals = take(3) if bwd and not own or got_layer is not None else None
    sent = take(2) if bwd and not own else None
    ab_hbm, xu_hbm = take(2) if save else (ab_hbm, xu_hbm)
    tab_ref, idx, gate_ref, land, table, gat = take(6)
    acc, row_ref = take(2) if own else (None, None)
    gu_ref, wd_ref, g_ref, x_u = take(4)
    x_c = take(1)[0] if bwd else None
    ab_ref = take(1)[0]
    dh_ref = take(1)[0] if bwd else None
    h_ref = take(1)[0]
    dab_ref, sums = take(2) if bwd else (None, None)
    keep_buf = take(1)[0] if bwd and not own else None
    got_buf = take(1)[0] if got is not None else None
    list_sem, land_sem, w_sem = take(3)
    sum_sem = take(1)[0] if bwd else None
    keep_sem = take(1)[0] if bwd and not own else None
    read_sem, write_sem = take(2) if got is not None else (None, None)
    stage_f, out_sem = take(2) if own else (None, None)
    ab_sem, xu_sem = take(2) if save or load else (None, None)

    split = first_piece(n_exp)
    copy = pltpu.make_async_copy
    cols = spans(d)
    lo = ff // 256 * 256
    hi = ff - lo
    dot = functools.partial(lax.dot_general, preferred_element_type=F32)
    nn = (((1,), (0,)), ((), ()))
    nt = (((1,), (1,)), ((), ()))
    tn = (((0,), (0,)), ((), ()))
    al = pl.multiple_of
    n_row = N_SRC * n_blk
    glane = lax.broadcasted_iota(I32, (GRP, LANES), 1)
    gsub = lax.broadcasted_iota(I32, (GRP, LANES), 0)

    def row_at(r):
        return pl.ds(r * PITCH, FULL)

    def codes_of(tile):
        at = ROW_GOFF * LANES + tile
        if own and bwd:
            return lambda q: tab_ref[tab_ref[at] + q]
        view = tab_ref.at[pl.ds(tab_ref[at], PER_TILE)]
        return lambda q: view[q]

    def gather(codes, q):
        ids = idx.at[pl.ds(codes(q) >> 4, GRP)]
        for k in range(GRP):
            gat[row_at(q * GRP + k), :] = table[pl.ds(ids[k], FULL), :]

    def gate_column(code):
        pos = code >> 4
        row, shift = pos >> 7, pos & (LANES - 1)
        want = glane == gsub + shift
        over = glane == gsub + (shift - LANES)
        here = gate_ref[pl.ds(row, GRP, stride=0), :]
        there = gate_ref[pl.ds(row + 1, GRP, stride=0), :]
        v = jnp.where(want, here, jnp.where(over, there, 0.0))
        return jnp.where(gsub < (code & 15), jnp.sum(v, axis=1, keepdims=True), 0.0)

    def scatter(codes, q):
        ids = idx.at[pl.ds(codes(q) >> 4, GRP)]
        new = []
        for k in range(GRP):
            at = pl.ds(ids[k], FULL)
            new.append((at, acc[at, :] + row_ref[row_at(q * GRP + k), :]))
        for at, value in reversed(new):
            acc[at, :] = value

    def keep_ab(t):
        ends = (ab_ref.at[t & 1], ab_hbm.at[t])
        return copy(*(ends if save else ends[::-1]), ab_sem.at[t & 1])

    def keep_xu(t):
        ends = (x_u.at[t & 1], xu_hbm.at[t])
        return copy(*(ends if save else ends[::-1]), xu_sem.at[t & 1])

    def of(ref, t):
        return ref.at[t & 1] if save or load else ref

    def convert(codes, t):
        for q in range(0, PER_TILE, 2):
            part = []
            for p in (q, q + 1):
                code = codes(p)
                rows = [gat[pl.ds(GRP * PITCH * p + j, GRP, stride=PITCH), :]
                        for j in range(HALF if load else 0, FULL if bwd else HALF)]
                real = gsub < (code & 15)
                gate = gate_column(code)
                g_ref[GRP * p:GRP * (p + 1), :] = gate
                us, dys = ([], rows) if load else (rows[:HALF], rows[HALF:])
                part.append([jnp.where(real, v, 0.0) for v in us] + [v * gate for v in dys])
            at = slice(GRP * q, GRP * (q + 2))
            for x, o in ((None if load else of(x_u, t), 0), (x_c, 0 if load else HALF)):
                if x is None:
                    continue
                for j, (c, w) in enumerate(cols):
                    both = jnp.concatenate([part[0][o + j], part[1][o + j]], axis=0)
                    x[at, c:c + w] = both[:, :w].astype(BF16)

    def put_rows(o, value, s0):
        value = value.astype(BF16).astype(F32)
        n = value.shape[0]
        for j, (c, w) in enumerate(cols):
            row_ref[pl.ds(PITCH * s0 + o + j, n, stride=PITCH), 0:w] = value[:, c:c + w] * g_ref[s0:s0 + n, 0:w]

    low = lax.broadcasted_iota(I32, (16, 2 * hi), 1) < hi

    def middle(a, b, dh):
        sig = 0.5 * jnp.tanh(0.5 * a) + 0.5
        act = a * sig
        h = act * b
        if dh is None:
            return h, None, None
        slope = sig * (1.0 + a * (1.0 - sig))
        return h, dh * b * slope, dh * act

    def weights(e, slot):
        at = (layer, tab_ref[ROW_EXPERT * LANES + e])
        moves = []
        for i, w in enumerate((wg_hbm, wu_hbm)):
            moves.append((w.at[at + (pl.ds(0, lo),)], gu_ref.at[slot, pl.ds(i * lo, lo)]))
            moves.append((w.at[at + (pl.ds(lo, hi),)], gu_ref.at[slot, pl.ds(2 * lo + i * hi, hi)]))
        moves.append((wd_hbm.at[at], wd_ref.at[slot]))
        return [copy(a, b, w_sem.at[slot, i]) for i, (a, b) in enumerate(moves)]

    def sums_in(e, slot):
        return copy(prev.at[e], sums.at[slot], sum_sem.at[slot])

    def sums_out(e, slot):
        return copy(sums.at[slot], grad.at[e], sum_sem.at[slot])

    def keeps(e, slot):
        at = (layer, tab_ref[ROW_EXPERT * LANES + e])
        return [copy(keep_buf.at[slot, i], finals[i].at[at], keep_sem.at[slot, i]) for i in range(3)]

    def send(e, slot, part):
        return copy(keep_buf.at[slot], sent[part].at[e - part * split], keep_sem.at[slot, 3])

    def read(e, slot, part=0):
        return copy(got[part].at[e - part * split], got_buf.at[slot], read_sem.at[slot])

    def writes(e, slot):
        to = tab_ref[TAB_ROWS * LANES + e]
        return [copy(got_buf.at[slot, i], finals[i].at[got_layer, to], write_sem.at[slot, i]) for i in range(3)]

    def start(moves):
        for m in moves:
            m.start()

    def wait(moves):
        for m in moves:
            m.wait()

    n_tab = TAB_ROWS * LANES
    lists = [copy(tab_hbm.at[pl.ds(row_id * n_tab, n_tab)], tab_ref.at[pl.ds(0, n_tab)], list_sem.at[0]),
             copy(idx_hbm.at[pl.ds(row_id * N_SRC * list_len, N_SRC * list_len)], idx.at[pl.ds(0, N_SRC * list_len)],
                  list_sem.at[1]),
             copy(gate_hbm.at[pl.ds(row_id * gate_ref.shape[0], gate_ref.shape[0])], gate_ref, list_sem.at[2])]
    if got is not None:
        at = (got_layer * TAB_ROWS + ROW_PARTNER) * LANES
        lists.append(copy(tab_hbm.at[pl.ds(at, LANES)], tab_ref.at[pl.ds(n_tab, LANES)], list_sem.at[3]))
    start(lists)
    pieces = []
    for s in range(N_SRC):
        if not load:
            pieces.append((u_pieces[s], picks[0][s], s, 0, fwd))
        if bwd:
            pieces.append((dy_pieces[s], picks[1][s], s, HALF, own))
    lands = [copy(ref.at[pick], land.at[i % N_SRC], land_sem.at[i % N_SRC]) for i, (ref, pick, *_) in enumerate(pieces)]
    start(lands[:N_SRC])
    lists[0].wait()
    for e in range(DEPTH - 1):
        start(weights(e, e))
        if bwd and not own:
            sums_in(e, e).start()
    if got is not None:
        lists[3].wait()
        read(0, 0).start()
    if own:
        def clear(c, _):
            for k in range(4):
                acc[pl.ds(al(c * 1152 + 288 * k, 8), 288), :] = jnp.zeros((288, LANES), F32)
            return 0

        lax.fori_loop(0, acc.shape[0] // 1152, clear, 0)
        row_ref[...] = jnp.zeros(row_ref.shape, F32)
    rows = 256
    for i, (_, _, s, o, seed) in enumerate(pieces):
        lands[i].wait()

        def fill(c, _, i=i, o=o, seed=seed, s=s):
            r = al(c * rows, rows)
            for j in range(HALF):
                vals = land[i % N_SRC, pl.ds(r, rows), LANES * j:LANES * (j + 1)].astype(F32)
                to = pl.ds(PITCH * (s * n_blk + r) + o + j, rows, stride=PITCH)
                table[to, :] = vals
                if seed and s == 0:
                    acc[to, :] = vals
            return 0

        lax.fori_loop(0, n_blk // rows, fill, 0)
        if i + N_SRC < len(pieces):
            lands[i + N_SRC].start()
    wait(lists[1:3])
    for k in range(GRP):
        idx[N_SRC * list_len + k] = 0

    def first(q, _):
        gather(begin, 2 * q)
        gather(begin, 2 * q + 1)
        return 0

    begin = codes_of(0)
    lax.fori_loop(0, PER_TILE // 2, first, 0)
    convert(begin, 0)
    if save:
        keep_xu(0).start()
    if load:
        keep_ab(0).start()
        keep_xu(0).start()

    def expert(e, _):
        slot = e & 1
        deep = lax.rem(e, DEPTH)
        sum_slot = slot if own else deep
        wait(weights(e, deep))
        if bwd and not own:
            sums_in(e, deep).wait()
        if got is not None:
            read(0, slot).wait()
            start(writes(e, slot))

            @pl.when((e > 0) & (e < n_exp - 1))
            def _():
                wait(writes(e - 1, 1 - slot))

        @pl.when(e < n_exp - (DEPTH - 1))
        def _():
            ahead = lax.rem(e + DEPTH - 1, DEPTH)
            start(weights(e + DEPTH - 1, ahead))
            if bwd and not own:
                sums_in(e + DEPTH - 1, ahead).start()

        @pl.when(e < n_exp - 1)
        def _():
            if got is not None:
                for part in range(2):
                    @pl.when((e + 1 >= split) if part else (e + 1 < split))
                    def _(part=part):
                        read(e + 1, 1 - slot, part).start()

        if bwd and own:
            @pl.when(e > 1)
            def _():
                sums_out(e - 2, slot).wait()

            sums[slot] = jnp.zeros(sums.shape[1:], F32)

        def tile(t, _):
            if save:
                @pl.when(t > 1)
                def _():
                    keep_ab(t - 2).wait()

                @pl.when(t > 0)
                def _():
                    keep_xu(t - 1).wait()
            if load:
                keep_ab(t).wait()
                keep_xu(t).wait()
                keep_ab(t + 1).start()
                keep_xu(t + 1).start()
            ab, xu = of(ab_ref, t), of(x_u, t)
            before, after = codes_of(jnp.maximum(t - 1, 0)), codes_of(t + 1)
            for q in range(PER_TILE):
                if own:
                    scatter(before, q)
                gather(after, q)
            front = ROWS if own and bwd else ROWS // 2
            for s0 in range(0, ROWS, front):
                sl = slice(s0, s0 + front)
                if not load:
                    ab[sl, :] = dot(xu[sl, :], gu_ref[deep], nt)
                if bwd:
                    dh_ref[sl, :] = dot(x_c[sl, :], wd_ref[deep], nt)
            for r in range(0, ROWS, 16):
                rows = slice(r, r + 16)
                for c in range(0, lo, LANES):
                    h, da, db = middle(ab[rows, c:c + LANES], ab[rows, lo + c:lo + c + LANES],
                                       dh_ref[rows, c:c + LANES] if bwd else None)
                    h_ref[rows, c:c + LANES] = h.astype(BF16)
                    if bwd:
                        dab_ref[rows, c:c + LANES] = da.astype(BF16)
                        dab_ref[rows, lo + c:lo + c + LANES] = db.astype(BF16)
                a = ab[rows, 2 * lo:]
                b = pltpu.roll(a, hi, 1)
                dh = dh_ref[rows, lo:] if bwd else None
                if bwd:
                    dh = jnp.concatenate([dh, dh], axis=1)
                h, da, db = middle(a, b, dh)
                h_ref[rows, lo:] = h[:, :hi].astype(BF16)
                if bwd:
                    dab_ref[rows, 2 * lo:] = jnp.where(low, da, pltpu.roll(db, hi, 1)).astype(BF16)
            half = ROWS // 2
            for s0 in range(0, ROWS, half):
                sl = slice(s0, s0 + half)
                if fwd:
                    put_rows(0, dot(h_ref[sl, :], wd_ref[deep], nn), s0)
                if bwd and own:
                    put_rows(HALF, dot(dab_ref[sl, :], gu_ref[deep], nn), s0)
            if bwd:
                view = sums.at[sum_slot]
                view[0:2 * ff, :] += dot(dab_ref[...], xu[...], tn)
                view[2 * ff:, :] += dot(h_ref[...], x_c[...], tn)
            convert(after, t + 1)
            if save:
                keep_ab(t).start()
                keep_xu(t + 1).start()
            return 0

        lax.fori_loop(tab_ref[ROW_BOUND * LANES + e], tab_ref[ROW_BOUND * LANES + e + 1], tile, 0)
        if bwd and own:
            sums_out(e, slot).start()
        if bwd and not own:
            @pl.when(e > 1)
            def _():
                wait(keeps(e - 2, slot) + [send(0, slot, 0)])

            for i in range(2):
                keep_buf[slot, i, 0:lo, :] = sums[deep, i * lo:(i + 1) * lo, :].astype(BF16)
                keep_buf[slot, i, lo:, :] = sums[deep, 2 * lo + i * hi:2 * lo + (i + 1) * hi, :].astype(BF16)
            keep_buf[slot, 2] = sums[deep, 2 * ff:, :].astype(BF16)
            start(keeps(e, slot))
            for part in range(2):
                @pl.when((e >= split) if part else (e < split))
                def _(part=part):
                    send(e, slot, part).start()
        return 0

    lax.fori_loop(0, n_exp, expert, 0)
    ends = ((n_exp - 2, (n_exp - 2) % 2), (n_exp - 1, (n_exp - 1) % 2))
    n_tiles = tab_ref[ROW_BOUND * LANES + n_exp]
    if save:
        wait([keep_ab(n_tiles - 2), keep_ab(n_tiles - 1), keep_xu(n_tiles - 1)])
    if save or load:
        keep_xu(n_tiles).wait()
    if load:
        keep_ab(n_tiles).wait()
    if own:
        end = codes_of(tab_ref[ROW_BOUND * LANES + n_exp] - 1)
        lax.fori_loop(0, PER_TILE, lambda q, _: (scatter(end, q), 0)[1], 0)
        flights = {}
        for o, out in ((HALF, du_outs), (0, y_outs)):
            for s in range(N_SRC if out else 0):
                wide = s == 0 or p_f32
                stage = stage_f.at[s] if wide else land.at[s]
                if s in flights:
                    flights[s].wait()

                def fetch(c, _, stage=stage, s=s, o=o):
                    r = al(c * rows, rows)
                    for j in range(HALF):
                        at = pl.ds(PITCH * (s * n_blk + r) + o + j, rows, stride=PITCH)
                        stage[pl.ds(r, rows), LANES * j:LANES * (j + 1)] = acc[at, :].astype(stage.dtype)
                    return 0

                lax.fori_loop(0, n_blk // rows, fetch, 0)
                flights[s] = copy(stage, out[s], out_sem.at[s])
                flights[s].start()
        wait(flights.values())
        if bwd:
            for e, slot in ends:
                sums_out(e, slot).wait()
    else:
        for e, slot in ends:
            wait(keeps(e, slot) + [send(0, slot, 0)])
    if got is not None:
        for e, slot in ends:
            wait(writes(e, slot))


def run_experts(routes, layer, u, dy, weights, prev, finals, fwd, own, p_f32=False, got=None, kept=None):
    tab, idx, gates = routes
    bwd = dy is not None
    wg, wu, wd = weights
    save, load = fwd and not bwd, kept is not None
    n_blk, wide = (dy or u)[0][0].shape[-2:]
    n_layers, n_local, ff, d = wd.shape
    n_exp = n_local // 2
    row_id = layer
    list_len = idx.shape[0] // (n_layers * N_SRC)

    arrays = lambda pieces: [v for v, _ in pieces]
    operands = [tab, idx, gates] + ([] if load else arrays(u)) + (arrays(dy) if bwd else []) + [wg, wu, wd] + list(kept or ())
    out_shape, aliases = [], {}
    for use in (fwd, bwd and own):
        if use:
            out_shape += [jax.ShapeDtypeStruct((n_blk, wide), F32 if s == 0 or p_f32 else BF16) for s in range(N_SRC)]
    if bwd and own:
        out_shape.append(jax.ShapeDtypeStruct((n_exp, 3 * ff, d), F32))
    if bwd and not own:
        operands.append(prev)
    if got is not None:
        operands += got
    for i, f in enumerate(finals or ()):
        aliases[len(operands)] = len(out_shape) + i
        operands.append(f)
    if bwd and not own or finals:
        out_shape += [jax.ShapeDtypeStruct((n_layers, n_local, ff, d), BF16)] * 3
    if bwd and not own:
        out_shape += [jax.ShapeDtypeStruct((n, 3, ff, d), BF16) for n in (first_piece(n_exp), n_exp - first_piece(n_exp))]
    if save:
        most = n_exp * (SLOT_GROUPS // PER_TILE) + 2
        out_shape += [jax.ShapeDtypeStruct((most, ROWS, 2 * ff), F32), jax.ShapeDtypeStruct((most, ROWS, d), BF16)]
    sem = lambda *s: pltpu.SemaphoreType.DMA(s)
    mid = lambda n, dt: pltpu.VMEM((ROWS, n), dt)
    twin = lambda n, dt: pltpu.VMEM((2, ROWS, n), dt) if save or load else mid(n, dt)
    table, rows = pltpu.VMEM((PITCH * N_SRC * n_blk, LANES), F32), pltpu.VMEM((PITCH * ROWS, LANES), F32)
    scratch = [pltpu.SMEM(((TAB_ROWS + 1) * LANES,), I32), pltpu.SMEM((N_SRC * list_len + LANES,), I32),
               pltpu.VMEM((N_SRC * list_len // LANES + 8, LANES), F32), pltpu.VMEM((N_SRC, n_blk, wide), BF16)]
    scratch += [table, rows] * (1 + own)
    scratch += [pltpu.VMEM((DEPTH, 2 * ff, d), BF16), pltpu.VMEM((DEPTH, ff, d), BF16), mid(LANES, F32)]
    scratch += [twin(d, BF16)] + [mid(d, BF16)] * bwd + [twin(2 * ff, F32)] + [mid(ff, F32)] * bwd + [mid(ff, BF16)]
    scratch += [mid(2 * ff, BF16), pltpu.VMEM((2 if own else DEPTH, 3 * ff, d), F32)] * bwd
    if bwd and not own:
        scratch.append(pltpu.VMEM((2, 3, ff, d), BF16))
    if got is not None:
        scratch.append(pltpu.VMEM((2, 3, ff, d), BF16))
    scratch += [sem(4), sem(N_SRC), sem(DEPTH, 5)] + [sem(DEPTH)] * bwd
    if bwd and not own:
        scratch.append(sem(2, 4))
    if got is not None:
        scratch += [sem(2), sem(2, 3)]
    if own:
        scratch += [pltpu.VMEM((N_SRC if p_f32 else 1, n_blk, wide), F32), sem(N_SRC)]
    if save or load:
        scratch += [sem(2), sem(2)]
    passes = 2 + fwd + bwd * (4 + 2 * own)
    flops = 2 * d * ff * passes * n_blk * N_SRC * 2
    hoist = 1300 if not own else 600 if load else 750 if save else 900
    picks = [[i for _, i in u] if u else None, [i for _, i in dy] if bwd else None]
    cfg = (fwd, bwd, own, layer, n_blk, d, ff, n_exp, picks, row_id, list_len, p_f32, len(aliases),
           None if got is None else 1 - layer)
    return pl.pallas_call(
        functools.partial(expert_kernel, cfg),
        out_shape=out_shape,
        in_specs=[any_space] * len(operands),
        out_specs=[any_space] * len(out_shape),
        scratch_shapes=scratch,
        input_output_aliases=aliases,
        compiler_params=pltpu.CompilerParams(
            vmem_limit_bytes=VMEM_LIMIT),
        cost_estimate=pl.CostEstimate(flops=flops, bytes_accessed=3 * 2 * n_exp * d * ff, transcendentals=0),
        name=f"experts_{'f' if fwd else ''}{'b' if bwd else ''}_{'own' if own else 'other'}_{layer}",
    )(*operands)


def place_kernel(layer, n_exp, at, tab_ref, got_ref, *refs):
    outs, (buf, in_sem, out_sem) = refs[3:6], refs[6:]
    reads = [pltpu.make_async_copy(got_ref.at[i], buf.at[i], in_sem.at[i]) for i in range(n_exp)]
    for read in reads:
        read.start()
    writes = []
    for i, read in enumerate(reads):
        read.wait()
        e = tab_ref[at + i]
        for k, out in enumerate(outs):
            writes.append(pltpu.make_async_copy(buf.at[i, k], out.at[layer, e], out_sem.at[i, k]))
            writes[-1].start()
    for write in writes:
        write.wait()


def place(partner, at, layer, got, finals):
    n_exp = got.shape[0]
    return pl.pallas_call(
        functools.partial(place_kernel, layer, n_exp, at),
        out_shape=[jax.ShapeDtypeStruct(f.shape, f.dtype) for f in finals],
        grid_spec=pltpu.PrefetchScalarGridSpec(
            num_scalar_prefetch=1, grid=(1,), in_specs=[any_space] * 4, out_specs=[any_space] * 3,
            scratch_shapes=[pltpu.VMEM(got.shape, got.dtype), pltpu.SemaphoreType.DMA((n_exp,)),
                            pltpu.SemaphoreType.DMA((n_exp, 3))]),
        input_output_aliases={2: 0, 3: 1, 4: 2},
        compiler_params=pltpu.CompilerParams(vmem_limit_bytes=VMEM_LIMIT),
        cost_estimate=pl.CostEstimate(flops=0, bytes_accessed=4 * got.size, transcendentals=0),
        name=f"place_{layer}",
    )(partner, got, *finals)


def peer(rel):
    return {name: (lax.axis_index(name) + ((rel >> bit) & 1)) % 2 for bit, name in enumerate(("ep", "core", "x"))}


def meet(rels):
    barrier = pltpu.get_barrier_semaphore()
    for rel in rels:
        pl.semaphore_signal(barrier, inc=1, device_id=peer(rel), device_id_type=MESH)
    pl.semaphore_wait(barrier, len(rels))


def remote(src, dst, send, recv, rel):
    return pltpu.make_async_remote_copy(src_ref=src, dst_ref=dst, send_sem=send, recv_sem=recv,
                                        device_id=peer(rel), device_id_type=MESH)


def share_kernel(n_rel, mine_ref, all_ref, send_sem, recv_sem):
    meet(range(1, n_rel))
    copies = [remote(mine_ref, all_ref.at[rel], send_sem.at[rel], recv_sem.at[rel], rel) for rel in range(1, n_rel)]
    for copy in copies:
        copy.start()
    all_ref[0] = mine_ref[...]
    for copy in copies:
        copy.wait()


def share(mine, n_rel):
    return pl.pallas_call(
        functools.partial(share_kernel, n_rel),
        out_shape=jax.ShapeDtypeStruct((n_rel,) + mine.shape, mine.dtype),
        in_specs=[in_vmem],
        out_specs=in_vmem,
        scratch_shapes=[pltpu.SemaphoreType.DMA((n_rel,)), pltpu.SemaphoreType.DMA((n_rel,))],
        compiler_params=pltpu.CompilerParams(collective_id=0, has_side_effects=True),
        cost_estimate=pl.CostEstimate(flops=10 ** 7, bytes_accessed=mine.size * 4 * n_rel, transcendentals=0),
        name="share_lists",
    )(mine)


def blocks_kernel(cfg, *refs):
    n_chunk, reduce, back, d, sizes = cfg
    refs = list(refs)
    take = lambda n: [refs.pop(0) for _ in range(n)]
    parts = take(N_SRC)
    m_ref = take(1)[0]
    list_refs, left_ref = take(2) if sizes else (), take(1)[0] if back else None
    o_total, o_a, o_b = take(3)
    plan_refs, grad_ref = take(3) if sizes else (), take(1)[0] if back else None
    in_f, in_b, got_f, s_wire, r_wire, u_wire, y_wire, t_buf, u_buf, y_buf, load, send, recv, put = take(14)
    n_rows = t_buf.shape[0] // n_chunk
    cut = [pl.ds(k * n_rows, n_rows) for k in range(n_chunk)]
    thin = [pl.ds(k * n_rows // 2, n_rows // 2) for k in range(n_chunk)]
    side = lax.broadcasted_iota(I32, (n_rows // 2, LANES), 1) < LANES // 2
    tiles = d // LANES
    turn = lambda v: pltpu.roll(v, LANES // 2, 1)
    lanes = lambda v, j: v[:, LANES * j:LANES * (j + 1)]

    def pack(wire, k, value):
        top, low = value[:n_rows // 2], value[n_rows // 2:]
        turned = [turn(lanes(low, j)) for j in range(tiles + 1)]
        parts = [lanes(top, j) for j in range(tiles)] + [jnp.where(side, lanes(top, tiles), turned[0])]
        parts += [jnp.where(side, turned[j], turned[j + 1]) for j in range(tiles)]
        for j, part in enumerate(parts):
            wire[thin[k], LANES * j:LANES * (j + 1)] = part.astype(BF16)

    def unpack(wire, k):
        value = wire[thin[k], :].astype(F32)
        turned = [turn(lanes(value, tiles + j)) for j in range(tiles + 1)]
        top = [lanes(value, j) for j in range(tiles)] + [jnp.where(side, lanes(value, tiles), 0.0)]
        low = [jnp.where(side, turned[j], turned[j + 1]) for j in range(tiles)] + [jnp.where(side, turned[tiles], 0.0)]
        return jnp.concatenate([jnp.concatenate(top, axis=1), jnp.concatenate(low, axis=1)], axis=0)

    chunks = range(n_chunk)
    loads = {}
    for i, part in enumerate(parts[:2] if reduce else parts):
        buf = in_f.at[i] if reduce or i == 0 else in_b.at[i - 1]
        for k in chunks:
            loads[i, k] = pltpu.make_async_copy(part.at[cut[k]], buf.at[cut[k]], load.at[i, k])
    order = (1, 0) if reduce else range(N_SRC)
    for i in order:
        for k in chunks:
            loads[i, k].start()
    u_buf[...] = jnp.zeros(u_buf.shape, BF16)
    meet((Y, CORE))
    links = []
    copy_in = pltpu.make_async_copy

    def link(src, dst, rel, cut=cut):
        n = len(links)
        links.append([remote(src.at[cut[k]], dst.at[cut[k]], send.at[n, k], recv.at[n, k], rel) for k in chunks])
        return links[-1]

    if reduce:
        first = link(parts[3], got_f.at[1], CORE)
        second = link(parts[2], got_f.at[0], CORE)
        over = link(s_wire, r_wire, Y, thin)
        for copies in (first, second):
            for copy in copies:
                copy.start()
        for k in chunks:
            loads[1, k].wait()
            first[k].wait_recv()
            pack(s_wire, k, in_f[1, cut[k], :] + got_f[1, cut[k], :])
            over[k].start()
    to_y = link(u_wire, y_wire, Y, thin)
    to_core = link(u_buf, o_b.at[0], CORE)
    puts = []
    for k in chunks:
        if reduce:
            loads[0, k].wait()
            second[k].wait_recv()
            over[k].wait_recv()
            total = in_f[0, cut[k], :] + got_f[0, cut[k], :] + unpack(r_wire, k)
        else:
            for i in range(N_SRC):
                loads[i, k].wait()
            total = in_f[0, cut[k], :]
            for i in range(N_SRC - 1):
                total = total + in_b[i, cut[k], :].astype(F32)
        total = total.astype(BF16)
        t_buf[cut[k], :] = total
        dims = (((1,), (1 if back else 0,)), ((), ()))
        mixed = lax.dot_general(total[:, :d], m_ref[...], dims, preferred_element_type=F32)
        u_buf[cut[k], 0:d] = (total[:, :d].astype(F32) + mixed).astype(BF16)
        pack(u_wire, k, u_buf[cut[k], :].astype(F32))
        to_y[k].start()
        to_core[k].start()
        puts.append(pltpu.make_async_copy(u_buf.at[cut[k]], o_a.at[0, cut[k]], put.at[0, k]))
        puts.append(pltpu.make_async_copy(t_buf.at[cut[k]], o_total.at[cut[k]], put.at[1, k]))
        for copy in puts[-2:]:
            copy.start()
    if sizes:
        plan_kernel(*sizes, *list_refs, *plan_refs)
    if back:
        grad_ref[...] = lax.dot_general(left_ref[:, :d], t_buf[:, :d], (((0,), (0,)), ((), ())), preferred_element_type=F32)
    on = link(y_buf, o_b.at[1], CORE)
    for k in chunks:
        to_y[k].wait_recv()
        y_buf[cut[k], :] = unpack(y_wire, k).astype(BF16)
        on[k].start()
        puts.append(copy_in(y_buf.at[cut[k]], o_a.at[1, cut[k]], put.at[2, k]))
        puts[-1].start()
    waited = [to_y] + ([first, second, over] if reduce else [])
    for copies in links:
        for copy in copies:
            if any(copies is w for w in waited):
                copy.wait_send()
            else:
                copy.wait()
    for copy in puts:
        copy.wait()


def complete_blocks(parts, m, reduce, back, ident, sizes=None, lists=(), left=(), n_chunk=4):
    n_blk, wide = parts[0].shape
    d = m.shape[0]
    sem = lambda *s: pltpu.SemaphoreType.DMA(s)
    pair = jax.ShapeDtypeStruct((2, n_blk, wide), BF16)
    extra = plan_shapes(sizes) if sizes else []
    extra += [jax.ShapeDtypeStruct((d, d), F32)] * len(left)
    buf = lambda n, dt: pltpu.VMEM((n, n_blk, wide) if n else (n_blk, wide), dt)
    return pl.pallas_call(
        functools.partial(blocks_kernel, (n_chunk, reduce, back, d, sizes)),
        out_shape=[jax.ShapeDtypeStruct((n_blk, wide), BF16)] + [pair] * 2 + extra,
        in_specs=[any_space] * N_SRC + [in_vmem] * (1 + len(lists) + len(left)),
        out_specs=[any_space] * 3 + [in_vmem] * len(extra),
        scratch_shapes=[buf(2, F32), buf(3, BF16), buf(2, F32)] + [pltpu.VMEM((n_blk // 2, 2 * d), BF16)] * 4 + [
            buf(0, BF16), buf(0, BF16), buf(0, BF16), sem(4, n_chunk), sem(6, n_chunk), sem(6, n_chunk), sem(3, n_chunk)],
        compiler_params=pltpu.CompilerParams(collective_id=ident, has_side_effects=True, vmem_limit_bytes=VMEM_LIMIT),
        cost_estimate=pl.CostEstimate(flops=10 ** 8, bytes_accessed=n_blk * wide * 40, transcendentals=0),
        name=f"complete_blocks_{ident}",
    )(*parts, m, *lists, *left)


def solution(mesh):
    ep_size, dp_size = mesh.shape['ep'], mesh.shape['dp']
    sub = Mesh(mesh.devices.reshape(ep_size, dp_size // 2, 2), ('ep', 'x', 'core'))
    tok_axes = ('x', 'core', 'ep')
    tok_spec = P(tok_axes, None)
    route_spec = P(None, tok_axes, None)
    whole_spec = P(None, None, None)
    expert_spec = P(None, 'ep', None, None)
    flip = [(0, 1), (1, 0)]
    move = lambda v, axis: lax.ppermute(v, axis, flip)
    move_diag = lambda v: lax.ppermute(v, ('ep', 'core'), [(0, 3), (1, 2), (2, 1), (3, 0)])
    fence = lax.optimization_barrier

    def device_step(tokens, d_out, expert_ids, gate_vals, w_mix, w_gate, w_up, w_down):
        n_layers, d = w_mix.shape[0], w_mix.shape[1]
        n_tok = tokens.shape[0]
        top = expert_ids.shape[2]
        n_local = w_gate.shape[1]
        n_exp = n_local * ep_size
        n = n_tok * top
        n_rel = 2 * N_SRC
        wide = cdiv(d, LANES) * LANES
        weights = (jnp.swapaxes(w_gate, 2, 3), jnp.swapaxes(w_up, 2, 3), w_down)
        pad = lambda v: jnp.pad(v, ((0, 0), (0, wide - d)))
        send_three = lambda p: [move(p[1], 'ep'), move(p[2], 'core'), move_diag(p[3])]

        def own_sum(p, got):
            return sum([g.astype(F32) for g in got], p)[:, :d].astype(BF16)

        one = lambda v: v.reshape(1, n_tok, wide)
        pairs = lambda a, b: [(a, 0), (a, 1), (b, 0), (b, 1)]

        one = lambda v: v.reshape(1, n_tok, wide)
        pairs = lambda a, b: [(a, 0), (a, 1), (b, 0), (b, 1)]
        singles = lambda *v: [(one(a), 0) for a in v]

        u0 = pad((tokens.astype(F32) + jnp.dot(tokens, w_mix[0], preferred_element_type=F32)).astype(BF16))
        u0_y, u0_c = move(u0, 'ep'), move(u0, 'core')
        lists = [sorted_list(expert_ids[l], gate_vals[l]) for l in range(n_layers)]
        counts = jnp.sum((expert_ids.transpose(0, 2, 1).reshape(n_layers, n, 1) == jnp.arange(n_exp, dtype=I32)).astype(F32), axis=1)
        packed = jnp.concatenate([jnp.concatenate([v[0] for v in lists] + [v[1] for v in lists]).reshape(-1, LANES),
                                  jnp.pad(counts, ((0, 8 - n_layers), (0, LANES - n_exp)))], axis=0)
        dy = pad(d_out)
        packed, dy = fence((packed, dy))
        shared = share(packed, N_SRC)
        u0_y, u0_c, dy, shared = fence((u0_y, u0_c, dy, shared))
        u0_d = move(u0_y, 'core')
        shared_x = move(shared, 'x')
        dy_y, dy_x = move(dy, 'ep'), move(dy, 'x')
        sizes = (n_layers, n_local, n_tok, n // LANES)
        routes = plan(shared, shared, sizes)
        u0_half = singles(u0, u0_y, u0_c, u0_d)
        add = lambda a, b: a.astype(F32) + b.astype(F32)
        to_chips = lambda v: [move(v, 'ep'), move(v, 'x'), lax.ppermute(v, ('ep', 'x'), [(0, 3), (1, 2), (2, 1), (3, 0)])]
        of_chips = lambda v, t: (add(v, t[0]) + add(t[1], t[2])).astype(BF16)
        piece = first_piece(n_local // 2)
        rows = lax.slice_in_dim(routes[0], ROW_PARTNER * LANES, ROW_PARTNER * LANES + n_local // 2)
        *part, ab0, xu0 = run_experts(routes, 0, u0_half, None, weights, None, None, True, True, p_f32=True)
        dy_y, dy_x, shared_x, part = fence((dy_y, dy_x, shared_x, part))
        dy_c, dy_d, dy_xy, dy_xc = move(dy, 'core'), move(dy_y, 'core'), move(dy_y, 'x'), move(dy_x, 'core')
        y0, u1_a, u1_b, *routes_x = complete_blocks(part, w_mix[1], True, False, 1, sizes, (shared, shared_x))
        routes_x = flat(*routes_x)
        dy_c, dy_d, dy_xy, dy_xc, u0_p, u0_q, y0, u1_a, u1_b = fence(
            (dy_c, dy_d, dy_xy, dy_xc, u0, u0_y, y0, u1_a, u1_b))
        dy_xd = move(dy_xy, 'core')
        u1_xa = move(u1_a, 'x')
        out = run_experts(routes, 1, pairs(u1_a, u1_b), singles(dy, dy_y, dy_c, dy_d), weights, None, None, True, True)
        u1_xa, dy_xd, u0_p, u0_q, out = fence((u1_xa, dy_xd, u0_p, u0_q, out))
        y_part, du_part, g1 = out[:4], out[4:8], out[8]
        u1_xb = move(u1_xa, 'core')
        got = send_three(du_part)
        u0_x, u0_xy = move(u0_p, 'x'), move(u0_q, 'x')
        out = run_experts(routes_x, 1, pairs(u1_xa, u1_xb), singles(dy_x, dy_xy, dy_xc, dy_xd), weights, g1, None,
                          False, False)
        got, u0_x, u0_xy, out = fence((got, u0_x, u0_xy, out))
        *finals, sent_a, sent_b = out
        got1 = [move(sent_a, 'core'), move(sent_b, 'core')]
        du1, dx_a, dx_b, g_mix1 = complete_blocks([du_part[0], *got], w_mix[1], False, True, 2, left=(y0,))
        tx = lambda x, du: jnp.einsum('td,te->de', x, du, preferred_element_type=F32)
        dx_a, y_part, got1, u0_x, u0_xy, g_mix1 = fence((dx_a, y_part, got1, u0_x, u0_xy, g_mix1))
        dx_xa = move(dx_a, 'x')
        part1 = g_mix1.astype(BF16)
        theirs1 = to_chips(part1)
        got_y = send_three(y_part)
        u0_xc, u0_xd = move(u0_x, 'core'), move(u0_xy, 'core')
        out = run_experts(routes, 0, None, pairs(dx_a, dx_b), weights, None, finals, False, True, got=got1, kept=(ab0, xu0))
        dx_xa, got_y, u0_xc, u0_xd, theirs1, out = fence((dx_xa, got_y, u0_xc, u0_xd, theirs1, out))
        du_part, g0, finals = out[:4], out[4], out[5:]
        dx_xb = move(dx_xa, 'core')
        got = send_three(du_part)
        part1 = of_chips(part1, theirs1)
        theirs1 = move(part1, 'core')
        du_part, dx_xb, part1 = fence((du_part, dx_xb, part1))
        out = run_experts(routes_x, 0, singles(u0_x, u0_xy, u0_xc, u0_xd), pairs(dx_xa, dx_xb), weights, g0, finals,
                          False, False)
        got, theirs1, got_y, y_own, rows, out = fence((got, theirs1, got_y, y_part[0], rows, out))
        *finals, sent_a, sent_b = out
        got_a, got_b = move(sent_a, 'core'), move(sent_b, 'core')
        du0 = own_sum(du_part[0], got)
        part0 = tx(tokens, du0).astype(BF16)
        theirs0 = to_chips(part0)
        dx0 = (du0.astype(F32) + jnp.einsum('te,de->td', du0, w_mix[0], preferred_element_type=F32)).astype(BF16)
        y1 = own_sum(y_own, got_y).T
        dx0, y1, got_a, finals = fence((dx0, y1, got_a, finals))
        finals = place(rows, 0, 0, got_a, finals)
        dx0, got_b, finals = fence((dx0.T, got_b, finals))
        finals = place(rows, piece, 0, got_b, finals)
        theirs0, finals = fence((theirs0, finals))
        total0 = of_chips(part0, theirs0)
        g_mix = jnp.stack([add(total0, move(total0, 'core')), add(part1, theirs1)]).astype(BF16)
        return (y1.T, dx0.T, g_mix, jnp.swapaxes(finals[0], 2, 3), jnp.swapaxes(finals[1], 2, 3), finals[2])

    return jax.shard_map(device_step, mesh=sub,
                         in_specs=(tok_spec, tok_spec, route_spec, route_spec, whole_spec,
                                   expert_spec, expert_spec, expert_spec),
                         out_specs=(tok_spec, tok_spec, whole_spec, expert_spec, expert_spec, expert_spec),
                         check_vma=False)
```

```python
import functools

import jax
import jax.numpy as jnp
from jax import lax
from jax.experimental import pallas as pl
from jax.experimental.pallas import tpu as pltpu
from jax.sharding import Mesh, PartitionSpec as P

F32, BF16, I32 = jnp.float32, jnp.bfloat16, jnp.int32
MESH = pl.DeviceIdType.MESH
ROWS = 384
GRP = 8
PITCH = 9
DEPTH = 3
FULL = 8
HALF = 4
CAP_FACTOR = 3
LANES = 128
N_SRC = 4
Y, CORE, X = 1, 2, 4
VMEM_LIMIT = 62 * 1024 * 1024
PER_TILE = ROWS // GRP
ROW_BOUND, ROW_GOFF, ROW_EXPERT, ROW_PARTNER, TAB_ROWS = 32, 33, 34, 35, 40
SLOT_GROUPS = 256


def cdiv(a, b):
    return (a + b - 1) // b


def first_piece(n_exp):
    return n_exp * 5 // 8


def spans(d):
    return [(LANES * j, min(LANES, d - LANES * j)) for j in range(cdiv(d, LANES))]


any_space = pl.BlockSpec(memory_space=pl.ANY)
in_vmem = pl.BlockSpec(memory_space=pltpu.VMEM)


def sorted_list(expert_ids, gate_vals):
    n_tok, top = expert_ids.shape
    n = n_tok * top
    keys = expert_ids.T.reshape(n) * n + jnp.arange(n, dtype=I32)
    keys, gates = lax.sort((keys, gate_vals.T.reshape(n)), num_keys=1, is_stable=False)
    return (keys % n_tok).astype(F32), gates


def plan_kernel(n_layers, n_local, n_tok, list_rows, deal_ref, all_ref, tab_ref, idx_ref, gate_ref):
    n_mine = n_local // 2
    core, ep = lax.axis_index('core'), lax.axis_index('ep')
    list_len = list_rows * LANES
    lane = lambda n: lax.broadcasted_iota(I32, (n, LANES), 1).astype(F32)
    sub = lambda n: lax.broadcasted_iota(I32, (n, LANES), 0).astype(F32)
    over_lanes = lambda v: jnp.sum(v, axis=1, keepdims=True)
    over_subs = lambda v: jnp.sum(v, axis=0, keepdims=True)
    l16, s16 = lane(n_mine), sub(n_mine)
    groups = lambda c: jnp.floor((c + (GRP - 0.5)) * (1.0 / GRP))
    for l in range(n_layers):
        cnt = all_ref[:, 2 * n_layers * list_rows + l, :]
        ends = cnt
        step = 1
        while step < 2 * n_local:
            ends = ends + jnp.where(lane(N_SRC) >= step, pltpu.roll(ends, step, 1), 0.0)
            step *= 2
        starts = ends - cnt
        second = (ep > 0)
        local = lambda v: jnp.where(lane(N_SRC) < n_local, jnp.where(second, pltpu.roll(v, LANES - n_local, 1), v), 0.0)
        cnt, starts = local(cnt), local(starts)
        tiles = jnp.floor((over_subs(groups(local(deal_ref[:, 2 * n_layers * list_rows + l, :]))) + (PER_TILE - 0.5))
                          * (1.0 / PER_TILE))
        load = jnp.where(lane(1) < n_local, jnp.maximum(1.0, tiles), -1.0)
        wide = jnp.broadcast_to(load, (n_local, LANES))
        col = over_lanes(jnp.where(lane(n_local) == sub(n_local), wide, 0.0))
        ahead = (col > wide) | ((col == wide) & (sub(n_local) < lane(n_local)))
        rank = over_subs(jnp.where(ahead, 1.0, 0.0))
        odd = s16 - 2.0 * jnp.floor(s16 * 0.5 + 0.25)
        flip = jnp.where(core > 0, 1.0 - odd, odd)
        dealt = lambda f: (jnp.broadcast_to(rank, (n_mine, LANES)) == 2.0 * s16 + f) & (l16 < n_local)
        pick = dealt(flip)
        choose = lambda p, row: over_lanes(jnp.where(p, jnp.broadcast_to(row, (n_mine, LANES)), 0.0))
        mine = lambda row: choose(pick, row)
        as_row = lambda c: over_subs(jnp.where(l16 == s16, c, 0.0))
        experts = as_row(mine(lane(1)))
        partner = as_row(choose(dealt(1.0 - flip), lane(1)))
        at = l * TAB_ROWS
        off = jnp.zeros((n_mine, 1), F32)
        pos = [jnp.zeros((n_mine, LANES), F32) for _ in range(SLOT_GROUPS // LANES)]
        for s in range(N_SRC):
            c, st = mine(cnt[s:s + 1]), mine(starts[s:s + 1]) + float(s * list_len)
            ng = groups(c)
            for i in range(len(pos)):
                rel = l16 + float(LANES * i) - off
                code = (st + GRP * rel) * 16.0 + jnp.minimum(float(GRP), c - GRP * rel)
                pos[i] = jnp.where((rel >= 0) & (rel < ng), code, pos[i])
            off = off + ng
        for i in range(len(pos)):
            tab_ref[pl.ds(at + i, n_mine, stride=len(pos)), :] = pos[i].astype(I32)
        n_tiles = jnp.maximum(1.0, jnp.floor((off + (PER_TILE - 0.5)) * (1.0 / PER_TILE)))
        bounds = over_subs(jnp.where(s16 < l16, n_tiles, 0.0))
        before = over_lanes(jnp.where(l16 == s16, jnp.broadcast_to(bounds, (n_mine, LANES)), 0.0))
        t = jnp.minimum(l16, over_subs(jnp.broadcast_to(n_tiles, (n_mine, LANES))) - 1.0)
        inside = (t >= before) & (t < before + n_tiles)
        goff = over_subs(jnp.where(inside, s16 * float(SLOT_GROUPS) + (t - before) * float(PER_TILE), 0.0))
        rows = [(ROW_BOUND, bounds), (ROW_GOFF, goff), (ROW_EXPERT, experts), (ROW_PARTNER, partner)]
        for row, value in rows:
            tab_ref[at + row:at + row + 1, :] = value.astype(I32)
    for l in range(n_layers):
        pad = l * (N_SRC * list_rows + 8) + N_SRC * list_rows
        gate_ref[pad:pad + 8, :] = jnp.zeros((8, LANES), F32)
        for s in range(N_SRC):
            to = (l * N_SRC + s) * list_rows
            toks = all_ref[s, l * list_rows:(l + 1) * list_rows, :]
            idx_ref[to:to + list_rows, :] = ((toks + float(s * n_tok)) * float(PITCH)).astype(I32)
            to = l * (N_SRC * list_rows + 8) + s * list_rows
            gate_ref[to:to + list_rows, :] = all_ref[s, (n_layers + l) * list_rows:(n_layers + l + 1) * list_rows, :]


def plan_shapes(sizes):
    n_layers, _, _, list_rows = sizes
    rows = (n_layers * TAB_ROWS, n_layers * N_SRC * list_rows, n_layers * (N_SRC * list_rows + 8))
    return [jax.ShapeDtypeStruct((n, LANES), dt) for n, dt in zip(rows, (I32, I32, F32))]


def flat(tab, idx, gates):
    return tab.reshape(-1), idx.reshape(-1), gates


def plan(deal, shared, sizes):
    return flat(*pl.pallas_call(
        functools.partial(plan_kernel, *sizes),
        out_shape=plan_shapes(sizes),
        in_specs=[in_vmem] * 2, out_specs=[in_vmem] * 3,
        cost_estimate=pl.CostEstimate(flops=10 ** 7, bytes_accessed=10 ** 6, transcendentals=0),
        name="plan",
    )(deal, shared))


def expert_kernel(cfg, *refs):
    fwd, bwd, own, layer, n_blk, d, ff, n_exp, picks, row_id, list_len, p_f32, n_alias, got_layer = cfg
    save, load = fwd and not bwd, own and bwd and not fwd
    refs = list(refs)
    take = lambda n: [refs.pop(0) for _ in range(n)]
    tab_hbm, idx_hbm, gate_hbm = take(3)
    u_pieces = take(N_SRC) if not load else []
    dy_pieces = take(N_SRC) if bwd else []
    wg_hbm, wu_hbm, wd_hbm = take(3)
    ab_hbm, xu_hbm = take(2) if load else (None, None)
    prev = take(1)[0] if bwd and not own else None
    got = take(2) if got_layer is not None else None
    take(n_alias)
    y_outs = take(N_SRC) if fwd else []
    du_outs = take(N_SRC) if bwd and own else []
    grad = take(1)[0] if bwd and own else None
    finals = take(3) if bwd and not own or got_layer is not None else None
    sent = take(2) if bwd and not own else None
    ab_hbm, xu_hbm = take(2) if save else (ab_hbm, xu_hbm)
    tab_ref, idx, gate_ref, land, table, gat = take(6)
    acc, row_ref = take(2) if own else (None, None)
    gu_ref, wd_ref, g_ref, x_u = take(4)
    x_c = take(1)[0] if bwd else None
    ab_ref = take(1)[0]
    dh_ref = take(1)[0] if bwd else None
    h_ref = take(1)[0]
    dab_ref, sums = take(2) if bwd else (None, None)
    keep_buf = take(1)[0] if bwd and not own else None
    got_buf = take(1)[0] if got is not None else None
    list_sem, land_sem, w_sem = take(3)
    sum_sem = take(1)[0] if bwd else None
    keep_sem = take(1)[0] if bwd and not own else None
    read_sem, write_sem = take(2) if got is not None else (None, None)
    stage_f, out_sem = take(2) if own else (None, None)
    ab_sem, xu_sem = take(2) if save or load else (None, None)

    split = first_piece(n_exp)
    copy = pltpu.make_async_copy
    cols = spans(d)
    lo = ff // 256 * 256
    hi = ff - lo
    dot = functools.partial(lax.dot_general, preferred_element_type=F32)
    nn = (((1,), (0,)), ((), ()))
    nt = (((1,), (1,)), ((), ()))
    tn = (((0,), (0,)), ((), ()))
    al = pl.multiple_of
    n_row = N_SRC * n_blk
    glane = lax.broadcasted_iota(I32, (GRP, LANES), 1)
    gsub = lax.broadcasted_iota(I32, (GRP, LANES), 0)

    def row_at(r):
        return pl.ds(r * PITCH, FULL)

    def codes_of(tile):
        at = ROW_GOFF * LANES + tile
        if own and bwd:
            return lambda q: tab_ref[tab_ref[at] + q]
        view = tab_ref.at[pl.ds(tab_ref[at], PER_TILE)]
        return lambda q: view[q]

    def gather(codes, q):
        ids = idx.at[pl.ds(codes(q) >> 4, GRP)]
        for k in range(GRP):
            gat[row_at(q * GRP + k), :] = table[pl.ds(ids[k], FULL), :]

    def gate_column(code):
        pos = code >> 4
        row, shift = pos >> 7, pos & (LANES - 1)
        want = glane == gsub + shift
        over = glane == gsub + (shift - LANES)
        here = gate_ref[pl.ds(row, GRP, stride=0), :]
        there = gate_ref[pl.ds(row + 1, GRP, stride=0), :]
        v = jnp.where(want, here, jnp.where(over, there, 0.0))
        return jnp.where(gsub < (code & 15), jnp.sum(v, axis=1, keepdims=True), 0.0)

    def scatter(codes, q):
        ids = idx.at[pl.ds(codes(q) >> 4, GRP)]
        new = []
        for k in range(GRP):
            at = pl.ds(ids[k], FULL)
            new.append((at, acc[at, :] + row_ref[row_at(q * GRP + k), :]))
        for at, value in reversed(new):
            acc[at, :] = value

    def keep_ab(t):
        ends = (ab_ref.at[t & 1], ab_hbm.at[t])
        return copy(*(ends if save else ends[::-1]), ab_sem.at[t & 1])

    def keep_xu(t):
        ends = (x_u.at[t & 1], xu_hbm.at[t])
        return copy(*(ends if save else ends[::-1]), xu_sem.at[t & 1])

    def of(ref, t):
        return ref.at[t & 1] if save or load else ref

    def convert(codes, t):
        for q in range(0, PER_TILE, 2):
            part = []
            for p in (q, q + 1):
                code = codes(p)
                rows = [gat[pl.ds(GRP * PITCH * p + j, GRP, stride=PITCH), :]
                        for j in range(HALF if load else 0, FULL if bwd else HALF)]
                real = gsub < (code & 15)
                gate = gate_column(code)
                g_ref[GRP * p:GRP * (p + 1), :] = gate
                us, dys = ([], rows) if load else (rows[:HALF], rows[HALF:])
                part.append([jnp.where(real, v, 0.0) for v in us] + [v * gate for v in dys])
            at = slice(GRP * q, GRP * (q + 2))
            for x, o in ((None if load else of(x_u, t), 0), (x_c, 0 if load else HALF)):
                if x is None:
                    continue
                for j, (c, w) in enumerate(cols):
                    both = jnp.concatenate([part[0][o + j], part[1][o + j]], axis=0)
                    x[at, c:c + w] = both[:, :w].astype(BF16)

    def put_rows(o, value, s0):
        value = value.astype(BF16).astype(F32)
        n = value.shape[0]
        for j, (c, w) in enumerate(cols):
            row_ref[pl.ds(PITCH * s0 + o + j, n, stride=PITCH), 0:w] = value[:, c:c + w] * g_ref[s0:s0 + n, 0:w]

    low = lax.broadcasted_iota(I32, (16, 2 * hi), 1) < hi

    def middle(a, b, dh):
        sig = 0.5 * jnp.tanh(0.5 * a) + 0.5
        act = a * sig
        h = act * b
        if dh is None:
            return h, None, None
        slope = sig * (1.0 + a * (1.0 - sig))
        return h, dh * b * slope, dh * act

    def weights(e, slot):
        at = (layer, tab_ref[ROW_EXPERT * LANES + e])
        moves = []
        for i, w in enumerate((wg_hbm, wu_hbm)):
            moves.append((w.at[at + (pl.ds(0, lo),)], gu_ref.at[slot, pl.ds(i * lo, lo)]))
            moves.append((w.at[at + (pl.ds(lo, hi),)], gu_ref.at[slot, pl.ds(2 * lo + i * hi, hi)]))
        moves.append((wd_hbm.at[at], wd_ref.at[slot]))
        return [copy(a, b, w_sem.at[slot, i]) for i, (a, b) in enumerate(moves)]

    def sums_in(e, slot):
        return copy(prev.at[e], sums.at[slot], sum_sem.at[slot])

    def sums_out(e, slot):
        return copy(sums.at[slot], grad.at[e], sum_sem.at[slot])

    def keeps(e, slot):
        at = (layer, tab_ref[ROW_EXPERT * LANES + e])
        return [copy(keep_buf.at[slot, i], finals[i].at[at], keep_sem.at[slot, i]) for i in range(3)]

    def send(e, slot, part):
        return copy(keep_buf.at[slot], sent[part].at[e - part * split], keep_sem.at[slot, 3])

    def read(e, slot, part=0):
        return copy(got[part].at[e - part * split], got_buf.at[slot], read_sem.at[slot])

    def writes(e, slot):
        to = tab_ref[TAB_ROWS * LANES + e]
        return [copy(got_buf.at[slot, i], finals[i].at[got_layer, to], write_sem.at[slot, i]) for i in range(3)]

    def start(moves):
        for m in moves:
            m.start()

    def wait(moves):
        for m in moves:
            m.wait()

    n_tab = TAB_ROWS * LANES
    lists = [copy(tab_hbm.at[pl.ds(row_id * n_tab, n_tab)], tab_ref.at[pl.ds(0, n_tab)], list_sem.at[0]),
             copy(idx_hbm.at[pl.ds(row_id * N_SRC * list_len, N_SRC * list_len)], idx.at[pl.ds(0, N_SRC * list_len)],
                  list_sem.at[1]),
             copy(gate_hbm.at[pl.ds(row_id * gate_ref.shape[0], gate_ref.shape[0])], gate_ref, list_sem.at[2])]
    if got is not None:
        at = (got_layer * TAB_ROWS + ROW_PARTNER) * LANES
        lists.append(copy(tab_hbm.at[pl.ds(at, LANES)], tab_ref.at[pl.ds(n_tab, LANES)], list_sem.at[3]))
    start(lists)
    pieces = []
    for s in range(N_SRC):
        if not load:
            pieces.append((u_pieces[s], picks[0][s], s, 0, fwd))
        if bwd:
            pieces.append((dy_pieces[s], picks[1][s], s, HALF, own))
    lands = [copy(ref.at[pick], land.at[i % N_SRC], land_sem.at[i % N_SRC]) for i, (ref, pick, *_) in enumerate(pieces)]
    start(lands[:N_SRC])
    lists[0].wait()
    for e in range(DEPTH - 1):
        start(weights(e, e))
        if bwd and not own:
            sums_in(e, e).start()
    if got is not None:
        lists[3].wait()
        read(0, 0).start()
    if own:
        def clear(c, _):
            for k in range(4):
                acc[pl.ds(al(c * 1152 + 288 * k, 8), 288), :] = jnp.zeros((288, LANES), F32)
            return 0

        lax.fori_loop(0, acc.shape[0] // 1152, clear, 0)
        row_ref[...] = jnp.zeros(row_ref.shape, F32)
    rows = 256
    for i, (_, _, s, o, seed) in enumerate(pieces):
        lands[i].wait()

        def fill(c, _, i=i, o=o, seed=seed, s=s):
            r = al(c * rows, rows)
            for j in range(HALF):
                vals = land[i % N_SRC, pl.ds(r, rows), LANES * j:LANES * (j + 1)].astype(F32)
                to = pl.ds(PITCH * (s * n_blk + r) + o + j, rows, stride=PITCH)
                table[to, :] = vals
                if seed and s == 0:
                    acc[to, :] = vals
            return 0

        lax.fori_loop(0, n_blk // rows, fill, 0)
        if i + N_SRC < len(pieces):
            lands[i + N_SRC].start()
    wait(lists[1:3])
    for k in range(GRP):
        idx[N_SRC * list_len + k] = 0

    def first(q, _):
        gather(begin, 2 * q)
        gather(begin, 2 * q + 1)
        return 0

    begin = codes_of(0)
    lax.fori_loop(0, PER_TILE // 2, first, 0)
    convert(begin, 0)
    if save:
        keep_xu(0).start()
    if load:
        keep_ab(0).start()
        keep_xu(0).start()

    def expert(e, _):
        slot = e & 1
        deep = lax.rem(e, DEPTH)
        sum_slot = slot if own else deep
        wait(weights(e, deep))
        if bwd and not own:
            sums_in(e, deep).wait()
        if got is not None:
            read(0, slot).wait()
            start(writes(e, slot))

            @pl.when((e > 0) & (e < n_exp - 1))
            def _():
                wait(writes(e - 1, 1 - slot))

        @pl.when(e < n_exp - (DEPTH - 1))
        def _():
            ahead = lax.rem(e + DEPTH - 1, DEPTH)
            start(weights(e + DEPTH - 1, ahead))
            if bwd and not own:
                sums_in(e + DEPTH - 1, ahead).start()

        @pl.when(e < n_exp - 1)
        def _():
            if got is not None:
                for part in range(2):
                    @pl.when((e + 1 >= split) if part else (e + 1 < split))
                    def _(part=part):
                        read(e + 1, 1 - slot, part).start()

        if bwd and own:
            @pl.when(e > 1)
            def _():
                sums_out(e - 2, slot).wait()

            sums[slot] = jnp.zeros(sums.shape[1:], F32)

        def tile(t, _):
            if save:
                @pl.when(t > 1)
                def _():
                    keep_ab(t - 2).wait()

                @pl.when(t > 0)
                def _():
                    keep_xu(t - 1).wait()
            if load:
                keep_ab(t).wait()
                keep_xu(t).wait()
                keep_ab(t + 1).start()
                keep_xu(t + 1).start()
            ab, xu = of(ab_ref, t), of(x_u, t)
            before, after = codes_of(jnp.maximum(t - 1, 0)), codes_of(t + 1)
            for q in range(PER_TILE):
                if own:
                    scatter(before, q)
                gather(after, q)
            front = ROWS if own and bwd else ROWS // 2
            for s0 in range(0, ROWS, front):
                sl = slice(s0, s0 + front)
                if not load:
                    ab[sl, :] = dot(xu[sl, :], gu_ref[deep], nt)
                if bwd:
                    dh_ref[sl, :] = dot(x_c[sl, :], wd_ref[deep], nt)
            for r in range(0, ROWS, 16):
                rows = slice(r, r + 16)
                for c in range(0, lo, LANES):
                    h, da, db = middle(ab[rows, c:c + LANES], ab[rows, lo + c:lo + c + LANES],
                                       dh_ref[rows, c:c + LANES] if bwd else None)
                    h_ref[rows, c:c + LANES] = h.astype(BF16)
                    if bwd:
                        dab_ref[rows, c:c + LANES] = da.astype(BF16)
                        dab_ref[rows, lo + c:lo + c + LANES] = db.astype(BF16)
                a = ab[rows, 2 * lo:]
                b = pltpu.roll(a, hi, 1)
                dh = dh_ref[rows, lo:] if bwd else None
                if bwd:
                    dh = jnp.concatenate([dh, dh], axis=1)
                h, da, db = middle(a, b, dh)
                h_ref[rows, lo:] = h[:, :hi].astype(BF16)
                if bwd:
                    dab_ref[rows, 2 * lo:] = jnp.where(low, da, pltpu.roll(db, hi, 1)).astype(BF16)
            half = ROWS // 2
            for s0 in range(0, ROWS, half):
                sl = slice(s0, s0 + half)
                if fwd:
                    put_rows(0, dot(h_ref[sl, :], wd_ref[deep], nn), s0)
                if bwd and own:
                    put_rows(HALF, dot(dab_ref[sl, :], gu_ref[deep], nn), s0)
            if bwd:
                view = sums.at[sum_slot]
                view[0:2 * ff, :] += dot(dab_ref[...], xu[...], tn)
                view[2 * ff:, :] += dot(h_ref[...], x_c[...], tn)
            convert(after, t + 1)
            if save:
                keep_ab(t).start()
                keep_xu(t + 1).start()
            return 0

        lax.fori_loop(tab_ref[ROW_BOUND * LANES + e], tab_ref[ROW_BOUND * LANES + e + 1], tile, 0)
        if bwd and own:
            sums_out(e, slot).start()
        if bwd and not own:
            @pl.when(e > 1)
            def _():
                wait(keeps(e - 2, slot) + [send(0, slot, 0)])

            for i in range(2):
                keep_buf[slot, i, 0:lo, :] = sums[deep, i * lo:(i + 1) * lo, :].astype(BF16)
                keep_buf[slot, i, lo:, :] = sums[deep, 2 * lo + i * hi:2 * lo + (i + 1) * hi, :].astype(BF16)
            keep_buf[slot, 2] = sums[deep, 2 * ff:, :].astype(BF16)
            start(keeps(e, slot))
            for part in range(2):
                @pl.when((e >= split) if part else (e < split))
                def _(part=part):
                    send(e, slot, part).start()
        return 0

    lax.fori_loop(0, n_exp, expert, 0)
    ends = ((n_exp - 2, (n_exp - 2) % 2), (n_exp - 1, (n_exp - 1) % 2))
    n_tiles = tab_ref[ROW_BOUND * LANES + n_exp]
    if save:
        wait([keep_ab(n_tiles - 2), keep_ab(n_tiles - 1), keep_xu(n_tiles - 1)])
    if save or load:
        keep_xu(n_tiles).wait()
    if load:
        keep_ab(n_tiles).wait()
    if own:
        end = codes_of(tab_ref[ROW_BOUND * LANES + n_exp] - 1)
        lax.fori_loop(0, PER_TILE, lambda q, _: (scatter(end, q), 0)[1], 0)
        flights = {}
        for o, out in ((HALF, du_outs), (0, y_outs)):
            for s in range(N_SRC if out else 0):
                wide = s == 0 or p_f32
                stage = stage_f.at[s] if wide else land.at[s]
                if s in flights:
                    flights[s].wait()

                def fetch(c, _, stage=stage, s=s, o=o):
                    r = al(c * rows, rows)
                    for j in range(HALF):
                        at = pl.ds(PITCH * (s * n_blk + r) + o + j, rows, stride=PITCH)
                        stage[pl.ds(r, rows), LANES * j:LANES * (j + 1)] = acc[at, :].astype(stage.dtype)
                    return 0

                lax.fori_loop(0, n_blk // rows, fetch, 0)
                flights[s] = copy(stage, out[s], out_sem.at[s])
                flights[s].start()
        wait(flights.values())
        if bwd:
            for e, slot in ends:
                sums_out(e, slot).wait()
    else:
        for e, slot in ends:
            wait(keeps(e, slot) + [send(0, slot, 0)])
    if got is not None:
        for e, slot in ends:
            wait(writes(e, slot))


def run_experts(routes, layer, u, dy, weights, prev, finals, fwd, own, p_f32=False, got=None, kept=None):
    tab, idx, gates = routes
    bwd = dy is not None
    wg, wu, wd = weights
    save, load = fwd and not bwd, kept is not None
    n_blk, wide = (dy or u)[0][0].shape[-2:]
    n_layers, n_local, ff, d = wd.shape
    n_exp = n_local // 2
    row_id = layer
    list_len = idx.shape[0] // (n_layers * N_SRC)

    arrays = lambda pieces: [v for v, _ in pieces]
    operands = [tab, idx, gates] + ([] if load else arrays(u)) + (arrays(dy) if bwd else []) + [wg, wu, wd] + list(kept or ())
    out_shape, aliases = [], {}
    for use in (fwd, bwd and own):
        if use:
            out_shape += [jax.ShapeDtypeStruct((n_blk, wide), F32 if s == 0 or p_f32 else BF16) for s in range(N_SRC)]
    if bwd and own:
        out_shape.append(jax.ShapeDtypeStruct((n_exp, 3 * ff, d), F32))
    if bwd and not own:
        operands.append(prev)
    if got is not None:
        operands += got
    for i, f in enumerate(finals or ()):
        aliases[len(operands)] = len(out_shape) + i
        operands.append(f)
    if bwd and not own or finals:
        out_shape += [jax.ShapeDtypeStruct((n_layers, n_local, ff, d), BF16)] * 3
    if bwd and not own:
        out_shape += [jax.ShapeDtypeStruct((n, 3, ff, d), BF16) for n in (first_piece(n_exp), n_exp - first_piece(n_exp))]
    if save:
        most = n_exp * (SLOT_GROUPS // PER_TILE) + 2
        out_shape += [jax.ShapeDtypeStruct((most, ROWS, 2 * ff), F32), jax.ShapeDtypeStruct((most, ROWS, d), BF16)]
    sem = lambda *s: pltpu.SemaphoreType.DMA(s)
    mid = lambda n, dt: pltpu.VMEM((ROWS, n), dt)
    twin = lambda n, dt: pltpu.VMEM((2, ROWS, n), dt) if save or load else mid(n, dt)
    table, rows = pltpu.VMEM((PITCH * N_SRC * n_blk, LANES), F32), pltpu.VMEM((PITCH * ROWS, LANES), F32)
    scratch = [pltpu.SMEM(((TAB_ROWS + 1) * LANES,), I32), pltpu.SMEM((N_SRC * list_len + LANES,), I32),
               pltpu.VMEM((N_SRC * list_len // LANES + 8, LANES), F32), pltpu.VMEM((N_SRC, n_blk, wide), BF16)]
    scratch += [table, rows] * (1 + own)
    scratch += [pltpu.VMEM((DEPTH, 2 * ff, d), BF16), pltpu.VMEM((DEPTH, ff, d), BF16), mid(LANES, F32)]
    scratch += [twin(d, BF16)] + [mid(d, BF16)] * bwd + [twin(2 * ff, F32)] + [mid(ff, F32)] * bwd + [mid(ff, BF16)]
    scratch += [mid(2 * ff, BF16), pltpu.VMEM((2 if own else DEPTH, 3 * ff, d), F32)] * bwd
    if bwd and not own:
        scratch.append(pltpu.VMEM((2, 3, ff, d), BF16))
    if got is not None:
        scratch.append(pltpu.VMEM((2, 3, ff, d), BF16))
    scratch += [sem(4), sem(N_SRC), sem(DEPTH, 5)] + [sem(DEPTH)] * bwd
    if bwd and not own:
        scratch.append(sem(2, 4))
    if got is not None:
        scratch += [sem(2), sem(2, 3)]
    if own:
        scratch += [pltpu.VMEM((N_SRC if p_f32 else 1, n_blk, wide), F32), sem(N_SRC)]
    if save or load:
        scratch += [sem(2), sem(2)]
    passes = 2 + fwd + bwd * (4 + 2 * own)
    flops = 2 * d * ff * passes * n_blk * N_SRC * 2
    hoist = 1300 if not own else 600 if load else 750 if save else 900
    picks = [[i for _, i in u] if u else None, [i for _, i in dy] if bwd else None]
    cfg = (fwd, bwd, own, layer, n_blk, d, ff, n_exp, picks, row_id, list_len, p_f32, len(aliases),
           None if got is None else 1 - layer)
    return pl.pallas_call(
        functools.partial(expert_kernel, cfg),
        out_shape=out_shape,
        in_specs=[any_space] * len(operands),
        out_specs=[any_space] * len(out_shape),
        scratch_shapes=scratch,
        input_output_aliases=aliases,
        compiler_params=pltpu.CompilerParams(
            vmem_limit_bytes=VMEM_LIMIT),
        cost_estimate=pl.CostEstimate(flops=flops, bytes_accessed=3 * 2 * n_exp * d * ff, transcendentals=0),
        name=f"experts_{'f' if fwd else ''}{'b' if bwd else ''}_{'own' if own else 'other'}_{layer}",
    )(*operands)


def place_kernel(layer, n_exp, at, tab_ref, got_ref, *refs):
    outs, (buf, in_sem, out_sem) = refs[3:6], refs[6:]
    reads = [pltpu.make_async_copy(got_ref.at[i], buf.at[i], in_sem.at[i]) for i in range(n_exp)]
    for read in reads:
        read.start()
    writes = []
    for i, read in enumerate(reads):
        read.wait()
        e = tab_ref[at + i]
        for k, out in enumerate(outs):
            writes.append(pltpu.make_async_copy(buf.at[i, k], out.at[layer, e], out_sem.at[i, k]))
            writes[-1].start()
    for write in writes:
        write.wait()


def place(partner, at, layer, got, finals):
    n_exp = got.shape[0]
    return pl.pallas_call(
        functools.partial(place_kernel, layer, n_exp, at),
        out_shape=[jax.ShapeDtypeStruct(f.shape, f.dtype) for f in finals],
        grid_spec=pltpu.PrefetchScalarGridSpec(
            num_scalar_prefetch=1, grid=(1,), in_specs=[any_space] * 4, out_specs=[any_space] * 3,
            scratch_shapes=[pltpu.VMEM(got.shape, got.dtype), pltpu.SemaphoreType.DMA((n_exp,)),
                            pltpu.SemaphoreType.DMA((n_exp, 3))]),
        input_output_aliases={2: 0, 3: 1, 4: 2},
        compiler_params=pltpu.CompilerParams(vmem_limit_bytes=VMEM_LIMIT),
        cost_estimate=pl.CostEstimate(flops=0, bytes_accessed=4 * got.size, transcendentals=0),
        name=f"place_{layer}",
    )(partner, got, *finals)


def peer(rel):
    return {name: (lax.axis_index(name) + ((rel >> bit) & 1)) % 2 for bit, name in enumerate(("ep", "core", "x"))}


def meet(rels):
    barrier = pltpu.get_barrier_semaphore()
    for rel in rels:
        pl.semaphore_signal(barrier, inc=1, device_id=peer(rel), device_id_type=MESH)
    pl.semaphore_wait(barrier, len(rels))


def remote(src, dst, send, recv, rel):
    return pltpu.make_async_remote_copy(src_ref=src, dst_ref=dst, send_sem=send, recv_sem=recv,
                                        device_id=peer(rel), device_id_type=MESH)


def share_kernel(n_rel, mine_ref, all_ref, send_sem, recv_sem):
    meet(range(1, n_rel))
    copies = [remote(mine_ref, all_ref.at[rel], send_sem.at[rel], recv_sem.at[rel], rel) for rel in range(1, n_rel)]
    for copy in copies:
        copy.start()
    all_ref[0] = mine_ref[...]
    for copy in copies:
        copy.wait()


def share(mine, n_rel):
    return pl.pallas_call(
        functools.partial(share_kernel, n_rel),
        out_shape=jax.ShapeDtypeStruct((n_rel,) + mine.shape, mine.dtype),
        in_specs=[in_vmem],
        out_specs=in_vmem,
        scratch_shapes=[pltpu.SemaphoreType.DMA((n_rel,)), pltpu.SemaphoreType.DMA((n_rel,))],
        compiler_params=pltpu.CompilerParams(collective_id=0, has_side_effects=True),
        cost_estimate=pl.CostEstimate(flops=10 ** 7, bytes_accessed=mine.size * 4 * n_rel, transcendentals=0),
        name="share_lists",
    )(mine)


def blocks_kernel(cfg, *refs):
    n_chunk, reduce, back, d, sizes = cfg
    refs = list(refs)
    take = lambda n: [refs.pop(0) for _ in range(n)]
    parts = take(N_SRC)
    m_ref = take(1)[0]
    list_refs, left_ref = take(2) if sizes else (), take(1)[0] if back else None
    o_total, o_a, o_b = take(3)
    plan_refs, grad_ref = take(3) if sizes else (), take(1)[0] if back else None
    in_f, in_b, got_f, s_wire, r_wire, u_wire, y_wire, t_buf, u_buf, y_buf, load, send, recv, put = take(14)
    n_rows = t_buf.shape[0] // n_chunk
    cut = [pl.ds(k * n_rows, n_rows) for k in range(n_chunk)]
    thin = [pl.ds(k * n_rows // 2, n_rows // 2) for k in range(n_chunk)]
    side = lax.broadcasted_iota(I32, (n_rows // 2, LANES), 1) < LANES // 2
    tiles = d // LANES
    turn = lambda v: pltpu.roll(v, LANES // 2, 1)
    lanes = lambda v, j: v[:, LANES * j:LANES * (j + 1)]

    def pack(wire, k, value):
        top, low = value[:n_rows // 2], value[n_rows // 2:]
        turned = [turn(lanes(low, j)) for j in range(tiles + 1)]
        parts = [lanes(top, j) for j in range(tiles)] + [jnp.where(side, lanes(top, tiles), turned[0])]
        parts += [jnp.where(side, turned[j], turned[j + 1]) for j in range(tiles)]
        for j, part in enumerate(parts):
            wire[thin[k], LANES * j:LANES * (j + 1)] = part.astype(BF16)

    def unpack(wire, k):
        value = wire[thin[k], :].astype(F32)
        turned = [turn(lanes(value, tiles + j)) for j in range(tiles + 1)]
        top = [lanes(value, j) for j in range(tiles)] + [jnp.where(side, lanes(value, tiles), 0.0)]
        low = [jnp.where(side, turned[j], turned[j + 1]) for j in range(tiles)] + [jnp.where(side, turned[tiles], 0.0)]
        return jnp.concatenate([jnp.concatenate(top, axis=1), jnp.concatenate(low, axis=1)], axis=0)

    chunks = range(n_chunk)
    loads = {}
    for i, part in enumerate(parts[:2] if reduce else parts):
        buf = in_f.at[i] if reduce or i == 0 else in_b.at[i - 1]
        for k in chunks:
            loads[i, k] = pltpu.make_async_copy(part.at[cut[k]], buf.at[cut[k]], load.at[i, k])
    order = (1, 0) if reduce else range(N_SRC)
    for i in order:
        for k in chunks:
            loads[i, k].start()
    u_buf[...] = jnp.zeros(u_buf.shape, BF16)
    meet((Y, CORE))
    links = []
    copy_in = pltpu.make_async_copy

    def link(src, dst, rel, cut=cut):
        n = len(links)
        links.append([remote(src.at[cut[k]], dst.at[cut[k]], send.at[n, k], recv.at[n, k], rel) for k in chunks])
        return links[-1]

    if reduce:
        first = link(parts[3], got_f.at[1], CORE)
        second = link(parts[2], got_f.at[0], CORE)
        over = link(s_wire, r_wire, Y, thin)
        for copies in (first, second):
            for copy in copies:
                copy.start()
        for k in chunks:
            loads[1, k].wait()
            first[k].wait_recv()
            pack(s_wire, k, in_f[1, cut[k], :] + got_f[1, cut[k], :])
            over[k].start()
    to_y = link(u_wire, y_wire, Y, thin)
    to_core = link(u_buf, o_b.at[0], CORE)
    puts = []
    for k in chunks:
        if reduce:
            loads[0, k].wait()
            second[k].wait_recv()
            over[k].wait_recv()
            total = in_f[0, cut[k], :] + got_f[0, cut[k], :] + unpack(r_wire, k)
        else:
            for i in range(N_SRC):
                loads[i, k].wait()
            total = in_f[0, cut[k], :]
            for i in range(N_SRC - 1):
                total = total + in_b[i, cut[k], :].astype(F32)
        total = total.astype(BF16)
        t_buf[cut[k], :] = total
        dims = (((1,), (1 if back else 0,)), ((), ()))
        mixed = lax.dot_general(total[:, :d], m_ref[...], dims, preferred_element_type=F32)
        u_buf[cut[k], 0:d] = (total[:, :d].astype(F32) + mixed).astype(BF16)
        pack(u_wire, k, u_buf[cut[k], :].astype(F32))
        to_y[k].start()
        to_core[k].start()
        puts.append(pltpu.make_async_copy(u_buf.at[cut[k]], o_a.at[0, cut[k]], put.at[0, k]))
        puts.append(pltpu.make_async_copy(t_buf.at[cut[k]], o_total.at[cut[k]], put.at[1, k]))
        for copy in puts[-2:]:
            copy.start()
    if sizes:
        plan_kernel(*sizes, *list_refs, *plan_refs)
    if back:
        grad_ref[...] = lax.dot_general(left_ref[:, :d], t_buf[:, :d], (((0,), (0,)), ((), ())), preferred_element_type=F32)
    on = link(y_buf, o_b.at[1], CORE)
    for k in chunks:
        to_y[k].wait_recv()
        y_buf[cut[k], :] = unpack(y_wire, k).astype(BF16)
        on[k].start()
        puts.append(copy_in(y_buf.at[cut[k]], o_a.at[1, cut[k]], put.at[2, k]))
        puts[-1].start()
    waited = [to_y] + ([first, second, over] if reduce else [])
    for copies in links:
        for copy in copies:
            if any(copies is w for w in waited):
                copy.wait_send()
            else:
                copy.wait()
    for copy in puts:
        copy.wait()


def complete_blocks(parts, m, reduce, back, ident, sizes=None, lists=(), left=(), n_chunk=4):
    n_blk, wide = parts[0].shape
    d = m.shape[0]
    sem = lambda *s: pltpu.SemaphoreType.DMA(s)
    pair = jax.ShapeDtypeStruct((2, n_blk, wide), BF16)
    extra = plan_shapes(sizes) if sizes else []
    extra += [jax.ShapeDtypeStruct((d, d), F32)] * len(left)
    buf = lambda n, dt: pltpu.VMEM((n, n_blk, wide) if n else (n_blk, wide), dt)
    return pl.pallas_call(
        functools.partial(blocks_kernel, (n_chunk, reduce, back, d, sizes)),
        out_shape=[jax.ShapeDtypeStruct((n_blk, wide), BF16)] + [pair] * 2 + extra,
        in_specs=[any_space] * N_SRC + [in_vmem] * (1 + len(lists) + len(left)),
        out_specs=[any_space] * 3 + [in_vmem] * len(extra),
        scratch_shapes=[buf(2, F32), buf(3, BF16), buf(2, F32)] + [pltpu.VMEM((n_blk // 2, 2 * d), BF16)] * 4 + [
            buf(0, BF16), buf(0, BF16), buf(0, BF16), sem(4, n_chunk), sem(6, n_chunk), sem(6, n_chunk), sem(3, n_chunk)],
        compiler_params=pltpu.CompilerParams(collective_id=ident, has_side_effects=True, vmem_limit_bytes=VMEM_LIMIT),
        cost_estimate=pl.CostEstimate(flops=10 ** 8, bytes_accessed=n_blk * wide * 40, transcendentals=0),
        name=f"complete_blocks_{ident}",
    )(*parts, m, *lists, *left)


def solution(mesh):
    ep_size, dp_size = mesh.shape['ep'], mesh.shape['dp']
    sub = Mesh(mesh.devices.reshape(ep_size, dp_size // 2, 2), ('ep', 'x', 'core'))
    tok_axes = ('x', 'core', 'ep')
    tok_spec = P(tok_axes, None)
    route_spec = P(None, tok_axes, None)
    whole_spec = P(None, None, None)
    expert_spec = P(None, 'ep', None, None)
    flip = [(0, 1), (1, 0)]
    move = lambda v, axis: lax.ppermute(v, axis, flip)
    move_diag = lambda v: lax.ppermute(v, ('ep', 'core'), [(0, 3), (1, 2), (2, 1), (3, 0)])
    fence = lax.optimization_barrier

    def device_step(tokens, d_out, expert_ids, gate_vals, w_mix, w_gate, w_up, w_down):
        n_layers, d = w_mix.shape[0], w_mix.shape[1]
        n_tok = tokens.shape[0]
        top = expert_ids.shape[2]
        n_local = w_gate.shape[1]
        n_exp = n_local * ep_size
        n = n_tok * top
        n_rel = 2 * N_SRC
        wide = cdiv(d, LANES) * LANES
        weights = (jnp.swapaxes(w_gate, 2, 3), jnp.swapaxes(w_up, 2, 3), w_down)
        pad = lambda v: jnp.pad(v, ((0, 0), (0, wide - d)))
        send_three = lambda p: [move(p[1], 'ep'), move(p[2], 'core'), move_diag(p[3])]

        def own_sum(p, got):
            return sum([g.astype(F32) for g in got], p)[:, :d].astype(BF16)

        one = lambda v: v.reshape(1, n_tok, wide)
        pairs = lambda a, b: [(a, 0), (a, 1), (b, 0), (b, 1)]

        one = lambda v: v.reshape(1, n_tok, wide)
        pairs = lambda a, b: [(a, 0), (a, 1), (b, 0), (b, 1)]
        singles = lambda *v: [(one(a), 0) for a in v]

        same = jnp.eye(d, dtype=BF16)
        u0 = (jnp.dot(tokens, pad(same), preferred_element_type=F32)
              + jnp.dot(tokens, pad(w_mix[0]), preferred_element_type=F32)).astype(BF16)
        u0_y, u0_c = move(u0, 'ep'), move(u0, 'core')
        lists = [sorted_list(expert_ids[l], gate_vals[l]) for l in range(n_layers)]
        counts = jnp.sum((expert_ids.transpose(0, 2, 1).reshape(n_layers, n, 1) == jnp.arange(n_exp, dtype=I32)).astype(F32), axis=1)
        packed = jnp.concatenate([jnp.concatenate([v[0] for v in lists] + [v[1] for v in lists]).reshape(-1, LANES),
                                  jnp.pad(counts, ((0, 8 - n_layers), (0, LANES - n_exp)))], axis=0)
        dy = pad(d_out)
        packed, dy = fence((packed, dy))
        shared = share(packed, N_SRC)
        u0_y, u0_c, dy, shared = fence((u0_y, u0_c, dy, shared))
        u0_d = move(u0_y, 'core')
        shared_x = move(shared, 'x')
        dy_y, dy_x = move(dy, 'ep'), move(dy, 'x')
        sizes = (n_layers, n_local, n_tok, n // LANES)
        routes = plan(shared, shared, sizes)
        u0_half = singles(u0, u0_y, u0_c, u0_d)
        add = lambda a, b: a.astype(F32) + b.astype(F32)
        to_chips = lambda v: [move(v, 'ep'), move(v, 'x'), lax.ppermute(v, ('ep', 'x'), [(0, 3), (1, 2), (2, 1), (3, 0)])]
        of_chips = lambda v, t: (add(v, t[0]) + add(t[1], t[2])).astype(BF16)
        piece = first_piece(n_local // 2)
        rows = lax.slice_in_dim(routes[0], ROW_PARTNER * LANES, ROW_PARTNER * LANES + n_local // 2)
        *part, ab0, xu0 = run_experts(routes, 0, u0_half, None, weights, None, None, True, True, p_f32=True)
        dy_y, dy_x, shared_x, part = fence((dy_y, dy_x, shared_x, part))
        dy_c, dy_d, dy_xy, dy_xc = move(dy, 'core'), move(dy_y, 'core'), move(dy_y, 'x'), move(dy_x, 'core')
        y0, u1_a, u1_b, *routes_x = complete_blocks(part, w_mix[1], True, False, 1, sizes, (shared, shared_x))
        routes_x = flat(*routes_x)
        dy_c, dy_d, dy_xy, dy_xc, u0_p, u0_q, y0, u1_a, u1_b = fence(
            (dy_c, dy_d, dy_xy, dy_xc, u0, u0_y, y0, u1_a, u1_b))
        dy_xd = move(dy_xy, 'core')
        u1_xa = move(u1_a, 'x')
        out = run_experts(routes, 1, pairs(u1_a, u1_b), singles(dy, dy_y, dy_c, dy_d), weights, None, None, True, True)
        u1_xa, dy_xd, u0_p, u0_q, out = fence((u1_xa, dy_xd, u0_p, u0_q, out))
        y_part, du_part, g1 = out[:4], out[4:8], out[8]
        u1_xb = move(u1_xa, 'core')
        got = send_three(du_part)
        u0_x, u0_xy = move(u0_p, 'x'), move(u0_q, 'x')
        out = run_experts(routes_x, 1, pairs(u1_xa, u1_xb), singles(dy_x, dy_xy, dy_xc, dy_xd), weights, g1, None,
                          False, False)
        got, u0_x, u0_xy, out = fence((got, u0_x, u0_xy, out))
        *finals, sent_a, sent_b = out
        got1 = [move(sent_a, 'core'), move(sent_b, 'core')]
        du1, dx_a, dx_b, g_mix1 = complete_blocks([du_part[0], *got], w_mix[1], False, True, 2, left=(y0,))
        tx = lambda x, du: jnp.einsum('td,te->de', x, du, preferred_element_type=F32)
        dx_a, y_part, got1, u0_x, u0_xy, g_mix1 = fence((dx_a, y_part, got1, u0_x, u0_xy, g_mix1))
        dx_xa = move(dx_a, 'x')
        part1 = g_mix1.astype(BF16)
        theirs1 = to_chips(part1)
        got_y = send_three(y_part)
        u0_xc, u0_xd = move(u0_x, 'core'), move(u0_xy, 'core')
        out = run_experts(routes, 0, None, pairs(dx_a, dx_b), weights, None, finals, False, True, got=got1, kept=(ab0, xu0))
        dx_xa, got_y, u0_xc, u0_xd, theirs1, out = fence((dx_xa, got_y, u0_xc, u0_xd, theirs1, out))
        du_part, g0, finals = out[:4], out[4], out[5:]
        dx_xb = move(dx_xa, 'core')
        got = send_three(du_part)
        part1 = of_chips(part1, theirs1)
        theirs1 = move(part1, 'core')
        du_part, dx_xb, part1 = fence((du_part, dx_xb, part1))
        out = run_experts(routes_x, 0, singles(u0_x, u0_xy, u0_xc, u0_xd), pairs(dx_xa, dx_xb), weights, g0, finals,
                          False, False)
        got, theirs1, got_y, y_own, rows, out = fence((got, theirs1, got_y, y_part[0], rows, out))
        *finals, sent_a, sent_b = out
        got_a, got_b = move(sent_a, 'core'), move(sent_b, 'core')
        du0 = own_sum(du_part[0], got)
        part0 = tx(tokens, du0).astype(BF16)
        theirs0 = to_chips(part0)
        turned = lambda v, w: jnp.einsum('te,de->dt', v, w, preferred_element_type=F32)
        dx0 = (turned(du0, same) + turned(du0, w_mix[0])).astype(BF16)
        y1 = turned(own_sum(y_own, got_y), same).astype(BF16)
        dx0, y1, got_a, finals = fence((dx0, y1, got_a, finals))
        finals = place(rows, 0, 0, got_a, finals)
        dx0, got_b, finals = fence((dx0, got_b, finals))
        finals = place(rows, piece, 0, got_b, finals)
        theirs0, finals = fence((theirs0, finals))
        total0 = of_chips(part0, theirs0)
        g_mix = jnp.stack([add(total0, move(total0, 'core')), add(part1, theirs1)]).astype(BF16)
        return (y1.T, dx0.T, g_mix, jnp.swapaxes(finals[0], 2, 3), jnp.swapaxes(finals[1], 2, 3), finals[2])

    return jax.shard_map(device_step, mesh=sub,
                         in_specs=(tok_spec, tok_spec, route_spec, route_spec, whole_spec,
                                   expert_spec, expert_spec, expert_spec),
                         out_specs=(tok_spec, tok_spec, whole_spec, expert_spec, expert_spec, expert_spec),
                         check_vma=False)
```

```python
import functools

import jax
import jax.numpy as jnp
from jax import lax
from jax.experimental import pallas as pl
from jax.experimental.pallas import tpu as pltpu
from jax.sharding import Mesh, PartitionSpec as P

F32, BF16, I32 = jnp.float32, jnp.bfloat16, jnp.int32
MESH = pl.DeviceIdType.MESH
ROWS = 384
GRP = 8
PITCH = 9
DEPTH = 3
FULL = 8
HALF = 4
CAP_FACTOR = 3
LANES = 128
N_SRC = 4
Y, CORE, X = 1, 2, 4
VMEM_LIMIT = 62 * 1024 * 1024
PER_TILE = ROWS // GRP
ROW_BOUND, ROW_GOFF, ROW_EXPERT, ROW_PARTNER, TAB_ROWS = 32, 33, 34, 35, 40
SLOT_GROUPS = 256


def cdiv(a, b):
    return (a + b - 1) // b


def first_piece(n_exp):
    return n_exp * 5 // 8


def spans(d):
    return [(LANES * j, min(LANES, d - LANES * j)) for j in range(cdiv(d, LANES))]


any_space = pl.BlockSpec(memory_space=pl.ANY)
in_vmem = pl.BlockSpec(memory_space=pltpu.VMEM)


def sorted_list(expert_ids, gate_vals):
    n_tok, top = expert_ids.shape
    n = n_tok * top
    keys = expert_ids.T.reshape(n) * n + jnp.arange(n, dtype=I32)
    keys, gates = lax.sort((keys, gate_vals.T.reshape(n)), num_keys=1, is_stable=False)
    return (keys % n_tok).astype(F32), gates


def plan_kernel(n_layers, n_local, n_tok, list_rows, deal_ref, all_ref, tab_ref, idx_ref, gate_ref):
    n_mine = n_local // 2
    core, ep = lax.axis_index('core'), lax.axis_index('ep')
    list_len = list_rows * LANES
    lane = lambda n: lax.broadcasted_iota(I32, (n, LANES), 1).astype(F32)
    sub = lambda n: lax.broadcasted_iota(I32, (n, LANES), 0).astype(F32)
    over_lanes = lambda v: jnp.sum(v, axis=1, keepdims=True)
    over_subs = lambda v: jnp.sum(v, axis=0, keepdims=True)
    l16, s16 = lane(n_mine), sub(n_mine)
    groups = lambda c: jnp.floor((c + (GRP - 0.5)) * (1.0 / GRP))
    for l in range(n_layers):
        cnt = all_ref[:, 2 * n_layers * list_rows + l, :]
        ends = cnt
        step = 1
        while step < 2 * n_local:
            ends = ends + jnp.where(lane(N_SRC) >= step, pltpu.roll(ends, step, 1), 0.0)
            step *= 2
        starts = ends - cnt
        second = (ep > 0)
        local = lambda v: jnp.where(lane(N_SRC) < n_local, jnp.where(second, pltpu.roll(v, LANES - n_local, 1), v), 0.0)
        cnt, starts = local(cnt), local(starts)
        tiles = jnp.floor((over_subs(groups(local(deal_ref[:, 2 * n_layers * list_rows + l, :]))) + (PER_TILE - 0.5))
                          * (1.0 / PER_TILE))
        load = jnp.where(lane(1) < n_local, jnp.maximum(1.0, tiles), -1.0)
        wide = jnp.broadcast_to(load, (n_local, LANES))
        col = over_lanes(jnp.where(lane(n_local) == sub(n_local), wide, 0.0))
        ahead = (col > wide) | ((col == wide) & (sub(n_local) < lane(n_local)))
        rank = over_subs(jnp.where(ahead, 1.0, 0.0))
        odd = s16 - 2.0 * jnp.floor(s16 * 0.5 + 0.25)
        flip = jnp.where(core > 0, 1.0 - odd, odd)
        dealt = lambda f: (jnp.broadcast_to(rank, (n_mine, LANES)) == 2.0 * s16 + f) & (l16 < n_local)
        pick = dealt(flip)
        choose = lambda p, row: over_lanes(jnp.where(p, jnp.broadcast_to(row, (n_mine, LANES)), 0.0))
        mine = lambda row: choose(pick, row)
        as_row = lambda c: over_subs(jnp.where(l16 == s16, c, 0.0))
        experts = as_row(mine(lane(1)))
        partner = as_row(choose(dealt(1.0 - flip), lane(1)))
        at = l * TAB_ROWS
        off = jnp.zeros((n_mine, 1), F32)
        pos = [jnp.zeros((n_mine, LANES), F32) for _ in range(SLOT_GROUPS // LANES)]
        for s in range(N_SRC):
            c, st = mine(cnt[s:s + 1]), mine(starts[s:s + 1]) + float(s * list_len)
            ng = groups(c)
            for i in range(len(pos)):
                rel = l16 + float(LANES * i) - off
                code = (st + GRP * rel) * 16.0 + jnp.minimum(float(GRP), c - GRP * rel)
                pos[i] = jnp.where((rel >= 0) & (rel < ng), code, pos[i])
            off = off + ng
        for i in range(len(pos)):
            tab_ref[pl.ds(at + i, n_mine, stride=len(pos)), :] = pos[i].astype(I32)
        n_tiles = jnp.maximum(1.0, jnp.floor((off + (PER_TILE - 0.5)) * (1.0 / PER_TILE)))
        bounds = over_subs(jnp.where(s16 < l16, n_tiles, 0.0))
        before = over_lanes(jnp.where(l16 == s16, jnp.broadcast_to(bounds, (n_mine, LANES)), 0.0))
        t = jnp.minimum(l16, over_subs(jnp.broadcast_to(n_tiles, (n_mine, LANES))) - 1.0)
        inside = (t >= before) & (t < before + n_tiles)
        goff = over_subs(jnp.where(inside, s16 * float(SLOT_GROUPS) + (t - before) * float(PER_TILE), 0.0))
        rows = [(ROW_BOUND, bounds), (ROW_GOFF, goff), (ROW_EXPERT, experts), (ROW_PARTNER, partner)]
        for row, value in rows:
            tab_ref[at + row:at + row + 1, :] = value.astype(I32)
    for l in range(n_layers):
        pad = l * (N_SRC * list_rows + 8) + N_SRC * list_rows
        gate_ref[pad:pad + 8, :] = jnp.zeros((8, LANES), F32)
        for s in range(N_SRC):
            to = (l * N_SRC + s) * list_rows
            toks = all_ref[s, l * list_rows:(l + 1) * list_rows, :]
            idx_ref[to:to + list_rows, :] = ((toks + float(s * n_tok)) * float(PITCH)).astype(I32)
            to = l * (N_SRC * list_rows + 8) + s * list_rows
            gate_ref[to:to + list_rows, :] = all_ref[s, (n_layers + l) * list_rows:(n_layers + l + 1) * list_rows, :]


def plan_shapes(sizes):
    n_layers, _, _, list_rows = sizes
    rows = (n_layers * TAB_ROWS, n_layers * N_SRC * list_rows, n_layers * (N_SRC * list_rows + 8))
    return [jax.ShapeDtypeStruct((n, LANES), dt) for n, dt in zip(rows, (I32, I32, F32))]


def flat(tab, idx, gates):
    return tab.reshape(-1), idx.reshape(-1), gates


def plan(deal, shared, sizes):
    return flat(*pl.pallas_call(
        functools.partial(plan_kernel, *sizes),
        out_shape=plan_shapes(sizes),
        in_specs=[in_vmem] * 2, out_specs=[in_vmem] * 3,
        cost_estimate=pl.CostEstimate(flops=10 ** 7, bytes_accessed=10 ** 6, transcendentals=0),
        name="plan",
    )(deal, shared))


def expert_kernel(cfg, *refs):
    fwd, bwd, own, layer, n_blk, d, ff, n_exp, picks, row_id, list_len, p_f32, n_alias, got_layer = cfg
    save, load = fwd and not bwd, own and bwd and not fwd
    refs = list(refs)
    take = lambda n: [refs.pop(0) for _ in range(n)]
    tab_hbm, idx_hbm, gate_hbm = take(3)
    u_pieces = take(N_SRC) if not load else []
    dy_pieces = take(N_SRC) if bwd else []
    wg_hbm, wu_hbm, wd_hbm = take(3)
    ab_hbm, xu_hbm = take(2) if load else (None, None)
    prev = take(1)[0] if bwd and not own else None
    got = take(2) if got_layer is not None else None
    take(n_alias)
    y_outs = take(N_SRC) if fwd else []
    du_outs = take(N_SRC) if bwd and own else []
    grad = take(1)[0] if bwd and own else None
    finals = take(3) if bwd and not own or got_layer is not None else None
    sent = take(2) if bwd and not own else None
    ab_hbm, xu_hbm = take(2) if save else (ab_hbm, xu_hbm)
    tab_ref, idx, gate_ref, land, table, gat = take(6)
    acc, row_ref = take(2) if own else (None, None)
    gu_ref, wd_ref, g_ref, x_u = take(4)
    x_c = take(1)[0] if bwd else None
    ab_ref = take(1)[0]
    dh_ref = take(1)[0] if bwd else None
    h_ref = take(1)[0]
    dab_ref, sums = take(2) if bwd else (None, None)
    keep_buf = take(1)[0] if bwd and not own else None
    got_buf = take(1)[0] if got is not None else None
    list_sem, land_sem, w_sem = take(3)
    sum_sem = take(1)[0] if bwd else None
    keep_sem = take(1)[0] if bwd and not own else None
    read_sem, write_sem = take(2) if got is not None else (None, None)
    stage_f, out_sem = take(2) if own else (None, None)
    ab_sem, xu_sem = take(2) if save or load else (None, None)

    split = first_piece(n_exp)
    copy = pltpu.make_async_copy
    cols = spans(d)
    lo = ff // 256 * 256
    hi = ff - lo
    dot = functools.partial(lax.dot_general, preferred_element_type=F32)
    nn = (((1,), (0,)), ((), ()))
    nt = (((1,), (1,)), ((), ()))
    tn = (((0,), (0,)), ((), ()))
    al = pl.multiple_of
    n_row = N_SRC * n_blk
    glane = lax.broadcasted_iota(I32, (GRP, LANES), 1)
    gsub = lax.broadcasted_iota(I32, (GRP, LANES), 0)

    def row_at(r):
        return pl.ds(r * PITCH, FULL)

    def codes_of(tile):
        at = ROW_GOFF * LANES + tile
        if own and bwd:
            return lambda q: tab_ref[tab_ref[at] + q]
        view = tab_ref.at[pl.ds(tab_ref[at], PER_TILE)]
        return lambda q: view[q]

    def gather(codes, q):
        ids = idx.at[pl.ds(codes(q) >> 4, GRP)]
        for k in range(GRP):
            gat[row_at(q * GRP + k), :] = table[pl.ds(ids[k], FULL), :]

    def gate_column(code):
        pos = code >> 4
        row, shift = pos >> 7, pos & (LANES - 1)
        want = glane == gsub + shift
        over = glane == gsub + (shift - LANES)
        here = gate_ref[pl.ds(row, GRP, stride=0), :]
        there = gate_ref[pl.ds(row + 1, GRP, stride=0), :]
        v = jnp.where(want, here, jnp.where(over, there, 0.0))
        return jnp.where(gsub < (code & 15), jnp.sum(v, axis=1, keepdims=True), 0.0)

    def scatter(codes, q):
        ids = idx.at[pl.ds(codes(q) >> 4, GRP)]
        new = []
        for k in range(GRP):
            at = pl.ds(ids[k], FULL)
            new.append((at, acc[at, :] + row_ref[row_at(q * GRP + k), :]))
        for at, value in reversed(new):
            acc[at, :] = value

    def keep_ab(t):
        ends = (ab_ref.at[t & 1], ab_hbm.at[t])
        return copy(*(ends if save else ends[::-1]), ab_sem.at[t & 1])

    def keep_xu(t):
        ends = (x_u.at[t & 1], xu_hbm.at[t])
        return copy(*(ends if save else ends[::-1]), xu_sem.at[t & 1])

    def of(ref, t):
        return ref.at[t & 1] if save or load else ref

    def convert(codes, t):
        for q in range(0, PER_TILE, 2):
            part = []
            for p in (q, q + 1):
                code = codes(p)
                rows = [gat[pl.ds(GRP * PITCH * p + j, GRP, stride=PITCH), :]
                        for j in range(HALF if load else 0, FULL if bwd else HALF)]
                real = gsub < (code & 15)
                gate = gate_column(code)
                g_ref[GRP * p:GRP * (p + 1), :] = gate
                us, dys = ([], rows) if load else (rows[:HALF], rows[HALF:])
                part.append([jnp.where(real, v, 0.0) for v in us] + [v * gate for v in dys])
            at = slice(GRP * q, GRP * (q + 2))
            for x, o in ((None if load else of(x_u, t), 0), (x_c, 0 if load else HALF)):
                if x is None:
                    continue
                for j, (c, w) in enumerate(cols):
                    both = jnp.concatenate([part[0][o + j], part[1][o + j]], axis=0)
                    x[at, c:c + w] = both[:, :w].astype(BF16)

    def put_rows(o, value, s0):
        value = value.astype(BF16).astype(F32)
        n = value.shape[0]
        for j, (c, w) in enumerate(cols):
            row_ref[pl.ds(PITCH * s0 + o + j, n, stride=PITCH), 0:w] = value[:, c:c + w] * g_ref[s0:s0 + n, 0:w]

    low = lax.broadcasted_iota(I32, (16, 2 * hi), 1) < hi

    def middle(a, b, dh):
        sig = 0.5 * jnp.tanh(0.5 * a) + 0.5
        act = a * sig
        h = act * b
        if dh is None:
            return h, None, None
        slope = sig * (1.0 + a * (1.0 - sig))
        return h, dh * b * slope, dh * act

    def weights(e, slot):
        at = (layer, tab_ref[ROW_EXPERT * LANES + e])
        moves = []
        for i, w in enumerate((wg_hbm, wu_hbm)):
            moves.append((w.at[at + (pl.ds(0, lo),)], gu_ref.at[slot, pl.ds(i * lo, lo)]))
            moves.append((w.at[at + (pl.ds(lo, hi),)], gu_ref.at[slot, pl.ds(2 * lo + i * hi, hi)]))
        moves.append((wd_hbm.at[at], wd_ref.at[slot]))
        return [copy(a, b, w_sem.at[slot, i]) for i, (a, b) in enumerate(moves)]

    def sums_in(e, slot):
        return copy(prev.at[e], sums.at[slot], sum_sem.at[slot])

    def sums_out(e, slot):
        return copy(sums.at[slot], grad.at[e], sum_sem.at[slot])

    def keeps(e, slot):
        at = (layer, tab_ref[ROW_EXPERT * LANES + e])
        return [copy(keep_buf.at[slot, i], finals[i].at[at], keep_sem.at[slot, i]) for i in range(3)]

    def send(e, slot, part):
        return copy(keep_buf.at[slot], sent[part].at[e - part * split], keep_sem.at[slot, 3])

    def read(e, slot, part=0):
        return copy(got[part].at[e - part * split], got_buf.at[slot], read_sem.at[slot])

    def writes(e, slot):
        to = tab_ref[TAB_ROWS * LANES + e]
        return [copy(got_buf.at[slot, i], finals[i].at[got_layer, to], write_sem.at[slot, i]) for i in range(3)]

    def start(moves):
        for m in moves:
            m.start()

    def wait(moves):
        for m in moves:
            m.wait()

    n_tab = TAB_ROWS * LANES
    lists = [copy(tab_hbm.at[pl.ds(row_id * n_tab, n_tab)], tab_ref.at[pl.ds(0, n_tab)], list_sem.at[0]),
             copy(idx_hbm.at[pl.ds(row_id * N_SRC * list_len, N_SRC * list_len)], idx.at[pl.ds(0, N_SRC * list_len)],
                  list_sem.at[1]),
             copy(gate_hbm.at[pl.ds(row_id * gate_ref.shape[0], gate_ref.shape[0])], gate_ref, list_sem.at[2])]
    if got is not None:
        at = (got_layer * TAB_ROWS + ROW_PARTNER) * LANES
        lists.append(copy(tab_hbm.at[pl.ds(at, LANES)], tab_ref.at[pl.ds(n_tab, LANES)], list_sem.at[3]))
    start(lists)
    pieces = []
    for s in range(N_SRC):
        if not load:
            pieces.append((u_pieces[s], picks[0][s], s, 0, fwd))
        if bwd:
            pieces.append((dy_pieces[s], picks[1][s], s, HALF, own))
    lands = [copy(ref.at[pick], land.at[i % N_SRC], land_sem.at[i % N_SRC]) for i, (ref, pick, *_) in enumerate(pieces)]
    start(lands[:N_SRC])
    lists[0].wait()
    for e in range(DEPTH - 1):
        start(weights(e, e))
        if bwd and not own:
            sums_in(e, e).start()
    if got is not None:
        lists[3].wait()
        read(0, 0).start()
    if own:
        def clear(c, _):
            for k in range(4):
                acc[pl.ds(al(c * 1152 + 288 * k, 8), 288), :] = jnp.zeros((288, LANES), F32)
            return 0

        lax.fori_loop(0, acc.shape[0] // 1152, clear, 0)
        row_ref[...] = jnp.zeros(row_ref.shape, F32)
    rows = 256
    for i, (_, _, s, o, seed) in enumerate(pieces):
        lands[i].wait()

        def fill(c, _, i=i, o=o, seed=seed, s=s):
            r = al(c * rows, rows)
            for j in range(HALF):
                vals = land[i % N_SRC, pl.ds(r, rows), LANES * j:LANES * (j + 1)].astype(F32)
                to = pl.ds(PITCH * (s * n_blk + r) + o + j, rows, stride=PITCH)
                table[to, :] = vals
                if seed and s == 0:
                    acc[to, :] = vals
            return 0

        lax.fori_loop(0, n_blk // rows, fill, 0)
        if i + N_SRC < len(pieces):
            lands[i + N_SRC].start()
    wait(lists[1:3])
    for k in range(GRP):
        idx[N_SRC * list_len + k] = 0

    def first(q, _):
        gather(begin, 2 * q)
        gather(begin, 2 * q + 1)
        return 0

    begin = codes_of(0)
    lax.fori_loop(0, PER_TILE // 2, first, 0)
    convert(begin, 0)
    if save:
        keep_xu(0).start()
    if load:
        keep_ab(0).start()
        keep_xu(0).start()

    def expert(e, _):
        slot = e & 1
        deep = lax.rem(e, DEPTH)
        sum_slot = slot if own else deep
        wait(weights(e, deep))
        if bwd and not own:
            sums_in(e, deep).wait()
        if got is not None:
            read(0, slot).wait()
            start(writes(e, slot))

            @pl.when((e > 0) & (e < n_exp - 1))
            def _():
                wait(writes(e - 1, 1 - slot))

        @pl.when(e < n_exp - (DEPTH - 1))
        def _():
            ahead = lax.rem(e + DEPTH - 1, DEPTH)
            start(weights(e + DEPTH - 1, ahead))
            if bwd and not own:
                sums_in(e + DEPTH - 1, ahead).start()

        @pl.when(e < n_exp - 1)
        def _():
            if got is not None:
                for part in range(2):
                    @pl.when((e + 1 >= split) if part else (e + 1 < split))
                    def _(part=part):
                        read(e + 1, 1 - slot, part).start()

        if bwd and own:
            @pl.when(e > 1)
            def _():
                sums_out(e - 2, slot).wait()

            sums[slot] = jnp.zeros(sums.shape[1:], F32)

        def tile(t, _):
            if save:
                @pl.when(t > 1)
                def _():
                    keep_ab(t - 2).wait()

                @pl.when(t > 0)
                def _():
                    keep_xu(t - 1).wait()
            if load:
                keep_ab(t).wait()
                keep_xu(t).wait()
                keep_ab(t + 1).start()
                keep_xu(t + 1).start()
            ab, xu = of(ab_ref, t), of(x_u, t)
            before, after = codes_of(jnp.maximum(t - 1, 0)), codes_of(t + 1)
            for q in range(PER_TILE):
                if own:
                    scatter(before, q)
                gather(after, q)
            front = ROWS if own and bwd else ROWS // 2
            for s0 in range(0, ROWS, front):
                sl = slice(s0, s0 + front)
                if not load:
                    ab[sl, :] = dot(xu[sl, :], gu_ref[deep], nt)
                if bwd:
                    dh_ref[sl, :] = dot(x_c[sl, :], wd_ref[deep], nt)
            for r in range(0, ROWS, 16):
                rows = slice(r, r + 16)
                for c in range(0, lo, LANES):
                    h, da, db = middle(ab[rows, c:c + LANES], ab[rows, lo + c:lo + c + LANES],
                                       dh_ref[rows, c:c + LANES] if bwd else None)
                    h_ref[rows, c:c + LANES] = h.astype(BF16)
                    if bwd:
                        dab_ref[rows, c:c + LANES] = da.astype(BF16)
                        dab_ref[rows, lo + c:lo + c + LANES] = db.astype(BF16)
                a = ab[rows, 2 * lo:]
                b = pltpu.roll(a, hi, 1)
                dh = dh_ref[rows, lo:] if bwd else None
                if bwd:
                    dh = jnp.concatenate([dh, dh], axis=1)
                h, da, db = middle(a, b, dh)
                h_ref[rows, lo:] = h[:, :hi].astype(BF16)
                if bwd:
                    dab_ref[rows, 2 * lo:] = jnp.where(low, da, pltpu.roll(db, hi, 1)).astype(BF16)
            half = ROWS // 2
            for s0 in range(0, ROWS, half):
                sl = slice(s0, s0 + half)
                if fwd:
                    put_rows(0, dot(h_ref[sl, :], wd_ref[deep], nn), s0)
                if bwd and own:
                    put_rows(HALF, dot(dab_ref[sl, :], gu_ref[deep], nn), s0)
            if bwd:
                view = sums.at[sum_slot]
                view[0:2 * ff, :] += dot(dab_ref[...], xu[...], tn)
                view[2 * ff:, :] += dot(h_ref[...], x_c[...], tn)
            convert(after, t + 1)
            if save:
                keep_ab(t).start()
                keep_xu(t + 1).start()
            return 0

        lax.fori_loop(tab_ref[ROW_BOUND * LANES + e], tab_ref[ROW_BOUND * LANES + e + 1], tile, 0)
        if bwd and own:
            sums_out(e, slot).start()
        if bwd and not own:
            @pl.when(e > 1)
            def _():
                wait(keeps(e - 2, slot) + [send(0, slot, 0)])

            for i in range(2):
                keep_buf[slot, i, 0:lo, :] = sums[deep, i * lo:(i + 1) * lo, :].astype(BF16)
                keep_buf[slot, i, lo:, :] = sums[deep, 2 * lo + i * hi:2 * lo + (i + 1) * hi, :].astype(BF16)
            keep_buf[slot, 2] = sums[deep, 2 * ff:, :].astype(BF16)
            start(keeps(e, slot))
            for part in range(2):
                @pl.when((e >= split) if part else (e < split))
                def _(part=part):
                    send(e, slot, part).start()
        return 0

    lax.fori_loop(0, n_exp, expert, 0)
    ends = ((n_exp - 2, (n_exp - 2) % 2), (n_exp - 1, (n_exp - 1) % 2))
    n_tiles = tab_ref[ROW_BOUND * LANES + n_exp]
    if save:
        wait([keep_ab(n_tiles - 2), keep_ab(n_tiles - 1), keep_xu(n_tiles - 1)])
    if save or load:
        keep_xu(n_tiles).wait()
    if load:
        keep_ab(n_tiles).wait()
    if own:
        end = codes_of(tab_ref[ROW_BOUND * LANES + n_exp] - 1)
        lax.fori_loop(0, PER_TILE, lambda q, _: (scatter(end, q), 0)[1], 0)
        flights = {}
        for o, out in ((HALF, du_outs), (0, y_outs)):
            for s in range(N_SRC if out else 0):
                wide = s == 0 or p_f32
                stage = stage_f.at[s] if wide else land.at[s]
                if s in flights:
                    flights[s].wait()

                def fetch(c, _, stage=stage, s=s, o=o):
                    r = al(c * rows, rows)
                    for j in range(HALF):
                        at = pl.ds(PITCH * (s * n_blk + r) + o + j, rows, stride=PITCH)
                        stage[pl.ds(r, rows), LANES * j:LANES * (j + 1)] = acc[at, :].astype(stage.dtype)
                    return 0

                lax.fori_loop(0, n_blk // rows, fetch, 0)
                flights[s] = copy(stage, out[s], out_sem.at[s])
                flights[s].start()
        wait(flights.values())
        if bwd:
            for e, slot in ends:
                sums_out(e, slot).wait()
    else:
        for e, slot in ends:
            wait(keeps(e, slot) + [send(0, slot, 0)])
    if got is not None:
        for e, slot in ends:
            wait(writes(e, slot))


def run_experts(routes, layer, u, dy, weights, prev, finals, fwd, own, p_f32=False, got=None, kept=None):
    tab, idx, gates = routes
    bwd = dy is not None
    wg, wu, wd = weights
    save, load = fwd and not bwd, kept is not None
    n_blk, wide = (dy or u)[0][0].shape[-2:]
    n_layers, n_local, ff, d = wd.shape
    n_exp = n_local // 2
    row_id = layer
    list_len = idx.shape[0] // (n_layers * N_SRC)

    arrays = lambda pieces: [v for v, _ in pieces]
    operands = [tab, idx, gates] + ([] if load else arrays(u)) + (arrays(dy) if bwd else []) + [wg, wu, wd] + list(kept or ())
    out_shape, aliases = [], {}
    for use in (fwd, bwd and own):
        if use:
            out_shape += [jax.ShapeDtypeStruct((n_blk, wide), F32 if s == 0 or p_f32 else BF16) for s in range(N_SRC)]
    if bwd and own:
        out_shape.append(jax.ShapeDtypeStruct((n_exp, 3 * ff, d), F32))
    if bwd and not own:
        operands.append(prev)
    if got is not None:
        operands += got
    for i, f in enumerate(finals or ()):
        aliases[len(operands)] = len(out_shape) + i
        operands.append(f)
    if bwd and not own or finals:
        out_shape += [jax.ShapeDtypeStruct((n_layers, n_local, ff, d), BF16)] * 3
    if bwd and not own:
        out_shape += [jax.ShapeDtypeStruct((n, 3, ff, d), BF16) for n in (first_piece(n_exp), n_exp - first_piece(n_exp))]
    if save:
        most = n_exp * (SLOT_GROUPS // PER_TILE) + 2
        out_shape += [jax.ShapeDtypeStruct((most, ROWS, 2 * ff), F32), jax.ShapeDtypeStruct((most, ROWS, d), BF16)]
    sem = lambda *s: pltpu.SemaphoreType.DMA(s)
    mid = lambda n, dt: pltpu.VMEM((ROWS, n), dt)
    twin = lambda n, dt: pltpu.VMEM((2, ROWS, n), dt) if save or load else mid(n, dt)
    table, rows = pltpu.VMEM((PITCH * N_SRC * n_blk, LANES), F32), pltpu.VMEM((PITCH * ROWS, LANES), F32)
    scratch = [pltpu.SMEM(((TAB_ROWS + 1) * LANES,), I32), pltpu.SMEM((N_SRC * list_len + LANES,), I32),
               pltpu.VMEM((N_SRC * list_len // LANES + 8, LANES), F32), pltpu.VMEM((N_SRC, n_blk, wide), BF16)]
    scratch += [table, rows] * (1 + own)
    scratch += [pltpu.VMEM((DEPTH, 2 * ff, d), BF16), pltpu.VMEM((DEPTH, ff, d), BF16), mid(LANES, F32)]
    scratch += [twin(d, BF16)] + [mid(d, BF16)] * bwd + [twin(2 * ff, F32)] + [mid(ff, F32)] * bwd + [mid(ff, BF16)]
    scratch += [mid(2 * ff, BF16), pltpu.VMEM((2 if own else DEPTH, 3 * ff, d), F32)] * bwd
    if bwd and not own:
        scratch.append(pltpu.VMEM((2, 3, ff, d), BF16))
    if got is not None:
        scratch.append(pltpu.VMEM((2, 3, ff, d), BF16))
    scratch += [sem(4), sem(N_SRC), sem(DEPTH, 5)] + [sem(DEPTH)] * bwd
    if bwd and not own:
        scratch.append(sem(2, 4))
    if got is not None:
        scratch += [sem(2), sem(2, 3)]
    if own:
        scratch += [pltpu.VMEM((N_SRC if p_f32 else 1, n_blk, wide), F32), sem(N_SRC)]
    if save or load:
        scratch += [sem(2), sem(2)]
    passes = 2 + fwd + bwd * (4 + 2 * own)
    flops = 2 * d * ff * passes * n_blk * N_SRC * 2
    hoist = 1300 if not own else 640 if load else 750 if save else 950
    picks = [[i for _, i in u] if u else None, [i for _, i in dy] if bwd else None]
    cfg = (fwd, bwd, own, layer, n_blk, d, ff, n_exp, picks, row_id, list_len, p_f32, len(aliases),
           None if got is None else 1 - layer)
    return pl.pallas_call(
        functools.partial(expert_kernel, cfg),
        out_shape=out_shape,
        in_specs=[any_space] * len(operands),
        out_specs=[any_space] * len(out_shape),
        scratch_shapes=scratch,
        input_output_aliases=aliases,
        compiler_params=pltpu.CompilerParams(
            vmem_limit_bytes=VMEM_LIMIT),
        cost_estimate=pl.CostEstimate(flops=flops, bytes_accessed=3 * 2 * n_exp * d * ff, transcendentals=0),
        name=f"experts_{'f' if fwd else ''}{'b' if bwd else ''}_{'own' if own else 'other'}_{layer}",
    )(*operands)


def place_kernel(layer, n_exp, at, tab_hbm, got_ref, *refs):
    outs, (tab_ref, buf, tab_sem, in_sem, out_sem) = refs[3:6], refs[6:]
    table = pltpu.make_async_copy(tab_hbm.at[pl.ds((layer * TAB_ROWS + ROW_PARTNER) * LANES, LANES)], tab_ref, tab_sem)
    table.start()
    reads = [pltpu.make_async_copy(got_ref.at[i], buf.at[i], in_sem.at[i]) for i in range(n_exp)]
    for read in reads:
        read.start()
    writes = []
    table.wait()
    for i, read in enumerate(reads):
        read.wait()
        e = tab_ref[at + i]
        for k, out in enumerate(outs):
            writes.append(pltpu.make_async_copy(buf.at[i, k], out.at[layer, e], out_sem.at[i, k]))
            writes[-1].start()
    for write in writes:
        write.wait()


def place(tab, at, layer, got, finals):
    n_exp = got.shape[0]
    return pl.pallas_call(
        functools.partial(place_kernel, layer, n_exp, at),
        out_shape=[jax.ShapeDtypeStruct(f.shape, f.dtype) for f in finals],
        in_specs=[any_space] * 5, out_specs=[any_space] * 3,
        scratch_shapes=[pltpu.SMEM((LANES,), I32), pltpu.VMEM(got.shape, got.dtype), pltpu.SemaphoreType.DMA,
                        pltpu.SemaphoreType.DMA((n_exp,)), pltpu.SemaphoreType.DMA((n_exp, 3))],
        input_output_aliases={2: 0, 3: 1, 4: 2},
        compiler_params=pltpu.CompilerParams(vmem_limit_bytes=VMEM_LIMIT),
        cost_estimate=pl.CostEstimate(flops=0, bytes_accessed=4 * got.size, transcendentals=0),
        name=f"place_{layer}",
    )(tab, got, *finals)


def peer(rel):
    return {name: (lax.axis_index(name) + ((rel >> bit) & 1)) % 2 for bit, name in enumerate(("ep", "core", "x"))}


def meet(rels):
    barrier = pltpu.get_barrier_semaphore()
    for rel in rels:
        pl.semaphore_signal(barrier, inc=1, device_id=peer(rel), device_id_type=MESH)
    pl.semaphore_wait(barrier, len(rels))


def remote(src, dst, send, recv, rel):
    return pltpu.make_async_remote_copy(src_ref=src, dst_ref=dst, send_sem=send, recv_sem=recv,
                                        device_id=peer(rel), device_id_type=MESH)


def share_kernel(n_rel, mine_ref, all_ref, send_sem, recv_sem):
    meet(range(1, n_rel))
    copies = [remote(mine_ref, all_ref.at[rel], send_sem.at[rel], recv_sem.at[rel], rel) for rel in range(1, n_rel)]
    for copy in copies:
        copy.start()
    all_ref[0] = mine_ref[...]
    for copy in copies:
        copy.wait()


def share(mine, n_rel):
    return pl.pallas_call(
        functools.partial(share_kernel, n_rel),
        out_shape=jax.ShapeDtypeStruct((n_rel,) + mine.shape, mine.dtype),
        in_specs=[in_vmem],
        out_specs=in_vmem,
        scratch_shapes=[pltpu.SemaphoreType.DMA((n_rel,)), pltpu.SemaphoreType.DMA((n_rel,))],
        compiler_params=pltpu.CompilerParams(collective_id=0, has_side_effects=True),
        cost_estimate=pl.CostEstimate(flops=10 ** 7, bytes_accessed=mine.size * 4 * n_rel, transcendentals=0),
        name="share_lists",
    )(mine)


def blocks_kernel(cfg, *refs):
    n_chunk, reduce, back, d, sizes = cfg
    refs = list(refs)
    take = lambda n: [refs.pop(0) for _ in range(n)]
    parts = take(N_SRC)
    m_ref = take(1)[0]
    list_refs, left_ref = take(2) if sizes else (), take(1)[0] if back else None
    o_total, o_a, o_b = take(3)
    plan_refs, grad_ref = take(3) if sizes else (), take(1)[0] if back else None
    in_f, in_b, got_f, s_wire, r_wire, u_wire, y_wire, t_buf, u_buf, y_buf, load, send, recv, put = take(14)
    n_rows = t_buf.shape[0] // n_chunk
    cut = [pl.ds(k * n_rows, n_rows) for k in range(n_chunk)]
    thin = [pl.ds(k * n_rows // 2, n_rows // 2) for k in range(n_chunk)]
    side = lax.broadcasted_iota(I32, (n_rows // 2, LANES), 1) < LANES // 2
    tiles = d // LANES
    turn = lambda v: pltpu.roll(v, LANES // 2, 1)
    lanes = lambda v, j: v[:, LANES * j:LANES * (j + 1)]

    def pack(wire, k, value):
        top, low = value[:n_rows // 2], value[n_rows // 2:]
        turned = [turn(lanes(low, j)) for j in range(tiles + 1)]
        parts = [lanes(top, j) for j in range(tiles)] + [jnp.where(side, lanes(top, tiles), turned[0])]
        parts += [jnp.where(side, turned[j], turned[j + 1]) for j in range(tiles)]
        for j, part in enumerate(parts):
            wire[thin[k], LANES * j:LANES * (j + 1)] = part.astype(BF16)

    def unpack(wire, k):
        value = wire[thin[k], :].astype(F32)
        turned = [turn(lanes(value, tiles + j)) for j in range(tiles + 1)]
        top = [lanes(value, j) for j in range(tiles)] + [jnp.where(side, lanes(value, tiles), 0.0)]
        low = [jnp.where(side, turned[j], turned[j + 1]) for j in range(tiles)] + [jnp.where(side, turned[tiles], 0.0)]
        return jnp.concatenate([jnp.concatenate(top, axis=1), jnp.concatenate(low, axis=1)], axis=0)

    chunks = range(n_chunk)
    loads = {}
    for i, part in enumerate(parts[:2] if reduce else parts):
        buf = in_f.at[i] if reduce or i == 0 else in_b.at[i - 1]
        for k in chunks:
            loads[i, k] = pltpu.make_async_copy(part.at[cut[k]], buf.at[cut[k]], load.at[i, k])
    order = (1, 0) if reduce else range(N_SRC)
    for i in order:
        for k in chunks:
            loads[i, k].start()
    u_buf[...] = jnp.zeros(u_buf.shape, BF16)
    meet((Y, CORE))
    links = []
    copy_in = pltpu.make_async_copy

    def link(src, dst, rel, cut=cut):
        n = len(links)
        links.append([remote(src.at[cut[k]], dst.at[cut[k]], send.at[n, k], recv.at[n, k], rel) for k in chunks])
        return links[-1]

    if reduce:
        first = link(parts[3], got_f.at[1], CORE)
        second = link(parts[2], got_f.at[0], CORE)
        over = link(s_wire, r_wire, Y, thin)
        for copies in (first, second):
            for copy in copies:
                copy.start()
        for k in chunks:
            loads[1, k].wait()
            first[k].wait_recv()
            pack(s_wire, k, in_f[1, cut[k], :] + got_f[1, cut[k], :])
            over[k].start()
    to_y = link(u_wire, y_wire, Y, thin)
    to_core = link(u_buf, o_b.at[0], CORE)
    puts = []
    for k in chunks:
        if reduce:
            loads[0, k].wait()
            second[k].wait_recv()
            over[k].wait_recv()
            total = in_f[0, cut[k], :] + got_f[0, cut[k], :] + unpack(r_wire, k)
        else:
            for i in range(N_SRC):
                loads[i, k].wait()
            total = in_f[0, cut[k], :]
            for i in range(N_SRC - 1):
                total = total + in_b[i, cut[k], :].astype(F32)
        total = total.astype(BF16)
        t_buf[cut[k], :] = total
        dims = (((1,), (1 if back else 0,)), ((), ()))
        mixed = lax.dot_general(total[:, :d], m_ref[...], dims, preferred_element_type=F32)
        u_buf[cut[k], 0:d] = (total[:, :d].astype(F32) + mixed).astype(BF16)
        pack(u_wire, k, u_buf[cut[k], :].astype(F32))
        to_y[k].start()
        to_core[k].start()
        puts.append(pltpu.make_async_copy(u_buf.at[cut[k]], o_a.at[0, cut[k]], put.at[0, k]))
        puts.append(pltpu.make_async_copy(t_buf.at[cut[k]], o_total.at[cut[k]], put.at[1, k]))
        for copy in puts[-2:]:
            copy.start()
    if sizes:
        plan_kernel(*sizes, *list_refs, *plan_refs)
    if back:
        grad_ref[...] = lax.dot_general(left_ref[:, :d], t_buf[:, :d], (((0,), (0,)), ((), ())), preferred_element_type=F32)
    on = link(y_buf, o_b.at[1], CORE)
    for k in chunks:
        to_y[k].wait_recv()
        y_buf[cut[k], :] = unpack(y_wire, k).astype(BF16)
        on[k].start()
        puts.append(copy_in(y_buf.at[cut[k]], o_a.at[1, cut[k]], put.at[2, k]))
        puts[-1].start()
    waited = [to_y] + ([first, second, over] if reduce else [])
    for copies in links:
        for copy in copies:
            if any(copies is w for w in waited):
                copy.wait_send()
            else:
                copy.wait()
    for copy in puts:
        copy.wait()


def complete_blocks(parts, m, reduce, back, ident, sizes=None, lists=(), left=(), n_chunk=4):
    n_blk, wide = parts[0].shape
    d = m.shape[0]
    sem = lambda *s: pltpu.SemaphoreType.DMA(s)
    pair = jax.ShapeDtypeStruct((2, n_blk, wide), BF16)
    extra = plan_shapes(sizes) if sizes else []
    extra += [jax.ShapeDtypeStruct((d, d), F32)] * len(left)
    buf = lambda n, dt: pltpu.VMEM((n, n_blk, wide) if n else (n_blk, wide), dt)
    return pl.pallas_call(
        functools.partial(blocks_kernel, (n_chunk, reduce, back, d, sizes)),
        out_shape=[jax.ShapeDtypeStruct((n_blk, wide), BF16)] + [pair] * 2 + extra,
        in_specs=[any_space] * N_SRC + [in_vmem] * (1 + len(lists) + len(left)),
        out_specs=[any_space] * 3 + [in_vmem] * len(extra),
        scratch_shapes=[buf(2, F32), buf(3, BF16), buf(2, F32)] + [pltpu.VMEM((n_blk // 2, 2 * d), BF16)] * 4 + [
            buf(0, BF16), buf(0, BF16), buf(0, BF16), sem(4, n_chunk), sem(6, n_chunk), sem(6, n_chunk), sem(3, n_chunk)],
        compiler_params=pltpu.CompilerParams(collective_id=ident, has_side_effects=True, vmem_limit_bytes=VMEM_LIMIT),
        cost_estimate=pl.CostEstimate(flops=10 ** 8, bytes_accessed=n_blk * wide * 40, transcendentals=0),
        name=f"complete_blocks_{ident}",
    )(*parts, m, *lists, *left)


def solution(mesh):
    ep_size, dp_size = mesh.shape['ep'], mesh.shape['dp']
    sub = Mesh(mesh.devices.reshape(ep_size, dp_size // 2, 2), ('ep', 'x', 'core'))
    tok_axes = ('x', 'core', 'ep')
    tok_spec = P(tok_axes, None)
    route_spec = P(None, tok_axes, None)
    whole_spec = P(None, None, None)
    expert_spec = P(None, 'ep', None, None)
    flip = [(0, 1), (1, 0)]
    move = lambda v, axis: lax.ppermute(v, axis, flip)
    move_diag = lambda v: lax.ppermute(v, ('ep', 'core'), [(0, 3), (1, 2), (2, 1), (3, 0)])
    fence = lax.optimization_barrier

    def device_step(tokens, d_out, expert_ids, gate_vals, w_mix, w_gate, w_up, w_down):
        n_layers, d = w_mix.shape[0], w_mix.shape[1]
        n_tok = tokens.shape[0]
        top = expert_ids.shape[2]
        n_local = w_gate.shape[1]
        n_exp = n_local * ep_size
        n = n_tok * top
        n_rel = 2 * N_SRC
        wide = cdiv(d, LANES) * LANES
        weights = (jnp.swapaxes(w_gate, 2, 3), jnp.swapaxes(w_up, 2, 3), w_down)
        pad = lambda v: jnp.pad(v, ((0, 0), (0, wide - d)))
        send_three = lambda p: [move(p[1], 'ep'), move(p[2], 'core'), move_diag(p[3])]

        def own_sum(p, got):
            return sum([g.astype(F32) for g in got], p)[:, :d].astype(BF16)

        one = lambda v: v.reshape(1, n_tok, wide)
        pairs = lambda a, b: [(a, 0), (a, 1), (b, 0), (b, 1)]

        one = lambda v: v.reshape(1, n_tok, wide)
        pairs = lambda a, b: [(a, 0), (a, 1), (b, 0), (b, 1)]
        singles = lambda *v: [(one(a), 0) for a in v]

        same = jnp.eye(d, dtype=BF16)
        u0 = (jnp.dot(tokens, pad(same), preferred_element_type=F32)
              + jnp.dot(tokens, pad(w_mix[0]), preferred_element_type=F32)).astype(BF16)
        u0_y, u0_c = move(u0, 'ep'), move(u0, 'core')
        lists = [sorted_list(expert_ids[l], gate_vals[l]) for l in range(n_layers)]
        counts = jnp.sum((expert_ids.transpose(0, 2, 1).reshape(n_layers, n, 1) == jnp.arange(n_exp, dtype=I32)).astype(F32), axis=1)
        packed = jnp.concatenate([jnp.concatenate([v[0] for v in lists] + [v[1] for v in lists]).reshape(-1, LANES),
                                  jnp.pad(counts, ((0, 8 - n_layers), (0, LANES - n_exp)))], axis=0)
        dy = jnp.dot(d_out, pad(same), preferred_element_type=F32).astype(BF16)
        packed, dy = fence((packed, dy))
        shared = share(packed, N_SRC)
        u0_y, u0_c, dy, shared = fence((u0_y, u0_c, dy, shared))
        u0_d = move(u0_y, 'core')
        shared_x = move(shared, 'x')
        dy_y, dy_x = move(dy, 'ep'), move(dy, 'x')
        sizes = (n_layers, n_local, n_tok, n // LANES)
        routes = plan(shared, shared, sizes)
        u0_half = singles(u0, u0_y, u0_c, u0_d)
        add = lambda a, b: a.astype(F32) + b.astype(F32)
        to_chips = lambda v: [move(v, 'ep'), move(v, 'x'), lax.ppermute(v, ('ep', 'x'), [(0, 3), (1, 2), (2, 1), (3, 0)])]
        of_chips = lambda v, t: (add(v, t[0]) + add(t[1], t[2])).astype(BF16)
        piece = first_piece(n_local // 2)
        *part, ab0, xu0 = run_experts(routes, 0, u0_half, None, weights, None, None, True, True, p_f32=True)
        dy_y, dy_x, shared_x, part = fence((dy_y, dy_x, shared_x, part))
        dy_c, dy_d, dy_xy, dy_xc = move(dy, 'core'), move(dy_y, 'core'), move(dy_y, 'x'), move(dy_x, 'core')
        y0, u1_a, u1_b, *routes_x = complete_blocks(part, w_mix[1], True, False, 1, sizes, (shared, shared_x))
        routes_x = flat(*routes_x)
        dy_c, dy_d, dy_xy, dy_xc, u0_p, u0_q, y0, u1_a, u1_b = fence(
            (dy_c, dy_d, dy_xy, dy_xc, u0, u0_y, y0, u1_a, u1_b))
        dy_xd = move(dy_xy, 'core')
        u1_xa = move(u1_a, 'x')
        out = run_experts(routes, 1, pairs(u1_a, u1_b), singles(dy, dy_y, dy_c, dy_d), weights, None, None, True, True)
        u1_xa, dy_xd, u0_p, u0_q, out = fence((u1_xa, dy_xd, u0_p, u0_q, out))
        y_part, du_part, g1 = out[:4], out[4:8], out[8]
        u1_xb = move(u1_xa, 'core')
        got = send_three(du_part)
        u0_x, u0_xy = move(u0_p, 'x'), move(u0_q, 'x')
        out = run_experts(routes_x, 1, pairs(u1_xa, u1_xb), singles(dy_x, dy_xy, dy_xc, dy_xd), weights, g1, None,
                          False, False)
        got, u0_x, u0_xy, out = fence((got, u0_x, u0_xy, out))
        *finals, sent_a, sent_b = out
        got1 = [move(sent_a, 'core'), move(sent_b, 'core')]
        du1, dx_a, dx_b, g_mix1 = complete_blocks([du_part[0], *got], w_mix[1], False, True, 2, left=(y0,))
        tx = lambda x, du: jnp.einsum('td,te->de', x, du, preferred_element_type=F32)
        dx_a, y_part, got1, u0_x, u0_xy, g_mix1 = fence((dx_a, y_part, got1, u0_x, u0_xy, g_mix1))
        dx_xa = move(dx_a, 'x')
        part1 = g_mix1.astype(BF16)
        theirs1 = to_chips(part1)
        got_y = send_three(y_part)
        u0_xc, u0_xd = move(u0_x, 'core'), move(u0_xy, 'core')
        out = run_experts(routes, 0, None, pairs(dx_a, dx_b), weights, None, finals, False, True, got=got1, kept=(ab0, xu0))
        dx_xa, got_y, u0_xc, u0_xd, theirs1, out = fence((dx_xa, got_y, u0_xc, u0_xd, theirs1, out))
        du_part, g0, finals = out[:4], out[4], out[5:]
        dx_xb = move(dx_xa, 'core')
        got = send_three(du_part)
        part1 = of_chips(part1, theirs1)
        theirs1 = move(part1, 'core')
        du_part, dx_xb, part1 = fence((du_part, dx_xb, part1))
        out = run_experts(routes_x, 0, singles(u0_x, u0_xy, u0_xc, u0_xd), pairs(dx_xa, dx_xb), weights, g0, finals,
                          False, False)
        got, theirs1, got_y, y_own, out = fence((got, theirs1, got_y, y_part[0], out))
        *finals, sent_a, sent_b = out
        got_a, got_b = move(sent_a, 'core'), move(sent_b, 'core')
        du0 = own_sum(du_part[0], got)
        part0 = tx(tokens, du0).astype(BF16)
        theirs0 = to_chips(part0)
        turned = lambda v, w: jnp.einsum('te,de->dt', v, w, preferred_element_type=F32)
        dx0 = (turned(du0, same) + turned(du0, w_mix[0])).astype(BF16)
        y1 = turned(own_sum(y_own, got_y), same).astype(BF16)
        dx0, y1, got_a, finals = fence((dx0, y1, got_a, finals))
        finals = place(routes[0], 0, 0, got_a, finals)
        dx0, got_b, finals = fence((dx0, got_b, finals))
        finals = place(routes[0], piece, 0, got_b, finals)
        theirs0, finals = fence((theirs0, finals))
        total0 = of_chips(part0, theirs0)
        g_mix = jnp.stack([add(total0, move(total0, 'core')), add(part1, theirs1)]).astype(BF16)
        return (y1.T, dx0.T, g_mix, jnp.swapaxes(finals[0], 2, 3), jnp.swapaxes(finals[1], 2, 3), finals[2])

    return jax.shard_map(device_step, mesh=sub,
                         in_specs=(tok_spec, tok_spec, route_spec, route_spec, whole_spec,
                                   expert_spec, expert_spec, expert_spec),
                         out_specs=(tok_spec, tok_spec, whole_spec, expert_spec, expert_spec, expert_spec),
                         check_vma=False)
```

```python
import functools

import jax
import jax.numpy as jnp
from jax import lax
from jax.experimental import pallas as pl
from jax.experimental.pallas import tpu as pltpu
from jax.sharding import Mesh, PartitionSpec as P

F32, BF16, I32 = jnp.float32, jnp.bfloat16, jnp.int32
MESH = pl.DeviceIdType.MESH
ROWS = 384
GRP = 8
PITCH = 9
DEPTH = 3
FULL = 8
HALF = 4
CAP_FACTOR = 3
LANES = 128
N_SRC = 4
Y, CORE, X = 1, 2, 4
VMEM_LIMIT = 62 * 1024 * 1024
PER_TILE = ROWS // GRP
ROW_BOUND, ROW_GOFF, ROW_EXPERT, ROW_PARTNER, TAB_ROWS = 32, 33, 34, 35, 40
SLOT_GROUPS = 256


def cdiv(a, b):
    return (a + b - 1) // b


def first_piece(n_exp):
    return n_exp * 5 // 8


def spans(d):
    return [(LANES * j, min(LANES, d - LANES * j)) for j in range(cdiv(d, LANES))]


any_space = pl.BlockSpec(memory_space=pl.ANY)
in_vmem = pl.BlockSpec(memory_space=pltpu.VMEM)


def sorted_list(expert_ids, gate_vals):
    n_tok, top = expert_ids.shape
    n = n_tok * top
    keys = expert_ids.T.reshape(n) * n + jnp.arange(n, dtype=I32)
    keys, gates = lax.sort((keys, gate_vals.T.reshape(n)), num_keys=1, is_stable=False)
    return (keys % n_tok).astype(F32), gates


def plan_kernel(n_layers, n_local, n_tok, list_rows, deal_ref, all_ref, tab_ref, idx_ref, gate_ref):
    n_mine = n_local // 2
    core, ep = lax.axis_index('core'), lax.axis_index('ep')
    list_len = list_rows * LANES
    lane = lambda n: lax.broadcasted_iota(I32, (n, LANES), 1).astype(F32)
    sub = lambda n: lax.broadcasted_iota(I32, (n, LANES), 0).astype(F32)
    over_lanes = lambda v: jnp.sum(v, axis=1, keepdims=True)
    over_subs = lambda v: jnp.sum(v, axis=0, keepdims=True)
    l16, s16 = lane(n_mine), sub(n_mine)
    groups = lambda c: jnp.floor((c + (GRP - 0.5)) * (1.0 / GRP))
    for l in range(n_layers):
        cnt = all_ref[:, 2 * n_layers * list_rows + l, :]
        ends = cnt
        step = 1
        while step < 2 * n_local:
            ends = ends + jnp.where(lane(N_SRC) >= step, pltpu.roll(ends, step, 1), 0.0)
            step *= 2
        starts = ends - cnt
        second = (ep > 0)
        local = lambda v: jnp.where(lane(N_SRC) < n_local, jnp.where(second, pltpu.roll(v, LANES - n_local, 1), v), 0.0)
        cnt, starts = local(cnt), local(starts)
        tiles = jnp.floor((over_subs(groups(local(deal_ref[:, 2 * n_layers * list_rows + l, :]))) + (PER_TILE - 0.5))
                          * (1.0 / PER_TILE))
        load = jnp.where(lane(1) < n_local, jnp.maximum(1.0, tiles), -1.0)
        wide = jnp.broadcast_to(load, (n_local, LANES))
        col = over_lanes(jnp.where(lane(n_local) == sub(n_local), wide, 0.0))
        ahead = (col > wide) | ((col == wide) & (sub(n_local) < lane(n_local)))
        rank = over_subs(jnp.where(ahead, 1.0, 0.0))
        odd = s16 - 2.0 * jnp.floor(s16 * 0.5 + 0.25)
        flip = jnp.where(core > 0, 1.0 - odd, odd)
        dealt = lambda f: (jnp.broadcast_to(rank, (n_mine, LANES)) == 2.0 * s16 + f) & (l16 < n_local)
        pick = dealt(flip)
        choose = lambda p, row: over_lanes(jnp.where(p, jnp.broadcast_to(row, (n_mine, LANES)), 0.0))
        mine = lambda row: choose(pick, row)
        as_row = lambda c: over_subs(jnp.where(l16 == s16, c, 0.0))
        experts = as_row(mine(lane(1)))
        partner = as_row(choose(dealt(1.0 - flip), lane(1)))
        at = l * TAB_ROWS
        off = jnp.zeros((n_mine, 1), F32)
        pos = [jnp.zeros((n_mine, LANES), F32) for _ in range(SLOT_GROUPS // LANES)]
        for s in range(N_SRC):
            c, st = mine(cnt[s:s + 1]), mine(starts[s:s + 1]) + float(s * list_len)
            ng = groups(c)
            for i in range(len(pos)):
                rel = l16 + float(LANES * i) - off
                code = (st + GRP * rel) * 16.0 + jnp.minimum(float(GRP), c - GRP * rel)
                pos[i] = jnp.where((rel >= 0) & (rel < ng), code, pos[i])
            off = off + ng
        for i in range(len(pos)):
            tab_ref[pl.ds(at + i, n_mine, stride=len(pos)), :] = pos[i].astype(I32)
        n_tiles = jnp.maximum(1.0, jnp.floor((off + (PER_TILE - 0.5)) * (1.0 / PER_TILE)))
        bounds = over_subs(jnp.where(s16 < l16, n_tiles, 0.0))
        before = over_lanes(jnp.where(l16 == s16, jnp.broadcast_to(bounds, (n_mine, LANES)), 0.0))
        t = jnp.minimum(l16, over_subs(jnp.broadcast_to(n_tiles, (n_mine, LANES))) - 1.0)
        inside = (t >= before) & (t < before + n_tiles)
        goff = over_subs(jnp.where(inside, s16 * float(SLOT_GROUPS) + (t - before) * float(PER_TILE), 0.0))
        rows = [(ROW_BOUND, bounds), (ROW_GOFF, goff), (ROW_EXPERT, experts), (ROW_PARTNER, partner)]
        for row, value in rows:
            tab_ref[at + row:at + row + 1, :] = value.astype(I32)
    for l in range(n_layers):
        pad = l * (N_SRC * list_rows + 8) + N_SRC * list_rows
        gate_ref[pad:pad + 8, :] = jnp.zeros((8, LANES), F32)
        for s in range(N_SRC):
            to = (l * N_SRC + s) * list_rows
            toks = all_ref[s, l * list_rows:(l + 1) * list_rows, :]
            idx_ref[to:to + list_rows, :] = ((toks + float(s * n_tok)) * float(PITCH)).astype(I32)
            to = l * (N_SRC * list_rows + 8) + s * list_rows
            gate_ref[to:to + list_rows, :] = all_ref[s, (n_layers + l) * list_rows:(n_layers + l + 1) * list_rows, :]


def plan_shapes(sizes):
    n_layers, _, _, list_rows = sizes
    rows = (n_layers * TAB_ROWS, n_layers * N_SRC * list_rows, n_layers * (N_SRC * list_rows + 8))
    return [jax.ShapeDtypeStruct((n, LANES), dt) for n, dt in zip(rows, (I32, I32, F32))]


def flat(tab, idx, gates):
    return tab.reshape(-1), idx.reshape(-1), gates


def plan(deal, shared, sizes):
    return flat(*pl.pallas_call(
        functools.partial(plan_kernel, *sizes),
        out_shape=plan_shapes(sizes),
        in_specs=[in_vmem] * 2, out_specs=[in_vmem] * 3,
        cost_estimate=pl.CostEstimate(flops=10 ** 7, bytes_accessed=10 ** 6, transcendentals=0),
        name="plan",
    )(deal, shared))


def expert_kernel(cfg, *refs):
    fwd, bwd, own, layer, n_blk, d, ff, n_exp, picks, row_id, list_len, p_f32, n_alias, got_layer = cfg
    save, load = fwd and not bwd, own and bwd and not fwd
    refs = list(refs)
    take = lambda n: [refs.pop(0) for _ in range(n)]
    tab_hbm, idx_hbm, gate_hbm = take(3)
    u_pieces = take(N_SRC) if not load else []
    dy_pieces = take(N_SRC) if bwd else []
    wg_hbm, wu_hbm, wd_hbm = take(3)
    ab_hbm, xu_hbm = take(2) if load else (None, None)
    prev = take(1)[0] if bwd and not own else None
    got = take(2) if got_layer is not None else None
    take(n_alias)
    y_outs = take(N_SRC) if fwd else []
    du_outs = take(N_SRC) if bwd and own else []
    grad = take(1)[0] if bwd and own else None
    finals = take(3) if bwd and not own or got_layer is not None else None
    sent = take(2) if bwd and not own else None
    ab_hbm, xu_hbm = take(2) if save else (ab_hbm, xu_hbm)
    tab_ref, idx, gate_ref, land, table, gat = take(6)
    acc, row_ref = take(2) if own else (None, None)
    gu_ref, wd_ref, g_ref, x_u = take(4)
    x_c = take(1)[0] if bwd else None
    ab_ref = take(1)[0]
    dh_ref = take(1)[0] if bwd else None
    h_ref = take(1)[0]
    dab_ref, sums = take(2) if bwd else (None, None)
    keep_buf = take(1)[0] if bwd and not own else None
    got_buf = take(1)[0] if got is not None else None
    list_sem, land_sem, w_sem = take(3)
    sum_sem = take(1)[0] if bwd else None
    keep_sem = take(1)[0] if bwd and not own else None
    read_sem, write_sem = take(2) if got is not None else (None, None)
    stage_f, out_sem = take(2) if own else (None, None)
    ab_sem, xu_sem = take(2) if save or load else (None, None)

    split = first_piece(n_exp)
    copy = pltpu.make_async_copy
    cols = spans(d)
    lo = ff // 256 * 256
    hi = ff - lo
    dot = functools.partial(lax.dot_general, preferred_element_type=F32)
    nn = (((1,), (0,)), ((), ()))
    nt = (((1,), (1,)), ((), ()))
    tn = (((0,), (0,)), ((), ()))
    al = pl.multiple_of
    n_row = N_SRC * n_blk
    glane = lax.broadcasted_iota(I32, (GRP, LANES), 1)
    gsub = lax.broadcasted_iota(I32, (GRP, LANES), 0)

    def row_at(r):
        return pl.ds(r * PITCH, FULL)

    def codes_of(tile):
        at = ROW_GOFF * LANES + tile
        if own and bwd:
            return lambda q: tab_ref[tab_ref[at] + q]
        view = tab_ref.at[pl.ds(tab_ref[at], PER_TILE)]
        return lambda q: view[q]

    def gather(codes, q):
        ids = idx.at[pl.ds(codes(q) >> 4, GRP)]
        for k in range(GRP):
            gat[row_at(q * GRP + k), :] = table[pl.ds(ids[k], FULL), :]

    def gate_column(code):
        pos = code >> 4
        row, shift = pos >> 7, pos & (LANES - 1)
        want = glane == gsub + shift
        over = glane == gsub + (shift - LANES)
        here = gate_ref[pl.ds(row, GRP, stride=0), :]
        there = gate_ref[pl.ds(row + 1, GRP, stride=0), :]
        v = jnp.where(want, here, jnp.where(over, there, 0.0))
        return jnp.where(gsub < (code & 15), jnp.sum(v, axis=1, keepdims=True), 0.0)

    def scatter(codes, q):
        ids = idx.at[pl.ds(codes(q) >> 4, GRP)]
        new = []
        for k in range(GRP):
            at = pl.ds(ids[k], FULL)
            new.append((at, acc[at, :] + row_ref[row_at(q * GRP + k), :]))
        for at, value in reversed(new):
            acc[at, :] = value

    def keep_ab(t):
        ends = (ab_ref.at[t & 1], ab_hbm.at[t])
        return copy(*(ends if save else ends[::-1]), ab_sem.at[t & 1])

    def keep_xu(t):
        ends = (x_u.at[t & 1], xu_hbm.at[t])
        return copy(*(ends if save else ends[::-1]), xu_sem.at[t & 1])

    def of(ref, t):
        return ref.at[t & 1] if save or load else ref

    def convert(codes, t):
        for q in range(0, PER_TILE, 2):
            part = []
            for p in (q, q + 1):
                code = codes(p)
                rows = [gat[pl.ds(GRP * PITCH * p + j, GRP, stride=PITCH), :]
                        for j in range(HALF if load else 0, FULL if bwd else HALF)]
                real = gsub < (code & 15)
                gate = gate_column(code)
                g_ref[GRP * p:GRP * (p + 1), :] = gate
                us, dys = ([], rows) if load else (rows[:HALF], rows[HALF:])
                part.append([jnp.where(real, v, 0.0) for v in us] + [v * gate for v in dys])
            at = slice(GRP * q, GRP * (q + 2))
            for x, o in ((None if load else of(x_u, t), 0), (x_c, 0 if load else HALF)):
                if x is None:
                    continue
                for j, (c, w) in enumerate(cols):
                    both = jnp.concatenate([part[0][o + j], part[1][o + j]], axis=0)
                    x[at, c:c + w] = both[:, :w].astype(BF16)

    def put_rows(o, value, s0):
        value = value.astype(BF16).astype(F32)
        n = value.shape[0]
        for j, (c, w) in enumerate(cols):
            row_ref[pl.ds(PITCH * s0 + o + j, n, stride=PITCH), 0:w] = value[:, c:c + w] * g_ref[s0:s0 + n, 0:w]

    low = lax.broadcasted_iota(I32, (16, 2 * hi), 1) < hi

    def middle(a, b, dh):
        sig = 0.5 * jnp.tanh(0.5 * a) + 0.5
        act = a * sig
        h = act * b
        if dh is None:
            return h, None, None
        slope = sig * (1.0 + a * (1.0 - sig))
        return h, dh * b * slope, dh * act

    def weights(e, slot):
        at = (layer, tab_ref[ROW_EXPERT * LANES + e])
        moves = []
        for i, w in enumerate((wg_hbm, wu_hbm)):
            moves.append((w.at[at + (pl.ds(0, lo),)], gu_ref.at[slot, pl.ds(i * lo, lo)]))
            moves.append((w.at[at + (pl.ds(lo, hi),)], gu_ref.at[slot, pl.ds(2 * lo + i * hi, hi)]))
        moves.append((wd_hbm.at[at], wd_ref.at[slot]))
        return [copy(a, b, w_sem.at[slot, i]) for i, (a, b) in enumerate(moves)]

    def sums_in(e, slot):
        return copy(prev.at[e], sums.at[slot], sum_sem.at[slot])

    def sums_out(e, slot):
        return copy(sums.at[slot], grad.at[e], sum_sem.at[slot])

    def keeps(e, slot):
        at = (layer, tab_ref[ROW_EXPERT * LANES + e])
        return [copy(keep_buf.at[slot, i], finals[i].at[at], keep_sem.at[slot, i]) for i in range(3)]

    def send(e, slot, part):
        return copy(keep_buf.at[slot], sent[part].at[e - part * split], keep_sem.at[slot, 3])

    def read(e, slot, part=0):
        return copy(got[part].at[e - part * split], got_buf.at[slot], read_sem.at[slot])

    def writes(e, slot):
        to = tab_ref[TAB_ROWS * LANES + e]
        return [copy(got_buf.at[slot, i], finals[i].at[got_layer, to], write_sem.at[slot, i]) for i in range(3)]

    def start(moves):
        for m in moves:
            m.start()

    def wait(moves):
        for m in moves:
            m.wait()

    n_tab = TAB_ROWS * LANES
    lists = [copy(tab_hbm.at[pl.ds(row_id * n_tab, n_tab)], tab_ref.at[pl.ds(0, n_tab)], list_sem.at[0]),
             copy(idx_hbm.at[pl.ds(row_id * N_SRC * list_len, N_SRC * list_len)], idx.at[pl.ds(0, N_SRC * list_len)],
                  list_sem.at[1]),
             copy(gate_hbm.at[pl.ds(row_id * gate_ref.shape[0], gate_ref.shape[0])], gate_ref, list_sem.at[2])]
    if got is not None:
        at = (got_layer * TAB_ROWS + ROW_PARTNER) * LANES
        lists.append(copy(tab_hbm.at[pl.ds(at, LANES)], tab_ref.at[pl.ds(n_tab, LANES)], list_sem.at[3]))
    start(lists)
    pieces = []
    for s in range(N_SRC):
        if not load:
            pieces.append((u_pieces[s], picks[0][s], s, 0, fwd))
        if bwd:
            pieces.append((dy_pieces[s], picks[1][s], s, HALF, own))
    lands = [copy(ref.at[pick], land.at[i % N_SRC], land_sem.at[i % N_SRC]) for i, (ref, pick, *_) in enumerate(pieces)]
    start(lands[:N_SRC])
    lists[0].wait()
    for e in range(DEPTH - 1):
        start(weights(e, e))
        if bwd and not own:
            sums_in(e, e).start()
    if got is not None:
        lists[3].wait()
        read(0, 0).start()
    if own:
        def clear(c, _):
            for k in range(4):
                acc[pl.ds(al(c * 1152 + 288 * k, 8), 288), :] = jnp.zeros((288, LANES), F32)
            return 0

        lax.fori_loop(0, acc.shape[0] // 1152, clear, 0)
        row_ref[...] = jnp.zeros(row_ref.shape, F32)
    rows = 256
    for i, (_, _, s, o, seed) in enumerate(pieces):
        lands[i].wait()

        def fill(c, _, i=i, o=o, seed=seed, s=s):
            r = al(c * rows, rows)
            for j in range(HALF):
                vals = land[i % N_SRC, pl.ds(r, rows), LANES * j:LANES * (j + 1)].astype(F32)
                to = pl.ds(PITCH * (s * n_blk + r) + o + j, rows, stride=PITCH)
                table[to, :] = vals
                if seed and s == 0:
                    acc[to, :] = vals
            return 0

        lax.fori_loop(0, n_blk // rows, fill, 0)
        if i + N_SRC < len(pieces):
            lands[i + N_SRC].start()
    wait(lists[1:3])
    for k in range(GRP):
        idx[N_SRC * list_len + k] = 0

    def first(q, _):
        gather(begin, 2 * q)
        gather(begin, 2 * q + 1)
        return 0

    begin = codes_of(0)
    lax.fori_loop(0, PER_TILE // 2, first, 0)
    convert(begin, 0)
    if save:
        keep_xu(0).start()
    if load:
        keep_ab(0).start()
        keep_xu(0).start()

    def expert(e, _):
        slot = e & 1
        deep = lax.rem(e, DEPTH)
        sum_slot = slot if own else deep
        wait(weights(e, deep))
        if bwd and not own:
            sums_in(e, deep).wait()
        if got is not None:
            read(0, slot).wait()
            start(writes(e, slot))

            @pl.when((e > 0) & (e < n_exp - 1))
            def _():
                wait(writes(e - 1, 1 - slot))

        @pl.when(e < n_exp - (DEPTH - 1))
        def _():
            ahead = lax.rem(e + DEPTH - 1, DEPTH)
            start(weights(e + DEPTH - 1, ahead))
            if bwd and not own:
                sums_in(e + DEPTH - 1, ahead).start()

        @pl.when(e < n_exp - 1)
        def _():
            if got is not None:
                for part in range(2):
                    @pl.when((e + 1 >= split) if part else (e + 1 < split))
                    def _(part=part):
                        read(e + 1, 1 - slot, part).start()

        if bwd and own:
            @pl.when(e > 1)
            def _():
                sums_out(e - 2, slot).wait()

            sums[slot] = jnp.zeros(sums.shape[1:], F32)

        def tile(t, _):
            if save:
                @pl.when(t > 1)
                def _():
                    keep_ab(t - 2).wait()

                @pl.when(t > 0)
                def _():
                    keep_xu(t - 1).wait()
            if load:
                keep_ab(t).wait()
                keep_xu(t).wait()
                keep_ab(t + 1).start()
                keep_xu(t + 1).start()
            ab, xu = of(ab_ref, t), of(x_u, t)
            before, after = codes_of(jnp.maximum(t - 1, 0)), codes_of(t + 1)
            for q in range(PER_TILE):
                if own:
                    scatter(before, q)
                gather(after, q)
            front = ROWS if own and bwd else ROWS // 2
            for s0 in range(0, ROWS, front):
                sl = slice(s0, s0 + front)
                if not load:
                    ab[sl, :] = dot(xu[sl, :], gu_ref[deep], nt)
                if bwd:
                    dh_ref[sl, :] = dot(x_c[sl, :], wd_ref[deep], nt)
            for r in range(0, ROWS, 16):
                rows = slice(r, r + 16)
                for c in range(0, lo, LANES):
                    h, da, db = middle(ab[rows, c:c + LANES], ab[rows, lo + c:lo + c + LANES],
                                       dh_ref[rows, c:c + LANES] if bwd else None)
                    h_ref[rows, c:c + LANES] = h.astype(BF16)
                    if bwd:
                        dab_ref[rows, c:c + LANES] = da.astype(BF16)
                        dab_ref[rows, lo + c:lo + c + LANES] = db.astype(BF16)
                a = ab[rows, 2 * lo:]
                b = pltpu.roll(a, hi, 1)
                dh = dh_ref[rows, lo:] if bwd else None
                if bwd:
                    dh = jnp.concatenate([dh, dh], axis=1)
                h, da, db = middle(a, b, dh)
                h_ref[rows, lo:] = h[:, :hi].astype(BF16)
                if bwd:
                    dab_ref[rows, 2 * lo:] = jnp.where(low, da, pltpu.roll(db, hi, 1)).astype(BF16)
            half = ROWS // 2
            for s0 in range(0, ROWS, half):
                sl = slice(s0, s0 + half)
                if fwd:
                    put_rows(0, dot(h_ref[sl, :], wd_ref[deep], nn), s0)
                if bwd and own:
                    put_rows(HALF, dot(dab_ref[sl, :], gu_ref[deep], nn), s0)
            if bwd:
                view = sums.at[sum_slot]
                view[0:2 * ff, :] += dot(dab_ref[...], xu[...], tn)
                view[2 * ff:, :] += dot(h_ref[...], x_c[...], tn)
            convert(after, t + 1)
            if save:
                keep_ab(t).start()
                keep_xu(t + 1).start()
            return 0

        lax.fori_loop(tab_ref[ROW_BOUND * LANES + e], tab_ref[ROW_BOUND * LANES + e + 1], tile, 0)
        if bwd and own:
            sums_out(e, slot).start()
        if bwd and not own:
            @pl.when(e > 1)
            def _():
                wait(keeps(e - 2, slot) + [send(0, slot, 0)])

            for i in range(2):
                keep_buf[slot, i, 0:lo, :] = sums[deep, i * lo:(i + 1) * lo, :].astype(BF16)
                keep_buf[slot, i, lo:, :] = sums[deep, 2 * lo + i * hi:2 * lo + (i + 1) * hi, :].astype(BF16)
            keep_buf[slot, 2] = sums[deep, 2 * ff:, :].astype(BF16)
            start(keeps(e, slot))
            for part in range(2):
                @pl.when((e >= split) if part else (e < split))
                def _(part=part):
                    send(e, slot, part).start()
        return 0

    lax.fori_loop(0, n_exp, expert, 0)
    ends = ((n_exp - 2, (n_exp - 2) % 2), (n_exp - 1, (n_exp - 1) % 2))
    n_tiles = tab_ref[ROW_BOUND * LANES + n_exp]
    if save:
        wait([keep_ab(n_tiles - 2), keep_ab(n_tiles - 1), keep_xu(n_tiles - 1)])
    if save or load:
        keep_xu(n_tiles).wait()
    if load:
        keep_ab(n_tiles).wait()
    if own:
        end = codes_of(tab_ref[ROW_BOUND * LANES + n_exp] - 1)
        lax.fori_loop(0, PER_TILE, lambda q, _: (scatter(end, q), 0)[1], 0)
        flights = {}
        for o, out in ((HALF, du_outs), (0, y_outs)):
            for s in range(N_SRC if out else 0):
                wide = s == 0 or p_f32
                stage = stage_f.at[s] if wide else land.at[s]
                if s in flights:
                    flights[s].wait()

                def fetch(c, _, stage=stage, s=s, o=o):
                    r = al(c * rows, rows)
                    for j in range(HALF):
                        at = pl.ds(PITCH * (s * n_blk + r) + o + j, rows, stride=PITCH)
                        stage[pl.ds(r, rows), LANES * j:LANES * (j + 1)] = acc[at, :].astype(stage.dtype)
                    return 0

                lax.fori_loop(0, n_blk // rows, fetch, 0)
                flights[s] = copy(stage, out[s], out_sem.at[s])
                flights[s].start()
        wait(flights.values())
        if bwd:
            for e, slot in ends:
                sums_out(e, slot).wait()
    else:
        for e, slot in ends:
            wait(keeps(e, slot) + [send(0, slot, 0)])
    if got is not None:
        for e, slot in ends:
            wait(writes(e, slot))


def run_experts(routes, layer, u, dy, weights, prev, finals, fwd, own, p_f32=False, got=None, kept=None):
    tab, idx, gates = routes
    bwd = dy is not None
    wg, wu, wd = weights
    save, load = fwd and not bwd, kept is not None
    n_blk, wide = (dy or u)[0][0].shape[-2:]
    n_layers, n_local, ff, d = wd.shape
    n_exp = n_local // 2
    row_id = layer
    list_len = idx.shape[0] // (n_layers * N_SRC)

    arrays = lambda pieces: [v for v, _ in pieces]
    operands = [tab, idx, gates] + ([] if load else arrays(u)) + (arrays(dy) if bwd else []) + [wg, wu, wd] + list(kept or ())
    out_shape, aliases = [], {}
    for use in (fwd, bwd and own):
        if use:
            out_shape += [jax.ShapeDtypeStruct((n_blk, wide), F32 if s == 0 or p_f32 else BF16) for s in range(N_SRC)]
    if bwd and own:
        out_shape.append(jax.ShapeDtypeStruct((n_exp, 3 * ff, d), F32))
    if bwd and not own:
        operands.append(prev)
    if got is not None:
        operands += got
    for i, f in enumerate(finals or ()):
        aliases[len(operands)] = len(out_shape) + i
        operands.append(f)
    if bwd and not own or finals:
        out_shape += [jax.ShapeDtypeStruct((n_layers, n_local, ff, d), BF16)] * 3
    if bwd and not own:
        out_shape += [jax.ShapeDtypeStruct((n, 3, ff, d), BF16) for n in (first_piece(n_exp), n_exp - first_piece(n_exp))]
    if save:
        most = n_exp * (SLOT_GROUPS // PER_TILE) + 2
        out_shape += [jax.ShapeDtypeStruct((most, ROWS, 2 * ff), F32), jax.ShapeDtypeStruct((most, ROWS, d), BF16)]
    sem = lambda *s: pltpu.SemaphoreType.DMA(s)
    mid = lambda n, dt: pltpu.VMEM((ROWS, n), dt)
    twin = lambda n, dt: pltpu.VMEM((2, ROWS, n), dt) if save or load else mid(n, dt)
    table, rows = pltpu.VMEM((PITCH * N_SRC * n_blk, LANES), F32), pltpu.VMEM((PITCH * ROWS, LANES), F32)
    scratch = [pltpu.SMEM(((TAB_ROWS + 1) * LANES,), I32), pltpu.SMEM((N_SRC * list_len + LANES,), I32),
               pltpu.VMEM((N_SRC * list_len // LANES + 8, LANES), F32), pltpu.VMEM((N_SRC, n_blk, wide), BF16)]
    scratch += [table, rows] * (1 + own)
    scratch += [pltpu.VMEM((DEPTH, 2 * ff, d), BF16), pltpu.VMEM((DEPTH, ff, d), BF16), mid(LANES, F32)]
    scratch += [twin(d, BF16)] + [mid(d, BF16)] * bwd + [twin(2 * ff, F32)] + [mid(ff, F32)] * bwd + [mid(ff, BF16)]
    scratch += [mid(2 * ff, BF16), pltpu.VMEM((2 if own else DEPTH, 3 * ff, d), F32)] * bwd
    if bwd and not own:
        scratch.append(pltpu.VMEM((2, 3, ff, d), BF16))
    if got is not None:
        scratch.append(pltpu.VMEM((2, 3, ff, d), BF16))
    scratch += [sem(4), sem(N_SRC), sem(DEPTH, 5)] + [sem(DEPTH)] * bwd
    if bwd and not own:
        scratch.append(sem(2, 4))
    if got is not None:
        scratch += [sem(2), sem(2, 3)]
    if own:
        scratch += [pltpu.VMEM((N_SRC if p_f32 else 1, n_blk, wide), F32), sem(N_SRC)]
    if save or load:
        scratch += [sem(2), sem(2)]
    passes = 2 + fwd + bwd * (4 + 2 * own)
    flops = 2 * d * ff * passes * n_blk * N_SRC * 2
    hoist = 1300 if not own else 640 if load else 750 if save else 950
    picks = [[i for _, i in u] if u else None, [i for _, i in dy] if bwd else None]
    cfg = (fwd, bwd, own, layer, n_blk, d, ff, n_exp, picks, row_id, list_len, p_f32, len(aliases),
           None if got is None else 1 - layer)
    return pl.pallas_call(
        functools.partial(expert_kernel, cfg),
        out_shape=out_shape,
        in_specs=[any_space] * len(operands),
        out_specs=[any_space] * len(out_shape),
        scratch_shapes=scratch,
        input_output_aliases=aliases,
        compiler_params=pltpu.CompilerParams(
            vmem_limit_bytes=VMEM_LIMIT),
        cost_estimate=pl.CostEstimate(flops=flops, bytes_accessed=3 * 2 * n_exp * d * ff, transcendentals=0),
        name=f"experts_{'f' if fwd else ''}{'b' if bwd else ''}_{'own' if own else 'other'}_{layer}",
    )(*operands)


def place_kernel(layer, n_exp, at, tab_hbm, got_ref, *refs):
    outs, (tab_ref, buf, tab_sem, in_sem, out_sem) = refs[3:6], refs[6:]
    table = pltpu.make_async_copy(tab_hbm.at[pl.ds((layer * TAB_ROWS + ROW_PARTNER) * LANES, LANES)], tab_ref, tab_sem)
    table.start()
    reads = [pltpu.make_async_copy(got_ref.at[i], buf.at[i], in_sem.at[i]) for i in range(n_exp)]
    for read in reads:
        read.start()
    writes = []
    table.wait()
    for i, read in enumerate(reads):
        read.wait()
        e = tab_ref[at + i]
        for k, out in enumerate(outs):
            writes.append(pltpu.make_async_copy(buf.at[i, k], out.at[layer, e], out_sem.at[i, k]))
            writes[-1].start()
    for write in writes:
        write.wait()


def place(tab, at, layer, got, finals):
    n_exp = got.shape[0]
    return pl.pallas_call(
        functools.partial(place_kernel, layer, n_exp, at),
        out_shape=[jax.ShapeDtypeStruct(f.shape, f.dtype) for f in finals],
        in_specs=[any_space] * 5, out_specs=[any_space] * 3,
        scratch_shapes=[pltpu.SMEM((LANES,), I32), pltpu.VMEM(got.shape, got.dtype), pltpu.SemaphoreType.DMA,
                        pltpu.SemaphoreType.DMA((n_exp,)), pltpu.SemaphoreType.DMA((n_exp, 3))],
        input_output_aliases={2: 0, 3: 1, 4: 2},
        compiler_params=pltpu.CompilerParams(vmem_limit_bytes=VMEM_LIMIT),
        cost_estimate=pl.CostEstimate(flops=0, bytes_accessed=4 * got.size, transcendentals=0),
        name=f"place_{layer}",
    )(tab, got, *finals)


def peer(rel):
    return {name: (lax.axis_index(name) + ((rel >> bit) & 1)) % 2 for bit, name in enumerate(("ep", "core", "x"))}


def meet(rels):
    barrier = pltpu.get_barrier_semaphore()
    for rel in rels:
        pl.semaphore_signal(barrier, inc=1, device_id=peer(rel), device_id_type=MESH)
    pl.semaphore_wait(barrier, len(rels))


def remote(src, dst, send, recv, rel):
    return pltpu.make_async_remote_copy(src_ref=src, dst_ref=dst, send_sem=send, recv_sem=recv,
                                        device_id=peer(rel), device_id_type=MESH)


def share_kernel(n_rel, mine_ref, all_ref, send_sem, recv_sem):
    meet(range(1, n_rel))
    copies = [remote(mine_ref, all_ref.at[rel], send_sem.at[rel], recv_sem.at[rel], rel) for rel in range(1, n_rel)]
    for copy in copies:
        copy.start()
    all_ref[0] = mine_ref[...]
    for copy in copies:
        copy.wait()


def share(mine, n_rel):
    return pl.pallas_call(
        functools.partial(share_kernel, n_rel),
        out_shape=jax.ShapeDtypeStruct((n_rel,) + mine.shape, mine.dtype),
        in_specs=[in_vmem],
        out_specs=in_vmem,
        scratch_shapes=[pltpu.SemaphoreType.DMA((n_rel,)), pltpu.SemaphoreType.DMA((n_rel,))],
        compiler_params=pltpu.CompilerParams(collective_id=0, has_side_effects=True),
        cost_estimate=pl.CostEstimate(flops=10 ** 7, bytes_accessed=mine.size * 4 * n_rel, transcendentals=0),
        name="share_lists",
    )(mine)


def blocks_kernel(cfg, *refs):
    n_chunk, reduce, back, d, sizes = cfg
    refs = list(refs)
    take = lambda n: [refs.pop(0) for _ in range(n)]
    parts = take(N_SRC)
    m_ref = take(1)[0]
    list_refs, left_ref = take(2) if sizes else (), take(1)[0] if back else None
    o_total, o_a, o_b = take(3)
    plan_refs, grad_ref = take(3) if sizes else (), take(1)[0] if back else None
    in_f, in_b, got_f, s_wire, r_wire, u_wire, y_wire, t_buf, u_buf, y_buf, load, send, recv, put = take(14)
    n_rows = t_buf.shape[0] // n_chunk
    cut = [pl.ds(k * n_rows, n_rows) for k in range(n_chunk)]
    thin = [pl.ds(k * n_rows // 2, n_rows // 2) for k in range(n_chunk)]
    side = lax.broadcasted_iota(I32, (n_rows // 2, LANES), 1) < LANES // 2
    tiles = d // LANES
    turn = lambda v: pltpu.roll(v, LANES // 2, 1)
    lanes = lambda v, j: v[:, LANES * j:LANES * (j + 1)]

    def pack(wire, k, value):
        top, low = value[:n_rows // 2], value[n_rows // 2:]
        turned = [turn(lanes(low, j)) for j in range(tiles + 1)]
        parts = [lanes(top, j) for j in range(tiles)] + [jnp.where(side, lanes(top, tiles), turned[0])]
        parts += [jnp.where(side, turned[j], turned[j + 1]) for j in range(tiles)]
        for j, part in enumerate(parts):
            wire[thin[k], LANES * j:LANES * (j + 1)] = part.astype(BF16)

    def unpack(wire, k):
        value = wire[thin[k], :].astype(F32)
        turned = [turn(lanes(value, tiles + j)) for j in range(tiles + 1)]
        top = [lanes(value, j) for j in range(tiles)] + [jnp.where(side, lanes(value, tiles), 0.0)]
        low = [jnp.where(side, turned[j], turned[j + 1]) for j in range(tiles)] + [jnp.where(side, turned[tiles], 0.0)]
        return jnp.concatenate([jnp.concatenate(top, axis=1), jnp.concatenate(low, axis=1)], axis=0)

    chunks = range(n_chunk)
    loads = {}
    for i, part in enumerate(parts[:2] if reduce else parts):
        buf = in_f.at[i] if reduce or i == 0 else in_b.at[i - 1]
        for k in chunks:
            loads[i, k] = pltpu.make_async_copy(part.at[cut[k]], buf.at[cut[k]], load.at[i, k])
    order = (1, 0) if reduce else range(N_SRC)
    for i in order:
        for k in chunks:
            loads[i, k].start()
    u_buf[...] = jnp.zeros(u_buf.shape, BF16)
    meet((Y, CORE))
    links = []
    copy_in = pltpu.make_async_copy

    def link(src, dst, rel, cut=cut):
        n = len(links)
        links.append([remote(src.at[cut[k]], dst.at[cut[k]], send.at[n, k], recv.at[n, k], rel) for k in chunks])
        return links[-1]

    if reduce:
        first = link(parts[3], got_f.at[1], CORE)
        second = link(parts[2], got_f.at[0], CORE)
        over = link(s_wire, r_wire, Y, thin)
        for copies in (first, second):
            for copy in copies:
                copy.start()
        for k in chunks:
            loads[1, k].wait()
            first[k].wait_recv()
            pack(s_wire, k, in_f[1, cut[k], :] + got_f[1, cut[k], :])
            over[k].start()
    to_y = link(u_wire, y_wire, Y, thin)
    to_core = link(u_buf, o_b.at[0], CORE)
    puts = []
    for k in chunks:
        if reduce:
            loads[0, k].wait()
            second[k].wait_recv()
            over[k].wait_recv()
            total = in_f[0, cut[k], :] + got_f[0, cut[k], :] + unpack(r_wire, k)
        else:
            for i in range(N_SRC):
                loads[i, k].wait()
            total = in_f[0, cut[k], :]
            for i in range(N_SRC - 1):
                total = total + in_b[i, cut[k], :].astype(F32)
        total = total.astype(BF16)
        t_buf[cut[k], :] = total
        dims = (((1,), (1 if back else 0,)), ((), ()))
        mixed = lax.dot_general(total[:, :d], m_ref[...], dims, preferred_element_type=F32)
        u_buf[cut[k], 0:d] = (total[:, :d].astype(F32) + mixed).astype(BF16)
        pack(u_wire, k, u_buf[cut[k], :].astype(F32))
        to_y[k].start()
        to_core[k].start()
        puts.append(pltpu.make_async_copy(u_buf.at[cut[k]], o_a.at[0, cut[k]], put.at[0, k]))
        puts.append(pltpu.make_async_copy(t_buf.at[cut[k]], o_total.at[cut[k]], put.at[1, k]))
        for copy in puts[-2:]:
            copy.start()
    if sizes:
        plan_kernel(*sizes, *list_refs, *plan_refs)
    if back:
        grad_ref[...] = lax.dot_general(left_ref[:, :d], t_buf[:, :d], (((0,), (0,)), ((), ())), preferred_element_type=F32)
    on = link(y_buf, o_b.at[1], CORE)
    for k in chunks:
        to_y[k].wait_recv()
        y_buf[cut[k], :] = unpack(y_wire, k).astype(BF16)
        on[k].start()
        puts.append(copy_in(y_buf.at[cut[k]], o_a.at[1, cut[k]], put.at[2, k]))
        puts[-1].start()
    waited = [to_y] + ([first, second, over] if reduce else [])
    for copies in links:
        for copy in copies:
            if any(copies is w for w in waited):
                copy.wait_send()
            else:
                copy.wait()
    for copy in puts:
        copy.wait()


def complete_blocks(parts, m, reduce, back, ident, sizes=None, lists=(), left=(), n_chunk=4):
    n_blk, wide = parts[0].shape
    d = m.shape[0]
    sem = lambda *s: pltpu.SemaphoreType.DMA(s)
    pair = jax.ShapeDtypeStruct((2, n_blk, wide), BF16)
    extra = plan_shapes(sizes) if sizes else []
    extra += [jax.ShapeDtypeStruct((d, d), F32)] * len(left)
    buf = lambda n, dt: pltpu.VMEM((n, n_blk, wide) if n else (n_blk, wide), dt)
    return pl.pallas_call(
        functools.partial(blocks_kernel, (n_chunk, reduce, back, d, sizes)),
        out_shape=[jax.ShapeDtypeStruct((n_blk, wide), BF16)] + [pair] * 2 + extra,
        in_specs=[any_space] * N_SRC + [in_vmem] * (1 + len(lists) + len(left)),
        out_specs=[any_space] * 3 + [in_vmem] * len(extra),
        scratch_shapes=[buf(2, F32), buf(3, BF16), buf(2, F32)] + [pltpu.VMEM((n_blk // 2, 2 * d), BF16)] * 4 + [
            buf(0, BF16), buf(0, BF16), buf(0, BF16), sem(4, n_chunk), sem(6, n_chunk), sem(6, n_chunk), sem(3, n_chunk)],
        compiler_params=pltpu.CompilerParams(collective_id=ident, has_side_effects=True, vmem_limit_bytes=VMEM_LIMIT),
        cost_estimate=pl.CostEstimate(flops=10 ** 8, bytes_accessed=n_blk * wide * 40, transcendentals=0),
        name=f"complete_blocks_{ident}",
    )(*parts, m, *lists, *left)


def solution(mesh):
    ep_size, dp_size = mesh.shape['ep'], mesh.shape['dp']
    sub = Mesh(mesh.devices.reshape(ep_size, dp_size // 2, 2), ('ep', 'x', 'core'))
    tok_axes = ('x', 'core', 'ep')
    tok_spec = P(tok_axes, None)
    route_spec = P(None, tok_axes, None)
    whole_spec = P(None, None, None)
    expert_spec = P(None, 'ep', None, None)
    flip = [(0, 1), (1, 0)]
    move = lambda v, axis: lax.ppermute(v, axis, flip)
    move_diag = lambda v: lax.ppermute(v, ('ep', 'core'), [(0, 3), (1, 2), (2, 1), (3, 0)])
    fence = lax.optimization_barrier

    def device_step(tokens, d_out, expert_ids, gate_vals, w_mix, w_gate, w_up, w_down):
        n_layers, d = w_mix.shape[0], w_mix.shape[1]
        n_tok = tokens.shape[0]
        top = expert_ids.shape[2]
        n_local = w_gate.shape[1]
        n_exp = n_local * ep_size
        n = n_tok * top
        n_rel = 2 * N_SRC
        wide = cdiv(d, LANES) * LANES
        weights = (jnp.swapaxes(w_gate, 2, 3), jnp.swapaxes(w_up, 2, 3), w_down)
        pad = lambda v: jnp.pad(v, ((0, 0), (0, wide - d)))
        send_three = lambda p: [move(p[1], 'ep'), move(p[2], 'core'), move_diag(p[3])]

        def own_sum(p, got):
            return sum([g.astype(F32) for g in got], p)[:, :d].astype(BF16)

        one = lambda v: v.reshape(1, n_tok, wide)
        pairs = lambda a, b: [(a, 0), (a, 1), (b, 0), (b, 1)]

        one = lambda v: v.reshape(1, n_tok, wide)
        pairs = lambda a, b: [(a, 0), (a, 1), (b, 0), (b, 1)]
        singles = lambda *v: [(one(a), 0) for a in v]

        same = jnp.eye(d, dtype=BF16)
        u0 = (jnp.dot(tokens, pad(same), preferred_element_type=F32)
              + jnp.dot(tokens, pad(w_mix[0]), preferred_element_type=F32)).astype(BF16)
        u0_y, u0_c = move(u0, 'ep'), move(u0, 'core')
        lists = [sorted_list(expert_ids[l], gate_vals[l]) for l in range(n_layers)]
        counts = jnp.sum((expert_ids.transpose(0, 2, 1).reshape(n_layers, n, 1) == jnp.arange(n_exp, dtype=I32)).astype(F32), axis=1)
        packed = jnp.concatenate([jnp.concatenate([v[0] for v in lists] + [v[1] for v in lists]).reshape(-1, LANES),
                                  jnp.pad(counts, ((0, 8 - n_layers), (0, LANES - n_exp)))], axis=0)
        dy = pad(d_out)
        packed, dy = fence((packed, dy))
        shared = share(packed, N_SRC)
        u0_y, u0_c, dy, shared, w_mix = fence((u0_y, u0_c, dy, shared, w_mix))
        u0_d = move(u0_y, 'core')
        shared_x = move(shared, 'x')
        dy_y, dy_x = move(dy, 'ep'), move(dy, 'x')
        sizes = (n_layers, n_local, n_tok, n // LANES)
        routes = plan(shared, shared, sizes)
        u0_half = singles(u0, u0_y, u0_c, u0_d)
        add = lambda a, b: a.astype(F32) + b.astype(F32)
        to_chips = lambda v: [move(v, 'ep'), move(v, 'x'), lax.ppermute(v, ('ep', 'x'), [(0, 3), (1, 2), (2, 1), (3, 0)])]
        of_chips = lambda v, t: (add(v, t[0]) + add(t[1], t[2])).astype(BF16)
        piece = first_piece(n_local // 2)
        *part, ab0, xu0 = run_experts(routes, 0, u0_half, None, weights, None, None, True, True, p_f32=True)
        dy_y, dy_x, shared_x, part = fence((dy_y, dy_x, shared_x, part))
        dy_c, dy_d, dy_xy, dy_xc = move(dy, 'core'), move(dy_y, 'core'), move(dy_y, 'x'), move(dy_x, 'core')
        y0, u1_a, u1_b, *routes_x = complete_blocks(part, w_mix[1], True, False, 1, sizes, (shared, shared_x))
        routes_x = flat(*routes_x)
        dy_c, dy_d, dy_xy, dy_xc, u0_p, u0_q, y0, u1_a, u1_b = fence(
            (dy_c, dy_d, dy_xy, dy_xc, u0, u0_y, y0, u1_a, u1_b))
        dy_xd = move(dy_xy, 'core')
        u1_xa = move(u1_a, 'x')
        out = run_experts(routes, 1, pairs(u1_a, u1_b), singles(dy, dy_y, dy_c, dy_d), weights, None, None, True, True)
        u1_xa, dy_xd, u0_p, u0_q, out = fence((u1_xa, dy_xd, u0_p, u0_q, out))
        y_part, du_part, g1 = out[:4], out[4:8], out[8]
        u1_xb = move(u1_xa, 'core')
        got = send_three(du_part)
        u0_x, u0_xy = move(u0_p, 'x'), move(u0_q, 'x')
        out = run_experts(routes_x, 1, pairs(u1_xa, u1_xb), singles(dy_x, dy_xy, dy_xc, dy_xd), weights, g1, None,
                          False, False)
        got, u0_x, u0_xy, out = fence((got, u0_x, u0_xy, out))
        *finals, sent_a, sent_b = out
        got1 = [move(sent_a, 'core'), move(sent_b, 'core')]
        du1, dx_a, dx_b, g_mix1 = complete_blocks([du_part[0], *got], w_mix[1], False, True, 2, left=(y0,))
        tx = lambda x, du: jnp.einsum('td,te->de', x, du, preferred_element_type=F32)
        dx_a, y_part, got1, u0_x, u0_xy, g_mix1 = fence((dx_a, y_part, got1, u0_x, u0_xy, g_mix1))
        dx_xa = move(dx_a, 'x')
        part1 = g_mix1.astype(BF16)
        theirs1 = to_chips(part1)
        got_y = send_three(y_part)
        u0_xc, u0_xd = move(u0_x, 'core'), move(u0_xy, 'core')
        out = run_experts(routes, 0, None, pairs(dx_a, dx_b), weights, None, finals, False, True, got=got1, kept=(ab0, xu0))
        dx_xa, got_y, u0_xc, u0_xd, theirs1, out = fence((dx_xa, got_y, u0_xc, u0_xd, theirs1, out))
        du_part, g0, finals = out[:4], out[4], out[5:]
        dx_xb = move(dx_xa, 'core')
        got = send_three(du_part)
        part1 = of_chips(part1, theirs1)
        theirs1 = move(part1, 'core')
        du_part, dx_xb, part1 = fence((du_part, dx_xb, part1))
        out = run_experts(routes_x, 0, singles(u0_x, u0_xy, u0_xc, u0_xd), pairs(dx_xa, dx_xb), weights, g0, finals,
                          False, False)
        got, theirs1, got_y, y_own, out = fence((got, theirs1, got_y, y_part[0], out))
        *finals, sent_a, sent_b = out
        got_a, got_b = move(sent_a, 'core'), move(sent_b, 'core')
        du0 = own_sum(du_part[0], got)
        part0 = tx(tokens, du0).astype(BF16)
        theirs0 = to_chips(part0)
        turned = lambda v, w: jnp.einsum('te,de->dt', v, w, preferred_element_type=F32)
        dx0 = (turned(du0, same) + turned(du0, w_mix[0])).astype(BF16)
        y1 = turned(own_sum(y_own, got_y), same).astype(BF16)
        dx0, y1, got_a, finals = fence((dx0, y1, got_a, finals))
        finals = place(routes[0], 0, 0, got_a, finals)
        dx0, got_b, finals = fence((dx0, got_b, finals))
        finals = place(routes[0], piece, 0, got_b, finals)
        theirs0, finals = fence((theirs0, finals))
        total0 = of_chips(part0, theirs0)
        g_mix = jnp.stack([add(total0, move(total0, 'core')), add(part1, theirs1)]).astype(BF16)
        return (y1.T, dx0.T, g_mix, jnp.swapaxes(finals[0], 2, 3), jnp.swapaxes(finals[1], 2, 3), finals[2])

    return jax.shard_map(device_step, mesh=sub,
                         in_specs=(tok_spec, tok_spec, route_spec, route_spec, whole_spec,
                                   expert_spec, expert_spec, expert_spec),
                         out_specs=(tok_spec, tok_spec, whole_spec, expert_spec, expert_spec, expert_spec),
                         check_vma=False)
```

```python
import functools

import jax
import jax.numpy as jnp
from jax import lax
from jax.experimental import pallas as pl
from jax.experimental.pallas import tpu as pltpu
from jax.sharding import Mesh, PartitionSpec as P

F32, BF16, I32 = jnp.float32, jnp.bfloat16, jnp.int32
MESH = pl.DeviceIdType.MESH
ROWS = 384
GRP = 8
PITCH = 9
DEPTH = 3
FULL = 8
HALF = 4
CAP_FACTOR = 3
LANES = 128
N_SRC = 4
Y, CORE, X = 1, 2, 4
VMEM_LIMIT = 62 * 1024 * 1024
PER_TILE = ROWS // GRP
ROW_BOUND, ROW_GOFF, ROW_EXPERT, ROW_PARTNER, TAB_ROWS = 32, 33, 34, 35, 40
SLOT_GROUPS = 256


def cdiv(a, b):
    return (a + b - 1) // b


def first_piece(n_exp):
    return n_exp * 5 // 8


def spans(d):
    return [(LANES * j, min(LANES, d - LANES * j)) for j in range(cdiv(d, LANES))]


any_space = pl.BlockSpec(memory_space=pl.ANY)
in_vmem = pl.BlockSpec(memory_space=pltpu.VMEM)


def sorted_list(expert_ids, gate_vals):
    n_tok, top = expert_ids.shape
    n = n_tok * top
    keys = expert_ids.T.reshape(n) * n + jnp.arange(n, dtype=I32)
    keys, gates = lax.sort((keys, gate_vals.T.reshape(n)), num_keys=1, is_stable=False)
    return (keys % n_tok).astype(F32), gates


def plan_kernel(n_layers, n_local, n_tok, list_rows, deal_ref, all_ref, tab_ref, idx_ref, gate_ref):
    n_mine = n_local // 2
    core, ep = lax.axis_index('core'), lax.axis_index('ep')
    list_len = list_rows * LANES
    lane = lambda n: lax.broadcasted_iota(I32, (n, LANES), 1).astype(F32)
    sub = lambda n: lax.broadcasted_iota(I32, (n, LANES), 0).astype(F32)
    over_lanes = lambda v: jnp.sum(v, axis=1, keepdims=True)
    over_subs = lambda v: jnp.sum(v, axis=0, keepdims=True)
    l16, s16 = lane(n_mine), sub(n_mine)
    groups = lambda c: jnp.floor((c + (GRP - 0.5)) * (1.0 / GRP))
    for l in range(n_layers):
        cnt = all_ref[:, 2 * n_layers * list_rows + l, :]
        ends = cnt
        step = 1
        while step < 2 * n_local:
            ends = ends + jnp.where(lane(N_SRC) >= step, pltpu.roll(ends, step, 1), 0.0)
            step *= 2
        starts = ends - cnt
        second = (ep > 0)
        local = lambda v: jnp.where(lane(N_SRC) < n_local, jnp.where(second, pltpu.roll(v, LANES - n_local, 1), v), 0.0)
        cnt, starts = local(cnt), local(starts)
        tiles = jnp.floor((over_subs(groups(local(deal_ref[:, 2 * n_layers * list_rows + l, :]))) + (PER_TILE - 0.5))
                          * (1.0 / PER_TILE))
        load = jnp.where(lane(1) < n_local, jnp.maximum(1.0, tiles), -1.0)
        wide = jnp.broadcast_to(load, (n_local, LANES))
        col = over_lanes(jnp.where(lane(n_local) == sub(n_local), wide, 0.0))
        ahead = (col > wide) | ((col == wide) & (sub(n_local) < lane(n_local)))
        rank = over_subs(jnp.where(ahead, 1.0, 0.0))
        odd = s16 - 2.0 * jnp.floor(s16 * 0.5 + 0.25)
        flip = jnp.where(core > 0, 1.0 - odd, odd)
        dealt = lambda f: (jnp.broadcast_to(rank, (n_mine, LANES)) == 2.0 * s16 + f) & (l16 < n_local)
        pick = dealt(flip)
        choose = lambda p, row: over_lanes(jnp.where(p, jnp.broadcast_to(row, (n_mine, LANES)), 0.0))
        mine = lambda row: choose(pick, row)
        as_row = lambda c: over_subs(jnp.where(l16 == s16, c, 0.0))
        experts = as_row(mine(lane(1)))
        partner = as_row(choose(dealt(1.0 - flip), lane(1)))
        at = l * TAB_ROWS
        off = jnp.zeros((n_mine, 1), F32)
        pos = [jnp.zeros((n_mine, LANES), F32) for _ in range(SLOT_GROUPS // LANES)]
        for s in range(N_SRC):
            c, st = mine(cnt[s:s + 1]), mine(starts[s:s + 1]) + float(s * list_len)
            ng = groups(c)
            for i in range(len(pos)):
                rel = l16 + float(LANES * i) - off
                code = (st + GRP * rel) * 16.0 + jnp.minimum(float(GRP), c - GRP * rel)
                pos[i] = jnp.where((rel >= 0) & (rel < ng), code, pos[i])
            off = off + ng
        for i in range(len(pos)):
            tab_ref[pl.ds(at + i, n_mine, stride=len(pos)), :] = pos[i].astype(I32)
        n_tiles = jnp.maximum(1.0, jnp.floor((off + (PER_TILE - 0.5)) * (1.0 / PER_TILE)))
        bounds = over_subs(jnp.where(s16 < l16, n_tiles, 0.0))
        before = over_lanes(jnp.where(l16 == s16, jnp.broadcast_to(bounds, (n_mine, LANES)), 0.0))
        t = jnp.minimum(l16, over_subs(jnp.broadcast_to(n_tiles, (n_mine, LANES))) - 1.0)
        inside = (t >= before) & (t < before + n_tiles)
        goff = over_subs(jnp.where(inside, s16 * float(SLOT_GROUPS) + (t - before) * float(PER_TILE), 0.0))
        rows = [(ROW_BOUND, bounds), (ROW_GOFF, goff), (ROW_EXPERT, experts), (ROW_PARTNER, partner)]
        for row, value in rows:
            tab_ref[at + row:at + row + 1, :] = value.astype(I32)
    for l in range(n_layers):
        pad = l * (N_SRC * list_rows + 8) + N_SRC * list_rows
        gate_ref[pad:pad + 8, :] = jnp.zeros((8, LANES), F32)
        for s in range(N_SRC):
            to = (l * N_SRC + s) * list_rows
            toks = all_ref[s, l * list_rows:(l + 1) * list_rows, :]
            idx_ref[to:to + list_rows, :] = ((toks + float(s * n_tok)) * float(PITCH)).astype(I32)
            to = l * (N_SRC * list_rows + 8) + s * list_rows
            gate_ref[to:to + list_rows, :] = all_ref[s, (n_layers + l) * list_rows:(n_layers + l + 1) * list_rows, :]


def plan_shapes(sizes):
    n_layers, _, _, list_rows = sizes
    rows = (n_layers * TAB_ROWS, n_layers * N_SRC * list_rows, n_layers * (N_SRC * list_rows + 8))
    return [jax.ShapeDtypeStruct((n, LANES), dt) for n, dt in zip(rows, (I32, I32, F32))]


def flat(tab, idx, gates):
    return tab.reshape(-1), idx.reshape(-1), gates


def plan(deal, shared, sizes):
    return flat(*pl.pallas_call(
        functools.partial(plan_kernel, *sizes),
        out_shape=plan_shapes(sizes),
        in_specs=[in_vmem] * 2, out_specs=[in_vmem] * 3,
        cost_estimate=pl.CostEstimate(flops=10 ** 7, bytes_accessed=10 ** 6, transcendentals=0),
        name="plan",
    )(deal, shared))


def expert_kernel(cfg, *refs):
    fwd, bwd, own, layer, n_blk, d, ff, n_exp, picks, row_id, list_len, p_f32, n_alias, got_layer = cfg
    save, load = fwd and not bwd, own and bwd and not fwd
    refs = list(refs)
    take = lambda n: [refs.pop(0) for _ in range(n)]
    tab_hbm, idx_hbm, gate_hbm = take(3)
    u_pieces = take(N_SRC) if not load else []
    dy_pieces = take(N_SRC) if bwd else []
    wg_hbm, wu_hbm, wd_hbm = take(3)
    ab_hbm, xu_hbm = take(2) if load else (None, None)
    prev = take(1)[0] if bwd and not own else None
    got = take(2) if got_layer is not None else None
    take(n_alias)
    y_outs = take(N_SRC) if fwd else []
    du_outs = take(N_SRC) if bwd and own else []
    grad = take(1)[0] if bwd and own else None
    finals = take(3) if bwd and not own or got_layer is not None else None
    sent = take(2) if bwd and not own else None
    ab_hbm, xu_hbm = take(2) if save else (ab_hbm, xu_hbm)
    tab_ref, idx, gate_ref, land, table, gat = take(6)
    acc, row_ref = take(2) if own else (None, None)
    gu_ref, wd_ref, g_ref, x_u = take(4)
    x_c = take(1)[0] if bwd else None
    ab_ref = take(1)[0]
    dh_ref = take(1)[0] if bwd else None
    h_ref = take(1)[0]
    dab_ref, sums = take(2) if bwd else (None, None)
    keep_buf = take(1)[0] if bwd and not own else None
    got_buf = take(1)[0] if got is not None else None
    list_sem, land_sem, w_sem = take(3)
    sum_sem = take(1)[0] if bwd else None
    keep_sem = take(1)[0] if bwd and not own else None
    read_sem, write_sem = take(2) if got is not None else (None, None)
    stage_f, out_sem = take(2) if own else (None, None)
    ab_sem, xu_sem = take(2) if save or load else (None, None)

    split = first_piece(n_exp)
    copy = pltpu.make_async_copy
    cols = spans(d)
    lo = ff // 256 * 256
    hi = ff - lo
    dot = functools.partial(lax.dot_general, preferred_element_type=F32)
    nn = (((1,), (0,)), ((), ()))
    nt = (((1,), (1,)), ((), ()))
    tn = (((0,), (0,)), ((), ()))
    al = pl.multiple_of
    n_row = N_SRC * n_blk
    glane = lax.broadcasted_iota(I32, (GRP, LANES), 1)
    gsub = lax.broadcasted_iota(I32, (GRP, LANES), 0)

    def row_at(r):
        return pl.ds(r * PITCH, FULL)

    def codes_of(tile):
        at = ROW_GOFF * LANES + tile
        if own and bwd:
            return lambda q: tab_ref[tab_ref[at] + q]
        view = tab_ref.at[pl.ds(tab_ref[at], PER_TILE)]
        return lambda q: view[q]

    def gather(codes, q):
        ids = idx.at[pl.ds(codes(q) >> 4, GRP)]
        for k in range(GRP):
            gat[row_at(q * GRP + k), :] = table[pl.ds(ids[k], FULL), :]

    def gate_column(code):
        pos = code >> 4
        row, shift = pos >> 7, pos & (LANES - 1)
        want = glane == gsub + shift
        over = glane == gsub + (shift - LANES)
        here = gate_ref[pl.ds(row, GRP, stride=0), :]
        there = gate_ref[pl.ds(row + 1, GRP, stride=0), :]
        v = jnp.where(want, here, jnp.where(over, there, 0.0))
        return jnp.where(gsub < (code & 15), jnp.sum(v, axis=1, keepdims=True), 0.0)

    def scatter(codes, q):
        ids = idx.at[pl.ds(codes(q) >> 4, GRP)]
        new = []
        for k in range(GRP):
            at = pl.ds(ids[k], FULL)
            new.append((at, acc[at, :] + row_ref[row_at(q * GRP + k), :]))
        for at, value in reversed(new):
            acc[at, :] = value

    def keep_ab(t):
        ends = (ab_ref.at[t & 1], ab_hbm.at[t])
        return copy(*(ends if save else ends[::-1]), ab_sem.at[t & 1])

    def keep_xu(t):
        ends = (x_u.at[t & 1], xu_hbm.at[t])
        return copy(*(ends if save else ends[::-1]), xu_sem.at[t & 1])

    def of(ref, t):
        return ref.at[t & 1] if save or load else ref

    def convert(codes, t):
        for q in range(0, PER_TILE, 2):
            part = []
            for p in (q, q + 1):
                code = codes(p)
                rows = [gat[pl.ds(GRP * PITCH * p + j, GRP, stride=PITCH), :]
                        for j in range(HALF if load else 0, FULL if bwd else HALF)]
                real = gsub < (code & 15)
                gate = gate_column(code)
                g_ref[GRP * p:GRP * (p + 1), :] = gate
                us, dys = ([], rows) if load else (rows[:HALF], rows[HALF:])
                part.append([jnp.where(real, v, 0.0) for v in us] + [v * gate for v in dys])
            at = slice(GRP * q, GRP * (q + 2))
            for x, o in ((None if load else of(x_u, t), 0), (x_c, 0 if load else HALF)):
                if x is None:
                    continue
                for j, (c, w) in enumerate(cols):
                    both = jnp.concatenate([part[0][o + j], part[1][o + j]], axis=0)
                    x[at, c:c + w] = both[:, :w].astype(BF16)

    def put_rows(o, value, s0):
        value = value.astype(BF16).astype(F32)
        n = value.shape[0]
        for j, (c, w) in enumerate(cols):
            row_ref[pl.ds(PITCH * s0 + o + j, n, stride=PITCH), 0:w] = value[:, c:c + w] * g_ref[s0:s0 + n, 0:w]

    low = lax.broadcasted_iota(I32, (16, 2 * hi), 1) < hi

    def middle(a, b, dh):
        sig = 0.5 * jnp.tanh(0.5 * a) + 0.5
        act = a * sig
        h = act * b
        if dh is None:
            return h, None, None
        slope = sig * (1.0 + a * (1.0 - sig))
        return h, dh * b * slope, dh * act

    def weights(e, slot):
        at = (layer, tab_ref[ROW_EXPERT * LANES + e])
        moves = []
        for i, w in enumerate((wg_hbm, wu_hbm)):
            moves.append((w.at[at + (pl.ds(0, lo),)], gu_ref.at[slot, pl.ds(i * lo, lo)]))
            moves.append((w.at[at + (pl.ds(lo, hi),)], gu_ref.at[slot, pl.ds(2 * lo + i * hi, hi)]))
        moves.append((wd_hbm.at[at], wd_ref.at[slot]))
        return [copy(a, b, w_sem.at[slot, i]) for i, (a, b) in enumerate(moves)]

    def sums_in(e, slot):
        return copy(prev.at[e], sums.at[slot], sum_sem.at[slot])

    def sums_out(e, slot):
        return copy(sums.at[slot], grad.at[e], sum_sem.at[slot])

    def keeps(e, slot):
        at = (layer, tab_ref[ROW_EXPERT * LANES + e])
        return [copy(keep_buf.at[slot, i], finals[i].at[at], keep_sem.at[slot, i]) for i in range(3)]

    def send(e, slot, part):
        return copy(keep_buf.at[slot], sent[part].at[e - part * split], keep_sem.at[slot, 3])

    def read(e, slot, part=0):
        return copy(got[part].at[e - part * split], got_buf.at[slot], read_sem.at[slot])

    def writes(e, slot):
        to = tab_ref[TAB_ROWS * LANES + e]
        return [copy(got_buf.at[slot, i], finals[i].at[got_layer, to], write_sem.at[slot, i]) for i in range(3)]

    def start(moves):
        for m in moves:
            m.start()

    def wait(moves):
        for m in moves:
            m.wait()

    n_tab = TAB_ROWS * LANES
    lists = [copy(tab_hbm.at[pl.ds(row_id * n_tab, n_tab)], tab_ref.at[pl.ds(0, n_tab)], list_sem.at[0]),
             copy(idx_hbm.at[pl.ds(row_id * N_SRC * list_len, N_SRC * list_len)], idx.at[pl.ds(0, N_SRC * list_len)],
                  list_sem.at[1]),
             copy(gate_hbm.at[pl.ds(row_id * gate_ref.shape[0], gate_ref.shape[0])], gate_ref, list_sem.at[2])]
    if got is not None:
        at = (got_layer * TAB_ROWS + ROW_PARTNER) * LANES
        lists.append(copy(tab_hbm.at[pl.ds(at, LANES)], tab_ref.at[pl.ds(n_tab, LANES)], list_sem.at[3]))
    start(lists)
    pieces = []
    for s in range(N_SRC):
        if not load:
            pieces.append((u_pieces[s], picks[0][s], s, 0, fwd))
        if bwd:
            pieces.append((dy_pieces[s], picks[1][s], s, HALF, own))
    lands = [copy(ref.at[pick], land.at[i % N_SRC], land_sem.at[i % N_SRC]) for i, (ref, pick, *_) in enumerate(pieces)]
    start(lands[:N_SRC])
    lists[0].wait()
    for e in range(DEPTH - 1):
        start(weights(e, e))
        if bwd and not own:
            sums_in(e, e).start()
    if got is not None:
        lists[3].wait()
        read(0, 0).start()
    if own:
        def clear(c, _):
            for k in range(4):
                acc[pl.ds(al(c * 1152 + 288 * k, 8), 288), :] = jnp.zeros((288, LANES), F32)
            return 0

        lax.fori_loop(0, acc.shape[0] // 1152, clear, 0)
        row_ref[...] = jnp.zeros(row_ref.shape, F32)
    rows = 256
    for i, (_, _, s, o, seed) in enumerate(pieces):
        lands[i].wait()

        def fill(c, _, i=i, o=o, seed=seed, s=s):
            r = al(c * rows, rows)
            for j in range(HALF):
                vals = land[i % N_SRC, pl.ds(r, rows), LANES * j:LANES * (j + 1)].astype(F32)
                to = pl.ds(PITCH * (s * n_blk + r) + o + j, rows, stride=PITCH)
                table[to, :] = vals
                if seed and s == 0:
                    acc[to, :] = vals
            return 0

        lax.fori_loop(0, n_blk // rows, fill, 0)
        if i + N_SRC < len(pieces):
            lands[i + N_SRC].start()
    wait(lists[1:3])
    for k in range(GRP):
        idx[N_SRC * list_len + k] = 0

    def first(q, _):
        gather(begin, 2 * q)
        gather(begin, 2 * q + 1)
        return 0

    begin = codes_of(0)
    lax.fori_loop(0, PER_TILE // 2, first, 0)
    convert(begin, 0)
    if save:
        keep_xu(0).start()
    if load:
        keep_ab(0).start()
        keep_xu(0).start()

    def expert(e, _):
        slot = e & 1
        deep = lax.rem(e, DEPTH)
        sum_slot = slot if own else deep
        wait(weights(e, deep))
        if bwd and not own:
            sums_in(e, deep).wait()
        if got is not None:
            read(0, slot).wait()
            start(writes(e, slot))

            @pl.when((e > 0) & (e < n_exp - 1))
            def _():
                wait(writes(e - 1, 1 - slot))

        @pl.when(e < n_exp - (DEPTH - 1))
        def _():
            ahead = lax.rem(e + DEPTH - 1, DEPTH)
            start(weights(e + DEPTH - 1, ahead))
            if bwd and not own:
                sums_in(e + DEPTH - 1, ahead).start()

        @pl.when(e < n_exp - 1)
        def _():
            if got is not None:
                for part in range(2):
                    @pl.when((e + 1 >= split) if part else (e + 1 < split))
                    def _(part=part):
                        read(e + 1, 1 - slot, part).start()

        if bwd and own:
            @pl.when(e > 1)
            def _():
                sums_out(e - 2, slot).wait()

            sums[slot] = jnp.zeros(sums.shape[1:], F32)

        def tile(t, _):
            if save:
                @pl.when(t > 1)
                def _():
                    keep_ab(t - 2).wait()

                @pl.when(t > 0)
                def _():
                    keep_xu(t - 1).wait()
            if load:
                keep_ab(t).wait()
                keep_xu(t).wait()
                keep_ab(t + 1).start()
                keep_xu(t + 1).start()
            ab, xu = of(ab_ref, t), of(x_u, t)
            before, after = codes_of(jnp.maximum(t - 1, 0)), codes_of(t + 1)
            for q in range(PER_TILE):
                if own:
                    scatter(before, q)
                gather(after, q)
            front = ROWS if own and bwd else ROWS // 2
            for s0 in range(0, ROWS, front):
                sl = slice(s0, s0 + front)
                if not load:
                    ab[sl, :] = dot(xu[sl, :], gu_ref[deep], nt)
                if bwd:
                    dh_ref[sl, :] = dot(x_c[sl, :], wd_ref[deep], nt)
            for r in range(0, ROWS, 16):
                rows = slice(r, r + 16)
                for c in range(0, lo, LANES):
                    h, da, db = middle(ab[rows, c:c + LANES], ab[rows, lo + c:lo + c + LANES],
                                       dh_ref[rows, c:c + LANES] if bwd else None)
                    h_ref[rows, c:c + LANES] = h.astype(BF16)
                    if bwd:
                        dab_ref[rows, c:c + LANES] = da.astype(BF16)
                        dab_ref[rows, lo + c:lo + c + LANES] = db.astype(BF16)
                a = ab[rows, 2 * lo:]
                b = pltpu.roll(a, hi, 1)
                dh = dh_ref[rows, lo:] if bwd else None
                if bwd:
                    dh = jnp.concatenate([dh, dh], axis=1)
                h, da, db = middle(a, b, dh)
                h_ref[rows, lo:] = h[:, :hi].astype(BF16)
                if bwd:
                    dab_ref[rows, 2 * lo:] = jnp.where(low, da, pltpu.roll(db, hi, 1)).astype(BF16)
            half = ROWS // 2
            for s0 in range(0, ROWS, half):
                sl = slice(s0, s0 + half)
                if fwd:
                    put_rows(0, dot(h_ref[sl, :], wd_ref[deep], nn), s0)
                if bwd and own:
                    put_rows(HALF, dot(dab_ref[sl, :], gu_ref[deep], nn), s0)
            if bwd:
                view = sums.at[sum_slot]
                view[0:2 * ff, :] += dot(dab_ref[...], xu[...], tn)
                view[2 * ff:, :] += dot(h_ref[...], x_c[...], tn)
            convert(after, t + 1)
            if save:
                keep_ab(t).start()
                keep_xu(t + 1).start()
            return 0

        lax.fori_loop(tab_ref[ROW_BOUND * LANES + e], tab_ref[ROW_BOUND * LANES + e + 1], tile, 0)
        if bwd and own:
            sums_out(e, slot).start()
        if bwd and not own:
            @pl.when(e > 1)
            def _():
                wait(keeps(e - 2, slot) + [send(0, slot, 0)])

            for i in range(2):
                keep_buf[slot, i, 0:lo, :] = sums[deep, i * lo:(i + 1) * lo, :].astype(BF16)
                keep_buf[slot, i, lo:, :] = sums[deep, 2 * lo + i * hi:2 * lo + (i + 1) * hi, :].astype(BF16)
            keep_buf[slot, 2] = sums[deep, 2 * ff:, :].astype(BF16)
            start(keeps(e, slot))
            for part in range(2):
                @pl.when((e >= split) if part else (e < split))
                def _(part=part):
                    send(e, slot, part).start()
        return 0

    lax.fori_loop(0, n_exp, expert, 0)
    ends = ((n_exp - 2, (n_exp - 2) % 2), (n_exp - 1, (n_exp - 1) % 2))
    n_tiles = tab_ref[ROW_BOUND * LANES + n_exp]
    if save:
        wait([keep_ab(n_tiles - 2), keep_ab(n_tiles - 1), keep_xu(n_tiles - 1)])
    if save or load:
        keep_xu(n_tiles).wait()
    if load:
        keep_ab(n_tiles).wait()
    if own:
        end = codes_of(tab_ref[ROW_BOUND * LANES + n_exp] - 1)
        lax.fori_loop(0, PER_TILE, lambda q, _: (scatter(end, q), 0)[1], 0)
        flights = {}
        for o, out in ((HALF, du_outs), (0, y_outs)):
            for s in range(N_SRC if out else 0):
                wide = s == 0 or p_f32
                stage = stage_f.at[s] if wide else land.at[s]
                if s in flights:
                    flights[s].wait()

                def fetch(c, _, stage=stage, s=s, o=o):
                    r = al(c * rows, rows)
                    for j in range(HALF):
                        at = pl.ds(PITCH * (s * n_blk + r) + o + j, rows, stride=PITCH)
                        stage[pl.ds(r, rows), LANES * j:LANES * (j + 1)] = acc[at, :].astype(stage.dtype)
                    return 0

                lax.fori_loop(0, n_blk // rows, fetch, 0)
                flights[s] = copy(stage, out[s], out_sem.at[s])
                flights[s].start()
        wait(flights.values())
        if bwd:
            for e, slot in ends:
                sums_out(e, slot).wait()
    else:
        for e, slot in ends:
            wait(keeps(e, slot) + [send(0, slot, 0)])
    if got is not None:
        for e, slot in ends:
            wait(writes(e, slot))


def run_experts(routes, layer, u, dy, weights, prev, finals, fwd, own, p_f32=False, got=None, kept=None):
    tab, idx, gates = routes
    bwd = dy is not None
    wg, wu, wd = weights
    save, load = fwd and not bwd, kept is not None
    n_blk, wide = (dy or u)[0][0].shape[-2:]
    n_layers, n_local, ff, d = wd.shape
    n_exp = n_local // 2
    row_id = layer
    list_len = idx.shape[0] // (n_layers * N_SRC)

    arrays = lambda pieces: [v for v, _ in pieces]
    operands = [tab, idx, gates] + ([] if load else arrays(u)) + (arrays(dy) if bwd else []) + [wg, wu, wd] + list(kept or ())
    out_shape, aliases = [], {}
    for use in (fwd, bwd and own):
        if use:
            out_shape += [jax.ShapeDtypeStruct((n_blk, wide), F32 if s == 0 or p_f32 else BF16) for s in range(N_SRC)]
    if bwd and own:
        out_shape.append(jax.ShapeDtypeStruct((n_exp, 3 * ff, d), F32))
    if bwd and not own:
        operands.append(prev)
    if got is not None:
        operands += got
    for i, f in enumerate(finals or ()):
        aliases[len(operands)] = len(out_shape) + i
        operands.append(f)
    if bwd and not own or finals:
        out_shape += [jax.ShapeDtypeStruct((n_layers, n_local, ff, d), BF16)] * 3
    if bwd and not own:
        out_shape += [jax.ShapeDtypeStruct((n, 3, ff, d), BF16) for n in (first_piece(n_exp), n_exp - first_piece(n_exp))]
    if save:
        most = n_exp * (SLOT_GROUPS // PER_TILE) + 2
        out_shape += [jax.ShapeDtypeStruct((most, ROWS, 2 * ff), F32), jax.ShapeDtypeStruct((most, ROWS, d), BF16)]
    sem = lambda *s: pltpu.SemaphoreType.DMA(s)
    mid = lambda n, dt: pltpu.VMEM((ROWS, n), dt)
    twin = lambda n, dt: pltpu.VMEM((2, ROWS, n), dt) if save or load else mid(n, dt)
    table, rows = pltpu.VMEM((PITCH * N_SRC * n_blk, LANES), F32), pltpu.VMEM((PITCH * ROWS, LANES), F32)
    scratch = [pltpu.SMEM(((TAB_ROWS + 1) * LANES,), I32), pltpu.SMEM((N_SRC * list_len + LANES,), I32),
               pltpu.VMEM((N_SRC * list_len // LANES + 8, LANES), F32), pltpu.VMEM((N_SRC, n_blk, wide), BF16)]
    scratch += [table, rows] * (1 + own)
    scratch += [pltpu.VMEM((DEPTH, 2 * ff, d), BF16), pltpu.VMEM((DEPTH, ff, d), BF16), mid(LANES, F32)]
    scratch += [twin(d, BF16)] + [mid(d, BF16)] * bwd + [twin(2 * ff, F32)] + [mid(ff, F32)] * bwd + [mid(ff, BF16)]
    scratch += [mid(2 * ff, BF16), pltpu.VMEM((2 if own else DEPTH, 3 * ff, d), F32)] * bwd
    if bwd and not own:
        scratch.append(pltpu.VMEM((2, 3, ff, d), BF16))
    if got is not None:
        scratch.append(pltpu.VMEM((2, 3, ff, d), BF16))
    scratch += [sem(4), sem(N_SRC), sem(DEPTH, 5)] + [sem(DEPTH)] * bwd
    if bwd and not own:
        scratch.append(sem(2, 4))
    if got is not None:
        scratch += [sem(2), sem(2, 3)]
    if own:
        scratch += [pltpu.VMEM((N_SRC if p_f32 else 1, n_blk, wide), F32), sem(N_SRC)]
    if save or load:
        scratch += [sem(2), sem(2)]
    passes = 2 + fwd + bwd * (4 + 2 * own)
    flops = 2 * d * ff * passes * n_blk * N_SRC * 2
    hoist = 1300 if not own else 640 if load else 750 if save else 950
    picks = [[i for _, i in u] if u else None, [i for _, i in dy] if bwd else None]
    cfg = (fwd, bwd, own, layer, n_blk, d, ff, n_exp, picks, row_id, list_len, p_f32, len(aliases),
           None if got is None else 1 - layer)
    return pl.pallas_call(
        functools.partial(expert_kernel, cfg),
        out_shape=out_shape,
        in_specs=[any_space] * len(operands),
        out_specs=[any_space] * len(out_shape),
        scratch_shapes=scratch,
        input_output_aliases=aliases,
        compiler_params=pltpu.CompilerParams(
            vmem_limit_bytes=VMEM_LIMIT),
        cost_estimate=pl.CostEstimate(flops=flops, bytes_accessed=3 * 2 * n_exp * d * ff, transcendentals=0),
        name=f"experts_{'f' if fwd else ''}{'b' if bwd else ''}_{'own' if own else 'other'}_{layer}",
    )(*operands)


def place_kernel(layer, n_exp, at, tab_hbm, got_ref, *refs):
    outs, (tab_ref, buf, tab_sem, in_sem, out_sem) = refs[3:6], refs[6:]
    table = pltpu.make_async_copy(tab_hbm.at[pl.ds((layer * TAB_ROWS + ROW_PARTNER) * LANES, LANES)], tab_ref, tab_sem)
    table.start()
    reads = [pltpu.make_async_copy(got_ref.at[i], buf.at[i], in_sem.at[i]) for i in range(n_exp)]
    for read in reads:
        read.start()
    writes = []
    table.wait()
    for i, read in enumerate(reads):
        read.wait()
        e = tab_ref[at + i]
        for k, out in enumerate(outs):
            writes.append(pltpu.make_async_copy(buf.at[i, k], out.at[layer, e], out_sem.at[i, k]))
            writes[-1].start()
    for write in writes:
        write.wait()


def place(tab, at, layer, got, finals):
    n_exp = got.shape[0]
    return pl.pallas_call(
        functools.partial(place_kernel, layer, n_exp, at),
        out_shape=[jax.ShapeDtypeStruct(f.shape, f.dtype) for f in finals],
        in_specs=[any_space] * 5, out_specs=[any_space] * 3,
        scratch_shapes=[pltpu.SMEM((LANES,), I32), pltpu.VMEM(got.shape, got.dtype), pltpu.SemaphoreType.DMA,
                        pltpu.SemaphoreType.DMA((n_exp,)), pltpu.SemaphoreType.DMA((n_exp, 3))],
        input_output_aliases={2: 0, 3: 1, 4: 2},
        compiler_params=pltpu.CompilerParams(vmem_limit_bytes=VMEM_LIMIT),
        cost_estimate=pl.CostEstimate(flops=0, bytes_accessed=4 * got.size, transcendentals=0),
        name=f"place_{layer}",
    )(tab, got, *finals)


def peer(rel):
    return {name: (lax.axis_index(name) + ((rel >> bit) & 1)) % 2 for bit, name in enumerate(("ep", "core", "x"))}


def meet(rels):
    barrier = pltpu.get_barrier_semaphore()
    for rel in rels:
        pl.semaphore_signal(barrier, inc=1, device_id=peer(rel), device_id_type=MESH)
    pl.semaphore_wait(barrier, len(rels))


def remote(src, dst, send, recv, rel):
    return pltpu.make_async_remote_copy(src_ref=src, dst_ref=dst, send_sem=send, recv_sem=recv,
                                        device_id=peer(rel), device_id_type=MESH)


def share_kernel(mine_ref, all_ref, send_sem, recv_sem):
    meet((Y, CORE))
    direct = [remote(mine_ref, all_ref.at[rel], send_sem.at[rel], recv_sem.at[rel], rel) for rel in (Y, CORE)]
    for copy in direct:
        copy.start()
    all_ref[0] = mine_ref[...]
    on = remote(all_ref.at[Y], all_ref.at[Y + CORE], send_sem.at[Y + CORE], recv_sem.at[Y + CORE], CORE)
    direct[0].wait_recv()
    on.start()
    direct[0].wait_send()
    direct[1].wait()
    on.wait()


def share(mine, n_rel):
    return pl.pallas_call(
        share_kernel,
        out_shape=jax.ShapeDtypeStruct((n_rel,) + mine.shape, mine.dtype),
        in_specs=[in_vmem],
        out_specs=in_vmem,
        scratch_shapes=[pltpu.SemaphoreType.DMA((n_rel,)), pltpu.SemaphoreType.DMA((n_rel,))],
        compiler_params=pltpu.CompilerParams(collective_id=0, has_side_effects=True),
        cost_estimate=pl.CostEstimate(flops=10 ** 7, bytes_accessed=mine.size * 4 * n_rel, transcendentals=0),
        name="share_lists",
    )(mine)


def blocks_kernel(cfg, *refs):
    n_chunk, reduce, back, d, sizes = cfg
    refs = list(refs)
    take = lambda n: [refs.pop(0) for _ in range(n)]
    parts = take(N_SRC)
    m_ref = take(1)[0]
    list_refs, left_ref = take(2) if sizes else (), take(1)[0] if back else None
    o_total, o_a, o_b = take(3)
    plan_refs, grad_ref = take(3) if sizes else (), take(1)[0] if back else None
    in_f, in_b, got_f, s_wire, r_wire, u_wire, y_wire, t_buf, u_buf, y_buf, load, send, recv, put = take(14)
    n_rows = t_buf.shape[0] // n_chunk
    cut = [pl.ds(k * n_rows, n_rows) for k in range(n_chunk)]
    thin = [pl.ds(k * n_rows // 2, n_rows // 2) for k in range(n_chunk)]
    side = lax.broadcasted_iota(I32, (n_rows // 2, LANES), 1) < LANES // 2
    tiles = d // LANES
    turn = lambda v: pltpu.roll(v, LANES // 2, 1)
    lanes = lambda v, j: v[:, LANES * j:LANES * (j + 1)]

    def pack(wire, k, value):
        top, low = value[:n_rows // 2], value[n_rows // 2:]
        turned = [turn(lanes(low, j)) for j in range(tiles + 1)]
        parts = [lanes(top, j) for j in range(tiles)] + [jnp.where(side, lanes(top, tiles), turned[0])]
        parts += [jnp.where(side, turned[j], turned[j + 1]) for j in range(tiles)]
        for j, part in enumerate(parts):
            wire[thin[k], LANES * j:LANES * (j + 1)] = part.astype(BF16)

    def unpack(wire, k):
        value = wire[thin[k], :].astype(F32)
        turned = [turn(lanes(value, tiles + j)) for j in range(tiles + 1)]
        top = [lanes(value, j) for j in range(tiles)] + [jnp.where(side, lanes(value, tiles), 0.0)]
        low = [jnp.where(side, turned[j], turned[j + 1]) for j in range(tiles)] + [jnp.where(side, turned[tiles], 0.0)]
        return jnp.concatenate([jnp.concatenate(top, axis=1), jnp.concatenate(low, axis=1)], axis=0)

    chunks = range(n_chunk)
    loads = {}
    for i, part in enumerate(parts[:2] if reduce else parts):
        buf = in_f.at[i] if reduce or i == 0 else in_b.at[i - 1]
        for k in chunks:
            loads[i, k] = pltpu.make_async_copy(part.at[cut[k]], buf.at[cut[k]], load.at[i, k])
    order = (1, 0) if reduce else range(N_SRC)
    for i in order:
        for k in chunks:
            loads[i, k].start()
    u_buf[...] = jnp.zeros(u_buf.shape, BF16)
    meet((Y, CORE))
    links = []
    copy_in = pltpu.make_async_copy

    def link(src, dst, rel, cut=cut):
        n = len(links)
        links.append([remote(src.at[cut[k]], dst.at[cut[k]], send.at[n, k], recv.at[n, k], rel) for k in chunks])
        return links[-1]

    if reduce:
        first = link(parts[3], got_f.at[1], CORE)
        second = link(parts[2], got_f.at[0], CORE)
        over = link(s_wire, r_wire, Y, thin)
        for copies in (first, second):
            for copy in copies:
                copy.start()
        for k in chunks:
            loads[1, k].wait()
            first[k].wait_recv()
            pack(s_wire, k, in_f[1, cut[k], :] + got_f[1, cut[k], :])
            over[k].start()
    to_y = link(u_wire, y_wire, Y, thin)
    to_core = link(u_buf, o_b.at[0], CORE)
    puts = []
    for k in chunks:
        if reduce:
            loads[0, k].wait()
            second[k].wait_recv()
            over[k].wait_recv()
            total = in_f[0, cut[k], :] + got_f[0, cut[k], :] + unpack(r_wire, k)
        else:
            for i in range(N_SRC):
                loads[i, k].wait()
            total = in_f[0, cut[k], :]
            for i in range(N_SRC - 1):
                total = total + in_b[i, cut[k], :].astype(F32)
        total = total.astype(BF16)
        t_buf[cut[k], :] = total
        dims = (((1,), (1 if back else 0,)), ((), ()))
        mixed = lax.dot_general(total[:, :d], m_ref[...], dims, preferred_element_type=F32)
        u_buf[cut[k], 0:d] = (total[:, :d].astype(F32) + mixed).astype(BF16)
        pack(u_wire, k, u_buf[cut[k], :].astype(F32))
        to_y[k].start()
        to_core[k].start()
        puts.append(pltpu.make_async_copy(u_buf.at[cut[k]], o_a.at[0, cut[k]], put.at[0, k]))
        puts.append(pltpu.make_async_copy(t_buf.at[cut[k]], o_total.at[cut[k]], put.at[1, k]))
        for copy in puts[-2:]:
            copy.start()
    if sizes:
        plan_kernel(*sizes, *list_refs, *plan_refs)
    if back:
        grad_ref[...] = lax.dot_general(left_ref[:, :d], t_buf[:, :d], (((0,), (0,)), ((), ())), preferred_element_type=F32)
    on = link(y_buf, o_b.at[1], CORE)
    for k in chunks:
        to_y[k].wait_recv()
        y_buf[cut[k], :] = unpack(y_wire, k).astype(BF16)
        on[k].start()
        puts.append(copy_in(y_buf.at[cut[k]], o_a.at[1, cut[k]], put.at[2, k]))
        puts[-1].start()
    waited = [to_y] + ([first, second, over] if reduce else [])
    for copies in links:
        for copy in copies:
            if any(copies is w for w in waited):
                copy.wait_send()
            else:
                copy.wait()
    for copy in puts:
        copy.wait()


def complete_blocks(parts, m, reduce, back, ident, sizes=None, lists=(), left=(), n_chunk=4):
    n_blk, wide = parts[0].shape
    d = m.shape[0]
    sem = lambda *s: pltpu.SemaphoreType.DMA(s)
    pair = jax.ShapeDtypeStruct((2, n_blk, wide), BF16)
    extra = plan_shapes(sizes) if sizes else []
    extra += [jax.ShapeDtypeStruct((d, d), F32)] * len(left)
    buf = lambda n, dt: pltpu.VMEM((n, n_blk, wide) if n else (n_blk, wide), dt)
    return pl.pallas_call(
        functools.partial(blocks_kernel, (n_chunk, reduce, back, d, sizes)),
        out_shape=[jax.ShapeDtypeStruct((n_blk, wide), BF16)] + [pair] * 2 + extra,
        in_specs=[any_space] * N_SRC + [in_vmem] * (1 + len(lists) + len(left)),
        out_specs=[any_space] * 3 + [in_vmem] * len(extra),
        scratch_shapes=[buf(2, F32), buf(3, BF16), buf(2, F32)] + [pltpu.VMEM((n_blk // 2, 2 * d), BF16)] * 4 + [
            buf(0, BF16), buf(0, BF16), buf(0, BF16), sem(4, n_chunk), sem(6, n_chunk), sem(6, n_chunk), sem(3, n_chunk)],
        compiler_params=pltpu.CompilerParams(collective_id=ident, has_side_effects=True, vmem_limit_bytes=VMEM_LIMIT),
        cost_estimate=pl.CostEstimate(flops=10 ** 8, bytes_accessed=n_blk * wide * 40, transcendentals=0),
        name=f"complete_blocks_{ident}",
    )(*parts, m, *lists, *left)


def solution(mesh):
    ep_size, dp_size = mesh.shape['ep'], mesh.shape['dp']
    sub = Mesh(mesh.devices.reshape(ep_size, dp_size // 2, 2), ('ep', 'x', 'core'))
    tok_axes = ('x', 'core', 'ep')
    tok_spec = P(tok_axes, None)
    route_spec = P(None, tok_axes, None)
    whole_spec = P(None, None, None)
    expert_spec = P(None, 'ep', None, None)
    flip = [(0, 1), (1, 0)]
    move = lambda v, axis: lax.ppermute(v, axis, flip)
    move_diag = lambda v: lax.ppermute(v, ('ep', 'core'), [(0, 3), (1, 2), (2, 1), (3, 0)])
    fence = lax.optimization_barrier

    def device_step(tokens, d_out, expert_ids, gate_vals, w_mix, w_gate, w_up, w_down):
        n_layers, d = w_mix.shape[0], w_mix.shape[1]
        n_tok = tokens.shape[0]
        top = expert_ids.shape[2]
        n_local = w_gate.shape[1]
        n_exp = n_local * ep_size
        n = n_tok * top
        n_rel = 2 * N_SRC
        wide = cdiv(d, LANES) * LANES
        weights = (jnp.swapaxes(w_gate, 2, 3), jnp.swapaxes(w_up, 2, 3), w_down)
        pad = lambda v: jnp.pad(v, ((0, 0), (0, wide - d)))
        send_three = lambda p: [move(p[1], 'ep'), move(p[2], 'core'), move_diag(p[3])]

        def own_sum(p, got):
            return sum([g.astype(F32) for g in got], p)[:, :d].astype(BF16)

        one = lambda v: v.reshape(1, n_tok, wide)
        pairs = lambda a, b: [(a, 0), (a, 1), (b, 0), (b, 1)]

        one = lambda v: v.reshape(1, n_tok, wide)
        pairs = lambda a, b: [(a, 0), (a, 1), (b, 0), (b, 1)]
        singles = lambda *v: [(one(a), 0) for a in v]

        same = jnp.eye(d, dtype=BF16)
        u0 = (jnp.dot(tokens, pad(same), preferred_element_type=F32)
              + jnp.dot(tokens, pad(w_mix[0]), preferred_element_type=F32)).astype(BF16)
        u0_y, u0_c = move(u0, 'ep'), move(u0, 'core')
        lists = [sorted_list(expert_ids[l], gate_vals[l]) for l in range(n_layers)]
        counts = jnp.sum((expert_ids.transpose(0, 2, 1).reshape(n_layers, n, 1) == jnp.arange(n_exp, dtype=I32)).astype(F32), axis=1)
        packed = jnp.concatenate([jnp.concatenate([v[0] for v in lists] + [v[1] for v in lists]).reshape(-1, LANES),
                                  jnp.pad(counts, ((0, 8 - n_layers), (0, LANES - n_exp)))], axis=0)
        dy = pad(d_out)
        packed, dy = fence((packed, dy))
        shared = share(packed, N_SRC)
        u0_y, u0_c, dy, shared, w_mix = fence((u0_y, u0_c, dy, shared, w_mix))
        u0_d = move(u0_y, 'core')
        shared_x = move(shared, 'x')
        dy_y, dy_x = move(dy, 'ep'), move(dy, 'x')
        sizes = (n_layers, n_local, n_tok, n // LANES)
        routes = plan(shared, shared, sizes)
        u0_half = singles(u0, u0_y, u0_c, u0_d)
        add = lambda a, b: a.astype(F32) + b.astype(F32)
        to_chips = lambda v: [move(v, 'ep'), move(v, 'x'), lax.ppermute(v, ('ep', 'x'), [(0, 3), (1, 2), (2, 1), (3, 0)])]
        of_chips = lambda v, t: (add(v, t[0]) + add(t[1], t[2])).astype(BF16)
        piece = first_piece(n_local // 2)
        *part, ab0, xu0 = run_experts(routes, 0, u0_half, None, weights, None, None, True, True, p_f32=True)
        dy_y, dy_x, shared_x, part = fence((dy_y, dy_x, shared_x, part))
        dy_c, dy_d, dy_xy, dy_xc = move(dy, 'core'), move(dy_y, 'core'), move(dy_y, 'x'), move(dy_x, 'core')
        y0, u1_a, u1_b, *routes_x = complete_blocks(part, w_mix[1], True, False, 1, sizes, (shared, shared_x))
        routes_x = flat(*routes_x)
        dy_c, dy_d, dy_xy, dy_xc, u0_p, u0_q, y0, u1_a, u1_b = fence(
            (dy_c, dy_d, dy_xy, dy_xc, u0, u0_y, y0, u1_a, u1_b))
        dy_xd = move(dy_xy, 'core')
        u1_xa = move(u1_a, 'x')
        out = run_experts(routes, 1, pairs(u1_a, u1_b), singles(dy, dy_y, dy_c, dy_d), weights, None, None, True, True)
        u1_xa, dy_xd, u0_p, u0_q, out = fence((u1_xa, dy_xd, u0_p, u0_q, out))
        y_part, du_part, g1 = out[:4], out[4:8], out[8]
        u1_xb = move(u1_xa, 'core')
        got = send_three(du_part)
        u0_x, u0_xy = move(u0_p, 'x'), move(u0_q, 'x')
        out = run_experts(routes_x, 1, pairs(u1_xa, u1_xb), singles(dy_x, dy_xy, dy_xc, dy_xd), weights, g1, None,
                          False, False)
        got, u0_x, u0_xy, out = fence((got, u0_x, u0_xy, out))
        *finals, sent_a, sent_b = out
        got1 = [move(sent_a, 'core'), move(sent_b, 'core')]
        du1, dx_a, dx_b, g_mix1 = complete_blocks([du_part[0], *got], w_mix[1], False, True, 2, left=(y0,))
        tx = lambda x, du: jnp.einsum('td,te->de', x, du, preferred_element_type=F32)
        dx_a, y_part, got1, u0_x, u0_xy, g_mix1 = fence((dx_a, y_part, got1, u0_x, u0_xy, g_mix1))
        dx_xa = move(dx_a, 'x')
        part1 = g_mix1.astype(BF16)
        theirs1 = to_chips(part1)
        got_y = send_three(y_part)
        u0_xc, u0_xd = move(u0_x, 'core'), move(u0_xy, 'core')
        out = run_experts(routes, 0, None, pairs(dx_a, dx_b), weights, None, finals, False, True, got=got1, kept=(ab0, xu0))
        dx_xa, got_y, u0_xc, u0_xd, theirs1, out = fence((dx_xa, got_y, u0_xc, u0_xd, theirs1, out))
        du_part, g0, finals = out[:4], out[4], out[5:]
        dx_xb = move(dx_xa, 'core')
        got = send_three(du_part)
        part1 = of_chips(part1, theirs1)
        theirs1 = move(part1, 'core')
        du_part, dx_xb, part1 = fence((du_part, dx_xb, part1))
        out = run_experts(routes_x, 0, singles(u0_x, u0_xy, u0_xc, u0_xd), pairs(dx_xa, dx_xb), weights, g0, finals,
                          False, False)
        got, theirs1, got_y, y_own, out = fence((got, theirs1, got_y, y_part[0], out))
        *finals, sent_a, sent_b = out
        got_a, got_b = move(sent_a, 'core'), move(sent_b, 'core')
        du0 = own_sum(du_part[0], got)
        part0 = tx(tokens, du0).astype(BF16)
        theirs0 = to_chips(part0)
        turned = lambda v, w: jnp.einsum('te,de->dt', v, w, preferred_element_type=F32)
        dx0 = (turned(du0, same) + turned(du0, w_mix[0])).astype(BF16)
        y1 = turned(own_sum(y_own, got_y), same).astype(BF16)
        dx0, y1, got_a, finals = fence((dx0, y1, got_a, finals))
        finals = place(routes[0], 0, 0, got_a, finals)
        dx0, got_b, finals = fence((dx0, got_b, finals))
        finals = place(routes[0], piece, 0, got_b, finals)
        theirs0, finals = fence((theirs0, finals))
        total0 = of_chips(part0, theirs0)
        g_mix = jnp.stack([add(total0, move(total0, 'core')), add(part1, theirs1)]).astype(BF16)
        return (y1.T, dx0.T, g_mix, jnp.swapaxes(finals[0], 2, 3), jnp.swapaxes(finals[1], 2, 3), finals[2])

    return jax.shard_map(device_step, mesh=sub,
                         in_specs=(tok_spec, tok_spec, route_spec, route_spec, whole_spec,
                                   expert_spec, expert_spec, expert_spec),
                         out_specs=(tok_spec, tok_spec, whole_spec, expert_spec, expert_spec, expert_spec),
                         check_vma=False)
```

```python
import functools

import jax
import jax.numpy as jnp
from jax import lax
from jax.experimental import pallas as pl
from jax.experimental.pallas import tpu as pltpu
from jax.sharding import Mesh, PartitionSpec as P

F32, BF16, I32 = jnp.float32, jnp.bfloat16, jnp.int32
MESH = pl.DeviceIdType.MESH
ROWS = 384
GRP = 8
PITCH = 9
DEPTH = 3
FULL = 8
HALF = 4
CAP_FACTOR = 3
LANES = 128
N_SRC = 4
Y, CORE, X = 1, 2, 4
VMEM_LIMIT = 62 * 1024 * 1024
PER_TILE = ROWS // GRP
ROW_BOUND, ROW_GOFF, ROW_EXPERT, ROW_PARTNER, TAB_ROWS = 32, 33, 34, 35, 40
SLOT_GROUPS = 256


def cdiv(a, b):
    return (a + b - 1) // b


def first_piece(n_exp):
    return n_exp * 5 // 8


def spans(d):
    return [(LANES * j, min(LANES, d - LANES * j)) for j in range(cdiv(d, LANES))]


any_space = pl.BlockSpec(memory_space=pl.ANY)
in_vmem = pl.BlockSpec(memory_space=pltpu.VMEM)


def sorted_list(expert_ids, gate_vals):
    n_tok, top = expert_ids.shape
    n = n_tok * top
    keys = expert_ids.T.reshape(n) * n + jnp.arange(n, dtype=I32)
    keys, gates = lax.sort((keys, gate_vals.T.reshape(n)), num_keys=1, is_stable=False)
    return (keys % n_tok).astype(F32), gates


def plan_kernel(n_layers, n_local, n_tok, list_rows, deal_ref, all_ref, tab_ref, idx_ref, gate_ref):
    n_mine = n_local // 2
    core, ep = lax.axis_index('core'), lax.axis_index('ep')
    list_len = list_rows * LANES
    lane = lambda n: lax.broadcasted_iota(I32, (n, LANES), 1).astype(F32)
    sub = lambda n: lax.broadcasted_iota(I32, (n, LANES), 0).astype(F32)
    over_lanes = lambda v: jnp.sum(v, axis=1, keepdims=True)
    over_subs = lambda v: jnp.sum(v, axis=0, keepdims=True)
    l16, s16 = lane(n_mine), sub(n_mine)
    groups = lambda c: jnp.floor((c + (GRP - 0.5)) * (1.0 / GRP))
    for l in range(n_layers):
        cnt = all_ref[:, 2 * n_layers * list_rows + l, :]
        ends = cnt
        step = 1
        while step < 2 * n_local:
            ends = ends + jnp.where(lane(N_SRC) >= step, pltpu.roll(ends, step, 1), 0.0)
            step *= 2
        starts = ends - cnt
        second = (ep > 0)
        local = lambda v: jnp.where(lane(N_SRC) < n_local, jnp.where(second, pltpu.roll(v, LANES - n_local, 1), v), 0.0)
        cnt, starts = local(cnt), local(starts)
        tiles = jnp.floor((over_subs(groups(local(deal_ref[:, 2 * n_layers * list_rows + l, :]))) + (PER_TILE - 0.5))
                          * (1.0 / PER_TILE))
        load = jnp.where(lane(1) < n_local, jnp.maximum(1.0, tiles), -1.0)
        wide = jnp.broadcast_to(load, (n_local, LANES))
        col = over_lanes(jnp.where(lane(n_local) == sub(n_local), wide, 0.0))
        ahead = (col > wide) | ((col == wide) & (sub(n_local) < lane(n_local)))
        rank = over_subs(jnp.where(ahead, 1.0, 0.0))
        odd = s16 - 2.0 * jnp.floor(s16 * 0.5 + 0.25)
        flip = jnp.where(core > 0, 1.0 - odd, odd)
        dealt = lambda f: (jnp.broadcast_to(rank, (n_mine, LANES)) == 2.0 * s16 + f) & (l16 < n_local)
        pick = dealt(flip)
        choose = lambda p, row: over_lanes(jnp.where(p, jnp.broadcast_to(row, (n_mine, LANES)), 0.0))
        mine = lambda row: choose(pick, row)
        as_row = lambda c: over_subs(jnp.where(l16 == s16, c, 0.0))
        experts = as_row(mine(lane(1)))
        partner = as_row(choose(dealt(1.0 - flip), lane(1)))
        at = l * TAB_ROWS
        off = jnp.zeros((n_mine, 1), F32)
        pos = [jnp.zeros((n_mine, LANES), F32) for _ in range(SLOT_GROUPS // LANES)]
        for s in range(N_SRC):
            c, st = mine(cnt[s:s + 1]), mine(starts[s:s + 1]) + float(s * list_len)
            ng = groups(c)
            for i in range(len(pos)):
                rel = l16 + float(LANES * i) - off
                code = (st + GRP * rel) * 16.0 + jnp.minimum(float(GRP), c - GRP * rel)
                pos[i] = jnp.where((rel >= 0) & (rel < ng), code, pos[i])
            off = off + ng
        for i in range(len(pos)):
            tab_ref[pl.ds(at + i, n_mine, stride=len(pos)), :] = pos[i].astype(I32)
        n_tiles = jnp.maximum(1.0, jnp.floor((off + (PER_TILE - 0.5)) * (1.0 / PER_TILE)))
        bounds = over_subs(jnp.where(s16 < l16, n_tiles, 0.0))
        before = over_lanes(jnp.where(l16 == s16, jnp.broadcast_to(bounds, (n_mine, LANES)), 0.0))
        t = jnp.minimum(l16, over_subs(jnp.broadcast_to(n_tiles, (n_mine, LANES))) - 1.0)
        inside = (t >= before) & (t < before + n_tiles)
        goff = over_subs(jnp.where(inside, s16 * float(SLOT_GROUPS) + (t - before) * float(PER_TILE), 0.0))
        rows = [(ROW_BOUND, bounds), (ROW_GOFF, goff), (ROW_EXPERT, experts), (ROW_PARTNER, partner)]
        for row, value in rows:
            tab_ref[at + row:at + row + 1, :] = value.astype(I32)
    for l in range(n_layers):
        pad = l * (N_SRC * list_rows + 8) + N_SRC * list_rows
        gate_ref[pad:pad + 8, :] = jnp.zeros((8, LANES), F32)
        for s in range(N_SRC):
            to = (l * N_SRC + s) * list_rows
            toks = all_ref[s, l * list_rows:(l + 1) * list_rows, :]
            idx_ref[to:to + list_rows, :] = ((toks + float(s * n_tok)) * float(PITCH)).astype(I32)
            to = l * (N_SRC * list_rows + 8) + s * list_rows
            gate_ref[to:to + list_rows, :] = all_ref[s, (n_layers + l) * list_rows:(n_layers + l + 1) * list_rows, :]


def plan_shapes(sizes):
    n_layers, _, _, list_rows = sizes
    rows = (n_layers * TAB_ROWS, n_layers * N_SRC * list_rows, n_layers * (N_SRC * list_rows + 8))
    return [jax.ShapeDtypeStruct((n, LANES), dt) for n, dt in zip(rows, (I32, I32, F32))]


def flat(tab, idx, gates):
    return tab.reshape(-1), idx.reshape(-1), gates


def plan(deal, shared, sizes):
    return flat(*pl.pallas_call(
        functools.partial(plan_kernel, *sizes),
        out_shape=plan_shapes(sizes),
        in_specs=[in_vmem] * 2, out_specs=[in_vmem] * 3,
        cost_estimate=pl.CostEstimate(flops=10 ** 7, bytes_accessed=10 ** 6, transcendentals=0),
        name="plan",
    )(deal, shared))


def expert_kernel(cfg, *refs):
    fwd, bwd, own, layer, n_blk, d, ff, n_exp, picks, row_id, list_len, p_f32, n_alias, got_layer = cfg
    save, load = fwd and not bwd, own and bwd and not fwd
    refs = list(refs)
    take = lambda n: [refs.pop(0) for _ in range(n)]
    tab_hbm, idx_hbm, gate_hbm = take(3)
    u_pieces = take(N_SRC) if not load else []
    dy_pieces = take(N_SRC) if bwd else []
    wg_hbm, wu_hbm, wd_hbm = take(3)
    ab_hbm, xu_hbm = take(2) if load else (None, None)
    prev = take(1)[0] if bwd and not own else None
    got = take(2) if got_layer is not None else None
    take(n_alias)
    y_outs = take(N_SRC) if fwd else []
    du_outs = take(N_SRC) if bwd and own else []
    grad = take(1)[0] if bwd and own else None
    finals = take(3) if bwd and not own or got_layer is not None else None
    sent = take(2) if bwd and not own else None
    ab_hbm, xu_hbm = take(2) if save else (ab_hbm, xu_hbm)
    tab_ref, idx, gate_ref, land, table, gat = take(6)
    acc, row_ref = take(2) if own else (None, None)
    gu_ref, wd_ref, g_ref, x_u = take(4)
    x_c = take(1)[0] if bwd else None
    ab_ref = take(1)[0]
    dh_ref = take(1)[0] if bwd else None
    h_ref = take(1)[0]
    dab_ref, sums = take(2) if bwd else (None, None)
    keep_buf = take(1)[0] if bwd and not own else None
    got_buf = take(1)[0] if got is not None else None
    list_sem, land_sem, w_sem = take(3)
    sum_sem = take(1)[0] if bwd else None
    keep_sem = take(1)[0] if bwd and not own else None
    read_sem, write_sem = take(2) if got is not None else (None, None)
    stage_f, out_sem = take(2) if own else (None, None)
    ab_sem, xu_sem = take(2) if save or load else (None, None)

    split = first_piece(n_exp)
    copy = pltpu.make_async_copy
    cols = spans(d)
    lo = ff // 256 * 256
    hi = ff - lo
    dot = functools.partial(lax.dot_general, preferred_element_type=F32)
    nn = (((1,), (0,)), ((), ()))
    nt = (((1,), (1,)), ((), ()))
    tn = (((0,), (0,)), ((), ()))
    al = pl.multiple_of
    n_row = N_SRC * n_blk
    glane = lax.broadcasted_iota(I32, (GRP, LANES), 1)
    gsub = lax.broadcasted_iota(I32, (GRP, LANES), 0)

    def row_at(r):
        return pl.ds(r * PITCH, FULL)

    def codes_of(tile):
        at = ROW_GOFF * LANES + tile
        if own and bwd:
            return lambda q: tab_ref[tab_ref[at] + q]
        view = tab_ref.at[pl.ds(tab_ref[at], PER_TILE)]
        return lambda q: view[q]

    def gather(codes, q):
        ids = idx.at[pl.ds(codes(q) >> 4, GRP)]
        for k in range(GRP):
            gat[row_at(q * GRP + k), :] = table[pl.ds(ids[k], FULL), :]

    def gate_column(code):
        pos = code >> 4
        row, shift = pos >> 7, pos & (LANES - 1)
        want = glane == gsub + shift
        over = glane == gsub + (shift - LANES)
        here = gate_ref[pl.ds(row, GRP, stride=0), :]
        there = gate_ref[pl.ds(row + 1, GRP, stride=0), :]
        v = jnp.where(want, here, jnp.where(over, there, 0.0))
        return jnp.where(gsub < (code & 15), jnp.sum(v, axis=1, keepdims=True), 0.0)

    def scatter(codes, q):
        ids = idx.at[pl.ds(codes(q) >> 4, GRP)]
        new = []
        for k in range(GRP):
            at = pl.ds(ids[k], FULL)
            new.append((at, acc[at, :] + row_ref[row_at(q * GRP + k), :]))
        for at, value in reversed(new):
            acc[at, :] = value

    def keep_ab(t):
        ends = (ab_ref.at[t & 1], ab_hbm.at[t])
        return copy(*(ends if save else ends[::-1]), ab_sem.at[t & 1])

    def keep_xu(t):
        ends = (x_u.at[t & 1], xu_hbm.at[t])
        return copy(*(ends if save else ends[::-1]), xu_sem.at[t & 1])

    def of(ref, t):
        return ref.at[t & 1] if save or load else ref

    def convert(codes, t):
        for q in range(0, PER_TILE, 2):
            part = []
            for p in (q, q + 1):
                code = codes(p)
                rows = [gat[pl.ds(GRP * PITCH * p + j, GRP, stride=PITCH), :]
                        for j in range(HALF if load else 0, FULL if bwd else HALF)]
                real = gsub < (code & 15)
                gate = gate_column(code)
                g_ref[GRP * p:GRP * (p + 1), :] = gate
                us, dys = ([], rows) if load else (rows[:HALF], rows[HALF:])
                part.append([jnp.where(real, v, 0.0) for v in us] + [v * gate for v in dys])
            at = slice(GRP * q, GRP * (q + 2))
            for x, o in ((None if load else of(x_u, t), 0), (x_c, 0 if load else HALF)):
                if x is None:
                    continue
                for j, (c, w) in enumerate(cols):
                    both = jnp.concatenate([part[0][o + j], part[1][o + j]], axis=0)
                    x[at, c:c + w] = both[:, :w].astype(BF16)

    def put_rows(o, value, s0):
        value = value.astype(BF16).astype(F32)
        n = value.shape[0]
        for j, (c, w) in enumerate(cols):
            row_ref[pl.ds(PITCH * s0 + o + j, n, stride=PITCH), 0:w] = value[:, c:c + w] * g_ref[s0:s0 + n, 0:w]

    low = lax.broadcasted_iota(I32, (16, 2 * hi), 1) < hi

    def middle(a, b, dh):
        sig = 0.5 * jnp.tanh(0.5 * a) + 0.5
        act = a * sig
        h = act * b
        if dh is None:
            return h, None, None
        slope = sig * (1.0 + a * (1.0 - sig))
        return h, dh * b * slope, dh * act

    def weights(e, slot):
        at = (layer, tab_ref[ROW_EXPERT * LANES + e])
        moves = []
        for i, w in enumerate((wg_hbm, wu_hbm)):
            moves.append((w.at[at + (pl.ds(0, lo),)], gu_ref.at[slot, pl.ds(i * lo, lo)]))
            moves.append((w.at[at + (pl.ds(lo, hi),)], gu_ref.at[slot, pl.ds(2 * lo + i * hi, hi)]))
        moves.append((wd_hbm.at[at], wd_ref.at[slot]))
        return [copy(a, b, w_sem.at[slot, i]) for i, (a, b) in enumerate(moves)]

    def sums_in(e, slot):
        return copy(prev.at[e], sums.at[slot], sum_sem.at[slot])

    def sums_out(e, slot):
        return copy(sums.at[slot], grad.at[e], sum_sem.at[slot])

    def keeps(e, slot):
        at = (layer, tab_ref[ROW_EXPERT * LANES + e])
        return [copy(keep_buf.at[slot, i], finals[i].at[at], keep_sem.at[slot, i]) for i in range(3)]

    def send(e, slot, part):
        return copy(keep_buf.at[slot], sent[part].at[e - part * split], keep_sem.at[slot, 3])

    def read(e, slot, part=0):
        return copy(got[part].at[e - part * split], got_buf.at[slot], read_sem.at[slot])

    def writes(e, slot):
        to = tab_ref[TAB_ROWS * LANES + e]
        return [copy(got_buf.at[slot, i], finals[i].at[got_layer, to], write_sem.at[slot, i]) for i in range(3)]

    def start(moves):
        for m in moves:
            m.start()

    def wait(moves):
        for m in moves:
            m.wait()

    n_tab = TAB_ROWS * LANES
    lists = [copy(tab_hbm.at[pl.ds(row_id * n_tab, n_tab)], tab_ref.at[pl.ds(0, n_tab)], list_sem.at[0]),
             copy(idx_hbm.at[pl.ds(row_id * N_SRC * list_len, N_SRC * list_len)], idx.at[pl.ds(0, N_SRC * list_len)],
                  list_sem.at[1]),
             copy(gate_hbm.at[pl.ds(row_id * gate_ref.shape[0], gate_ref.shape[0])], gate_ref, list_sem.at[2])]
    if got is not None:
        at = (got_layer * TAB_ROWS + ROW_PARTNER) * LANES
        lists.append(copy(tab_hbm.at[pl.ds(at, LANES)], tab_ref.at[pl.ds(n_tab, LANES)], list_sem.at[3]))
    start(lists)
    pieces = []
    for s in range(N_SRC):
        if not load:
            pieces.append((u_pieces[s], picks[0][s], s, 0, fwd))
        if bwd:
            pieces.append((dy_pieces[s], picks[1][s], s, HALF, own))
    lands = [copy(ref.at[pick], land.at[i % N_SRC], land_sem.at[i % N_SRC]) for i, (ref, pick, *_) in enumerate(pieces)]
    start(lands[:N_SRC])
    lists[0].wait()
    for e in range(DEPTH - 1):
        start(weights(e, e))
        if bwd and not own:
            sums_in(e, e).start()
    if got is not None:
        lists[3].wait()
        read(0, 0).start()
    if own:
        def clear(c, _):
            for k in range(4):
                acc[pl.ds(al(c * 1152 + 288 * k, 8), 288), :] = jnp.zeros((288, LANES), F32)
            return 0

        lax.fori_loop(0, acc.shape[0] // 1152, clear, 0)
        row_ref[...] = jnp.zeros(row_ref.shape, F32)
    rows = 256
    for i, (_, _, s, o, seed) in enumerate(pieces):
        lands[i].wait()

        def fill(c, _, i=i, o=o, seed=seed, s=s):
            r = al(c * rows, rows)
            for j in range(HALF):
                vals = land[i % N_SRC, pl.ds(r, rows), LANES * j:LANES * (j + 1)].astype(F32)
                to = pl.ds(PITCH * (s * n_blk + r) + o + j, rows, stride=PITCH)
                table[to, :] = vals
                if seed and s == 0:
                    acc[to, :] = vals
            return 0

        lax.fori_loop(0, n_blk // rows, fill, 0)
        if i + N_SRC < len(pieces):
            lands[i + N_SRC].start()
    wait(lists[1:3])
    for k in range(GRP):
        idx[N_SRC * list_len + k] = 0

    def first(q, _):
        gather(begin, 2 * q)
        gather(begin, 2 * q + 1)
        return 0

    begin = codes_of(0)
    lax.fori_loop(0, PER_TILE // 2, first, 0)
    convert(begin, 0)
    if save:
        keep_xu(0).start()
    if load:
        keep_ab(0).start()
        keep_xu(0).start()

    def expert(e, _):
        slot = e & 1
        deep = lax.rem(e, DEPTH)
        sum_slot = slot if own else deep
        wait(weights(e, deep))
        if bwd and not own:
            sums_in(e, deep).wait()
        if got is not None:
            read(0, slot).wait()
            start(writes(e, slot))

            @pl.when((e > 0) & (e < n_exp - 1))
            def _():
                wait(writes(e - 1, 1 - slot))

        @pl.when(e < n_exp - (DEPTH - 1))
        def _():
            ahead = lax.rem(e + DEPTH - 1, DEPTH)
            start(weights(e + DEPTH - 1, ahead))
            if bwd and not own:
                sums_in(e + DEPTH - 1, ahead).start()

        @pl.when(e < n_exp - 1)
        def _():
            if got is not None:
                for part in range(2):
                    @pl.when((e + 1 >= split) if part else (e + 1 < split))
                    def _(part=part):
                        read(e + 1, 1 - slot, part).start()

        if bwd and own:
            @pl.when(e > 1)
            def _():
                sums_out(e - 2, slot).wait()

            sums[slot] = jnp.zeros(sums.shape[1:], F32)

        def tile(t, _):
            if save:
                @pl.when(t > 1)
                def _():
                    keep_ab(t - 2).wait()

                @pl.when(t > 0)
                def _():
                    keep_xu(t - 1).wait()
            if load:
                keep_ab(t).wait()
                keep_xu(t).wait()
                keep_ab(t + 1).start()
                keep_xu(t + 1).start()
            ab, xu = of(ab_ref, t), of(x_u, t)
            before, after = codes_of(jnp.maximum(t - 1, 0)), codes_of(t + 1)
            for q in range(PER_TILE):
                if own:
                    scatter(before, q)
                gather(after, q)
            front = ROWS if own and bwd else ROWS // 2
            for s0 in range(0, ROWS, front):
                sl = slice(s0, s0 + front)
                if not load:
                    ab[sl, :] = dot(xu[sl, :], gu_ref[deep], nt)
                if bwd:
                    dh_ref[sl, :] = dot(x_c[sl, :], wd_ref[deep], nt)
            for r in range(0, ROWS, 16):
                rows = slice(r, r + 16)
                for c in range(0, lo, LANES):
                    h, da, db = middle(ab[rows, c:c + LANES], ab[rows, lo + c:lo + c + LANES],
                                       dh_ref[rows, c:c + LANES] if bwd else None)
                    h_ref[rows, c:c + LANES] = h.astype(BF16)
                    if bwd:
                        dab_ref[rows, c:c + LANES] = da.astype(BF16)
                        dab_ref[rows, lo + c:lo + c + LANES] = db.astype(BF16)
                a = ab[rows, 2 * lo:]
                b = pltpu.roll(a, hi, 1)
                dh = dh_ref[rows, lo:] if bwd else None
                if bwd:
                    dh = jnp.concatenate([dh, dh], axis=1)
                h, da, db = middle(a, b, dh)
                h_ref[rows, lo:] = h[:, :hi].astype(BF16)
                if bwd:
                    dab_ref[rows, 2 * lo:] = jnp.where(low, da, pltpu.roll(db, hi, 1)).astype(BF16)
            half = ROWS // 2
            for s0 in range(0, ROWS, half):
                sl = slice(s0, s0 + half)
                if fwd:
                    put_rows(0, dot(h_ref[sl, :], wd_ref[deep], nn), s0)
                if bwd and own:
                    put_rows(HALF, dot(dab_ref[sl, :], gu_ref[deep], nn), s0)
            if bwd:
                view = sums.at[sum_slot]
                view[0:2 * ff, :] += dot(dab_ref[...], xu[...], tn)
                view[2 * ff:, :] += dot(h_ref[...], x_c[...], tn)
            convert(after, t + 1)
            if save:
                keep_ab(t).start()
                keep_xu(t + 1).start()
            return 0

        lax.fori_loop(tab_ref[ROW_BOUND * LANES + e], tab_ref[ROW_BOUND * LANES + e + 1], tile, 0)
        if bwd and own:
            sums_out(e, slot).start()
        if bwd and not own:
            @pl.when(e > 1)
            def _():
                wait(keeps(e - 2, slot) + [send(0, slot, 0)])

            for i in range(2):
                keep_buf[slot, i, 0:lo, :] = sums[deep, i * lo:(i + 1) * lo, :].astype(BF16)
                keep_buf[slot, i, lo:, :] = sums[deep, 2 * lo + i * hi:2 * lo + (i + 1) * hi, :].astype(BF16)
            keep_buf[slot, 2] = sums[deep, 2 * ff:, :].astype(BF16)
            start(keeps(e, slot))
            for part in range(2):
                @pl.when((e >= split) if part else (e < split))
                def _(part=part):
                    send(e, slot, part).start()
        return 0

    lax.fori_loop(0, n_exp, expert, 0)
    ends = ((n_exp - 2, (n_exp - 2) % 2), (n_exp - 1, (n_exp - 1) % 2))
    n_tiles = tab_ref[ROW_BOUND * LANES + n_exp]
    if save:
        wait([keep_ab(n_tiles - 2), keep_ab(n_tiles - 1), keep_xu(n_tiles - 1)])
    if save or load:
        keep_xu(n_tiles).wait()
    if load:
        keep_ab(n_tiles).wait()
    if own:
        end = codes_of(tab_ref[ROW_BOUND * LANES + n_exp] - 1)
        lax.fori_loop(0, PER_TILE, lambda q, _: (scatter(end, q), 0)[1], 0)
        flights = {}
        for o, out in ((HALF, du_outs), (0, y_outs)):
            for s in range(N_SRC if out else 0):
                wide = s == 0 or p_f32
                stage = stage_f.at[s] if wide else land.at[s]
                if s in flights:
                    flights[s].wait()

                def fetch(c, _, stage=stage, s=s, o=o):
                    r = al(c * rows, rows)
                    for j in range(HALF):
                        at = pl.ds(PITCH * (s * n_blk + r) + o + j, rows, stride=PITCH)
                        stage[pl.ds(r, rows), LANES * j:LANES * (j + 1)] = acc[at, :].astype(stage.dtype)
                    return 0

                lax.fori_loop(0, n_blk // rows, fetch, 0)
                flights[s] = copy(stage, out[s], out_sem.at[s])
                flights[s].start()
        wait(flights.values())
        if bwd:
            for e, slot in ends:
                sums_out(e, slot).wait()
    else:
        for e, slot in ends:
            wait(keeps(e, slot) + [send(0, slot, 0)])
    if got is not None:
        for e, slot in ends:
            wait(writes(e, slot))


def run_experts(routes, layer, u, dy, weights, prev, finals, fwd, own, p_f32=False, got=None, kept=None):
    tab, idx, gates = routes
    bwd = dy is not None
    wg, wu, wd = weights
    save, load = fwd and not bwd, kept is not None
    n_blk, wide = (dy or u)[0][0].shape[-2:]
    n_layers, n_local, ff, d = wd.shape
    n_exp = n_local // 2
    row_id = layer
    list_len = idx.shape[0] // (n_layers * N_SRC)

    arrays = lambda pieces: [v for v, _ in pieces]
    operands = [tab, idx, gates] + ([] if load else arrays(u)) + (arrays(dy) if bwd else []) + [wg, wu, wd] + list(kept or ())
    out_shape, aliases = [], {}
    for use in (fwd, bwd and own):
        if use:
            out_shape += [jax.ShapeDtypeStruct((n_blk, wide), F32 if s == 0 or p_f32 else BF16) for s in range(N_SRC)]
    if bwd and own:
        out_shape.append(jax.ShapeDtypeStruct((n_exp, 3 * ff, d), F32))
    if bwd and not own:
        operands.append(prev)
    if got is not None:
        operands += got
    for i, f in enumerate(finals or ()):
        aliases[len(operands)] = len(out_shape) + i
        operands.append(f)
    if bwd and not own or finals:
        out_shape += [jax.ShapeDtypeStruct((n_layers, n_local, ff, d), BF16)] * 3
    if bwd and not own:
        out_shape += [jax.ShapeDtypeStruct((n, 3, ff, d), BF16) for n in (first_piece(n_exp), n_exp - first_piece(n_exp))]
    if save:
        most = n_exp * (SLOT_GROUPS // PER_TILE) + 2
        out_shape += [jax.ShapeDtypeStruct((most, ROWS, 2 * ff), F32), jax.ShapeDtypeStruct((most, ROWS, d), BF16)]
    sem = lambda *s: pltpu.SemaphoreType.DMA(s)
    mid = lambda n, dt: pltpu.VMEM((ROWS, n), dt)
    twin = lambda n, dt: pltpu.VMEM((2, ROWS, n), dt) if save or load else mid(n, dt)
    table, rows = pltpu.VMEM((PITCH * N_SRC * n_blk, LANES), F32), pltpu.VMEM((PITCH * ROWS, LANES), F32)
    scratch = [pltpu.SMEM(((TAB_ROWS + 1) * LANES,), I32), pltpu.SMEM((N_SRC * list_len + LANES,), I32),
               pltpu.VMEM((N_SRC * list_len // LANES + 8, LANES), F32), pltpu.VMEM((N_SRC, n_blk, wide), BF16)]
    scratch += [table, rows] * (1 + own)
    scratch += [pltpu.VMEM((DEPTH, 2 * ff, d), BF16), pltpu.VMEM((DEPTH, ff, d), BF16), mid(LANES, F32)]
    scratch += [twin(d, BF16)] + [mid(d, BF16)] * bwd + [twin(2 * ff, F32)] + [mid(ff, F32)] * bwd + [mid(ff, BF16)]
    scratch += [mid(2 * ff, BF16), pltpu.VMEM((2 if own else DEPTH, 3 * ff, d), F32)] * bwd
    if bwd and not own:
        scratch.append(pltpu.VMEM((2, 3, ff, d), BF16))
    if got is not None:
        scratch.append(pltpu.VMEM((2, 3, ff, d), BF16))
    scratch += [sem(4), sem(N_SRC), sem(DEPTH, 5)] + [sem(DEPTH)] * bwd
    if bwd and not own:
        scratch.append(sem(2, 4))
    if got is not None:
        scratch += [sem(2), sem(2, 3)]
    if own:
        scratch += [pltpu.VMEM((N_SRC if p_f32 else 1, n_blk, wide), F32), sem(N_SRC)]
    if save or load:
        scratch += [sem(2), sem(2)]
    passes = 2 + fwd + bwd * (4 + 2 * own)
    flops = 2 * d * ff * passes * n_blk * N_SRC * 2
    hoist = 1300 if not own else 640 if load else 750 if save else 950
    picks = [[i for _, i in u] if u else None, [i for _, i in dy] if bwd else None]
    cfg = (fwd, bwd, own, layer, n_blk, d, ff, n_exp, picks, row_id, list_len, p_f32, len(aliases),
           None if got is None else 1 - layer)
    return pl.pallas_call(
        functools.partial(expert_kernel, cfg),
        out_shape=out_shape,
        in_specs=[any_space] * len(operands),
        out_specs=[any_space] * len(out_shape),
        scratch_shapes=scratch,
        input_output_aliases=aliases,
        compiler_params=pltpu.CompilerParams(
            vmem_limit_bytes=VMEM_LIMIT),
        cost_estimate=pl.CostEstimate(flops=flops, bytes_accessed=3 * 2 * n_exp * d * ff, transcendentals=0),
        name=f"experts_{'f' if fwd else ''}{'b' if bwd else ''}_{'own' if own else 'other'}_{layer}",
    )(*operands)


def place_kernel(layer, n_exp, at, tab_hbm, got_ref, *refs):
    outs, (tab_ref, buf, tab_sem, in_sem, out_sem) = refs[3:6], refs[6:]
    table = pltpu.make_async_copy(tab_hbm.at[pl.ds((layer * TAB_ROWS + ROW_PARTNER) * LANES, LANES)], tab_ref, tab_sem)
    table.start()
    reads = [pltpu.make_async_copy(got_ref.at[i], buf.at[i], in_sem.at[i]) for i in range(n_exp)]
    for read in reads:
        read.start()
    writes = []
    table.wait()
    for i, read in enumerate(reads):
        read.wait()
        e = tab_ref[at + i]
        for k, out in enumerate(outs):
            writes.append(pltpu.make_async_copy(buf.at[i, k], out.at[layer, e], out_sem.at[i, k]))
            writes[-1].start()
    for write in writes:
        write.wait()


def place(tab, at, layer, got, finals):
    n_exp = got.shape[0]
    return pl.pallas_call(
        functools.partial(place_kernel, layer, n_exp, at),
        out_shape=[jax.ShapeDtypeStruct(f.shape, f.dtype) for f in finals],
        in_specs=[any_space] * 5, out_specs=[any_space] * 3,
        scratch_shapes=[pltpu.SMEM((LANES,), I32), pltpu.VMEM(got.shape, got.dtype), pltpu.SemaphoreType.DMA,
                        pltpu.SemaphoreType.DMA((n_exp,)), pltpu.SemaphoreType.DMA((n_exp, 3))],
        input_output_aliases={2: 0, 3: 1, 4: 2},
        compiler_params=pltpu.CompilerParams(vmem_limit_bytes=VMEM_LIMIT),
        cost_estimate=pl.CostEstimate(flops=0, bytes_accessed=4 * got.size, transcendentals=0),
        name=f"place_{layer}",
    )(tab, got, *finals)


def peer(rel):
    return {name: (lax.axis_index(name) + ((rel >> bit) & 1)) % 2 for bit, name in enumerate(("ep", "core", "x"))}


def meet(rels):
    barrier = pltpu.get_barrier_semaphore()
    for rel in rels:
        pl.semaphore_signal(barrier, inc=1, device_id=peer(rel), device_id_type=MESH)
    pl.semaphore_wait(barrier, len(rels))


def remote(src, dst, send, recv, rel):
    return pltpu.make_async_remote_copy(src_ref=src, dst_ref=dst, send_sem=send, recv_sem=recv,
                                        device_id=peer(rel), device_id_type=MESH)


def share_kernel(mine_ref, all_ref, send_sem, recv_sem):
    meet((Y, CORE))
    direct = [remote(mine_ref, all_ref.at[rel], send_sem.at[rel], recv_sem.at[rel], rel) for rel in (Y, CORE)]
    for copy in direct:
        copy.start()
    all_ref[0] = mine_ref[...]
    on = remote(all_ref.at[Y], all_ref.at[Y + CORE], send_sem.at[Y + CORE], recv_sem.at[Y + CORE], CORE)
    direct[0].wait_recv()
    on.start()
    direct[0].wait_send()
    direct[1].wait()
    on.wait()


def share(mine, n_rel):
    return pl.pallas_call(
        share_kernel,
        out_shape=jax.ShapeDtypeStruct((n_rel,) + mine.shape, mine.dtype),
        in_specs=[in_vmem],
        out_specs=in_vmem,
        scratch_shapes=[pltpu.SemaphoreType.DMA((n_rel,)), pltpu.SemaphoreType.DMA((n_rel,))],
        compiler_params=pltpu.CompilerParams(collective_id=0, has_side_effects=True),
        cost_estimate=pl.CostEstimate(flops=10 ** 7, bytes_accessed=mine.size * 4 * n_rel, transcendentals=0),
        name="share_lists",
    )(mine)


def blocks_kernel(cfg, *refs):
    n_chunk, reduce, back, d, sizes = cfg
    refs = list(refs)
    take = lambda n: [refs.pop(0) for _ in range(n)]
    parts = take(N_SRC)
    m_ref = take(1)[0]
    list_refs, left_ref = take(2) if sizes else (), take(1)[0] if back else None
    o_total, o_a, o_b = take(3)
    plan_refs, grad_ref = take(3) if sizes else (), take(1)[0] if back else None
    in_f, in_b, got_f, s_wire, r_wire, u_wire, y_wire, t_buf, u_buf, y_buf, load, send, recv, put = take(14)
    n_rows = t_buf.shape[0] // n_chunk
    cut = [pl.ds(k * n_rows, n_rows) for k in range(n_chunk)]
    thin = [pl.ds(k * n_rows // 2, n_rows // 2) for k in range(n_chunk)]
    side = lax.broadcasted_iota(I32, (n_rows // 2, LANES), 1) < LANES // 2
    tiles = d // LANES
    turn = lambda v: pltpu.roll(v, LANES // 2, 1)
    lanes = lambda v, j: v[:, LANES * j:LANES * (j + 1)]

    def pack(wire, k, value):
        top, low = value[:n_rows // 2], value[n_rows // 2:]
        turned = [turn(lanes(low, j)) for j in range(tiles + 1)]
        parts = [lanes(top, j) for j in range(tiles)] + [jnp.where(side, lanes(top, tiles), turned[0])]
        parts += [jnp.where(side, turned[j], turned[j + 1]) for j in range(tiles)]
        for j, part in enumerate(parts):
            wire[thin[k], LANES * j:LANES * (j + 1)] = part.astype(BF16)

    def unpack(wire, k):
        value = wire[thin[k], :].astype(F32)
        turned = [turn(lanes(value, tiles + j)) for j in range(tiles + 1)]
        top = [lanes(value, j) for j in range(tiles)] + [jnp.where(side, lanes(value, tiles), 0.0)]
        low = [jnp.where(side, turned[j], turned[j + 1]) for j in range(tiles)] + [jnp.where(side, turned[tiles], 0.0)]
        return jnp.concatenate([jnp.concatenate(top, axis=1), jnp.concatenate(low, axis=1)], axis=0)

    chunks = range(n_chunk)
    loads = {}
    for i, part in enumerate(parts[:2] if reduce else parts):
        buf = in_f.at[i] if reduce or i == 0 else in_b.at[i - 1]
        for k in chunks:
            loads[i, k] = pltpu.make_async_copy(part.at[cut[k]], buf.at[cut[k]], load.at[i, k])
    order = (1, 0) if reduce else range(N_SRC)
    for i in order:
        for k in chunks:
            loads[i, k].start()
    u_buf[...] = jnp.zeros(u_buf.shape, BF16)
    meet((Y, CORE))
    links = []
    copy_in = pltpu.make_async_copy

    def link(src, dst, rel, cut=cut):
        n = len(links)
        links.append([remote(src.at[cut[k]], dst.at[cut[k]], send.at[n, k], recv.at[n, k], rel) for k in chunks])
        return links[-1]

    if reduce:
        first = link(parts[3], got_f.at[1], CORE)
        second = link(parts[2], got_f.at[0], CORE)
        over = link(s_wire, r_wire, Y, thin)
        for copies in (first, second):
            for copy in copies:
                copy.start()
        for k in chunks:
            loads[1, k].wait()
            first[k].wait_recv()
            pack(s_wire, k, in_f[1, cut[k], :] + got_f[1, cut[k], :])
            over[k].start()
    to_y = link(u_wire, y_wire, Y, thin)
    to_core = link(u_buf, o_b.at[0], CORE)
    puts = []
    for k in chunks:
        if reduce:
            loads[0, k].wait()
            second[k].wait_recv()
            over[k].wait_recv()
            total = in_f[0, cut[k], :] + got_f[0, cut[k], :] + unpack(r_wire, k)
        else:
            for i in range(N_SRC):
                loads[i, k].wait()
            total = in_f[0, cut[k], :]
            for i in range(N_SRC - 1):
                total = total + in_b[i, cut[k], :].astype(F32)
        total = total.astype(BF16)
        t_buf[cut[k], :] = total
        dims = (((1,), (1 if back else 0,)), ((), ()))
        mixed = lax.dot_general(total[:, :d], m_ref[...], dims, preferred_element_type=F32)
        u_buf[cut[k], 0:d] = (total[:, :d].astype(F32) + mixed).astype(BF16)
        pack(u_wire, k, u_buf[cut[k], :].astype(F32))
        to_y[k].start()
        to_core[k].start()
        puts.append(pltpu.make_async_copy(u_buf.at[cut[k]], o_a.at[0, cut[k]], put.at[0, k]))
        puts.append(pltpu.make_async_copy(t_buf.at[cut[k]], o_total.at[cut[k]], put.at[1, k]))
        for copy in puts[-2:]:
            copy.start()
    if sizes:
        plan_kernel(*sizes, *list_refs, *plan_refs)
    if back:
        grad_ref[...] = lax.dot_general(left_ref[:, :d], t_buf[:, :d], (((0,), (0,)), ((), ())), preferred_element_type=F32)
    on = link(y_buf, o_b.at[1], CORE)
    for k in chunks:
        to_y[k].wait_recv()
        y_buf[cut[k], :] = unpack(y_wire, k).astype(BF16)
        on[k].start()
        puts.append(copy_in(y_buf.at[cut[k]], o_a.at[1, cut[k]], put.at[2, k]))
        puts[-1].start()
    waited = [to_y] + ([first, second, over] if reduce else [])
    for copies in links:
        for copy in copies:
            if any(copies is w for w in waited):
                copy.wait_send()
            else:
                copy.wait()
    for copy in puts:
        copy.wait()


def complete_blocks(parts, m, reduce, back, ident, sizes=None, lists=(), left=(), n_chunk=4):
    n_blk, wide = parts[0].shape
    d = m.shape[0]
    sem = lambda *s: pltpu.SemaphoreType.DMA(s)
    pair = jax.ShapeDtypeStruct((2, n_blk, wide), BF16)
    extra = plan_shapes(sizes) if sizes else []
    extra += [jax.ShapeDtypeStruct((d, d), F32)] * len(left)
    buf = lambda n, dt: pltpu.VMEM((n, n_blk, wide) if n else (n_blk, wide), dt)
    return pl.pallas_call(
        functools.partial(blocks_kernel, (n_chunk, reduce, back, d, sizes)),
        out_shape=[jax.ShapeDtypeStruct((n_blk, wide), BF16)] + [pair] * 2 + extra,
        in_specs=[any_space] * N_SRC + [in_vmem] * (1 + len(lists) + len(left)),
        out_specs=[any_space] * 3 + [in_vmem] * len(extra),
        scratch_shapes=[buf(2, F32), buf(3, BF16), buf(2, F32)] + [pltpu.VMEM((n_blk // 2, 2 * d), BF16)] * 4 + [
            buf(0, BF16), buf(0, BF16), buf(0, BF16), sem(4, n_chunk), sem(6, n_chunk), sem(6, n_chunk), sem(3, n_chunk)],
        compiler_params=pltpu.CompilerParams(collective_id=ident, has_side_effects=True, vmem_limit_bytes=VMEM_LIMIT),
        cost_estimate=pl.CostEstimate(flops=10 ** 8, bytes_accessed=n_blk * wide * 40, transcendentals=0),
        name=f"complete_blocks_{ident}",
    )(*parts, m, *lists, *left)


def solution(mesh):
    ep_size, dp_size = mesh.shape['ep'], mesh.shape['dp']
    sub = Mesh(mesh.devices.reshape(ep_size, dp_size // 2, 2), ('ep', 'x', 'core'))
    tok_axes = ('x', 'core', 'ep')
    tok_spec = P(tok_axes, None)
    route_spec = P(None, tok_axes, None)
    whole_spec = P(None, None, None)
    expert_spec = P(None, 'ep', None, None)
    flip = [(0, 1), (1, 0)]
    move = lambda v, axis: lax.ppermute(v, axis, flip)
    move_diag = lambda v: lax.ppermute(v, ('ep', 'core'), [(0, 3), (1, 2), (2, 1), (3, 0)])
    fence = lax.optimization_barrier

    def device_step(tokens, d_out, expert_ids, gate_vals, w_mix, w_gate, w_up, w_down):
        n_layers, d = w_mix.shape[0], w_mix.shape[1]
        n_tok = tokens.shape[0]
        top = expert_ids.shape[2]
        n_local = w_gate.shape[1]
        n_exp = n_local * ep_size
        n = n_tok * top
        n_rel = 2 * N_SRC
        wide = cdiv(d, LANES) * LANES
        weights = (jnp.swapaxes(w_gate, 2, 3), jnp.swapaxes(w_up, 2, 3), w_down)
        pad = lambda v: jnp.pad(v, ((0, 0), (0, wide - d)))
        send_three = lambda p: [move(p[1], 'ep'), move(p[2], 'core'), move_diag(p[3])]

        def own_sum(p, got):
            return sum([g.astype(F32) for g in got], p)[:, :d].astype(BF16)

        one = lambda v: v.reshape(1, n_tok, wide)
        pairs = lambda a, b: [(a, 0), (a, 1), (b, 0), (b, 1)]

        one = lambda v: v.reshape(1, n_tok, wide)
        pairs = lambda a, b: [(a, 0), (a, 1), (b, 0), (b, 1)]
        singles = lambda *v: [(one(a), 0) for a in v]

        same = jnp.eye(d, dtype=BF16)
        u0 = (jnp.dot(tokens, pad(same), preferred_element_type=F32)
              + jnp.dot(tokens, pad(w_mix[0]), preferred_element_type=F32)).astype(BF16)
        u0_y, u0_c = move(u0, 'ep'), move(u0, 'core')
        lists = [sorted_list(expert_ids[l], gate_vals[l]) for l in range(n_layers)]
        counts = jnp.sum((expert_ids.transpose(0, 2, 1).reshape(n_layers, n, 1) == jnp.arange(n_exp, dtype=I32)).astype(F32), axis=1)
        packed = jnp.concatenate([jnp.concatenate([v[0] for v in lists] + [v[1] for v in lists]).reshape(-1, LANES),
                                  jnp.pad(counts, ((0, 8 - n_layers), (0, LANES - n_exp)))], axis=0)
        dy = pad(d_out)
        packed, dy = fence((packed, dy))
        shared = share(packed, N_SRC)
        u0_y, u0_c, dy, shared, w_mix = fence((u0_y, u0_c, dy, shared, w_mix))
        u0_d = move(u0_y, 'core')
        shared_x = move(shared, 'x')
        dy_y, dy_x = move(dy, 'ep'), move(dy, 'x')
        sizes = (n_layers, n_local, n_tok, n // LANES)
        routes = plan(shared, shared, sizes)
        u0_half = singles(u0, u0_y, u0_c, u0_d)
        add = lambda a, b: a.astype(F32) + b.astype(F32)
        to_chips = lambda v: [move(v, 'ep'), move(v, 'x'), lax.ppermute(v, ('ep', 'x'), [(0, 3), (1, 2), (2, 1), (3, 0)])]
        of_chips = lambda v, t: (add(v, t[0]) + add(t[1], t[2])).astype(BF16)
        piece = first_piece(n_local // 2)
        *part, ab0, xu0 = run_experts(routes, 0, u0_half, None, weights, None, None, True, True, p_f32=True)
        dy_y, dy_x, shared_x, part = fence((dy_y, dy_x, shared_x, part))
        dy_c, dy_d, dy_xy, dy_xc = move(dy, 'core'), move(dy_y, 'core'), move(dy_y, 'x'), move(dy_x, 'core')
        y0, u1_a, u1_b, *routes_x = complete_blocks(part, w_mix[1], True, False, 1, sizes, (shared, shared_x))
        routes_x = flat(*routes_x)
        dy_c, dy_d, dy_xy, dy_xc, u0_p, u0_q, y0, u1_a, u1_b = fence(
            (dy_c, dy_d, dy_xy, dy_xc, u0, u0_y, y0, u1_a, u1_b))
        dy_xd = move(dy_xy, 'core')
        u1_xa = move(u1_a, 'x')
        out = run_experts(routes, 1, pairs(u1_a, u1_b), singles(dy, dy_y, dy_c, dy_d), weights, None, None, True, True)
        u1_xa, dy_xd, u0_p, u0_q, out = fence((u1_xa, dy_xd, u0_p, u0_q, out))
        y_part, du_part, g1 = out[:4], out[4:8], out[8]
        u1_xb = move(u1_xa, 'core')
        got = send_three(du_part)
        u0_x, u0_xy = move(u0_p, 'x'), move(u0_q, 'x')
        out = run_experts(routes_x, 1, pairs(u1_xa, u1_xb), singles(dy_x, dy_xy, dy_xc, dy_xd), weights, g1, None,
                          False, False)
        got, u0_x, u0_xy, out = fence((got, u0_x, u0_xy, out))
        *finals, sent_a, sent_b = out
        got1 = [move(sent_a, 'core'), move(sent_b, 'core')]
        du1, dx_a, dx_b, g_mix1 = complete_blocks([du_part[0], *got], w_mix[1], False, True, 2, left=(y0,))
        tx = lambda x, du: jnp.einsum('td,te->de', x, du, preferred_element_type=F32)
        dx_a, y_part, got1, u0_x, u0_xy, g_mix1 = fence((dx_a, y_part, got1, u0_x, u0_xy, g_mix1))
        dx_xa = move(dx_a, 'x')
        part1 = g_mix1.astype(BF16)
        theirs1 = to_chips(part1)
        got_y = send_three(y_part)
        u0_xc, u0_xd = move(u0_x, 'core'), move(u0_xy, 'core')
        out = run_experts(routes, 0, None, pairs(dx_a, dx_b), weights, None, finals, False, True, got=got1, kept=(ab0, xu0))
        dx_xa, got_y, u0_xc, u0_xd, theirs1, out = fence((dx_xa, got_y, u0_xc, u0_xd, theirs1, out))
        du_part, g0, finals = out[:4], out[4], out[5:]
        dx_xb = move(dx_xa, 'core')
        got = send_three(du_part)
        part1 = of_chips(part1, theirs1)
        theirs1 = move(part1, 'core')
        du_part, dx_xb, part1 = fence((du_part, dx_xb, part1))
        out = run_experts(routes_x, 0, singles(u0_x, u0_xy, u0_xc, u0_xd), pairs(dx_xa, dx_xb), weights, g0, finals,
                          False, False)
        got, theirs1, got_y, y_own, out = fence((got, theirs1, got_y, y_part[0], out))
        *finals, sent_a, sent_b = out
        got_a, got_b = move(sent_a, 'core'), move(sent_b, 'core')
        du0 = own_sum(du_part[0], got)
        part0 = tx(tokens, du0).astype(BF16)
        theirs0 = to_chips(part0)
        turned = lambda v, w: jnp.einsum('te,de->dt', v, w, preferred_element_type=F32)
        dx0 = (turned(du0, same) + turned(du0, w_mix[0])).astype(BF16)
        y1 = turned(own_sum(y_own, got_y), same).astype(BF16)
        dx0, y1, got_a, finals = fence((dx0, y1, got_a, finals))
        finals = place(routes[0], 0, 0, got_a, finals)
        dx0, got_b, finals = fence((dx0, got_b, finals))
        finals = place(routes[0], piece, 0, got_b, finals)
        theirs0, finals = fence((theirs0, finals))
        total0 = of_chips(part0, theirs0)
        which = lax.broadcasted_iota(I32, (n_layers, d, d), 0)
        g_mix = jnp.where(which == 0, add(total0, move(total0, 'core'))[None], add(part1, theirs1)[None]).astype(BF16)
        return (y1.T, dx0.T, g_mix, jnp.swapaxes(finals[0], 2, 3), jnp.swapaxes(finals[1], 2, 3), finals[2])

    return jax.shard_map(device_step, mesh=sub,
                         in_specs=(tok_spec, tok_spec, route_spec, route_spec, whole_spec,
                                   expert_spec, expert_spec, expert_spec),
                         out_specs=(tok_spec, tok_spec, whole_spec, expert_spec, expert_spec, expert_spec),
                         check_vma=False)
```

```python
import functools

import jax
import jax.numpy as jnp
from jax import lax
from jax.experimental import pallas as pl
from jax.experimental.pallas import tpu as pltpu
from jax.sharding import Mesh, PartitionSpec as P

F32, BF16, I32 = jnp.float32, jnp.bfloat16, jnp.int32
MESH = pl.DeviceIdType.MESH
ROWS = 384
GRP = 8
PITCH = 9
DEPTH = 3
FULL = 8
HALF = 4
CAP_FACTOR = 3
LANES = 128
N_SRC = 4
Y, CORE, X = 1, 2, 4
VMEM_LIMIT = 62 * 1024 * 1024
PER_TILE = ROWS // GRP
ROW_BOUND, ROW_GOFF, ROW_EXPERT, ROW_PARTNER, TAB_ROWS = 32, 33, 34, 35, 40
SLOT_GROUPS = 256


def cdiv(a, b):
    return (a + b - 1) // b


def first_piece(n_exp):
    return n_exp * 5 // 8


def spans(d):
    return [(LANES * j, min(LANES, d - LANES * j)) for j in range(cdiv(d, LANES))]


any_space = pl.BlockSpec(memory_space=pl.ANY)
in_vmem = pl.BlockSpec(memory_space=pltpu.VMEM)


def sorted_list(expert_ids, gate_vals):
    n_tok, top = expert_ids.shape
    n = n_tok * top
    keys = expert_ids.T.reshape(n) * n + jnp.arange(n, dtype=I32)
    keys, gates = lax.sort((keys, gate_vals.T.reshape(n)), num_keys=1, is_stable=False)
    return (keys % n_tok).astype(F32), gates


def plan_kernel(n_layers, n_local, n_tok, list_rows, deal_ref, all_ref, tab_ref, idx_ref, gate_ref):
    n_mine = n_local // 2
    core, ep = lax.axis_index('core'), lax.axis_index('ep')
    list_len = list_rows * LANES
    lane = lambda n: lax.broadcasted_iota(I32, (n, LANES), 1).astype(F32)
    sub = lambda n: lax.broadcasted_iota(I32, (n, LANES), 0).astype(F32)
    over_lanes = lambda v: jnp.sum(v, axis=1, keepdims=True)
    over_subs = lambda v: jnp.sum(v, axis=0, keepdims=True)
    l16, s16 = lane(n_mine), sub(n_mine)
    groups = lambda c: jnp.floor((c + (GRP - 0.5)) * (1.0 / GRP))
    for l in range(n_layers):
        cnt = all_ref[:, 2 * n_layers * list_rows + l, :]
        ends = cnt
        step = 1
        while step < 2 * n_local:
            ends = ends + jnp.where(lane(N_SRC) >= step, pltpu.roll(ends, step, 1), 0.0)
            step *= 2
        starts = ends - cnt
        second = (ep > 0)
        local = lambda v: jnp.where(lane(N_SRC) < n_local, jnp.where(second, pltpu.roll(v, LANES - n_local, 1), v), 0.0)
        cnt, starts = local(cnt), local(starts)
        tiles = jnp.floor((over_subs(groups(local(deal_ref[:, 2 * n_layers * list_rows + l, :]))) + (PER_TILE - 0.5))
                          * (1.0 / PER_TILE))
        load = jnp.where(lane(1) < n_local, jnp.maximum(1.0, tiles), -1.0)
        wide = jnp.broadcast_to(load, (n_local, LANES))
        col = over_lanes(jnp.where(lane(n_local) == sub(n_local), wide, 0.0))
        ahead = (col > wide) | ((col == wide) & (sub(n_local) < lane(n_local)))
        rank = over_subs(jnp.where(ahead, 1.0, 0.0))
        odd = s16 - 2.0 * jnp.floor(s16 * 0.5 + 0.25)
        flip = jnp.where(core > 0, 1.0 - odd, odd)
        dealt = lambda f: (jnp.broadcast_to(rank, (n_mine, LANES)) == 2.0 * s16 + f) & (l16 < n_local)
        pick = dealt(flip)
        choose = lambda p, row: over_lanes(jnp.where(p, jnp.broadcast_to(row, (n_mine, LANES)), 0.0))
        mine = lambda row: choose(pick, row)
        as_row = lambda c: over_subs(jnp.where(l16 == s16, c, 0.0))
        experts = as_row(mine(lane(1)))
        partner = as_row(choose(dealt(1.0 - flip), lane(1)))
        at = l * TAB_ROWS
        off = jnp.zeros((n_mine, 1), F32)
        pos = [jnp.zeros((n_mine, LANES), F32) for _ in range(SLOT_GROUPS // LANES)]
        for s in range(N_SRC):
            c, st = mine(cnt[s:s + 1]), mine(starts[s:s + 1]) + float(s * list_len)
            ng = groups(c)
            for i in range(len(pos)):
                rel = l16 + float(LANES * i) - off
                code = (st + GRP * rel) * 16.0 + jnp.minimum(float(GRP), c - GRP * rel)
                pos[i] = jnp.where((rel >= 0) & (rel < ng), code, pos[i])
            off = off + ng
        for i in range(len(pos)):
            tab_ref[pl.ds(at + i, n_mine, stride=len(pos)), :] = pos[i].astype(I32)
        n_tiles = jnp.maximum(1.0, jnp.floor((off + (PER_TILE - 0.5)) * (1.0 / PER_TILE)))
        bounds = over_subs(jnp.where(s16 < l16, n_tiles, 0.0))
        before = over_lanes(jnp.where(l16 == s16, jnp.broadcast_to(bounds, (n_mine, LANES)), 0.0))
        t = jnp.minimum(l16, over_subs(jnp.broadcast_to(n_tiles, (n_mine, LANES))) - 1.0)
        inside = (t >= before) & (t < before + n_tiles)
        goff = over_subs(jnp.where(inside, s16 * float(SLOT_GROUPS) + (t - before) * float(PER_TILE), 0.0))
        rows = [(ROW_BOUND, bounds), (ROW_GOFF, goff), (ROW_EXPERT, experts), (ROW_PARTNER, partner)]
        for row, value in rows:
            tab_ref[at + row:at + row + 1, :] = value.astype(I32)
    for l in range(n_layers):
        pad = l * (N_SRC * list_rows + 8) + N_SRC * list_rows
        gate_ref[pad:pad + 8, :] = jnp.zeros((8, LANES), F32)
        for s in range(N_SRC):
            to = (l * N_SRC + s) * list_rows
            toks = all_ref[s, l * list_rows:(l + 1) * list_rows, :]
            idx_ref[to:to + list_rows, :] = ((toks + float(s * n_tok)) * float(PITCH)).astype(I32)
            to = l * (N_SRC * list_rows + 8) + s * list_rows
            gate_ref[to:to + list_rows, :] = all_ref[s, (n_layers + l) * list_rows:(n_layers + l + 1) * list_rows, :]


def plan_shapes(sizes):
    n_layers, _, _, list_rows = sizes
    rows = (n_layers * TAB_ROWS, n_layers * N_SRC * list_rows, n_layers * (N_SRC * list_rows + 8))
    return [jax.ShapeDtypeStruct((n, LANES), dt) for n, dt in zip(rows, (I32, I32, F32))]


def flat(tab, idx, gates):
    return tab.reshape(-1), idx.reshape(-1), gates


def plan(deal, shared, sizes):
    return flat(*pl.pallas_call(
        functools.partial(plan_kernel, *sizes),
        out_shape=plan_shapes(sizes),
        in_specs=[in_vmem] * 2, out_specs=[in_vmem] * 3,
        cost_estimate=pl.CostEstimate(flops=10 ** 7, bytes_accessed=10 ** 6, transcendentals=0),
        name="plan",
    )(deal, shared))


def expert_kernel(cfg, *refs):
    fwd, bwd, own, layer, n_blk, d, ff, n_exp, picks, row_id, list_len, p_f32, n_alias, got_layer = cfg
    save, load = fwd and not bwd, own and bwd and not fwd
    refs = list(refs)
    take = lambda n: [refs.pop(0) for _ in range(n)]
    tab_hbm, idx_hbm, gate_hbm = take(3)
    u_pieces = take(N_SRC) if not load else []
    dy_pieces = take(N_SRC) if bwd else []
    wg_hbm, wu_hbm, wd_hbm = take(3)
    ab_hbm, xu_hbm = take(2) if load else (None, None)
    prev = take(1)[0] if bwd and not own else None
    got = take(2) if got_layer is not None else None
    take(n_alias)
    y_outs = take(N_SRC) if fwd else []
    du_outs = take(N_SRC) if bwd and own else []
    grad = take(1)[0] if bwd and own else None
    finals = take(3) if bwd and not own or got_layer is not None else None
    sent = take(2) if bwd and not own else None
    ab_hbm, xu_hbm = take(2) if save else (ab_hbm, xu_hbm)
    tab_ref, idx, gate_ref, land, table, gat = take(6)
    acc, row_ref = take(2) if own else (None, None)
    gu_ref, wd_ref, g_ref, x_u = take(4)
    x_c = take(1)[0] if bwd else None
    ab_ref = take(1)[0]
    dh_ref = take(1)[0] if bwd else None
    h_ref = take(1)[0]
    dab_ref, sums = take(2) if bwd else (None, None)
    keep_buf = take(1)[0] if bwd and not own else None
    got_buf = take(1)[0] if got is not None else None
    list_sem, land_sem, w_sem = take(3)
    sum_sem = take(1)[0] if bwd else None
    keep_sem = take(1)[0] if bwd and not own else None
    read_sem, write_sem = take(2) if got is not None else (None, None)
    stage_f, out_sem = take(2) if own else (None, None)
    ab_sem, xu_sem = take(2) if save or load else (None, None)

    split = first_piece(n_exp)
    copy = pltpu.make_async_copy
    cols = spans(d)
    lo = ff // 256 * 256
    hi = ff - lo
    dot = functools.partial(lax.dot_general, preferred_element_type=F32)
    nn = (((1,), (0,)), ((), ()))
    nt = (((1,), (1,)), ((), ()))
    tn = (((0,), (0,)), ((), ()))
    al = pl.multiple_of
    n_row = N_SRC * n_blk
    glane = lax.broadcasted_iota(I32, (GRP, LANES), 1)
    gsub = lax.broadcasted_iota(I32, (GRP, LANES), 0)

    def row_at(r):
        return pl.ds(r * PITCH, FULL)

    def codes_of(tile):
        at = ROW_GOFF * LANES + tile
        if own and bwd:
            return lambda q: tab_ref[tab_ref[at] + q]
        view = tab_ref.at[pl.ds(tab_ref[at], PER_TILE)]
        return lambda q: view[q]

    def gather(codes, q):
        ids = idx.at[pl.ds(codes(q) >> 4, GRP)]
        for k in range(GRP):
            gat[row_at(q * GRP + k), :] = table[pl.ds(ids[k], FULL), :]

    def gate_column(code):
        pos = code >> 4
        row, shift = pos >> 7, pos & (LANES - 1)
        want = glane == gsub + shift
        over = glane == gsub + (shift - LANES)
        here = gate_ref[pl.ds(row, GRP, stride=0), :]
        there = gate_ref[pl.ds(row + 1, GRP, stride=0), :]
        v = jnp.where(want, here, jnp.where(over, there, 0.0))
        return jnp.where(gsub < (code & 15), jnp.sum(v, axis=1, keepdims=True), 0.0)

    def scatter(codes, q):
        ids = idx.at[pl.ds(codes(q) >> 4, GRP)]
        new = []
        for k in range(GRP):
            at = pl.ds(ids[k], FULL)
            new.append((at, acc[at, :] + row_ref[row_at(q * GRP + k), :]))
        for at, value in reversed(new):
            acc[at, :] = value

    def keep_ab(t):
        ends = (ab_ref.at[t & 1], ab_hbm.at[t])
        return copy(*(ends if save else ends[::-1]), ab_sem.at[t & 1])

    def keep_xu(t):
        ends = (x_u.at[t & 1], xu_hbm.at[t])
        return copy(*(ends if save else ends[::-1]), xu_sem.at[t & 1])

    def of(ref, t):
        return ref.at[t & 1] if save or load else ref

    def convert(codes, t):
        for q in range(0, PER_TILE, 2):
            part = []
            for p in (q, q + 1):
                code = codes(p)
                rows = [gat[pl.ds(GRP * PITCH * p + j, GRP, stride=PITCH), :]
                        for j in range(HALF if load else 0, FULL if bwd else HALF)]
                real = gsub < (code & 15)
                gate = gate_column(code)
                g_ref[GRP * p:GRP * (p + 1), :] = gate
                us, dys = ([], rows) if load else (rows[:HALF], rows[HALF:])
                part.append([jnp.where(real, v, 0.0) for v in us] + [v * gate for v in dys])
            at = slice(GRP * q, GRP * (q + 2))
            for x, o in ((None if load else of(x_u, t), 0), (x_c, 0 if load else HALF)):
                if x is None:
                    continue
                for j, (c, w) in enumerate(cols):
                    both = jnp.concatenate([part[0][o + j], part[1][o + j]], axis=0)
                    x[at, c:c + w] = both[:, :w].astype(BF16)

    def put_rows(o, value, s0):
        value = value.astype(BF16).astype(F32)
        n = value.shape[0]
        for j, (c, w) in enumerate(cols):
            row_ref[pl.ds(PITCH * s0 + o + j, n, stride=PITCH), 0:w] = value[:, c:c + w] * g_ref[s0:s0 + n, 0:w]

    low = lax.broadcasted_iota(I32, (16, 2 * hi), 1) < hi

    def middle(a, b, dh):
        sig = 0.5 * jnp.tanh(0.5 * a) + 0.5
        act = a * sig
        h = act * b
        if dh is None:
            return h, None, None
        slope = sig * (1.0 + a * (1.0 - sig))
        return h, dh * b * slope, dh * act

    def weights(e, slot):
        at = (layer, tab_ref[ROW_EXPERT * LANES + e])
        moves = []
        for i, w in enumerate((wg_hbm, wu_hbm)):
            moves.append((w.at[at + (pl.ds(0, lo),)], gu_ref.at[slot, pl.ds(i * lo, lo)]))
            moves.append((w.at[at + (pl.ds(lo, hi),)], gu_ref.at[slot, pl.ds(2 * lo + i * hi, hi)]))
        moves.append((wd_hbm.at[at], wd_ref.at[slot]))
        return [copy(a, b, w_sem.at[slot, i]) for i, (a, b) in enumerate(moves)]

    def sums_in(e, slot):
        return copy(prev.at[e], sums.at[slot], sum_sem.at[slot])

    def sums_out(e, slot):
        return copy(sums.at[slot], grad.at[e], sum_sem.at[slot])

    def keeps(e, slot):
        at = (layer, tab_ref[ROW_EXPERT * LANES + e])
        return [copy(keep_buf.at[slot, i], finals[i].at[at], keep_sem.at[slot, i]) for i in range(3)]

    def send(e, slot, part):
        return copy(keep_buf.at[slot], sent[part].at[e - part * split], keep_sem.at[slot, 3])

    def read(e, slot, part=0):
        return copy(got[part].at[e - part * split], got_buf.at[slot], read_sem.at[slot])

    def writes(e, slot):
        to = tab_ref[TAB_ROWS * LANES + e]
        return [copy(got_buf.at[slot, i], finals[i].at[got_layer, to], write_sem.at[slot, i]) for i in range(3)]

    def start(moves):
        for m in moves:
            m.start()

    def wait(moves):
        for m in moves:
            m.wait()

    n_tab = TAB_ROWS * LANES
    lists = [copy(tab_hbm.at[pl.ds(row_id * n_tab, n_tab)], tab_ref.at[pl.ds(0, n_tab)], list_sem.at[0]),
             copy(idx_hbm.at[pl.ds(row_id * N_SRC * list_len, N_SRC * list_len)], idx.at[pl.ds(0, N_SRC * list_len)],
                  list_sem.at[1]),
             copy(gate_hbm.at[pl.ds(row_id * gate_ref.shape[0], gate_ref.shape[0])], gate_ref, list_sem.at[2])]
    if got is not None:
        at = (got_layer * TAB_ROWS + ROW_PARTNER) * LANES
        lists.append(copy(tab_hbm.at[pl.ds(at, LANES)], tab_ref.at[pl.ds(n_tab, LANES)], list_sem.at[3]))
    start(lists)
    pieces = []
    for s in range(N_SRC):
        if not load:
            pieces.append((u_pieces[s], picks[0][s], s, 0, fwd))
        if bwd:
            pieces.append((dy_pieces[s], picks[1][s], s, HALF, own))
    lands = [copy(ref.at[pick], land.at[i % N_SRC], land_sem.at[i % N_SRC]) for i, (ref, pick, *_) in enumerate(pieces)]
    start(lands[:N_SRC])
    lists[0].wait()
    for e in range(DEPTH - 1):
        start(weights(e, e))
        if bwd and not own:
            sums_in(e, e).start()
    if got is not None:
        lists[3].wait()
        read(0, 0).start()
    if own:
        def clear(c, _):
            for k in range(4):
                acc[pl.ds(al(c * 1152 + 288 * k, 8), 288), :] = jnp.zeros((288, LANES), F32)
            return 0

        lax.fori_loop(0, acc.shape[0] // 1152, clear, 0)
        row_ref[...] = jnp.zeros(row_ref.shape, F32)
    rows = 256
    for i, (_, _, s, o, seed) in enumerate(pieces):
        lands[i].wait()

        def fill(c, _, i=i, o=o, seed=seed, s=s):
            r = al(c * rows, rows)
            for j in range(HALF):
                vals = land[i % N_SRC, pl.ds(r, rows), LANES * j:LANES * (j + 1)].astype(F32)
                to = pl.ds(PITCH * (s * n_blk + r) + o + j, rows, stride=PITCH)
                table[to, :] = vals
                if seed and s == 0:
                    acc[to, :] = vals
            return 0

        lax.fori_loop(0, n_blk // rows, fill, 0)
        if i + N_SRC < len(pieces):
            lands[i + N_SRC].start()
    wait(lists[1:3])
    for k in range(GRP):
        idx[N_SRC * list_len + k] = 0

    def first(q, _):
        gather(begin, 2 * q)
        gather(begin, 2 * q + 1)
        return 0

    begin = codes_of(0)
    lax.fori_loop(0, PER_TILE // 2, first, 0)
    convert(begin, 0)
    if save:
        keep_xu(0).start()
    if load:
        keep_ab(0).start()
        keep_xu(0).start()

    def expert(e, _):
        slot = e & 1
        deep = lax.rem(e, DEPTH)
        sum_slot = slot if own else deep
        wait(weights(e, deep))
        if bwd and not own:
            sums_in(e, deep).wait()
        if got is not None:
            read(0, slot).wait()
            start(writes(e, slot))

            @pl.when((e > 0) & (e < n_exp - 1))
            def _():
                wait(writes(e - 1, 1 - slot))

        @pl.when(e < n_exp - (DEPTH - 1))
        def _():
            ahead = lax.rem(e + DEPTH - 1, DEPTH)
            start(weights(e + DEPTH - 1, ahead))
            if bwd and not own:
                sums_in(e + DEPTH - 1, ahead).start()

        @pl.when(e < n_exp - 1)
        def _():
            if got is not None:
                for part in range(2):
                    @pl.when((e + 1 >= split) if part else (e + 1 < split))
                    def _(part=part):
                        read(e + 1, 1 - slot, part).start()

        if bwd and own:
            @pl.when(e > 1)
            def _():
                sums_out(e - 2, slot).wait()

            sums[slot] = jnp.zeros(sums.shape[1:], F32)

        def tile(t, _):
            if save:
                @pl.when(t > 1)
                def _():
                    keep_ab(t - 2).wait()

                @pl.when(t > 0)
                def _():
                    keep_xu(t - 1).wait()
            if load:
                keep_ab(t).wait()
                keep_xu(t).wait()
                keep_ab(t + 1).start()
                keep_xu(t + 1).start()
            ab, xu = of(ab_ref, t), of(x_u, t)
            before, after = codes_of(jnp.maximum(t - 1, 0)), codes_of(t + 1)
            for q in range(PER_TILE):
                if own:
                    scatter(before, q)
                gather(after, q)
            front = ROWS if own and bwd else ROWS // 2
            for s0 in range(0, ROWS, front):
                sl = slice(s0, s0 + front)
                if not load:
                    ab[sl, :] = dot(xu[sl, :], gu_ref[deep], nt)
                if bwd:
                    dh_ref[sl, :] = dot(x_c[sl, :], wd_ref[deep], nt)
            for r in range(0, ROWS, 16):
                rows = slice(r, r + 16)
                for c in range(0, lo, LANES):
                    h, da, db = middle(ab[rows, c:c + LANES], ab[rows, lo + c:lo + c + LANES],
                                       dh_ref[rows, c:c + LANES] if bwd else None)
                    h_ref[rows, c:c + LANES] = h.astype(BF16)
                    if bwd:
                        dab_ref[rows, c:c + LANES] = da.astype(BF16)
                        dab_ref[rows, lo + c:lo + c + LANES] = db.astype(BF16)
                a = ab[rows, 2 * lo:]
                b = pltpu.roll(a, hi, 1)
                dh = dh_ref[rows, lo:] if bwd else None
                if bwd:
                    dh = jnp.concatenate([dh, dh], axis=1)
                h, da, db = middle(a, b, dh)
                h_ref[rows, lo:] = h[:, :hi].astype(BF16)
                if bwd:
                    dab_ref[rows, 2 * lo:] = jnp.where(low, da, pltpu.roll(db, hi, 1)).astype(BF16)
            half = ROWS // 2
            for s0 in range(0, ROWS, half):
                sl = slice(s0, s0 + half)
                if fwd:
                    put_rows(0, dot(h_ref[sl, :], wd_ref[deep], nn), s0)
                if bwd and own:
                    put_rows(HALF, dot(dab_ref[sl, :], gu_ref[deep], nn), s0)
            if bwd:
                view = sums.at[sum_slot]
                view[0:2 * ff, :] += dot(dab_ref[...], xu[...], tn)
                view[2 * ff:, :] += dot(h_ref[...], x_c[...], tn)
            convert(after, t + 1)
            if save:
                keep_ab(t).start()
                keep_xu(t + 1).start()
            return 0

        lax.fori_loop(tab_ref[ROW_BOUND * LANES + e], tab_ref[ROW_BOUND * LANES + e + 1], tile, 0)
        if bwd and own:
            sums_out(e, slot).start()
        if bwd and not own:
            @pl.when(e > 1)
            def _():
                wait(keeps(e - 2, slot) + [send(0, slot, 0)])

            for i in range(2):
                keep_buf[slot, i, 0:lo, :] = sums[deep, i * lo:(i + 1) * lo, :].astype(BF16)
                keep_buf[slot, i, lo:, :] = sums[deep, 2 * lo + i * hi:2 * lo + (i + 1) * hi, :].astype(BF16)
            keep_buf[slot, 2] = sums[deep, 2 * ff:, :].astype(BF16)
            start(keeps(e, slot))
            for part in range(2):
                @pl.when((e >= split) if part else (e < split))
                def _(part=part):
                    send(e, slot, part).start()
        return 0

    lax.fori_loop(0, n_exp, expert, 0)
    ends = ((n_exp - 2, (n_exp - 2) % 2), (n_exp - 1, (n_exp - 1) % 2))
    n_tiles = tab_ref[ROW_BOUND * LANES + n_exp]
    if save:
        wait([keep_ab(n_tiles - 2), keep_ab(n_tiles - 1), keep_xu(n_tiles - 1)])
    if save or load:
        keep_xu(n_tiles).wait()
    if load:
        keep_ab(n_tiles).wait()
    if own:
        end = codes_of(tab_ref[ROW_BOUND * LANES + n_exp] - 1)
        lax.fori_loop(0, PER_TILE, lambda q, _: (scatter(end, q), 0)[1], 0)
        flights = {}
        for o, out in ((HALF, du_outs), (0, y_outs)):
            for s in range(N_SRC if out else 0):
                wide = s == 0 or p_f32
                stage = stage_f.at[s] if wide else land.at[s]
                if s in flights:
                    flights[s].wait()

                def fetch(c, _, stage=stage, s=s, o=o):
                    r = al(c * rows, rows)
                    for j in range(HALF):
                        at = pl.ds(PITCH * (s * n_blk + r) + o + j, rows, stride=PITCH)
                        stage[pl.ds(r, rows), LANES * j:LANES * (j + 1)] = acc[at, :].astype(stage.dtype)
                    return 0

                lax.fori_loop(0, n_blk // rows, fetch, 0)
                flights[s] = copy(stage, out[s], out_sem.at[s])
                flights[s].start()
        wait(flights.values())
        if bwd:
            for e, slot in ends:
                sums_out(e, slot).wait()
    else:
        for e, slot in ends:
            wait(keeps(e, slot) + [send(0, slot, 0)])
    if got is not None:
        for e, slot in ends:
            wait(writes(e, slot))


def run_experts(routes, layer, u, dy, weights, prev, finals, fwd, own, p_f32=False, got=None, kept=None):
    tab, idx, gates = routes
    bwd = dy is not None
    wg, wu, wd = weights
    save, load = fwd and not bwd, kept is not None
    n_blk, wide = (dy or u)[0][0].shape[-2:]
    n_layers, n_local, ff, d = wd.shape
    n_exp = n_local // 2
    row_id = layer
    list_len = idx.shape[0] // (n_layers * N_SRC)

    arrays = lambda pieces: [v for v, _ in pieces]
    operands = [tab, idx, gates] + ([] if load else arrays(u)) + (arrays(dy) if bwd else []) + [wg, wu, wd] + list(kept or ())
    out_shape, aliases = [], {}
    for use in (fwd, bwd and own):
        if use:
            out_shape += [jax.ShapeDtypeStruct((n_blk, wide), F32 if s == 0 or p_f32 else BF16) for s in range(N_SRC)]
    if bwd and own:
        out_shape.append(jax.ShapeDtypeStruct((n_exp, 3 * ff, d), F32))
    if bwd and not own:
        operands.append(prev)
    if got is not None:
        operands += got
    for i, f in enumerate(finals or ()):
        aliases[len(operands)] = len(out_shape) + i
        operands.append(f)
    if bwd and not own or finals:
        out_shape += [jax.ShapeDtypeStruct((n_layers, n_local, ff, d), BF16)] * 3
    if bwd and not own:
        out_shape += [jax.ShapeDtypeStruct((n, 3, ff, d), BF16) for n in (first_piece(n_exp), n_exp - first_piece(n_exp))]
    if save:
        most = n_exp * (SLOT_GROUPS // PER_TILE) + 2
        out_shape += [jax.ShapeDtypeStruct((most, ROWS, 2 * ff), F32), jax.ShapeDtypeStruct((most, ROWS, d), BF16)]
    sem = lambda *s: pltpu.SemaphoreType.DMA(s)
    mid = lambda n, dt: pltpu.VMEM((ROWS, n), dt)
    twin = lambda n, dt: pltpu.VMEM((2, ROWS, n), dt) if save or load else mid(n, dt)
    table, rows = pltpu.VMEM((PITCH * N_SRC * n_blk, LANES), F32), pltpu.VMEM((PITCH * ROWS, LANES), F32)
    scratch = [pltpu.SMEM(((TAB_ROWS + 1) * LANES,), I32), pltpu.SMEM((N_SRC * list_len + LANES,), I32),
               pltpu.VMEM((N_SRC * list_len // LANES + 8, LANES), F32), pltpu.VMEM((N_SRC, n_blk, wide), BF16)]
    scratch += [table, rows] * (1 + own)
    scratch += [pltpu.VMEM((DEPTH, 2 * ff, d), BF16), pltpu.VMEM((DEPTH, ff, d), BF16), mid(LANES, F32)]
    scratch += [twin(d, BF16)] + [mid(d, BF16)] * bwd + [twin(2 * ff, F32)] + [mid(ff, F32)] * bwd + [mid(ff, BF16)]
    scratch += [mid(2 * ff, BF16), pltpu.VMEM((2 if own else DEPTH, 3 * ff, d), F32)] * bwd
    if bwd and not own:
        scratch.append(pltpu.VMEM((2, 3, ff, d), BF16))
    if got is not None:
        scratch.append(pltpu.VMEM((2, 3, ff, d), BF16))
    scratch += [sem(4), sem(N_SRC), sem(DEPTH, 5)] + [sem(DEPTH)] * bwd
    if bwd and not own:
        scratch.append(sem(2, 4))
    if got is not None:
        scratch += [sem(2), sem(2, 3)]
    if own:
        scratch += [pltpu.VMEM((N_SRC if p_f32 else 1, n_blk, wide), F32), sem(N_SRC)]
    if save or load:
        scratch += [sem(2), sem(2)]
    passes = 2 + fwd + bwd * (4 + 2 * own)
    flops = 2 * d * ff * passes * n_blk * N_SRC * 2
    hoist = 1300 if not own else 640 if load else 750 if save else 950
    picks = [[i for _, i in u] if u else None, [i for _, i in dy] if bwd else None]
    cfg = (fwd, bwd, own, layer, n_blk, d, ff, n_exp, picks, row_id, list_len, p_f32, len(aliases),
           None if got is None else 1 - layer)
    return pl.pallas_call(
        functools.partial(expert_kernel, cfg),
        out_shape=out_shape,
        in_specs=[any_space] * len(operands),
        out_specs=[any_space] * len(out_shape),
        scratch_shapes=scratch,
        input_output_aliases=aliases,
        compiler_params=pltpu.CompilerParams(
            vmem_limit_bytes=VMEM_LIMIT),
        cost_estimate=pl.CostEstimate(flops=flops, bytes_accessed=3 * 2 * n_exp * d * ff, transcendentals=0),
        name=f"experts_{'f' if fwd else ''}{'b' if bwd else ''}_{'own' if own else 'other'}_{layer}",
    )(*operands)


def place_kernel(layer, n_exp, at, tab_hbm, got_ref, *refs):
    outs, (tab_ref, buf, tab_sem, in_sem, out_sem) = refs[3:6], refs[6:]
    table = pltpu.make_async_copy(tab_hbm.at[pl.ds((layer * TAB_ROWS + ROW_PARTNER) * LANES, LANES)], tab_ref, tab_sem)
    table.start()
    reads = [pltpu.make_async_copy(got_ref.at[i], buf.at[i], in_sem.at[i]) for i in range(n_exp)]
    for read in reads:
        read.start()
    writes = []
    table.wait()
    for i, read in enumerate(reads):
        read.wait()
        e = tab_ref[at + i]
        for k, out in enumerate(outs):
            writes.append(pltpu.make_async_copy(buf.at[i, k], out.at[layer, e], out_sem.at[i, k]))
            writes[-1].start()
    for write in writes:
        write.wait()


def place(tab, at, layer, got, finals):
    n_exp = got.shape[0]
    return pl.pallas_call(
        functools.partial(place_kernel, layer, n_exp, at),
        out_shape=[jax.ShapeDtypeStruct(f.shape, f.dtype) for f in finals],
        in_specs=[any_space] * 5, out_specs=[any_space] * 3,
        scratch_shapes=[pltpu.SMEM((LANES,), I32), pltpu.VMEM(got.shape, got.dtype), pltpu.SemaphoreType.DMA,
                        pltpu.SemaphoreType.DMA((n_exp,)), pltpu.SemaphoreType.DMA((n_exp, 3))],
        input_output_aliases={2: 0, 3: 1, 4: 2},
        compiler_params=pltpu.CompilerParams(vmem_limit_bytes=VMEM_LIMIT),
        cost_estimate=pl.CostEstimate(flops=0, bytes_accessed=4 * got.size, transcendentals=0),
        name=f"place_{layer}",
    )(tab, got, *finals)


def peer(rel):
    return {name: (lax.axis_index(name) + ((rel >> bit) & 1)) % 2 for bit, name in enumerate(("ep", "core", "x"))}


def meet(rels):
    barrier = pltpu.get_barrier_semaphore()
    for rel in rels:
        pl.semaphore_signal(barrier, inc=1, device_id=peer(rel), device_id_type=MESH)
    pl.semaphore_wait(barrier, len(rels))


def remote(src, dst, send, recv, rel):
    return pltpu.make_async_remote_copy(src_ref=src, dst_ref=dst, send_sem=send, recv_sem=recv,
                                        device_id=peer(rel), device_id_type=MESH)


def share_kernel(mine_ref, all_ref, send_sem, recv_sem):
    meet((Y, CORE))
    direct = [remote(mine_ref, all_ref.at[rel], send_sem.at[rel], recv_sem.at[rel], rel) for rel in (Y, CORE)]
    for copy in direct:
        copy.start()
    all_ref[0] = mine_ref[...]
    on = remote(all_ref.at[Y], all_ref.at[Y + CORE], send_sem.at[Y + CORE], recv_sem.at[Y + CORE], CORE)
    direct[0].wait_recv()
    on.start()
    direct[0].wait_send()
    direct[1].wait()
    on.wait()


def share(mine, n_rel):
    return pl.pallas_call(
        share_kernel,
        out_shape=jax.ShapeDtypeStruct((n_rel,) + mine.shape, mine.dtype),
        in_specs=[in_vmem],
        out_specs=in_vmem,
        scratch_shapes=[pltpu.SemaphoreType.DMA((n_rel,)), pltpu.SemaphoreType.DMA((n_rel,))],
        compiler_params=pltpu.CompilerParams(collective_id=0, has_side_effects=True),
        cost_estimate=pl.CostEstimate(flops=10 ** 7, bytes_accessed=mine.size * 4 * n_rel, transcendentals=0),
        name="share_lists",
    )(mine)


def blocks_kernel(cfg, *refs):
    n_chunk, reduce, back, d, sizes = cfg
    refs = list(refs)
    take = lambda n: [refs.pop(0) for _ in range(n)]
    parts = take(N_SRC)
    m_ref = take(1)[0]
    list_refs, left_ref = take(2) if sizes else (), take(1)[0] if back else None
    o_total, o_a, o_b = take(3)
    plan_refs, grad_ref = take(3) if sizes else (), take(1)[0] if back else None
    in_f, in_b, got_f, s_wire, r_wire, u_wire, y_wire, t_buf, u_buf, y_buf, load, send, recv, put = take(14)
    n_rows = t_buf.shape[0] // n_chunk
    cut = [pl.ds(k * n_rows, n_rows) for k in range(n_chunk)]
    thin = [pl.ds(k * n_rows // 2, n_rows // 2) for k in range(n_chunk)]
    side = lax.broadcasted_iota(I32, (n_rows // 2, LANES), 1) < LANES // 2
    tiles = d // LANES
    turn = lambda v: pltpu.roll(v, LANES // 2, 1)
    lanes = lambda v, j: v[:, LANES * j:LANES * (j + 1)]

    def pack(wire, k, value):
        top, low = value[:n_rows // 2], value[n_rows // 2:]
        turned = [turn(lanes(low, j)) for j in range(tiles + 1)]
        parts = [lanes(top, j) for j in range(tiles)] + [jnp.where(side, lanes(top, tiles), turned[0])]
        parts += [jnp.where(side, turned[j], turned[j + 1]) for j in range(tiles)]
        for j, part in enumerate(parts):
            wire[thin[k], LANES * j:LANES * (j + 1)] = part.astype(BF16)

    def unpack(wire, k):
        value = wire[thin[k], :].astype(F32)
        turned = [turn(lanes(value, tiles + j)) for j in range(tiles + 1)]
        top = [lanes(value, j) for j in range(tiles)] + [jnp.where(side, lanes(value, tiles), 0.0)]
        low = [jnp.where(side, turned[j], turned[j + 1]) for j in range(tiles)] + [jnp.where(side, turned[tiles], 0.0)]
        return jnp.concatenate([jnp.concatenate(top, axis=1), jnp.concatenate(low, axis=1)], axis=0)

    chunks = range(n_chunk)
    loads = {}
    for i, part in enumerate(parts[:2] if reduce else parts):
        buf = in_f.at[i] if reduce or i == 0 else in_b.at[i - 1]
        for k in chunks:
            loads[i, k] = pltpu.make_async_copy(part.at[cut[k]], buf.at[cut[k]], load.at[i, k])
    order = (1, 0) if reduce else range(N_SRC)
    for i in order:
        for k in chunks:
            loads[i, k].start()
    u_buf[...] = jnp.zeros(u_buf.shape, BF16)
    meet((Y, CORE))
    links = []
    copy_in = pltpu.make_async_copy

    def link(src, dst, rel, cut=cut):
        n = len(links)
        links.append([remote(src.at[cut[k]], dst.at[cut[k]], send.at[n, k], recv.at[n, k], rel) for k in chunks])
        return links[-1]

    if reduce:
        first = link(parts[3], got_f.at[1], CORE)
        second = link(parts[2], got_f.at[0], CORE)
        over = link(s_wire, r_wire, Y, thin)
        for copies in (first, second):
            for copy in copies:
                copy.start()
        for k in chunks:
            loads[1, k].wait()
            first[k].wait_recv()
            pack(s_wire, k, in_f[1, cut[k], :] + got_f[1, cut[k], :])
            over[k].start()
    to_y = link(u_wire, y_wire, Y, thin)
    to_core = link(u_buf, o_b.at[0], CORE)
    puts = []
    for k in chunks:
        if reduce:
            loads[0, k].wait()
            second[k].wait_recv()
            over[k].wait_recv()
            total = in_f[0, cut[k], :] + got_f[0, cut[k], :] + unpack(r_wire, k)
        else:
            for i in range(N_SRC):
                loads[i, k].wait()
            total = in_f[0, cut[k], :]
            for i in range(N_SRC - 1):
                total = total + in_b[i, cut[k], :].astype(F32)
        total = total.astype(BF16)
        t_buf[cut[k], :] = total
        dims = (((1,), (1 if back else 0,)), ((), ()))
        mixed = lax.dot_general(total[:, :d], m_ref[...], dims, preferred_element_type=F32)
        u_buf[cut[k], 0:d] = (total[:, :d].astype(F32) + mixed).astype(BF16)
        pack(u_wire, k, u_buf[cut[k], :].astype(F32))
        to_y[k].start()
        to_core[k].start()
        puts.append(pltpu.make_async_copy(u_buf.at[cut[k]], o_a.at[0, cut[k]], put.at[0, k]))
        puts.append(pltpu.make_async_copy(t_buf.at[cut[k]], o_total.at[cut[k]], put.at[1, k]))
        for copy in puts[-2:]:
            copy.start()
    if sizes:
        plan_kernel(*sizes, *list_refs, *plan_refs)
    if back:
        grad_ref[...] = lax.dot_general(left_ref[:, :d], t_buf[:, :d], (((0,), (0,)), ((), ())), preferred_element_type=F32)
    on = link(y_buf, o_b.at[1], CORE)
    for k in chunks:
        to_y[k].wait_recv()
        y_buf[cut[k], :] = unpack(y_wire, k).astype(BF16)
        on[k].start()
        puts.append(copy_in(y_buf.at[cut[k]], o_a.at[1, cut[k]], put.at[2, k]))
        puts[-1].start()
    waited = [to_y] + ([first, second, over] if reduce else [])
    for copies in links:
        for copy in copies:
            if any(copies is w for w in waited):
                copy.wait_send()
            else:
                copy.wait()
    for copy in puts:
        copy.wait()


def complete_blocks(parts, m, reduce, back, ident, sizes=None, lists=(), left=(), n_chunk=4):
    n_blk, wide = parts[0].shape
    d = m.shape[0]
    sem = lambda *s: pltpu.SemaphoreType.DMA(s)
    pair = jax.ShapeDtypeStruct((2, n_blk, wide), BF16)
    extra = plan_shapes(sizes) if sizes else []
    extra += [jax.ShapeDtypeStruct((d, d), F32)] * len(left)
    buf = lambda n, dt: pltpu.VMEM((n, n_blk, wide) if n else (n_blk, wide), dt)
    return pl.pallas_call(
        functools.partial(blocks_kernel, (n_chunk, reduce, back, d, sizes)),
        out_shape=[jax.ShapeDtypeStruct((n_blk, wide), BF16)] + [pair] * 2 + extra,
        in_specs=[any_space] * N_SRC + [in_vmem] * (1 + len(lists) + len(left)),
        out_specs=[any_space] * 3 + [in_vmem] * len(extra),
        scratch_shapes=[buf(2, F32), buf(3, BF16), buf(2, F32)] + [pltpu.VMEM((n_blk // 2, 2 * d), BF16)] * 4 + [
            buf(0, BF16), buf(0, BF16), buf(0, BF16), sem(4, n_chunk), sem(6, n_chunk), sem(6, n_chunk), sem(3, n_chunk)],
        compiler_params=pltpu.CompilerParams(collective_id=ident, has_side_effects=True, vmem_limit_bytes=VMEM_LIMIT),
        cost_estimate=pl.CostEstimate(flops=10 ** 8, bytes_accessed=n_blk * wide * 40, transcendentals=0),
        name=f"complete_blocks_{ident}",
    )(*parts, m, *lists, *left)


def solution(mesh):
    ep_size, dp_size = mesh.shape['ep'], mesh.shape['dp']
    sub = Mesh(mesh.devices.reshape(ep_size, dp_size // 2, 2), ('ep', 'x', 'core'))
    tok_axes = ('x', 'core', 'ep')
    tok_spec = P(tok_axes, None)
    route_spec = P(None, tok_axes, None)
    whole_spec = P(None, None, None)
    expert_spec = P(None, 'ep', None, None)
    flip = [(0, 1), (1, 0)]
    move = lambda v, axis: lax.ppermute(v, axis, flip)
    move_diag = lambda v: lax.ppermute(v, ('ep', 'core'), [(0, 3), (1, 2), (2, 1), (3, 0)])
    fence = lax.optimization_barrier

    def device_step(tokens, d_out, expert_ids, gate_vals, w_mix, w_gate, w_up, w_down):
        n_layers, d = w_mix.shape[0], w_mix.shape[1]
        n_tok = tokens.shape[0]
        top = expert_ids.shape[2]
        n_local = w_gate.shape[1]
        n_exp = n_local * ep_size
        n = n_tok * top
        n_rel = 2 * N_SRC
        wide = cdiv(d, LANES) * LANES
        weights = (jnp.swapaxes(w_gate, 2, 3), jnp.swapaxes(w_up, 2, 3), w_down)
        pad = lambda v: jnp.pad(v, ((0, 0), (0, wide - d)))
        send_three = lambda p: [move(p[1], 'ep'), move(p[2], 'core'), move_diag(p[3])]

        def own_sum(p, got):
            return sum([g.astype(F32) for g in got], p)[:, :d].astype(BF16)

        one = lambda v: v.reshape(1, n_tok, wide)
        pairs = lambda a, b: [(a, 0), (a, 1), (b, 0), (b, 1)]

        one = lambda v: v.reshape(1, n_tok, wide)
        pairs = lambda a, b: [(a, 0), (a, 1), (b, 0), (b, 1)]
        singles = lambda *v: [(one(a), 0) for a in v]

        same = jnp.eye(d, dtype=BF16)
        u0 = (jnp.dot(tokens, pad(same), preferred_element_type=F32)
              + jnp.dot(tokens, pad(w_mix[0]), preferred_element_type=F32)).astype(BF16)
        u0_y = move(u0, 'ep')
        lists = [sorted_list(expert_ids[l], gate_vals[l]) for l in range(n_layers)]
        counts = jnp.sum((expert_ids.transpose(0, 2, 1).reshape(n_layers, n, 1) == jnp.arange(n_exp, dtype=I32)).astype(F32), axis=1)
        packed = jnp.concatenate([jnp.concatenate([v[0] for v in lists] + [v[1] for v in lists]).reshape(-1, LANES),
                                  jnp.pad(counts, ((0, 8 - n_layers), (0, LANES - n_exp)))], axis=0)
        dy = pad(d_out)
        packed, dy, u0_late = fence((packed, dy, u0))
        u0_c = move(u0_late, 'core')
        shared = share(packed, N_SRC)
        u0_y, u0_c, dy, shared, w_mix = fence((u0_y, u0_c, dy, shared, w_mix))
        u0_d = move(u0_y, 'core')
        shared_x = move(shared, 'x')
        dy_y, dy_x = move(dy, 'ep'), move(dy, 'x')
        sizes = (n_layers, n_local, n_tok, n // LANES)
        routes = plan(shared, shared, sizes)
        u0_half = singles(u0, u0_y, u0_c, u0_d)
        add = lambda a, b: a.astype(F32) + b.astype(F32)
        to_chips = lambda v: [move(v, 'ep'), move(v, 'x'), lax.ppermute(v, ('ep', 'x'), [(0, 3), (1, 2), (2, 1), (3, 0)])]
        of_chips = lambda v, t: (add(v, t[0]) + add(t[1], t[2])).astype(BF16)
        piece = first_piece(n_local // 2)
        *part, ab0, xu0 = run_experts(routes, 0, u0_half, None, weights, None, None, True, True, p_f32=True)
        dy_y, dy_x, shared_x, part = fence((dy_y, dy_x, shared_x, part))
        dy_c, dy_d, dy_xy, dy_xc = move(dy, 'core'), move(dy_y, 'core'), move(dy_y, 'x'), move(dy_x, 'core')
        y0, u1_a, u1_b, *routes_x = complete_blocks(part, w_mix[1], True, False, 1, sizes, (shared, shared_x))
        routes_x = flat(*routes_x)
        dy_c, dy_d, dy_xy, dy_xc, u0_p, u0_q, y0, u1_a, u1_b = fence(
            (dy_c, dy_d, dy_xy, dy_xc, u0, u0_y, y0, u1_a, u1_b))
        dy_xd = move(dy_xy, 'core')
        u1_xa = move(u1_a, 'x')
        out = run_experts(routes, 1, pairs(u1_a, u1_b), singles(dy, dy_y, dy_c, dy_d), weights, None, None, True, True)
        u1_xa, dy_xd, u0_p, u0_q, out = fence((u1_xa, dy_xd, u0_p, u0_q, out))
        y_part, du_part, g1 = out[:4], out[4:8], out[8]
        u1_xb = move(u1_xa, 'core')
        got = send_three(du_part)
        u0_x, u0_xy = move(u0_p, 'x'), move(u0_q, 'x')
        out = run_experts(routes_x, 1, pairs(u1_xa, u1_xb), singles(dy_x, dy_xy, dy_xc, dy_xd), weights, g1, None,
                          False, False)
        got, u0_x, u0_xy, out = fence((got, u0_x, u0_xy, out))
        *finals, sent_a, sent_b = out
        got1 = [move(sent_a, 'core'), move(sent_b, 'core')]
        du1, dx_a, dx_b, g_mix1 = complete_blocks([du_part[0], *got], w_mix[1], False, True, 2, left=(y0,))
        tx = lambda x, du: jnp.einsum('td,te->de', x, du, preferred_element_type=F32)
        dx_a, y_part, got1, u0_x, u0_xy, g_mix1 = fence((dx_a, y_part, got1, u0_x, u0_xy, g_mix1))
        dx_xa = move(dx_a, 'x')
        part1 = g_mix1.astype(BF16)
        theirs1 = to_chips(part1)
        got_y = send_three(y_part)
        u0_xc, u0_xd = move(u0_x, 'core'), move(u0_xy, 'core')
        out = run_experts(routes, 0, None, pairs(dx_a, dx_b), weights, None, finals, False, True, got=got1, kept=(ab0, xu0))
        dx_xa, got_y, u0_xc, u0_xd, theirs1, out = fence((dx_xa, got_y, u0_xc, u0_xd, theirs1, out))
        du_part, g0, finals = out[:4], out[4], out[5:]
        dx_xb = move(dx_xa, 'core')
        got = send_three(du_part)
        part1 = of_chips(part1, theirs1)
        theirs1 = move(part1, 'core')
        du_part, dx_xb, part1 = fence((du_part, dx_xb, part1))
        out = run_experts(routes_x, 0, singles(u0_x, u0_xy, u0_xc, u0_xd), pairs(dx_xa, dx_xb), weights, g0, finals,
                          False, False)
        got, theirs1, got_y, y_own, out = fence((got, theirs1, got_y, y_part[0], out))
        *finals, sent_a, sent_b = out
        got_a, got_b = move(sent_a, 'core'), move(sent_b, 'core')
        du0 = own_sum(du_part[0], got)
        part0 = tx(tokens, du0).astype(BF16)
        theirs0 = to_chips(part0)
        turned = lambda v, w: jnp.einsum('te,de->dt', v, w, preferred_element_type=F32)
        dx0 = (turned(du0, same) + turned(du0, w_mix[0])).astype(BF16)
        y1 = turned(own_sum(y_own, got_y), same).astype(BF16)
        dx0, y1, got_a, finals = fence((dx0, y1, got_a, finals))
        finals = place(routes[0], 0, 0, got_a, finals)
        dx0, got_b, finals = fence((dx0, got_b, finals))
        finals = place(routes[0], piece, 0, got_b, finals)
        theirs0, finals = fence((theirs0, finals))
        total0 = of_chips(part0, theirs0)
        which = lax.broadcasted_iota(I32, (n_layers, d, d), 0)
        g_mix = jnp.where(which == 0, add(total0, move(total0, 'core'))[None], add(part1, theirs1)[None]).astype(BF16)
        return (y1.T, dx0.T, g_mix, jnp.swapaxes(finals[0], 2, 3), jnp.swapaxes(finals[1], 2, 3), finals[2])

    return jax.shard_map(device_step, mesh=sub,
                         in_specs=(tok_spec, tok_spec, route_spec, route_spec, whole_spec,
                                   expert_spec, expert_spec, expert_spec),
                         out_specs=(tok_spec, tok_spec, whole_spec, expert_spec, expert_spec, expert_spec),
                         check_vma=False)
```
